32 devices in a mesh: tp: 8 (over z, y), dp: 4 (over x, core).
Axes of the slice: x: 2, y: 2, z: 4, core: 2. Of those that a mesh axis runs over, the one named last changes fastest.
Arguments:
- tokens: int32 [16, 1024], P('dp')
- labels: int32 [16, 1024], P('dp')
- embed: float32 [50304, 512], P('tp')
- ln_scales: float32 [2, 512], replicated
- w_q: float32 [512, 512], P(None, 'tp')
- w_kv: float32 [2, 512, 64], replicated
- w_o: float32 [512, 512], P('tp')
- w_gu: float32 [2, 512, 2048], P(None, None, 'tp')
- w_down: float32 [2048, 512], P('tp')
- m_embed: float32 [50304, 512], P('tp')
- m_ln_scales: float32 [2, 512], replicated
- m_w_q: float32 [512, 512], P(None, 'tp')
- m_w_kv: float32 [2, 512, 64], replicated
- m_w_o: float32 [512, 512], P('tp')
- m_w_gu: float32 [2, 512, 2048], P(None, None, 'tp')
- m_w_down: float32 [2048, 512], P('tp')
- v_embed: float32 [50304, 512], P('tp')
- v_ln_scales: float32 [2, 512], replicated
- v_w_q: float32 [512, 512], P(None, 'tp')
- v_w_kv: float32 [2, 512, 64], replicated
- v_w_o: float32 [512, 512], P('tp')
- v_w_gu: float32 [2, 512, 2048], P(None, None, 'tp')
- v_w_down: float32 [2048, 512], P('tp')
Outputs:
- output 1: float32 [50304, 512], P('tp')
- output 2: float32 [2, 512], replicated
- output 3: float32 [512, 512], P(None, 'tp')
- output 4: float32 [2, 512, 64], replicated
- output 5: float32 [512, 512], P('tp')
- output 6: float32 [2, 512, 2048], P(None, None, 'tp')
- output 7: float32 [2048, 512], P('tp')
- output 8: float32 [50304, 512], P('tp')
- output 9: float32 [2, 512], replicated
- output 10: float32 [512, 512], P(None, 'tp')
- output 11: float32 [2, 512, 64], replicated
- output 12: float32 [512, 512], P('tp')
- output 13: float32 [2, 512, 2048], P(None, None, 'tp')
- output 14: float32 [2048, 512], P('tp')
- output 15: float32 [50304, 512], P('tp')
- output 16: float32 [2, 512], replicated
- output 17: float32 [512, 512], P(None, 'tp')
- output 18: float32 [2, 512, 64], replicated
- output 19: float32 [512, 512], P('tp')
- output 20: float32 [2, 512, 2048], P(None, None, 'tp')
- output 21: float32 [2048, 512], P('tp')
- output 22: float32 [], replicated
All inputs are finite; a program needn't handle non-finite values.
Results may differ from the reference program's by a relative error of at most 0.00961239.
Values sent between devices are 32-bit elements.
A program may use at most 1 GiB of HBM per device.

```python
import jax
import jax.numpy as jnp
from jax import lax

BATCH_ALL = 16
SEQ_LEN = 1024
D_MODEL = 512
N_HEADS = 8
HEAD_DIM = 64
FF_DIM = 2048
VOCAB_SIZE = 50304

LN_EPS = 1e-5
LOGIT_ZLOSS = 1e-4
LEARN_RATE = 1e-2
BETA_ONE = 0.9
BETA_TWO = 0.95
ADAM_EPS = 1e-8
ROPE_BASE = 10000.0


def layer_norm(x_in, scale):
    x_f32 = x_in.astype(jnp.float32)
    centered = x_f32 - jnp.mean(x_f32, axis=-1, keepdims=True)
    variance = jnp.mean(centered * centered, axis=-1, keepdims=True)
    return (centered * lax.rsqrt(variance + LN_EPS) * scale).astype(jnp.bfloat16)


def rope_tables(seq_len, head_dim):
    positions = jnp.arange(seq_len).astype(jnp.float32)
    inv_freq = ROPE_BASE ** (-jnp.arange(0, head_dim, 2).astype(jnp.float32) / head_dim)
    angles = positions[:, None] * inv_freq[None, :]
    return jnp.cos(angles), jnp.sin(angles)


def rotate(x_in, cos_t, sin_t):
    half_dim = x_in.shape[-1] // 2
    x_lo = x_in[..., :half_dim]
    x_hi = x_in[..., half_dim:]
    return jnp.concatenate([x_lo * cos_t - x_hi * sin_t, x_hi * cos_t + x_lo * sin_t], axis=-1)


def adam_update(param_in, grad_in, mom_in, vel_in):
    mom_new = BETA_ONE * mom_in + (1.0 - BETA_ONE) * grad_in
    vel_new = BETA_TWO * vel_in + (1.0 - BETA_TWO) * grad_in * grad_in
    return param_in - LEARN_RATE * mom_new / (jnp.sqrt(vel_new) + ADAM_EPS), mom_new, vel_new


def setup_inputs(seed: int = 0) -> dict:
    keys = jax.random.split(jax.random.key(seed), 24)
    drawn = {}
    drawn['tokens'] = jax.random.randint(keys[0], (BATCH_ALL, SEQ_LEN), 0, VOCAB_SIZE, dtype=jnp.int32)
    drawn['labels'] = jax.random.randint(keys[1], (BATCH_ALL, SEQ_LEN), 0, VOCAB_SIZE, dtype=jnp.int32)
    names = ['embed', 'ln_scales', 'w_q', 'w_kv', 'w_o', 'w_gu', 'w_down']
    params = [
        jax.random.normal(keys[2], (VOCAB_SIZE, D_MODEL), jnp.float32),
        jax.random.uniform(keys[3], (2, D_MODEL), jnp.float32, 0.5, 1.5),
        jax.random.normal(keys[4], (D_MODEL, N_HEADS * HEAD_DIM), jnp.float32) * D_MODEL ** -0.5,
        jax.random.normal(keys[5], (2, D_MODEL, HEAD_DIM), jnp.float32) * D_MODEL ** -0.5,
        jax.random.normal(keys[6], (N_HEADS * HEAD_DIM, D_MODEL), jnp.float32) * (N_HEADS * HEAD_DIM) ** -0.5,
        jax.random.normal(keys[7], (2, D_MODEL, FF_DIM), jnp.float32) * D_MODEL ** -0.5,
        jax.random.normal(keys[8], (FF_DIM, D_MODEL), jnp.float32) * FF_DIM ** -0.5,
    ]
    for index in range(7):
        drawn[names[index]] = params[index]
    grad_scale = (BATCH_ALL * SEQ_LEN * D_MODEL) ** -0.5
    mom_scales = [grad_scale * VOCAB_SIZE ** -0.5, 8.0 / D_MODEL, grad_scale, grad_scale, grad_scale, grad_scale, grad_scale]
    vel_scales = [grad_scale * VOCAB_SIZE ** -0.5, 3.0 / D_MODEL, grad_scale, grad_scale, grad_scale, grad_scale, grad_scale]
    for index in range(7):
        drawn['m_' + names[index]] = mom_scales[index] * jax.random.normal(keys[9 + index], params[index].shape, jnp.float32)
    for index in range(7):
        drawn['v_' + names[index]] = vel_scales[index] * vel_scales[index] * jax.random.uniform(keys[16 + index], params[index].shape, jnp.float32, 0.5, 2.0)
    return drawn


def sequence_loss(param_set, tok_row, lab_row):
    emb_b = param_set[0].astype(jnp.bfloat16)
    ln_scales = param_set[1]
    wq_b = param_set[2].astype(jnp.bfloat16)
    wkv_b = param_set[3].astype(jnp.bfloat16)
    wo_b = param_set[4].astype(jnp.bfloat16)
    wgu_b = param_set[5].astype(jnp.bfloat16)
    wdown_b = param_set[6].astype(jnp.bfloat16)
    x_zero = jnp.take(emb_b, tok_row, axis=0)
    u_norm = layer_norm(x_zero, ln_scales[0])
    q_raw = jnp.dot(u_norm, wq_b, preferred_element_type=jnp.float32).reshape(SEQ_LEN, N_HEADS, HEAD_DIM)
    k_raw = jnp.dot(u_norm, wkv_b[0], preferred_element_type=jnp.float32)
    values = jnp.dot(u_norm, wkv_b[1], preferred_element_type=jnp.float32).astype(jnp.bfloat16)
    cos_t, sin_t = rope_tables(SEQ_LEN, HEAD_DIM)
    queries = rotate(q_raw, cos_t[:, None, :], sin_t[:, None, :]).astype(jnp.bfloat16)
    key_rot = rotate(k_raw, cos_t, sin_t).astype(jnp.bfloat16)
    scores = jnp.einsum('qhe,ke->hqk', queries.astype(jnp.float32), key_rot.astype(jnp.float32)) * HEAD_DIM ** -0.5
    causal = jnp.arange(SEQ_LEN)[:, None] >= jnp.arange(SEQ_LEN)[None, :]
    prob_b16 = jax.nn.softmax(jnp.where(causal, scores, -1e30), axis=-1).astype(jnp.bfloat16)
    context = jnp.einsum('hqk,ke->qhe', prob_b16.astype(jnp.float32), values.astype(jnp.float32)).astype(jnp.bfloat16)
    att_out = jnp.dot(context.reshape(SEQ_LEN, N_HEADS * HEAD_DIM), wo_b, preferred_element_type=jnp.float32)
    gate = jnp.dot(u_norm, wgu_b[0], preferred_element_type=jnp.float32)
    up_val = jnp.dot(u_norm, wgu_b[1], preferred_element_type=jnp.float32)
    hidden = (jax.nn.silu(gate) * up_val).astype(jnp.bfloat16)
    mlp_out = jnp.dot(hidden, wdown_b, preferred_element_type=jnp.float32)
    x_one = x_zero.astype(jnp.float32) + att_out + mlp_out
    f_norm = layer_norm(x_one, ln_scales[1])
    logits = jnp.dot(f_norm, emb_b.T, preferred_element_type=jnp.float32) * D_MODEL ** -0.5
    log_norm = jax.nn.logsumexp(logits, axis=-1)
    lab_logit = jnp.take_along_axis(logits, lab_row[:, None], axis=-1)[:, 0]
    return jnp.sum(log_norm - lab_logit + LOGIT_ZLOSS * log_norm * log_norm)


def reference(tokens, labels, embed, ln_scales, w_q, w_kv, w_o, w_gu, w_down, m_embed, m_ln_scales, m_w_q, m_w_kv, m_w_o, m_w_gu, m_w_down, v_embed, v_ln_scales, v_w_q, v_w_kv, v_w_o, v_w_gu, v_w_down):
    params = (embed, ln_scales, w_q, w_kv, w_o, w_gu, w_down)

    def total_loss(param_set):
        def one_seq(row_pair):
            return sequence_loss(param_set, row_pair[0], row_pair[1])
        per_seq = lax.map(jax.checkpoint(one_seq), (tokens, labels))
        return jnp.sum(per_seq) / (BATCH_ALL * SEQ_LEN)

    loss, gradients = jax.value_and_grad(total_loss)(params)
    new_embed, new_m_embed, new_v_embed = adam_update(embed, gradients[0], m_embed, v_embed)
    new_ln_scales, new_m_ln_scales, new_v_ln_scales = adam_update(ln_scales, gradients[1], m_ln_scales, v_ln_scales)
    new_w_q, new_m_w_q, new_v_w_q = adam_update(w_q, gradients[2], m_w_q, v_w_q)
    new_w_kv, new_m_w_kv, new_v_w_kv = adam_update(w_kv, gradients[3], m_w_kv, v_w_kv)
    new_w_o, new_m_w_o, new_v_w_o = adam_update(w_o, gradients[4], m_w_o, v_w_o)
    new_w_gu, new_m_w_gu, new_v_w_gu = adam_update(w_gu, gradients[5], m_w_gu, v_w_gu)
    new_w_down, new_m_w_down, new_v_w_down = adam_update(w_down, gradients[6], m_w_down, v_w_down)
    return (new_embed, new_ln_scales, new_w_q, new_w_kv, new_w_o, new_w_gu, new_w_down,
            new_m_embed, new_m_ln_scales, new_m_w_q, new_m_w_kv, new_m_w_o, new_m_w_gu, new_m_w_down,
            new_v_embed, new_v_ln_scales, new_v_w_q, new_v_w_kv, new_v_w_o, new_v_w_gu, new_v_w_down,
            loss)
```

```python
import functools

import jax
import jax.numpy as jnp
from jax import lax
from jax.experimental import pallas as pl
from jax.experimental.pallas import tpu as pltpu
from jax.sharding import PartitionSpec as P

LN_EPS = 1e-5
LOGIT_ZLOSS = 1e-4
LEARN_RATE = 1e-2
BETA_ONE = 0.9
BETA_TWO = 0.95
ADAM_EPS = 1e-8
ROPE_BASE = 10000.0
NZ = 4
CAP = 96
F32 = jnp.float32
BF16 = jnp.bfloat16
ANY = pl.BlockSpec(memory_space=pl.ANY)
VMEM = pl.BlockSpec(memory_space=pltpu.VMEM)

ARRIVALS = {
    0: (("R", 1), ("R", 2), ("R", 3)),
    1: (("L", 0), ("R", 2), ("R", 3)),
    2: (("R", 3), ("L", 1), ("L", 0)),
    3: (("L", 2), ("L", 1), ("L", 0)),
}
REDUCE_ORDER = {0: (3, 2, 1, 0), 1: (3, 0, 2, 1), 2: (0, 3, 1, 2), 3: (0, 1, 2, 3)}


def remote(src, dst, send_sem, recv_sem, tp, dp):
    return pltpu.make_async_remote_copy(src_ref=src, dst_ref=dst, send_sem=send_sem, recv_sem=recv_sem,
                                        device_id=(tp, dp), device_id_type=pl.DeviceIdType.MESH)


def place():
    tp = lax.axis_index("tp")
    dp = lax.axis_index("dp")
    return tp, dp, tp // 2, tp % 2


def signal(tp, dp):
    pl.semaphore_signal(pltpu.get_barrier_semaphore(), inc=1, device_id=(tp, dp), device_id_type=pl.DeviceIdType.MESH)


def line_barrier(k, tp, dp, others):
    peers = [(tp + 1 - 2 * (tp % 2), dp)] + others
    if k > 0:
        peers.append((tp - 2, dp))
    if k < NZ - 1:
        peers.append((tp + 2, dp))
    for peer in peers:
        signal(*peer)
    pl.semaphore_wait(pltpu.get_barrier_semaphore(), len(peers))


def gather_kernel(x_ref, out_ref, own_sem, send_y, send_l, send_r, recv):
    tp, dp, z, y = place()
    partner = tp + 1 - 2 * y

    def program(k):
        line_barrier(k, tp, dp, [])

        def send(src, slot, sems, to):
            copy = remote(src, out_ref.at[slot], sems.at[slot], recv.at[slot], to, dp)
            copy.start()
            return copy

        def arrived(slot):
            remote(x_ref, out_ref.at[slot], send_y.at[slot], recv.at[slot], partner, dp).wait_recv()

        sends = []
        if k > 0:
            sends.append(send(x_ref, tp, send_l, tp - 2))
        if k < NZ - 1:
            sends.append(send(x_ref, tp, send_r, tp + 2))
        sends.append(send(x_ref, tp, send_y, partner))
        own = pltpu.make_async_copy(x_ref, out_ref.at[tp], own_sem)
        own.start()
        for side, zz in ARRIVALS[k]:
            slot = 2 * zz + y
            arrived(slot)
            if side == "L" and k < NZ - 1:
                sends.append(send(out_ref.at[slot], slot, send_r, tp + 2))
            if side == "R" and k > 0:
                sends.append(send(out_ref.at[slot], slot, send_l, tp - 2))
            sends.append(send(out_ref.at[slot], slot, send_y, partner))
        for zz in range(NZ):
            arrived(2 * zz + 1 - y)
        own.wait()
        for copy in sends:
            copy.wait_send()

    for k in range(NZ):
        pl.when(z == k)(functools.partial(program, k))


def plane_gather(x, collective_id):
    return pl.pallas_call(
        gather_kernel,
        out_shape=jax.ShapeDtypeStruct((2 * NZ,) + x.shape, x.dtype),
        in_specs=[ANY],
        out_specs=ANY,
        scratch_shapes=[pltpu.SemaphoreType.DMA] + [pltpu.SemaphoreType.DMA((2 * NZ,))] * 4,
        compiler_params=pltpu.CompilerParams(collective_id=collective_id, has_side_effects=True),
        name="plane_gather",
    )(x)


def weight_gather_kernel(x_ref, out_ref, own_sem, send_y, send_l, send_r, send_c, recv):
    tp, dp, z, y = place()
    partner = tp + 1 - 2 * y
    core = dp % 2
    twin = dp + 1 - 2 * core

    def program(k):
        line_barrier(k, tp, dp, [(tp, twin)])

        def send(src, slot, sems, to, to_dp):
            copy = remote(src, out_ref.at[slot, core], sems.at[slot], recv.at[slot, core], to, to_dp)
            copy.start()
            return copy

        def arrived(slot, half):
            remote(x_ref.at[0], out_ref.at[slot, half], send_y.at[slot], recv.at[slot, half], partner, dp).wait_recv()

        mine = x_ref.at[core]
        sends = []
        if k > 0:
            sends.append(send(mine, tp, send_l, tp - 2, dp))
        if k < NZ - 1:
            sends.append(send(mine, tp, send_r, tp + 2, dp))
        sends.append(send(mine, tp, send_y, partner, dp))
        own = pltpu.make_async_copy(x_ref, out_ref.at[tp], own_sem)
        own.start()
        across = [k] + [zz for _, zz in ARRIVALS[k]]
        for n, (side, zz) in enumerate(ARRIVALS[k]):
            slot = 2 * zz + y
            arrived(slot, core)
            if side == "L" and k < NZ - 1:
                sends.append(send(out_ref.at[slot, core], slot, send_r, tp + 2, dp))
            if side == "R" and k > 0:
                sends.append(send(out_ref.at[slot, core], slot, send_l, tp - 2, dp))
            sends.append(send(out_ref.at[slot, core], slot, send_y, partner, dp))
            sends.append(send(out_ref.at[slot, core], slot, send_c, tp, twin))
            slot = 2 * across[n] + 1 - y
            arrived(slot, core)
            sends.append(send(out_ref.at[slot, core], slot, send_c, tp, twin))
        slot = 2 * across[-1] + 1 - y
        arrived(slot, core)
        sends.append(send(out_ref.at[slot, core], slot, send_c, tp, twin))
        for zz in range(NZ):
            if zz != k:
                arrived(2 * zz + y, 1 - core)
            arrived(2 * zz + 1 - y, 1 - core)
        own.wait()
        for copy in sends:
            copy.wait_send()

    for k in range(NZ):
        pl.when(z == k)(functools.partial(program, k))


def weight_gather(x, collective_id):
    rows, width = x.shape
    halves = x.reshape(2, rows // 2, width)
    out = pl.pallas_call(
        weight_gather_kernel,
        out_shape=jax.ShapeDtypeStruct((2 * NZ,) + halves.shape, x.dtype),
        in_specs=[ANY],
        out_specs=ANY,
        scratch_shapes=[pltpu.SemaphoreType.DMA] + [pltpu.SemaphoreType.DMA((2 * NZ,))] * 4
        + [pltpu.SemaphoreType.DMA((2 * NZ, 2))],
        compiler_params=pltpu.CompilerParams(collective_id=collective_id, has_side_effects=True),
        name="weight_gather",
    )(halves)
    return out.reshape(2 * NZ, rows, width)


def add_into(acc, other):
    rows = acc.shape[0]
    step = 64 if rows % 64 == 0 else rows

    def body(n, carry):
        at = pl.ds(pl.multiple_of(n * step, step), step)
        acc[at, :] = acc[at, :] + other[at, :]
        return carry

    lax.fori_loop(0, rows // step, body, 0)


def scatter_kernel(p_ref, out_ref, acc, from_y, from_l, from_r, load_sem, out_sem, send_y, send_l, send_r, recv_y, recv_l, recv_r):
    tp, dp, z, y = place()
    partner = tp + 1 - 2 * y

    def program(k):
        line_barrier(k, tp, dp, [])
        sends = []
        loads = []
        for zz in REDUCE_ORDER[k]:
            copy = remote(p_ref.at[2 * zz + 1 - y], from_y.at[zz], send_y.at[zz], recv_y.at[zz], partner, dp)
            copy.start()
            sends.append(copy)
        for zz in REDUCE_ORDER[k]:
            load = pltpu.make_async_copy(p_ref.at[2 * zz + y], acc.at[zz], load_sem.at[zz])
            load.start()
            loads.append(load)
        for n, zz in enumerate(REDUCE_ORDER[k]):
            loads[n].wait()
            remote(acc.at[zz], from_y.at[zz], send_y.at[zz], recv_y.at[zz], partner, dp).wait_recv()
            add_into(acc.at[zz], from_y.at[zz])
            if zz >= k and k > 0:
                remote(acc.at[zz], from_l.at[zz], send_l.at[zz], recv_l.at[zz], partner, dp).wait_recv()
                add_into(acc.at[zz], from_l.at[zz])
            if zz <= k and k < NZ - 1:
                remote(acc.at[zz], from_r.at[zz], send_r.at[zz], recv_r.at[zz], partner, dp).wait_recv()
                add_into(acc.at[zz], from_r.at[zz])
            if zz > k:
                copy = remote(acc.at[zz], from_l.at[zz], send_r.at[zz], recv_l.at[zz], tp + 2, dp)
                copy.start()
                sends.append(copy)
            if zz < k:
                copy = remote(acc.at[zz], from_r.at[zz], send_l.at[zz], recv_r.at[zz], tp - 2, dp)
                copy.start()
                sends.append(copy)
        out = pltpu.make_async_copy(acc.at[k], out_ref, out_sem)
        out.start()
        out.wait()
        for copy in sends:
            copy.wait_send()

    for k in range(NZ):
        pl.when(z == k)(functools.partial(program, k))


def plane_scatter(p, collective_id):
    _, rows, width = p.shape
    line = (NZ, rows, width)
    return pl.pallas_call(
        scatter_kernel,
        out_shape=jax.ShapeDtypeStruct((rows, width), p.dtype),
        in_specs=[ANY],
        out_specs=ANY,
        scratch_shapes=[pltpu.VMEM(line, p.dtype)] * 4
        + [pltpu.SemaphoreType.DMA((NZ,)), pltpu.SemaphoreType.DMA]
        + [pltpu.SemaphoreType.DMA((NZ,))] * 6,
        compiler_params=pltpu.CompilerParams(collective_id=collective_id, has_side_effects=True),
        name="plane_scatter",
    )(p)


def weight_scatter_kernel(p_ref, out_ref, acc, from_c, from_y, from_l, from_r, from_x, load_sem, out_sem, send_c, send_y, send_l, send_r,
                          last_send, recv_c, recv_y, recv_l, recv_r, last_recv):
    tp, dp, z, y = place()
    partner = tp + 1 - 2 * y
    core = dp % 2
    twin = dp + 1 - 2 * core
    facing = lax.rem(dp + 2, 4)

    def program(k):
        line_barrier(k, tp, dp, [(tp, twin), (tp, facing)])
        sends = []
        for zz in REDUCE_ORDER[k]:
            for slot in (2 * zz + 1 - y, 2 * zz + y):
                copy = remote(p_ref.at[slot, 1 - core], from_c.at[slot], send_c.at[slot], recv_c.at[slot], tp, twin)
                copy.start()
                sends.append(copy)
                pltpu.make_async_copy(p_ref.at[slot, core], acc.at[slot], load_sem.at[slot]).start()

        def chip_sum(slot):
            pltpu.make_async_copy(p_ref.at[slot, core], acc.at[slot], load_sem.at[slot]).wait()
            remote(acc.at[slot], from_c.at[slot], send_c.at[slot], recv_c.at[slot], tp, twin).wait_recv()
            add_into(acc.at[slot], from_c.at[slot])

        for zz in REDUCE_ORDER[k]:
            slot = 2 * zz + 1 - y
            chip_sum(slot)
            copy = remote(acc.at[slot], from_y.at[zz], send_y.at[zz], recv_y.at[zz], partner, dp)
            copy.start()
            sends.append(copy)
        for zz in REDUCE_ORDER[k]:
            chip_sum(2 * zz + y)
        for zz in REDUCE_ORDER[k]:
            slot = 2 * zz + y
            line = acc.at[slot]
            remote(line, from_y.at[zz], send_y.at[zz], recv_y.at[zz], partner, dp).wait_recv()
            add_into(line, from_y.at[zz])
            if zz >= k and k > 0:
                remote(line, from_l.at[zz], send_l.at[zz], recv_l.at[zz], partner, dp).wait_recv()
                add_into(line, from_l.at[zz])
            if zz <= k and k < NZ - 1:
                remote(line, from_r.at[zz], send_r.at[zz], recv_r.at[zz], partner, dp).wait_recv()
                add_into(line, from_r.at[zz])
            if zz > k:
                copy = remote(line, from_l.at[zz], send_r.at[zz], recv_l.at[zz], tp + 2, dp)
                copy.start()
                sends.append(copy)
            if zz < k:
                copy = remote(line, from_r.at[zz], send_l.at[zz], recv_r.at[zz], tp - 2, dp)
                copy.start()
                sends.append(copy)
        total = acc.at[2 * k + y]
        copy = remote(total, from_x, last_send.at[0], last_recv.at[0], tp, facing)
        copy.start()
        copy.wait()
        add_into(total, from_x)
        copy = remote(total, out_ref.at[core], last_send.at[1], last_recv.at[1], tp, twin)
        copy.start()
        out = pltpu.make_async_copy(total, out_ref.at[core], out_sem)
        out.start()
        copy.wait_send()
        remote(total, out_ref.at[1 - core], last_send.at[1], last_recv.at[1], tp, twin).wait_recv()
        out.wait()
        for copy in sends:
            copy.wait_send()

    for k in range(NZ):
        pl.when(z == k)(functools.partial(program, k))


def weight_scatter(p, collective_id):
    _, rows, width = p.shape
    half = (rows // 2, width)
    out = pl.pallas_call(
        weight_scatter_kernel,
        out_shape=jax.ShapeDtypeStruct((2,) + half, p.dtype),
        in_specs=[ANY],
        out_specs=ANY,
        scratch_shapes=[pltpu.VMEM((2 * NZ,) + half, p.dtype)] * 2 + [pltpu.VMEM((NZ,) + half, p.dtype)] * 3
        + [pltpu.VMEM(half, p.dtype)]
        + [pltpu.SemaphoreType.DMA((2 * NZ,)), pltpu.SemaphoreType.DMA]
        + ([pltpu.SemaphoreType.DMA((2 * NZ,))] + [pltpu.SemaphoreType.DMA((NZ,))] * 3 + [pltpu.SemaphoreType.DMA((2,))]) * 2,
        compiler_params=pltpu.CompilerParams(collective_id=collective_id, has_side_effects=True),
        name="weight_scatter",
    )(p.reshape((2 * NZ, 2) + half))
    return out.reshape(rows, width)


def plane_barrier(tp, dp, others):
    peers = [(lax.rem(tp + n, 2 * NZ), dp) for n in range(1, 2 * NZ)] + others
    for peer in peers:
        signal(*peer)
    pl.semaphore_wait(pltpu.get_barrier_semaphore(), len(peers))


def swap_kernel(spread, x_ref, out_ref, own_sem, send, recv):
    tp, dp, _, _ = place()
    plane_barrier(tp, dp, [])
    copies = []
    for n in range(1, 2 * NZ):
        to = lax.rem(tp + n, 2 * NZ)
        copy = remote(x_ref if spread else x_ref.at[to], out_ref.at[tp], send.at[to], recv.at[tp], to, dp)
        copy.start()
        copies.append(copy)
    own = pltpu.make_async_copy(x_ref if spread else x_ref.at[tp], out_ref.at[tp], own_sem)
    own.start()
    for n in range(1, 2 * NZ):
        source = lax.rem(tp + n, 2 * NZ)
        remote(out_ref.at[source], out_ref.at[source], send.at[source], recv.at[source], source, dp).wait_recv()
    own.wait()
    for copy in copies:
        copy.wait_send()


def plane_swap(x, spread, collective_id):
    return pl.pallas_call(
        functools.partial(swap_kernel, spread),
        out_shape=jax.ShapeDtypeStruct((2 * NZ,) + x.shape if spread else x.shape, x.dtype),
        in_specs=[ANY],
        out_specs=ANY,
        scratch_shapes=[pltpu.SemaphoreType.DMA] + [pltpu.SemaphoreType.DMA((2 * NZ,))] * 2,
        compiler_params=pltpu.CompilerParams(collective_id=collective_id, has_side_effects=True),
        name="plane_spread" if spread else "plane_swap",
    )(x)


def row_return_kernel(x_ref, out_ref, own_sem, send, send_c, send_x, recv):
    tp, dp, _, _ = place()
    core = dp % 2
    twin = dp + 1 - 2 * core
    facing = lax.rem(dp + 2, 4)
    plane_barrier(tp, dp, [(tp, twin), (tp, facing)])
    copies = []

    def forward(group, source, sems, to_dp):
        copy = remote(out_ref.at[group, source], out_ref.at[group, source], sems.at[source], recv.at[group, source], tp, to_dp)
        copy.start()
        copies.append(copy)

    def arrived(group, source):
        remote(out_ref.at[group, source], out_ref.at[group, source], send.at[source], recv.at[group, source], tp, twin).wait_recv()

    for n in range(1, 2 * NZ):
        to = lax.rem(tp + n, 2 * NZ)
        copy = remote(x_ref.at[to], out_ref.at[dp, tp], send.at[to], recv.at[dp, tp], to, dp)
        copy.start()
        copies.append(copy)
    own = pltpu.make_async_copy(x_ref.at[tp], out_ref.at[dp, tp], own_sem)
    own.start()
    own.wait()
    forward(dp, tp, send_x, facing)
    forward(dp, tp, send_c.at[0], twin)
    for n in range(1, 2 * NZ):
        source = lax.rem(tp + 2 * NZ - n, 2 * NZ)
        arrived(dp, source)
        forward(dp, source, send_x, facing)
        forward(dp, source, send_c.at[0], twin)
    for n in range(2 * NZ):
        source = lax.rem(tp + 2 * NZ - n, 2 * NZ)
        arrived(facing, source)
        forward(facing, source, send_c.at[1], twin)
    for n in range(2 * NZ):
        source = lax.rem(tp + 2 * NZ - n, 2 * NZ)
        arrived(twin, source)
        arrived(lax.rem(twin + 2, 4), source)
    for copy in copies:
        copy.wait_send()


def row_return(x, collective_id):
    return pl.pallas_call(
        row_return_kernel,
        out_shape=jax.ShapeDtypeStruct((4,) + x.shape, x.dtype),
        in_specs=[ANY],
        out_specs=ANY,
        scratch_shapes=[pltpu.SemaphoreType.DMA, pltpu.SemaphoreType.DMA((2 * NZ,)), pltpu.SemaphoreType.DMA((2, 2 * NZ)),
                        pltpu.SemaphoreType.DMA((2 * NZ,)), pltpu.SemaphoreType.DMA((4, 2 * NZ))],
        compiler_params=pltpu.CompilerParams(collective_id=collective_id, has_side_effects=True),
        name="row_return",
    )(x)


def pair_kernel(x_ref, out_ref, send, recv):
    tp, dp, _, y = place()
    partner = tp + 1 - 2 * y
    signal(partner, dp)
    pl.semaphore_wait(pltpu.get_barrier_semaphore(), 1)
    copy = remote(x_ref, out_ref, send, recv, partner, dp)
    copy.start()
    copy.wait()


def pair_swap(x, collective_id):
    return pl.pallas_call(
        pair_kernel,
        out_shape=jax.ShapeDtypeStruct(x.shape, x.dtype),
        in_specs=[VMEM],
        out_specs=VMEM,
        scratch_shapes=[pltpu.SemaphoreType.DMA, pltpu.SemaphoreType.DMA],
        compiler_params=pltpu.CompilerParams(collective_id=collective_id, has_side_effects=True),
        name="pair_swap",
    )(x)


def norm_fwd(x_f32, scale):
    centered = x_f32 - jnp.mean(x_f32, axis=-1, keepdims=True)
    inv_std = lax.rsqrt(jnp.mean(centered * centered, axis=-1, keepdims=True) + LN_EPS)
    x_hat = centered * inv_std
    return (x_hat * scale).astype(BF16), x_hat, inv_std


def norm_bwd(d_out, x_hat, inv_std, scale):
    d_scale = jnp.sum(d_out * x_hat, axis=0)
    d_hat = d_out * scale
    d_in = inv_std * (d_hat - jnp.mean(d_hat, axis=-1, keepdims=True) - x_hat * jnp.mean(d_hat * x_hat, axis=-1, keepdims=True))
    return d_in, d_scale


def rope_tables(positions, head_dim):
    inv_freq = ROPE_BASE ** (-jnp.arange(0, head_dim, 2).astype(F32) / head_dim)
    angles = positions.astype(F32)[:, None] * inv_freq[None, :]
    return jnp.cos(angles), jnp.sin(angles)


def rotate(x_in, cos_t, sin_t):
    half_dim = x_in.shape[-1] // 2
    x_lo = x_in[..., :half_dim]
    x_hi = x_in[..., half_dim:]
    return jnp.concatenate([x_lo * cos_t - x_hi * sin_t, x_hi * cos_t + x_lo * sin_t], axis=-1)


def adam_update(param_in, grad_in, mom_in, vel_in):
    mom_new = BETA_ONE * mom_in + (1.0 - BETA_ONE) * grad_in
    vel_new = BETA_TWO * vel_in + (1.0 - BETA_TWO) * grad_in * grad_in
    return param_in - LEARN_RATE * mom_new / (jnp.sqrt(vel_new) + ADAM_EPS), mom_new, vel_new


def dot(spec, a, b):
    return jnp.einsum(spec, a, b, preferred_element_type=F32)


def solution(mesh):
    param_specs = (P('tp', None), P(None, None), P(None, 'tp'), P(None, None, None), P('tp', None), P(None, None, 'tp'), P('tp', None))
    n_tp = mesh.shape['tp']
    n_dp = mesh.shape['dp']

    def local_step(tokens, labels, *state_arrays):
        embed, ln_scales, w_q, w_kv, w_o, w_gu, w_down = state_arrays[0:7]
        batch_loc, seq_len = tokens.shape
        vocab_loc, d_model = embed.shape
        head_dim = w_kv.shape[2]
        q_loc = w_q.shape[1]
        f_loc = w_down.shape[0]
        heads = n_tp * q_loc // head_dim
        tok_loc = batch_loc * seq_len
        tok_total = tok_loc * n_dp
        own = tok_loc // n_tp
        tp_rank = lax.axis_index('tp')
        half = tp_rank % 2
        emb_b = embed.astype(BF16)

        all_tokens = lax.all_gather(tokens, 'dp').reshape(n_dp * n_tp, own)
        strict = (jnp.arange(own)[:, None] > jnp.arange(own)[None, :]).astype(BF16)

        def routing(chunks):
            shard = chunks // vocab_loc
            row = chunks - shard * vocab_loc
            hot = (shard[:, :, None] == jnp.arange(n_tp)[None, None, :])
            before = dot('rs,nsj->nrj', strict, hot.astype(BF16))
            rank = jnp.sum(jnp.where(hot, before, 0.0), axis=-1).astype(jnp.int32)
            most = jnp.max(jnp.sum(hot.astype(jnp.int32), axis=1))
            return shard, row, rank, (most + CAP - 1) // CAP

        chunks = tokens.reshape(n_tp, own)
        shard, row, rank, _ = routing(chunks)
        shard_all, row_all, rank_all, rounds_all = routing(all_tokens)
        slots = jnp.arange(CAP)
        my_shard = lax.dynamic_index_in_dim(shard, tp_rank, 0, keepdims=False)
        my_rank = lax.dynamic_index_in_dim(rank, tp_rank, 0, keepdims=False)

        def fetch(step, x_sum, collective_id):
            here = (shard[:, None, :] == tp_rank) & (rank[:, None, :] == slots[None, :, None] + step * CAP)
            ids = jnp.sum(jnp.where(here, row[:, None, :], 0), axis=-1).reshape(-1)
            rows_out = jnp.take(embed, ids, axis=0).astype(BF16).astype(F32).reshape(n_tp, CAP, d_model)
            rows_in = plane_swap(rows_out, False, collective_id).reshape(n_tp * CAP, d_model).astype(BF16)
            pick = (my_shard[:, None, None] == jnp.arange(n_tp)[None, :, None]) & (my_rank[:, None, None] == slots[None, None, :] + step * CAP)
            return x_sum + dot('rc,cd->rd', pick.reshape(own, n_tp * CAP).astype(BF16), rows_in)

        x_zero = fetch(0, jnp.zeros((own, d_model), F32), 0)
        x_zero = lax.while_loop(lambda s: s[0] < rounds_all, lambda s: (s[0] + 1, fetch(s[0], s[1], 1)), (jnp.int32(1), x_zero))[1]

        w_rows = jnp.concatenate([w_q.T, w_o, w_gu.transpose(0, 2, 1).reshape(2 * f_loc, d_model), w_down], axis=0)
        w_all = weight_gather(w_rows, 2).astype(BF16)
        cuts = (q_loc, 2 * q_loc, 2 * q_loc + f_loc, 2 * q_loc + 2 * f_loc)
        wq_t = w_all[:, :cuts[0]].reshape(-1, d_model)
        wo_b = w_all[:, cuts[0]:cuts[1]].reshape(-1, d_model)
        wg_t = w_all[:, cuts[1]:cuts[2]].reshape(-1, d_model)
        wu_t = w_all[:, cuts[2]:cuts[3]].reshape(-1, d_model)
        wd_b = w_all[:, cuts[3]:].reshape(-1, d_model)
        wkv_b = w_kv.astype(BF16)

        u_norm, u_hat, u_inv = norm_fwd(x_zero, ln_scales[0])
        q_pos = half * own + jnp.arange(own)
        cos_t, sin_t = rope_tables(q_pos, head_dim)
        q_raw = dot('rd,nd->rn', u_norm, wq_t).reshape(own, heads, head_dim)
        queries = rotate(q_raw, cos_t[:, None, :], sin_t[:, None, :]).astype(BF16)
        kv_raw = dot('rd,cde->cre', u_norm, wkv_b)
        kv_own = jnp.concatenate([rotate(kv_raw[0], cos_t, sin_t), kv_raw[1]], axis=-1)
        kv_other = pair_swap(kv_own, 3)
        kv_seq = jnp.concatenate([jnp.where(half == 0, kv_own, kv_other), jnp.where(half == 0, kv_other, kv_own)], axis=0).astype(BF16)
        keys = kv_seq[:, :head_dim]
        values = kv_seq[:, head_dim:]
        causal = q_pos[:, None] >= jnp.arange(2 * own)[None, :]
        scores = dot('qhe,ke->hqk', queries, keys) * head_dim ** -0.5
        prob_f32 = jax.nn.softmax(jnp.where(causal, scores, -1e30), axis=-1)
        prob_b16 = prob_f32.astype(BF16)
        context = dot('hqk,ke->qhe', prob_b16, values).astype(BF16).reshape(own, heads * head_dim)
        att_out = dot('rf,fe->re', context, wo_b)
        gate = dot('rd,fd->rf', u_norm, wg_t)
        up = dot('rd,fd->rf', u_norm, wu_t)
        gate_sig = jax.nn.sigmoid(gate)
        hidden = (gate * gate_sig * up).astype(BF16)
        x_one = x_zero + att_out + dot('rf,fd->rd', hidden, wd_b)
        f_own, f_hat, f_inv = norm_fwd(x_one, ln_scales[1])

        f_norm = plane_gather(f_own.astype(F32), 4).reshape(tok_loc, d_model).astype(BF16)
        logit_scale = d_model ** -0.5
        logits = dot('rd,vd->rv', f_norm, emb_b) * logit_scale
        lab_loc = labels.reshape(tok_loc) - tp_rank * vocab_loc
        lab_hit = jnp.arange(vocab_loc)[None, :] == lab_loc[:, None]
        row_max = jnp.max(logits, axis=-1)
        exp_sum = jnp.sum(jnp.exp(logits - row_max[:, None]), axis=-1)
        lab_val = jnp.sum(jnp.where(lab_hit, logits, 0.0), axis=-1)
        stats = plane_swap(jnp.stack([row_max, exp_sum, lab_val]).reshape(3 * tok_loc // 128, 128), True, 5).reshape(n_tp, 3, tok_loc)
        top = jnp.max(stats[:, 0], axis=0)
        log_norm = top + jnp.log(jnp.sum(stats[:, 1] * jnp.exp(stats[:, 0] - top), axis=0))
        tok_loss = log_norm - jnp.sum(stats[:, 2], axis=0) + LOGIT_ZLOSS * log_norm * log_norm
        loss_part = jnp.sum(tok_loss) / (n_tp * tok_total)

        coef = 1.0 + 2.0 * LOGIT_ZLOSS * log_norm
        d_logits = ((jnp.exp(logits - log_norm[:, None]) * coef[:, None] - lab_hit.astype(F32)) * (logit_scale / tok_total)).astype(BF16)
        d_fin_part = dot('rv,vd->rd', d_logits, emb_b).reshape(n_tp, own, d_model)
        g_head = lax.psum(dot('rv,rd->vd', d_logits, f_norm), 'dp')
        d_fin = plane_scatter(d_fin_part, 6)
        d_one, g_ln_fin = norm_bwd(d_fin, f_hat, f_inv, ln_scales[1])
        d_one_b = d_one.astype(BF16)

        d_hidden = dot('rd,fd->rf', d_one_b, wd_b)
        g_down = dot('rf,rd->fd', hidden, d_one_b)
        d_gate = (d_hidden * up * gate_sig * (1.0 + gate * (1.0 - gate_sig))).astype(BF16)
        d_up = (d_hidden * gate * gate_sig).astype(BF16)
        g_gate = dot('rf,rd->fd', d_gate, u_norm)
        g_up = dot('rf,rd->fd', d_up, u_norm)
        d_u_mlp = dot('rf,fd->rd', d_gate, wg_t) + dot('rf,fd->rd', d_up, wu_t)

        d_context = dot('re,fe->rf', d_one_b, wo_b).astype(BF16).reshape(own, heads, head_dim)
        g_o = dot('rf,re->fe', context, d_one_b)
        d_probs = dot('qhe,ke->hqk', d_context, values)
        d_values = dot('hqk,qhe->ke', prob_b16, d_context)
        d_scores = (prob_f32 * (d_probs - jnp.sum(d_probs * prob_f32, axis=-1, keepdims=True)) * head_dim ** -0.5).astype(BF16)
        d_queries = dot('hqk,ke->qhe', d_scores, keys)
        d_keys = dot('hqk,qhe->ke', d_scores, queries)
        d_kv_seq = jnp.concatenate([d_keys, d_values], axis=-1)
        d_kv_lo = d_kv_seq[:own]
        d_kv_hi = d_kv_seq[own:]
        d_kv_own = jnp.where(half == 0, d_kv_lo, d_kv_hi) + pair_swap(jnp.where(half == 0, d_kv_hi, d_kv_lo), 7)
        d_q_raw = rotate(d_queries, cos_t[:, None, :], -sin_t[:, None, :]).astype(BF16).reshape(own, heads * head_dim)
        d_kv = jnp.stack([rotate(d_kv_own[:, :head_dim], cos_t, -sin_t), d_kv_own[:, head_dim:]]).astype(BF16)
        g_q_t = dot('rn,rd->nd', d_q_raw, u_norm)
        g_kv_part = dot('cre,rd->cde', d_kv, u_norm)
        d_u = dot('rn,nd->rd', d_q_raw, wq_t) + dot('cre,cde->rd', d_kv, wkv_b) + d_u_mlp
        d_zero_norm, g_ln_in = norm_bwd(d_u, u_hat, u_inv, ln_scales[0])
        d_zero = d_one + d_zero_norm

        my_row_shard = my_shard

        def give_back(step, g_look, collective_id):
            mine = (my_row_shard[None, None, :] == jnp.arange(n_tp)[:, None, None]) & (my_rank[None, None, :] == slots[None, :, None] + step * CAP)
            ids = jnp.sum(jnp.where(mine, jnp.arange(own)[None, None, :], 0), axis=-1).reshape(-1)
            rows_out = jnp.take(d_zero, ids, axis=0).reshape(n_tp, CAP, d_model)
            rows_in = row_return(rows_out, collective_id).reshape(-1, d_model)
            here = (shard_all[:, None, :] == tp_rank) & (rank_all[:, None, :] == slots[None, :, None] + step * CAP)
            row_id = jnp.where(jnp.any(here, axis=-1), jnp.sum(jnp.where(here, row_all[:, None, :], 0), axis=-1), vocab_loc).reshape(-1)
            return g_look.at[row_id].add(rows_in, mode='drop')

        g_look = give_back(0, jnp.zeros((vocab_loc, d_model), F32), 8)
        g_look = lax.while_loop(lambda s: s[0] < rounds_all, lambda s: (s[0] + 1, give_back(s[0], s[1], 9)), (jnp.int32(1), g_look))[1]

        g_gu_t = jnp.stack([g_gate.reshape(n_tp, f_loc, d_model), g_up.reshape(n_tp, f_loc, d_model)], axis=1)
        g_rows = jnp.concatenate([g_q_t.reshape(n_tp, q_loc, d_model), g_o.reshape(n_tp, q_loc, d_model),
                                  g_gu_t.reshape(n_tp, 2 * f_loc, d_model), g_down.reshape(n_tp, f_loc, d_model)], axis=1)
        g_shard = weight_scatter(g_rows, 10)
        g_kv, g_ln, loss = lax.psum((g_kv_part, jnp.stack([g_ln_in, g_ln_fin]), loss_part), ('tp', 'dp'))
        gradients = (g_head + g_look, g_ln, g_shard[:cuts[0]].T, g_kv, g_shard[cuts[0]:cuts[1]],
                     g_shard[cuts[1]:cuts[3]].reshape(2, f_loc, d_model).transpose(0, 2, 1), g_shard[cuts[3]:])

        outs_p = []
        outs_m = []
        outs_v = []
        for index in range(7):
            new_p, new_m, new_v = adam_update(state_arrays[index], gradients[index], state_arrays[7 + index], state_arrays[14 + index])
            outs_p.append(new_p)
            outs_m.append(new_m)
            outs_v.append(new_v)
        return tuple(outs_p) + tuple(outs_m) + tuple(outs_v) + (loss,)

    return jax.shard_map(local_step, mesh=mesh, in_specs=(P('dp', None), P('dp', None)) + param_specs * 3,
                         out_specs=param_specs * 3 + (P(),), check_vma=False)
```

```python
import functools

import jax
import jax.numpy as jnp
from jax import lax
from jax.experimental import pallas as pl
from jax.experimental.pallas import tpu as pltpu
from jax.sharding import PartitionSpec as P

LN_EPS = 1e-5
LOGIT_ZLOSS = 1e-4
LEARN_RATE = 1e-2
BETA_ONE = 0.9
BETA_TWO = 0.95
ADAM_EPS = 1e-8
ROPE_BASE = 10000.0
NZ = 4
CAP = 96
F32 = jnp.float32
BF16 = jnp.bfloat16
ANY = pl.BlockSpec(memory_space=pl.ANY)
VMEM = pl.BlockSpec(memory_space=pltpu.VMEM)

ARRIVALS = {
    0: (("R", 1), ("R", 2), ("R", 3)),
    1: (("L", 0), ("R", 2), ("R", 3)),
    2: (("R", 3), ("L", 1), ("L", 0)),
    3: (("L", 2), ("L", 1), ("L", 0)),
}
REDUCE_ORDER = {0: (3, 2, 1, 0), 1: (3, 0, 2, 1), 2: (0, 3, 1, 2), 3: (0, 1, 2, 3)}


def remote(src, dst, send_sem, recv_sem, tp, dp):
    return pltpu.make_async_remote_copy(src_ref=src, dst_ref=dst, send_sem=send_sem, recv_sem=recv_sem,
                                        device_id=(tp, dp), device_id_type=pl.DeviceIdType.MESH)


def place():
    tp = lax.axis_index("tp")
    dp = lax.axis_index("dp")
    return tp, dp, tp // 2, tp % 2


def signal(tp, dp):
    pl.semaphore_signal(pltpu.get_barrier_semaphore(), inc=1, device_id=(tp, dp), device_id_type=pl.DeviceIdType.MESH)


def line_barrier(k, tp, dp, others):
    peers = [(tp + 1 - 2 * (tp % 2), dp)] + others
    if k > 0:
        peers.append((tp - 2, dp))
    if k < NZ - 1:
        peers.append((tp + 2, dp))
    for peer in peers:
        signal(*peer)
    pl.semaphore_wait(pltpu.get_barrier_semaphore(), len(peers))


def gather_kernel(x_ref, out_ref, own_sem, send_y, send_l, send_r, recv):
    tp, dp, z, y = place()
    partner = tp + 1 - 2 * y

    def program(k):
        line_barrier(k, tp, dp, [])

        def send(src, slot, sems, to):
            copy = remote(src, out_ref.at[slot], sems.at[slot], recv.at[slot], to, dp)
            copy.start()
            return copy

        def arrived(slot):
            remote(x_ref, out_ref.at[slot], send_y.at[slot], recv.at[slot], partner, dp).wait_recv()

        sends = []
        if k > 0:
            sends.append(send(x_ref, tp, send_l, tp - 2))
        if k < NZ - 1:
            sends.append(send(x_ref, tp, send_r, tp + 2))
        sends.append(send(x_ref, tp, send_y, partner))
        own = pltpu.make_async_copy(x_ref, out_ref.at[tp], own_sem)
        own.start()
        for side, zz in ARRIVALS[k]:
            slot = 2 * zz + y
            arrived(slot)
            if side == "L" and k < NZ - 1:
                sends.append(send(out_ref.at[slot], slot, send_r, tp + 2))
            if side == "R" and k > 0:
                sends.append(send(out_ref.at[slot], slot, send_l, tp - 2))
            sends.append(send(out_ref.at[slot], slot, send_y, partner))
        for zz in range(NZ):
            arrived(2 * zz + 1 - y)
        own.wait()
        for copy in sends:
            copy.wait_send()

    for k in range(NZ):
        pl.when(z == k)(functools.partial(program, k))


def plane_gather(x, collective_id):
    return pl.pallas_call(
        gather_kernel,
        out_shape=jax.ShapeDtypeStruct((2 * NZ,) + x.shape, x.dtype),
        in_specs=[ANY],
        out_specs=ANY,
        scratch_shapes=[pltpu.SemaphoreType.DMA] + [pltpu.SemaphoreType.DMA((2 * NZ,))] * 4,
        compiler_params=pltpu.CompilerParams(collective_id=collective_id, has_side_effects=True),
        name="plane_gather",
    )(x)


def weight_gather_kernel(x_ref, out_ref, own_sem, send_y, send_l, send_r, send_c, recv):
    tp, dp, z, y = place()
    partner = tp + 1 - 2 * y
    core = dp % 2
    twin = dp + 1 - 2 * core

    def program(k):
        line_barrier(k, tp, dp, [(tp, twin)])

        def send(src, slot, sems, to, to_dp):
            copy = remote(src, out_ref.at[slot, core], sems.at[slot], recv.at[slot, core], to, to_dp)
            copy.start()
            return copy

        def arrived(slot, half):
            remote(x_ref.at[0], out_ref.at[slot, half], send_y.at[slot], recv.at[slot, half], partner, dp).wait_recv()

        mine = x_ref.at[core]
        sends = []
        if k > 0:
            sends.append(send(mine, tp, send_l, tp - 2, dp))
        if k < NZ - 1:
            sends.append(send(mine, tp, send_r, tp + 2, dp))
        sends.append(send(mine, tp, send_y, partner, dp))
        own = pltpu.make_async_copy(x_ref, out_ref.at[tp], own_sem)
        own.start()
        across = [k] + [zz for _, zz in ARRIVALS[k]]
        for n, (side, zz) in enumerate(ARRIVALS[k]):
            slot = 2 * zz + y
            arrived(slot, core)
            if side == "L" and k < NZ - 1:
                sends.append(send(out_ref.at[slot, core], slot, send_r, tp + 2, dp))
            if side == "R" and k > 0:
                sends.append(send(out_ref.at[slot, core], slot, send_l, tp - 2, dp))
            sends.append(send(out_ref.at[slot, core], slot, send_y, partner, dp))
            sends.append(send(out_ref.at[slot, core], slot, send_c, tp, twin))
            slot = 2 * across[n] + 1 - y
            arrived(slot, core)
            sends.append(send(out_ref.at[slot, core], slot, send_c, tp, twin))
        slot = 2 * across[-1] + 1 - y
        arrived(slot, core)
        sends.append(send(out_ref.at[slot, core], slot, send_c, tp, twin))
        for zz in range(NZ):
            if zz != k:
                arrived(2 * zz + y, 1 - core)
            arrived(2 * zz + 1 - y, 1 - core)
        own.wait()
        for copy in sends:
            copy.wait_send()

    for k in range(NZ):
        pl.when(z == k)(functools.partial(program, k))


def weight_gather(x, collective_id):
    rows, width = x.shape
    halves = x.reshape(2, rows // 2, width)
    out = pl.pallas_call(
        weight_gather_kernel,
        out_shape=jax.ShapeDtypeStruct((2 * NZ,) + halves.shape, x.dtype),
        in_specs=[ANY],
        out_specs=ANY,
        scratch_shapes=[pltpu.SemaphoreType.DMA] + [pltpu.SemaphoreType.DMA((2 * NZ,))] * 4
        + [pltpu.SemaphoreType.DMA((2 * NZ, 2))],
        compiler_params=pltpu.CompilerParams(collective_id=collective_id, has_side_effects=True),
        name="weight_gather",
    )(halves)
    return out.reshape(2 * NZ, rows, width)


def add_into(acc, other):
    rows = acc.shape[0]
    step = 64 if rows % 64 == 0 else rows

    def body(n, carry):
        at = pl.ds(pl.multiple_of(n * step, step), step)
        acc[at, :] = acc[at, :] + other[at, :]
        return carry

    lax.fori_loop(0, rows // step, body, 0)


def scatter_kernel(p_ref, out_ref, acc, from_y, from_l, from_r, load_sem, out_sem, send_y, send_l, send_r, recv_y, recv_l, recv_r):
    tp, dp, z, y = place()
    partner = tp + 1 - 2 * y

    def program(k):
        line_barrier(k, tp, dp, [])
        sends = []
        loads = []
        for zz in REDUCE_ORDER[k]:
            copy = remote(p_ref.at[2 * zz + 1 - y], from_y.at[zz], send_y.at[zz], recv_y.at[zz], partner, dp)
            copy.start()
            sends.append(copy)
        for zz in REDUCE_ORDER[k]:
            load = pltpu.make_async_copy(p_ref.at[2 * zz + y], acc.at[zz], load_sem.at[zz])
            load.start()
            loads.append(load)
        for n, zz in enumerate(REDUCE_ORDER[k]):
            loads[n].wait()
            remote(acc.at[zz], from_y.at[zz], send_y.at[zz], recv_y.at[zz], partner, dp).wait_recv()
            add_into(acc.at[zz], from_y.at[zz])
            if zz >= k and k > 0:
                remote(acc.at[zz], from_l.at[zz], send_l.at[zz], recv_l.at[zz], partner, dp).wait_recv()
                add_into(acc.at[zz], from_l.at[zz])
            if zz <= k and k < NZ - 1:
                remote(acc.at[zz], from_r.at[zz], send_r.at[zz], recv_r.at[zz], partner, dp).wait_recv()
                add_into(acc.at[zz], from_r.at[zz])
            if zz > k:
                copy = remote(acc.at[zz], from_l.at[zz], send_r.at[zz], recv_l.at[zz], tp + 2, dp)
                copy.start()
                sends.append(copy)
            if zz < k:
                copy = remote(acc.at[zz], from_r.at[zz], send_l.at[zz], recv_r.at[zz], tp - 2, dp)
                copy.start()
                sends.append(copy)
        out = pltpu.make_async_copy(acc.at[k], out_ref, out_sem)
        out.start()
        out.wait()
        for copy in sends:
            copy.wait_send()

    for k in range(NZ):
        pl.when(z == k)(functools.partial(program, k))


def plane_scatter(p, collective_id):
    _, rows, width = p.shape
    line = (NZ, rows, width)
    return pl.pallas_call(
        scatter_kernel,
        out_shape=jax.ShapeDtypeStruct((rows, width), p.dtype),
        in_specs=[ANY],
        out_specs=ANY,
        scratch_shapes=[pltpu.VMEM(line, p.dtype)] * 4
        + [pltpu.SemaphoreType.DMA((NZ,)), pltpu.SemaphoreType.DMA]
        + [pltpu.SemaphoreType.DMA((NZ,))] * 6,
        compiler_params=pltpu.CompilerParams(collective_id=collective_id, has_side_effects=True),
        name="plane_scatter",
    )(p)


def weight_scatter_kernel(p_ref, out_ref, acc, from_c, from_y, from_l, from_r, from_x, load_sem, out_sem, send_c, send_y, send_l, send_r,
                          last_send, recv_c, recv_y, recv_l, recv_r, last_recv):
    tp, dp, z, y = place()
    partner = tp + 1 - 2 * y
    core = dp % 2
    twin = dp + 1 - 2 * core
    facing = lax.rem(dp + 2, 4)

    def program(k):
        line_barrier(k, tp, dp, [(tp, twin), (tp, facing)])
        sends = []
        for zz in REDUCE_ORDER[k]:
            for slot in (2 * zz + 1 - y, 2 * zz + y):
                copy = remote(p_ref.at[slot, 1 - core], from_c.at[slot], send_c.at[slot], recv_c.at[slot], tp, twin)
                copy.start()
                sends.append(copy)
                pltpu.make_async_copy(p_ref.at[slot, core], acc.at[slot], load_sem.at[slot]).start()

        def chip_sum(slot):
            pltpu.make_async_copy(p_ref.at[slot, core], acc.at[slot], load_sem.at[slot]).wait()
            remote(acc.at[slot], from_c.at[slot], send_c.at[slot], recv_c.at[slot], tp, twin).wait_recv()
            add_into(acc.at[slot], from_c.at[slot])

        for zz in REDUCE_ORDER[k]:
            slot = 2 * zz + 1 - y
            chip_sum(slot)
            copy = remote(acc.at[slot], from_y.at[zz], send_y.at[zz], recv_y.at[zz], partner, dp)
            copy.start()
            sends.append(copy)
        for zz in REDUCE_ORDER[k]:
            chip_sum(2 * zz + y)
        for zz in REDUCE_ORDER[k]:
            slot = 2 * zz + y
            line = acc.at[slot]
            remote(line, from_y.at[zz], send_y.at[zz], recv_y.at[zz], partner, dp).wait_recv()
            add_into(line, from_y.at[zz])
            if zz >= k and k > 0:
                remote(line, from_l.at[zz], send_l.at[zz], recv_l.at[zz], partner, dp).wait_recv()
                add_into(line, from_l.at[zz])
            if zz <= k and k < NZ - 1:
                remote(line, from_r.at[zz], send_r.at[zz], recv_r.at[zz], partner, dp).wait_recv()
                add_into(line, from_r.at[zz])
            if zz > k:
                copy = remote(line, from_l.at[zz], send_r.at[zz], recv_l.at[zz], tp + 2, dp)
                copy.start()
                sends.append(copy)
            if zz < k:
                copy = remote(line, from_r.at[zz], send_l.at[zz], recv_r.at[zz], tp - 2, dp)
                copy.start()
                sends.append(copy)
        total = acc.at[2 * k + y]
        copy = remote(total, from_x, last_send.at[0], last_recv.at[0], tp, facing)
        copy.start()
        copy.wait()
        add_into(total, from_x)
        copy = remote(total, out_ref.at[core], last_send.at[1], last_recv.at[1], tp, twin)
        copy.start()
        out = pltpu.make_async_copy(total, out_ref.at[core], out_sem)
        out.start()
        copy.wait_send()
        remote(total, out_ref.at[1 - core], last_send.at[1], last_recv.at[1], tp, twin).wait_recv()
        out.wait()
        for copy in sends:
            copy.wait_send()

    for k in range(NZ):
        pl.when(z == k)(functools.partial(program, k))


def weight_scatter(p, collective_id):
    _, rows, width = p.shape
    half = (rows // 2, width)
    out = pl.pallas_call(
        weight_scatter_kernel,
        out_shape=jax.ShapeDtypeStruct((2,) + half, p.dtype),
        in_specs=[ANY],
        out_specs=ANY,
        scratch_shapes=[pltpu.VMEM((2 * NZ,) + half, p.dtype)] * 2 + [pltpu.VMEM((NZ,) + half, p.dtype)] * 3
        + [pltpu.VMEM(half, p.dtype)]
        + [pltpu.SemaphoreType.DMA((2 * NZ,)), pltpu.SemaphoreType.DMA]
        + ([pltpu.SemaphoreType.DMA((2 * NZ,))] + [pltpu.SemaphoreType.DMA((NZ,))] * 3 + [pltpu.SemaphoreType.DMA((2,))]) * 2,
        compiler_params=pltpu.CompilerParams(collective_id=collective_id, has_side_effects=True),
        name="weight_scatter",
    )(p.reshape((2 * NZ, 2) + half))
    return out.reshape(rows, width)


def plane_barrier(tp, dp, others):
    peers = [(lax.rem(tp + n, 2 * NZ), dp) for n in range(1, 2 * NZ)] + others
    for peer in peers:
        signal(*peer)
    pl.semaphore_wait(pltpu.get_barrier_semaphore(), len(peers))


def swap_kernel(spread, x_ref, out_ref, own_sem, send, recv):
    tp, dp, _, _ = place()
    plane_barrier(tp, dp, [])
    copies = []
    for n in range(1, 2 * NZ):
        to = lax.rem(tp + n, 2 * NZ)
        copy = remote(x_ref if spread else x_ref.at[to], out_ref.at[tp], send.at[to], recv.at[tp], to, dp)
        copy.start()
        copies.append(copy)
    own = pltpu.make_async_copy(x_ref if spread else x_ref.at[tp], out_ref.at[tp], own_sem)
    own.start()
    for n in range(1, 2 * NZ):
        source = lax.rem(tp + n, 2 * NZ)
        remote(out_ref.at[source], out_ref.at[source], send.at[source], recv.at[source], source, dp).wait_recv()
    own.wait()
    for copy in copies:
        copy.wait_send()


def plane_swap(x, spread, collective_id):
    return pl.pallas_call(
        functools.partial(swap_kernel, spread),
        out_shape=jax.ShapeDtypeStruct((2 * NZ,) + x.shape if spread else x.shape, x.dtype),
        in_specs=[ANY],
        out_specs=ANY,
        scratch_shapes=[pltpu.SemaphoreType.DMA] + [pltpu.SemaphoreType.DMA((2 * NZ,))] * 2,
        compiler_params=pltpu.CompilerParams(collective_id=collective_id, has_side_effects=True),
        name="plane_spread" if spread else "plane_swap",
    )(x)


def row_return_kernel(x_ref, out_ref, own_sem, send, send_c, send_x, recv):
    tp, dp, _, _ = place()
    core = dp % 2
    twin = dp + 1 - 2 * core
    facing = lax.rem(dp + 2, 4)
    plane_barrier(tp, dp, [(tp, twin), (tp, facing)])
    copies = []

    def forward(group, source, sems, to_dp):
        copy = remote(out_ref.at[group, source], out_ref.at[group, source], sems.at[source], recv.at[group, source], tp, to_dp)
        copy.start()
        copies.append(copy)

    def arrived(group, source):
        remote(out_ref.at[group, source], out_ref.at[group, source], send.at[source], recv.at[group, source], tp, twin).wait_recv()

    for n in range(1, 2 * NZ):
        to = lax.rem(tp + n, 2 * NZ)
        copy = remote(x_ref.at[to], out_ref.at[dp, tp], send.at[to], recv.at[dp, tp], to, dp)
        copy.start()
        copies.append(copy)
    own = pltpu.make_async_copy(x_ref.at[tp], out_ref.at[dp, tp], own_sem)
    own.start()
    own.wait()
    forward(dp, tp, send_x, facing)
    forward(dp, tp, send_c.at[0], twin)
    for n in range(1, 2 * NZ):
        source = lax.rem(tp + 2 * NZ - n, 2 * NZ)
        arrived(dp, source)
        forward(dp, source, send_x, facing)
        forward(dp, source, send_c.at[0], twin)
    for n in range(2 * NZ):
        source = lax.rem(tp + 2 * NZ - n, 2 * NZ)
        arrived(facing, source)
        forward(facing, source, send_c.at[1], twin)
    for n in range(2 * NZ):
        source = lax.rem(tp + 2 * NZ - n, 2 * NZ)
        arrived(twin, source)
        arrived(lax.rem(twin + 2, 4), source)
    for copy in copies:
        copy.wait_send()


def row_return(x, collective_id):
    return pl.pallas_call(
        row_return_kernel,
        out_shape=jax.ShapeDtypeStruct((4,) + x.shape, x.dtype),
        in_specs=[ANY],
        out_specs=ANY,
        scratch_shapes=[pltpu.SemaphoreType.DMA, pltpu.SemaphoreType.DMA((2 * NZ,)), pltpu.SemaphoreType.DMA((2, 2 * NZ)),
                        pltpu.SemaphoreType.DMA((2 * NZ,)), pltpu.SemaphoreType.DMA((4, 2 * NZ))],
        compiler_params=pltpu.CompilerParams(collective_id=collective_id, has_side_effects=True),
        name="row_return",
    )(x)


def pair_kernel(x_ref, out_ref, send, recv):
    tp, dp, _, y = place()
    partner = tp + 1 - 2 * y
    signal(partner, dp)
    pl.semaphore_wait(pltpu.get_barrier_semaphore(), 1)
    copy = remote(x_ref, out_ref, send, recv, partner, dp)
    copy.start()
    copy.wait()


def pair_swap(x, collective_id):
    return pl.pallas_call(
        pair_kernel,
        out_shape=jax.ShapeDtypeStruct(x.shape, x.dtype),
        in_specs=[VMEM],
        out_specs=VMEM,
        scratch_shapes=[pltpu.SemaphoreType.DMA, pltpu.SemaphoreType.DMA],
        compiler_params=pltpu.CompilerParams(collective_id=collective_id, has_side_effects=True),
        name="pair_swap",
    )(x)


FORWARD = {
    0: {1: (("R", 1),), 3: (("R", 2),), 5: (("R", 3),)},
    1: {1: (("L", 0), ("R", 2)), 3: (("R", 3),)},
    2: {1: (("R", 3), ("L", 1)), 3: (("L", 0),)},
    3: {1: (("L", 2),), 3: (("L", 1),), 5: (("L", 0),)},
}
REDUCE = {
    0: {2: (3,), 4: (2,), 6: (1,), 7: (0,)},
    1: {4: (3,), 6: (2, 0), 7: (1,)},
    2: {4: (0,), 6: (1, 3), 7: (2,)},
    3: {2: (0,), 4: (1,), 6: (2,), 7: (3,)},
}
SUB = 256
GROUP = 6


def lookup(table, z, step):
    value = jnp.int32(0)
    for k in range(NZ):
        for s in range(2 * NZ):
            value = value + jnp.where((z == k) & (step == s), table[k][s], 0)
    return value


def head_kernel(scale, token_scale, f_ref, lab_ref, e_ref, dfin_ref, ghead_ref, norm_ref, labsum_ref,
                e_b, e_t, fbuf, f_b, g_acc, from_y, from_l, from_r, dl, lse_all, load_sem, ag_y, ag_l, ag_r, ag_recv,
                rs_y, rs_l, rs_r, recv_y, recv_l, recv_r, st_send, st_recv):
    tp, dp, z, y = place()
    partner = tp + 1 - 2 * y
    vocab, width = e_ref.shape
    own = f_ref.shape[0]
    whole = vocab // (SUB * GROUP)
    rest = vocab - whole * SUB * GROUP
    log2e = 1.4426950408889634
    slope = scale * log2e
    blocks = [(j * SUB, SUB) for j in range(GROUP)]
    tail = [(n, min(SUB, rest - n)) for n in range(0, rest, SUB)]

    plane_barrier(tp, dp, [])

    def send(src, slot, sems, to):
        remote(src, fbuf.at[slot], sems.at[slot], ag_recv.at[slot], to, dp).start()

    def arrived(slot):
        remote(f_ref, fbuf.at[slot], ag_y.at[slot], ag_recv.at[slot], partner, dp).wait_recv()

    def first_sends(k):
        if k > 0:
            send(f_ref, tp, ag_l, tp - 2)
        if k < NZ - 1:
            send(f_ref, tp, ag_r, tp + 2)
        send(f_ref, tp, ag_y, partner)

    for k in range(NZ):
        pl.when(z == k)(functools.partial(first_sends, k))
    load = pltpu.make_async_copy(e_ref, g_acc, load_sem.at[0])
    load.start()
    own_copy = pltpu.make_async_copy(f_ref, fbuf.at[tp], load_sem.at[1])
    own_copy.start()
    load.wait()

    def prepare(at, size):
        part = g_acc[at, :]
        e_b[at, :] = part.astype(BF16)
        e_t[:, at] = part.T.astype(BF16)

    def prepare_body(n, carry):
        prepare(pl.ds(pl.multiple_of(n * SUB, SUB), SUB), SUB)
        return carry

    lax.fori_loop(0, vocab // SUB, prepare_body, 0)
    if vocab % SUB:
        prepare(pl.ds(vocab // SUB * SUB, vocab % SUB), vocab % SUB)
    own_copy.wait()

    def over_blocks(group, carry):
        def body(n, c):
            return group(pl.multiple_of(n * SUB * GROUP, SUB * GROUP), blocks, c)
        carry = lax.fori_loop(0, whole, body, carry)
        return group(whole * SUB * GROUP, tail, carry) if tail else carry

    order1 = {k: (k,) + tuple(v for pair in zip([a[1] for a in ARRIVALS[k]], [k] + [a[1] for a in ARRIVALS[k]]) for v in pair) + (ARRIVALS[k][-1][1],) for k in range(NZ)}
    order1 = {k: [2 * zz + (s % 2 == 0 and s > 0 or s == 7) for s, zz in enumerate(order1[k])] for k in range(NZ)}

    def chunk_of(table, step):
        code = lookup(table, z, step)
        other = code % 2
        return code // 2 * 2 + y + other - 2 * y * other

    def gather_step(step, carry):
        slot = chunk_of(order1, step)
        for k in range(NZ):
            for s, shards in FORWARD[k].items():
                def pass_on(k=k, shards=shards):
                    for side, zz in shards:
                        at = 2 * zz + y
                        arrived(at)
                        if side == "L" and k < NZ - 1:
                            send(fbuf.at[at], at, ag_r, tp + 2)
                        if side == "R" and k > 0:
                            send(fbuf.at[at], at, ag_l, tp - 2)
                        send(fbuf.at[at], at, ag_y, partner)
                pl.when((z == k) & (step == s))(pass_on)
        pl.when(slot % 2 != y)(lambda: arrived(slot))
        f_b[slot] = fbuf[slot].astype(BF16)
        f_now = f_b[slot]

        def group(base, parts, c):
            top, total = c
            for first, size in parts:
                logit = lax.dot_general(e_b[pl.ds(base + first, size), :], f_now, (((1,), (1,)), ((), ())), preferred_element_type=F32)
                logit = logit.reshape(size // 8, 8, own)
                new = jnp.maximum(top, jnp.max(logit, axis=0))
                total = total * jnp.exp2((top - new) * slope) + jnp.sum(jnp.exp2((logit - new[None]) * slope), axis=0)
                top = new
            return top, total

        top, total = over_blocks(group, (jnp.full((8, own), -3e38, F32), jnp.zeros((8, own), F32)))
        most = jnp.max(top, axis=0, keepdims=True)
        total = jnp.sum(total * jnp.exp2((top - most) * slope), axis=0, keepdims=True)
        lse_all[tp, pl.ds(slot, 1), :] = most * scale + jnp.log(total)
        return carry

    lax.fori_loop(0, 2 * NZ, gather_step, 0)

    for n in range(1, 2 * NZ):
        to = lax.rem(tp + n, 2 * NZ)
        remote(lse_all.at[tp], lse_all.at[tp], st_send.at[to], st_recv.at[tp], to, dp).start()

    def gathers_done(k):
        def done(sems, slot):
            remote(f_ref, fbuf.at[slot], sems.at[slot], ag_recv.at[slot], partner, dp).wait_send()
        if k > 0:
            done(ag_l, tp)
        if k < NZ - 1:
            done(ag_r, tp)
        done(ag_y, tp)
        for side, zz in ARRIVALS[k]:
            at = 2 * zz + y
            if side == "L" and k < NZ - 1:
                done(ag_r, at)
            if side == "R" and k > 0:
                done(ag_l, at)
            done(ag_y, at)

    for k in range(NZ):
        pl.when(z == k)(functools.partial(gathers_done, k))

    def clear(n, carry):
        g_acc[pl.ds(pl.multiple_of(n * 16, 16), 16), :] = jnp.zeros((16, width), F32)
        return carry

    lax.fori_loop(0, vocab // 16, clear, 0)
    for n in range(1, 2 * NZ):
        source = lax.rem(tp + n, 2 * NZ)
        remote(lse_all.at[source], lse_all.at[source], st_send.at[source], st_recv.at[source], source, dp).wait_recv()
    peak = jnp.max(lse_all[...], axis=0)
    log_norm = peak + jnp.log(jnp.sum(jnp.exp(lse_all[...] - peak[None]), axis=0))
    norm_ref[...] = log_norm

    order2 = {k: [2 * zz + 1 - s for zz in REDUCE_ORDER[k] for s in range(2)] for k in range(NZ)}

    def scatter_step(step, lab_sum):
        slot = chunk_of(order2, step)
        f_now = f_b[slot]
        acc = fbuf.at[slot]
        norm = norm_ref[pl.ds(slot, 1), :]
        shift = norm * log2e
        coef = (1.0 + 2.0 * LOGIT_ZLOSS * norm) * token_scale
        lab = lab_ref[pl.ds(slot, 1), :]
        acc[...] = jnp.zeros((width, own), F32)

        def group(base, parts, hits):
            for first, size in parts:
                at = pl.ds(base + first, size)
                logit = lax.dot_general(e_b[at, :], f_now, (((1,), (1,)), ((), ())), preferred_element_type=F32)
                hit = lax.broadcasted_iota(jnp.int32, (size, own), 0) == lab - (base + first)
                prob = jnp.exp2(logit * slope - shift) * coef
                grad = jnp.where(hit, prob - token_scale, prob).astype(BF16)
                hits = hits + jnp.sum(jnp.where(hit, logit, 0.0).reshape(size // 8, 8, own), axis=0)
                dl[pl.ds(first, size), :] = grad
                g_acc[at, :] += jnp.dot(grad, f_now, preferred_element_type=F32)
            size = parts[-1][0] + parts[-1][1]
            acc[...] += jnp.dot(e_t[:, pl.ds(base, size)], dl[pl.ds(0, size), :], preferred_element_type=F32)
            return hits

        lab_sum = over_blocks(group, lab_sum)

        def hand_over():
            remote(acc, from_y.at[slot // 2], rs_y.at[slot // 2], recv_y.at[slot // 2], partner, dp).start()
        pl.when(slot % 2 != y)(hand_over)

        for k in range(NZ):
            for s, shards in REDUCE[k].items():
                def reduce(k=k, shards=shards):
                    for zz in shards:
                        line = fbuf.at[2 * zz + y]
                        remote(line, from_y.at[zz], rs_y.at[zz], recv_y.at[zz], partner, dp).wait_recv()
                        add_into(line, from_y.at[zz])
                        if zz >= k and k > 0:
                            remote(line, from_l.at[zz - 1], rs_l.at[zz], recv_l.at[zz], partner, dp).wait_recv()
                            add_into(line, from_l.at[zz - 1])
                        if zz <= k and k < NZ - 1:
                            remote(line, from_r.at[zz], rs_r.at[zz], recv_r.at[zz], partner, dp).wait_recv()
                            add_into(line, from_r.at[zz])
                        if zz > k:
                            remote(line, from_l.at[zz - 1], rs_r.at[zz], recv_l.at[zz], tp + 2, dp).start()
                        if zz < k:
                            remote(line, from_r.at[zz], rs_l.at[zz], recv_r.at[zz], tp - 2, dp).start()
                pl.when((z == k) & (step == s))(reduce)
        return lab_sum

    lab_sum = lax.fori_loop(0, 2 * NZ, scatter_step, jnp.zeros((8, own), F32))
    labsum_ref[...] = lab_sum
    store = pltpu.make_async_copy(g_acc, ghead_ref, load_sem.at[0])
    store.start()
    dfin_ref[...] = fbuf[tp].T

    def scatters_done(k):
        for zz in range(NZ):
            line = fbuf.at[2 * zz + y]
            remote(line, from_y.at[zz], rs_y.at[zz], recv_y.at[zz], partner, dp).wait_send()
            if zz > k:
                remote(line, from_l.at[zz - 1], rs_r.at[zz], recv_l.at[zz], partner, dp).wait_send()
            if zz < k:
                remote(line, from_r.at[zz], rs_l.at[zz], recv_r.at[zz], partner, dp).wait_send()

    for k in range(NZ):
        pl.when(z == k)(functools.partial(scatters_done, k))
    for n in range(1, 2 * NZ):
        to = lax.rem(tp + n, 2 * NZ)
        remote(lse_all.at[tp], lse_all.at[tp], st_send.at[to], st_recv.at[tp], to, dp).wait_send()
    store.wait()


def head(f_own, labels, embed, scale, token_scale, collective_id):
    own, width = f_own.shape
    vocab = embed.shape[0]
    chunk = (own, width)
    dma8 = pltpu.SemaphoreType.DMA((2 * NZ,))
    dma4 = pltpu.SemaphoreType.DMA((NZ,))
    return pl.pallas_call(
        functools.partial(head_kernel, scale, token_scale),
        out_shape=(jax.ShapeDtypeStruct((own, width), F32), jax.ShapeDtypeStruct((vocab, width), F32),
                   jax.ShapeDtypeStruct((2 * NZ, own), F32), jax.ShapeDtypeStruct((8, own), F32)),
        in_specs=[VMEM, VMEM, ANY],
        out_specs=(VMEM, ANY, VMEM, VMEM),
        scratch_shapes=[pltpu.VMEM((vocab, width), BF16), pltpu.VMEM((width, vocab), BF16),
                        pltpu.VMEM((2 * NZ,) + chunk, F32), pltpu.VMEM((2 * NZ,) + chunk, BF16), pltpu.VMEM((vocab, width), F32),
                        pltpu.VMEM((NZ,) + chunk, F32), pltpu.VMEM((NZ - 1,) + chunk, F32), pltpu.VMEM((NZ - 1,) + chunk, F32),
                        pltpu.VMEM((SUB * GROUP, own), BF16), pltpu.VMEM((2 * NZ, 2 * NZ, own), F32),
                        pltpu.SemaphoreType.DMA((2,)), dma8, dma8, dma8, dma8, dma4, dma4, dma4, dma4, dma4, dma4, dma8, dma8],
        compiler_params=pltpu.CompilerParams(collective_id=collective_id, has_side_effects=True, vmem_limit_bytes=67000000),
        cost_estimate=pl.CostEstimate(flops=8 * vocab * width * own * 8, bytes_accessed=3 * 4 * vocab * width, transcendentals=2 * vocab * own * 8),
        name="head",
    )(f_own, labels, embed)


def norm_fwd(x_f32, scale):
    centered = x_f32 - jnp.mean(x_f32, axis=-1, keepdims=True)
    inv_std = lax.rsqrt(jnp.mean(centered * centered, axis=-1, keepdims=True) + LN_EPS)
    x_hat = centered * inv_std
    return (x_hat * scale).astype(BF16), x_hat, inv_std


def norm_bwd(d_out, x_hat, inv_std, scale):
    d_scale = jnp.sum(d_out * x_hat, axis=0)
    d_hat = d_out * scale
    d_in = inv_std * (d_hat - jnp.mean(d_hat, axis=-1, keepdims=True) - x_hat * jnp.mean(d_hat * x_hat, axis=-1, keepdims=True))
    return d_in, d_scale


def rope_tables(positions, head_dim):
    inv_freq = ROPE_BASE ** (-jnp.arange(0, head_dim, 2).astype(F32) / head_dim)
    angles = positions.astype(F32)[:, None] * inv_freq[None, :]
    return jnp.cos(angles), jnp.sin(angles)


def rotate(x_in, cos_t, sin_t):
    half_dim = x_in.shape[-1] // 2
    x_lo = x_in[..., :half_dim]
    x_hi = x_in[..., half_dim:]
    return jnp.concatenate([x_lo * cos_t - x_hi * sin_t, x_hi * cos_t + x_lo * sin_t], axis=-1)


def adam_update(param_in, grad_in, mom_in, vel_in):
    mom_new = BETA_ONE * mom_in + (1.0 - BETA_ONE) * grad_in
    vel_new = BETA_TWO * vel_in + (1.0 - BETA_TWO) * grad_in * grad_in
    return param_in - LEARN_RATE * mom_new / (jnp.sqrt(vel_new) + ADAM_EPS), mom_new, vel_new


def dot(spec, a, b):
    return jnp.einsum(spec, a, b, preferred_element_type=F32)


def solution(mesh):
    param_specs = (P('tp', None), P(None, None), P(None, 'tp'), P(None, None, None), P('tp', None), P(None, None, 'tp'), P('tp', None))
    n_tp = mesh.shape['tp']
    n_dp = mesh.shape['dp']

    def local_step(tokens, labels, *state_arrays):
        embed, ln_scales, w_q, w_kv, w_o, w_gu, w_down = state_arrays[0:7]
        batch_loc, seq_len = tokens.shape
        vocab_loc, d_model = embed.shape
        head_dim = w_kv.shape[2]
        q_loc = w_q.shape[1]
        f_loc = w_down.shape[0]
        heads = n_tp * q_loc // head_dim
        tok_loc = batch_loc * seq_len
        tok_total = tok_loc * n_dp
        own = tok_loc // n_tp
        tp_rank = lax.axis_index('tp')
        half = tp_rank % 2

        all_tokens = lax.all_gather(tokens, 'dp').reshape(n_dp * n_tp, own)
        strict = (jnp.arange(own)[:, None] > jnp.arange(own)[None, :]).astype(BF16)

        def routing(chunks):
            shard = chunks // vocab_loc
            row = chunks - shard * vocab_loc
            hot = (shard[:, :, None] == jnp.arange(n_tp)[None, None, :])
            before = dot('rs,nsj->nrj', strict, hot.astype(BF16))
            rank = jnp.sum(jnp.where(hot, before, 0.0), axis=-1).astype(jnp.int32)
            most = jnp.max(jnp.sum(hot.astype(jnp.int32), axis=1))
            return shard, row, rank, (most + CAP - 1) // CAP

        chunks = tokens.reshape(n_tp, own)
        shard, row, rank, _ = routing(chunks)
        shard_all, row_all, rank_all, rounds_all = routing(all_tokens)
        slots = jnp.arange(CAP)
        my_shard = lax.dynamic_index_in_dim(shard, tp_rank, 0, keepdims=False)
        my_rank = lax.dynamic_index_in_dim(rank, tp_rank, 0, keepdims=False)

        def fetch(step, x_sum, collective_id):
            here = (shard[:, None, :] == tp_rank) & (rank[:, None, :] == slots[None, :, None] + step * CAP)
            ids = jnp.sum(jnp.where(here, row[:, None, :], 0), axis=-1).reshape(-1)
            rows_out = jnp.take(embed, ids, axis=0).astype(BF16).astype(F32).reshape(n_tp, CAP, d_model)
            rows_in = plane_swap(rows_out, False, collective_id).reshape(n_tp * CAP, d_model).astype(BF16)
            pick = (my_shard[:, None, None] == jnp.arange(n_tp)[None, :, None]) & (my_rank[:, None, None] == slots[None, None, :] + step * CAP)
            return x_sum + dot('rc,cd->rd', pick.reshape(own, n_tp * CAP).astype(BF16), rows_in)

        x_zero = fetch(0, jnp.zeros((own, d_model), F32), 0)
        x_zero = lax.while_loop(lambda s: s[0] < rounds_all, lambda s: (s[0] + 1, fetch(s[0], s[1], 1)), (jnp.int32(1), x_zero))[1]

        w_rows = jnp.concatenate([w_q.T, w_o, w_gu.transpose(0, 2, 1).reshape(2 * f_loc, d_model), w_down], axis=0)
        w_all = weight_gather(w_rows, 2).astype(BF16)
        cuts = (q_loc, 2 * q_loc, 2 * q_loc + f_loc, 2 * q_loc + 2 * f_loc)
        wq_t = w_all[:, :cuts[0]].reshape(-1, d_model)
        wo_b = w_all[:, cuts[0]:cuts[1]].reshape(-1, d_model)
        wg_t = w_all[:, cuts[1]:cuts[2]].reshape(-1, d_model)
        wu_t = w_all[:, cuts[2]:cuts[3]].reshape(-1, d_model)
        wd_b = w_all[:, cuts[3]:].reshape(-1, d_model)
        wkv_b = w_kv.astype(BF16)

        u_norm, u_hat, u_inv = norm_fwd(x_zero, ln_scales[0])
        q_pos = half * own + jnp.arange(own)
        cos_t, sin_t = rope_tables(q_pos, head_dim)
        q_raw = dot('rd,nd->rn', u_norm, wq_t).reshape(own, heads, head_dim)
        queries = rotate(q_raw, cos_t[:, None, :], sin_t[:, None, :]).astype(BF16)
        kv_raw = dot('rd,cde->cre', u_norm, wkv_b)
        kv_own = jnp.concatenate([rotate(kv_raw[0], cos_t, sin_t), kv_raw[1]], axis=-1)
        kv_other = pair_swap(kv_own, 3)
        kv_seq = jnp.concatenate([jnp.where(half == 0, kv_own, kv_other), jnp.where(half == 0, kv_other, kv_own)], axis=0).astype(BF16)
        keys = kv_seq[:, :head_dim]
        values = kv_seq[:, head_dim:]
        causal = q_pos[:, None] >= jnp.arange(2 * own)[None, :]
        scores = dot('qhe,ke->hqk', queries, keys) * head_dim ** -0.5
        prob_f32 = jax.nn.softmax(jnp.where(causal, scores, -1e30), axis=-1)
        prob_b16 = prob_f32.astype(BF16)
        context = dot('hqk,ke->qhe', prob_b16, values).astype(BF16).reshape(own, heads * head_dim)
        att_out = dot('rf,fe->re', context, wo_b)
        gate = dot('rd,fd->rf', u_norm, wg_t)
        up = dot('rd,fd->rf', u_norm, wu_t)
        gate_sig = jax.nn.sigmoid(gate)
        hidden = (gate * gate_sig * up).astype(BF16)
        x_one = x_zero + att_out + dot('rf,fd->rd', hidden, wd_b)
        f_own, f_hat, f_inv = norm_fwd(x_one, ln_scales[1])

        logit_scale = d_model ** -0.5
        lab_loc = labels.reshape(n_tp, own) - tp_rank * vocab_loc
        d_fin, g_head_part, log_norm, lab_sum = head(f_own.astype(F32), lab_loc, embed, logit_scale, logit_scale / tok_total, 4)
        log_norm = lax.dynamic_index_in_dim(log_norm, tp_rank, 0, keepdims=False)
        loss_part = (jnp.sum(log_norm + LOGIT_ZLOSS * log_norm * log_norm) - jnp.sum(lab_sum) * logit_scale) / tok_total
        g_head = lax.psum(g_head_part, 'dp')
        d_one, g_ln_fin = norm_bwd(d_fin, f_hat, f_inv, ln_scales[1])
        d_one_b = d_one.astype(BF16)

        d_hidden = dot('rd,fd->rf', d_one_b, wd_b)
        g_down = dot('rf,rd->fd', hidden, d_one_b)
        d_gate = (d_hidden * up * gate_sig * (1.0 + gate * (1.0 - gate_sig))).astype(BF16)
        d_up = (d_hidden * gate * gate_sig).astype(BF16)
        g_gate = dot('rf,rd->fd', d_gate, u_norm)
        g_up = dot('rf,rd->fd', d_up, u_norm)
        d_u_mlp = dot('rf,fd->rd', d_gate, wg_t) + dot('rf,fd->rd', d_up, wu_t)

        d_context = dot('re,fe->rf', d_one_b, wo_b).astype(BF16).reshape(own, heads, head_dim)
        g_o = dot('rf,re->fe', context, d_one_b)
        d_probs = dot('qhe,ke->hqk', d_context, values)
        d_values = dot('hqk,qhe->ke', prob_b16, d_context)
        d_scores = (prob_f32 * (d_probs - jnp.sum(d_probs * prob_f32, axis=-1, keepdims=True)) * head_dim ** -0.5).astype(BF16)
        d_queries = dot('hqk,ke->qhe', d_scores, keys)
        d_keys = dot('hqk,qhe->ke', d_scores, queries)
        d_kv_seq = jnp.concatenate([d_keys, d_values], axis=-1)
        d_kv_lo = d_kv_seq[:own]
        d_kv_hi = d_kv_seq[own:]
        d_kv_own = jnp.where(half == 0, d_kv_lo, d_kv_hi) + pair_swap(jnp.where(half == 0, d_kv_hi, d_kv_lo), 7)
        d_q_raw = rotate(d_queries, cos_t[:, None, :], -sin_t[:, None, :]).astype(BF16).reshape(own, heads * head_dim)
        d_kv = jnp.stack([rotate(d_kv_own[:, :head_dim], cos_t, -sin_t), d_kv_own[:, head_dim:]]).astype(BF16)
        g_q_t = dot('rn,rd->nd', d_q_raw, u_norm)
        g_kv_part = dot('cre,rd->cde', d_kv, u_norm)
        d_u = dot('rn,nd->rd', d_q_raw, wq_t) + dot('cre,cde->rd', d_kv, wkv_b) + d_u_mlp
        d_zero_norm, g_ln_in = norm_bwd(d_u, u_hat, u_inv, ln_scales[0])
        d_zero = d_one + d_zero_norm

        my_row_shard = my_shard

        def give_back(step, g_look, collective_id):
            mine = (my_row_shard[None, None, :] == jnp.arange(n_tp)[:, None, None]) & (my_rank[None, None, :] == slots[None, :, None] + step * CAP)
            ids = jnp.sum(jnp.where(mine, jnp.arange(own)[None, None, :], 0), axis=-1).reshape(-1)
            rows_out = jnp.take(d_zero, ids, axis=0).reshape(n_tp, CAP, d_model)
            rows_in = row_return(rows_out, collective_id).reshape(-1, d_model)
            here = (shard_all[:, None, :] == tp_rank) & (rank_all[:, None, :] == slots[None, :, None] + step * CAP)
            row_id = jnp.where(jnp.any(here, axis=-1), jnp.sum(jnp.where(here, row_all[:, None, :], 0), axis=-1), vocab_loc).reshape(-1)
            return g_look.at[row_id].add(rows_in, mode='drop')

        g_look = give_back(0, jnp.zeros((vocab_loc, d_model), F32), 8)
        g_look = lax.while_loop(lambda s: s[0] < rounds_all, lambda s: (s[0] + 1, give_back(s[0], s[1], 9)), (jnp.int32(1), g_look))[1]

        g_gu_t = jnp.stack([g_gate.reshape(n_tp, f_loc, d_model), g_up.reshape(n_tp, f_loc, d_model)], axis=1)
        g_rows = jnp.concatenate([g_q_t.reshape(n_tp, q_loc, d_model), g_o.reshape(n_tp, q_loc, d_model),
                                  g_gu_t.reshape(n_tp, 2 * f_loc, d_model), g_down.reshape(n_tp, f_loc, d_model)], axis=1)
        g_shard = weight_scatter(g_rows, 10)
        g_kv, g_ln, loss = lax.psum((g_kv_part, jnp.stack([g_ln_in, g_ln_fin]), loss_part), ('tp', 'dp'))
        gradients = (g_head + g_look, g_ln, g_shard[:cuts[0]].T, g_kv, g_shard[cuts[0]:cuts[1]],
                     g_shard[cuts[1]:cuts[3]].reshape(2, f_loc, d_model).transpose(0, 2, 1), g_shard[cuts[3]:])

        outs_p = []
        outs_m = []
        outs_v = []
        for index in range(7):
            new_p, new_m, new_v = adam_update(state_arrays[index], gradients[index], state_arrays[7 + index], state_arrays[14 + index])
            outs_p.append(new_p)
            outs_m.append(new_m)
            outs_v.append(new_v)
        return tuple(outs_p) + tuple(outs_m) + tuple(outs_v) + (loss,)

    return jax.shard_map(local_step, mesh=mesh, in_specs=(P('dp', None), P('dp', None)) + param_specs * 3,
                         out_specs=param_specs * 3 + (P(),), check_vma=False)
```

```python
import functools

import jax
import jax.numpy as jnp
from jax import lax
from jax.experimental import pallas as pl
from jax.experimental.pallas import tpu as pltpu
from jax.sharding import PartitionSpec as P

LN_EPS = 1e-5
LOGIT_ZLOSS = 1e-4
LEARN_RATE = 1e-2
BETA_ONE = 0.9
BETA_TWO = 0.95
ADAM_EPS = 1e-8
ROPE_BASE = 10000.0
NZ = 4
CAP = 96
F32 = jnp.float32
BF16 = jnp.bfloat16
ANY = pl.BlockSpec(memory_space=pl.ANY)
VMEM = pl.BlockSpec(memory_space=pltpu.VMEM)

ARRIVALS = {
    0: (("R", 1), ("R", 2), ("R", 3)),
    1: (("L", 0), ("R", 2), ("R", 3)),
    2: (("R", 3), ("L", 1), ("L", 0)),
    3: (("L", 2), ("L", 1), ("L", 0)),
}
REDUCE_ORDER = {0: (3, 2, 1, 0), 1: (3, 0, 2, 1), 2: (0, 3, 1, 2), 3: (0, 1, 2, 3)}


def remote(src, dst, send_sem, recv_sem, tp, dp):
    return pltpu.make_async_remote_copy(src_ref=src, dst_ref=dst, send_sem=send_sem, recv_sem=recv_sem,
                                        device_id=(tp, dp), device_id_type=pl.DeviceIdType.MESH)


def place():
    tp = lax.axis_index("tp")
    dp = lax.axis_index("dp")
    return tp, dp, tp // 2, tp % 2


def signal(tp, dp):
    pl.semaphore_signal(pltpu.get_barrier_semaphore(), inc=1, device_id=(tp, dp), device_id_type=pl.DeviceIdType.MESH)


def line_barrier(k, tp, dp, others):
    peers = [(tp + 1 - 2 * (tp % 2), dp)] + others
    if k > 0:
        peers.append((tp - 2, dp))
    if k < NZ - 1:
        peers.append((tp + 2, dp))
    for peer in peers:
        signal(*peer)
    pl.semaphore_wait(pltpu.get_barrier_semaphore(), len(peers))


def gather_kernel(x_ref, out_ref, own_sem, send_y, send_l, send_r, recv):
    tp, dp, z, y = place()
    partner = tp + 1 - 2 * y

    def program(k):
        line_barrier(k, tp, dp, [])

        def send(src, slot, sems, to):
            copy = remote(src, out_ref.at[slot], sems.at[slot], recv.at[slot], to, dp)
            copy.start()
            return copy

        def arrived(slot):
            remote(x_ref, out_ref.at[slot], send_y.at[slot], recv.at[slot], partner, dp).wait_recv()

        sends = []
        if k > 0:
            sends.append(send(x_ref, tp, send_l, tp - 2))
        if k < NZ - 1:
            sends.append(send(x_ref, tp, send_r, tp + 2))
        sends.append(send(x_ref, tp, send_y, partner))
        own = pltpu.make_async_copy(x_ref, out_ref.at[tp], own_sem)
        own.start()
        for side, zz in ARRIVALS[k]:
            slot = 2 * zz + y
            arrived(slot)
            if side == "L" and k < NZ - 1:
                sends.append(send(out_ref.at[slot], slot, send_r, tp + 2))
            if side == "R" and k > 0:
                sends.append(send(out_ref.at[slot], slot, send_l, tp - 2))
            sends.append(send(out_ref.at[slot], slot, send_y, partner))
        for zz in range(NZ):
            arrived(2 * zz + 1 - y)
        own.wait()
        for copy in sends:
            copy.wait_send()

    for k in range(NZ):
        pl.when(z == k)(functools.partial(program, k))


def plane_gather(x, collective_id):
    return pl.pallas_call(
        gather_kernel,
        out_shape=jax.ShapeDtypeStruct((2 * NZ,) + x.shape, x.dtype),
        in_specs=[ANY],
        out_specs=ANY,
        scratch_shapes=[pltpu.SemaphoreType.DMA] + [pltpu.SemaphoreType.DMA((2 * NZ,))] * 4,
        compiler_params=pltpu.CompilerParams(collective_id=collective_id, has_side_effects=True),
        name="plane_gather",
    )(x)


def weight_gather_kernel(x_ref, out_ref, own_sem, send_y, send_l, send_r, send_c, recv):
    tp, dp, z, y = place()
    partner = tp + 1 - 2 * y
    core = dp % 2
    twin = dp + 1 - 2 * core

    def program(k):
        line_barrier(k, tp, dp, [(tp, twin)])

        def send(src, slot, sems, to, to_dp):
            copy = remote(src, out_ref.at[slot, core], sems.at[slot], recv.at[slot, core], to, to_dp)
            copy.start()
            return copy

        def arrived(slot, half):
            remote(x_ref.at[0], out_ref.at[slot, half], send_y.at[slot], recv.at[slot, half], partner, dp).wait_recv()

        mine = x_ref.at[core]
        sends = []
        if k > 0:
            sends.append(send(mine, tp, send_l, tp - 2, dp))
        if k < NZ - 1:
            sends.append(send(mine, tp, send_r, tp + 2, dp))
        sends.append(send(mine, tp, send_y, partner, dp))
        own = pltpu.make_async_copy(x_ref, out_ref.at[tp], own_sem)
        own.start()
        across = [k] + [zz for _, zz in ARRIVALS[k]]
        for n, (side, zz) in enumerate(ARRIVALS[k]):
            slot = 2 * zz + y
            arrived(slot, core)
            if side == "L" and k < NZ - 1:
                sends.append(send(out_ref.at[slot, core], slot, send_r, tp + 2, dp))
            if side == "R" and k > 0:
                sends.append(send(out_ref.at[slot, core], slot, send_l, tp - 2, dp))
            sends.append(send(out_ref.at[slot, core], slot, send_y, partner, dp))
            sends.append(send(out_ref.at[slot, core], slot, send_c, tp, twin))
            slot = 2 * across[n] + 1 - y
            arrived(slot, core)
            sends.append(send(out_ref.at[slot, core], slot, send_c, tp, twin))
        slot = 2 * across[-1] + 1 - y
        arrived(slot, core)
        sends.append(send(out_ref.at[slot, core], slot, send_c, tp, twin))
        for zz in range(NZ):
            if zz != k:
                arrived(2 * zz + y, 1 - core)
            arrived(2 * zz + 1 - y, 1 - core)
        own.wait()
        for copy in sends:
            copy.wait_send()

    for k in range(NZ):
        pl.when(z == k)(functools.partial(program, k))


def weight_gather(x, collective_id):
    rows, width = x.shape
    halves = x.reshape(2, rows // 2, width)
    out = pl.pallas_call(
        weight_gather_kernel,
        out_shape=jax.ShapeDtypeStruct((2 * NZ,) + halves.shape, x.dtype),
        in_specs=[ANY],
        out_specs=ANY,
        scratch_shapes=[pltpu.SemaphoreType.DMA] + [pltpu.SemaphoreType.DMA((2 * NZ,))] * 4
        + [pltpu.SemaphoreType.DMA((2 * NZ, 2))],
        compiler_params=pltpu.CompilerParams(collective_id=collective_id, has_side_effects=True),
        name="weight_gather",
    )(halves)
    return out.reshape(2 * NZ, rows, width)


def add_into(acc, other):
    rows = acc.shape[0]
    step = 64 if rows % 64 == 0 else rows

    def body(n, carry):
        at = pl.ds(pl.multiple_of(n * step, step), step)
        acc[at, :] = acc[at, :] + other[at, :]
        return carry

    lax.fori_loop(0, rows // step, body, 0)


def scatter_kernel(p_ref, out_ref, acc, from_y, from_l, from_r, load_sem, out_sem, send_y, send_l, send_r, recv_y, recv_l, recv_r):
    tp, dp, z, y = place()
    partner = tp + 1 - 2 * y

    def program(k):
        line_barrier(k, tp, dp, [])
        sends = []
        loads = []
        for zz in REDUCE_ORDER[k]:
            copy = remote(p_ref.at[2 * zz + 1 - y], from_y.at[zz], send_y.at[zz], recv_y.at[zz], partner, dp)
            copy.start()
            sends.append(copy)
        for zz in REDUCE_ORDER[k]:
            load = pltpu.make_async_copy(p_ref.at[2 * zz + y], acc.at[zz], load_sem.at[zz])
            load.start()
            loads.append(load)
        for n, zz in enumerate(REDUCE_ORDER[k]):
            loads[n].wait()
            remote(acc.at[zz], from_y.at[zz], send_y.at[zz], recv_y.at[zz], partner, dp).wait_recv()
            add_into(acc.at[zz], from_y.at[zz])
            if zz >= k and k > 0:
                remote(acc.at[zz], from_l.at[zz], send_l.at[zz], recv_l.at[zz], partner, dp).wait_recv()
                add_into(acc.at[zz], from_l.at[zz])
            if zz <= k and k < NZ - 1:
                remote(acc.at[zz], from_r.at[zz], send_r.at[zz], recv_r.at[zz], partner, dp).wait_recv()
                add_into(acc.at[zz], from_r.at[zz])
            if zz > k:
                copy = remote(acc.at[zz], from_l.at[zz], send_r.at[zz], recv_l.at[zz], tp + 2, dp)
                copy.start()
                sends.append(copy)
            if zz < k:
                copy = remote(acc.at[zz], from_r.at[zz], send_l.at[zz], recv_r.at[zz], tp - 2, dp)
                copy.start()
                sends.append(copy)
        out = pltpu.make_async_copy(acc.at[k], out_ref, out_sem)
        out.start()
        out.wait()
        for copy in sends:
            copy.wait_send()

    for k in range(NZ):
        pl.when(z == k)(functools.partial(program, k))


def plane_scatter(p, collective_id):
    _, rows, width = p.shape
    line = (NZ, rows, width)
    return pl.pallas_call(
        scatter_kernel,
        out_shape=jax.ShapeDtypeStruct((rows, width), p.dtype),
        in_specs=[ANY],
        out_specs=ANY,
        scratch_shapes=[pltpu.VMEM(line, p.dtype)] * 4
        + [pltpu.SemaphoreType.DMA((NZ,)), pltpu.SemaphoreType.DMA]
        + [pltpu.SemaphoreType.DMA((NZ,))] * 6,
        compiler_params=pltpu.CompilerParams(collective_id=collective_id, has_side_effects=True),
        name="plane_scatter",
    )(p)


def weight_scatter_kernel(p_ref, out_ref, small_ref, acc, from_c, from_y, from_l, from_r, from_x, load_sem, out_sem, send_c, send_y, send_l, send_r,
                          last_send, recv_c, recv_y, recv_l, recv_r, last_recv, small_send, small_recv):
    tp, dp, z, y = place()
    partner = tp + 1 - 2 * y
    core = dp % 2
    twin = dp + 1 - 2 * core
    facing = lax.rem(dp + 2, 4)

    def program(k):
        plane_barrier(tp, dp, [(tp, twin), (tp, facing)])
        sends = []
        for zz in REDUCE_ORDER[k]:
            for slot in (2 * zz + 1 - y, 2 * zz + y):
                copy = remote(p_ref.at[slot, 1 - core], from_c.at[slot], send_c.at[slot], recv_c.at[slot], tp, twin)
                copy.start()
                sends.append(copy)
                pltpu.make_async_copy(p_ref.at[slot, core], acc.at[slot], load_sem.at[slot]).start()

        def chip_sum(slot):
            pltpu.make_async_copy(p_ref.at[slot, core], acc.at[slot], load_sem.at[slot]).wait()
            remote(acc.at[slot], from_c.at[slot], send_c.at[slot], recv_c.at[slot], tp, twin).wait_recv()
            add_into(acc.at[slot], from_c.at[slot])

        for zz in REDUCE_ORDER[k]:
            slot = 2 * zz + 1 - y
            chip_sum(slot)
            copy = remote(acc.at[slot], from_y.at[zz], send_y.at[zz], recv_y.at[zz], partner, dp)
            copy.start()
            sends.append(copy)
        for zz in REDUCE_ORDER[k]:
            chip_sum(2 * zz + y)
        for zz in REDUCE_ORDER[k]:
            slot = 2 * zz + y
            line = acc.at[slot]
            remote(line, from_y.at[zz], send_y.at[zz], recv_y.at[zz], partner, dp).wait_recv()
            add_into(line, from_y.at[zz])
            if zz >= k and k > 0:
                remote(line, from_l.at[zz], send_l.at[zz], recv_l.at[zz], partner, dp).wait_recv()
                add_into(line, from_l.at[zz])
            if zz <= k and k < NZ - 1:
                remote(line, from_r.at[zz], send_r.at[zz], recv_r.at[zz], partner, dp).wait_recv()
                add_into(line, from_r.at[zz])
            if zz > k:
                copy = remote(line, from_l.at[zz], send_r.at[zz], recv_l.at[zz], tp + 2, dp)
                copy.start()
                sends.append(copy)
            if zz < k:
                copy = remote(line, from_r.at[zz], send_l.at[zz], recv_r.at[zz], tp - 2, dp)
                copy.start()
                sends.append(copy)
        total = acc.at[2 * k + y]
        copy = remote(total, from_x, last_send.at[0], last_recv.at[0], tp, facing)
        copy.start()
        copy.wait()
        add_into(total, from_x)
        copy = remote(total, out_ref.at[core], last_send.at[1], last_recv.at[1], tp, twin)
        copy.start()
        out = pltpu.make_async_copy(total, out_ref.at[core], out_sem)
        out.start()
        copy.wait_send()
        remote(total, out_ref.at[1 - core], last_send.at[1], last_recv.at[1], tp, twin).wait_recv()
        out.wait()

        n_small, n_rows = small_ref.shape[1], out_ref.shape[1]
        mine = out_ref.at[1, pl.ds(n_rows - 32, n_small), :]
        for n in range(1, 2 * NZ):
            to = lax.rem(tp + n, 2 * NZ)
            copy = remote(mine, small_ref.at[tp], small_send.at[to], small_recv.at[tp], to, dp)
            copy.start()
            sends.append(copy)
        here = pltpu.make_async_copy(mine, small_ref.at[tp], out_sem)
        here.start()
        for n in range(1, 2 * NZ):
            source = lax.rem(tp + n, 2 * NZ)
            remote(small_ref.at[source], small_ref.at[source], small_send.at[source], small_recv.at[source], source, dp).wait_recv()
        here.wait()
        for copy in sends:
            copy.wait_send()

    for k in range(NZ):
        pl.when(z == k)(functools.partial(program, k))


def weight_scatter(p, collective_id):
    _, rows, width = p.shape
    half = (rows // 2, width)
    out, small = pl.pallas_call(
        weight_scatter_kernel,
        out_shape=(jax.ShapeDtypeStruct((2,) + half, p.dtype), jax.ShapeDtypeStruct((2 * NZ, 24, width), p.dtype)),
        in_specs=[ANY],
        out_specs=(ANY, ANY),
        scratch_shapes=[pltpu.VMEM((2 * NZ,) + half, p.dtype)] * 2 + [pltpu.VMEM((NZ,) + half, p.dtype)] * 3
        + [pltpu.VMEM(half, p.dtype)]
        + [pltpu.SemaphoreType.DMA((2 * NZ,)), pltpu.SemaphoreType.DMA]
        + ([pltpu.SemaphoreType.DMA((2 * NZ,))] + [pltpu.SemaphoreType.DMA((NZ,))] * 3 + [pltpu.SemaphoreType.DMA((2,))]) * 2
        + [pltpu.SemaphoreType.DMA((2 * NZ,))] * 2,
        compiler_params=pltpu.CompilerParams(collective_id=collective_id, has_side_effects=True),
        name="weight_scatter",
    )(p.reshape((2 * NZ, 2) + half))
    return out.reshape(rows, width), small


def plane_barrier(tp, dp, others):
    peers = [(lax.rem(tp + n, 2 * NZ), dp) for n in range(1, 2 * NZ)] + others
    for peer in peers:
        signal(*peer)
    pl.semaphore_wait(pltpu.get_barrier_semaphore(), len(peers))


def swap_kernel(spread, x_ref, out_ref, own_sem, send, recv):
    tp, dp, _, _ = place()
    plane_barrier(tp, dp, [])
    copies = []
    for n in range(1, 2 * NZ):
        to = lax.rem(tp + n, 2 * NZ)
        copy = remote(x_ref if spread else x_ref.at[to], out_ref.at[tp], send.at[to], recv.at[tp], to, dp)
        copy.start()
        copies.append(copy)
    own = pltpu.make_async_copy(x_ref if spread else x_ref.at[tp], out_ref.at[tp], own_sem)
    own.start()
    for n in range(1, 2 * NZ):
        source = lax.rem(tp + n, 2 * NZ)
        remote(out_ref.at[source], out_ref.at[source], send.at[source], recv.at[source], source, dp).wait_recv()
    own.wait()
    for copy in copies:
        copy.wait_send()


def plane_swap(x, spread, collective_id):
    return pl.pallas_call(
        functools.partial(swap_kernel, spread),
        out_shape=jax.ShapeDtypeStruct((2 * NZ,) + x.shape if spread else x.shape, x.dtype),
        in_specs=[ANY],
        out_specs=ANY,
        scratch_shapes=[pltpu.SemaphoreType.DMA] + [pltpu.SemaphoreType.DMA((2 * NZ,))] * 2,
        compiler_params=pltpu.CompilerParams(collective_id=collective_id, has_side_effects=True),
        name="plane_spread" if spread else "plane_swap",
    )(x)


def row_return_kernel(x_ref, out_ref, own_sem, send, send_c, send_x, recv):
    tp, dp, _, _ = place()
    core = dp % 2
    twin = dp + 1 - 2 * core
    facing = lax.rem(dp + 2, 4)
    plane_barrier(tp, dp, [(tp, twin), (tp, facing)])
    copies = []

    def forward(group, source, sems, to_dp):
        copy = remote(out_ref.at[group, source], out_ref.at[group, source], sems.at[source], recv.at[group, source], tp, to_dp)
        copy.start()
        copies.append(copy)

    def arrived(group, source):
        remote(out_ref.at[group, source], out_ref.at[group, source], send.at[source], recv.at[group, source], tp, twin).wait_recv()

    for n in range(1, 2 * NZ):
        to = lax.rem(tp + n, 2 * NZ)
        copy = remote(x_ref.at[to], out_ref.at[dp, tp], send.at[to], recv.at[dp, tp], to, dp)
        copy.start()
        copies.append(copy)
    own = pltpu.make_async_copy(x_ref.at[tp], out_ref.at[dp, tp], own_sem)
    own.start()
    own.wait()
    forward(dp, tp, send_x, facing)
    forward(dp, tp, send_c.at[0], twin)
    for n in range(1, 2 * NZ):
        source = lax.rem(tp + 2 * NZ - n, 2 * NZ)
        arrived(dp, source)
        forward(dp, source, send_x, facing)
        forward(dp, source, send_c.at[0], twin)
    for n in range(2 * NZ):
        source = lax.rem(tp + 2 * NZ - n, 2 * NZ)
        arrived(facing, source)
        forward(facing, source, send_c.at[1], twin)
    for n in range(2 * NZ):
        source = lax.rem(tp + 2 * NZ - n, 2 * NZ)
        arrived(twin, source)
        arrived(lax.rem(twin + 2, 4), source)
    for copy in copies:
        copy.wait_send()


def row_return(x, collective_id):
    return pl.pallas_call(
        row_return_kernel,
        out_shape=jax.ShapeDtypeStruct((4,) + x.shape, x.dtype),
        in_specs=[ANY],
        out_specs=ANY,
        scratch_shapes=[pltpu.SemaphoreType.DMA, pltpu.SemaphoreType.DMA((2 * NZ,)), pltpu.SemaphoreType.DMA((2, 2 * NZ)),
                        pltpu.SemaphoreType.DMA((2 * NZ,)), pltpu.SemaphoreType.DMA((4, 2 * NZ))],
        compiler_params=pltpu.CompilerParams(collective_id=collective_id, has_side_effects=True),
        name="row_return",
    )(x)


def pair_kernel(x_ref, out_ref, send, recv):
    tp, dp, _, y = place()
    partner = tp + 1 - 2 * y
    signal(partner, dp)
    pl.semaphore_wait(pltpu.get_barrier_semaphore(), 1)
    copy = remote(x_ref, out_ref, send, recv, partner, dp)
    copy.start()
    copy.wait()


def pair_swap(x, collective_id):
    return pl.pallas_call(
        pair_kernel,
        out_shape=jax.ShapeDtypeStruct(x.shape, x.dtype),
        in_specs=[VMEM],
        out_specs=VMEM,
        scratch_shapes=[pltpu.SemaphoreType.DMA, pltpu.SemaphoreType.DMA],
        compiler_params=pltpu.CompilerParams(collective_id=collective_id, has_side_effects=True),
        name="pair_swap",
    )(x)


FORWARD = {
    0: {1: (("R", 1),), 3: (("R", 2),), 5: (("R", 3),)},
    1: {1: (("L", 0), ("R", 2)), 3: (("R", 3),)},
    2: {1: (("R", 3), ("L", 1)), 3: (("L", 0),)},
    3: {1: (("L", 2),), 3: (("L", 1),), 5: (("L", 0),)},
}
REDUCE = {
    0: {2: (3,), 4: (2,), 6: (1,), 7: (0,)},
    1: {4: (3,), 6: (2, 0), 7: (1,)},
    2: {4: (0,), 6: (1, 3), 7: (2,)},
    3: {2: (0,), 4: (1,), 6: (2,), 7: (3,)},
}
SUB = 256
GROUP = 6


def lookup(table, z, step):
    value = jnp.int32(0)
    for k in range(NZ):
        for s in range(2 * NZ):
            value = value + jnp.where((z == k) & (step == s), table[k][s], 0)
    return value


def head_kernel(scale, token_scale, f_ref, lab_ref, e_ref, dfin_ref, ghead_ref, norm_ref, labsum_ref,
                e_b, e_t, fbuf, f_b, g_acc, from_y, from_l, from_r, dl, lse_all, load_sem, ag_y, ag_l, ag_r, ag_recv,
                rs_y, rs_l, rs_r, recv_y, recv_l, recv_r, st_send, st_recv):
    tp, dp, z, y = place()
    partner = tp + 1 - 2 * y
    vocab, width = e_ref.shape
    own = f_ref.shape[0]
    whole = vocab // (SUB * GROUP)
    rest = vocab - whole * SUB * GROUP
    log2e = 1.4426950408889634
    slope = scale * log2e
    blocks = [(j * SUB, SUB) for j in range(GROUP)]
    tail = [(n, min(SUB, rest - n)) for n in range(0, rest, SUB)]

    plane_barrier(tp, dp, [])

    def send(src, slot, sems, to):
        remote(src, fbuf.at[slot], sems.at[slot], ag_recv.at[slot], to, dp).start()

    def arrived(slot):
        remote(f_ref, fbuf.at[slot], ag_y.at[slot], ag_recv.at[slot], partner, dp).wait_recv()

    def first_sends(k):
        if k > 0:
            send(f_ref, tp, ag_l, tp - 2)
        if k < NZ - 1:
            send(f_ref, tp, ag_r, tp + 2)
        send(f_ref, tp, ag_y, partner)

    for k in range(NZ):
        pl.when(z == k)(functools.partial(first_sends, k))
    load = pltpu.make_async_copy(e_ref, g_acc, load_sem.at[0])
    load.start()
    own_copy = pltpu.make_async_copy(f_ref, fbuf.at[tp], load_sem.at[1])
    own_copy.start()
    load.wait()

    def prepare(at, size):
        part = g_acc[at, :]
        e_b[at, :] = part.astype(BF16)
        e_t[:, at] = part.T.astype(BF16)

    def prepare_body(n, carry):
        prepare(pl.ds(pl.multiple_of(n * SUB, SUB), SUB), SUB)
        return carry

    lax.fori_loop(0, vocab // SUB, prepare_body, 0)
    if vocab % SUB:
        prepare(pl.ds(vocab // SUB * SUB, vocab % SUB), vocab % SUB)
    own_copy.wait()

    def over_blocks(group, carry):
        def body(n, c):
            return group(pl.multiple_of(n * SUB * GROUP, SUB * GROUP), blocks, c)
        carry = lax.fori_loop(0, whole, body, carry)
        return group(whole * SUB * GROUP, tail, carry) if tail else carry

    order1 = {k: (k,) + tuple(v for pair in zip([a[1] for a in ARRIVALS[k]], [k] + [a[1] for a in ARRIVALS[k]]) for v in pair) + (ARRIVALS[k][-1][1],) for k in range(NZ)}
    order1 = {k: [2 * zz + (s % 2 == 0 and s > 0 or s == 7) for s, zz in enumerate(order1[k])] for k in range(NZ)}

    def chunk_of(table, step):
        code = lookup(table, z, step)
        other = code % 2
        return code // 2 * 2 + y + other - 2 * y * other

    def gather_step(step, carry):
        slot = chunk_of(order1, step)
        for k in range(NZ):
            for s, shards in FORWARD[k].items():
                def pass_on(k=k, shards=shards):
                    for side, zz in shards:
                        at = 2 * zz + y
                        arrived(at)
                        if side == "L" and k < NZ - 1:
                            send(fbuf.at[at], at, ag_r, tp + 2)
                        if side == "R" and k > 0:
                            send(fbuf.at[at], at, ag_l, tp - 2)
                        send(fbuf.at[at], at, ag_y, partner)
                pl.when((z == k) & (step == s))(pass_on)
        pl.when(slot % 2 != y)(lambda: arrived(slot))
        f_b[slot] = fbuf[slot].astype(BF16)
        f_now = f_b[slot]

        def group(base, parts, c):
            top, total = c
            for first, size in parts:
                logit = lax.dot_general(e_b[pl.ds(base + first, size), :], f_now, (((1,), (1,)), ((), ())), preferred_element_type=F32)
                logit = logit.reshape(size // 8, 8, own)
                new = jnp.maximum(top, jnp.max(logit, axis=0))
                total = total * jnp.exp2((top - new) * slope) + jnp.sum(jnp.exp2((logit - new[None]) * slope), axis=0)
                top = new
            return top, total

        top, total = over_blocks(group, (jnp.full((8, own), -3e38, F32), jnp.zeros((8, own), F32)))
        most = jnp.max(top, axis=0, keepdims=True)
        total = jnp.sum(total * jnp.exp2((top - most) * slope), axis=0, keepdims=True)
        lse_all[tp, pl.ds(slot, 1), :] = most * scale + jnp.log(total)
        return carry

    lax.fori_loop(0, 2 * NZ, gather_step, 0)

    for n in range(1, 2 * NZ):
        to = lax.rem(tp + n, 2 * NZ)
        remote(lse_all.at[tp], lse_all.at[tp], st_send.at[to], st_recv.at[tp], to, dp).start()

    def gathers_done(k):
        def done(sems, slot):
            remote(f_ref, fbuf.at[slot], sems.at[slot], ag_recv.at[slot], partner, dp).wait_send()
        if k > 0:
            done(ag_l, tp)
        if k < NZ - 1:
            done(ag_r, tp)
        done(ag_y, tp)
        for side, zz in ARRIVALS[k]:
            at = 2 * zz + y
            if side == "L" and k < NZ - 1:
                done(ag_r, at)
            if side == "R" and k > 0:
                done(ag_l, at)
            done(ag_y, at)

    for k in range(NZ):
        pl.when(z == k)(functools.partial(gathers_done, k))

    def clear(n, carry):
        g_acc[pl.ds(pl.multiple_of(n * 16, 16), 16), :] = jnp.zeros((16, width), F32)
        return carry

    lax.fori_loop(0, vocab // 16, clear, 0)
    for n in range(1, 2 * NZ):
        source = lax.rem(tp + n, 2 * NZ)
        remote(lse_all.at[source], lse_all.at[source], st_send.at[source], st_recv.at[source], source, dp).wait_recv()
    peak = jnp.max(lse_all[...], axis=0)
    log_norm = peak + jnp.log(jnp.sum(jnp.exp(lse_all[...] - peak[None]), axis=0))
    norm_ref[...] = log_norm

    order2 = {k: [2 * zz + 1 - s for zz in REDUCE_ORDER[k] for s in range(2)] for k in range(NZ)}

    def scatter_step(step, lab_sum):
        slot = chunk_of(order2, step)
        f_now = f_b[slot]
        acc = fbuf.at[slot]
        norm = norm_ref[pl.ds(slot, 1), :]
        shift = norm * log2e
        coef = (1.0 + 2.0 * LOGIT_ZLOSS * norm) * token_scale
        lab = lab_ref[pl.ds(slot, 1), :]
        acc[...] = jnp.zeros((width, own), F32)

        def group(base, parts, hits):
            for first, size in parts:
                at = pl.ds(base + first, size)
                logit = lax.dot_general(e_b[at, :], f_now, (((1,), (1,)), ((), ())), preferred_element_type=F32)
                hit = lax.broadcasted_iota(jnp.int32, (size, own), 0) == lab - (base + first)
                prob = jnp.exp2(logit * slope - shift) * coef
                grad = jnp.where(hit, prob - token_scale, prob).astype(BF16)
                hits = hits + jnp.sum(jnp.where(hit, logit, 0.0).reshape(size // 8, 8, own), axis=0)
                dl[pl.ds(first, size), :] = grad
                g_acc[at, :] += jnp.dot(grad, f_now, preferred_element_type=F32)
            size = parts[-1][0] + parts[-1][1]
            acc[...] += jnp.dot(e_t[:, pl.ds(base, size)], dl[pl.ds(0, size), :], preferred_element_type=F32)
            return hits

        lab_sum = over_blocks(group, lab_sum)

        def hand_over():
            remote(acc, from_y.at[slot // 2], rs_y.at[slot // 2], recv_y.at[slot // 2], partner, dp).start()
        pl.when(slot % 2 != y)(hand_over)

        for k in range(NZ):
            for s, shards in REDUCE[k].items():
                def reduce(k=k, shards=shards):
                    for zz in shards:
                        line = fbuf.at[2 * zz + y]
                        remote(line, from_y.at[zz], rs_y.at[zz], recv_y.at[zz], partner, dp).wait_recv()
                        add_into(line, from_y.at[zz])
                        if zz >= k and k > 0:
                            remote(line, from_l.at[zz - 1], rs_l.at[zz], recv_l.at[zz], partner, dp).wait_recv()
                            add_into(line, from_l.at[zz - 1])
                        if zz <= k and k < NZ - 1:
                            remote(line, from_r.at[zz], rs_r.at[zz], recv_r.at[zz], partner, dp).wait_recv()
                            add_into(line, from_r.at[zz])
                        if zz > k:
                            remote(line, from_l.at[zz - 1], rs_r.at[zz], recv_l.at[zz], tp + 2, dp).start()
                        if zz < k:
                            remote(line, from_r.at[zz], rs_l.at[zz], recv_r.at[zz], tp - 2, dp).start()
                pl.when((z == k) & (step == s))(reduce)
        return lab_sum

    lab_sum = lax.fori_loop(0, 2 * NZ, scatter_step, jnp.zeros((8, own), F32))
    labsum_ref[...] = lab_sum
    store = pltpu.make_async_copy(g_acc, ghead_ref, load_sem.at[0])
    store.start()
    dfin_ref[...] = fbuf[tp].T

    def scatters_done(k):
        for zz in range(NZ):
            line = fbuf.at[2 * zz + y]
            remote(line, from_y.at[zz], rs_y.at[zz], recv_y.at[zz], partner, dp).wait_send()
            if zz > k:
                remote(line, from_l.at[zz - 1], rs_r.at[zz], recv_l.at[zz], partner, dp).wait_send()
            if zz < k:
                remote(line, from_r.at[zz], rs_l.at[zz], recv_r.at[zz], partner, dp).wait_send()

    for k in range(NZ):
        pl.when(z == k)(functools.partial(scatters_done, k))
    for n in range(1, 2 * NZ):
        to = lax.rem(tp + n, 2 * NZ)
        remote(lse_all.at[tp], lse_all.at[tp], st_send.at[to], st_recv.at[tp], to, dp).wait_send()
    store.wait()


def head(f_own, labels, embed, scale, token_scale, collective_id):
    own, width = f_own.shape
    vocab = embed.shape[0]
    chunk = (own, width)
    dma8 = pltpu.SemaphoreType.DMA((2 * NZ,))
    dma4 = pltpu.SemaphoreType.DMA((NZ,))
    return pl.pallas_call(
        functools.partial(head_kernel, scale, token_scale),
        out_shape=(jax.ShapeDtypeStruct((own, width), F32), jax.ShapeDtypeStruct((vocab, width), F32),
                   jax.ShapeDtypeStruct((2 * NZ, own), F32), jax.ShapeDtypeStruct((8, own), F32)),
        in_specs=[VMEM, VMEM, ANY],
        out_specs=(VMEM, ANY, VMEM, VMEM),
        scratch_shapes=[pltpu.VMEM((vocab, width), BF16), pltpu.VMEM((width, vocab), BF16),
                        pltpu.VMEM((2 * NZ,) + chunk, F32), pltpu.VMEM((2 * NZ,) + chunk, BF16), pltpu.VMEM((vocab, width), F32),
                        pltpu.VMEM((NZ,) + chunk, F32), pltpu.VMEM((NZ - 1,) + chunk, F32), pltpu.VMEM((NZ - 1,) + chunk, F32),
                        pltpu.VMEM((SUB * GROUP, own), BF16), pltpu.VMEM((2 * NZ, 2 * NZ, own), F32),
                        pltpu.SemaphoreType.DMA((2,)), dma8, dma8, dma8, dma8, dma4, dma4, dma4, dma4, dma4, dma4, dma8, dma8],
        compiler_params=pltpu.CompilerParams(collective_id=collective_id, has_side_effects=True, vmem_limit_bytes=67000000),
        cost_estimate=pl.CostEstimate(flops=8 * vocab * width * own * 8, bytes_accessed=3 * 4 * vocab * width, transcendentals=2 * vocab * own * 8),
        name="head",
    )(f_own, labels, embed)


TB = (((1,), (1,)), ((), ()))
TA = (((0,), (0,)), ((), ()))
LOG2E = 1.4426950408889634


def mm(a, b, dims=(((1,), (0,)), ((), ()))):
    return lax.dot_general(a, b, dims, preferred_element_type=F32)


def turn(lo, hi, cos_t, sin_t):
    return lo * cos_t - hi * sin_t, hi * cos_t + lo * sin_t


def layer_fwd_kernel(x0_ref, ln_ref, cos_ref, sin_ref, wq_ref, wkv_ref, wo_ref, wg_ref, wu_ref, wd_ref,
                     f_ref, x1_ref, q_ref, kv_ref, kvt_ref, lse_ref, ctx_ref, u_b, kv_out, kv_in, send_sem, recv_sem):
    tp, dp, _, y = place()
    partner = tp + 1 - 2 * y
    own, width = x0_ref.shape
    hd = kv_out.shape[0] // 2
    quarter = hd // 2
    heads = q_ref.shape[0] // hd
    signal(partner, dp)
    u_b[...] = norm_fwd(x0_ref[...], ln_ref[0:1, :])[0]
    u = u_b[...]
    cos_t = cos_ref[...]
    sin_t = sin_ref[...]
    kv = mm(wkv_ref[...], u, TB)
    lo, hi = turn(kv[:quarter], kv[quarter:hd], cos_t, sin_t)
    kv_out[0:quarter, :] = lo
    kv_out[quarter:hd, :] = hi
    kv_out[hd:, :] = kv[hd:]
    pl.semaphore_wait(pltpu.get_barrier_semaphore(), 1)
    copy = remote(kv_out, kv_in, send_sem, recv_sem, partner, dp)
    copy.start()

    q_all = mm(wq_ref[...], u, TB)
    for h in range(heads):
        lo, hi = turn(q_all[h * hd:h * hd + quarter], q_all[h * hd + quarter:(h + 1) * hd], cos_t, sin_t)
        q_ref[h * hd:h * hd + quarter, :] = lo.astype(BF16)
        q_ref[h * hd + quarter:(h + 1) * hd, :] = hi.astype(BF16)

    x1_ref[...] = x0_ref[...]
    step = min(512, wg_ref.shape[0])

    def mlp(n, carry):
        at = pl.ds(pl.multiple_of(n * step, step), step)
        gate = mm(u_b[...], wg_ref[at, :], TB)
        up = mm(u_b[...], wu_ref[at, :], TB)
        hidden = (gate * jax.nn.sigmoid(gate) * up).astype(BF16)
        x1_ref[...] += mm(hidden, wd_ref[at, :])
        return carry

    lax.fori_loop(0, wg_ref.shape[0] // step, mlp, 0)

    copy.wait()

    def fill(mine, other):
        kv_ref[mine * own:(mine + 1) * own, :] = kv_out[...].T.astype(BF16)
        kv_ref[other * own:(other + 1) * own, :] = kv_in[...].T.astype(BF16)
        kvt_ref[:, mine * own:(mine + 1) * own] = kv_out[...].astype(BF16)
        kvt_ref[:, other * own:(other + 1) * own] = kv_in[...].astype(BF16)

    pl.when(y == 0)(lambda: fill(0, 1))
    pl.when(y == 1)(lambda: fill(1, 0))
    blank = jnp.zeros((hd, own), BF16)
    slope = hd ** -0.5 * LOG2E

    def attend(h, carry):
        at = pl.ds(pl.multiple_of(h * hd, hd), hd)
        scores = mm(kv_ref[...], jnp.concatenate([q_ref[at, :], blank], axis=0))
        allowed = lax.broadcasted_iota(jnp.int32, scores.shape, 0) <= lax.broadcasted_iota(jnp.int32, scores.shape, 1) + y * own
        scores = jnp.where(allowed, scores * slope, -1e30)
        top = jnp.max(scores, axis=0, keepdims=True)
        prob = jnp.exp2(scores - top)
        total = jnp.sum(prob, axis=0, keepdims=True)
        lse_ref[pl.ds(h, 1), :] = top + jnp.log2(total)
        ctx_ref[at, :] = mm(kvt_ref[hd:, :], (prob * (1.0 / total)).astype(BF16)).astype(BF16)
        return carry

    lax.fori_loop(0, heads, attend, 0)
    x1_ref[...] += mm(ctx_ref[...], wo_ref[...], TA)
    f_ref[...] = norm_fwd(x1_ref[...], ln_ref[1:2, :])[0].astype(F32)


def layer_fwd(x0, ln, cos_t, sin_t, weights, collective_id):
    own, width = x0.shape
    two_hd = weights[1].shape[0]
    nq = weights[0].shape[0]
    return pl.pallas_call(
        layer_fwd_kernel,
        out_shape=(jax.ShapeDtypeStruct((own, width), F32), jax.ShapeDtypeStruct((own, width), F32),
                   jax.ShapeDtypeStruct((nq, own), BF16), jax.ShapeDtypeStruct((2 * own, two_hd), BF16),
                   jax.ShapeDtypeStruct((two_hd, 2 * own), BF16), jax.ShapeDtypeStruct((2 * nq // two_hd, own), F32),
                   jax.ShapeDtypeStruct((nq, own), BF16)),
        in_specs=[VMEM] * 10,
        out_specs=(VMEM,) * 7,
        scratch_shapes=[pltpu.VMEM((own, width), BF16), pltpu.VMEM((two_hd, own), F32), pltpu.VMEM((two_hd, own), F32),
                        pltpu.SemaphoreType.DMA, pltpu.SemaphoreType.DMA],
        compiler_params=pltpu.CompilerParams(collective_id=collective_id, has_side_effects=True, vmem_limit_bytes=60000000),
        name="layer_fwd",
    )(x0, ln, cos_t, sin_t, *weights)


def layer_bwd_kernel(dfin_ref, x0_ref, x1_ref, loss_ref, ln_ref, cos_ref, sin_ref, wq_ref, wkv_ref, wo_ref, wg_ref, wu_ref, wd_ref,
                     q_ref, kv_ref, kvt_ref, lse_ref, ctx_ref, rows_ref, d0_ref, d_one, d_b, u_b, dctx, dq, dkv, dkv_in,
                     g_q, g_o, g_g, g_u, g_d, small, out_sem, send_sem, recv_sem):
    tp, dp, _, y = place()
    partner = tp + 1 - 2 * y
    own, width = x0_ref.shape
    hd = kv_ref.shape[1] // 2
    quarter = hd // 2
    nq = q_ref.shape[0]
    heads = nq // hd
    ff = wg_ref.shape[0]
    signal(partner, dp)
    _, f_hat, f_inv = norm_fwd(x1_ref[...], ln_ref[1:2, :])
    d_in, g_fin = norm_bwd(dfin_ref[...], f_hat, f_inv, ln_ref[1:2, :])
    d_one[...] = d_in
    d_b[...] = d_in.astype(BF16)
    u_b[...] = norm_fwd(x0_ref[...], ln_ref[0:1, :])[0]
    dctx[...] = mm(wo_ref[...], d_b[...], TB).astype(BF16)
    g_o[...] = mm(ctx_ref[...], d_b[...])
    cos_t = cos_ref[...]
    sin_t = sin_ref[...]
    blank = jnp.zeros((hd, own), BF16)
    slope = hd ** -0.5 * LOG2E
    dkv[...] = jnp.zeros_like(dkv)

    def attend(h, carry):
        at = pl.ds(pl.multiple_of(h * hd, hd), hd)
        q_pad = jnp.concatenate([q_ref[at, :], blank], axis=0)
        d_pad = jnp.concatenate([blank, dctx[at, :]], axis=0)
        scores = mm(kv_ref[...], q_pad)
        allowed = lax.broadcasted_iota(jnp.int32, scores.shape, 0) <= lax.broadcasted_iota(jnp.int32, scores.shape, 1) + y * own
        prob = jnp.where(allowed, jnp.exp2(scores * slope - lse_ref[pl.ds(h, 1), :]), 0.0)
        d_prob = mm(kv_ref[...], d_pad)
        mean = jnp.sum(d_prob * prob, axis=0, keepdims=True)
        d_score = (prob * (d_prob - mean) * hd ** -0.5).astype(BF16)
        dkv[...] += mm(d_score, q_pad, TB) + mm(prob.astype(BF16), d_pad, TB)
        d_q = mm(kvt_ref[0:hd, :], d_score)
        lo, hi = turn(d_q[:quarter], d_q[quarter:], cos_t, -sin_t)
        dq[at, :] = jnp.concatenate([lo, hi], axis=0).astype(BF16)
        return carry

    lax.fori_loop(0, heads, attend, 0)
    pl.semaphore_wait(pltpu.get_barrier_semaphore(), 1)
    copy = remote(dkv.at[pl.ds(pl.multiple_of((1 - y) * own, own), own), :], dkv_in, send_sem, recv_sem, partner, dp)
    copy.start()

    d0_ref[...] = mm(dq[...], wq_ref[...], TA)
    g_q[...] = mm(dq[...], u_b[...])
    step = min(512, ff)

    def mlp(n, carry):
        at = pl.ds(pl.multiple_of(n * step, step), step)
        gate = mm(wg_ref[at, :], u_b[...], TB)
        up = mm(wu_ref[at, :], u_b[...], TB)
        d_hidden = mm(wd_ref[at, :], d_b[...], TB)
        sig = jax.nn.sigmoid(gate)
        g_d[at, :] = mm((gate * sig * up).astype(BF16), d_b[...])
        d_gate = (d_hidden * up * sig * (1.0 + gate * (1.0 - sig))).astype(BF16)
        d_up = (d_hidden * gate * sig).astype(BF16)
        g_g[at, :] = mm(d_gate, u_b[...])
        g_u[at, :] = mm(d_up, u_b[...])
        d0_ref[...] += mm(d_gate, wg_ref[at, :], TA) + mm(d_up, wu_ref[at, :], TA)
        return carry

    lax.fori_loop(0, ff // step, mlp, 0)
    copy.wait()
    d_kv = (dkv[pl.ds(pl.multiple_of(y * own, own), own), :] + dkv_in[...]).T
    lo, hi = turn(d_kv[:quarter], d_kv[quarter:hd], cos_t, -sin_t)
    d_kv = jnp.concatenate([lo, hi, d_kv[hd:]], axis=0).astype(BF16)
    small[0:2 * hd, :] = mm(d_kv, u_b[...])
    d_u = d0_ref[...] + mm(d_kv, wkv_ref[...], TA)
    _, u_hat, u_inv = norm_fwd(x0_ref[...], ln_ref[0:1, :])
    d_in, g_in = norm_bwd(d_u, u_hat, u_inv, ln_ref[0:1, :])
    d0_ref[...] = d_one[...] + d_in
    small[2 * hd:, :] = jnp.zeros_like(small[2 * hd:, :])
    small[2 * hd:2 * hd + 1, :] = g_in.reshape(1, width)
    small[2 * hd + 1:2 * hd + 2, :] = g_fin.reshape(1, width)
    small[2 * hd + 2:2 * hd + 3, :] = loss_ref[...]
    shards = rows_ref.shape[0]
    copies = []

    def put(src, first, size, s):
        copies.append(pltpu.make_async_copy(src, rows_ref.at[s, pl.ds(first, size), :], out_sem.at[len(copies)]))

    n_kv = 2 * hd // shards
    for s in range(shards):
        at = 0
        for g, size in ((g_q, nq // shards), (g_o, nq // shards), (g_g, ff // shards), (g_u, ff // shards), (g_d, ff // shards)):
            put(g.at[pl.ds(s * size, size), :], at, size, s)
            at += size
        put(small.at[pl.ds(s * n_kv, n_kv), :], at, n_kv, s)
        put(small.at[pl.ds(2 * hd + (0 if s == 0 else 16), 16), :], at + n_kv, 16, s)
    for c in copies:
        c.start()
    for c in copies:
        c.wait()


def layer_bwd(d_fin, x0, x1, loss_row, ln, cos_t, sin_t, weights, saved, collective_id):
    own, width = x0.shape
    nq = weights[0].shape[0]
    two_hd = weights[1].shape[0]
    ff = weights[3].shape[0]
    rows = (2 * nq + 3 * ff + two_hd) // (2 * NZ) + 16
    chunk = (own, width)
    return pl.pallas_call(
        layer_bwd_kernel,
        out_shape=(jax.ShapeDtypeStruct((2 * NZ, rows, width), F32), jax.ShapeDtypeStruct(chunk, F32)),
        in_specs=[VMEM] * 18,
        out_specs=(ANY, VMEM),
        scratch_shapes=[pltpu.VMEM(chunk, F32), pltpu.VMEM(chunk, BF16), pltpu.VMEM(chunk, BF16), pltpu.VMEM((nq, own), BF16),
                        pltpu.VMEM((nq, own), BF16), pltpu.VMEM((2 * own, two_hd), F32), pltpu.VMEM((own, two_hd), F32),
                        pltpu.VMEM((nq, width), F32), pltpu.VMEM((nq, width), F32)] + [pltpu.VMEM((ff, width), F32)] * 3
        + [pltpu.VMEM((two_hd + 32, width), F32), pltpu.SemaphoreType.DMA((14 * NZ,)), pltpu.SemaphoreType.DMA, pltpu.SemaphoreType.DMA],
        compiler_params=pltpu.CompilerParams(collective_id=collective_id, has_side_effects=True, vmem_limit_bytes=60000000),
        name="layer_bwd",
    )(d_fin, x0, x1, loss_row, ln, cos_t, sin_t, *weights, *saved)


def norm_fwd(x_f32, scale):
    centered = x_f32 - jnp.mean(x_f32, axis=-1, keepdims=True)
    inv_std = lax.rsqrt(jnp.mean(centered * centered, axis=-1, keepdims=True) + LN_EPS)
    x_hat = centered * inv_std
    return (x_hat * scale).astype(BF16), x_hat, inv_std


def norm_bwd(d_out, x_hat, inv_std, scale):
    d_scale = jnp.sum(d_out * x_hat, axis=0)
    d_hat = d_out * scale
    d_in = inv_std * (d_hat - jnp.mean(d_hat, axis=-1, keepdims=True) - x_hat * jnp.mean(d_hat * x_hat, axis=-1, keepdims=True))
    return d_in, d_scale


def rope_tables(positions, head_dim):
    inv_freq = ROPE_BASE ** (-jnp.arange(0, head_dim, 2).astype(F32) / head_dim)
    angles = positions.astype(F32)[:, None] * inv_freq[None, :]
    return jnp.cos(angles), jnp.sin(angles)


def rotate(x_in, cos_t, sin_t):
    half_dim = x_in.shape[-1] // 2
    x_lo = x_in[..., :half_dim]
    x_hi = x_in[..., half_dim:]
    return jnp.concatenate([x_lo * cos_t - x_hi * sin_t, x_hi * cos_t + x_lo * sin_t], axis=-1)


def adam_update(param_in, grad_in, mom_in, vel_in):
    mom_new = BETA_ONE * mom_in + (1.0 - BETA_ONE) * grad_in
    vel_new = BETA_TWO * vel_in + (1.0 - BETA_TWO) * grad_in * grad_in
    return param_in - LEARN_RATE * mom_new / (jnp.sqrt(vel_new) + ADAM_EPS), mom_new, vel_new


def dot(spec, a, b):
    return jnp.einsum(spec, a, b, preferred_element_type=F32)


def solution(mesh):
    param_specs = (P('tp', None), P(None, None), P(None, 'tp'), P(None, None, None), P('tp', None), P(None, None, 'tp'), P('tp', None))
    n_tp = mesh.shape['tp']
    n_dp = mesh.shape['dp']

    def local_step(tokens, labels, *state_arrays):
        embed, ln_scales, w_q, w_kv, w_o, w_gu, w_down = state_arrays[0:7]
        batch_loc, seq_len = tokens.shape
        vocab_loc, d_model = embed.shape
        head_dim = w_kv.shape[2]
        q_loc = w_q.shape[1]
        f_loc = w_down.shape[0]
        heads = n_tp * q_loc // head_dim
        tok_loc = batch_loc * seq_len
        tok_total = tok_loc * n_dp
        own = tok_loc // n_tp
        tp_rank = lax.axis_index('tp')
        half = tp_rank % 2

        all_tokens = lax.all_gather(tokens, 'dp').reshape(n_dp * n_tp, own)
        strict = (jnp.arange(own)[:, None] > jnp.arange(own)[None, :]).astype(BF16)

        def routing(chunks):
            shard = chunks // vocab_loc
            row = chunks - shard * vocab_loc
            hot = (shard[:, :, None] == jnp.arange(n_tp)[None, None, :])
            before = dot('rs,nsj->nrj', strict, hot.astype(BF16))
            rank = jnp.sum(jnp.where(hot, before, 0.0), axis=-1).astype(jnp.int32)
            most = jnp.max(jnp.sum(hot.astype(jnp.int32), axis=1))
            return shard, row, rank, (most + CAP - 1) // CAP

        chunks = tokens.reshape(n_tp, own)
        shard, row, rank, _ = routing(chunks)
        shard_all, row_all, rank_all, rounds_all = routing(all_tokens)
        slots = jnp.arange(CAP)
        my_shard = lax.dynamic_index_in_dim(shard, tp_rank, 0, keepdims=False)
        my_rank = lax.dynamic_index_in_dim(rank, tp_rank, 0, keepdims=False)

        def fetch(step, x_sum, collective_id):
            here = (shard[:, None, :] == tp_rank) & (rank[:, None, :] == slots[None, :, None] + step * CAP)
            ids = jnp.sum(jnp.where(here, row[:, None, :], 0), axis=-1).reshape(-1)
            rows_out = lax.optimization_barrier(jnp.take(embed, ids, axis=0)).astype(BF16).astype(F32).reshape(n_tp, CAP, d_model)
            rows_in = plane_swap(rows_out, False, collective_id).reshape(n_tp * CAP, d_model).astype(BF16)
            pick = (my_shard[:, None, None] == jnp.arange(n_tp)[None, :, None]) & (my_rank[:, None, None] == slots[None, None, :] + step * CAP)
            return x_sum + dot('rc,cd->rd', pick.reshape(own, n_tp * CAP).astype(BF16), rows_in)

        x_zero = fetch(0, jnp.zeros((own, d_model), F32), 0)
        x_zero = lax.while_loop(lambda s: s[0] < rounds_all, lambda s: (s[0] + 1, fetch(s[0], s[1], 1)), (jnp.int32(1), x_zero))[1]

        w_rows = jnp.concatenate([w_q.T, w_o, w_gu.transpose(0, 2, 1).reshape(2 * f_loc, d_model), w_down], axis=0)
        w_all = weight_gather(w_rows, 2).astype(BF16)
        cuts = (q_loc, 2 * q_loc, 2 * q_loc + f_loc, 2 * q_loc + 2 * f_loc)
        wq_t = w_all[:, :cuts[0]].reshape(-1, d_model)
        wo_b = w_all[:, cuts[0]:cuts[1]].reshape(-1, d_model)
        wg_t = w_all[:, cuts[1]:cuts[2]].reshape(-1, d_model)
        wu_t = w_all[:, cuts[2]:cuts[3]].reshape(-1, d_model)
        wd_b = w_all[:, cuts[3]:].reshape(-1, d_model)
        wkv_t = w_kv.transpose(0, 2, 1).reshape(2 * head_dim, d_model).astype(BF16)
        weights = (wq_t, wkv_t, wo_b, wg_t, wu_t, wd_b)
        inv_freq = ROPE_BASE ** (-jnp.arange(0, head_dim, 2).astype(F32) / head_dim)
        angles = inv_freq[:, None] * (half * own + jnp.arange(own)).astype(F32)[None, :]
        cos_t, sin_t = jnp.cos(angles), jnp.sin(angles)
        f_own, x_one, *saved = layer_fwd(x_zero, ln_scales, cos_t, sin_t, weights, 3)

        logit_scale = d_model ** -0.5
        lab_loc = labels.reshape(n_tp, own) - tp_rank * vocab_loc
        d_fin, g_head_part, log_norm, lab_sum = head(f_own, lab_loc, embed, logit_scale, logit_scale / tok_total, 4)
        log_norm = lax.dynamic_index_in_dim(log_norm, tp_rank, 0, keepdims=False)
        loss_row = (log_norm + LOGIT_ZLOSS * log_norm * log_norm - jnp.sum(lab_sum, axis=0) * logit_scale) / tok_total
        g_head = lax.psum(g_head_part, 'dp')
        g_rows, d_zero = layer_bwd(d_fin, x_zero, x_one, loss_row[None, :], ln_scales, cos_t, sin_t, weights, saved, 7)

        my_row_shard = my_shard

        def give_back(step, g_look, collective_id):
            mine = (my_row_shard[None, None, :] == jnp.arange(n_tp)[:, None, None]) & (my_rank[None, None, :] == slots[None, :, None] + step * CAP)
            ids = jnp.sum(jnp.where(mine, jnp.arange(own)[None, None, :], 0), axis=-1).reshape(-1)
            rows_out = jnp.take(d_zero, ids, axis=0).reshape(n_tp, CAP, d_model)
            rows_in = row_return(rows_out, collective_id).reshape(-1, d_model)
            here = (shard_all[:, None, :] == tp_rank) & (rank_all[:, None, :] == slots[None, :, None] + step * CAP)
            row_id = jnp.where(jnp.any(here, axis=-1), jnp.sum(jnp.where(here, row_all[:, None, :], 0), axis=-1), vocab_loc).reshape(-1)
            return g_look.at[row_id].add(rows_in, mode='drop')

        g_look = give_back(0, jnp.zeros((vocab_loc, d_model), F32), 8)
        g_look = lax.while_loop(lambda s: s[0] < rounds_all, lambda s: (s[0] + 1, give_back(s[0], s[1], 9)), (jnp.int32(1), g_look))[1]

        g_shard, g_small = weight_scatter(g_rows, 10)
        n_kv = 2 * head_dim // n_tp
        g_kv = g_small[:, :n_kv].reshape(2, head_dim, d_model).transpose(0, 2, 1)
        loss = jnp.sum(g_small[0, n_kv + 2])
        gradients = (g_head + g_look, g_small[0, n_kv:n_kv + 2], g_shard[:cuts[0]].T, g_kv, g_shard[cuts[0]:cuts[1]],
                     g_shard[cuts[1]:cuts[3]].reshape(2, f_loc, d_model).transpose(0, 2, 1), g_shard[cuts[3]:cuts[3] + f_loc])

        outs_p = []
        outs_m = []
        outs_v = []
        for index in range(7):
            new_p, new_m, new_v = adam_update(state_arrays[index], gradients[index], state_arrays[7 + index], state_arrays[14 + index])
            outs_p.append(new_p)
            outs_m.append(new_m)
            outs_v.append(new_v)
        return tuple(outs_p) + tuple(outs_m) + tuple(outs_v) + (loss,)

    return jax.shard_map(local_step, mesh=mesh, in_specs=(P('dp', None), P('dp', None)) + param_specs * 3,
                         out_specs=param_specs * 3 + (P(),), check_vma=False)
```

```python
import functools

import jax
import jax.numpy as jnp
from jax import lax
from jax.experimental import pallas as pl
from jax.experimental.pallas import tpu as pltpu
from jax.sharding import PartitionSpec as P

LN_EPS = 1e-5
LOGIT_ZLOSS = 1e-4
LEARN_RATE = 1e-2
BETA_ONE = 0.9
BETA_TWO = 0.95
ADAM_EPS = 1e-8
ROPE_BASE = 10000.0
NZ = 4
CAP = 96
F32 = jnp.float32
BF16 = jnp.bfloat16
ANY = pl.BlockSpec(memory_space=pl.ANY)
VMEM = pl.BlockSpec(memory_space=pltpu.VMEM)

ARRIVALS = {
    0: (("R", 1), ("R", 2), ("R", 3)),
    1: (("L", 0), ("R", 2), ("R", 3)),
    2: (("R", 3), ("L", 1), ("L", 0)),
    3: (("L", 2), ("L", 1), ("L", 0)),
}
REDUCE_ORDER = {0: (3, 2, 1, 0), 1: (3, 0, 2, 1), 2: (0, 3, 1, 2), 3: (0, 1, 2, 3)}


def remote(src, dst, send_sem, recv_sem, tp, dp):
    return pltpu.make_async_remote_copy(src_ref=src, dst_ref=dst, send_sem=send_sem, recv_sem=recv_sem,
                                        device_id=(tp, dp), device_id_type=pl.DeviceIdType.MESH)


def place():
    tp = lax.axis_index("tp")
    dp = lax.axis_index("dp")
    return tp, dp, tp // 2, tp % 2


def signal(tp, dp):
    pl.semaphore_signal(pltpu.get_barrier_semaphore(), inc=1, device_id=(tp, dp), device_id_type=pl.DeviceIdType.MESH)


def line_barrier(k, tp, dp, others):
    peers = [(tp + 1 - 2 * (tp % 2), dp)] + others
    if k > 0:
        peers.append((tp - 2, dp))
    if k < NZ - 1:
        peers.append((tp + 2, dp))
    for peer in peers:
        signal(*peer)
    pl.semaphore_wait(pltpu.get_barrier_semaphore(), len(peers))


def weight_gather_kernel(x_ref, out_ref, own_sem, send_y, send_l, send_r, send_c, recv):
    tp, dp, z, y = place()
    partner = tp + 1 - 2 * y
    core = dp % 2
    twin = dp + 1 - 2 * core

    def program(k):
        line_barrier(k, tp, dp, [(tp, twin)])

        def send(src, slot, sems, to, to_dp):
            copy = remote(src, out_ref.at[slot, core], sems.at[slot], recv.at[slot, core], to, to_dp)
            copy.start()
            return copy

        def arrived(slot, half):
            remote(x_ref.at[0], out_ref.at[slot, half], send_y.at[slot], recv.at[slot, half], partner, dp).wait_recv()

        mine = x_ref.at[core]
        sends = []
        if k > 0:
            sends.append(send(mine, tp, send_l, tp - 2, dp))
        if k < NZ - 1:
            sends.append(send(mine, tp, send_r, tp + 2, dp))
        sends.append(send(mine, tp, send_y, partner, dp))
        own = pltpu.make_async_copy(x_ref, out_ref.at[tp], own_sem)
        own.start()
        across = [k] + [zz for _, zz in ARRIVALS[k]]
        for n, (side, zz) in enumerate(ARRIVALS[k]):
            slot = 2 * zz + y
            arrived(slot, core)
            if side == "L" and k < NZ - 1:
                sends.append(send(out_ref.at[slot, core], slot, send_r, tp + 2, dp))
            if side == "R" and k > 0:
                sends.append(send(out_ref.at[slot, core], slot, send_l, tp - 2, dp))
            sends.append(send(out_ref.at[slot, core], slot, send_y, partner, dp))
            sends.append(send(out_ref.at[slot, core], slot, send_c, tp, twin))
            slot = 2 * across[n] + 1 - y
            arrived(slot, core)
            sends.append(send(out_ref.at[slot, core], slot, send_c, tp, twin))
        slot = 2 * across[-1] + 1 - y
        arrived(slot, core)
        sends.append(send(out_ref.at[slot, core], slot, send_c, tp, twin))
        for zz in range(NZ):
            if zz != k:
                arrived(2 * zz + y, 1 - core)
            arrived(2 * zz + 1 - y, 1 - core)
        own.wait()
        for copy in sends:
            copy.wait_send()

    for k in range(NZ):
        pl.when(z == k)(functools.partial(program, k))


def weight_gather(x, collective_id):
    rows, width = x.shape
    halves = x.reshape(2, rows // 2, width)
    out = pl.pallas_call(
        weight_gather_kernel,
        out_shape=jax.ShapeDtypeStruct((2 * NZ,) + halves.shape, x.dtype),
        in_specs=[ANY],
        out_specs=ANY,
        scratch_shapes=[pltpu.SemaphoreType.DMA] + [pltpu.SemaphoreType.DMA((2 * NZ,))] * 4
        + [pltpu.SemaphoreType.DMA((2 * NZ, 2))],
        compiler_params=pltpu.CompilerParams(collective_id=collective_id, has_side_effects=True),
        name="weight_gather",
    )(halves)
    return out.reshape(2 * NZ, rows, width)


def add_into(acc, other, step=None):
    rows = acc.shape[0]
    step = step or (64 if rows % 64 == 0 else 8)

    def body(n, carry):
        at = pl.ds(pl.multiple_of(n * step, step), step)
        acc[at, :] = acc[at, :] + other[at, :]
        return carry

    lax.fori_loop(0, rows // step, body, 0)


def plane_barrier(tp, dp, others):
    peers = [(lax.rem(tp + n, 2 * NZ), dp) for n in range(1, 2 * NZ)] + others
    for peer in peers:
        signal(*peer)
    pl.semaphore_wait(pltpu.get_barrier_semaphore(), len(peers))


def swap_kernel(spread, x_ref, out_ref, own_sem, send, recv):
    tp, dp, _, _ = place()
    plane_barrier(tp, dp, [])
    copies = []
    for n in range(1, 2 * NZ):
        to = lax.rem(tp + n, 2 * NZ)
        copy = remote(x_ref if spread else x_ref.at[to], out_ref.at[tp], send.at[to], recv.at[tp], to, dp)
        copy.start()
        copies.append(copy)
    own = pltpu.make_async_copy(x_ref if spread else x_ref.at[tp], out_ref.at[tp], own_sem)
    own.start()
    for n in range(1, 2 * NZ):
        source = lax.rem(tp + n, 2 * NZ)
        remote(out_ref.at[source], out_ref.at[source], send.at[source], recv.at[source], source, dp).wait_recv()
    own.wait()
    for copy in copies:
        copy.wait_send()


def plane_swap(x, spread, collective_id):
    return pl.pallas_call(
        functools.partial(swap_kernel, spread),
        out_shape=jax.ShapeDtypeStruct((2 * NZ,) + x.shape if spread else x.shape, x.dtype),
        in_specs=[ANY],
        out_specs=ANY,
        scratch_shapes=[pltpu.SemaphoreType.DMA] + [pltpu.SemaphoreType.DMA((2 * NZ,))] * 2,
        compiler_params=pltpu.CompilerParams(collective_id=collective_id, has_side_effects=True),
        name="plane_spread" if spread else "plane_swap",
    )(x)


FORWARD = {
    0: {1: (("R", 1),), 3: (("R", 2),), 5: (("R", 3),)},
    1: {1: (("L", 0), ("R", 2)), 3: (("R", 3),)},
    2: {1: (("R", 3), ("L", 1)), 3: (("L", 0),)},
    3: {1: (("L", 2),), 3: (("L", 1),), 5: (("L", 0),)},
}
REDUCE = {
    0: {2: (3,), 4: (2,), 6: (1,), 7: (0,)},
    1: {4: (3,), 6: (2, 0), 7: (1,)},
    2: {4: (0,), 6: (1, 3), 7: (2,)},
    3: {2: (0,), 4: (1,), 6: (2,), 7: (3,)},
}
SUB = 256
GROUP = 6


def lookup(table, z, step):
    value = jnp.int32(0)
    for k in range(NZ):
        for s in range(2 * NZ):
            value = value + jnp.where((z == k) & (step == s), table[k][s], 0)
    return value


def head_kernel(scale, token_scale, f_ref, lab_ref, e_ref, dfin_ref, ghead_ref, norm_ref, labsum_ref,
                e_b, e_t, fbuf, f_b, g_acc, from_y, from_l, from_r, dl, lse_all, load_sem, ag_y, ag_l, ag_r, ag_recv,
                rs_y, rs_l, rs_r, recv_y, recv_l, recv_r, st_send, st_recv):
    tp, dp, z, y = place()
    partner = tp + 1 - 2 * y
    vocab, width = e_ref.shape
    own = f_ref.shape[0]
    whole = vocab // (SUB * GROUP)
    rest = vocab - whole * SUB * GROUP
    log2e = 1.4426950408889634
    slope = scale * log2e
    blocks = [(j * SUB, SUB) for j in range(GROUP)]
    tail = [(n, min(SUB, rest - n)) for n in range(0, rest, SUB)]

    plane_barrier(tp, dp, [])

    def send(src, slot, sems, to):
        remote(src, fbuf.at[slot], sems.at[slot], ag_recv.at[slot], to, dp).start()

    def arrived(slot):
        remote(f_ref, fbuf.at[slot], ag_y.at[slot], ag_recv.at[slot], partner, dp).wait_recv()

    def first_sends(k):
        if k > 0:
            send(f_ref, tp, ag_l, tp - 2)
        if k < NZ - 1:
            send(f_ref, tp, ag_r, tp + 2)
        send(f_ref, tp, ag_y, partner)

    for k in range(NZ):
        pl.when(z == k)(functools.partial(first_sends, k))
    load = pltpu.make_async_copy(e_ref, g_acc, load_sem.at[0])
    load.start()
    own_copy = pltpu.make_async_copy(f_ref, fbuf.at[tp], load_sem.at[1])
    own_copy.start()
    load.wait()

    def prepare(at, size):
        part = g_acc[at, :]
        e_b[at, :] = part.astype(BF16)
        e_t[:, at] = part.T.astype(BF16)

    def prepare_body(n, carry):
        prepare(pl.ds(pl.multiple_of(n * SUB, SUB), SUB), SUB)
        return carry

    lax.fori_loop(0, vocab // SUB, prepare_body, 0)
    if vocab % SUB:
        prepare(pl.ds(vocab // SUB * SUB, vocab % SUB), vocab % SUB)
    own_copy.wait()

    def over_blocks(group, carry):
        def body(n, c):
            return group(pl.multiple_of(n * SUB * GROUP, SUB * GROUP), blocks, c)
        carry = lax.fori_loop(0, whole, body, carry)
        return group(whole * SUB * GROUP, tail, carry) if tail else carry

    order1 = {k: (k,) + tuple(v for pair in zip([a[1] for a in ARRIVALS[k]], [k] + [a[1] for a in ARRIVALS[k]]) for v in pair) + (ARRIVALS[k][-1][1],) for k in range(NZ)}
    order1 = {k: [2 * zz + (s % 2 == 0 and s > 0 or s == 7) for s, zz in enumerate(order1[k])] for k in range(NZ)}

    def chunk_of(table, step):
        code = lookup(table, z, step)
        other = code % 2
        return code // 2 * 2 + y + other - 2 * y * other

    def gather_step(step, carry):
        slot = chunk_of(order1, step)
        for k in range(NZ):
            for s, shards in FORWARD[k].items():
                def pass_on(k=k, shards=shards):
                    for side, zz in shards:
                        at = 2 * zz + y
                        arrived(at)
                        if side == "L" and k < NZ - 1:
                            send(fbuf.at[at], at, ag_r, tp + 2)
                        if side == "R" and k > 0:
                            send(fbuf.at[at], at, ag_l, tp - 2)
                        send(fbuf.at[at], at, ag_y, partner)
                pl.when((z == k) & (step == s))(pass_on)
        pl.when(slot % 2 != y)(lambda: arrived(slot))
        f_b[slot] = fbuf[slot].astype(BF16)
        f_now = f_b[slot]

        def group(base, parts, c):
            top, total = c
            for first, size in parts:
                logit = lax.dot_general(e_b[pl.ds(base + first, size), :], f_now, (((1,), (1,)), ((), ())), preferred_element_type=F32)
                logit = logit.reshape(size // 8, 8, own)
                new = jnp.maximum(top, jnp.max(logit, axis=0))
                total = total * jnp.exp2((top - new) * slope) + jnp.sum(jnp.exp2((logit - new[None]) * slope), axis=0)
                top = new
            return top, total

        top, total = over_blocks(group, (jnp.full((8, own), -3e38, F32), jnp.zeros((8, own), F32)))
        most = jnp.max(top, axis=0, keepdims=True)
        total = jnp.sum(total * jnp.exp2((top - most) * slope), axis=0, keepdims=True)
        lse_all[tp, pl.ds(slot, 1), :] = most * scale + jnp.log(total)
        return carry

    lax.fori_loop(0, 2 * NZ, gather_step, 0)

    for n in range(1, 2 * NZ):
        to = lax.rem(tp + n, 2 * NZ)
        remote(lse_all.at[tp], lse_all.at[tp], st_send.at[to], st_recv.at[tp], to, dp).start()

    def gathers_done(k):
        def done(sems, slot):
            remote(f_ref, fbuf.at[slot], sems.at[slot], ag_recv.at[slot], partner, dp).wait_send()
        if k > 0:
            done(ag_l, tp)
        if k < NZ - 1:
            done(ag_r, tp)
        done(ag_y, tp)
        for side, zz in ARRIVALS[k]:
            at = 2 * zz + y
            if side == "L" and k < NZ - 1:
                done(ag_r, at)
            if side == "R" and k > 0:
                done(ag_l, at)
            done(ag_y, at)

    for k in range(NZ):
        pl.when(z == k)(functools.partial(gathers_done, k))

    def clear(n, carry):
        g_acc[pl.ds(pl.multiple_of(n * 16, 16), 16), :] = jnp.zeros((16, width), F32)
        return carry

    lax.fori_loop(0, vocab // 16, clear, 0)
    for n in range(1, 2 * NZ):
        source = lax.rem(tp + n, 2 * NZ)
        remote(lse_all.at[source], lse_all.at[source], st_send.at[source], st_recv.at[source], source, dp).wait_recv()
    peak = jnp.max(lse_all[...], axis=0)
    log_norm = peak + jnp.log(jnp.sum(jnp.exp(lse_all[...] - peak[None]), axis=0))
    norm_ref[...] = log_norm

    order2 = {k: [2 * zz + 1 - s for zz in REDUCE_ORDER[k] for s in range(2)] for k in range(NZ)}

    def scatter_step(step, lab_sum):
        slot = chunk_of(order2, step)
        f_now = f_b[slot]
        acc = fbuf.at[slot]
        norm = norm_ref[pl.ds(slot, 1), :]
        shift = norm * log2e
        coef = (1.0 + 2.0 * LOGIT_ZLOSS * norm) * token_scale
        lab = lab_ref[pl.ds(slot, 1), :]
        acc[...] = jnp.zeros((width, own), F32)

        def group(base, parts, hits):
            for first, size in parts:
                at = pl.ds(base + first, size)
                logit = lax.dot_general(e_b[at, :], f_now, (((1,), (1,)), ((), ())), preferred_element_type=F32)
                hit = lax.broadcasted_iota(jnp.int32, (size, own), 0) == lab - (base + first)
                prob = jnp.exp2(logit * slope - shift) * coef
                grad = jnp.where(hit, prob - token_scale, prob).astype(BF16)
                hits = hits + jnp.sum(jnp.where(hit, logit, 0.0).reshape(size // 8, 8, own), axis=0)
                dl[pl.ds(first, size), :] = grad
                g_acc[at, :] += jnp.dot(grad, f_now, preferred_element_type=F32)
            size = parts[-1][0] + parts[-1][1]
            acc[...] += jnp.dot(e_t[:, pl.ds(base, size)], dl[pl.ds(0, size), :], preferred_element_type=F32)
            return hits

        lab_sum = over_blocks(group, lab_sum)

        def hand_over():
            remote(acc, from_y.at[slot // 2], rs_y.at[slot // 2], recv_y.at[slot // 2], partner, dp).start()
        pl.when(slot % 2 != y)(hand_over)

        for k in range(NZ):
            for s, shards in REDUCE[k].items():
                def reduce(k=k, shards=shards):
                    for zz in shards:
                        line = fbuf.at[2 * zz + y]
                        remote(line, from_y.at[zz], rs_y.at[zz], recv_y.at[zz], partner, dp).wait_recv()
                        add_into(line, from_y.at[zz])
                        if zz >= k and k > 0:
                            remote(line, from_l.at[zz - 1], rs_l.at[zz], recv_l.at[zz], partner, dp).wait_recv()
                            add_into(line, from_l.at[zz - 1])
                        if zz <= k and k < NZ - 1:
                            remote(line, from_r.at[zz], rs_r.at[zz], recv_r.at[zz], partner, dp).wait_recv()
                            add_into(line, from_r.at[zz])
                        if zz > k:
                            remote(line, from_l.at[zz - 1], rs_r.at[zz], recv_l.at[zz], tp + 2, dp).start()
                        if zz < k:
                            remote(line, from_r.at[zz], rs_l.at[zz], recv_r.at[zz], tp - 2, dp).start()
                pl.when((z == k) & (step == s))(reduce)
        return lab_sum

    lab_sum = lax.fori_loop(0, 2 * NZ, scatter_step, jnp.zeros((8, own), F32))
    labsum_ref[...] = lab_sum
    store = pltpu.make_async_copy(g_acc, ghead_ref, load_sem.at[0])
    store.start()
    dfin_ref[...] = fbuf[tp].T

    def scatters_done(k):
        for zz in range(NZ):
            line = fbuf.at[2 * zz + y]
            remote(line, from_y.at[zz], rs_y.at[zz], recv_y.at[zz], partner, dp).wait_send()
            if zz > k:
                remote(line, from_l.at[zz - 1], rs_r.at[zz], recv_l.at[zz], partner, dp).wait_send()
            if zz < k:
                remote(line, from_r.at[zz], rs_l.at[zz], recv_r.at[zz], partner, dp).wait_send()

    for k in range(NZ):
        pl.when(z == k)(functools.partial(scatters_done, k))
    for n in range(1, 2 * NZ):
        to = lax.rem(tp + n, 2 * NZ)
        remote(lse_all.at[tp], lse_all.at[tp], st_send.at[to], st_recv.at[tp], to, dp).wait_send()
    store.wait()


def head(f_own, labels, embed, scale, token_scale, collective_id):
    own, width = f_own.shape
    vocab = embed.shape[0]
    chunk = (own, width)
    dma8 = pltpu.SemaphoreType.DMA((2 * NZ,))
    dma4 = pltpu.SemaphoreType.DMA((NZ,))
    return pl.pallas_call(
        functools.partial(head_kernel, scale, token_scale),
        out_shape=(jax.ShapeDtypeStruct((own, width), F32), jax.ShapeDtypeStruct((vocab, width), F32),
                   jax.ShapeDtypeStruct((2 * NZ, own), F32), jax.ShapeDtypeStruct((8, own), F32)),
        in_specs=[VMEM, VMEM, ANY],
        out_specs=(VMEM, ANY, VMEM, VMEM),
        scratch_shapes=[pltpu.VMEM((vocab, width), BF16), pltpu.VMEM((width, vocab), BF16),
                        pltpu.VMEM((2 * NZ,) + chunk, F32), pltpu.VMEM((2 * NZ,) + chunk, BF16), pltpu.VMEM((vocab, width), F32),
                        pltpu.VMEM((NZ,) + chunk, F32), pltpu.VMEM((NZ - 1,) + chunk, F32), pltpu.VMEM((NZ - 1,) + chunk, F32),
                        pltpu.VMEM((SUB * GROUP, own), BF16), pltpu.VMEM((2 * NZ, 2 * NZ, own), F32),
                        pltpu.SemaphoreType.DMA((2,)), dma8, dma8, dma8, dma8, dma4, dma4, dma4, dma4, dma4, dma4, dma8, dma8],
        compiler_params=pltpu.CompilerParams(collective_id=collective_id, has_side_effects=True, vmem_limit_bytes=67000000),
        cost_estimate=pl.CostEstimate(flops=8 * vocab * width * own * 8, bytes_accessed=3 * 4 * vocab * width, transcendentals=2 * vocab * own * 8),
        name="head",
    )(f_own, labels, embed)


TB = (((1,), (1,)), ((), ()))
TA = (((0,), (0,)), ((), ()))
LOG2E = 1.4426950408889634


def mm(a, b, dims=(((1,), (0,)), ((), ()))):
    return lax.dot_general(a, b, dims, preferred_element_type=F32)


def turn(lo, hi, cos_t, sin_t):
    return lo * cos_t - hi * sin_t, hi * cos_t + lo * sin_t


def layer_fwd_kernel(x0_ref, ln_ref, cos_ref, sin_ref, wq_ref, wkv_ref, wo_ref, wg_ref, wu_ref, wd_ref,
                     f_ref, x1_ref, q_ref, kv_ref, kvt_ref, lse_ref, ctx_ref, u_b, kv_out, kv_in, send_sem, recv_sem):
    tp, dp, _, y = place()
    partner = tp + 1 - 2 * y
    own, width = x0_ref.shape
    hd = kv_out.shape[0] // 2
    quarter = hd // 2
    heads = q_ref.shape[0] // hd
    signal(partner, dp)
    u_b[...] = norm_fwd(x0_ref[...], ln_ref[0:1, :])[0]
    u = u_b[...]
    cos_t = cos_ref[...]
    sin_t = sin_ref[...]
    kv = mm(wkv_ref[...], u, TB)
    lo, hi = turn(kv[:quarter], kv[quarter:hd], cos_t, sin_t)
    kv_out[0:quarter, :] = lo
    kv_out[quarter:hd, :] = hi
    kv_out[hd:, :] = kv[hd:]
    pl.semaphore_wait(pltpu.get_barrier_semaphore(), 1)
    copy = remote(kv_out, kv_in, send_sem, recv_sem, partner, dp)
    copy.start()

    q_all = mm(wq_ref[...], u, TB)
    for h in range(heads):
        lo, hi = turn(q_all[h * hd:h * hd + quarter], q_all[h * hd + quarter:(h + 1) * hd], cos_t, sin_t)
        q_ref[h * hd:h * hd + quarter, :] = lo.astype(BF16)
        q_ref[h * hd + quarter:(h + 1) * hd, :] = hi.astype(BF16)

    x1_ref[...] = x0_ref[...]
    step = min(512, wg_ref.shape[0])

    def mlp(n, carry):
        at = pl.ds(pl.multiple_of(n * step, step), step)
        gate = mm(u_b[...], wg_ref[at, :], TB)
        up = mm(u_b[...], wu_ref[at, :], TB)
        hidden = (gate * jax.nn.sigmoid(gate) * up).astype(BF16)
        x1_ref[...] += mm(hidden, wd_ref[at, :])
        return carry

    lax.fori_loop(0, wg_ref.shape[0] // step, mlp, 0)

    copy.wait()

    def fill(mine, other):
        kv_ref[mine * own:(mine + 1) * own, :] = kv_out[...].T.astype(BF16)
        kv_ref[other * own:(other + 1) * own, :] = kv_in[...].T.astype(BF16)
        kvt_ref[:, mine * own:(mine + 1) * own] = kv_out[...].astype(BF16)
        kvt_ref[:, other * own:(other + 1) * own] = kv_in[...].astype(BF16)

    pl.when(y == 0)(lambda: fill(0, 1))
    pl.when(y == 1)(lambda: fill(1, 0))
    blank = jnp.zeros((hd, own), BF16)
    slope = hd ** -0.5 * LOG2E

    def attend(h, carry):
        at = pl.ds(pl.multiple_of(h * hd, hd), hd)
        scores = mm(kv_ref[...], jnp.concatenate([q_ref[at, :], blank], axis=0))
        allowed = lax.broadcasted_iota(jnp.int32, scores.shape, 0) <= lax.broadcasted_iota(jnp.int32, scores.shape, 1) + y * own
        scores = jnp.where(allowed, scores * slope, -1e30)
        top = jnp.max(scores, axis=0, keepdims=True)
        prob = jnp.exp2(scores - top)
        total = jnp.sum(prob, axis=0, keepdims=True)
        lse_ref[pl.ds(h, 1), :] = top + jnp.log2(total)
        ctx_ref[at, :] = mm(kvt_ref[hd:, :], (prob * (1.0 / total)).astype(BF16)).astype(BF16)
        return carry

    lax.fori_loop(0, heads, attend, 0)
    x1_ref[...] += mm(ctx_ref[...], wo_ref[...], TA)
    f_ref[...] = norm_fwd(x1_ref[...], ln_ref[1:2, :])[0].astype(F32)


def layer_fwd(x0, ln, cos_t, sin_t, weights, collective_id):
    own, width = x0.shape
    two_hd = weights[1].shape[0]
    nq = weights[0].shape[0]
    return pl.pallas_call(
        layer_fwd_kernel,
        out_shape=(jax.ShapeDtypeStruct((own, width), F32), jax.ShapeDtypeStruct((own, width), F32),
                   jax.ShapeDtypeStruct((nq, own), BF16), jax.ShapeDtypeStruct((2 * own, two_hd), BF16),
                   jax.ShapeDtypeStruct((two_hd, 2 * own), BF16), jax.ShapeDtypeStruct((2 * nq // two_hd, own), F32),
                   jax.ShapeDtypeStruct((nq, own), BF16)),
        in_specs=[VMEM] * 10,
        out_specs=(VMEM,) * 7,
        scratch_shapes=[pltpu.VMEM((own, width), BF16), pltpu.VMEM((two_hd, own), F32), pltpu.VMEM((two_hd, own), F32),
                        pltpu.SemaphoreType.DMA, pltpu.SemaphoreType.DMA],
        compiler_params=pltpu.CompilerParams(collective_id=collective_id, has_side_effects=True, vmem_limit_bytes=60000000),
        name="layer_fwd",
    )(x0, ln, cos_t, sin_t, *weights)


def layer_bwd_kernel(dfin_ref, x0_ref, x1_ref, loss_ref, ln_ref, cos_ref, sin_ref, wq_ref, wkv_ref, wo_ref, wg_ref, wu_ref, wd_ref,
                     q_ref, kv_ref, kvt_ref, lse_ref, ctx_ref, rows_ref, d0_ref, d_one, d_b, u_b, dctx, dq, dkv, dkv_in,
                     g_q, g_o, g_g, g_u, g_d, small, out_sem, send_sem, recv_sem):
    tp, dp, _, y = place()
    partner = tp + 1 - 2 * y
    own, width = x0_ref.shape
    hd = kv_ref.shape[1] // 2
    quarter = hd // 2
    nq = q_ref.shape[0]
    heads = nq // hd
    ff = wg_ref.shape[0]
    signal(partner, dp)
    _, f_hat, f_inv = norm_fwd(x1_ref[...], ln_ref[1:2, :])
    d_in, g_fin = norm_bwd(dfin_ref[...], f_hat, f_inv, ln_ref[1:2, :])
    d_one[...] = d_in
    d_b[...] = d_in.astype(BF16)
    u_b[...] = norm_fwd(x0_ref[...], ln_ref[0:1, :])[0]
    dctx[...] = mm(wo_ref[...], d_b[...], TB).astype(BF16)
    g_o[...] = mm(ctx_ref[...], d_b[...])
    cos_t = cos_ref[...]
    sin_t = sin_ref[...]
    blank = jnp.zeros((hd, own), BF16)
    slope = hd ** -0.5 * LOG2E
    dkv[...] = jnp.zeros_like(dkv)

    def attend(h, carry):
        at = pl.ds(pl.multiple_of(h * hd, hd), hd)
        q_pad = jnp.concatenate([q_ref[at, :], blank], axis=0)
        d_pad = jnp.concatenate([blank, dctx[at, :]], axis=0)
        scores = mm(kv_ref[...], q_pad)
        allowed = lax.broadcasted_iota(jnp.int32, scores.shape, 0) <= lax.broadcasted_iota(jnp.int32, scores.shape, 1) + y * own
        prob = jnp.where(allowed, jnp.exp2(scores * slope - lse_ref[pl.ds(h, 1), :]), 0.0)
        d_prob = mm(kv_ref[...], d_pad)
        mean = jnp.sum(d_prob * prob, axis=0, keepdims=True)
        d_score = (prob * (d_prob - mean) * hd ** -0.5).astype(BF16)
        dkv[...] += mm(d_score, q_pad, TB) + mm(prob.astype(BF16), d_pad, TB)
        d_q = mm(kvt_ref[0:hd, :], d_score)
        lo, hi = turn(d_q[:quarter], d_q[quarter:], cos_t, -sin_t)
        dq[at, :] = jnp.concatenate([lo, hi], axis=0).astype(BF16)
        return carry

    lax.fori_loop(0, heads, attend, 0)
    pl.semaphore_wait(pltpu.get_barrier_semaphore(), 1)
    copy = remote(dkv.at[pl.ds(pl.multiple_of((1 - y) * own, own), own), :], dkv_in, send_sem, recv_sem, partner, dp)
    copy.start()

    d0_ref[...] = mm(dq[...], wq_ref[...], TA)
    g_q[...] = mm(dq[...], u_b[...])
    step = min(512, ff)

    def mlp(n, carry):
        at = pl.ds(pl.multiple_of(n * step, step), step)
        gate = mm(wg_ref[at, :], u_b[...], TB)
        up = mm(wu_ref[at, :], u_b[...], TB)
        d_hidden = mm(wd_ref[at, :], d_b[...], TB)
        sig = jax.nn.sigmoid(gate)
        g_d[at, :] = mm((gate * sig * up).astype(BF16), d_b[...])
        d_gate = (d_hidden * up * sig * (1.0 + gate * (1.0 - sig))).astype(BF16)
        d_up = (d_hidden * gate * sig).astype(BF16)
        g_g[at, :] = mm(d_gate, u_b[...])
        g_u[at, :] = mm(d_up, u_b[...])
        d0_ref[...] += mm(d_gate, wg_ref[at, :], TA) + mm(d_up, wu_ref[at, :], TA)
        return carry

    lax.fori_loop(0, ff // step, mlp, 0)
    copy.wait()
    d_kv = (dkv[pl.ds(pl.multiple_of(y * own, own), own), :] + dkv_in[...]).T
    lo, hi = turn(d_kv[:quarter], d_kv[quarter:hd], cos_t, -sin_t)
    d_kv = jnp.concatenate([lo, hi, d_kv[hd:]], axis=0).astype(BF16)
    small[0:2 * hd, :] = mm(d_kv, u_b[...])
    d_u = d0_ref[...] + mm(d_kv, wkv_ref[...], TA)
    _, u_hat, u_inv = norm_fwd(x0_ref[...], ln_ref[0:1, :])
    d_in, g_in = norm_bwd(d_u, u_hat, u_inv, ln_ref[0:1, :])
    d0_ref[...] = d_one[...] + d_in
    small[2 * hd:, :] = jnp.zeros_like(small[2 * hd:, :])
    small[2 * hd:2 * hd + 1, :] = g_in.reshape(1, width)
    small[2 * hd + 1:2 * hd + 2, :] = g_fin.reshape(1, width)
    small[2 * hd + 2:2 * hd + 3, :] = loss_ref[...]
    shards = rows_ref.shape[0]
    copies = []

    def put(src, first, size, s):
        copies.append(pltpu.make_async_copy(src, rows_ref.at[s, pl.ds(first, size), :], out_sem.at[len(copies)]))

    n_kv = 2 * hd // shards
    for s in range(shards):
        at = 0
        for g, size in ((g_q, nq // shards), (g_o, nq // shards), (g_g, ff // shards), (g_u, ff // shards), (g_d, ff // shards)):
            put(g.at[pl.ds(s * size, size), :], at, size, s)
            at += size
        put(small.at[pl.ds(s * n_kv, n_kv), :], at, n_kv, s)
        put(small.at[pl.ds(2 * hd + (0 if s == 0 else 16), 16), :], at + n_kv, 16, s)
    for c in copies:
        c.start()
    for c in copies:
        c.wait()


def layer_bwd(d_fin, x0, x1, loss_row, ln, cos_t, sin_t, weights, saved, collective_id):
    own, width = x0.shape
    nq = weights[0].shape[0]
    two_hd = weights[1].shape[0]
    ff = weights[3].shape[0]
    rows = (2 * nq + 3 * ff + two_hd) // (2 * NZ) + 16
    chunk = (own, width)
    return pl.pallas_call(
        layer_bwd_kernel,
        out_shape=(jax.ShapeDtypeStruct((2 * NZ, rows, width), F32), jax.ShapeDtypeStruct(chunk, F32)),
        in_specs=[VMEM] * 18,
        out_specs=(ANY, VMEM),
        scratch_shapes=[pltpu.VMEM(chunk, F32), pltpu.VMEM(chunk, BF16), pltpu.VMEM(chunk, BF16), pltpu.VMEM((nq, own), BF16),
                        pltpu.VMEM((nq, own), BF16), pltpu.VMEM((2 * own, two_hd), F32), pltpu.VMEM((own, two_hd), F32),
                        pltpu.VMEM((nq, width), F32), pltpu.VMEM((nq, width), F32)] + [pltpu.VMEM((ff, width), F32)] * 3
        + [pltpu.VMEM((two_hd + 32, width), F32), pltpu.SemaphoreType.DMA((14 * NZ,)), pltpu.SemaphoreType.DMA, pltpu.SemaphoreType.DMA],
        compiler_params=pltpu.CompilerParams(collective_id=collective_id, has_side_effects=True, vmem_limit_bytes=60000000),
        name="layer_bwd",
    )(d_fin, x0, x1, loss_row, ln, cos_t, sin_t, *weights, *saved)


N_BLOCK = 12
EARLY = 9
W_REDUCE = {
    0: {0: (3,), 2: (2,), 4: (1,), 6: (0,)},
    1: {2: (3,), 4: (2, 0), 6: (1,)},
    2: {2: (0,), 4: (1, 3), 6: (2,)},
    3: {0: (0,), 2: (1,), 4: (2,), 6: (3,)},
}


def tail_kernel(g_ref, p_ref, e_ref, m_ref, v_ref, e_new, m_new, v_new, w_out, small_ref,
                s_buf, from_c, from_x, t_buf, state_in, state_out, acc, w_c, w_y, w_l, w_r, w_x,
                g_load, g_send_c, g_recv_c, g_send_x, g_recv_x, g_send_t, g_recv_t, in_sem, out_sem,
                w_load, w_out_sem, send_c, send_y, send_l, send_r, recv_c, recv_y, recv_l, recv_r, last_send, last_recv, small_send, small_recv):
    tp, dp, z, y = place()
    partner = tp + 1 - 2 * y
    core = dp % 2
    twin = dp + 1 - 2 * core
    facing = lax.rem(dp + 2, 4)
    half = g_ref.shape[0] // 2
    size = s_buf.shape[1]
    sizes = [min(size, half - b * size) for b in range(N_BLOCK)]

    def rows(which, b):
        return pl.ds(pl.multiple_of(which * half + b * size, 8), sizes[b])

    def part(buf, b):
        return buf.at[b, pl.ds(0, sizes[b]), :]

    todo = [(0, 0)] + [pair for b in range(1, N_BLOCK) for pair in ((0, b), (1, b - 1))] + [(1, N_BLOCK - 1)]

    def state_loads(q):
        other, b = todo[q]
        at = rows(core + other - 2 * core * other, b)
        return [pltpu.make_async_copy(ref.at[at, :], state_in.at[q % 2, n, pl.ds(0, sizes[b]), :], in_sem.at[q % 2, n])
                for n, ref in enumerate((e_ref, m_ref, v_ref))]

    def state_stores(q):
        other, b = todo[q]
        at = rows(core + other - 2 * core * other, b)
        return [pltpu.make_async_copy(state_out.at[q % 2, n, pl.ds(0, sizes[b]), :], ref.at[at, :], out_sem.at[q % 2, n])
                for n, ref in enumerate((e_new, m_new, v_new))]

    def update(q):
        other, b = todo[q]
        grad = from_x if other == 0 else t_buf
        for c in state_loads(q):
            c.wait()
        if q >= 2:
            for c in state_stores(q - 2):
                c.wait()

        def body(n, carry):
            at = pl.ds(pl.multiple_of(n * 24, 8), 24)
            new = adam_update(state_in[q % 2, 0, at, :], grad[b, at, :], state_in[q % 2, 1, at, :], state_in[q % 2, 2, at, :])
            for i in range(3):
                state_out[q % 2, i, at, :] = new[i]
            return carry

        lax.fori_loop(0, sizes[b] // 24, body, 0)
        for c in state_stores(q):
            c.start()
        if q + 2 < len(todo):
            for c in state_loads(q + 2):
                c.start()

    plane_barrier(tp, dp, [(tp, twin), (tp, facing)])
    for q in range(2):
        for c in state_loads(q):
            c.start()

    def g_first(b):
        remote(g_ref.at[rows(1 - core, b), :], part(from_c, b), g_send_c.at[b], g_recv_c.at[b], tp, twin).start()
        pltpu.make_async_copy(g_ref.at[rows(core, b), :], part(s_buf, b), g_load.at[b]).start()

    def g_chip_sum(b):
        pltpu.make_async_copy(g_ref.at[rows(core, b), :], part(s_buf, b), g_load.at[b]).wait()
        remote(part(s_buf, b), part(from_c, b), g_send_c.at[b], g_recv_c.at[b], tp, twin).wait_recv()
        add_into(part(s_buf, b), part(from_c, b), 24)

    def g_copy_x(b):
        return remote(part(s_buf, b), part(from_x, b), g_send_x.at[b], g_recv_x.at[b], tp, facing)

    def g_copy_t(b):
        return remote(part(from_x, b), part(t_buf, b), g_send_t.at[b], g_recv_t.at[b], tp, twin)

    def w_first(k):
        for zz in REDUCE_ORDER[k]:
            for slot in (2 * zz + 1 - y, 2 * zz + y):
                remote(p_ref.at[slot, 1 - core], w_c.at[slot], send_c.at[slot], recv_c.at[slot], tp, twin).start()
                pltpu.make_async_copy(p_ref.at[slot, core], acc.at[slot], w_load.at[slot]).start()

    def w_chip_sum(slot):
        pltpu.make_async_copy(p_ref.at[slot, core], acc.at[slot], w_load.at[slot]).wait()
        remote(acc.at[slot], w_c.at[slot], send_c.at[slot], recv_c.at[slot], tp, twin).wait_recv()
        add_into(acc.at[slot], w_c.at[slot])

    def w_second(k):
        for zz in REDUCE_ORDER[k]:
            slot = 2 * zz + 1 - y
            w_chip_sum(slot)
            remote(acc.at[slot], w_y.at[zz], send_y.at[zz], recv_y.at[zz], partner, dp).start()
        for zz in REDUCE_ORDER[k]:
            w_chip_sum(2 * zz + y)

    def w_reduce(k, shards):
        for zz in shards:
            line = acc.at[2 * zz + y]
            remote(line, w_y.at[zz], send_y.at[zz], recv_y.at[zz], partner, dp).wait_recv()
            add_into(line, w_y.at[zz])
            if zz >= k and k > 0:
                remote(line, w_l.at[zz - 1], send_l.at[zz], recv_l.at[zz], partner, dp).wait_recv()
                add_into(line, w_l.at[zz - 1])
            if zz <= k and k < NZ - 1:
                remote(line, w_r.at[zz], send_r.at[zz], recv_r.at[zz], partner, dp).wait_recv()
                add_into(line, w_r.at[zz])
            if zz > k:
                remote(line, w_l.at[zz - 1], send_r.at[zz], recv_l.at[zz], tp + 2, dp).start()
            if zz < k:
                remote(line, w_r.at[zz], send_l.at[zz], recv_r.at[zz], tp - 2, dp).start()

    def on_position(f):
        for k in range(NZ):
            pl.when(z == k)(functools.partial(f, k))

    g_first(0)
    g_first(1)
    on_position(w_first)
    for b in range(2, N_BLOCK):
        g_first(b)
    for b in range(2):
        g_chip_sum(b)
        g_copy_x(b).start()
    on_position(w_second)
    for b in range(2, EARLY):
        g_chip_sum(b)
        g_copy_x(b).start()

    total = acc.at[tp]
    w_copy_x = remote(total, w_x, last_send.at[0], last_recv.at[0], tp, facing)
    w_copy_c = remote(total, w_out.at[core], last_send.at[1], last_recv.at[1], tp, twin)
    w_store = pltpu.make_async_copy(total, w_out.at[core], w_out_sem)
    n_small, n_rows = small_ref.shape[1], w_out.shape[1]
    mine = w_out.at[1, pl.ds(n_rows - 32, n_small), :]
    small_here = pltpu.make_async_copy(mine, small_ref.at[tp], w_out_sem)
    peers = [lax.rem(tp + n, 2 * NZ) for n in range(1, 2 * NZ)]
    q = 0
    for b in range(N_BLOCK):
        g_copy_x(b).wait_recv()
        add_into(part(from_x, b), part(s_buf, b), 24)
        g_copy_t(b).start()
        update(q)
        q += 1
        if b > 0:
            g_copy_t(b - 1).wait_recv()
            update(q)
            q += 1
        for k in range(NZ):
            if b in W_REDUCE[k]:
                pl.when(z == k)(functools.partial(w_reduce, k, W_REDUCE[k][b]))
        if b == 6:
            w_copy_x.start()
            for late in range(EARLY, N_BLOCK):
                g_chip_sum(late)
                g_copy_x(late).start()
        if b == 8:
            w_copy_x.wait()
            add_into(total, w_x)
            w_copy_c.start()
            w_store.start()
        if b == 9:
            w_copy_c.wait_send()
            remote(total, w_out.at[1 - core], last_send.at[1], last_recv.at[1], tp, twin).wait_recv()
            w_store.wait()
            for to in peers:
                remote(mine, small_ref.at[tp], small_send.at[to], small_recv.at[tp], to, dp).start()
            small_here.start()
    g_copy_t(N_BLOCK - 1).wait_recv()
    update(q)
    for source in peers:
        remote(small_ref.at[source], small_ref.at[source], small_send.at[source], small_recv.at[source], source, dp).wait_recv()
        remote(mine, small_ref.at[tp], small_send.at[source], small_recv.at[tp], source, dp).wait_send()
    small_here.wait()
    for b in range(N_BLOCK):
        remote(g_ref.at[rows(1 - core, b), :], part(from_c, b), g_send_c.at[b], g_recv_c.at[b], tp, twin).wait_send()
        g_copy_x(b).wait_send()
        g_copy_t(b).wait_send()

    def w_done(k):
        for zz in range(NZ):
            line = acc.at[2 * zz + y]
            for slot in (2 * zz + 1 - y, 2 * zz + y):
                remote(p_ref.at[slot, 1 - core], w_c.at[slot], send_c.at[slot], recv_c.at[slot], tp, twin).wait_send()
            remote(line, w_y.at[zz], send_y.at[zz], recv_y.at[zz], partner, dp).wait_send()
            if zz > k:
                remote(line, w_l.at[zz - 1], send_r.at[zz], recv_l.at[zz], tp + 2, dp).wait_send()
            if zz < k:
                remote(line, w_r.at[zz], send_l.at[zz], recv_r.at[zz], tp - 2, dp).wait_send()

    on_position(w_done)
    for last in (len(todo) - 2, len(todo) - 1):
        for c in state_stores(last):
            c.wait()


def tail(g_table, g_rows, embed, m_embed, v_embed, collective_id):
    vocab, width = embed.shape
    rows = g_rows.shape[1]
    half = (rows // 2, width)
    size = -(-vocab // (2 * N_BLOCK * 24)) * 24
    blocks = pltpu.VMEM((N_BLOCK, size, width), F32)
    dma = lambda *n: pltpu.SemaphoreType.DMA(n)
    table = jax.ShapeDtypeStruct((vocab, width), F32)
    *new, w_sum, small = pl.pallas_call(
        tail_kernel,
        out_shape=(table, table, table, jax.ShapeDtypeStruct((2,) + half, F32), jax.ShapeDtypeStruct((2 * NZ, 24, width), F32)),
        in_specs=[ANY] * 5,
        out_specs=(ANY,) * 5,
        scratch_shapes=[blocks] * 4 + [pltpu.VMEM((2, 3, size, width), F32)] * 2
        + [pltpu.VMEM((2 * NZ,) + half, F32)] * 2 + [pltpu.VMEM((NZ,) + half, F32)] + [pltpu.VMEM((NZ - 1,) + half, F32)] * 2
        + [pltpu.VMEM(half, F32)]
        + [dma(N_BLOCK)] * 7 + [dma(2, 3)] * 2
        + [dma(2 * NZ), pltpu.SemaphoreType.DMA] + [dma(2 * NZ), dma(NZ), dma(NZ), dma(NZ)] * 2 + [dma(2)] * 2 + [dma(2 * NZ)] * 2,
        compiler_params=pltpu.CompilerParams(collective_id=collective_id, has_side_effects=True, vmem_limit_bytes=67000000),
        name="tail",
    )(g_table, g_rows.reshape((2 * NZ, 2) + half), embed, m_embed, v_embed)
    return new, w_sum.reshape(rows, width), small


def norm_fwd(x_f32, scale):
    centered = x_f32 - jnp.mean(x_f32, axis=-1, keepdims=True)
    inv_std = lax.rsqrt(jnp.mean(centered * centered, axis=-1, keepdims=True) + LN_EPS)
    x_hat = centered * inv_std
    return (x_hat * scale).astype(BF16), x_hat, inv_std


def norm_bwd(d_out, x_hat, inv_std, scale):
    d_scale = jnp.sum(d_out * x_hat, axis=0)
    d_hat = d_out * scale
    d_in = inv_std * (d_hat - jnp.mean(d_hat, axis=-1, keepdims=True) - x_hat * jnp.mean(d_hat * x_hat, axis=-1, keepdims=True))
    return d_in, d_scale


def rope_tables(positions, head_dim):
    inv_freq = ROPE_BASE ** (-jnp.arange(0, head_dim, 2).astype(F32) / head_dim)
    angles = positions.astype(F32)[:, None] * inv_freq[None, :]
    return jnp.cos(angles), jnp.sin(angles)


def rotate(x_in, cos_t, sin_t):
    half_dim = x_in.shape[-1] // 2
    x_lo = x_in[..., :half_dim]
    x_hi = x_in[..., half_dim:]
    return jnp.concatenate([x_lo * cos_t - x_hi * sin_t, x_hi * cos_t + x_lo * sin_t], axis=-1)


def adam_update(param_in, grad_in, mom_in, vel_in):
    mom_new = BETA_ONE * mom_in + (1.0 - BETA_ONE) * grad_in
    vel_new = BETA_TWO * vel_in + (1.0 - BETA_TWO) * grad_in * grad_in
    return param_in - LEARN_RATE * mom_new / (jnp.sqrt(vel_new) + ADAM_EPS), mom_new, vel_new


def dot(spec, a, b):
    return jnp.einsum(spec, a, b, preferred_element_type=F32)


def solution(mesh):
    param_specs = (P('tp', None), P(None, None), P(None, 'tp'), P(None, None, None), P('tp', None), P(None, None, 'tp'), P('tp', None))
    n_tp = mesh.shape['tp']
    n_dp = mesh.shape['dp']

    def local_step(tokens, labels, *state_arrays):
        embed, ln_scales, w_q, w_kv, w_o, w_gu, w_down = state_arrays[0:7]
        batch_loc, seq_len = tokens.shape
        vocab_loc, d_model = embed.shape
        head_dim = w_kv.shape[2]
        q_loc = w_q.shape[1]
        f_loc = w_down.shape[0]
        heads = n_tp * q_loc // head_dim
        tok_loc = batch_loc * seq_len
        tok_total = tok_loc * n_dp
        own = tok_loc // n_tp
        tp_rank = lax.axis_index('tp')
        half = tp_rank % 2

        all_tokens = lax.all_gather(tokens, 'dp').reshape(n_dp * n_tp, own)
        strict = (jnp.arange(own)[:, None] > jnp.arange(own)[None, :]).astype(BF16)

        def routing(chunks):
            shard = chunks // vocab_loc
            row = chunks - shard * vocab_loc
            hot = (shard[:, :, None] == jnp.arange(n_tp)[None, None, :])
            before = dot('rs,nsj->nrj', strict, hot.astype(BF16))
            rank = jnp.sum(jnp.where(hot, before, 0.0), axis=-1).astype(jnp.int32)
            most = jnp.max(jnp.sum(hot.astype(jnp.int32), axis=1))
            return shard, row, rank, (most + CAP - 1) // CAP

        chunks = tokens.reshape(n_tp, own)
        shard, row, rank, _ = routing(chunks)
        rounds_all = routing(all_tokens)[3]
        slots = jnp.arange(CAP)
        my_shard = lax.dynamic_index_in_dim(shard, tp_rank, 0, keepdims=False)
        my_rank = lax.dynamic_index_in_dim(rank, tp_rank, 0, keepdims=False)

        def fetch(step, x_sum, collective_id):
            here = (shard[:, None, :] == tp_rank) & (rank[:, None, :] == slots[None, :, None] + step * CAP)
            ids = jnp.sum(jnp.where(here, row[:, None, :], 0), axis=-1).reshape(-1)
            rows_out = lax.optimization_barrier(jnp.take(embed, ids, axis=0)).astype(BF16).astype(F32).reshape(n_tp, CAP, d_model)
            rows_in = plane_swap(rows_out, False, collective_id).reshape(n_tp * CAP, d_model).astype(BF16)
            pick = (my_shard[:, None, None] == jnp.arange(n_tp)[None, :, None]) & (my_rank[:, None, None] == slots[None, None, :] + step * CAP)
            return x_sum + dot('rc,cd->rd', pick.reshape(own, n_tp * CAP).astype(BF16), rows_in)

        x_zero = fetch(0, jnp.zeros((own, d_model), F32), 0)
        x_zero = lax.while_loop(lambda s: s[0] < rounds_all, lambda s: (s[0] + 1, fetch(s[0], s[1], 1)), (jnp.int32(1), x_zero))[1]

        w_rows = jnp.concatenate([w_q.T, w_o, w_gu.transpose(0, 2, 1).reshape(2 * f_loc, d_model), w_down], axis=0)
        w_all = weight_gather(w_rows, 2).astype(BF16)
        cuts = (q_loc, 2 * q_loc, 2 * q_loc + f_loc, 2 * q_loc + 2 * f_loc)
        wq_t = w_all[:, :cuts[0]].reshape(-1, d_model)
        wo_b = w_all[:, cuts[0]:cuts[1]].reshape(-1, d_model)
        wg_t = w_all[:, cuts[1]:cuts[2]].reshape(-1, d_model)
        wu_t = w_all[:, cuts[2]:cuts[3]].reshape(-1, d_model)
        wd_b = w_all[:, cuts[3]:].reshape(-1, d_model)
        wkv_t = w_kv.transpose(0, 2, 1).reshape(2 * head_dim, d_model).astype(BF16)
        weights = (wq_t, wkv_t, wo_b, wg_t, wu_t, wd_b)
        inv_freq = ROPE_BASE ** (-jnp.arange(0, head_dim, 2).astype(F32) / head_dim)
        angles = inv_freq[:, None] * (half * own + jnp.arange(own)).astype(F32)[None, :]
        cos_t, sin_t = jnp.cos(angles), jnp.sin(angles)
        f_own, x_one, *saved = layer_fwd(x_zero, ln_scales, cos_t, sin_t, weights, 3)

        logit_scale = d_model ** -0.5
        lab_loc = labels.reshape(n_tp, own) - tp_rank * vocab_loc
        d_fin, g_head_part, log_norm, lab_sum = head(f_own, lab_loc, embed, logit_scale, logit_scale / tok_total, 4)
        log_norm = lax.dynamic_index_in_dim(log_norm, tp_rank, 0, keepdims=False)
        loss_row = (log_norm + LOGIT_ZLOSS * log_norm * log_norm - jnp.sum(lab_sum, axis=0) * logit_scale) / tok_total
        g_rows, d_zero = layer_bwd(d_fin, x_zero, x_one, loss_row[None, :], ln_scales, cos_t, sin_t, weights, saved, 7)

        def give_back(step, g_sum, collective_id):
            mine = (my_shard[None, None, :] == jnp.arange(n_tp)[:, None, None]) & (my_rank[None, None, :] == slots[None, :, None] + step * CAP)
            ids = jnp.sum(jnp.where(mine, jnp.arange(own)[None, None, :], 0), axis=-1).reshape(-1)
            rows_out = jnp.take(d_zero, ids, axis=0).reshape(n_tp, CAP, d_model)
            rows_in = plane_swap(rows_out, False, collective_id).reshape(-1, d_model)
            here = (shard[:, None, :] == tp_rank) & (rank[:, None, :] == slots[None, :, None] + step * CAP)
            row_id = jnp.where(jnp.any(here, axis=-1), jnp.sum(jnp.where(here, row[:, None, :], 0), axis=-1), vocab_loc).reshape(-1)
            return g_sum.at[row_id].add(rows_in, mode='drop')

        g_table = give_back(0, g_head_part, 8)
        g_table = lax.while_loop(lambda s: s[0] < rounds_all, lambda s: (s[0] + 1, give_back(s[0], s[1], 9)), (jnp.int32(1), g_table))[1]

        new_table, g_shard, g_small = tail(g_table, g_rows, embed, state_arrays[7], state_arrays[14], 10)
        n_kv = 2 * head_dim // n_tp
        g_kv = g_small[:, :n_kv].reshape(2, head_dim, d_model).transpose(0, 2, 1)
        loss = jnp.sum(g_small[0, n_kv + 2])
        gradients = (None, g_small[0, n_kv:n_kv + 2], g_shard[:cuts[0]].T, g_kv, g_shard[cuts[0]:cuts[1]],
                     g_shard[cuts[1]:cuts[3]].reshape(2, f_loc, d_model).transpose(0, 2, 1), g_shard[cuts[3]:cuts[3] + f_loc])

        outs_p, outs_m, outs_v = ([array] for array in new_table)
        for index in range(1, 7):
            new_p, new_m, new_v = adam_update(state_arrays[index], gradients[index], state_arrays[7 + index], state_arrays[14 + index])
            outs_p.append(new_p)
            outs_m.append(new_m)
            outs_v.append(new_v)
        return tuple(outs_p) + tuple(outs_m) + tuple(outs_v) + (loss,)

    return jax.shard_map(local_step, mesh=mesh, in_specs=(P('dp', None), P('dp', None)) + param_specs * 3,
                         out_specs=param_specs * 3 + (P(),), check_vma=False)
```

```python
import functools

import jax
import jax.numpy as jnp
from jax import lax
from jax.experimental import pallas as pl
from jax.experimental.pallas import tpu as pltpu
from jax.sharding import PartitionSpec as P

LN_EPS = 1e-5
LOGIT_ZLOSS = 1e-4
LEARN_RATE = 1e-2
BETA_ONE = 0.9
BETA_TWO = 0.95
ADAM_EPS = 1e-8
ROPE_BASE = 10000.0
NZ = 4
CAP = 96
F32 = jnp.float32
BF16 = jnp.bfloat16
ANY = pl.BlockSpec(memory_space=pl.ANY)
VMEM = pl.BlockSpec(memory_space=pltpu.VMEM)

ARRIVALS = {
    0: (("R", 1), ("R", 2), ("R", 3)),
    1: (("L", 0), ("R", 2), ("R", 3)),
    2: (("R", 3), ("L", 1), ("L", 0)),
    3: (("L", 2), ("L", 1), ("L", 0)),
}
REDUCE_ORDER = {0: (3, 2, 1, 0), 1: (3, 0, 2, 1), 2: (0, 3, 1, 2), 3: (0, 1, 2, 3)}


def remote(src, dst, send_sem, recv_sem, tp, dp):
    return pltpu.make_async_remote_copy(src_ref=src, dst_ref=dst, send_sem=send_sem, recv_sem=recv_sem,
                                        device_id=(tp, dp), device_id_type=pl.DeviceIdType.MESH)


def place():
    tp = lax.axis_index("tp")
    dp = lax.axis_index("dp")
    return tp, dp, tp // 2, tp % 2


def signal(tp, dp):
    pl.semaphore_signal(pltpu.get_barrier_semaphore(), inc=1, device_id=(tp, dp), device_id_type=pl.DeviceIdType.MESH)


def add_into(acc, other, step=None):
    rows = acc.shape[0]
    step = step or (64 if rows % 64 == 0 else 8)

    def body(n, carry):
        at = pl.ds(pl.multiple_of(n * step, step), step)
        acc[at, :] = acc[at, :] + other[at, :]
        return carry

    lax.fori_loop(0, rows // step, body, 0)


def plane_barrier(tp, dp, others):
    peers = [(lax.rem(tp + n, 2 * NZ), dp) for n in range(1, 2 * NZ)] + others
    for peer in peers:
        signal(*peer)
    pl.semaphore_wait(pltpu.get_barrier_semaphore(), len(peers))


def swap_kernel(x_ref, out_ref, own_sem, send, recv):
    tp, dp, _, _ = place()
    plane_barrier(tp, dp, [])
    copies = []
    for n in range(1, 2 * NZ):
        to = lax.rem(tp + n, 2 * NZ)
        copy = remote(x_ref.at[to], out_ref.at[tp], send.at[to], recv.at[tp], to, dp)
        copy.start()
        copies.append(copy)
    own = pltpu.make_async_copy(x_ref.at[tp], out_ref.at[tp], own_sem)
    own.start()
    for n in range(1, 2 * NZ):
        source = lax.rem(tp + n, 2 * NZ)
        remote(out_ref.at[source], out_ref.at[source], send.at[source], recv.at[source], source, dp).wait_recv()
    own.wait()
    for copy in copies:
        copy.wait_send()


def plane_swap(x, collective_id):
    return pl.pallas_call(
        swap_kernel,
        out_shape=jax.ShapeDtypeStruct(x.shape, x.dtype),
        in_specs=[ANY],
        out_specs=ANY,
        scratch_shapes=[pltpu.SemaphoreType.DMA] + [pltpu.SemaphoreType.DMA((2 * NZ,))] * 2,
        compiler_params=pltpu.CompilerParams(collective_id=collective_id, has_side_effects=True),
        name="plane_swap",
    )(x)


FORWARD = {
    0: {1: (("R", 1),), 3: (("R", 2),), 5: (("R", 3),)},
    1: {1: (("L", 0), ("R", 2)), 3: (("R", 3),)},
    2: {1: (("R", 3), ("L", 1)), 3: (("L", 0),)},
    3: {1: (("L", 2),), 3: (("L", 1),), 5: (("L", 0),)},
}
REDUCE = {
    0: {2: (3,), 4: (2,), 6: (1,), 7: (0,)},
    1: {4: (3,), 6: (2, 0), 7: (1,)},
    2: {4: (0,), 6: (1, 3), 7: (2,)},
    3: {2: (0,), 4: (1,), 6: (2,), 7: (3,)},
}
SUB = 256
GROUP = 6


def lookup(table, z, step):
    value = jnp.int32(0)
    for k in range(NZ):
        for s in range(2 * NZ):
            value = value + jnp.where((z == k) & (step == s), table[k][s], 0)
    return value


def head_kernel(scale, token_scale, f_ref, lab_ref, e_ref, dfin_ref, ghead_ref, norm_ref, labsum_ref,
                e_b, e_t, fbuf, f_b, g_acc, from_y, from_l, from_r, dl, lse_all, load_sem, ag_y, ag_l, ag_r, ag_recv,
                rs_y, rs_l, rs_r, recv_y, recv_l, recv_r, st_send, st_recv):
    tp, dp, z, y = place()
    partner = tp + 1 - 2 * y
    vocab, width = e_ref.shape
    own = f_ref.shape[0]
    whole = vocab // (SUB * GROUP)
    rest = vocab - whole * SUB * GROUP
    log2e = 1.4426950408889634
    slope = scale * log2e
    blocks = [(j * SUB, SUB) for j in range(GROUP)]
    tail = [(n, min(SUB, rest - n)) for n in range(0, rest, SUB)]

    plane_barrier(tp, dp, [])

    def send(src, slot, sems, to):
        remote(src, fbuf.at[slot], sems.at[slot], ag_recv.at[slot], to, dp).start()

    def arrived(slot):
        remote(f_ref, fbuf.at[slot], ag_y.at[slot], ag_recv.at[slot], partner, dp).wait_recv()

    def first_sends(k):
        if k > 0:
            send(f_ref, tp, ag_l, tp - 2)
        if k < NZ - 1:
            send(f_ref, tp, ag_r, tp + 2)
        send(f_ref, tp, ag_y, partner)

    for k in range(NZ):
        pl.when(z == k)(functools.partial(first_sends, k))
    load = pltpu.make_async_copy(e_ref, g_acc, load_sem.at[0])
    load.start()
    own_copy = pltpu.make_async_copy(f_ref, fbuf.at[tp], load_sem.at[1])
    own_copy.start()
    load.wait()

    def prepare(at, size):
        part = g_acc[at, :]
        e_b[at, :] = part.astype(BF16)
        e_t[:, at] = part.T.astype(BF16)

    def prepare_body(n, carry):
        prepare(pl.ds(pl.multiple_of(n * SUB, SUB), SUB), SUB)
        return carry

    lax.fori_loop(0, vocab // SUB, prepare_body, 0)
    if vocab % SUB:
        prepare(pl.ds(vocab // SUB * SUB, vocab % SUB), vocab % SUB)
    own_copy.wait()

    def over_blocks(group, carry):
        def body(n, c):
            return group(pl.multiple_of(n * SUB * GROUP, SUB * GROUP), blocks, c)
        carry = lax.fori_loop(0, whole, body, carry)
        return group(whole * SUB * GROUP, tail, carry) if tail else carry

    order1 = {k: (k,) + tuple(v for pair in zip([a[1] for a in ARRIVALS[k]], [k] + [a[1] for a in ARRIVALS[k]]) for v in pair) + (ARRIVALS[k][-1][1],) for k in range(NZ)}
    order1 = {k: [2 * zz + (s % 2 == 0 and s > 0 or s == 7) for s, zz in enumerate(order1[k])] for k in range(NZ)}

    def chunk_of(table, step):
        code = lookup(table, z, step)
        other = code % 2
        return code // 2 * 2 + y + other - 2 * y * other

    def gather_step(step, carry):
        slot = chunk_of(order1, step)
        for k in range(NZ):
            for s, shards in FORWARD[k].items():
                def pass_on(k=k, shards=shards):
                    for side, zz in shards:
                        at = 2 * zz + y
                        arrived(at)
                        if side == "L" and k < NZ - 1:
                            send(fbuf.at[at], at, ag_r, tp + 2)
                        if side == "R" and k > 0:
                            send(fbuf.at[at], at, ag_l, tp - 2)
                        send(fbuf.at[at], at, ag_y, partner)
                pl.when((z == k) & (step == s))(pass_on)
        pl.when(slot % 2 != y)(lambda: arrived(slot))
        f_b[slot] = fbuf[slot].astype(BF16)
        f_now = f_b[slot]

        def group(base, parts, c):
            top, total = c
            for first, size in parts:
                logit = lax.dot_general(e_b[pl.ds(base + first, size), :], f_now, (((1,), (1,)), ((), ())), preferred_element_type=F32)
                logit = logit.reshape(size // 8, 8, own)
                new = jnp.maximum(top, jnp.max(logit, axis=0))
                total = total * jnp.exp2((top - new) * slope) + jnp.sum(jnp.exp2((logit - new[None]) * slope), axis=0)
                top = new
            return top, total

        top, total = over_blocks(group, (jnp.full((8, own), -3e38, F32), jnp.zeros((8, own), F32)))
        most = jnp.max(top, axis=0, keepdims=True)
        total = jnp.sum(total * jnp.exp2((top - most) * slope), axis=0, keepdims=True)
        lse_all[tp, pl.ds(slot, 1), :] = most * scale + jnp.log(total)
        return carry

    lax.fori_loop(0, 2 * NZ, gather_step, 0)

    for n in range(1, 2 * NZ):
        to = lax.rem(tp + n, 2 * NZ)
        remote(lse_all.at[tp], lse_all.at[tp], st_send.at[to], st_recv.at[tp], to, dp).start()

    def gathers_done(k):
        def done(sems, slot):
            remote(f_ref, fbuf.at[slot], sems.at[slot], ag_recv.at[slot], partner, dp).wait_send()
        if k > 0:
            done(ag_l, tp)
        if k < NZ - 1:
            done(ag_r, tp)
        done(ag_y, tp)
        for side, zz in ARRIVALS[k]:
            at = 2 * zz + y
            if side == "L" and k < NZ - 1:
                done(ag_r, at)
            if side == "R" and k > 0:
                done(ag_l, at)
            done(ag_y, at)

    for k in range(NZ):
        pl.when(z == k)(functools.partial(gathers_done, k))

    def clear(n, carry):
        g_acc[pl.ds(pl.multiple_of(n * 16, 16), 16), :] = jnp.zeros((16, width), F32)
        return carry

    lax.fori_loop(0, vocab // 16, clear, 0)
    for n in range(1, 2 * NZ):
        source = lax.rem(tp + n, 2 * NZ)
        remote(lse_all.at[source], lse_all.at[source], st_send.at[source], st_recv.at[source], source, dp).wait_recv()
    peak = jnp.max(lse_all[...], axis=0)
    log_norm = peak + jnp.log(jnp.sum(jnp.exp(lse_all[...] - peak[None]), axis=0))
    norm_ref[...] = log_norm

    order2 = {k: [2 * zz + 1 - s for zz in REDUCE_ORDER[k] for s in range(2)] for k in range(NZ)}

    def scatter_step(step, lab_sum):
        slot = chunk_of(order2, step)
        f_now = f_b[slot]
        acc = fbuf.at[slot]
        norm = norm_ref[pl.ds(slot, 1), :]
        shift = norm * log2e
        coef = (1.0 + 2.0 * LOGIT_ZLOSS * norm) * token_scale
        lab = lab_ref[pl.ds(slot, 1), :]
        acc[...] = jnp.zeros((width, own), F32)

        def group(base, parts, hits):
            for first, size in parts:
                at = pl.ds(base + first, size)
                logit = lax.dot_general(e_b[at, :], f_now, (((1,), (1,)), ((), ())), preferred_element_type=F32)
                hit = lax.broadcasted_iota(jnp.int32, (size, own), 0) == lab - (base + first)
                prob = jnp.exp2(logit * slope - shift) * coef
                grad = jnp.where(hit, prob - token_scale, prob).astype(BF16)
                hits = hits + jnp.sum(jnp.where(hit, logit, 0.0).reshape(size // 8, 8, own), axis=0)
                dl[pl.ds(first, size), :] = grad
                g_acc[at, :] += jnp.dot(grad, f_now, preferred_element_type=F32)
            size = parts[-1][0] + parts[-1][1]
            acc[...] += jnp.dot(e_t[:, pl.ds(base, size)], dl[pl.ds(0, size), :], preferred_element_type=F32)
            return hits

        lab_sum = over_blocks(group, lab_sum)

        def hand_over():
            remote(acc, from_y.at[slot // 2], rs_y.at[slot // 2], recv_y.at[slot // 2], partner, dp).start()
        pl.when(slot % 2 != y)(hand_over)

        for k in range(NZ):
            for s, shards in REDUCE[k].items():
                def reduce(k=k, shards=shards):
                    for zz in shards:
                        line = fbuf.at[2 * zz + y]
                        remote(line, from_y.at[zz], rs_y.at[zz], recv_y.at[zz], partner, dp).wait_recv()
                        add_into(line, from_y.at[zz])
                        if zz >= k and k > 0:
                            remote(line, from_l.at[zz - 1], rs_l.at[zz], recv_l.at[zz], partner, dp).wait_recv()
                            add_into(line, from_l.at[zz - 1])
                        if zz <= k and k < NZ - 1:
                            remote(line, from_r.at[zz], rs_r.at[zz], recv_r.at[zz], partner, dp).wait_recv()
                            add_into(line, from_r.at[zz])
                        if zz > k:
                            remote(line, from_l.at[zz - 1], rs_r.at[zz], recv_l.at[zz], tp + 2, dp).start()
                        if zz < k:
                            remote(line, from_r.at[zz], rs_l.at[zz], recv_r.at[zz], tp - 2, dp).start()
                pl.when((z == k) & (step == s))(reduce)
        return lab_sum

    lab_sum = lax.fori_loop(0, 2 * NZ, scatter_step, jnp.zeros((8, own), F32))
    labsum_ref[...] = lab_sum
    store = pltpu.make_async_copy(g_acc, ghead_ref, load_sem.at[0])
    store.start()
    dfin_ref[...] = fbuf[tp].T

    def scatters_done(k):
        for zz in range(NZ):
            line = fbuf.at[2 * zz + y]
            remote(line, from_y.at[zz], rs_y.at[zz], recv_y.at[zz], partner, dp).wait_send()
            if zz > k:
                remote(line, from_l.at[zz - 1], rs_r.at[zz], recv_l.at[zz], partner, dp).wait_send()
            if zz < k:
                remote(line, from_r.at[zz], rs_l.at[zz], recv_r.at[zz], partner, dp).wait_send()

    for k in range(NZ):
        pl.when(z == k)(functools.partial(scatters_done, k))
    for n in range(1, 2 * NZ):
        to = lax.rem(tp + n, 2 * NZ)
        remote(lse_all.at[tp], lse_all.at[tp], st_send.at[to], st_recv.at[tp], to, dp).wait_send()
    store.wait()


def head(f_own, labels, embed, scale, token_scale, collective_id):
    own, width = f_own.shape
    vocab = embed.shape[0]
    chunk = (own, width)
    dma8 = pltpu.SemaphoreType.DMA((2 * NZ,))
    dma4 = pltpu.SemaphoreType.DMA((NZ,))
    return pl.pallas_call(
        functools.partial(head_kernel, scale, token_scale),
        out_shape=(jax.ShapeDtypeStruct((own, width), F32), jax.ShapeDtypeStruct((vocab, width), F32),
                   jax.ShapeDtypeStruct((2 * NZ, own), F32), jax.ShapeDtypeStruct((8, own), F32)),
        in_specs=[VMEM, VMEM, ANY],
        out_specs=(VMEM, ANY, VMEM, VMEM),
        scratch_shapes=[pltpu.VMEM((vocab, width), BF16), pltpu.VMEM((width, vocab), BF16),
                        pltpu.VMEM((2 * NZ,) + chunk, F32), pltpu.VMEM((2 * NZ,) + chunk, BF16), pltpu.VMEM((vocab, width), F32),
                        pltpu.VMEM((NZ,) + chunk, F32), pltpu.VMEM((NZ - 1,) + chunk, F32), pltpu.VMEM((NZ - 1,) + chunk, F32),
                        pltpu.VMEM((SUB * GROUP, own), BF16), pltpu.VMEM((2 * NZ, 2 * NZ, own), F32),
                        pltpu.SemaphoreType.DMA((2,)), dma8, dma8, dma8, dma8, dma4, dma4, dma4, dma4, dma4, dma4, dma8, dma8],
        compiler_params=pltpu.CompilerParams(collective_id=collective_id, has_side_effects=True, vmem_limit_bytes=67000000),
        cost_estimate=pl.CostEstimate(flops=8 * vocab * width * own * 8, bytes_accessed=3 * 4 * vocab * width, transcendentals=2 * vocab * own * 8),
        name="head",
    )(f_own, labels, embed)


TB = (((1,), (1,)), ((), ()))
TA = (((0,), (0,)), ((), ()))
LOG2E = 1.4426950408889634


def mm(a, b, dims=(((1,), (0,)), ((), ()))):
    return lax.dot_general(a, b, dims, preferred_element_type=F32)


def turn(lo, hi, cos_t, sin_t):
    return lo * cos_t - hi * sin_t, hi * cos_t + lo * sin_t


EVENTS = {
    0: (((("R", 1),), (0,)), ((("R", 2),), (1,)), ((("R", 3),), (2,)), ((), (3,))),
    1: (((("L", 0), ("R", 2)), (1,)), ((("R", 3),), (0,)), ((), (2,)), ((), (3,))),
    2: (((("R", 3), ("L", 1)), (2,)), ((("L", 0),), (3,)), ((), (1,)), ((), (0,))),
    3: (((("L", 2),), (3,)), ((("L", 1),), (2,)), ((("L", 0),), (1,)), ((), (0,))),
}
MLP_ORDER = {k: [2 * k] + [code for line, other in EVENTS[k] for code in [2 * zz for _, zz in line] + [2 * zz + 1 for zz in other]] for k in range(NZ)}


def front_kernel(rows_ref, pick_ref, extra_ref, w_ref, wkv_ref, ln_ref, cos_ref, sin_ref,
                 f_ref, x1_ref, x0_ref, q_ref, kv_ref, kvt_ref, lse_ref, ctx_ref, wq_ref, wo_ref, wg_ref, wu_ref, wd_ref,
                 wl, rows_in, u_b, kv_out, kv_in, own_sem, r_send, r_recv, a_y, a_l, a_r, a_c, a_recv,
                 b_y, b_l, b_r, b_x, b_c, b_recv, kv_send, kv_recv):
    tp, dp, z, y = place()
    partner = tp + 1 - 2 * y
    core = dp % 2
    twin = dp + 1 - 2 * core
    facing = lax.rem(dp + 2, 4)
    own, width = x0_ref.shape
    shards, w_rows = wl.shape[0], wl.shape[1]
    nq = q_ref.shape[0]
    ff = wg_ref.shape[0]
    n_a = nq // shards
    n_f = ff // shards
    n_b = 3 * n_f // 4
    hd = kv_out.shape[0] // 2
    quarter = hd // 2
    heads = nq // hd

    def a_rows(c):
        return pl.ds(pl.multiple_of(c * n_a, 8), n_a)

    def b_rows(d):
        return pl.ds(pl.multiple_of(2 * n_a + d * n_b, 8), n_b)

    def a_copy(slot, sems, to, to_dp, first=False):
        src = w_ref.at[a_rows(core), :] if first else wl.at[slot, a_rows(core), :]
        return remote(src, wl.at[slot, a_rows(core), :], sems.at[slot], a_recv.at[slot, core], to, to_dp)

    def b_copy(slot, piece, sems, to, to_dp, first=False):
        src = w_ref.at[b_rows(piece), :] if first else wl.at[slot, b_rows(piece), :]
        return remote(src, wl.at[slot, b_rows(piece), :], sems.at[slot], b_recv.at[slot, piece], to, to_dp)

    def a_wait(slot, c):
        remote(w_ref.at[a_rows(c), :], wl.at[slot, a_rows(c), :], a_y.at[slot], a_recv.at[slot, c], partner, dp).wait_recv()

    def b_wait(slot, piece):
        remote(w_ref.at[b_rows(piece), :], wl.at[slot, b_rows(piece), :], b_y.at[slot], b_recv.at[slot, piece], partner, dp).wait_recv()

    def on_position(f):
        for k in range(NZ):
            pl.when(z == k)(functools.partial(f, k))

    def line_sends(k, make, y_sems, l_sems, r_sems, slot, side, first=False):
        sends = [make(slot, y_sems, partner, dp, first)]
        if k > 0 and side != "L":
            sends.append(make(slot, l_sems, tp - 2, dp, first))
        if k < NZ - 1 and side != "R":
            sends.append(make(slot, r_sems, tp + 2, dp, first))
        return sends

    def b_own(slot, sems, to, to_dp, first=False):
        return b_copy(slot, dp, sems, to, to_dp, first)

    def a_sends(k, slot, side, first=False):
        return line_sends(k, a_copy, a_y, a_l, a_r, slot, side, first)

    def b_sends(k, slot, side, first=False):
        return line_sends(k, b_own, b_y, b_l, b_r, slot, side, first)

    def start(copies):
        for c in copies:
            c.start()

    plane_barrier(tp, dp, [(tp, twin), (tp, facing)])
    peers = [lax.rem(tp + n, shards) for n in range(1, shards)]

    def row_copy(to):
        return remote(rows_ref.at[to], rows_in.at[tp], r_send.at[to], r_recv.at[tp], to, dp)

    on_position(lambda k: start(b_sends(k, tp, "", True)))
    start([row_copy(to) for to in peers])
    on_position(lambda k: start(a_sends(k, tp, "", True)))
    own_rows = pltpu.make_async_copy(rows_ref.at[tp], rows_in.at[tp], own_sem.at[0])
    own_rows.start()
    own_w = pltpu.make_async_copy(w_ref, wl.at[tp], own_sem.at[1])
    own_w.start()

    def a_event(t, k):
        line, other = EVENTS[k][t]
        for side, zz in line:
            slot = 2 * zz + y
            a_wait(slot, core)
            start(a_sends(k, slot, side))
            a_copy(slot, a_c, tp, twin).start()
        for zz in other:
            slot = 2 * zz + 1 - y
            a_wait(slot, core)
            a_copy(slot, a_c, tp, twin).start()

    def b_event(t, k):
        line, other = EVENTS[k][t]
        for side, zz in line:
            slot = 2 * zz + y
            b_wait(slot, dp)
            start(b_sends(k, slot, side))
            b_copy(slot, dp, b_x, tp, facing).start()
            b_copy(slot, dp, b_c.at[0], tp, twin).start()
        for zz in other:
            slot = 2 * zz + 1 - y
            b_wait(slot, dp)
            b_copy(slot, dp, b_x, tp, facing).start()
            b_copy(slot, dp, b_c.at[0], tp, twin).start()

    on_position(functools.partial(b_event, 0))

    own_rows.wait()
    for source in peers:
        remote(rows_ref.at[source], rows_in.at[source], r_send.at[source], r_recv.at[source], source, dp).wait_recv()
    x0_ref[...] = extra_ref[...] + mm(pick_ref[...], rows_in[...].reshape(pick_ref.shape[1], width).astype(BF16))
    u_b[...] = norm_fwd(x0_ref[...], ln_ref[0:1, :])[0]
    x1_ref[...] = x0_ref[...]
    cos_t = cos_ref[...]
    sin_t = sin_ref[...]
    kv = mm(wkv_ref[...], u_b[...], TB)
    lo, hi = turn(kv[:quarter], kv[quarter:hd], cos_t, sin_t)
    kv_out[0:quarter, :] = lo
    kv_out[quarter:hd, :] = hi
    kv_out[hd:, :] = kv[hd:]
    kv_copy = remote(kv_out, kv_in, kv_send, kv_recv, partner, dp)
    kv_copy.start()

    on_position(functools.partial(a_event, 0))
    on_position(functools.partial(b_event, 1))
    on_position(functools.partial(a_event, 1))
    on_position(functools.partial(b_event, 2))
    on_position(functools.partial(a_event, 2))
    on_position(functools.partial(a_event, 3))
    on_position(functools.partial(b_event, 3))
    own_w.wait()
    for source in peers:
        a_wait(source, 1 - core)
    for s in range(shards):
        wq_ref[s * n_a:(s + 1) * n_a, :] = wl[s, 0:n_a, :].astype(BF16)
        wo_ref[s * n_a:(s + 1) * n_a, :] = wl[s, n_a:2 * n_a, :].astype(BF16)

    q_all = mm(wq_ref[...], u_b[...], TB)
    for h in range(heads):
        lo, hi = turn(q_all[h * hd:h * hd + quarter], q_all[h * hd + quarter:(h + 1) * hd], cos_t, sin_t)
        q_ref[h * hd:h * hd + quarter, :] = lo.astype(BF16)
        q_ref[h * hd + quarter:(h + 1) * hd, :] = hi.astype(BF16)
    kv_copy.wait()

    def fill(mine, other):
        kv_ref[mine * own:(mine + 1) * own, :] = kv_out[...].T.astype(BF16)
        kv_ref[other * own:(other + 1) * own, :] = kv_in[...].T.astype(BF16)
        kvt_ref[:, mine * own:(mine + 1) * own] = kv_out[...].astype(BF16)
        kvt_ref[:, other * own:(other + 1) * own] = kv_in[...].astype(BF16)

    pl.when(y == 0)(lambda: fill(0, 1))
    pl.when(y == 1)(lambda: fill(1, 0))
    blank = jnp.zeros((hd, own), BF16)
    slope = hd ** -0.5 * LOG2E

    def attend(h, carry):
        at = pl.ds(pl.multiple_of(h * hd, hd), hd)
        scores = mm(kv_ref[...], jnp.concatenate([q_ref[at, :], blank], axis=0))
        allowed = lax.broadcasted_iota(jnp.int32, scores.shape, 0) <= lax.broadcasted_iota(jnp.int32, scores.shape, 1) + y * own
        scores = jnp.where(allowed, scores * slope, -1e30)
        top = jnp.max(scores, axis=0, keepdims=True)
        prob = jnp.exp2(scores - top)
        total = jnp.sum(prob, axis=0, keepdims=True)
        lse_ref[pl.ds(h, 1), :] = top + jnp.log2(total)
        ctx_ref[at, :] = mm(kvt_ref[hd:, :], (prob * (1.0 / total)).astype(BF16)).astype(BF16)
        return carry

    lax.fori_loop(0, heads, attend, 0)
    x1_ref[...] += mm(ctx_ref[...], wo_ref[...], TA)

    def slot_of(step):
        code = lookup(MLP_ORDER, z, step)
        other = code % 2
        return code // 2 * 2 + y + other - 2 * y * other

    def mlp(step, carry):
        def pass_on():
            slot = slot_of(step + 1)
            b_wait(slot, facing)
            b_copy(slot, facing, b_c.at[1], tp, twin).start()
        pl.when(step < shards - 1)(pass_on)
        slot = slot_of(step)

        def rest():
            b_wait(slot, twin)
            b_wait(slot, lax.rem(twin + 2, 4))
        pl.when(step > 0)(rest)
        at = pl.ds(pl.multiple_of(slot * n_f, n_f), n_f)
        wg_ref[at, :] = wl[slot, 2 * n_a:2 * n_a + n_f, :].astype(BF16)
        wu_ref[at, :] = wl[slot, 2 * n_a + n_f:2 * n_a + 2 * n_f, :].astype(BF16)
        wd_ref[at, :] = wl[slot, 2 * n_a + 2 * n_f:2 * n_a + 3 * n_f, :].astype(BF16)
        gate = mm(u_b[...], wg_ref[at, :], TB)
        up = mm(u_b[...], wu_ref[at, :], TB)
        x1_ref[...] += mm((gate * jax.nn.sigmoid(gate) * up).astype(BF16), wd_ref[at, :])
        return carry

    lax.fori_loop(0, shards, mlp, 0)
    f_ref[...] = norm_fwd(x1_ref[...], ln_ref[1:2, :])[0].astype(F32)

    def finish(k):
        done = a_sends(k, tp, "", True) + b_sends(k, tp, "", True)
        for line, other in EVENTS[k]:
            for side, zz in line:
                done += a_sends(k, 2 * zz + y, side) + b_sends(k, 2 * zz + y, side)
        for c in done:
            c.wait_send()

    on_position(finish)
    for to in peers:
        row_copy(to).wait_send()
        a_copy(to, a_c, tp, twin).wait_send()
        b_copy(to, dp, b_x, tp, facing).wait_send()
        b_copy(to, dp, b_c.at[0], tp, twin).wait_send()
        b_copy(to, facing, b_c.at[1], tp, twin).wait_send()


def front(rows, pick, extra, w_rows, wkv_t, ln, cos_t, sin_t, n_q, collective_id):
    own, width = extra.shape
    two_hd = wkv_t.shape[0]
    shards = 2 * NZ
    ff = (w_rows.shape[0] * shards - 2 * n_q) // 3
    dma = lambda *n: pltpu.SemaphoreType.DMA(n)
    s = jax.ShapeDtypeStruct
    return pl.pallas_call(
        front_kernel,
        out_shape=(s((own, width), F32),) * 3 + (s((n_q, own), BF16), s((2 * own, two_hd), BF16), s((two_hd, 2 * own), BF16),
                   s((2 * n_q // two_hd, own), F32), s((n_q, own), BF16), s((n_q, width), BF16), s((n_q, width), BF16))
        + (s((ff, width), BF16),) * 3,
        in_specs=[VMEM] * 3 + [ANY] + [VMEM] * 4,
        out_specs=(VMEM,) * 13,
        scratch_shapes=[pltpu.VMEM((shards,) + w_rows.shape, F32), pltpu.VMEM(rows.shape, F32), pltpu.VMEM((own, width), BF16),
                        pltpu.VMEM((two_hd, own), F32), pltpu.VMEM((two_hd, own), F32),
                        dma(2), dma(shards), dma(shards)] + [dma(shards)] * 4 + [dma(shards, 2)]
        + [dma(shards)] * 4 + [dma(2, shards), dma(shards, 4), pltpu.SemaphoreType.DMA, pltpu.SemaphoreType.DMA],
        compiler_params=pltpu.CompilerParams(collective_id=collective_id, has_side_effects=True, vmem_limit_bytes=60000000),
        name="front",
    )(rows, pick, extra, w_rows, wkv_t, ln, cos_t, sin_t)


def layer_bwd_kernel(dfin_ref, x0_ref, x1_ref, loss_ref, ln_ref, cos_ref, sin_ref, wq_ref, wkv_ref, wo_ref, wg_ref, wu_ref, wd_ref,
                     q_ref, kv_ref, kvt_ref, lse_ref, ctx_ref, rows_ref, d0_ref, d_one, d_b, u_b, dctx, dq, dkv, dkv_in,
                     g_q, g_o, g_g, g_u, g_d, small, out_sem, send_sem, recv_sem):
    tp, dp, _, y = place()
    partner = tp + 1 - 2 * y
    own, width = x0_ref.shape
    hd = kv_ref.shape[1] // 2
    quarter = hd // 2
    nq = q_ref.shape[0]
    heads = nq // hd
    ff = wg_ref.shape[0]
    signal(partner, dp)
    _, f_hat, f_inv = norm_fwd(x1_ref[...], ln_ref[1:2, :])
    d_in, g_fin = norm_bwd(dfin_ref[...], f_hat, f_inv, ln_ref[1:2, :])
    d_one[...] = d_in
    d_b[...] = d_in.astype(BF16)
    u_b[...] = norm_fwd(x0_ref[...], ln_ref[0:1, :])[0]
    dctx[...] = mm(wo_ref[...], d_b[...], TB).astype(BF16)
    g_o[...] = mm(ctx_ref[...], d_b[...])
    cos_t = cos_ref[...]
    sin_t = sin_ref[...]
    blank = jnp.zeros((hd, own), BF16)
    slope = hd ** -0.5 * LOG2E
    dkv[...] = jnp.zeros_like(dkv)

    def attend(h, carry):
        at = pl.ds(pl.multiple_of(h * hd, hd), hd)
        q_pad = jnp.concatenate([q_ref[at, :], blank], axis=0)
        d_pad = jnp.concatenate([blank, dctx[at, :]], axis=0)
        scores = mm(kv_ref[...], q_pad)
        allowed = lax.broadcasted_iota(jnp.int32, scores.shape, 0) <= lax.broadcasted_iota(jnp.int32, scores.shape, 1) + y * own
        prob = jnp.where(allowed, jnp.exp2(scores * slope - lse_ref[pl.ds(h, 1), :]), 0.0)
        d_prob = mm(kv_ref[...], d_pad)
        mean = jnp.sum(d_prob * prob, axis=0, keepdims=True)
        d_score = (prob * (d_prob - mean) * hd ** -0.5).astype(BF16)
        dkv[...] += mm(d_score, q_pad, TB) + mm(prob.astype(BF16), d_pad, TB)
        d_q = mm(kvt_ref[0:hd, :], d_score)
        lo, hi = turn(d_q[:quarter], d_q[quarter:], cos_t, -sin_t)
        dq[at, :] = jnp.concatenate([lo, hi], axis=0).astype(BF16)
        return carry

    lax.fori_loop(0, heads, attend, 0)
    pl.semaphore_wait(pltpu.get_barrier_semaphore(), 1)
    copy = remote(dkv.at[pl.ds(pl.multiple_of((1 - y) * own, own), own), :], dkv_in, send_sem, recv_sem, partner, dp)
    copy.start()

    d0_ref[...] = mm(dq[...], wq_ref[...], TA)
    g_q[...] = mm(dq[...], u_b[...])
    step = min(512, ff)

    def mlp(n, carry):
        at = pl.ds(pl.multiple_of(n * step, step), step)
        gate = mm(wg_ref[at, :], u_b[...], TB)
        up = mm(wu_ref[at, :], u_b[...], TB)
        d_hidden = mm(wd_ref[at, :], d_b[...], TB)
        sig = jax.nn.sigmoid(gate)
        g_d[at, :] = mm((gate * sig * up).astype(BF16), d_b[...])
        d_gate = (d_hidden * up * sig * (1.0 + gate * (1.0 - sig))).astype(BF16)
        d_up = (d_hidden * gate * sig).astype(BF16)
        g_g[at, :] = mm(d_gate, u_b[...])
        g_u[at, :] = mm(d_up, u_b[...])
        d0_ref[...] += mm(d_gate, wg_ref[at, :], TA) + mm(d_up, wu_ref[at, :], TA)
        return carry

    lax.fori_loop(0, ff // step, mlp, 0)
    copy.wait()
    d_kv = (dkv[pl.ds(pl.multiple_of(y * own, own), own), :] + dkv_in[...]).T
    lo, hi = turn(d_kv[:quarter], d_kv[quarter:hd], cos_t, -sin_t)
    d_kv = jnp.concatenate([lo, hi, d_kv[hd:]], axis=0).astype(BF16)
    small[0:2 * hd, :] = mm(d_kv, u_b[...])
    d_u = d0_ref[...] + mm(d_kv, wkv_ref[...], TA)
    _, u_hat, u_inv = norm_fwd(x0_ref[...], ln_ref[0:1, :])
    d_in, g_in = norm_bwd(d_u, u_hat, u_inv, ln_ref[0:1, :])
    d0_ref[...] = d_one[...] + d_in
    small[2 * hd:, :] = jnp.zeros_like(small[2 * hd:, :])
    small[2 * hd:2 * hd + 1, :] = g_in.reshape(1, width)
    small[2 * hd + 1:2 * hd + 2, :] = g_fin.reshape(1, width)
    small[2 * hd + 2:2 * hd + 3, :] = loss_ref[...]
    shards = rows_ref.shape[0]
    copies = []

    def put(src, first, size, s):
        copies.append(pltpu.make_async_copy(src, rows_ref.at[s, pl.ds(first, size), :], out_sem.at[len(copies)]))

    n_kv = 2 * hd // shards
    for s in range(shards):
        at = 0
        for g, size in ((g_q, nq // shards), (g_o, nq // shards), (g_g, ff // shards), (g_u, ff // shards), (g_d, ff // shards)):
            put(g.at[pl.ds(s * size, size), :], at, size, s)
            at += size
        put(small.at[pl.ds(s * n_kv, n_kv), :], at, n_kv, s)
        put(small.at[pl.ds(2 * hd + (0 if s == 0 else 16), 16), :], at + n_kv, 16, s)
    for c in copies:
        c.start()
    for c in copies:
        c.wait()


def layer_bwd(d_fin, x0, x1, loss_row, ln, cos_t, sin_t, weights, saved, collective_id):
    own, width = x0.shape
    nq = weights[0].shape[0]
    two_hd = weights[1].shape[0]
    ff = weights[3].shape[0]
    rows = (2 * nq + 3 * ff + two_hd) // (2 * NZ) + 16
    chunk = (own, width)
    return pl.pallas_call(
        layer_bwd_kernel,
        out_shape=(jax.ShapeDtypeStruct((2 * NZ, rows, width), F32), jax.ShapeDtypeStruct(chunk, F32)),
        in_specs=[VMEM] * 18,
        out_specs=(ANY, VMEM),
        scratch_shapes=[pltpu.VMEM(chunk, F32), pltpu.VMEM(chunk, BF16), pltpu.VMEM(chunk, BF16), pltpu.VMEM((nq, own), BF16),
                        pltpu.VMEM((nq, own), BF16), pltpu.VMEM((2 * own, two_hd), F32), pltpu.VMEM((own, two_hd), F32),
                        pltpu.VMEM((nq, width), F32), pltpu.VMEM((nq, width), F32)] + [pltpu.VMEM((ff, width), F32)] * 3
        + [pltpu.VMEM((two_hd + 32, width), F32), pltpu.SemaphoreType.DMA((14 * NZ,)), pltpu.SemaphoreType.DMA, pltpu.SemaphoreType.DMA],
        compiler_params=pltpu.CompilerParams(collective_id=collective_id, has_side_effects=True, vmem_limit_bytes=60000000),
        name="layer_bwd",
    )(d_fin, x0, x1, loss_row, ln, cos_t, sin_t, *weights, *saved)


N_BLOCK = 12
EARLY = 9
W_REDUCE = {
    0: {0: (3,), 2: (2,), 4: (1,), 6: (0,)},
    1: {2: (3,), 4: (2, 0), 6: (1,)},
    2: {2: (0,), 4: (1, 3), 6: (2,)},
    3: {0: (0,), 2: (1,), 4: (2,), 6: (3,)},
}


def tail_kernel(g_ref, p_ref, e_ref, m_ref, v_ref, e_new, m_new, v_new, w_out, small_ref,
                s_buf, from_c, from_x, t_buf, state_in, state_out, acc, w_c, w_y, w_l, w_r, w_x,
                g_load, g_send_c, g_recv_c, g_send_x, g_recv_x, g_send_t, g_recv_t, in_sem, out_sem,
                w_load, w_out_sem, send_c, send_y, send_l, send_r, recv_c, recv_y, recv_l, recv_r, last_send, last_recv, small_send, small_recv):
    tp, dp, z, y = place()
    partner = tp + 1 - 2 * y
    core = dp % 2
    twin = dp + 1 - 2 * core
    facing = lax.rem(dp + 2, 4)
    half = g_ref.shape[0] // 2
    size = s_buf.shape[1]
    sizes = [min(size, half - b * size) for b in range(N_BLOCK)]

    def rows(which, b):
        return pl.ds(pl.multiple_of(which * half + b * size, 8), sizes[b])

    def part(buf, b):
        return buf.at[b, pl.ds(0, sizes[b]), :]

    todo = [(0, 0)] + [pair for b in range(1, N_BLOCK) for pair in ((0, b), (1, b - 1))] + [(1, N_BLOCK - 1)]

    def state_loads(q):
        other, b = todo[q]
        at = rows(core + other - 2 * core * other, b)
        return [pltpu.make_async_copy(ref.at[at, :], state_in.at[q % 2, n, pl.ds(0, sizes[b]), :], in_sem.at[q % 2, n])
                for n, ref in enumerate((e_ref, m_ref, v_ref))]

    def state_stores(q):
        other, b = todo[q]
        at = rows(core + other - 2 * core * other, b)
        return [pltpu.make_async_copy(state_out.at[q % 2, n, pl.ds(0, sizes[b]), :], ref.at[at, :], out_sem.at[q % 2, n])
                for n, ref in enumerate((e_new, m_new, v_new))]

    def update(q):
        other, b = todo[q]
        grad = from_x if other == 0 else t_buf
        for c in state_loads(q):
            c.wait()
        if q >= 2:
            for c in state_stores(q - 2):
                c.wait()

        def body(n, carry):
            at = pl.ds(pl.multiple_of(n * 24, 8), 24)
            new = adam_update(state_in[q % 2, 0, at, :], grad[b, at, :], state_in[q % 2, 1, at, :], state_in[q % 2, 2, at, :])
            for i in range(3):
                state_out[q % 2, i, at, :] = new[i]
            return carry

        lax.fori_loop(0, sizes[b] // 24, body, 0)
        for c in state_stores(q):
            c.start()
        if q + 2 < len(todo):
            for c in state_loads(q + 2):
                c.start()

    plane_barrier(tp, dp, [(tp, twin), (tp, facing)])
    for q in range(2):
        for c in state_loads(q):
            c.start()

    def g_first(b):
        remote(g_ref.at[rows(1 - core, b), :], part(from_c, b), g_send_c.at[b], g_recv_c.at[b], tp, twin).start()
        pltpu.make_async_copy(g_ref.at[rows(core, b), :], part(s_buf, b), g_load.at[b]).start()

    def g_chip_sum(b):
        pltpu.make_async_copy(g_ref.at[rows(core, b), :], part(s_buf, b), g_load.at[b]).wait()
        remote(part(s_buf, b), part(from_c, b), g_send_c.at[b], g_recv_c.at[b], tp, twin).wait_recv()
        add_into(part(s_buf, b), part(from_c, b), 24)

    def g_copy_x(b):
        return remote(part(s_buf, b), part(from_x, b), g_send_x.at[b], g_recv_x.at[b], tp, facing)

    def g_copy_t(b):
        return remote(part(from_x, b), part(t_buf, b), g_send_t.at[b], g_recv_t.at[b], tp, twin)

    def w_first(k):
        for zz in REDUCE_ORDER[k]:
            for slot in (2 * zz + 1 - y, 2 * zz + y):
                remote(p_ref.at[slot, 1 - core], w_c.at[slot], send_c.at[slot], recv_c.at[slot], tp, twin).start()
                pltpu.make_async_copy(p_ref.at[slot, core], acc.at[slot], w_load.at[slot]).start()

    def w_chip_sum(slot):
        pltpu.make_async_copy(p_ref.at[slot, core], acc.at[slot], w_load.at[slot]).wait()
        remote(acc.at[slot], w_c.at[slot], send_c.at[slot], recv_c.at[slot], tp, twin).wait_recv()
        add_into(acc.at[slot], w_c.at[slot])

    def w_second(k):
        for zz in REDUCE_ORDER[k]:
            slot = 2 * zz + 1 - y
            w_chip_sum(slot)
            remote(acc.at[slot], w_y.at[zz], send_y.at[zz], recv_y.at[zz], partner, dp).start()
        for zz in REDUCE_ORDER[k]:
            w_chip_sum(2 * zz + y)

    def w_reduce(k, shards):
        for zz in shards:
            line = acc.at[2 * zz + y]
            remote(line, w_y.at[zz], send_y.at[zz], recv_y.at[zz], partner, dp).wait_recv()
            add_into(line, w_y.at[zz])
            if zz >= k and k > 0:
                remote(line, w_l.at[zz - 1], send_l.at[zz], recv_l.at[zz], partner, dp).wait_recv()
                add_into(line, w_l.at[zz - 1])
            if zz <= k and k < NZ - 1:
                remote(line, w_r.at[zz], send_r.at[zz], recv_r.at[zz], partner, dp).wait_recv()
                add_into(line, w_r.at[zz])
            if zz > k:
                remote(line, w_l.at[zz - 1], send_r.at[zz], recv_l.at[zz], tp + 2, dp).start()
            if zz < k:
                remote(line, w_r.at[zz], send_l.at[zz], recv_r.at[zz], tp - 2, dp).start()

    def on_position(f):
        for k in range(NZ):
            pl.when(z == k)(functools.partial(f, k))

    g_first(0)
    g_first(1)
    on_position(w_first)
    for b in range(2, N_BLOCK):
        g_first(b)
    for b in range(2):
        g_chip_sum(b)
        g_copy_x(b).start()
    on_position(w_second)
    for b in range(2, EARLY):
        g_chip_sum(b)
        g_copy_x(b).start()

    total = acc.at[tp]
    w_copy_x = remote(total, w_x, last_send.at[0], last_recv.at[0], tp, facing)
    w_copy_c = remote(total, w_out.at[core], last_send.at[1], last_recv.at[1], tp, twin)
    w_store = pltpu.make_async_copy(total, w_out.at[core], w_out_sem)
    n_small, n_rows = small_ref.shape[1], w_out.shape[1]
    mine = w_out.at[1, pl.ds(n_rows - 32, n_small), :]
    small_here = pltpu.make_async_copy(mine, small_ref.at[tp], w_out_sem)
    peers = [lax.rem(tp + n, 2 * NZ) for n in range(1, 2 * NZ)]
    q = 0
    for b in range(N_BLOCK):
        g_copy_x(b).wait_recv()
        add_into(part(from_x, b), part(s_buf, b), 24)
        g_copy_t(b).start()
        update(q)
        q += 1
        if b > 0:
            g_copy_t(b - 1).wait_recv()
            update(q)
            q += 1
        for k in range(NZ):
            if b in W_REDUCE[k]:
                pl.when(z == k)(functools.partial(w_reduce, k, W_REDUCE[k][b]))
        if b == 6:
            w_copy_x.start()
            for late in range(EARLY, N_BLOCK):
                g_chip_sum(late)
                g_copy_x(late).start()
        if b == 8:
            w_copy_x.wait()
            add_into(total, w_x)
            w_copy_c.start()
            w_store.start()
        if b == 9:
            w_copy_c.wait_send()
            remote(total, w_out.at[1 - core], last_send.at[1], last_recv.at[1], tp, twin).wait_recv()
            w_store.wait()
            for to in peers:
                remote(mine, small_ref.at[tp], small_send.at[to], small_recv.at[tp], to, dp).start()
            small_here.start()
    g_copy_t(N_BLOCK - 1).wait_recv()
    update(q)
    for source in peers:
        remote(small_ref.at[source], small_ref.at[source], small_send.at[source], small_recv.at[source], source, dp).wait_recv()
        remote(mine, small_ref.at[tp], small_send.at[source], small_recv.at[tp], source, dp).wait_send()
    small_here.wait()
    for b in range(N_BLOCK):
        remote(g_ref.at[rows(1 - core, b), :], part(from_c, b), g_send_c.at[b], g_recv_c.at[b], tp, twin).wait_send()
        g_copy_x(b).wait_send()
        g_copy_t(b).wait_send()

    def w_done(k):
        for zz in range(NZ):
            line = acc.at[2 * zz + y]
            for slot in (2 * zz + 1 - y, 2 * zz + y):
                remote(p_ref.at[slot, 1 - core], w_c.at[slot], send_c.at[slot], recv_c.at[slot], tp, twin).wait_send()
            remote(line, w_y.at[zz], send_y.at[zz], recv_y.at[zz], partner, dp).wait_send()
            if zz > k:
                remote(line, w_l.at[zz - 1], send_r.at[zz], recv_l.at[zz], tp + 2, dp).wait_send()
            if zz < k:
                remote(line, w_r.at[zz], send_l.at[zz], recv_r.at[zz], tp - 2, dp).wait_send()

    on_position(w_done)
    for last in (len(todo) - 2, len(todo) - 1):
        for c in state_stores(last):
            c.wait()


def tail(g_table, g_rows, embed, m_embed, v_embed, collective_id):
    vocab, width = embed.shape
    rows = g_rows.shape[1]
    half = (rows // 2, width)
    size = -(-vocab // (2 * N_BLOCK * 24)) * 24
    blocks = pltpu.VMEM((N_BLOCK, size, width), F32)
    dma = lambda *n: pltpu.SemaphoreType.DMA(n)
    table = jax.ShapeDtypeStruct((vocab, width), F32)
    *new, w_sum, small = pl.pallas_call(
        tail_kernel,
        out_shape=(table, table, table, jax.ShapeDtypeStruct((2,) + half, F32), jax.ShapeDtypeStruct((2 * NZ, 24, width), F32)),
        in_specs=[ANY] * 5,
        out_specs=(ANY,) * 5,
        scratch_shapes=[blocks] * 4 + [pltpu.VMEM((2, 3, size, width), F32)] * 2
        + [pltpu.VMEM((2 * NZ,) + half, F32)] * 2 + [pltpu.VMEM((NZ,) + half, F32)] + [pltpu.VMEM((NZ - 1,) + half, F32)] * 2
        + [pltpu.VMEM(half, F32)]
        + [dma(N_BLOCK)] * 7 + [dma(2, 3)] * 2
        + [dma(2 * NZ), pltpu.SemaphoreType.DMA] + [dma(2 * NZ), dma(NZ), dma(NZ), dma(NZ)] * 2 + [dma(2)] * 2 + [dma(2 * NZ)] * 2,
        compiler_params=pltpu.CompilerParams(collective_id=collective_id, has_side_effects=True, vmem_limit_bytes=67000000),
        name="tail",
    )(g_table, g_rows.reshape((2 * NZ, 2) + half), embed, m_embed, v_embed)
    return new, w_sum.reshape(rows, width), small


def norm_fwd(x_f32, scale):
    centered = x_f32 - jnp.mean(x_f32, axis=-1, keepdims=True)
    inv_std = lax.rsqrt(jnp.mean(centered * centered, axis=-1, keepdims=True) + LN_EPS)
    x_hat = centered * inv_std
    return (x_hat * scale).astype(BF16), x_hat, inv_std


def norm_bwd(d_out, x_hat, inv_std, scale):
    d_scale = jnp.sum(d_out * x_hat, axis=0)
    d_hat = d_out * scale
    d_in = inv_std * (d_hat - jnp.mean(d_hat, axis=-1, keepdims=True) - x_hat * jnp.mean(d_hat * x_hat, axis=-1, keepdims=True))
    return d_in, d_scale


def adam_update(param_in, grad_in, mom_in, vel_in):
    mom_new = BETA_ONE * mom_in + (1.0 - BETA_ONE) * grad_in
    vel_new = BETA_TWO * vel_in + (1.0 - BETA_TWO) * grad_in * grad_in
    return param_in - LEARN_RATE * mom_new / (jnp.sqrt(vel_new) + ADAM_EPS), mom_new, vel_new


def dot(spec, a, b):
    return jnp.einsum(spec, a, b, preferred_element_type=F32)


def solution(mesh):
    param_specs = (P('tp', None), P(None, None), P(None, 'tp'), P(None, None, None), P('tp', None), P(None, None, 'tp'), P('tp', None))
    n_tp = mesh.shape['tp']
    n_dp = mesh.shape['dp']

    def local_step(tokens, labels, *state_arrays):
        embed, ln_scales, w_q, w_kv, w_o, w_gu, w_down = state_arrays[0:7]
        batch_loc, seq_len = tokens.shape
        vocab_loc, d_model = embed.shape
        head_dim = w_kv.shape[2]
        q_loc = w_q.shape[1]
        f_loc = w_down.shape[0]
        tok_loc = batch_loc * seq_len
        tok_total = tok_loc * n_dp
        own = tok_loc // n_tp
        tp_rank = lax.axis_index('tp')
        half = tp_rank % 2

        strict = (jnp.arange(own)[:, None] > jnp.arange(own)[None, :]).astype(BF16)

        def routing(chunks):
            shard = chunks // vocab_loc
            row = chunks - shard * vocab_loc
            hot = (shard[:, :, None] == jnp.arange(n_tp)[None, None, :])
            before = dot('rs,nsj->nrj', strict, hot.astype(BF16))
            rank = jnp.sum(jnp.where(hot, before, 0.0), axis=-1).astype(jnp.int32)
            most = jnp.max(jnp.sum(hot.astype(jnp.int32), axis=1))
            return shard, row, rank, (most + CAP - 1) // CAP

        chunks = tokens.reshape(n_tp, own)
        shard, row, rank, rounds = routing(chunks)
        slots = jnp.arange(CAP)
        my_shard = lax.dynamic_index_in_dim(shard, tp_rank, 0, keepdims=False)
        my_rank = lax.dynamic_index_in_dim(rank, tp_rank, 0, keepdims=False)

        def fetch(step):
            here = (shard[:, None, :] == tp_rank) & (rank[:, None, :] == slots[None, :, None] + step * CAP)
            ids = jnp.sum(jnp.where(here, row[:, None, :], 0), axis=-1).reshape(-1)
            pick = (my_shard[:, None, None] == jnp.arange(n_tp)[None, :, None]) & (my_rank[:, None, None] == slots[None, None, :] + step * CAP)
            return jnp.take(embed, ids, axis=0).reshape(n_tp, CAP, d_model), pick.reshape(own, n_tp * CAP).astype(BF16)

        def fetch_more(state):
            rows_out, pick = fetch(state[0])
            rows_in = plane_swap(rows_out, 1).reshape(n_tp * CAP, d_model).astype(BF16)
            return state[0] + 1, state[1] + dot('rc,cd->rd', pick, rows_in)

        more_rows = lax.while_loop(lambda state: state[0] < rounds, fetch_more, (jnp.int32(1), jnp.zeros((own, d_model), F32)))[1]
        rows_first, pick_first = fetch(0)

        w_rows = jnp.concatenate([w_q.T, w_o, w_gu.transpose(0, 2, 1).reshape(2 * f_loc, d_model), w_down], axis=0)
        cuts = (q_loc, 2 * q_loc, 2 * q_loc + f_loc, 2 * q_loc + 2 * f_loc)
        wkv_t = w_kv.transpose(0, 2, 1).reshape(2 * head_dim, d_model).astype(BF16)
        inv_freq = ROPE_BASE ** (-jnp.arange(0, head_dim, 2).astype(F32) / head_dim)
        angles = inv_freq[:, None] * (half * own + jnp.arange(own)).astype(F32)[None, :]
        cos_t, sin_t = jnp.cos(angles), jnp.sin(angles)
        f_own, x_one, x_zero, *saved = front(rows_first, pick_first, more_rows, w_rows, wkv_t, ln_scales, cos_t, sin_t, n_tp * q_loc, 0)
        saved, (wq_t, wo_b, wg_t, wu_t, wd_b) = saved[:5], saved[5:]
        weights = (wq_t, wkv_t, wo_b, wg_t, wu_t, wd_b)

        logit_scale = d_model ** -0.5
        lab_loc = labels.reshape(n_tp, own) - tp_rank * vocab_loc
        d_fin, g_head_part, log_norm, lab_sum = head(f_own, lab_loc, embed, logit_scale, logit_scale / tok_total, 4)
        log_norm = lax.dynamic_index_in_dim(log_norm, tp_rank, 0, keepdims=False)
        loss_row = (log_norm + LOGIT_ZLOSS * log_norm * log_norm - jnp.sum(lab_sum, axis=0) * logit_scale) / tok_total
        g_rows, d_zero = layer_bwd(d_fin, x_zero, x_one, loss_row[None, :], ln_scales, cos_t, sin_t, weights, saved, 7)

        def give_back(step, g_sum, collective_id):
            mine = (my_shard[None, None, :] == jnp.arange(n_tp)[:, None, None]) & (my_rank[None, None, :] == slots[None, :, None] + step * CAP)
            ids = jnp.sum(jnp.where(mine, jnp.arange(own)[None, None, :], 0), axis=-1).reshape(-1)
            rows_out = jnp.take(d_zero, ids, axis=0).reshape(n_tp, CAP, d_model)
            rows_in = plane_swap(rows_out, collective_id).reshape(-1, d_model)
            here = (shard[:, None, :] == tp_rank) & (rank[:, None, :] == slots[None, :, None] + step * CAP)
            row_id = jnp.where(jnp.any(here, axis=-1), jnp.sum(jnp.where(here, row[:, None, :], 0), axis=-1), vocab_loc).reshape(-1)
            return g_sum.at[row_id].add(rows_in, mode='drop')

        g_table = give_back(0, g_head_part, 8)
        g_table = lax.while_loop(lambda s: s[0] < rounds, lambda s: (s[0] + 1, give_back(s[0], s[1], 9)), (jnp.int32(1), g_table))[1]

        new_table, g_shard, g_small = tail(g_table, g_rows, embed, state_arrays[7], state_arrays[14], 10)
        n_kv = 2 * head_dim // n_tp
        g_kv = g_small[:, :n_kv].reshape(2, head_dim, d_model).transpose(0, 2, 1)
        loss = jnp.sum(g_small[0, n_kv + 2])
        gradients = (None, g_small[0, n_kv:n_kv + 2], g_shard[:cuts[0]].T, g_kv, g_shard[cuts[0]:cuts[1]],
                     g_shard[cuts[1]:cuts[3]].reshape(2, f_loc, d_model).transpose(0, 2, 1), g_shard[cuts[3]:cuts[3] + f_loc])

        outs_p, outs_m, outs_v = ([array] for array in new_table)
        for index in range(1, 7):
            new_p, new_m, new_v = adam_update(state_arrays[index], gradients[index], state_arrays[7 + index], state_arrays[14 + index])
            outs_p.append(new_p)
            outs_m.append(new_m)
            outs_v.append(new_v)
        return tuple(outs_p) + tuple(outs_m) + tuple(outs_v) + (loss,)

    return jax.shard_map(local_step, mesh=mesh, in_specs=(P('dp', None), P('dp', None)) + param_specs * 3,
                         out_specs=param_specs * 3 + (P(),), check_vma=False)
```

```python
import functools

import jax
import jax.numpy as jnp
from jax import lax
from jax.experimental import pallas as pl
from jax.experimental.pallas import tpu as pltpu
from jax.sharding import PartitionSpec as P

LN_EPS = 1e-5
LOGIT_ZLOSS = 1e-4
LEARN_RATE = 1e-2
BETA_ONE = 0.9
BETA_TWO = 0.95
ADAM_EPS = 1e-8
ROPE_BASE = 10000.0
NZ = 4
CAP = 96
F32 = jnp.float32
BF16 = jnp.bfloat16
ANY = pl.BlockSpec(memory_space=pl.ANY)
VMEM = pl.BlockSpec(memory_space=pltpu.VMEM)

ARRIVALS = {
    0: (("R", 1), ("R", 2), ("R", 3)),
    1: (("L", 0), ("R", 2), ("R", 3)),
    2: (("R", 3), ("L", 1), ("L", 0)),
    3: (("L", 2), ("L", 1), ("L", 0)),
}
REDUCE_ORDER = {0: (3, 2, 1, 0), 1: (3, 0, 2, 1), 2: (0, 3, 1, 2), 3: (0, 1, 2, 3)}


def remote(src, dst, send_sem, recv_sem, tp, dp):
    return pltpu.make_async_remote_copy(src_ref=src, dst_ref=dst, send_sem=send_sem, recv_sem=recv_sem,
                                        device_id=(tp, dp), device_id_type=pl.DeviceIdType.MESH)


def place():
    tp = lax.axis_index("tp")
    dp = lax.axis_index("dp")
    return tp, dp, tp // 2, tp % 2


def signal(tp, dp):
    pl.semaphore_signal(pltpu.get_barrier_semaphore(), inc=1, device_id=(tp, dp), device_id_type=pl.DeviceIdType.MESH)


def add_into(acc, other, step=None):
    rows = acc.shape[0]
    step = step or (64 if rows % 64 == 0 else 8)

    def body(n, carry):
        at = pl.ds(pl.multiple_of(n * step, step), step)
        acc[at, :] = acc[at, :] + other[at, :]
        return carry

    lax.fori_loop(0, rows // step, body, 0)


def plane_barrier(tp, dp, others):
    peers = [(lax.rem(tp + n, 2 * NZ), dp) for n in range(1, 2 * NZ)] + others
    for peer in peers:
        signal(*peer)
    pl.semaphore_wait(pltpu.get_barrier_semaphore(), len(peers))


def swap_kernel(x_ref, out_ref, own_sem, send, recv):
    tp, dp, _, _ = place()
    plane_barrier(tp, dp, [])
    copies = []
    for n in range(1, 2 * NZ):
        to = lax.rem(tp + n, 2 * NZ)
        copy = remote(x_ref.at[to], out_ref.at[tp], send.at[to], recv.at[tp], to, dp)
        copy.start()
        copies.append(copy)
    own = pltpu.make_async_copy(x_ref.at[tp], out_ref.at[tp], own_sem)
    own.start()
    for n in range(1, 2 * NZ):
        source = lax.rem(tp + n, 2 * NZ)
        remote(out_ref.at[source], out_ref.at[source], send.at[source], recv.at[source], source, dp).wait_recv()
    own.wait()
    for copy in copies:
        copy.wait_send()


def plane_swap(x, collective_id):
    return pl.pallas_call(
        swap_kernel,
        out_shape=jax.ShapeDtypeStruct(x.shape, x.dtype),
        in_specs=[ANY],
        out_specs=ANY,
        scratch_shapes=[pltpu.SemaphoreType.DMA] + [pltpu.SemaphoreType.DMA((2 * NZ,))] * 2,
        compiler_params=pltpu.CompilerParams(collective_id=collective_id, has_side_effects=True),
        name="plane_swap",
    )(x)


FORWARD = {
    0: {1: (("R", 1),), 3: (("R", 2),), 5: (("R", 3),)},
    1: {1: (("L", 0), ("R", 2)), 3: (("R", 3),)},
    2: {1: (("R", 3), ("L", 1)), 3: (("L", 0),)},
    3: {1: (("L", 2),), 3: (("L", 1),), 5: (("L", 0),)},
}
REDUCE = {
    0: {2: (3,), 4: (2,), 6: (1,), 7: (0,)},
    1: {4: (3,), 6: (2, 0), 7: (1,)},
    2: {4: (0,), 6: (1, 3), 7: (2,)},
    3: {2: (0,), 4: (1,), 6: (2,), 7: (3,)},
}
SUB = 256
GROUP = 6


def lookup(table, z, step):
    value = jnp.int32(0)
    for k in range(NZ):
        for s in range(2 * NZ):
            value = value + jnp.where((z == k) & (step == s), table[k][s], 0)
    return value


def head_kernel(scale, token_scale, f_ref, lab_ref, e_ref, dfin_ref, ghead_ref, norm_ref, labsum_ref,
                e_b, e_t, fbuf, f_b, g_acc, from_y, from_l, from_r, dl, lse_all, load_sem, ag_y, ag_l, ag_r, ag_recv,
                rs_y, rs_l, rs_r, recv_y, recv_l, recv_r, st_send, st_recv):
    tp, dp, z, y = place()
    partner = tp + 1 - 2 * y
    vocab, width = e_ref.shape
    own = f_ref.shape[0]
    whole = vocab // (SUB * GROUP)
    rest = vocab - whole * SUB * GROUP
    log2e = 1.4426950408889634
    slope = scale * log2e
    blocks = [(j * SUB, SUB) for j in range(GROUP)]
    tail = [(n, min(SUB, rest - n)) for n in range(0, rest, SUB)]

    plane_barrier(tp, dp, [])

    def send(src, slot, sems, to):
        remote(src, fbuf.at[slot], sems.at[slot], ag_recv.at[slot], to, dp).start()

    def arrived(slot):
        remote(f_ref, fbuf.at[slot], ag_y.at[slot], ag_recv.at[slot], partner, dp).wait_recv()

    def first_sends(k):
        if k > 0:
            send(f_ref, tp, ag_l, tp - 2)
        if k < NZ - 1:
            send(f_ref, tp, ag_r, tp + 2)
        send(f_ref, tp, ag_y, partner)

    for k in range(NZ):
        pl.when(z == k)(functools.partial(first_sends, k))
    load = pltpu.make_async_copy(e_ref, g_acc, load_sem.at[0])
    load.start()
    own_copy = pltpu.make_async_copy(f_ref, fbuf.at[tp], load_sem.at[1])
    own_copy.start()
    load.wait()

    def prepare(at, size):
        part = g_acc[at, :]
        e_b[at, :] = part.astype(BF16)
        e_t[:, at] = part.T.astype(BF16)

    def prepare_body(n, carry):
        prepare(pl.ds(pl.multiple_of(n * SUB, SUB), SUB), SUB)
        return carry

    lax.fori_loop(0, vocab // SUB, prepare_body, 0)
    if vocab % SUB:
        prepare(pl.ds(vocab // SUB * SUB, vocab % SUB), vocab % SUB)
    own_copy.wait()

    def over_blocks(group, carry):
        def body(n, c):
            return group(pl.multiple_of(n * SUB * GROUP, SUB * GROUP), blocks, c)
        carry = lax.fori_loop(0, whole, body, carry)
        return group(whole * SUB * GROUP, tail, carry) if tail else carry

    order1 = {k: (k,) + tuple(v for pair in zip([a[1] for a in ARRIVALS[k]], [k] + [a[1] for a in ARRIVALS[k]]) for v in pair) + (ARRIVALS[k][-1][1],) for k in range(NZ)}
    order1 = {k: [2 * zz + (s % 2 == 0 and s > 0 or s == 7) for s, zz in enumerate(order1[k])] for k in range(NZ)}

    def chunk_of(table, step):
        code = lookup(table, z, step)
        other = code % 2
        return code // 2 * 2 + y + other - 2 * y * other

    def gather_step(step, carry):
        slot = chunk_of(order1, step)
        for k in range(NZ):
            for s, shards in FORWARD[k].items():
                def pass_on(k=k, shards=shards):
                    for side, zz in shards:
                        at = 2 * zz + y
                        arrived(at)
                        if side == "L" and k < NZ - 1:
                            send(fbuf.at[at], at, ag_r, tp + 2)
                        if side == "R" and k > 0:
                            send(fbuf.at[at], at, ag_l, tp - 2)
                        send(fbuf.at[at], at, ag_y, partner)
                pl.when((z == k) & (step == s))(pass_on)
        pl.when(slot % 2 != y)(lambda: arrived(slot))
        f_b[slot] = fbuf[slot].astype(BF16)
        f_now = f_b[slot]

        def group(base, parts, c):
            top, total = c
            for first, size in parts:
                logit = lax.dot_general(e_b[pl.ds(base + first, size), :], f_now, (((1,), (1,)), ((), ())), preferred_element_type=F32)
                logit = logit.reshape(size // 8, 8, own)
                new = jnp.maximum(top, jnp.max(logit, axis=0))
                total = total * jnp.exp2((top - new) * slope) + jnp.sum(jnp.exp2((logit - new[None]) * slope), axis=0)
                top = new
            return top, total

        top, total = over_blocks(group, (jnp.full((8, own), -3e38, F32), jnp.zeros((8, own), F32)))
        most = jnp.max(top, axis=0, keepdims=True)
        total = jnp.sum(total * jnp.exp2((top - most) * slope), axis=0, keepdims=True)
        lse_all[tp, pl.ds(slot, 1), :] = most * scale + jnp.log(total)
        return carry

    lax.fori_loop(0, 2 * NZ, gather_step, 0)

    for n in range(1, 2 * NZ):
        to = lax.rem(tp + n, 2 * NZ)
        remote(lse_all.at[tp], lse_all.at[tp], st_send.at[to], st_recv.at[tp], to, dp).start()

    def gathers_done(k):
        def done(sems, slot):
            remote(f_ref, fbuf.at[slot], sems.at[slot], ag_recv.at[slot], partner, dp).wait_send()
        if k > 0:
            done(ag_l, tp)
        if k < NZ - 1:
            done(ag_r, tp)
        done(ag_y, tp)
        for side, zz in ARRIVALS[k]:
            at = 2 * zz + y
            if side == "L" and k < NZ - 1:
                done(ag_r, at)
            if side == "R" and k > 0:
                done(ag_l, at)
            done(ag_y, at)

    for k in range(NZ):
        pl.when(z == k)(functools.partial(gathers_done, k))

    def clear(n, carry):
        g_acc[pl.ds(pl.multiple_of(n * 16, 16), 16), :] = jnp.zeros((16, width), F32)
        return carry

    lax.fori_loop(0, vocab // 16, clear, 0)
    for n in range(1, 2 * NZ):
        source = lax.rem(tp + n, 2 * NZ)
        remote(lse_all.at[source], lse_all.at[source], st_send.at[source], st_recv.at[source], source, dp).wait_recv()
    peak = jnp.max(lse_all[...], axis=0)
    log_norm = peak + jnp.log(jnp.sum(jnp.exp(lse_all[...] - peak[None]), axis=0))
    norm_ref[...] = log_norm

    order2 = {k: [2 * zz + 1 - s for zz in REDUCE_ORDER[k] for s in range(2)] for k in range(NZ)}

    def scatter_step(step, lab_sum):
        slot = chunk_of(order2, step)
        f_now = f_b[slot]
        acc = fbuf.at[slot]
        norm = norm_ref[pl.ds(slot, 1), :]
        shift = norm * log2e
        coef = (1.0 + 2.0 * LOGIT_ZLOSS * norm) * token_scale
        lab = lab_ref[pl.ds(slot, 1), :]
        acc[...] = jnp.zeros((width, own), F32)

        def group(base, parts, hits):
            for first, size in parts:
                at = pl.ds(base + first, size)
                logit = lax.dot_general(e_b[at, :], f_now, (((1,), (1,)), ((), ())), preferred_element_type=F32)
                hit = lax.broadcasted_iota(jnp.int32, (size, own), 0) == lab - (base + first)
                prob = jnp.exp2(logit * slope - shift) * coef
                grad = jnp.where(hit, prob - token_scale, prob).astype(BF16)
                hits = hits + jnp.sum(jnp.where(hit, logit, 0.0).reshape(size // 8, 8, own), axis=0)
                dl[pl.ds(first, size), :] = grad
                g_acc[at, :] += jnp.dot(grad, f_now, preferred_element_type=F32)
            size = parts[-1][0] + parts[-1][1]
            acc[...] += jnp.dot(e_t[:, pl.ds(base, size)], dl[pl.ds(0, size), :], preferred_element_type=F32)
            return hits

        lab_sum = over_blocks(group, lab_sum)

        def hand_over():
            remote(acc, from_y.at[slot // 2], rs_y.at[slot // 2], recv_y.at[slot // 2], partner, dp).start()
        pl.when(slot % 2 != y)(hand_over)

        for k in range(NZ):
            for s, shards in REDUCE[k].items():
                def reduce(k=k, shards=shards):
                    for zz in shards:
                        line = fbuf.at[2 * zz + y]
                        remote(line, from_y.at[zz], rs_y.at[zz], recv_y.at[zz], partner, dp).wait_recv()
                        add_into(line, from_y.at[zz])
                        if zz >= k and k > 0:
                            remote(line, from_l.at[zz - 1], rs_l.at[zz], recv_l.at[zz], partner, dp).wait_recv()
                            add_into(line, from_l.at[zz - 1])
                        if zz <= k and k < NZ - 1:
                            remote(line, from_r.at[zz], rs_r.at[zz], recv_r.at[zz], partner, dp).wait_recv()
                            add_into(line, from_r.at[zz])
                        if zz > k:
                            remote(line, from_l.at[zz - 1], rs_r.at[zz], recv_l.at[zz], tp + 2, dp).start()
                        if zz < k:
                            remote(line, from_r.at[zz], rs_l.at[zz], recv_r.at[zz], tp - 2, dp).start()
                pl.when((z == k) & (step == s))(reduce)
        return lab_sum

    lab_sum = lax.fori_loop(0, 2 * NZ, scatter_step, jnp.zeros((8, own), F32))
    labsum_ref[...] = lab_sum
    store = pltpu.make_async_copy(g_acc, ghead_ref, load_sem.at[0])
    store.start()
    dfin_ref[...] = fbuf[tp].T

    def scatters_done(k):
        for zz in range(NZ):
            line = fbuf.at[2 * zz + y]
            remote(line, from_y.at[zz], rs_y.at[zz], recv_y.at[zz], partner, dp).wait_send()
            if zz > k:
                remote(line, from_l.at[zz - 1], rs_r.at[zz], recv_l.at[zz], partner, dp).wait_send()
            if zz < k:
                remote(line, from_r.at[zz], rs_l.at[zz], recv_r.at[zz], partner, dp).wait_send()

    for k in range(NZ):
        pl.when(z == k)(functools.partial(scatters_done, k))
    for n in range(1, 2 * NZ):
        to = lax.rem(tp + n, 2 * NZ)
        remote(lse_all.at[tp], lse_all.at[tp], st_send.at[to], st_recv.at[tp], to, dp).wait_send()
    store.wait()


def head(f_own, labels, embed, scale, token_scale, collective_id):
    own, width = f_own.shape
    vocab = embed.shape[0]
    chunk = (own, width)
    dma8 = pltpu.SemaphoreType.DMA((2 * NZ,))
    dma4 = pltpu.SemaphoreType.DMA((NZ,))
    return pl.pallas_call(
        functools.partial(head_kernel, scale, token_scale),
        out_shape=(jax.ShapeDtypeStruct((own, width), F32), jax.ShapeDtypeStruct((vocab, width), F32),
                   jax.ShapeDtypeStruct((2 * NZ, own), F32), jax.ShapeDtypeStruct((8, own), F32)),
        in_specs=[VMEM, VMEM, ANY],
        out_specs=(VMEM, ANY, VMEM, VMEM),
        scratch_shapes=[pltpu.VMEM((vocab, width), BF16), pltpu.VMEM((width, vocab), BF16),
                        pltpu.VMEM((2 * NZ,) + chunk, F32), pltpu.VMEM((2 * NZ,) + chunk, BF16), pltpu.VMEM((vocab, width), F32),
                        pltpu.VMEM((NZ,) + chunk, F32), pltpu.VMEM((NZ - 1,) + chunk, F32), pltpu.VMEM((NZ - 1,) + chunk, F32),
                        pltpu.VMEM((SUB * GROUP, own), BF16), pltpu.VMEM((2 * NZ, 2 * NZ, own), F32),
                        pltpu.SemaphoreType.DMA((2,)), dma8, dma8, dma8, dma8, dma4, dma4, dma4, dma4, dma4, dma4, dma8, dma8],
        compiler_params=pltpu.CompilerParams(collective_id=collective_id, has_side_effects=True, vmem_limit_bytes=67000000),
        cost_estimate=pl.CostEstimate(flops=8 * vocab * width * own * 8, bytes_accessed=3 * 4 * vocab * width, transcendentals=2 * vocab * own * 8),
        name="head",
    )(f_own, labels, embed)


TB = (((1,), (1,)), ((), ()))
TA = (((0,), (0,)), ((), ()))
LOG2E = 1.4426950408889634


def mm(a, b, dims=(((1,), (0,)), ((), ()))):
    return lax.dot_general(a, b, dims, preferred_element_type=F32)


def turn(lo, hi, cos_t, sin_t):
    return lo * cos_t - hi * sin_t, hi * cos_t + lo * sin_t


EVENTS = {
    0: (((("R", 1),), (0,)), ((("R", 2),), (1,)), ((("R", 3),), (2,)), ((), (3,))),
    1: (((("L", 0), ("R", 2)), (1,)), ((("R", 3),), (0,)), ((), (2,)), ((), (3,))),
    2: (((("R", 3), ("L", 1)), (2,)), ((("L", 0),), (3,)), ((), (1,)), ((), (0,))),
    3: (((("L", 2),), (3,)), ((("L", 1),), (2,)), ((("L", 0),), (1,)), ((), (0,))),
}
MLP_ORDER = {k: [2 * k] + [code for line, other in EVENTS[k] for code in [2 * zz for _, zz in line] + [2 * zz + 1 for zz in other]] for k in range(NZ)}


def front_kernel(rows_ref, pick_ref, extra_ref, w_ref, wkv_ref, ln_ref, cos_ref, sin_ref,
                 f_ref, x1_ref, x0_ref, q_ref, kv_ref, kvt_ref, lse_ref, ctx_ref, wq_ref, wo_ref, wg_ref, wu_ref, wd_ref,
                 wl, rows_in, u_b, kv_out, kv_in, own_sem, r_send, r_recv, a_y, a_l, a_r, a_c, a_recv,
                 b_y, b_l, b_r, b_x, b_c, b_recv, kv_send, kv_recv):
    tp, dp, z, y = place()
    partner = tp + 1 - 2 * y
    core = dp % 2
    twin = dp + 1 - 2 * core
    facing = lax.rem(dp + 2, 4)
    own, width = x0_ref.shape
    shards, w_rows = wl.shape[0], wl.shape[1]
    nq = q_ref.shape[0]
    ff = wg_ref.shape[0]
    n_a = nq // shards
    n_f = ff // shards
    n_b = 3 * n_f // 4
    hd = kv_out.shape[0] // 2
    quarter = hd // 2
    heads = nq // hd

    def a_rows(c):
        return pl.ds(pl.multiple_of(c * n_a, 8), n_a)

    def b_rows(d):
        return pl.ds(pl.multiple_of(2 * n_a + d * n_b, 8), n_b)

    def a_copy(slot, sems, to, to_dp, first=False):
        src = w_ref.at[a_rows(core), :] if first else wl.at[slot, a_rows(core), :]
        return remote(src, wl.at[slot, a_rows(core), :], sems.at[slot], a_recv.at[slot, core], to, to_dp)

    def b_copy(slot, piece, sems, to, to_dp, first=False):
        src = w_ref.at[b_rows(piece), :] if first else wl.at[slot, b_rows(piece), :]
        return remote(src, wl.at[slot, b_rows(piece), :], sems.at[slot], b_recv.at[slot, piece], to, to_dp)

    def a_wait(slot, c):
        remote(w_ref.at[a_rows(c), :], wl.at[slot, a_rows(c), :], a_y.at[slot], a_recv.at[slot, c], partner, dp).wait_recv()

    def b_wait(slot, piece):
        remote(w_ref.at[b_rows(piece), :], wl.at[slot, b_rows(piece), :], b_y.at[slot], b_recv.at[slot, piece], partner, dp).wait_recv()

    def on_position(f):
        for k in range(NZ):
            pl.when(z == k)(functools.partial(f, k))

    def line_sends(k, make, y_sems, l_sems, r_sems, slot, side, first=False):
        sends = [make(slot, y_sems, partner, dp, first)]
        if k > 0 and side != "L":
            sends.append(make(slot, l_sems, tp - 2, dp, first))
        if k < NZ - 1 and side != "R":
            sends.append(make(slot, r_sems, tp + 2, dp, first))
        return sends

    def b_own(slot, sems, to, to_dp, first=False):
        return b_copy(slot, dp, sems, to, to_dp, first)

    def a_sends(k, slot, side, first=False):
        return line_sends(k, a_copy, a_y, a_l, a_r, slot, side, first)

    def b_sends(k, slot, side, first=False):
        return line_sends(k, b_own, b_y, b_l, b_r, slot, side, first)

    def start(copies):
        for c in copies:
            c.start()

    plane_barrier(tp, dp, [(tp, twin), (tp, facing)])
    peers = [lax.rem(tp + n, shards) for n in range(1, shards)]

    def row_copy(to):
        return remote(rows_ref.at[to], rows_in.at[tp], r_send.at[to], r_recv.at[tp], to, dp)

    on_position(lambda k: start(b_sends(k, tp, "", True)))
    start([row_copy(to) for to in peers])
    on_position(lambda k: start(a_sends(k, tp, "", True)))
    own_rows = pltpu.make_async_copy(rows_ref.at[tp], rows_in.at[tp], own_sem.at[0])
    own_rows.start()
    own_w = pltpu.make_async_copy(w_ref, wl.at[tp], own_sem.at[1])
    own_w.start()

    def a_event(t, k):
        line, other = EVENTS[k][t]
        for side, zz in line:
            slot = 2 * zz + y
            a_wait(slot, core)
            start(a_sends(k, slot, side))
            a_copy(slot, a_c, tp, twin).start()
        for zz in other:
            slot = 2 * zz + 1 - y
            a_wait(slot, core)
            a_copy(slot, a_c, tp, twin).start()

    def b_event(t, k):
        line, other = EVENTS[k][t]
        for side, zz in line:
            slot = 2 * zz + y
            b_wait(slot, dp)
            start(b_sends(k, slot, side))
            b_copy(slot, dp, b_x, tp, facing).start()
            b_copy(slot, dp, b_c.at[0], tp, twin).start()
        for zz in other:
            slot = 2 * zz + 1 - y
            b_wait(slot, dp)
            b_copy(slot, dp, b_x, tp, facing).start()
            b_copy(slot, dp, b_c.at[0], tp, twin).start()

    on_position(functools.partial(b_event, 0))

    own_rows.wait()
    for source in peers:
        remote(rows_ref.at[source], rows_in.at[source], r_send.at[source], r_recv.at[source], source, dp).wait_recv()
    x0_ref[...] = extra_ref[...] + mm(pick_ref[...], rows_in[...].reshape(pick_ref.shape[1], width).astype(BF16))
    u_b[...] = norm_fwd(x0_ref[...], ln_ref[0:1, :])[0]
    x1_ref[...] = x0_ref[...]
    cos_t = cos_ref[...]
    sin_t = sin_ref[...]
    kv = mm(wkv_ref[...], u_b[...], TB)
    lo, hi = turn(kv[:quarter], kv[quarter:hd], cos_t, sin_t)
    kv_out[0:quarter, :] = lo
    kv_out[quarter:hd, :] = hi
    kv_out[hd:, :] = kv[hd:]
    kv_copy = remote(kv_out, kv_in, kv_send, kv_recv, partner, dp)
    kv_copy.start()

    on_position(functools.partial(a_event, 0))
    on_position(functools.partial(b_event, 1))
    on_position(functools.partial(a_event, 1))
    on_position(functools.partial(b_event, 2))
    on_position(functools.partial(a_event, 2))
    on_position(functools.partial(a_event, 3))
    on_position(functools.partial(b_event, 3))
    own_w.wait()
    for source in peers:
        a_wait(source, 1 - core)
    for s in range(shards):
        wq_ref[s * n_a:(s + 1) * n_a, :] = wl[s, 0:n_a, :].astype(BF16)
        wo_ref[s * n_a:(s + 1) * n_a, :] = wl[s, n_a:2 * n_a, :].astype(BF16)

    q_all = mm(wq_ref[...], u_b[...], TB)
    for h in range(heads):
        lo, hi = turn(q_all[h * hd:h * hd + quarter], q_all[h * hd + quarter:(h + 1) * hd], cos_t, sin_t)
        q_ref[h * hd:h * hd + quarter, :] = lo.astype(BF16)
        q_ref[h * hd + quarter:(h + 1) * hd, :] = hi.astype(BF16)
    kv_copy.wait()

    def fill(mine, other):
        kv_ref[mine * own:(mine + 1) * own, :] = kv_out[...].T.astype(BF16)
        kv_ref[other * own:(other + 1) * own, :] = kv_in[...].T.astype(BF16)
        kvt_ref[:, mine * own:(mine + 1) * own] = kv_out[...].astype(BF16)
        kvt_ref[:, other * own:(other + 1) * own] = kv_in[...].astype(BF16)

    pl.when(y == 0)(lambda: fill(0, 1))
    pl.when(y == 1)(lambda: fill(1, 0))
    blank = jnp.zeros((hd, own), BF16)
    slope = hd ** -0.5 * LOG2E

    def attend(h, carry):
        at = pl.ds(pl.multiple_of(h * hd, hd), hd)
        scores = mm(kv_ref[...], jnp.concatenate([q_ref[at, :], blank], axis=0))
        allowed = lax.broadcasted_iota(jnp.int32, scores.shape, 0) <= lax.broadcasted_iota(jnp.int32, scores.shape, 1) + y * own
        scores = jnp.where(allowed, scores * slope, -1e30)
        top = jnp.max(scores, axis=0, keepdims=True)
        prob = jnp.exp2(scores - top)
        total = jnp.sum(prob, axis=0, keepdims=True)
        lse_ref[pl.ds(h, 1), :] = top + jnp.log2(total)
        ctx_ref[at, :] = mm(kvt_ref[hd:, :], (prob * (1.0 / total)).astype(BF16)).astype(BF16)
        return carry

    lax.fori_loop(0, heads, attend, 0)
    x1_ref[...] += mm(ctx_ref[...], wo_ref[...], TA)

    def slot_of(step):
        code = lookup(MLP_ORDER, z, step)
        other = code % 2
        return code // 2 * 2 + y + other - 2 * y * other

    def mlp(step, carry):
        def pass_on():
            slot = slot_of(step + 1)
            b_wait(slot, facing)
            b_copy(slot, facing, b_c.at[1], tp, twin).start()
        pl.when(step < shards - 1)(pass_on)
        slot = slot_of(step)

        def rest():
            b_wait(slot, twin)
            b_wait(slot, lax.rem(twin + 2, 4))
        pl.when(step > 0)(rest)
        at = pl.ds(pl.multiple_of(slot * n_f, n_f), n_f)
        wg_ref[at, :] = wl[slot, 2 * n_a:2 * n_a + n_f, :].astype(BF16)
        wu_ref[at, :] = wl[slot, 2 * n_a + n_f:2 * n_a + 2 * n_f, :].astype(BF16)
        wd_ref[at, :] = wl[slot, 2 * n_a + 2 * n_f:2 * n_a + 3 * n_f, :].astype(BF16)
        gate = mm(u_b[...], wg_ref[at, :], TB)
        up = mm(u_b[...], wu_ref[at, :], TB)
        x1_ref[...] += mm((gate * jax.nn.sigmoid(gate) * up).astype(BF16), wd_ref[at, :])
        return carry

    lax.fori_loop(0, shards, mlp, 0)
    f_ref[...] = norm_fwd(x1_ref[...], ln_ref[1:2, :])[0].astype(F32)

    def finish(k):
        done = a_sends(k, tp, "", True) + b_sends(k, tp, "", True)
        for line, other in EVENTS[k]:
            for side, zz in line:
                done += a_sends(k, 2 * zz + y, side) + b_sends(k, 2 * zz + y, side)
        for c in done:
            c.wait_send()

    on_position(finish)
    for to in peers:
        row_copy(to).wait_send()
        a_copy(to, a_c, tp, twin).wait_send()
        b_copy(to, dp, b_x, tp, facing).wait_send()
        b_copy(to, dp, b_c.at[0], tp, twin).wait_send()
        b_copy(to, facing, b_c.at[1], tp, twin).wait_send()


def front(rows, pick, extra, w_rows, wkv_t, ln, cos_t, sin_t, n_q, collective_id):
    own, width = extra.shape
    two_hd = wkv_t.shape[0]
    shards = 2 * NZ
    ff = (w_rows.shape[0] * shards - 2 * n_q) // 3
    dma = lambda *n: pltpu.SemaphoreType.DMA(n)
    s = jax.ShapeDtypeStruct
    return pl.pallas_call(
        front_kernel,
        out_shape=(s((own, width), F32),) * 3 + (s((n_q, own), BF16), s((2 * own, two_hd), BF16), s((two_hd, 2 * own), BF16),
                   s((2 * n_q // two_hd, own), F32), s((n_q, own), BF16), s((n_q, width), BF16), s((n_q, width), BF16))
        + (s((ff, width), BF16),) * 3,
        in_specs=[VMEM] * 3 + [ANY] + [VMEM] * 4,
        out_specs=(VMEM,) * 13,
        scratch_shapes=[pltpu.VMEM((shards,) + w_rows.shape, F32), pltpu.VMEM(rows.shape, F32), pltpu.VMEM((own, width), BF16),
                        pltpu.VMEM((two_hd, own), F32), pltpu.VMEM((two_hd, own), F32),
                        dma(2), dma(shards), dma(shards)] + [dma(shards)] * 4 + [dma(shards, 2)]
        + [dma(shards)] * 4 + [dma(2, shards), dma(shards, 4), pltpu.SemaphoreType.DMA, pltpu.SemaphoreType.DMA],
        compiler_params=pltpu.CompilerParams(collective_id=collective_id, has_side_effects=True, vmem_limit_bytes=60000000),
        name="front",
    )(rows, pick, extra, w_rows, wkv_t, ln, cos_t, sin_t)


def layer_bwd_kernel(dfin_ref, x0_ref, x1_ref, loss_ref, ln_ref, cos_ref, sin_ref, wq_ref, wkv_ref, wo_ref, wg_ref, wu_ref, wd_ref,
                     q_ref, kv_ref, kvt_ref, lse_ref, ctx_ref, pick_ref, rows_ref, d0_ref, back_ref, d_one, d_b, u_b, dctx, dq, dkv, dkv_in,
                     hid, d_gate, d_up, rows_out, g_q, g_o, g_g, g_u, g_d, small, out_sem, send_sem, recv_sem, r_send, r_recv):
    tp, dp, _, y = place()
    partner = tp + 1 - 2 * y
    own, width = x0_ref.shape
    hd = kv_ref.shape[1] // 2
    quarter = hd // 2
    nq = q_ref.shape[0]
    heads = nq // hd
    ff = wg_ref.shape[0]
    shards = rows_ref.shape[0]
    plane_barrier(tp, dp, [])
    _, f_hat, f_inv = norm_fwd(x1_ref[...], ln_ref[1:2, :])
    d_in, g_fin = norm_bwd(dfin_ref[...], f_hat, f_inv, ln_ref[1:2, :])
    d_one[...] = d_in
    d_b[...] = d_in.astype(BF16)
    u_b[...] = norm_fwd(x0_ref[...], ln_ref[0:1, :])[0]
    dctx[...] = mm(wo_ref[...], d_b[...], TB).astype(BF16)
    cos_t = cos_ref[...]
    sin_t = sin_ref[...]
    blank = jnp.zeros((hd, own), BF16)
    slope = hd ** -0.5 * LOG2E
    dkv[...] = jnp.zeros_like(dkv)

    def attend(h, carry):
        at = pl.ds(pl.multiple_of(h * hd, hd), hd)
        q_pad = jnp.concatenate([q_ref[at, :], blank], axis=0)
        d_pad = jnp.concatenate([blank, dctx[at, :]], axis=0)
        scores = mm(kv_ref[...], q_pad)
        allowed = lax.broadcasted_iota(jnp.int32, scores.shape, 0) <= lax.broadcasted_iota(jnp.int32, scores.shape, 1) + y * own
        prob = jnp.where(allowed, jnp.exp2(scores * slope - lse_ref[pl.ds(h, 1), :]), 0.0)
        d_prob = mm(kv_ref[...], d_pad)
        mean = jnp.sum(d_prob * prob, axis=0, keepdims=True)
        d_score = (prob * (d_prob - mean) * hd ** -0.5).astype(BF16)
        dkv[...] += mm(d_score, q_pad, TB) + mm(prob.astype(BF16), d_pad, TB)
        d_q = mm(kvt_ref[0:hd, :], d_score)
        lo, hi = turn(d_q[:quarter], d_q[quarter:], cos_t, -sin_t)
        dq[at, :] = jnp.concatenate([lo, hi], axis=0).astype(BF16)
        return carry

    lax.fori_loop(0, heads, attend, 0)
    copy = remote(dkv.at[pl.ds(pl.multiple_of((1 - y) * own, own), own), :], dkv_in, send_sem, recv_sem, partner, dp)
    copy.start()

    d0_ref[...] = mm(dq[...], wq_ref[...], TA)
    step = min(512, ff)

    def mlp(n, carry):
        at = pl.ds(pl.multiple_of(n * step, step), step)
        gate = mm(wg_ref[at, :], u_b[...], TB)
        up = mm(wu_ref[at, :], u_b[...], TB)
        d_hidden = mm(wd_ref[at, :], d_b[...], TB)
        sig = jax.nn.sigmoid(gate)
        hid[at, :] = (gate * sig * up).astype(BF16)
        d_gate[at, :] = (d_hidden * up * sig * (1.0 + gate * (1.0 - sig))).astype(BF16)
        d_up[at, :] = (d_hidden * gate * sig).astype(BF16)
        d0_ref[...] += mm(d_gate[at, :], wg_ref[at, :], TA) + mm(d_up[at, :], wu_ref[at, :], TA)
        return carry

    lax.fori_loop(0, ff // step, mlp, 0)
    copy.wait()
    d_kv = (dkv[pl.ds(pl.multiple_of(y * own, own), own), :] + dkv_in[...]).T
    lo, hi = turn(d_kv[:quarter], d_kv[quarter:hd], cos_t, -sin_t)
    d_kv = jnp.concatenate([lo, hi, d_kv[hd:]], axis=0).astype(BF16)
    small[0:2 * hd, :] = mm(d_kv, u_b[...])
    d_u = d0_ref[...] + mm(d_kv, wkv_ref[...], TA)
    _, u_hat, u_inv = norm_fwd(x0_ref[...], ln_ref[0:1, :])
    d_in, g_in = norm_bwd(d_u, u_hat, u_inv, ln_ref[0:1, :])
    d_zero = d_one[...] + d_in
    d0_ref[...] = d_zero
    high = d_zero.astype(BF16)
    left = d_zero - high.astype(F32)
    middle = left.astype(BF16)
    low = (left - middle.astype(F32)).astype(BF16)
    rows_out[...] = (mm(pick_ref[...], high, TA) + mm(pick_ref[...], middle, TA) + mm(pick_ref[...], low, TA)).reshape(rows_out.shape)

    def row_copy(to):
        return remote(rows_out.at[to], back_ref.at[tp], r_send.at[to], r_recv.at[tp], to, dp)

    peers = [lax.rem(tp + n, shards) for n in range(1, shards)]
    for to in peers:
        row_copy(to).start()
    own_rows = pltpu.make_async_copy(rows_out.at[tp], back_ref.at[tp], out_sem.at[7 * 2 * NZ])
    own_rows.start()

    g_o[...] = mm(ctx_ref[...], d_b[...])
    g_q[...] = mm(dq[...], u_b[...])

    def weight_grads(n, carry):
        at = pl.ds(pl.multiple_of(n * step, step), step)
        g_d[at, :] = mm(hid[at, :], d_b[...])
        g_g[at, :] = mm(d_gate[at, :], u_b[...])
        g_u[at, :] = mm(d_up[at, :], u_b[...])
        return carry

    lax.fori_loop(0, ff // step, weight_grads, 0)
    small[2 * hd:, :] = jnp.zeros_like(small[2 * hd:, :])
    small[2 * hd:2 * hd + 1, :] = g_in.reshape(1, width)
    small[2 * hd + 1:2 * hd + 2, :] = g_fin.reshape(1, width)
    small[2 * hd + 2:2 * hd + 3, :] = loss_ref[...]
    copies = []

    def put(src, first, size, s):
        copies.append(pltpu.make_async_copy(src, rows_ref.at[s, pl.ds(first, size), :], out_sem.at[len(copies)]))

    n_kv = 2 * hd // shards
    for s in range(shards):
        at = 0
        for g, size in ((g_q, nq // shards), (g_o, nq // shards), (g_g, ff // shards), (g_u, ff // shards), (g_d, ff // shards)):
            put(g.at[pl.ds(s * size, size), :], at, size, s)
            at += size
        put(small.at[pl.ds(s * n_kv, n_kv), :], at, n_kv, s)
        put(small.at[pl.ds(2 * hd + (0 if s == 0 else 16), 16), :], at + n_kv, 16, s)
    for c in copies:
        c.start()
    for c in copies:
        c.wait()
    own_rows.wait()
    for source in peers:
        remote(rows_out.at[source], back_ref.at[source], r_send.at[source], r_recv.at[source], source, dp).wait_recv()
        row_copy(source).wait_send()


def layer_bwd(d_fin, x0, x1, loss_row, ln, cos_t, sin_t, weights, saved, pick, collective_id):
    own, width = x0.shape
    nq = weights[0].shape[0]
    two_hd = weights[1].shape[0]
    ff = weights[3].shape[0]
    rows = (2 * nq + 3 * ff + two_hd) // (2 * NZ) + 16
    chunk = (own, width)
    back = (2 * NZ, pick.shape[1] // (2 * NZ), width)
    return pl.pallas_call(
        layer_bwd_kernel,
        out_shape=(jax.ShapeDtypeStruct((2 * NZ, rows, width), F32), jax.ShapeDtypeStruct(chunk, F32), jax.ShapeDtypeStruct(back, F32)),
        in_specs=[VMEM] * 19,
        out_specs=(ANY, VMEM, ANY),
        scratch_shapes=[pltpu.VMEM(chunk, F32), pltpu.VMEM(chunk, BF16), pltpu.VMEM(chunk, BF16), pltpu.VMEM((nq, own), BF16),
                        pltpu.VMEM((nq, own), BF16), pltpu.VMEM((2 * own, two_hd), F32), pltpu.VMEM((own, two_hd), F32)]
        + [pltpu.VMEM((ff, own), BF16)] * 3 + [pltpu.VMEM(back, F32), pltpu.VMEM((nq, width), F32), pltpu.VMEM((nq, width), F32)] + [pltpu.VMEM((ff, width), F32)] * 3
        + [pltpu.VMEM((two_hd + 32, width), F32), pltpu.SemaphoreType.DMA((14 * NZ + 1,)), pltpu.SemaphoreType.DMA, pltpu.SemaphoreType.DMA,
           pltpu.SemaphoreType.DMA((2 * NZ,)), pltpu.SemaphoreType.DMA((2 * NZ,))],
        compiler_params=pltpu.CompilerParams(collective_id=collective_id, has_side_effects=True, vmem_limit_bytes=60000000),
        name="layer_bwd",
    )(d_fin, x0, x1, loss_row, ln, cos_t, sin_t, *weights, *saved, pick)


N_BLOCK = 12
EARLY = 9
W_REDUCE = {
    0: {1: (3,), 3: (2,), 5: (1,), 7: (0,)},
    1: {3: (3,), 5: (2, 0), 7: (1,)},
    2: {3: (0,), 5: (1, 3), 7: (2,)},
    3: {1: (0,), 3: (1,), 5: (2,), 7: (3,)},
}


def tail_kernel(g_ref, p_ref, rows_ref, ids_ref, t_ref, w_out, small_ref,
                s_buf, from_c, from_x, rows_c, ids_c, parts, acc, w_c, w_y, w_l, w_r, w_x,
                g_load, g_send_c, g_recv_c, g_send_x, g_recv_x, g_send_t, g_recv_t, g_store, l_send, l_recv,
                w_load, w_out_sem, send_c, send_y, send_l, send_r, recv_c, recv_y, recv_l, recv_r, last_send, last_recv, small_send, small_recv):
    tp, dp, z, y = place()
    partner = tp + 1 - 2 * y
    core = dp % 2
    twin = dp + 1 - 2 * core
    facing = lax.rem(dp + 2, 4)
    half = g_ref.shape[0] // 2
    size = s_buf.shape[1]
    last = half - (N_BLOCK - 1) * size
    n_look = rows_ref.shape[0]

    def rows(which, b, n):
        return pl.ds(pl.multiple_of(which * half + b * size, 8), n)

    def part(buf, b, n):
        return buf.at[b, pl.ds(0, n), :]

    plane_barrier(tp, dp, [(tp, twin), (tp, facing)])

    look_copies = [remote(rows_ref, rows_c, l_send.at[0], l_recv.at[0], tp, twin), remote(ids_ref, ids_c, l_send.at[1], l_recv.at[1], tp, twin)]
    for c in look_copies:
        c.start()

    def c_copy(b, n):
        return remote(g_ref.at[rows(1 - core, b, n), :], part(from_c, b, n), g_send_c.at[b], g_recv_c.at[b], tp, twin)

    def own_load(b, n):
        return pltpu.make_async_copy(g_ref.at[rows(core, b, n), :], part(s_buf, b, n), g_load.at[b])

    def x_copy(b, n):
        return remote(part(s_buf, b, n), part(from_x, b, n), g_send_x.at[b], g_recv_x.at[b], tp, facing)

    def t_copy(b, n):
        return remote(part(from_x, b, n), t_ref.at[rows(core, b, n), :], g_send_t.at[b], g_recv_t.at[b], tp, twin)

    def t_store(b, n):
        return pltpu.make_async_copy(part(from_x, b, n), t_ref.at[rows(core, b, n), :], g_store.at[b])

    def every(f, first, end):
        def body(b, carry):
            f(b, size)
            return carry
        lax.fori_loop(first, min(end, N_BLOCK - 1), body, 0)
        if end == N_BLOCK:
            f(N_BLOCK - 1, last)

    def chip_sum(b, n):
        own_load(b, n).wait()
        c_copy(b, n).wait_recv()
        ids = jnp.concatenate([ids_ref[...], ids_c[...]], axis=1) - (core * half + b * size)
        hit = (lax.broadcasted_iota(jnp.int32, (n, 2 * n_look), 0) == ids).astype(F32).astype(BF16)
        look = mm(hit, parts[0]) + mm(hit, parts[1]) + mm(hit, parts[2])
        s_buf[b, 0:n, :] = s_buf[b, 0:n, :] + from_c[b, 0:n, :] + look
        x_copy(b, n).start()

    def w_first(k):
        for zz in REDUCE_ORDER[k]:
            for slot in (2 * zz + 1 - y, 2 * zz + y):
                remote(p_ref.at[slot, 1 - core], w_c.at[slot], send_c.at[slot], recv_c.at[slot], tp, twin).start()
                pltpu.make_async_copy(p_ref.at[slot, core], acc.at[slot], w_load.at[slot]).start()

    def w_chip_sum(slot):
        pltpu.make_async_copy(p_ref.at[slot, core], acc.at[slot], w_load.at[slot]).wait()
        remote(acc.at[slot], w_c.at[slot], send_c.at[slot], recv_c.at[slot], tp, twin).wait_recv()
        add_into(acc.at[slot], w_c.at[slot])

    def w_second(k):
        for zz in REDUCE_ORDER[k]:
            slot = 2 * zz + 1 - y
            w_chip_sum(slot)
            remote(acc.at[slot], w_y.at[zz], send_y.at[zz], recv_y.at[zz], partner, dp).start()
        for zz in REDUCE_ORDER[k]:
            w_chip_sum(2 * zz + y)

    def w_reduce(k, shards):
        for zz in shards:
            line = acc.at[2 * zz + y]
            remote(line, w_y.at[zz], send_y.at[zz], recv_y.at[zz], partner, dp).wait_recv()
            add_into(line, w_y.at[zz])
            if zz >= k and k > 0:
                remote(line, w_l.at[zz - 1], send_l.at[zz], recv_l.at[zz], partner, dp).wait_recv()
                add_into(line, w_l.at[zz - 1])
            if zz <= k and k < NZ - 1:
                remote(line, w_r.at[zz], send_r.at[zz], recv_r.at[zz], partner, dp).wait_recv()
                add_into(line, w_r.at[zz])
            if zz > k:
                remote(line, w_l.at[zz - 1], send_r.at[zz], recv_l.at[zz], tp + 2, dp).start()
            if zz < k:
                remote(line, w_r.at[zz], send_l.at[zz], recv_r.at[zz], tp - 2, dp).start()

    def on_position(f):
        for k in range(NZ):
            pl.when(z == k)(functools.partial(f, k))

    def first(b, n):
        c_copy(b, n).start()
        own_load(b, n).start()

    every(first, 0, 4)
    on_position(w_first)
    every(first, 4, N_BLOCK)

    def split(at, value):
        high = value.astype(BF16)
        left = value - high.astype(F32)
        middle = left.astype(BF16)
        parts[0, at, :] = high
        parts[1, at, :] = middle
        parts[2, at, :] = (left - middle.astype(F32)).astype(BF16)

    split(pl.ds(0, n_look), rows_ref[...])
    for c in look_copies:
        c.wait()
    split(pl.ds(n_look, n_look), rows_c[...])
    every(chip_sum, 0, EARLY)
    on_position(w_second)

    total = acc.at[tp]
    w_copy_x = remote(total, w_x, last_send.at[0], last_recv.at[0], tp, facing)
    w_copy_c = remote(total, w_out.at[core], last_send.at[1], last_recv.at[1], tp, twin)
    w_store = pltpu.make_async_copy(total, w_out.at[core], w_out_sem)
    n_small, n_rows = small_ref.shape[1], w_out.shape[1]
    mine = w_out.at[1, pl.ds(n_rows - 32, n_small), :]
    small_here = pltpu.make_async_copy(mine, small_ref.at[tp], w_out_sem)
    peers = [lax.rem(tp + n, 2 * NZ) for n in range(1, 2 * NZ)]
    for b in range(N_BLOCK):
        n = last if b == N_BLOCK - 1 else size
        x_copy(b, n).wait_recv()
        add_into(part(from_x, b, n), part(s_buf, b, n), 24)
        t_copy(b, n).start()
        t_store(b, n).start()
        for k in range(NZ):
            if b in W_REDUCE[k]:
                pl.when(z == k)(functools.partial(w_reduce, k, W_REDUCE[k][b]))
        if b == 7:
            w_copy_x.start()
            every(chip_sum, EARLY, N_BLOCK)
        if b == 8:
            w_copy_x.wait()
            add_into(total, w_x)
            w_copy_c.start()
            w_store.start()
        if b == 9:
            w_copy_c.wait_send()
            remote(total, w_out.at[1 - core], last_send.at[1], last_recv.at[1], tp, twin).wait_recv()
            w_store.wait()
            for to in peers:
                remote(mine, small_ref.at[tp], small_send.at[to], small_recv.at[tp], to, dp).start()
            small_here.start()
    for source in peers:
        remote(small_ref.at[source], small_ref.at[source], small_send.at[source], small_recv.at[source], source, dp).wait_recv()
        remote(mine, small_ref.at[tp], small_send.at[source], small_recv.at[tp], source, dp).wait_send()
    small_here.wait()

    def w_done(k):
        for zz in range(NZ):
            line = acc.at[2 * zz + y]
            for slot in (2 * zz + 1 - y, 2 * zz + y):
                remote(p_ref.at[slot, 1 - core], w_c.at[slot], send_c.at[slot], recv_c.at[slot], tp, twin).wait_send()
            remote(line, w_y.at[zz], send_y.at[zz], recv_y.at[zz], partner, dp).wait_send()
            if zz > k:
                remote(line, w_l.at[zz - 1], send_r.at[zz], recv_l.at[zz], tp + 2, dp).wait_send()
            if zz < k:
                remote(line, w_r.at[zz], send_l.at[zz], recv_r.at[zz], tp - 2, dp).wait_send()

    on_position(w_done)

    def drain(b, n):
        c_copy(b, n).wait_send()
        x_copy(b, n).wait_send()
        t_copy(b, n).wait_send()
        t_store(b, n).wait()
        remote(part(from_x, b, n), t_ref.at[rows(1 - core, b, n), :], g_send_t.at[b], g_recv_t.at[b], tp, twin).wait_recv()

    every(drain, 0, N_BLOCK)


def tail(g_table, g_rows, look_rows, look_ids, collective_id):
    vocab, width = g_table.shape
    rows = g_rows.shape[1]
    half = (rows // 2, width)
    n_look = look_ids.shape[1]
    size = -(-vocab // (2 * N_BLOCK * 24)) * 24
    blocks = pltpu.VMEM((N_BLOCK, size, width), F32)
    dma = lambda *n: pltpu.SemaphoreType.DMA(n)
    t, w_sum, small = pl.pallas_call(
        tail_kernel,
        out_shape=(jax.ShapeDtypeStruct((vocab, width), F32), jax.ShapeDtypeStruct((2,) + half, F32), jax.ShapeDtypeStruct((2 * NZ, 24, width), F32)),
        in_specs=[ANY, ANY, VMEM, VMEM],
        out_specs=(ANY,) * 3,
        scratch_shapes=[blocks] * 3 + [pltpu.VMEM((n_look, width), F32), pltpu.VMEM((1, n_look), jnp.int32), pltpu.VMEM((3, 2 * n_look, width), BF16)]
        + [pltpu.VMEM((2 * NZ,) + half, F32)] * 2 + [pltpu.VMEM((NZ,) + half, F32)] + [pltpu.VMEM((NZ - 1,) + half, F32)] * 2
        + [pltpu.VMEM(half, F32)]
        + [dma(N_BLOCK)] * 8 + [dma(2)] * 2
        + [dma(2 * NZ), pltpu.SemaphoreType.DMA] + [dma(2 * NZ), dma(NZ), dma(NZ), dma(NZ)] * 2 + [dma(2)] * 2 + [dma(2 * NZ)] * 2,
        compiler_params=pltpu.CompilerParams(collective_id=collective_id, has_side_effects=True, vmem_limit_bytes=67000000),
        name="tail",
    )(g_table, g_rows.reshape((2 * NZ, 2) + half), look_rows.reshape(n_look, width), look_ids)
    return t, w_sum.reshape(rows, width), small


UPDATE_ROWS = 512


def update_kernel(t_ref, w_ref, small_ref, *refs):
    state = [refs[7 * i:7 * i + 7] for i in range(3)]
    new = [refs[21 + 7 * i:28 + 7 * i] for i in range(3)]
    loss_ref = refs[42]
    held, made, in_sem, out_sem = refs[43:]
    vocab = t_ref.shape[0]
    n_kv, hd = 2 * state[0][3].shape[2] // small_ref.shape[0], state[0][3].shape[2]
    blocks = [(at, min(UPDATE_ROWS, vocab - at)) for at in range(0, vocab, UPDATE_ROWS)]

    def loads(q):
        at, n = blocks[q]
        return [pltpu.make_async_copy(ref.at[pl.ds(at, n), :], held.at[q % 3, i, pl.ds(0, n), :], in_sem.at[q % 3, i])
                for i, ref in enumerate((t_ref, state[0][0], state[1][0], state[2][0]))]

    def stores(q):
        at, n = blocks[q]
        return [pltpu.make_async_copy(made.at[q % 2, i, pl.ds(0, n), :], new[i][0].at[pl.ds(at, n), :], out_sem.at[q % 2, i]) for i in range(3)]

    for q in range(3):
        for c in loads(q):
            c.start()

    def small_update(index, grad, *where):
        got = adam_update(state[0][index][where], grad, state[1][index][where], state[2][index][where])
        for i in range(3):
            new[i][index][where] = got[i]

    n_q, n_f = state[0][2].shape[1], state[0][6].shape[0]
    small_update(1, small_ref[0, n_kv:n_kv + 2, :], Ellipsis)
    small_update(2, w_ref[0:n_q, :].T, Ellipsis)
    kv = small_ref[:, 0:n_kv, :].reshape(2 * hd, small_ref.shape[2]).T
    for i in range(2):
        small_update(3, kv[:, i * hd:(i + 1) * hd], i)
    small_update(4, w_ref[n_q:2 * n_q, :], Ellipsis)
    for i in range(2):
        small_update(5, w_ref[2 * n_q + i * n_f:2 * n_q + (i + 1) * n_f, :].T, i)
    small_update(6, w_ref[2 * n_q + 2 * n_f:2 * n_q + 3 * n_f, :], Ellipsis)
    loss_ref[...] = jnp.sum(small_ref[0, n_kv + 2:n_kv + 3, :], axis=1, keepdims=True)

    for q, (at, n) in enumerate(blocks):
        for c in loads(q):
            c.wait()
        if q >= 2:
            for c in stores(q - 2):
                c.wait()
        step = 32 if n % 32 == 0 else 16

        def body(j, carry):
            rows = pl.ds(pl.multiple_of(j * step, step), step)
            got = adam_update(held[q % 3, 1, rows, :], held[q % 3, 0, rows, :], held[q % 3, 2, rows, :], held[q % 3, 3, rows, :])
            for i in range(3):
                made[q % 2, i, rows, :] = got[i]
            return carry

        lax.fori_loop(0, n // step, body, 0)
        for c in stores(q):
            c.start()
        if q + 3 < len(blocks):
            for c in loads(q + 3):
                c.start()
    for q in range(len(blocks) - 2, len(blocks)):
        for c in stores(q):
            c.wait()


def update(g_table, g_shard, g_small, state_arrays):
    specs = [ANY] + [VMEM] * 6
    width = g_table.shape[1]
    return pl.pallas_call(
        update_kernel,
        out_shape=tuple(jax.ShapeDtypeStruct(a.shape, F32) for a in state_arrays) + (jax.ShapeDtypeStruct((1, 1), F32),),
        in_specs=[ANY, VMEM, VMEM] + specs * 3,
        out_specs=tuple(specs * 3) + (VMEM,),
        scratch_shapes=[pltpu.VMEM((3, 4, UPDATE_ROWS, width), F32), pltpu.VMEM((2, 3, UPDATE_ROWS, width), F32),
                        pltpu.SemaphoreType.DMA((3, 4)), pltpu.SemaphoreType.DMA((2, 3))],
        compiler_params=pltpu.CompilerParams(vmem_limit_bytes=60000000),
        name="update",
    )(g_table, g_shard, g_small, *state_arrays)


def norm_fwd(x_f32, scale):
    centered = x_f32 - jnp.mean(x_f32, axis=-1, keepdims=True)
    inv_std = lax.rsqrt(jnp.mean(centered * centered, axis=-1, keepdims=True) + LN_EPS)
    x_hat = centered * inv_std
    return (x_hat * scale).astype(BF16), x_hat, inv_std


def norm_bwd(d_out, x_hat, inv_std, scale):
    d_scale = jnp.sum(d_out * x_hat, axis=0)
    d_hat = d_out * scale
    d_in = inv_std * (d_hat - jnp.mean(d_hat, axis=-1, keepdims=True) - x_hat * jnp.mean(d_hat * x_hat, axis=-1, keepdims=True))
    return d_in, d_scale


def adam_update(param_in, grad_in, mom_in, vel_in):
    mom_new = BETA_ONE * mom_in + (1.0 - BETA_ONE) * grad_in
    vel_new = BETA_TWO * vel_in + (1.0 - BETA_TWO) * grad_in * grad_in
    return param_in - LEARN_RATE * mom_new / (jnp.sqrt(vel_new) + ADAM_EPS), mom_new, vel_new


def dot(spec, a, b):
    return jnp.einsum(spec, a, b, preferred_element_type=F32)


def solution(mesh):
    param_specs = (P('tp', None), P(None, None), P(None, 'tp'), P(None, None, None), P('tp', None), P(None, None, 'tp'), P('tp', None))
    n_tp = mesh.shape['tp']
    n_dp = mesh.shape['dp']

    def local_step(tokens, labels, *state_arrays):
        embed, ln_scales, w_q, w_kv, w_o, w_gu, w_down = state_arrays[0:7]
        batch_loc, seq_len = tokens.shape
        vocab_loc, d_model = embed.shape
        head_dim = w_kv.shape[2]
        q_loc = w_q.shape[1]
        f_loc = w_down.shape[0]
        tok_loc = batch_loc * seq_len
        tok_total = tok_loc * n_dp
        own = tok_loc // n_tp
        tp_rank = lax.axis_index('tp')
        half = tp_rank % 2

        strict = (jnp.arange(own)[:, None] > jnp.arange(own)[None, :]).astype(BF16)

        def routing(chunks):
            shard = chunks // vocab_loc
            row = chunks - shard * vocab_loc
            hot = (shard[:, :, None] == jnp.arange(n_tp)[None, None, :])
            before = dot('rs,nsj->nrj', strict, hot.astype(BF16))
            rank = jnp.sum(jnp.where(hot, before, 0.0), axis=-1).astype(jnp.int32)
            most = jnp.max(jnp.sum(hot.astype(jnp.int32), axis=1))
            return shard, row, rank, (most + CAP - 1) // CAP

        chunks = tokens.reshape(n_tp, own)
        shard, row, rank, rounds = routing(chunks)
        slots = jnp.arange(CAP)
        my_shard = lax.dynamic_index_in_dim(shard, tp_rank, 0, keepdims=False)
        my_rank = lax.dynamic_index_in_dim(rank, tp_rank, 0, keepdims=False)

        def fetch(step):
            here = (shard[:, None, :] == tp_rank) & (rank[:, None, :] == slots[None, :, None] + step * CAP)
            ids = jnp.sum(jnp.where(here, row[:, None, :], 0), axis=-1).reshape(-1)
            pick = (my_shard[:, None, None] == jnp.arange(n_tp)[None, :, None]) & (my_rank[:, None, None] == slots[None, None, :] + step * CAP)
            return jnp.take(embed, ids, axis=0).reshape(n_tp, CAP, d_model), pick.reshape(own, n_tp * CAP).astype(BF16)

        def fetch_more(state):
            rows_out, pick = fetch(state[0])
            rows_in = plane_swap(rows_out, 1).reshape(n_tp * CAP, d_model).astype(BF16)
            return state[0] + 1, state[1] + dot('rc,cd->rd', pick, rows_in)

        more_rows = lax.while_loop(lambda state: state[0] < rounds, fetch_more, (jnp.int32(1), jnp.zeros((own, d_model), F32)))[1]
        rows_first, pick_first = fetch(0)

        w_rows = jnp.concatenate([w_q.T, w_o, w_gu.transpose(0, 2, 1).reshape(2 * f_loc, d_model), w_down], axis=0)
        cuts = (q_loc, 2 * q_loc, 2 * q_loc + f_loc, 2 * q_loc + 2 * f_loc)
        wkv_t = w_kv.transpose(0, 2, 1).reshape(2 * head_dim, d_model).astype(BF16)
        inv_freq = ROPE_BASE ** (-jnp.arange(0, head_dim, 2).astype(F32) / head_dim)
        angles = inv_freq[:, None] * (half * own + jnp.arange(own)).astype(F32)[None, :]
        cos_t, sin_t = jnp.cos(angles), jnp.sin(angles)
        f_own, x_one, x_zero, *saved = front(rows_first, pick_first, more_rows, w_rows, wkv_t, ln_scales, cos_t, sin_t, n_tp * q_loc, 0)
        saved, (wq_t, wo_b, wg_t, wu_t, wd_b) = saved[:5], saved[5:]
        weights = (wq_t, wkv_t, wo_b, wg_t, wu_t, wd_b)

        logit_scale = d_model ** -0.5
        lab_loc = labels.reshape(n_tp, own) - tp_rank * vocab_loc
        d_fin, g_head_part, log_norm, lab_sum = head(f_own, lab_loc, embed, logit_scale, logit_scale / tok_total, 4)
        log_norm = lax.dynamic_index_in_dim(log_norm, tp_rank, 0, keepdims=False)
        loss_row = (log_norm + LOGIT_ZLOSS * log_norm * log_norm - jnp.sum(lab_sum, axis=0) * logit_scale) / tok_total
        g_rows, d_zero, rows_back = layer_bwd(d_fin, x_zero, x_one, loss_row[None, :], ln_scales, cos_t, sin_t, weights, saved, pick_first, 7)

        def row_ids(step):
            here = (shard[:, None, :] == tp_rank) & (rank[:, None, :] == slots[None, :, None] + step * CAP)
            return jnp.where(jnp.any(here, axis=-1), jnp.sum(jnp.where(here, row[:, None, :], 0), axis=-1), vocab_loc).reshape(-1)

        def give_back(state):
            mine = (my_shard[None, None, :] == jnp.arange(n_tp)[:, None, None]) & (my_rank[None, None, :] == slots[None, :, None] + state[0] * CAP)
            ids = jnp.sum(jnp.where(mine, jnp.arange(own)[None, None, :], 0), axis=-1).reshape(-1)
            rows_in = plane_swap(jnp.take(d_zero, ids, axis=0).reshape(n_tp, CAP, d_model), 9).reshape(-1, d_model)
            return state[0] + 1, state[1].at[row_ids(state[0])].add(rows_in, mode='drop')

        g_table = lax.while_loop(lambda state: state[0] < rounds, give_back, (jnp.int32(1), g_head_part))[1]
        g_table, g_shard, g_small = tail(g_table, g_rows, rows_back, row_ids(0)[None, :], 10)
        *new, loss = update(g_table, g_shard, g_small, state_arrays)
        return tuple(new) + (loss.reshape(()),)

    return jax.shard_map(local_step, mesh=mesh, in_specs=(P('dp', None), P('dp', None)) + param_specs * 3,
                         out_specs=param_specs * 3 + (P(),), check_vma=False)
```

```python
import functools

import jax
import jax.numpy as jnp
from jax import lax
from jax.experimental import pallas as pl
from jax.experimental.pallas import tpu as pltpu
from jax.sharding import PartitionSpec as P

LN_EPS = 1e-5
LOGIT_ZLOSS = 1e-4
LEARN_RATE = 1e-2
BETA_ONE = 0.9
BETA_TWO = 0.95
ADAM_EPS = 1e-8
ROPE_BASE = 10000.0
NZ = 4
CAP = 96
F32 = jnp.float32
BF16 = jnp.bfloat16
ANY = pl.BlockSpec(memory_space=pl.ANY)
VMEM = pl.BlockSpec(memory_space=pltpu.VMEM)

ARRIVALS = {
    0: (("R", 1), ("R", 2), ("R", 3)),
    1: (("L", 0), ("R", 2), ("R", 3)),
    2: (("R", 3), ("L", 1), ("L", 0)),
    3: (("L", 2), ("L", 1), ("L", 0)),
}
REDUCE_ORDER = {0: (3, 2, 1, 0), 1: (3, 0, 2, 1), 2: (0, 3, 1, 2), 3: (0, 1, 2, 3)}


def remote(src, dst, send_sem, recv_sem, tp, dp):
    return pltpu.make_async_remote_copy(src_ref=src, dst_ref=dst, send_sem=send_sem, recv_sem=recv_sem,
                                        device_id=(tp, dp), device_id_type=pl.DeviceIdType.MESH)


def place():
    tp = lax.axis_index("tp")
    dp = lax.axis_index("dp")
    return tp, dp, tp // 2, tp % 2


def signal(tp, dp):
    pl.semaphore_signal(pltpu.get_barrier_semaphore(), inc=1, device_id=(tp, dp), device_id_type=pl.DeviceIdType.MESH)


def add_into(acc, other, step=None):
    rows = acc.shape[0]
    step = step or (64 if rows % 64 == 0 else 8)

    def body(n, carry):
        at = pl.ds(pl.multiple_of(n * step, step), step)
        acc[at, :] = acc[at, :] + other[at, :]
        return carry

    lax.fori_loop(0, rows // step, body, 0)


def plane_barrier(tp, dp, others):
    peers = [(lax.rem(tp + n, 2 * NZ), dp) for n in range(1, 2 * NZ)] + others
    for peer in peers:
        signal(*peer)
    pl.semaphore_wait(pltpu.get_barrier_semaphore(), len(peers))


def swap_kernel(x_ref, out_ref, own_sem, send, recv):
    tp, dp, _, _ = place()
    plane_barrier(tp, dp, [])
    copies = []
    for n in range(1, 2 * NZ):
        to = lax.rem(tp + n, 2 * NZ)
        copy = remote(x_ref.at[to], out_ref.at[tp], send.at[to], recv.at[tp], to, dp)
        copy.start()
        copies.append(copy)
    own = pltpu.make_async_copy(x_ref.at[tp], out_ref.at[tp], own_sem)
    own.start()
    for n in range(1, 2 * NZ):
        source = lax.rem(tp + n, 2 * NZ)
        remote(out_ref.at[source], out_ref.at[source], send.at[source], recv.at[source], source, dp).wait_recv()
    own.wait()
    for copy in copies:
        copy.wait_send()


def plane_swap(x, collective_id):
    return pl.pallas_call(
        swap_kernel,
        out_shape=jax.ShapeDtypeStruct(x.shape, x.dtype),
        in_specs=[ANY],
        out_specs=ANY,
        scratch_shapes=[pltpu.SemaphoreType.DMA] + [pltpu.SemaphoreType.DMA((2 * NZ,))] * 2,
        compiler_params=pltpu.CompilerParams(collective_id=collective_id, has_side_effects=True),
        name="plane_swap",
    )(x)


FORWARD = {
    0: {1: (("R", 1),), 3: (("R", 2),), 5: (("R", 3),)},
    1: {1: (("L", 0), ("R", 2)), 3: (("R", 3),)},
    2: {1: (("R", 3), ("L", 1)), 3: (("L", 0),)},
    3: {1: (("L", 2),), 3: (("L", 1),), 5: (("L", 0),)},
}
REDUCE = {
    0: {2: (3,), 4: (2,), 6: (1,), 7: (0,)},
    1: {4: (3,), 6: (2, 0), 7: (1,)},
    2: {4: (0,), 6: (1, 3), 7: (2,)},
    3: {2: (0,), 4: (1,), 6: (2,), 7: (3,)},
}
SUB = 256
GROUP = 6


def lookup(table, z, step):
    value = jnp.int32(0)
    for k in range(NZ):
        for s in range(2 * NZ):
            value = value + jnp.where((z == k) & (step == s), table[k][s], 0)
    return value


def head_kernel(scale, token_scale, f_ref, lab_ref, e_ref, dfin_ref, ghead_ref, norm_ref, labsum_ref,
                e_b, e_t, fbuf, f_b, g_acc, from_y, from_l, from_r, dl, lse_all, load_sem, ag_y, ag_l, ag_r, ag_recv,
                rs_y, rs_l, rs_r, recv_y, recv_l, recv_r, st_send, st_recv):
    tp, dp, z, y = place()
    partner = tp + 1 - 2 * y
    vocab, width = e_ref.shape
    own = f_ref.shape[0]
    whole = vocab // (SUB * GROUP)
    rest = vocab - whole * SUB * GROUP
    log2e = 1.4426950408889634
    slope = scale * log2e
    blocks = [(j * SUB, SUB) for j in range(GROUP)]
    tail = [(n, min(SUB, rest - n)) for n in range(0, rest, SUB)]

    plane_barrier(tp, dp, [])

    def send(src, slot, sems, to):
        remote(src, fbuf.at[slot], sems.at[slot], ag_recv.at[slot], to, dp).start()

    def arrived(slot):
        remote(f_ref, fbuf.at[slot], ag_y.at[slot], ag_recv.at[slot], partner, dp).wait_recv()

    def first_sends(k):
        if k > 0:
            send(f_ref, tp, ag_l, tp - 2)
        if k < NZ - 1:
            send(f_ref, tp, ag_r, tp + 2)
        send(f_ref, tp, ag_y, partner)

    for k in range(NZ):
        pl.when(z == k)(functools.partial(first_sends, k))
    load = pltpu.make_async_copy(e_ref, g_acc, load_sem.at[0])
    load.start()
    own_copy = pltpu.make_async_copy(f_ref, fbuf.at[tp], load_sem.at[1])
    own_copy.start()
    load.wait()

    def prepare(at, size):
        part = g_acc[at, :]
        e_b[at, :] = part.astype(BF16)
        e_t[:, at] = part.T.astype(BF16)

    def prepare_body(n, carry):
        prepare(pl.ds(pl.multiple_of(n * SUB, SUB), SUB), SUB)
        return carry

    lax.fori_loop(0, vocab // SUB, prepare_body, 0)
    if vocab % SUB:
        prepare(pl.ds(vocab // SUB * SUB, vocab % SUB), vocab % SUB)
    own_copy.wait()

    def over_blocks(group, carry):
        def body(n, c):
            return group(pl.multiple_of(n * SUB * GROUP, SUB * GROUP), blocks, c)
        carry = lax.fori_loop(0, whole, body, carry)
        return group(whole * SUB * GROUP, tail, carry) if tail else carry

    order1 = {k: (k,) + tuple(v for pair in zip([a[1] for a in ARRIVALS[k]], [k] + [a[1] for a in ARRIVALS[k]]) for v in pair) + (ARRIVALS[k][-1][1],) for k in range(NZ)}
    order1 = {k: [2 * zz + (s % 2 == 0 and s > 0 or s == 7) for s, zz in enumerate(order1[k])] for k in range(NZ)}

    def chunk_of(table, step):
        code = lookup(table, z, step)
        other = code % 2
        return code // 2 * 2 + y + other - 2 * y * other

    def gather_step(step, carry):
        slot = chunk_of(order1, step)
        for k in range(NZ):
            for s, shards in FORWARD[k].items():
                def pass_on(k=k, shards=shards):
                    for side, zz in shards:
                        at = 2 * zz + y
                        arrived(at)
                        if side == "L" and k < NZ - 1:
                            send(fbuf.at[at], at, ag_r, tp + 2)
                        if side == "R" and k > 0:
                            send(fbuf.at[at], at, ag_l, tp - 2)
                        send(fbuf.at[at], at, ag_y, partner)
                pl.when((z == k) & (step == s))(pass_on)
        pl.when(slot % 2 != y)(lambda: arrived(slot))
        f_b[slot] = fbuf[slot].astype(BF16)
        f_now = f_b[slot]

        def group(base, parts, c):
            top, total = c
            for first, size in parts:
                logit = lax.dot_general(e_b[pl.ds(base + first, size), :], f_now, (((1,), (1,)), ((), ())), preferred_element_type=F32)
                logit = logit.reshape(size // 8, 8, own)
                new = jnp.maximum(top, jnp.max(logit, axis=0))
                total = total * jnp.exp2((top - new) * slope) + jnp.sum(jnp.exp2((logit - new[None]) * slope), axis=0)
                top = new
            return top, total

        top, total = over_blocks(group, (jnp.full((8, own), -3e38, F32), jnp.zeros((8, own), F32)))
        most = jnp.max(top, axis=0, keepdims=True)
        total = jnp.sum(total * jnp.exp2((top - most) * slope), axis=0, keepdims=True)
        lse_all[tp, pl.ds(slot, 1), :] = most * scale + jnp.log(total)
        return carry

    lax.fori_loop(0, 2 * NZ, gather_step, 0)

    for n in range(1, 2 * NZ):
        to = lax.rem(tp + n, 2 * NZ)
        remote(lse_all.at[tp], lse_all.at[tp], st_send.at[to], st_recv.at[tp], to, dp).start()

    def gathers_done(k):
        def done(sems, slot):
            remote(f_ref, fbuf.at[slot], sems.at[slot], ag_recv.at[slot], partner, dp).wait_send()
        if k > 0:
            done(ag_l, tp)
        if k < NZ - 1:
            done(ag_r, tp)
        done(ag_y, tp)
        for side, zz in ARRIVALS[k]:
            at = 2 * zz + y
            if side == "L" and k < NZ - 1:
                done(ag_r, at)
            if side == "R" and k > 0:
                done(ag_l, at)
            done(ag_y, at)

    for k in range(NZ):
        pl.when(z == k)(functools.partial(gathers_done, k))

    def clear(n, carry):
        g_acc[pl.ds(pl.multiple_of(n * 16, 16), 16), :] = jnp.zeros((16, width), F32)
        return carry

    lax.fori_loop(0, vocab // 16, clear, 0)
    for n in range(1, 2 * NZ):
        source = lax.rem(tp + n, 2 * NZ)
        remote(lse_all.at[source], lse_all.at[source], st_send.at[source], st_recv.at[source], source, dp).wait_recv()
    peak = jnp.max(lse_all[...], axis=0)
    log_norm = peak + jnp.log(jnp.sum(jnp.exp(lse_all[...] - peak[None]), axis=0))
    norm_ref[...] = log_norm

    order2 = {k: [2 * zz + 1 - s for zz in REDUCE_ORDER[k] for s in range(2)] for k in range(NZ)}

    def scatter_step(step, lab_sum):
        slot = chunk_of(order2, step)
        f_now = f_b[slot]
        acc = fbuf.at[slot]
        norm = norm_ref[pl.ds(slot, 1), :]
        shift = norm * log2e
        coef = (1.0 + 2.0 * LOGIT_ZLOSS * norm) * token_scale
        lab = lab_ref[pl.ds(slot, 1), :]
        acc[...] = jnp.zeros((width, own), F32)

        def group(base, parts, hits):
            for first, size in parts:
                at = pl.ds(base + first, size)
                logit = lax.dot_general(e_b[at, :], f_now, (((1,), (1,)), ((), ())), preferred_element_type=F32)
                hit = lax.broadcasted_iota(jnp.int32, (size, own), 0) == lab - (base + first)
                prob = jnp.exp2(logit * slope - shift) * coef
                grad = jnp.where(hit, prob - token_scale, prob).astype(BF16)
                hits = hits + jnp.sum(jnp.where(hit, logit, 0.0).reshape(size // 8, 8, own), axis=0)
                dl[pl.ds(first, size), :] = grad
                g_acc[at, :] += jnp.dot(grad, f_now, preferred_element_type=F32)
            size = parts[-1][0] + parts[-1][1]
            acc[...] += jnp.dot(e_t[:, pl.ds(base, size)], dl[pl.ds(0, size), :], preferred_element_type=F32)
            return hits

        lab_sum = over_blocks(group, lab_sum)

        def hand_over():
            remote(acc, from_y.at[slot // 2], rs_y.at[slot // 2], recv_y.at[slot // 2], partner, dp).start()
        pl.when(slot % 2 != y)(hand_over)

        for k in range(NZ):
            for s, shards in REDUCE[k].items():
                def reduce(k=k, shards=shards):
                    for zz in shards:
                        line = fbuf.at[2 * zz + y]
                        remote(line, from_y.at[zz], rs_y.at[zz], recv_y.at[zz], partner, dp).wait_recv()
                        add_into(line, from_y.at[zz])
                        if zz >= k and k > 0:
                            remote(line, from_l.at[zz - 1], rs_l.at[zz], recv_l.at[zz], partner, dp).wait_recv()
                            add_into(line, from_l.at[zz - 1])
                        if zz <= k and k < NZ - 1:
                            remote(line, from_r.at[zz], rs_r.at[zz], recv_r.at[zz], partner, dp).wait_recv()
                            add_into(line, from_r.at[zz])
                        if zz > k:
                            remote(line, from_l.at[zz - 1], rs_r.at[zz], recv_l.at[zz], tp + 2, dp).start()
                        if zz < k:
                            remote(line, from_r.at[zz], rs_l.at[zz], recv_r.at[zz], tp - 2, dp).start()
                pl.when((z == k) & (step == s))(reduce)
        return lab_sum

    lab_sum = lax.fori_loop(0, 2 * NZ, scatter_step, jnp.zeros((8, own), F32))
    labsum_ref[...] = lab_sum
    store = pltpu.make_async_copy(g_acc, ghead_ref, load_sem.at[0])
    store.start()
    dfin_ref[...] = fbuf[tp].T

    def scatters_done(k):
        for zz in range(NZ):
            line = fbuf.at[2 * zz + y]
            remote(line, from_y.at[zz], rs_y.at[zz], recv_y.at[zz], partner, dp).wait_send()
            if zz > k:
                remote(line, from_l.at[zz - 1], rs_r.at[zz], recv_l.at[zz], partner, dp).wait_send()
            if zz < k:
                remote(line, from_r.at[zz], rs_l.at[zz], recv_r.at[zz], partner, dp).wait_send()

    for k in range(NZ):
        pl.when(z == k)(functools.partial(scatters_done, k))
    for n in range(1, 2 * NZ):
        to = lax.rem(tp + n, 2 * NZ)
        remote(lse_all.at[tp], lse_all.at[tp], st_send.at[to], st_recv.at[tp], to, dp).wait_send()
    store.wait()


def head(f_own, labels, embed, scale, token_scale, collective_id):
    own, width = f_own.shape
    vocab = embed.shape[0]
    chunk = (own, width)
    dma8 = pltpu.SemaphoreType.DMA((2 * NZ,))
    dma4 = pltpu.SemaphoreType.DMA((NZ,))
    return pl.pallas_call(
        functools.partial(head_kernel, scale, token_scale),
        out_shape=(jax.ShapeDtypeStruct((own, width), F32), jax.ShapeDtypeStruct((vocab, width), F32),
                   jax.ShapeDtypeStruct((2 * NZ, own), F32), jax.ShapeDtypeStruct((8, own), F32)),
        in_specs=[VMEM, VMEM, ANY],
        out_specs=(VMEM, ANY, VMEM, VMEM),
        scratch_shapes=[pltpu.VMEM((vocab, width), BF16), pltpu.VMEM((width, vocab), BF16),
                        pltpu.VMEM((2 * NZ,) + chunk, F32), pltpu.VMEM((2 * NZ,) + chunk, BF16), pltpu.VMEM((vocab, width), F32),
                        pltpu.VMEM((NZ,) + chunk, F32), pltpu.VMEM((NZ - 1,) + chunk, F32), pltpu.VMEM((NZ - 1,) + chunk, F32),
                        pltpu.VMEM((SUB * GROUP, own), BF16), pltpu.VMEM((2 * NZ, 2 * NZ, own), F32),
                        pltpu.SemaphoreType.DMA((2,)), dma8, dma8, dma8, dma8, dma4, dma4, dma4, dma4, dma4, dma4, dma8, dma8],
        compiler_params=pltpu.CompilerParams(collective_id=collective_id, has_side_effects=True, vmem_limit_bytes=67000000),
        cost_estimate=pl.CostEstimate(flops=8 * vocab * width * own * 8, bytes_accessed=3 * 4 * vocab * width, transcendentals=2 * vocab * own * 8),
        name="head",
    )(f_own, labels, embed)


TB = (((1,), (1,)), ((), ()))
TA = (((0,), (0,)), ((), ()))
LOG2E = 1.4426950408889634


def mm(a, b, dims=(((1,), (0,)), ((), ()))):
    return lax.dot_general(a, b, dims, preferred_element_type=F32)


def turn(lo, hi, cos_t, sin_t):
    return lo * cos_t - hi * sin_t, hi * cos_t + lo * sin_t


EVENTS = {
    0: (((("R", 1),), (0,)), ((("R", 2),), (1,)), ((("R", 3),), (2,)), ((), (3,))),
    1: (((("L", 0), ("R", 2)), (1,)), ((("R", 3),), (0,)), ((), (2,)), ((), (3,))),
    2: (((("R", 3), ("L", 1)), (2,)), ((("L", 0),), (3,)), ((), (1,)), ((), (0,))),
    3: (((("L", 2),), (3,)), ((("L", 1),), (2,)), ((("L", 0),), (1,)), ((), (0,))),
}
MLP_ORDER = {k: [2 * k] + [code for line, other in EVENTS[k] for code in [2 * zz for _, zz in line] + [2 * zz + 1 for zz in other]] for k in range(NZ)}


def front_kernel(ids_ref, e_ref, pick_ref, extra_ref, w_ref, wkv_ref, ln_ref, cos_ref, sin_ref,
                 f_ref, x1_ref, x0_ref, q_ref, kv_ref, kvt_ref, lse_ref, ctx_ref, wq_ref, wo_ref, wg_ref, wu_ref, wd_ref,
                 table, rows_ref, wl, rows_in, u_b, kv_out, kv_in, own_sem, r_send, r_recv, a_y, a_l, a_r, a_c, a_recv,
                 b_y, b_l, b_r, b_x, b_c, b_recv, kv_send, kv_recv):
    tp, dp, z, y = place()
    partner = tp + 1 - 2 * y
    core = dp % 2
    twin = dp + 1 - 2 * core
    facing = lax.rem(dp + 2, 4)
    own, width = x0_ref.shape
    shards, w_rows = wl.shape[0], wl.shape[1]
    nq = q_ref.shape[0]
    ff = wg_ref.shape[0]
    n_a = nq // shards
    n_f = ff // shards
    n_b = 3 * n_f // 4
    hd = kv_out.shape[0] // 2
    quarter = hd // 2
    heads = nq // hd

    def a_rows(c):
        return pl.ds(pl.multiple_of(c * n_a, 8), n_a)

    def b_rows(d):
        return pl.ds(pl.multiple_of(2 * n_a + d * n_b, 8), n_b)

    def a_copy(slot, sems, to, to_dp, first=False):
        src = w_ref.at[a_rows(core), :] if first else wl.at[slot, a_rows(core), :]
        return remote(src, wl.at[slot, a_rows(core), :], sems.at[slot], a_recv.at[slot, core], to, to_dp)

    def b_copy(slot, piece, sems, to, to_dp, first=False):
        src = w_ref.at[b_rows(piece), :] if first else wl.at[slot, b_rows(piece), :]
        return remote(src, wl.at[slot, b_rows(piece), :], sems.at[slot], b_recv.at[slot, piece], to, to_dp)

    def a_wait(slot, c):
        remote(w_ref.at[a_rows(c), :], wl.at[slot, a_rows(c), :], a_y.at[slot], a_recv.at[slot, c], partner, dp).wait_recv()

    def b_wait(slot, piece):
        remote(w_ref.at[b_rows(piece), :], wl.at[slot, b_rows(piece), :], b_y.at[slot], b_recv.at[slot, piece], partner, dp).wait_recv()

    def on_position(f):
        for k in range(NZ):
            pl.when(z == k)(functools.partial(f, k))

    def line_sends(k, make, y_sems, l_sems, r_sems, slot, side, first=False):
        sends = [make(slot, y_sems, partner, dp, first)]
        if k > 0 and side != "L":
            sends.append(make(slot, l_sems, tp - 2, dp, first))
        if k < NZ - 1 and side != "R":
            sends.append(make(slot, r_sems, tp + 2, dp, first))
        return sends

    def b_own(slot, sems, to, to_dp, first=False):
        return b_copy(slot, dp, sems, to, to_dp, first)

    def a_sends(k, slot, side, first=False):
        return line_sends(k, a_copy, a_y, a_l, a_r, slot, side, first)

    def b_sends(k, slot, side, first=False):
        return line_sends(k, b_own, b_y, b_l, b_r, slot, side, first)

    def start(copies):
        for c in copies:
            c.start()

    load = pltpu.make_async_copy(e_ref, table, own_sem.at[2])
    load.start()
    plane_barrier(tp, dp, [(tp, twin), (tp, facing)])
    peers = [lax.rem(tp + n, shards) for n in range(1, shards)]

    def row_copy(to):
        return remote(rows_ref.at[to], rows_in.at[tp], r_send.at[to], r_recv.at[tp], to, dp)

    on_position(lambda k: start(b_sends(k, tp, "", True)))
    on_position(lambda k: start(a_sends(k, tp, "", True)))
    own_w = pltpu.make_async_copy(w_ref, wl.at[tp], own_sem.at[1])
    own_w.start()

    def a_event(t, k):
        line, other = EVENTS[k][t]
        for side, zz in line:
            slot = 2 * zz + y
            a_wait(slot, core)
            start(a_sends(k, slot, side))
            a_copy(slot, a_c, tp, twin).start()
        for zz in other:
            slot = 2 * zz + 1 - y
            a_wait(slot, core)
            a_copy(slot, a_c, tp, twin).start()

    def b_event(t, k):
        line, other = EVENTS[k][t]
        for side, zz in line:
            slot = 2 * zz + y
            b_wait(slot, dp)
            start(b_sends(k, slot, side))
            b_copy(slot, dp, b_x, tp, facing).start()
            b_copy(slot, dp, b_c.at[0], tp, twin).start()
        for zz in other:
            slot = 2 * zz + 1 - y
            b_wait(slot, dp)
            b_copy(slot, dp, b_x, tp, facing).start()
            b_copy(slot, dp, b_c.at[0], tp, twin).start()

    load.wait()
    cap = rows_ref.shape[1]

    def pick_rows(n, carry):
        for i in range(8):
            rows_ref[n // (cap // 8), pl.ds(lax.rem(n, cap // 8) * 8 + i, 1), :] = table[pl.ds(ids_ref[n * 8 + i], 1), :]
        return carry

    lax.fori_loop(0, shards * cap // 8, pick_rows, 0)
    on_position(functools.partial(b_event, 0))
    on_position(functools.partial(a_event, 0))
    start([row_copy(to) for to in peers])
    own_rows = pltpu.make_async_copy(rows_ref.at[tp], rows_in.at[tp], own_sem.at[0])
    own_rows.start()
    on_position(functools.partial(b_event, 1))
    on_position(functools.partial(a_event, 1))
    own_rows.wait()
    for source in peers:
        remote(rows_ref.at[source], rows_in.at[source], r_send.at[source], r_recv.at[source], source, dp).wait_recv()
    x0_ref[...] = extra_ref[...] + mm(pick_ref[...], rows_in[...].reshape(pick_ref.shape[1], width).astype(BF16))
    u_b[...] = norm_fwd(x0_ref[...], ln_ref[0:1, :])[0]
    x1_ref[...] = x0_ref[...]
    cos_t = cos_ref[...]
    sin_t = sin_ref[...]
    kv = mm(wkv_ref[...], u_b[...], TB)
    lo, hi = turn(kv[:quarter], kv[quarter:hd], cos_t, sin_t)
    kv_out[0:quarter, :] = lo
    kv_out[quarter:hd, :] = hi
    kv_out[hd:, :] = kv[hd:]
    kv_copy = remote(kv_out, kv_in, kv_send, kv_recv, partner, dp)
    kv_copy.start()

    def slot_of(step):
        code = lookup(MLP_ORDER, z, step)
        other = code % 2
        return code // 2 * 2 + y + other - 2 * y * other

    def mlp(step, carry):
        def pass_on():
            slot = slot_of(step + 1)
            b_wait(slot, facing)
            b_copy(slot, facing, b_c.at[1], tp, twin).start()
        pl.when(step < shards - 1)(pass_on)
        slot = slot_of(step)

        def rest():
            b_wait(slot, twin)
            b_wait(slot, lax.rem(twin + 2, 4))
        pl.when(step > 0)(rest)
        at = pl.ds(pl.multiple_of(slot * n_f, n_f), n_f)
        wg_ref[at, :] = wl[slot, 2 * n_a:2 * n_a + n_f, :].astype(BF16)
        wu_ref[at, :] = wl[slot, 2 * n_a + n_f:2 * n_a + 2 * n_f, :].astype(BF16)
        wd_ref[at, :] = wl[slot, 2 * n_a + 2 * n_f:2 * n_a + 3 * n_f, :].astype(BF16)
        gate = mm(u_b[...], wg_ref[at, :], TB)
        up = mm(u_b[...], wu_ref[at, :], TB)
        x1_ref[...] += mm((gate * jax.nn.sigmoid(gate) * up).astype(BF16), wd_ref[at, :])
        return carry

    own_w.wait()
    lax.fori_loop(0, 3, mlp, 0)
    on_position(functools.partial(b_event, 2))
    on_position(functools.partial(a_event, 2))
    lax.fori_loop(3, 4, mlp, 0)
    on_position(functools.partial(a_event, 3))
    on_position(functools.partial(b_event, 3))
    for source in peers:
        a_wait(source, 1 - core)
    for s in range(shards):
        wq_ref[s * n_a:(s + 1) * n_a, :] = wl[s, 0:n_a, :].astype(BF16)
        wo_ref[s * n_a:(s + 1) * n_a, :] = wl[s, n_a:2 * n_a, :].astype(BF16)

    q_all = mm(wq_ref[...], u_b[...], TB)
    for h in range(heads):
        lo, hi = turn(q_all[h * hd:h * hd + quarter], q_all[h * hd + quarter:(h + 1) * hd], cos_t, sin_t)
        q_ref[h * hd:h * hd + quarter, :] = lo.astype(BF16)
        q_ref[h * hd + quarter:(h + 1) * hd, :] = hi.astype(BF16)
    kv_copy.wait()

    def fill(mine, other):
        kv_ref[mine * own:(mine + 1) * own, :] = kv_out[...].T.astype(BF16)
        kv_ref[other * own:(other + 1) * own, :] = kv_in[...].T.astype(BF16)
        kvt_ref[:, mine * own:(mine + 1) * own] = kv_out[...].astype(BF16)
        kvt_ref[:, other * own:(other + 1) * own] = kv_in[...].astype(BF16)

    pl.when(y == 0)(lambda: fill(0, 1))
    pl.when(y == 1)(lambda: fill(1, 0))
    blank = jnp.zeros((hd, own), BF16)
    slope = hd ** -0.5 * LOG2E

    def attend(h, carry):
        at = pl.ds(pl.multiple_of(h * hd, hd), hd)
        scores = mm(kv_ref[...], jnp.concatenate([q_ref[at, :], blank], axis=0))
        allowed = lax.broadcasted_iota(jnp.int32, scores.shape, 0) <= lax.broadcasted_iota(jnp.int32, scores.shape, 1) + y * own
        scores = jnp.where(allowed, scores * slope, -1e30)
        top = jnp.max(scores, axis=0, keepdims=True)
        prob = jnp.exp2(scores - top)
        total = jnp.sum(prob, axis=0, keepdims=True)
        lse_ref[pl.ds(h, 1), :] = top + jnp.log2(total)
        ctx_ref[at, :] = mm(kvt_ref[hd:, :], (prob * (1.0 / total)).astype(BF16)).astype(BF16)
        return carry

    lax.fori_loop(0, heads, attend, 0)
    x1_ref[...] += mm(ctx_ref[...], wo_ref[...], TA)

    lax.fori_loop(4, shards, mlp, 0)
    f_ref[...] = norm_fwd(x1_ref[...], ln_ref[1:2, :])[0].astype(F32)

    def finish(k):
        done = a_sends(k, tp, "", True) + b_sends(k, tp, "", True)
        for line, other in EVENTS[k]:
            for side, zz in line:
                done += a_sends(k, 2 * zz + y, side) + b_sends(k, 2 * zz + y, side)
        for c in done:
            c.wait_send()

    on_position(finish)
    for to in peers:
        row_copy(to).wait_send()
        a_copy(to, a_c, tp, twin).wait_send()
        b_copy(to, dp, b_x, tp, facing).wait_send()
        b_copy(to, dp, b_c.at[0], tp, twin).wait_send()
        b_copy(to, facing, b_c.at[1], tp, twin).wait_send()


def front(ids, embed, pick, extra, w_rows, wkv_t, ln, cos_t, sin_t, n_q, collective_id):
    own, width = extra.shape
    two_hd = wkv_t.shape[0]
    shards = 2 * NZ
    ff = (w_rows.shape[0] * shards - 2 * n_q) // 3
    dma = lambda *n: pltpu.SemaphoreType.DMA(n)
    s = jax.ShapeDtypeStruct
    rows = (shards, ids.shape[0] // shards, width)
    return pl.pallas_call(
        front_kernel,
        out_shape=(s((own, width), F32),) * 3 + (s((n_q, own), BF16), s((2 * own, two_hd), BF16), s((two_hd, 2 * own), BF16),
                   s((2 * n_q // two_hd, own), F32), s((n_q, own), BF16), s((n_q, width), BF16), s((n_q, width), BF16))
        + (s((ff, width), BF16),) * 3,
        in_specs=[pl.BlockSpec(memory_space=pltpu.SMEM), ANY, VMEM, VMEM, ANY] + [VMEM] * 4,
        out_specs=(VMEM,) * 13,
        scratch_shapes=[pltpu.VMEM(embed.shape, F32), pltpu.VMEM(rows, F32), pltpu.VMEM((shards,) + w_rows.shape, F32), pltpu.VMEM(rows, F32), pltpu.VMEM((own, width), BF16),
                        pltpu.VMEM((two_hd, own), F32), pltpu.VMEM((two_hd, own), F32),
                        dma(3), dma(shards), dma(shards)] + [dma(shards)] * 4 + [dma(shards, 2)]
        + [dma(shards)] * 4 + [dma(2, shards), dma(shards, 4), pltpu.SemaphoreType.DMA, pltpu.SemaphoreType.DMA],
        compiler_params=pltpu.CompilerParams(collective_id=collective_id, has_side_effects=True, vmem_limit_bytes=60000000),
        name="front",
    )(ids, embed, pick, extra, w_rows, wkv_t, ln, cos_t, sin_t)


def layer_bwd_kernel(dfin_ref, x0_ref, x1_ref, loss_ref, ln_ref, cos_ref, sin_ref, wq_ref, wkv_ref, wo_ref, wg_ref, wu_ref, wd_ref,
                     q_ref, kv_ref, kvt_ref, lse_ref, ctx_ref, pick_ref, rows_ref, d0_ref, back_ref, d_one, d_b, u_b, dctx, dq, dkv, dkv_in,
                     hid, d_gate, d_up, rows_out, g_q, g_o, g_g, g_u, g_d, small, out_sem, send_sem, recv_sem, r_send, r_recv):
    tp, dp, _, y = place()
    partner = tp + 1 - 2 * y
    own, width = x0_ref.shape
    hd = kv_ref.shape[1] // 2
    quarter = hd // 2
    nq = q_ref.shape[0]
    heads = nq // hd
    ff = wg_ref.shape[0]
    shards = rows_ref.shape[0]
    plane_barrier(tp, dp, [])
    _, f_hat, f_inv = norm_fwd(x1_ref[...], ln_ref[1:2, :])
    d_in, g_fin = norm_bwd(dfin_ref[...], f_hat, f_inv, ln_ref[1:2, :])
    d_one[...] = d_in
    d_b[...] = d_in.astype(BF16)
    u_b[...] = norm_fwd(x0_ref[...], ln_ref[0:1, :])[0]
    dctx[...] = mm(wo_ref[...], d_b[...], TB).astype(BF16)
    cos_t = cos_ref[...]
    sin_t = sin_ref[...]
    blank = jnp.zeros((hd, own), BF16)
    slope = hd ** -0.5 * LOG2E
    dkv[...] = jnp.zeros_like(dkv)

    def attend(h, carry):
        at = pl.ds(pl.multiple_of(h * hd, hd), hd)
        q_pad = jnp.concatenate([q_ref[at, :], blank], axis=0)
        d_pad = jnp.concatenate([blank, dctx[at, :]], axis=0)
        scores = mm(kv_ref[...], q_pad)
        allowed = lax.broadcasted_iota(jnp.int32, scores.shape, 0) <= lax.broadcasted_iota(jnp.int32, scores.shape, 1) + y * own
        prob = jnp.where(allowed, jnp.exp2(scores * slope - lse_ref[pl.ds(h, 1), :]), 0.0)
        d_prob = mm(kv_ref[...], d_pad)
        mean = jnp.sum(d_prob * prob, axis=0, keepdims=True)
        d_score = (prob * (d_prob - mean) * hd ** -0.5).astype(BF16)
        dkv[...] += mm(d_score, q_pad, TB) + mm(prob.astype(BF16), d_pad, TB)
        d_q = mm(kvt_ref[0:hd, :], d_score)
        lo, hi = turn(d_q[:quarter], d_q[quarter:], cos_t, -sin_t)
        dq[at, :] = jnp.concatenate([lo, hi], axis=0).astype(BF16)
        return carry

    lax.fori_loop(0, heads, attend, 0)
    copy = remote(dkv.at[pl.ds(pl.multiple_of((1 - y) * own, own), own), :], dkv_in, send_sem, recv_sem, partner, dp)
    copy.start()

    d0_ref[...] = mm(dq[...], wq_ref[...], TA)
    step = min(512, ff)

    def mlp(n, carry):
        at = pl.ds(pl.multiple_of(n * step, step), step)
        gate = mm(wg_ref[at, :], u_b[...], TB)
        up = mm(wu_ref[at, :], u_b[...], TB)
        d_hidden = mm(wd_ref[at, :], d_b[...], TB)
        sig = jax.nn.sigmoid(gate)
        hid[at, :] = (gate * sig * up).astype(BF16)
        d_gate[at, :] = (d_hidden * up * sig * (1.0 + gate * (1.0 - sig))).astype(BF16)
        d_up[at, :] = (d_hidden * gate * sig).astype(BF16)
        d0_ref[...] += mm(d_gate[at, :], wg_ref[at, :], TA) + mm(d_up[at, :], wu_ref[at, :], TA)
        return carry

    lax.fori_loop(0, ff // step, mlp, 0)
    copy.wait()
    d_kv = (dkv[pl.ds(pl.multiple_of(y * own, own), own), :] + dkv_in[...]).T
    lo, hi = turn(d_kv[:quarter], d_kv[quarter:hd], cos_t, -sin_t)
    d_kv = jnp.concatenate([lo, hi, d_kv[hd:]], axis=0).astype(BF16)
    small[0:2 * hd, :] = mm(d_kv, u_b[...])
    d_u = d0_ref[...] + mm(d_kv, wkv_ref[...], TA)
    _, u_hat, u_inv = norm_fwd(x0_ref[...], ln_ref[0:1, :])
    d_in, g_in = norm_bwd(d_u, u_hat, u_inv, ln_ref[0:1, :])
    d_zero = d_one[...] + d_in
    d0_ref[...] = d_zero
    high = d_zero.astype(BF16)
    left = d_zero - high.astype(F32)
    middle = left.astype(BF16)
    low = (left - middle.astype(F32)).astype(BF16)
    rows_out[...] = (mm(pick_ref[...], high, TA) + mm(pick_ref[...], middle, TA) + mm(pick_ref[...], low, TA)).reshape(rows_out.shape)

    def row_copy(to):
        return remote(rows_out.at[to], back_ref.at[tp], r_send.at[to], r_recv.at[tp], to, dp)

    peers = [lax.rem(tp + n, shards) for n in range(1, shards)]
    for to in peers:
        row_copy(to).start()
    own_rows = pltpu.make_async_copy(rows_out.at[tp], back_ref.at[tp], out_sem.at[7 * 2 * NZ])
    own_rows.start()

    g_o[...] = mm(ctx_ref[...], d_b[...])
    g_q[...] = mm(dq[...], u_b[...])

    def weight_grads(n, carry):
        at = pl.ds(pl.multiple_of(n * step, step), step)
        g_d[at, :] = mm(hid[at, :], d_b[...])
        g_g[at, :] = mm(d_gate[at, :], u_b[...])
        g_u[at, :] = mm(d_up[at, :], u_b[...])
        return carry

    lax.fori_loop(0, ff // step, weight_grads, 0)
    small[2 * hd:, :] = jnp.zeros_like(small[2 * hd:, :])
    small[2 * hd:2 * hd + 1, :] = g_in.reshape(1, width)
    small[2 * hd + 1:2 * hd + 2, :] = g_fin.reshape(1, width)
    small[2 * hd + 2:2 * hd + 3, :] = loss_ref[...]
    copies = []

    def put(src, first, size, s):
        copies.append(pltpu.make_async_copy(src, rows_ref.at[s, pl.ds(first, size), :], out_sem.at[len(copies)]))

    n_kv = 2 * hd // shards
    for s in range(shards):
        at = 0
        for g, size in ((g_q, nq // shards), (g_o, nq // shards), (g_g, ff // shards), (g_u, ff // shards), (g_d, ff // shards)):
            put(g.at[pl.ds(s * size, size), :], at, size, s)
            at += size
        put(small.at[pl.ds(s * n_kv, n_kv), :], at, n_kv, s)
        put(small.at[pl.ds(2 * hd + (0 if s == 0 else 16), 16), :], at + n_kv, 16, s)
    for c in copies:
        c.start()
    for c in copies:
        c.wait()
    own_rows.wait()
    for source in peers:
        remote(rows_out.at[source], back_ref.at[source], r_send.at[source], r_recv.at[source], source, dp).wait_recv()
        row_copy(source).wait_send()


def layer_bwd(d_fin, x0, x1, loss_row, ln, cos_t, sin_t, weights, saved, pick, collective_id):
    own, width = x0.shape
    nq = weights[0].shape[0]
    two_hd = weights[1].shape[0]
    ff = weights[3].shape[0]
    rows = (2 * nq + 3 * ff + two_hd) // (2 * NZ) + 16
    chunk = (own, width)
    back = (2 * NZ, pick.shape[1] // (2 * NZ), width)
    return pl.pallas_call(
        layer_bwd_kernel,
        out_shape=(jax.ShapeDtypeStruct((2 * NZ, rows, width), F32), jax.ShapeDtypeStruct(chunk, F32), jax.ShapeDtypeStruct(back, F32)),
        in_specs=[VMEM] * 19,
        out_specs=(ANY, VMEM, ANY),
        scratch_shapes=[pltpu.VMEM(chunk, F32), pltpu.VMEM(chunk, BF16), pltpu.VMEM(chunk, BF16), pltpu.VMEM((nq, own), BF16),
                        pltpu.VMEM((nq, own), BF16), pltpu.VMEM((2 * own, two_hd), F32), pltpu.VMEM((own, two_hd), F32)]
        + [pltpu.VMEM((ff, own), BF16)] * 3 + [pltpu.VMEM(back, F32), pltpu.VMEM((nq, width), F32), pltpu.VMEM((nq, width), F32)] + [pltpu.VMEM((ff, width), F32)] * 3
        + [pltpu.VMEM((two_hd + 32, width), F32), pltpu.SemaphoreType.DMA((14 * NZ + 1,)), pltpu.SemaphoreType.DMA, pltpu.SemaphoreType.DMA,
           pltpu.SemaphoreType.DMA((2 * NZ,)), pltpu.SemaphoreType.DMA((2 * NZ,))],
        compiler_params=pltpu.CompilerParams(collective_id=collective_id, has_side_effects=True, vmem_limit_bytes=60000000),
        name="layer_bwd",
    )(d_fin, x0, x1, loss_row, ln, cos_t, sin_t, *weights, *saved, pick)


N_BLOCK = 12
EARLY = 9
W_REDUCE = {
    0: {1: (3,), 3: (2,), 5: (1,), 7: (0,)},
    1: {3: (3,), 5: (2, 0), 7: (1,)},
    2: {3: (0,), 5: (1, 3), 7: (2,)},
    3: {1: (0,), 3: (1,), 5: (2,), 7: (3,)},
}


def tail_kernel(g_ref, p_ref, rows_ref, ids_ref, t_ref, w_out, small_ref,
                s_buf, from_c, from_x, rows_c, ids_c, parts, acc, w_c, w_y, w_l, w_r, w_x,
                g_load, g_send_c, g_recv_c, g_send_x, g_recv_x, g_send_t, g_recv_t, g_store, l_send, l_recv,
                w_load, w_out_sem, send_c, send_y, send_l, send_r, recv_c, recv_y, recv_l, recv_r, last_send, last_recv, small_send, small_recv):
    tp, dp, z, y = place()
    partner = tp + 1 - 2 * y
    core = dp % 2
    twin = dp + 1 - 2 * core
    facing = lax.rem(dp + 2, 4)
    half = g_ref.shape[0] // 2
    size = s_buf.shape[1]
    last = half - (N_BLOCK - 1) * size
    n_look = rows_ref.shape[0]

    def rows(which, b, n):
        return pl.ds(pl.multiple_of(which * half + b * size, 8), n)

    def part(buf, b, n):
        return buf.at[b, pl.ds(0, n), :]

    plane_barrier(tp, dp, [(tp, twin), (tp, facing)])

    look_copies = [remote(rows_ref, rows_c, l_send.at[0], l_recv.at[0], tp, twin), remote(ids_ref, ids_c, l_send.at[1], l_recv.at[1], tp, twin)]
    for c in look_copies:
        c.start()

    def c_copy(b, n):
        return remote(g_ref.at[rows(1 - core, b, n), :], part(from_c, b, n), g_send_c.at[b], g_recv_c.at[b], tp, twin)

    def own_load(b, n):
        return pltpu.make_async_copy(g_ref.at[rows(core, b, n), :], part(s_buf, b, n), g_load.at[b])

    def x_copy(b, n):
        return remote(part(s_buf, b, n), part(from_x, b, n), g_send_x.at[b], g_recv_x.at[b], tp, facing)

    def t_copy(b, n):
        return remote(part(from_x, b, n), t_ref.at[rows(core, b, n), :], g_send_t.at[b], g_recv_t.at[b], tp, twin)

    def t_store(b, n):
        return pltpu.make_async_copy(part(from_x, b, n), t_ref.at[rows(core, b, n), :], g_store.at[b])

    def every(f, first, end):
        def body(b, carry):
            f(b, size)
            return carry
        lax.fori_loop(first, min(end, N_BLOCK - 1), body, 0)
        if end == N_BLOCK:
            f(N_BLOCK - 1, last)

    def chip_sum(b, n):
        own_load(b, n).wait()
        c_copy(b, n).wait_recv()
        ids = jnp.concatenate([ids_ref[...], ids_c[...]], axis=1) - (core * half + b * size)
        hit = (lax.broadcasted_iota(jnp.int32, (n, 2 * n_look), 0) == ids).astype(F32).astype(BF16)
        look = mm(hit, parts[0]) + mm(hit, parts[1]) + mm(hit, parts[2])
        s_buf[b, 0:n, :] = s_buf[b, 0:n, :] + from_c[b, 0:n, :] + look
        x_copy(b, n).start()

    def w_first(k):
        for zz in REDUCE_ORDER[k]:
            for slot in (2 * zz + 1 - y, 2 * zz + y):
                remote(p_ref.at[slot, 1 - core], w_c.at[slot], send_c.at[slot], recv_c.at[slot], tp, twin).start()
                pltpu.make_async_copy(p_ref.at[slot, core], acc.at[slot], w_load.at[slot]).start()

    def w_chip_sum(slot):
        pltpu.make_async_copy(p_ref.at[slot, core], acc.at[slot], w_load.at[slot]).wait()
        remote(acc.at[slot], w_c.at[slot], send_c.at[slot], recv_c.at[slot], tp, twin).wait_recv()
        add_into(acc.at[slot], w_c.at[slot])

    def w_second(k):
        for zz in REDUCE_ORDER[k]:
            slot = 2 * zz + 1 - y
            w_chip_sum(slot)
            remote(acc.at[slot], w_y.at[zz], send_y.at[zz], recv_y.at[zz], partner, dp).start()
        for zz in REDUCE_ORDER[k]:
            w_chip_sum(2 * zz + y)

    def w_reduce(k, shards):
        for zz in shards:
            line = acc.at[2 * zz + y]
            remote(line, w_y.at[zz], send_y.at[zz], recv_y.at[zz], partner, dp).wait_recv()
            add_into(line, w_y.at[zz])
            if zz >= k and k > 0:
                remote(line, w_l.at[zz - 1], send_l.at[zz], recv_l.at[zz], partner, dp).wait_recv()
                add_into(line, w_l.at[zz - 1])
            if zz <= k and k < NZ - 1:
                remote(line, w_r.at[zz], send_r.at[zz], recv_r.at[zz], partner, dp).wait_recv()
                add_into(line, w_r.at[zz])
            if zz > k:
                remote(line, w_l.at[zz - 1], send_r.at[zz], recv_l.at[zz], tp + 2, dp).start()
            if zz < k:
                remote(line, w_r.at[zz], send_l.at[zz], recv_r.at[zz], tp - 2, dp).start()

    def on_position(f):
        for k in range(NZ):
            pl.when(z == k)(functools.partial(f, k))

    def first(b, n):
        c_copy(b, n).start()
        own_load(b, n).start()

    every(first, 0, 4)
    on_position(w_first)
    every(first, 4, N_BLOCK)

    def split(at, value):
        high = value.astype(BF16)
        left = value - high.astype(F32)
        middle = left.astype(BF16)
        parts[0, at, :] = high
        parts[1, at, :] = middle
        parts[2, at, :] = (left - middle.astype(F32)).astype(BF16)

    split(pl.ds(0, n_look), rows_ref[...])
    for c in look_copies:
        c.wait()
    split(pl.ds(n_look, n_look), rows_c[...])
    every(chip_sum, 0, EARLY)
    on_position(w_second)

    total = acc.at[tp]
    w_copy_x = remote(total, w_x, last_send.at[0], last_recv.at[0], tp, facing)
    w_copy_c = remote(total, w_out.at[core], last_send.at[1], last_recv.at[1], tp, twin)
    w_store = pltpu.make_async_copy(total, w_out.at[core], w_out_sem)
    n_small, n_rows = small_ref.shape[1], w_out.shape[1]
    mine = w_out.at[1, pl.ds(n_rows - 32, n_small), :]
    small_here = pltpu.make_async_copy(mine, small_ref.at[tp], w_out_sem)
    peers = [lax.rem(tp + n, 2 * NZ) for n in range(1, 2 * NZ)]
    for b in range(N_BLOCK):
        n = last if b == N_BLOCK - 1 else size
        x_copy(b, n).wait_recv()
        add_into(part(from_x, b, n), part(s_buf, b, n), 24)
        t_copy(b, n).start()
        t_store(b, n).start()
        for k in range(NZ):
            if b in W_REDUCE[k]:
                pl.when(z == k)(functools.partial(w_reduce, k, W_REDUCE[k][b]))
        if b == 7:
            w_copy_x.start()
            every(chip_sum, EARLY, N_BLOCK)
        if b == 8:
            w_copy_x.wait()
            add_into(total, w_x)
            w_copy_c.start()
            w_store.start()
        if b == 9:
            w_copy_c.wait_send()
            remote(total, w_out.at[1 - core], last_send.at[1], last_recv.at[1], tp, twin).wait_recv()
            w_store.wait()
            for to in peers:
                remote(mine, small_ref.at[tp], small_send.at[to], small_recv.at[tp], to, dp).start()
            small_here.start()
    for source in peers:
        remote(small_ref.at[source], small_ref.at[source], small_send.at[source], small_recv.at[source], source, dp).wait_recv()
        remote(mine, small_ref.at[tp], small_send.at[source], small_recv.at[tp], source, dp).wait_send()
    small_here.wait()

    def w_done(k):
        for zz in range(NZ):
            line = acc.at[2 * zz + y]
            for slot in (2 * zz + 1 - y, 2 * zz + y):
                remote(p_ref.at[slot, 1 - core], w_c.at[slot], send_c.at[slot], recv_c.at[slot], tp, twin).wait_send()
            remote(line, w_y.at[zz], send_y.at[zz], recv_y.at[zz], partner, dp).wait_send()
            if zz > k:
                remote(line, w_l.at[zz - 1], send_r.at[zz], recv_l.at[zz], tp + 2, dp).wait_send()
            if zz < k:
                remote(line, w_r.at[zz], send_l.at[zz], recv_r.at[zz], tp - 2, dp).wait_send()

    on_position(w_done)

    def drain(b, n):
        c_copy(b, n).wait_send()
        x_copy(b, n).wait_send()
        t_copy(b, n).wait_send()
        t_store(b, n).wait()
        remote(part(from_x, b, n), t_ref.at[rows(1 - core, b, n), :], g_send_t.at[b], g_recv_t.at[b], tp, twin).wait_recv()

    every(drain, 0, N_BLOCK)


def tail(g_table, g_rows, look_rows, look_ids, collective_id):
    vocab, width = g_table.shape
    rows = g_rows.shape[1]
    half = (rows // 2, width)
    n_look = look_ids.shape[1]
    size = -(-vocab // (2 * N_BLOCK * 24)) * 24
    blocks = pltpu.VMEM((N_BLOCK, size, width), F32)
    dma = lambda *n: pltpu.SemaphoreType.DMA(n)
    t, w_sum, small = pl.pallas_call(
        tail_kernel,
        out_shape=(jax.ShapeDtypeStruct((vocab, width), F32), jax.ShapeDtypeStruct((2,) + half, F32), jax.ShapeDtypeStruct((2 * NZ, 24, width), F32)),
        in_specs=[ANY, ANY, VMEM, VMEM],
        out_specs=(ANY,) * 3,
        scratch_shapes=[blocks] * 3 + [pltpu.VMEM((n_look, width), F32), pltpu.VMEM((1, n_look), jnp.int32), pltpu.VMEM((3, 2 * n_look, width), BF16)]
        + [pltpu.VMEM((2 * NZ,) + half, F32)] * 2 + [pltpu.VMEM((NZ,) + half, F32)] + [pltpu.VMEM((NZ - 1,) + half, F32)] * 2
        + [pltpu.VMEM(half, F32)]
        + [dma(N_BLOCK)] * 8 + [dma(2)] * 2
        + [dma(2 * NZ), pltpu.SemaphoreType.DMA] + [dma(2 * NZ), dma(NZ), dma(NZ), dma(NZ)] * 2 + [dma(2)] * 2 + [dma(2 * NZ)] * 2,
        compiler_params=pltpu.CompilerParams(collective_id=collective_id, has_side_effects=True, vmem_limit_bytes=67000000),
        name="tail",
    )(g_table, g_rows.reshape((2 * NZ, 2) + half), look_rows.reshape(n_look, width), look_ids)
    return t, w_sum.reshape(rows, width), small


UPDATE_ROWS = 512


def update_kernel(t_ref, w_ref, small_ref, *refs):
    state = [refs[7 * i:7 * i + 7] for i in range(3)]
    new = [refs[21 + 7 * i:28 + 7 * i] for i in range(3)]
    loss_ref = refs[42]
    held, made, in_sem, out_sem = refs[43:]
    vocab = t_ref.shape[0]
    n_kv, hd = 2 * state[0][3].shape[1] // small_ref.shape[0], state[0][3].shape[1]
    blocks = [(at, min(UPDATE_ROWS, vocab - at)) for at in range(0, vocab, UPDATE_ROWS)]

    def loads(q):
        at, n = blocks[q]
        return [pltpu.make_async_copy(ref.at[pl.ds(at, n), :], held.at[q % 3, i, pl.ds(0, n), :], in_sem.at[q % 3, i])
                for i, ref in enumerate((t_ref, state[0][0], state[1][0], state[2][0]))]

    def stores(q):
        at, n = blocks[q]
        return [pltpu.make_async_copy(made.at[q % 2, i, pl.ds(0, n), :], new[i][0].at[pl.ds(at, n), :], out_sem.at[q % 2, i]) for i in range(3)]

    for q in range(3):
        for c in loads(q):
            c.start()

    def small_update(index, grad, *where):
        got = adam_update(state[0][index][where], grad, state[1][index][where], state[2][index][where])
        for i in range(3):
            new[i][index][where] = got[i]

    n_q, n_f = state[0][2].shape[0], state[0][6].shape[0]
    small_update(1, small_ref[0, n_kv:n_kv + 2, :], Ellipsis)
    small_update(2, w_ref[0:n_q, :], Ellipsis)
    kv = small_ref[:, 0:n_kv, :].reshape(2 * hd, small_ref.shape[2])
    for i in range(2):
        small_update(3, kv[i * hd:(i + 1) * hd], i)
    small_update(4, w_ref[n_q:2 * n_q, :], Ellipsis)
    for i in range(2):
        small_update(5, w_ref[2 * n_q + i * n_f:2 * n_q + (i + 1) * n_f, :].T, i)
    small_update(6, w_ref[2 * n_q + 2 * n_f:2 * n_q + 3 * n_f, :], Ellipsis)
    loss_ref[...] = jnp.sum(small_ref[0, n_kv + 2:n_kv + 3, :], axis=1, keepdims=True)

    for q, (at, n) in enumerate(blocks):
        for c in loads(q):
            c.wait()
        if q >= 2:
            for c in stores(q - 2):
                c.wait()
        step = 32 if n % 32 == 0 else 16

        def body(j, carry):
            rows = pl.ds(pl.multiple_of(j * step, step), step)
            got = adam_update(held[q % 3, 1, rows, :], held[q % 3, 0, rows, :], held[q % 3, 2, rows, :], held[q % 3, 3, rows, :])
            for i in range(3):
                made[q % 2, i, rows, :] = got[i]
            return carry

        lax.fori_loop(0, n // step, body, 0)
        for c in stores(q):
            c.start()
        if q + 3 < len(blocks):
            for c in loads(q + 3):
                c.start()
    for q in range(len(blocks) - 2, len(blocks)):
        for c in stores(q):
            c.wait()


def update(g_table, g_shard, g_small, state_arrays):
    specs = [ANY] + [VMEM] * 6
    width = g_table.shape[1]

    def flip(arrays):
        return [a.swapaxes(-1, -2) if i % 7 in (2, 3) else a for i, a in enumerate(arrays)]

    given = flip(state_arrays)
    *new, loss = pl.pallas_call(
        update_kernel,
        out_shape=tuple(jax.ShapeDtypeStruct(a.shape, F32) for a in given) + (jax.ShapeDtypeStruct((1, 1), F32),),
        in_specs=[ANY, VMEM, VMEM] + specs * 3,
        out_specs=tuple(specs * 3) + (VMEM,),
        scratch_shapes=[pltpu.VMEM((3, 4, UPDATE_ROWS, width), F32), pltpu.VMEM((2, 3, UPDATE_ROWS, width), F32),
                        pltpu.SemaphoreType.DMA((3, 4)), pltpu.SemaphoreType.DMA((2, 3))],
        compiler_params=pltpu.CompilerParams(vmem_limit_bytes=60000000),
        name="update",
    )(g_table, g_shard, g_small, *given)
    return flip(new) + [loss]


def norm_fwd(x_f32, scale):
    centered = x_f32 - jnp.mean(x_f32, axis=-1, keepdims=True)
    inv_std = lax.rsqrt(jnp.mean(centered * centered, axis=-1, keepdims=True) + LN_EPS)
    x_hat = centered * inv_std
    return (x_hat * scale).astype(BF16), x_hat, inv_std


def norm_bwd(d_out, x_hat, inv_std, scale):
    d_scale = jnp.sum(d_out * x_hat, axis=0)
    d_hat = d_out * scale
    d_in = inv_std * (d_hat - jnp.mean(d_hat, axis=-1, keepdims=True) - x_hat * jnp.mean(d_hat * x_hat, axis=-1, keepdims=True))
    return d_in, d_scale


def adam_update(param_in, grad_in, mom_in, vel_in):
    mom_new = BETA_ONE * mom_in + (1.0 - BETA_ONE) * grad_in
    vel_new = BETA_TWO * vel_in + (1.0 - BETA_TWO) * grad_in * grad_in
    return param_in - LEARN_RATE * mom_new / (jnp.sqrt(vel_new) + ADAM_EPS), mom_new, vel_new


def dot(spec, a, b):
    return jnp.einsum(spec, a, b, preferred_element_type=F32)


def solution(mesh):
    param_specs = (P('tp', None), P(None, None), P(None, 'tp'), P(None, None, None), P('tp', None), P(None, None, 'tp'), P('tp', None))
    n_tp = mesh.shape['tp']
    n_dp = mesh.shape['dp']

    def local_step(tokens, labels, *state_arrays):
        embed, ln_scales, w_q, w_kv, w_o, w_gu, w_down = state_arrays[0:7]
        batch_loc, seq_len = tokens.shape
        vocab_loc, d_model = embed.shape
        head_dim = w_kv.shape[2]
        q_loc = w_q.shape[1]
        f_loc = w_down.shape[0]
        tok_loc = batch_loc * seq_len
        tok_total = tok_loc * n_dp
        own = tok_loc // n_tp
        tp_rank = lax.axis_index('tp')
        half = tp_rank % 2

        strict = (jnp.arange(own)[:, None] > jnp.arange(own)[None, :]).astype(BF16)

        def routing(chunks):
            shard = chunks // vocab_loc
            row = chunks - shard * vocab_loc
            hot = (shard[:, :, None] == jnp.arange(n_tp)[None, None, :])
            before = dot('rs,nsj->nrj', strict, hot.astype(BF16))
            rank = jnp.sum(jnp.where(hot, before, 0.0), axis=-1).astype(jnp.int32)
            most = jnp.max(jnp.sum(hot.astype(jnp.int32), axis=1))
            return shard, row, rank, (most + CAP - 1) // CAP

        chunks = tokens.reshape(n_tp, own)
        shard, row, rank, rounds = routing(chunks)
        slots = jnp.arange(CAP)
        my_shard = lax.dynamic_index_in_dim(shard, tp_rank, 0, keepdims=False)
        my_rank = lax.dynamic_index_in_dim(rank, tp_rank, 0, keepdims=False)

        def fetch(step):
            here = (shard[:, None, :] == tp_rank) & (rank[:, None, :] == slots[None, :, None] + step * CAP)
            ids = jnp.sum(jnp.where(here, row[:, None, :], 0), axis=-1).reshape(-1)
            pick = (my_shard[:, None, None] == jnp.arange(n_tp)[None, :, None]) & (my_rank[:, None, None] == slots[None, None, :] + step * CAP)
            return ids, pick.reshape(own, n_tp * CAP).astype(BF16)

        def fetch_more(state):
            ids, pick = fetch(state[0])
            rows_in = plane_swap(jnp.take(embed, ids, axis=0).reshape(n_tp, CAP, d_model), 1).reshape(n_tp * CAP, d_model).astype(BF16)
            return state[0] + 1, state[1] + dot('rc,cd->rd', pick, rows_in)

        more_rows = lax.while_loop(lambda state: state[0] < rounds, fetch_more, (jnp.int32(1), jnp.zeros((own, d_model), F32)))[1]
        ids_first, pick_first = fetch(0)

        w_rows = jnp.concatenate([w_q.T, w_o, w_gu.transpose(0, 2, 1).reshape(2 * f_loc, d_model), w_down], axis=0)
        cuts = (q_loc, 2 * q_loc, 2 * q_loc + f_loc, 2 * q_loc + 2 * f_loc)
        wkv_t = w_kv.transpose(0, 2, 1).reshape(2 * head_dim, d_model).astype(BF16)
        inv_freq = ROPE_BASE ** (-jnp.arange(0, head_dim, 2).astype(F32) / head_dim)
        angles = inv_freq[:, None] * (half * own + jnp.arange(own)).astype(F32)[None, :]
        cos_t, sin_t = jnp.cos(angles), jnp.sin(angles)
        f_own, x_one, x_zero, *saved = front(ids_first, embed, pick_first, more_rows, w_rows, wkv_t, ln_scales, cos_t, sin_t, n_tp * q_loc, 0)
        saved, (wq_t, wo_b, wg_t, wu_t, wd_b) = saved[:5], saved[5:]
        weights = (wq_t, wkv_t, wo_b, wg_t, wu_t, wd_b)

        logit_scale = d_model ** -0.5
        lab_loc = labels.reshape(n_tp, own) - tp_rank * vocab_loc
        d_fin, g_head_part, log_norm, lab_sum = head(f_own, lab_loc, embed, logit_scale, logit_scale / tok_total, 4)
        log_norm = lax.dynamic_index_in_dim(log_norm, tp_rank, 0, keepdims=False)
        loss_row = (log_norm + LOGIT_ZLOSS * log_norm * log_norm - jnp.sum(lab_sum, axis=0) * logit_scale) / tok_total
        g_rows, d_zero, rows_back = layer_bwd(d_fin, x_zero, x_one, loss_row[None, :], ln_scales, cos_t, sin_t, weights, saved, pick_first, 7)

        def row_ids(step):
            here = (shard[:, None, :] == tp_rank) & (rank[:, None, :] == slots[None, :, None] + step * CAP)
            return jnp.where(jnp.any(here, axis=-1), jnp.sum(jnp.where(here, row[:, None, :], 0), axis=-1), vocab_loc).reshape(-1)

        def give_back(state):
            mine = (my_shard[None, None, :] == jnp.arange(n_tp)[:, None, None]) & (my_rank[None, None, :] == slots[None, :, None] + state[0] * CAP)
            ids = jnp.sum(jnp.where(mine, jnp.arange(own)[None, None, :], 0), axis=-1).reshape(-1)
            rows_in = plane_swap(jnp.take(d_zero, ids, axis=0).reshape(n_tp, CAP, d_model), 9).reshape(-1, d_model)
            return state[0] + 1, state[1].at[row_ids(state[0])].add(rows_in, mode='drop')

        g_table = lax.while_loop(lambda state: state[0] < rounds, give_back, (jnp.int32(1), g_head_part))[1]
        g_table, g_shard, g_small = tail(g_table, g_rows, rows_back, row_ids(0)[None, :], 10)
        *new, loss = update(g_table, g_shard, g_small, state_arrays)
        return tuple(new) + (loss.reshape(()),)

    return jax.shard_map(local_step, mesh=mesh, in_specs=(P('dp', None), P('dp', None)) + param_specs * 3,
                         out_specs=param_specs * 3 + (P(),), check_vma=False)
```

```python
import functools

import jax
import jax.numpy as jnp
from jax import lax
from jax.experimental import pallas as pl
from jax.experimental.pallas import tpu as pltpu
from jax.sharding import PartitionSpec as P

LN_EPS = 1e-5
LOGIT_ZLOSS = 1e-4
LEARN_RATE = 1e-2
BETA_ONE = 0.9
BETA_TWO = 0.95
ADAM_EPS = 1e-8
ROPE_BASE = 10000.0
NZ = 4
CAP = 96
F32 = jnp.float32
BF16 = jnp.bfloat16
ANY = pl.BlockSpec(memory_space=pl.ANY)
VMEM = pl.BlockSpec(memory_space=pltpu.VMEM)

ARRIVALS = {
    0: (("R", 1), ("R", 2), ("R", 3)),
    1: (("L", 0), ("R", 2), ("R", 3)),
    2: (("R", 3), ("L", 1), ("L", 0)),
    3: (("L", 2), ("L", 1), ("L", 0)),
}
REDUCE_ORDER = {0: (3, 2, 1, 0), 1: (3, 0, 2, 1), 2: (0, 3, 1, 2), 3: (0, 1, 2, 3)}


def remote(src, dst, send_sem, recv_sem, tp, dp):
    return pltpu.make_async_remote_copy(src_ref=src, dst_ref=dst, send_sem=send_sem, recv_sem=recv_sem,
                                        device_id=(tp, dp), device_id_type=pl.DeviceIdType.MESH)


def place():
    tp = lax.axis_index("tp")
    dp = lax.axis_index("dp")
    return tp, dp, tp // 2, tp % 2


def signal(tp, dp):
    pl.semaphore_signal(pltpu.get_barrier_semaphore(), inc=1, device_id=(tp, dp), device_id_type=pl.DeviceIdType.MESH)


def add_into(acc, other, step=None):
    rows = acc.shape[0]
    step = step or (64 if rows % 64 == 0 else 8)

    def body(n, carry):
        at = pl.ds(pl.multiple_of(n * step, step), step)
        acc[at, :] = acc[at, :] + other[at, :]
        return carry

    lax.fori_loop(0, rows // step, body, 0)


def plane_barrier(tp, dp, others):
    peers = [(lax.rem(tp + n, 2 * NZ), dp) for n in range(1, 2 * NZ)] + others
    for peer in peers:
        signal(*peer)
    pl.semaphore_wait(pltpu.get_barrier_semaphore(), len(peers))


def swap_kernel(x_ref, out_ref, own_sem, send, recv):
    tp, dp, _, _ = place()
    plane_barrier(tp, dp, [])
    copies = []
    for n in range(1, 2 * NZ):
        to = lax.rem(tp + n, 2 * NZ)
        copy = remote(x_ref.at[to], out_ref.at[tp], send.at[to], recv.at[tp], to, dp)
        copy.start()
        copies.append(copy)
    own = pltpu.make_async_copy(x_ref.at[tp], out_ref.at[tp], own_sem)
    own.start()
    for n in range(1, 2 * NZ):
        source = lax.rem(tp + n, 2 * NZ)
        remote(out_ref.at[source], out_ref.at[source], send.at[source], recv.at[source], source, dp).wait_recv()
    own.wait()
    for copy in copies:
        copy.wait_send()


def plane_swap(x, collective_id):
    return pl.pallas_call(
        swap_kernel,
        out_shape=jax.ShapeDtypeStruct(x.shape, x.dtype),
        in_specs=[ANY],
        out_specs=ANY,
        scratch_shapes=[pltpu.SemaphoreType.DMA] + [pltpu.SemaphoreType.DMA((2 * NZ,))] * 2,
        compiler_params=pltpu.CompilerParams(collective_id=collective_id, has_side_effects=True),
        name="plane_swap",
    )(x)


GATHER_ORDER = ((0, 0), (0, -1), (0, 1), (1, 0), (1, -1), (1, 1), (0, 2), (1, 2))
GATHER_EVENTS = {
    0: ((1, 0, 2, "lr"), (0, -1, 0, "ry"), (0, 1, 0, "y")),
    1: ((1, 0, 3, "lr"), (0, -1, 1, "y"), (0, 1, 1, "ly"), (0, -1, 2, "r"), (0, 1, 2, ""), (0, 1, 3, "l"), (0, -1, 3, "")),
    3: ((1, -1, 2, "r"), (1, 0, 0, ""), (1, 0, 1, "")),
    4: ((0, 2, 0, "y"), (0, 2, 1, "y"), (1, 1, 3, "l"), (1, -1, 0, ""), (1, -1, 1, ""), (1, -1, 3, "")),
    5: ((1, 1, 0, ""), (1, 1, 1, ""), (1, 1, 2, "")),
    6: ((0, 2, 2, ""), (0, 2, 3, "")),
    7: ((1, 2, 0, ""), (1, 2, 1, ""), (1, 2, 2, ""), (1, 2, 3, "")),
}
SCATTER_ORDER = ((1, 2), (1, -1), (1, 1), (0, 2), (1, 0), (0, -1), (0, 1), (0, 0))
SUB = 256
GROUP = 6


def lookup(table, z, step):
    value = jnp.int32(0)
    for k in range(NZ):
        for s in range(2 * NZ):
            value = value + jnp.where((z == k) & (step == s), table[k][s], 0)
    return value


def head_kernel(scale, token_scale, f_ref, lab_ref, e_ref, dfin_ref, ghead_ref, norm_ref, labsum_ref,
                e_b, e_t, fbuf, f_b, g_acc, from_y, from_l, from_r, dl, lse_all, load_sem, ag_send, ag_recv,
                send_y, send_l, send_r, recv_y, recv_l, recv_r, st_send, st_recv):
    tp, dp, z, y = place()
    partner = tp + 1 - 2 * y
    left = 2 * lax.rem(z + NZ - 1, NZ) + y
    right = 2 * lax.rem(z + 1, NZ) + y
    vocab, width = e_ref.shape
    own = f_ref.shape[0]
    quarter = own // 4
    whole = vocab // (SUB * GROUP)
    rest = vocab - whole * SUB * GROUP
    slope = scale * LOG2E
    blocks = [(j * SUB, SUB) for j in range(GROUP)]
    tail_blocks = [(n, min(SUB, rest - n)) for n in range(0, rest, SUB)]

    plane_barrier(tp, dp, [])

    def slot_of(o, d):
        return 2 * lax.rem(z + d + NZ, NZ) + y + o - 2 * y * o

    def slot_at(order, step):
        o = jnp.int32(0)
        d = jnp.int32(0)
        for s in range(2 * NZ):
            o = o + jnp.where(step == s, order[s][0], 0)
            d = d + jnp.where(step == s, order[s][1], 0)
        return slot_of(o, d)

    def piece(ref, q):
        return ref.at[pl.ds(q * quarter, quarter), :]

    def pass_on(o, d, q, to):
        slot = slot_of(o, d)
        src = piece(f_ref if (o, d) == (0, 0) else fbuf.at[slot], q)
        return remote(src, piece(fbuf.at[slot], q), ag_send.at["lry".index(to), slot, q], ag_recv.at[slot, q],
                      {"l": left, "r": right, "y": partner}[to], dp)

    def arrived(o, d, q):
        slot = slot_of(o, d)
        remote(piece(f_ref, q), piece(fbuf.at[slot], q), ag_send.at[0, slot, q], ag_recv.at[slot, q], partner, dp).wait_recv()

    for q in range(4):
        pass_on(0, 0, q, "l").start()
        pass_on(0, 0, q, "r").start()
        pass_on(0, 0, (q + 2) % 4, "y").start()
    load = pltpu.make_async_copy(e_ref, g_acc, load_sem.at[0])
    load.start()
    own_copy = pltpu.make_async_copy(f_ref, fbuf.at[tp], load_sem.at[1])
    own_copy.start()
    load.wait()

    def prepare(at, size):
        part = g_acc[at, :]
        e_b[at, :] = part.astype(BF16)
        e_t[:, at] = part.T.astype(BF16)

    def prepare_body(n, carry):
        prepare(pl.ds(pl.multiple_of(n * SUB, SUB), SUB), SUB)
        return carry

    lax.fori_loop(0, vocab // SUB, prepare_body, 0)
    if vocab % SUB:
        prepare(pl.ds(vocab // SUB * SUB, vocab % SUB), vocab % SUB)
    own_copy.wait()

    def over_blocks(group, carry):
        def body(n, c):
            return group(pl.multiple_of(n * SUB * GROUP, SUB * GROUP), blocks, c)
        carry = lax.fori_loop(0, whole, body, carry)
        return group(whole * SUB * GROUP, tail_blocks, carry) if tail_blocks else carry

    def gather_step(step, carry):
        for s, events in GATHER_EVENTS.items():
            def serve(events=events):
                for o, d, q, to in events:
                    arrived(o, d, q)
                    for t in to:
                        pass_on(o, d, q, t).start()
            pl.when(step == s)(serve)
        slot = slot_at(GATHER_ORDER, step)
        f_b[slot] = fbuf[slot].astype(BF16)
        f_now = f_b[slot]

        def group(base, parts, c):
            top, total = c
            for first, size in parts:
                logit = lax.dot_general(e_b[pl.ds(base + first, size), :], f_now, (((1,), (1,)), ((), ())), preferred_element_type=F32)
                logit = logit.reshape(size // 8, 8, own)
                new = jnp.maximum(top, jnp.max(logit, axis=0))
                total = total * jnp.exp2((top - new) * slope) + jnp.sum(jnp.exp2((logit - new[None]) * slope), axis=0)
                top = new
            return top, total

        top, total = over_blocks(group, (jnp.full((8, own), -3e38, F32), jnp.zeros((8, own), F32)))
        most = jnp.max(top, axis=0, keepdims=True)
        total = jnp.sum(total * jnp.exp2((top - most) * slope), axis=0, keepdims=True)
        lse_all[tp, pl.ds(slot, 1), :] = most * scale + jnp.log(total)
        return carry

    lax.fori_loop(0, 2 * NZ, gather_step, 0)

    for n in range(1, 2 * NZ):
        to = lax.rem(tp + n, 2 * NZ)
        remote(lse_all.at[tp], lse_all.at[tp], st_send.at[to], st_recv.at[tp], to, dp).start()
    for q in range(4):
        for to in "lry":
            pass_on(0, 0, q, to).wait_send()
    for events in GATHER_EVENTS.values():
        for o, d, q, to in events:
            for t in to:
                pass_on(o, d, q, t).wait_send()

    def clear(n, carry):
        g_acc[pl.ds(pl.multiple_of(n * 16, 16), 16), :] = jnp.zeros((16, width), F32)
        return carry

    lax.fori_loop(0, vocab // 16, clear, 0)
    for n in range(1, 2 * NZ):
        source = lax.rem(tp + n, 2 * NZ)
        remote(lse_all.at[source], lse_all.at[source], st_send.at[source], st_recv.at[source], source, dp).wait_recv()
    peak = jnp.max(lse_all[...], axis=0)
    log_norm = peak + jnp.log(jnp.sum(jnp.exp(lse_all[...] - peak[None]), axis=0))
    norm_ref[...] = log_norm

    def part(o, d, q):
        return piece(fbuf.at[slot_of(o, d)], q)

    def to_y(d, q):
        return remote(part(1, d, q), from_y.at[d % 4, q], send_y.at[d % 4, q], recv_y.at[d % 4, q], partner, dp)

    def to_left(o, d, q):
        rel = 1 if d == 2 else 0
        return remote(part(o, d, q), from_r.at[o, rel, q], send_l.at[o, rel, q], recv_r.at[o, rel, q], left, dp)

    def to_right(o, d, q):
        rel = 1 if d == 2 else 0
        return remote(part(o, d, q), from_l.at[o, rel, q], send_r.at[o, rel, q], recv_l.at[o, rel, q], right, dp)

    def add(o, d, q, buf, sem):
        remote(part(o, d, q), buf, send_y.at[0, 0], sem, partner, dp).wait_recv()
        add_into(part(o, d, q), buf)

    def add_y(d, q):
        add(0, d, q, from_y.at[d % 4, q], recv_y.at[d % 4, q])

    def add_r(o, rel, q):
        add(o, -rel, q, from_r.at[o, rel, q], recv_r.at[o, rel, q])

    def add_l(o, rel, q):
        add(o, rel, q, from_l.at[o, rel, q], recv_l.at[o, rel, q])

    def needs(o, d):
        if (o, d) == (0, 2):
            return [(add_y, 2, 0), (add_y, 2, 1)]
        if d == -1:
            return ([(add_y, -1, 0), (add_y, -1, 1), (add_r, 0, 1, 0)] if o == 0 else []) + [(add_r, o, 1, 2)]
        if d == 1:
            return ([(add_y, 1, 0), (add_y, 1, 1), (add_l, 0, 1, 1)] if o == 0 else []) + [(add_l, o, 1, 3)]
        if (o, d) == (1, 0):
            return [(f, 1, 0, q) for q in (2, 3) for f in (add_r, add_l)]
        if (o, d) == (0, 0):
            return [(add_y, 0, q) for q in range(4)] + [(f, 0, 0, q) for f in (add_r, add_l) for q in range(4)]
        return []

    def leaves(o, d):
        if d == 2:
            first = [to_y(2, 0), to_y(2, 1)] if o == 1 else [to_left(0, 2, 0), to_right(0, 2, 1)]
            return first + [to_left(o, 2, 2), to_right(o, 2, 3)]
        if d in (-1, 1):
            along = to_left if d == -1 else to_right
            return [to_y(d, 0), to_y(d, 1)] + [along(1, d, 2), along(1, d, 3)] if o == 1 else [along(0, d, q) for q in range(4)]
        return [to_y(0, q) for q in range(4)] if o == 1 else []

    def scatter_step(step, lab_sum):
        slot = slot_at(SCATTER_ORDER, step)
        f_now = f_b[slot]
        acc = fbuf.at[slot]
        norm = norm_ref[pl.ds(slot, 1), :]
        shift = norm * LOG2E
        coef = (1.0 + 2.0 * LOGIT_ZLOSS * norm) * token_scale
        lab = lab_ref[pl.ds(slot, 1), :]
        acc[...] = jnp.zeros((width, own), F32)

        def group(base, parts, hits):
            for first, size in parts:
                at = pl.ds(base + first, size)
                logit = lax.dot_general(e_b[at, :], f_now, (((1,), (1,)), ((), ())), preferred_element_type=F32)
                hit = lax.broadcasted_iota(jnp.int32, (size, own), 0) == lab - (base + first)
                prob = jnp.exp2(logit * slope - shift) * coef
                grad = jnp.where(hit, prob - token_scale, prob).astype(BF16)
                hits = hits + jnp.sum(jnp.where(hit, logit, 0.0).reshape(size // 8, 8, own), axis=0)
                dl[pl.ds(first, size), :] = grad
                g_acc[at, :] += jnp.dot(grad, f_now, preferred_element_type=F32)
            size = parts[-1][0] + parts[-1][1]
            acc[...] += jnp.dot(e_t[:, pl.ds(base, size)], dl[pl.ds(0, size), :], preferred_element_type=F32)
            return hits

        lab_sum = over_blocks(group, lab_sum)
        for s, (o, d) in enumerate(SCATTER_ORDER):
            def reduce(o=o, d=d):
                for f, *args in needs(o, d):
                    f(*args)
                for c in leaves(o, d):
                    c.start()
            pl.when(step == s)(reduce)
        return lab_sum

    lab_sum = lax.fori_loop(0, 2 * NZ, scatter_step, jnp.zeros((8, own), F32))
    labsum_ref[...] = lab_sum
    store = pltpu.make_async_copy(g_acc, ghead_ref, load_sem.at[0])
    store.start()
    dfin_ref[...] = fbuf[tp].T
    for o, d in SCATTER_ORDER:
        for c in leaves(o, d):
            c.wait_send()
    for n in range(1, 2 * NZ):
        to = lax.rem(tp + n, 2 * NZ)
        remote(lse_all.at[tp], lse_all.at[tp], st_send.at[to], st_recv.at[tp], to, dp).wait_send()
    store.wait()


def head(f_own, labels, embed, scale, token_scale, collective_id):
    own, width = f_own.shape
    vocab = embed.shape[0]
    chunk = (own, width)
    strip = (own // 4, width)
    dma = lambda *n: pltpu.SemaphoreType.DMA(n)
    return pl.pallas_call(
        functools.partial(head_kernel, scale, token_scale),
        out_shape=(jax.ShapeDtypeStruct((own, width), F32), jax.ShapeDtypeStruct((vocab, width), F32),
                   jax.ShapeDtypeStruct((2 * NZ, own), F32), jax.ShapeDtypeStruct((8, own), F32)),
        in_specs=[VMEM, VMEM, ANY],
        out_specs=(VMEM, ANY, VMEM, VMEM),
        scratch_shapes=[pltpu.VMEM((vocab, width), BF16), pltpu.VMEM((width, vocab), BF16),
                        pltpu.VMEM((2 * NZ,) + chunk, F32), pltpu.VMEM((2 * NZ,) + chunk, BF16), pltpu.VMEM((vocab, width), F32),
                        pltpu.VMEM((NZ, 4) + strip, F32), pltpu.VMEM((2, 2, 4) + strip, F32), pltpu.VMEM((2, 2, 4) + strip, F32),
                        pltpu.VMEM((SUB * GROUP, own), BF16), pltpu.VMEM((2 * NZ, 2 * NZ, own), F32),
                        dma(2), dma(3, 2 * NZ, 4), dma(2 * NZ, 4), dma(NZ, 4), dma(2, 2, 4), dma(2, 2, 4), dma(NZ, 4), dma(2, 2, 4), dma(2, 2, 4),
                        dma(2 * NZ), dma(2 * NZ)],
        compiler_params=pltpu.CompilerParams(collective_id=collective_id, has_side_effects=True, vmem_limit_bytes=67000000),
        cost_estimate=pl.CostEstimate(flops=8 * vocab * width * own * 8, bytes_accessed=3 * 4 * vocab * width, transcendentals=2 * vocab * own * 8),
        name="head",
    )(f_own, labels, embed)


TB = (((1,), (1,)), ((), ()))
TA = (((0,), (0,)), ((), ()))
LOG2E = 1.4426950408889634


def mm(a, b, dims=(((1,), (0,)), ((), ()))):
    return lax.dot_general(a, b, dims, preferred_element_type=F32)


def turn(lo, hi, cos_t, sin_t):
    return lo * cos_t - hi * sin_t, hi * cos_t + lo * sin_t


EVENTS = {
    0: (((("R", 1),), (0,)), ((("R", 2),), (1,)), ((("R", 3),), (2,)), ((), (3,))),
    1: (((("L", 0), ("R", 2)), (1,)), ((("R", 3),), (0,)), ((), (2,)), ((), (3,))),
    2: (((("R", 3), ("L", 1)), (2,)), ((("L", 0),), (3,)), ((), (1,)), ((), (0,))),
    3: (((("L", 2),), (3,)), ((("L", 1),), (2,)), ((("L", 0),), (1,)), ((), (0,))),
}
MLP_ORDER = {k: [2 * k] + [code for line, other in EVENTS[k] for code in [2 * zz for _, zz in line] + [2 * zz + 1 for zz in other]] for k in range(NZ)}


def front_kernel(ids_ref, e_ref, pick_ref, extra_ref, w_ref, wkv_ref, ln_ref, cos_ref, sin_ref,
                 f_ref, x1_ref, x0_ref, q_ref, kv_ref, kvt_ref, lse_ref, ctx_ref, wq_ref, wo_ref, wg_ref, wu_ref, wd_ref,
                 table, rows_ref, wl, rows_in, u_b, kv_out, kv_in, own_sem, r_send, r_recv, a_y, a_l, a_r, a_c, a_recv,
                 b_y, b_l, b_r, b_x, b_c, b_recv, kv_send, kv_recv):
    tp, dp, z, y = place()
    partner = tp + 1 - 2 * y
    core = dp % 2
    twin = dp + 1 - 2 * core
    facing = lax.rem(dp + 2, 4)
    own, width = x0_ref.shape
    shards, w_rows = wl.shape[0], wl.shape[1]
    nq = q_ref.shape[0]
    ff = wg_ref.shape[0]
    n_a = nq // shards
    n_f = ff // shards
    n_b = 3 * n_f // 4
    hd = kv_out.shape[0] // 2
    quarter = hd // 2
    heads = nq // hd

    def a_rows(c):
        return pl.ds(pl.multiple_of(c * n_a, 8), n_a)

    def b_rows(d):
        return pl.ds(pl.multiple_of(2 * n_a + d * n_b, 8), n_b)

    def a_copy(slot, sems, to, to_dp, first=False):
        src = w_ref.at[a_rows(core), :] if first else wl.at[slot, a_rows(core), :]
        return remote(src, wl.at[slot, a_rows(core), :], sems.at[slot], a_recv.at[slot, core], to, to_dp)

    def b_copy(slot, piece, sems, to, to_dp, first=False):
        src = w_ref.at[b_rows(piece), :] if first else wl.at[slot, b_rows(piece), :]
        return remote(src, wl.at[slot, b_rows(piece), :], sems.at[slot], b_recv.at[slot, piece], to, to_dp)

    def a_wait(slot, c):
        remote(w_ref.at[a_rows(c), :], wl.at[slot, a_rows(c), :], a_y.at[slot], a_recv.at[slot, c], partner, dp).wait_recv()

    def b_wait(slot, piece):
        remote(w_ref.at[b_rows(piece), :], wl.at[slot, b_rows(piece), :], b_y.at[slot], b_recv.at[slot, piece], partner, dp).wait_recv()

    def on_position(f):
        for k in range(NZ):
            pl.when(z == k)(functools.partial(f, k))

    def line_sends(k, make, y_sems, l_sems, r_sems, slot, side, first=False):
        sends = [make(slot, y_sems, partner, dp, first)]
        if k > 0 and side != "L":
            sends.append(make(slot, l_sems, tp - 2, dp, first))
        if k < NZ - 1 and side != "R":
            sends.append(make(slot, r_sems, tp + 2, dp, first))
        return sends

    def b_own(slot, sems, to, to_dp, first=False):
        return b_copy(slot, dp, sems, to, to_dp, first)

    def a_sends(k, slot, side, first=False):
        return line_sends(k, a_copy, a_y, a_l, a_r, slot, side, first)

    def b_sends(k, slot, side, first=False):
        return line_sends(k, b_own, b_y, b_l, b_r, slot, side, first)

    def start(copies):
        for c in copies:
            c.start()

    load = pltpu.make_async_copy(e_ref, table, own_sem.at[2])
    load.start()
    plane_barrier(tp, dp, [(tp, twin), (tp, facing)])
    peers = [lax.rem(tp + n, shards) for n in range(1, shards)]

    def row_copy(to):
        return remote(rows_ref.at[to], rows_in.at[tp], r_send.at[to], r_recv.at[tp], to, dp)

    on_position(lambda k: start(b_sends(k, tp, "", True)))
    on_position(lambda k: start(a_sends(k, tp, "", True)))
    own_w = pltpu.make_async_copy(w_ref, wl.at[tp], own_sem.at[1])
    own_w.start()

    def a_event(t, k):
        line, other = EVENTS[k][t]
        for side, zz in line:
            slot = 2 * zz + y
            a_wait(slot, core)
            start(a_sends(k, slot, side))
            a_copy(slot, a_c, tp, twin).start()
        for zz in other:
            slot = 2 * zz + 1 - y
            a_wait(slot, core)
            a_copy(slot, a_c, tp, twin).start()

    def b_event(t, k):
        line, other = EVENTS[k][t]
        for side, zz in line:
            slot = 2 * zz + y
            b_wait(slot, dp)
            start(b_sends(k, slot, side))
            b_copy(slot, dp, b_x, tp, facing).start()
            b_copy(slot, dp, b_c.at[0], tp, twin).start()
        for zz in other:
            slot = 2 * zz + 1 - y
            b_wait(slot, dp)
            b_copy(slot, dp, b_x, tp, facing).start()
            b_copy(slot, dp, b_c.at[0], tp, twin).start()

    load.wait()
    cap = rows_ref.shape[1]

    def pick_rows(n, carry):
        for i in range(8):
            rows_ref[n // (cap // 8), pl.ds(lax.rem(n, cap // 8) * 8 + i, 1), :] = table[pl.ds(ids_ref[n * 8 + i], 1), :]
        return carry

    lax.fori_loop(0, shards * cap // 8, pick_rows, 0)
    on_position(functools.partial(b_event, 0))
    on_position(functools.partial(a_event, 0))
    start([row_copy(to) for to in peers])
    own_rows = pltpu.make_async_copy(rows_ref.at[tp], rows_in.at[tp], own_sem.at[0])
    own_rows.start()
    on_position(functools.partial(b_event, 1))
    on_position(functools.partial(a_event, 1))
    own_rows.wait()
    for source in peers:
        remote(rows_ref.at[source], rows_in.at[source], r_send.at[source], r_recv.at[source], source, dp).wait_recv()
    x0_ref[...] = extra_ref[...] + mm(pick_ref[...], rows_in[...].reshape(pick_ref.shape[1], width).astype(BF16))
    u_b[...] = norm_fwd(x0_ref[...], ln_ref[0:1, :])[0]
    x1_ref[...] = x0_ref[...]
    cos_t = cos_ref[...]
    sin_t = sin_ref[...]
    kv = mm(wkv_ref[...], u_b[...], TB)
    lo, hi = turn(kv[:quarter], kv[quarter:hd], cos_t, sin_t)
    kv_out[0:quarter, :] = lo
    kv_out[quarter:hd, :] = hi
    kv_out[hd:, :] = kv[hd:]
    kv_copy = remote(kv_out, kv_in, kv_send, kv_recv, partner, dp)
    kv_copy.start()

    def slot_of(step):
        code = lookup(MLP_ORDER, z, step)
        other = code % 2
        return code // 2 * 2 + y + other - 2 * y * other

    def mlp(step, carry):
        def pass_on():
            slot = slot_of(step + 1)
            b_wait(slot, facing)
            b_copy(slot, facing, b_c.at[1], tp, twin).start()
        pl.when(step < shards - 1)(pass_on)
        slot = slot_of(step)

        def rest():
            b_wait(slot, twin)
            b_wait(slot, lax.rem(twin + 2, 4))
        pl.when(step > 0)(rest)
        at = pl.ds(pl.multiple_of(slot * n_f, n_f), n_f)
        wg_ref[at, :] = wl[slot, 2 * n_a:2 * n_a + n_f, :].astype(BF16)
        wu_ref[at, :] = wl[slot, 2 * n_a + n_f:2 * n_a + 2 * n_f, :].astype(BF16)
        wd_ref[at, :] = wl[slot, 2 * n_a + 2 * n_f:2 * n_a + 3 * n_f, :].astype(BF16)
        gate = mm(u_b[...], wg_ref[at, :], TB)
        up = mm(u_b[...], wu_ref[at, :], TB)
        x1_ref[...] += mm((gate * jax.nn.sigmoid(gate) * up).astype(BF16), wd_ref[at, :])
        return carry

    own_w.wait()
    lax.fori_loop(0, 3, mlp, 0)
    on_position(functools.partial(b_event, 2))
    on_position(functools.partial(a_event, 2))
    lax.fori_loop(3, 4, mlp, 0)
    on_position(functools.partial(a_event, 3))
    on_position(functools.partial(b_event, 3))
    for source in peers:
        a_wait(source, 1 - core)
    for s in range(shards):
        wq_ref[s * n_a:(s + 1) * n_a, :] = wl[s, 0:n_a, :].astype(BF16)
        wo_ref[s * n_a:(s + 1) * n_a, :] = wl[s, n_a:2 * n_a, :].astype(BF16)

    q_all = mm(wq_ref[...], u_b[...], TB)
    for h in range(heads):
        lo, hi = turn(q_all[h * hd:h * hd + quarter], q_all[h * hd + quarter:(h + 1) * hd], cos_t, sin_t)
        q_ref[h * hd:h * hd + quarter, :] = lo.astype(BF16)
        q_ref[h * hd + quarter:(h + 1) * hd, :] = hi.astype(BF16)
    kv_copy.wait()

    def fill(mine, other):
        kv_ref[mine * own:(mine + 1) * own, :] = kv_out[...].T.astype(BF16)
        kv_ref[other * own:(other + 1) * own, :] = kv_in[...].T.astype(BF16)
        kvt_ref[:, mine * own:(mine + 1) * own] = kv_out[...].astype(BF16)
        kvt_ref[:, other * own:(other + 1) * own] = kv_in[...].astype(BF16)

    pl.when(y == 0)(lambda: fill(0, 1))
    pl.when(y == 1)(lambda: fill(1, 0))
    blank = jnp.zeros((hd, own), BF16)
    slope = hd ** -0.5 * LOG2E

    def attend(h, carry):
        at = pl.ds(pl.multiple_of(h * hd, hd), hd)
        scores = mm(kv_ref[...], jnp.concatenate([q_ref[at, :], blank], axis=0))
        allowed = lax.broadcasted_iota(jnp.int32, scores.shape, 0) <= lax.broadcasted_iota(jnp.int32, scores.shape, 1) + y * own
        scores = jnp.where(allowed, scores * slope, -1e30)
        top = jnp.max(scores, axis=0, keepdims=True)
        prob = jnp.exp2(scores - top)
        total = jnp.sum(prob, axis=0, keepdims=True)
        lse_ref[pl.ds(h, 1), :] = top + jnp.log2(total)
        ctx_ref[at, :] = mm(kvt_ref[hd:, :], (prob * (1.0 / total)).astype(BF16)).astype(BF16)
        return carry

    lax.fori_loop(0, heads, attend, 0)
    x1_ref[...] += mm(ctx_ref[...], wo_ref[...], TA)

    lax.fori_loop(4, shards, mlp, 0)
    f_ref[...] = norm_fwd(x1_ref[...], ln_ref[1:2, :])[0].astype(F32)

    def finish(k):
        done = a_sends(k, tp, "", True) + b_sends(k, tp, "", True)
        for line, other in EVENTS[k]:
            for side, zz in line:
                done += a_sends(k, 2 * zz + y, side) + b_sends(k, 2 * zz + y, side)
        for c in done:
            c.wait_send()

    on_position(finish)
    for to in peers:
        row_copy(to).wait_send()
        a_copy(to, a_c, tp, twin).wait_send()
        b_copy(to, dp, b_x, tp, facing).wait_send()
        b_copy(to, dp, b_c.at[0], tp, twin).wait_send()
        b_copy(to, facing, b_c.at[1], tp, twin).wait_send()


def front(ids, embed, pick, extra, w_rows, wkv_t, ln, cos_t, sin_t, n_q, collective_id):
    own, width = extra.shape
    two_hd = wkv_t.shape[0]
    shards = 2 * NZ
    ff = (w_rows.shape[0] * shards - 2 * n_q) // 3
    dma = lambda *n: pltpu.SemaphoreType.DMA(n)
    s = jax.ShapeDtypeStruct
    rows = (shards, ids.shape[0] // shards, width)
    return pl.pallas_call(
        front_kernel,
        out_shape=(s((own, width), F32),) * 3 + (s((n_q, own), BF16), s((2 * own, two_hd), BF16), s((two_hd, 2 * own), BF16),
                   s((2 * n_q // two_hd, own), F32), s((n_q, own), BF16), s((n_q, width), BF16), s((n_q, width), BF16))
        + (s((ff, width), BF16),) * 3,
        in_specs=[pl.BlockSpec(memory_space=pltpu.SMEM), ANY, VMEM, VMEM, ANY] + [VMEM] * 4,
        out_specs=(VMEM,) * 13,
        scratch_shapes=[pltpu.VMEM(embed.shape, F32), pltpu.VMEM(rows, F32), pltpu.VMEM((shards,) + w_rows.shape, F32), pltpu.VMEM(rows, F32), pltpu.VMEM((own, width), BF16),
                        pltpu.VMEM((two_hd, own), F32), pltpu.VMEM((two_hd, own), F32),
                        dma(3), dma(shards), dma(shards)] + [dma(shards)] * 4 + [dma(shards, 2)]
        + [dma(shards)] * 4 + [dma(2, shards), dma(shards, 4), pltpu.SemaphoreType.DMA, pltpu.SemaphoreType.DMA],
        compiler_params=pltpu.CompilerParams(collective_id=collective_id, has_side_effects=True, vmem_limit_bytes=60000000),
        name="front",
    )(ids, embed, pick, extra, w_rows, wkv_t, ln, cos_t, sin_t)


def layer_bwd_kernel(dfin_ref, x0_ref, x1_ref, loss_ref, ln_ref, cos_ref, sin_ref, wq_ref, wkv_ref, wo_ref, wg_ref, wu_ref, wd_ref,
                     q_ref, kv_ref, kvt_ref, lse_ref, ctx_ref, pick_ref, rows_ref, d0_ref, back_ref, d_one, d_b, u_b, dctx, dq, dkv, dkv_in,
                     hid, d_gate, d_up, rows_out, g_q, g_o, g_g, g_u, g_d, small, out_sem, send_sem, recv_sem, r_send, r_recv):
    tp, dp, _, y = place()
    partner = tp + 1 - 2 * y
    own, width = x0_ref.shape
    hd = kv_ref.shape[1] // 2
    quarter = hd // 2
    nq = q_ref.shape[0]
    heads = nq // hd
    ff = wg_ref.shape[0]
    shards = rows_ref.shape[0]
    plane_barrier(tp, dp, [])
    _, f_hat, f_inv = norm_fwd(x1_ref[...], ln_ref[1:2, :])
    d_in, g_fin = norm_bwd(dfin_ref[...], f_hat, f_inv, ln_ref[1:2, :])
    d_one[...] = d_in
    d_b[...] = d_in.astype(BF16)
    u_b[...] = norm_fwd(x0_ref[...], ln_ref[0:1, :])[0]
    dctx[...] = mm(wo_ref[...], d_b[...], TB).astype(BF16)
    cos_t = cos_ref[...]
    sin_t = sin_ref[...]
    blank = jnp.zeros((hd, own), BF16)
    slope = hd ** -0.5 * LOG2E
    dkv[...] = jnp.zeros_like(dkv)

    def attend(h, carry):
        at = pl.ds(pl.multiple_of(h * hd, hd), hd)
        q_pad = jnp.concatenate([q_ref[at, :], blank], axis=0)
        d_pad = jnp.concatenate([blank, dctx[at, :]], axis=0)
        scores = mm(kv_ref[...], q_pad)
        allowed = lax.broadcasted_iota(jnp.int32, scores.shape, 0) <= lax.broadcasted_iota(jnp.int32, scores.shape, 1) + y * own
        prob = jnp.where(allowed, jnp.exp2(scores * slope - lse_ref[pl.ds(h, 1), :]), 0.0)
        d_prob = mm(kv_ref[...], d_pad)
        mean = jnp.sum(d_prob * prob, axis=0, keepdims=True)
        d_score = (prob * (d_prob - mean) * hd ** -0.5).astype(BF16)
        dkv[...] += mm(d_score, q_pad, TB) + mm(prob.astype(BF16), d_pad, TB)
        d_q = mm(kvt_ref[0:hd, :], d_score)
        lo, hi = turn(d_q[:quarter], d_q[quarter:], cos_t, -sin_t)
        dq[at, :] = jnp.concatenate([lo, hi], axis=0).astype(BF16)
        return carry

    lax.fori_loop(0, heads, attend, 0)
    copy = remote(dkv.at[pl.ds(pl.multiple_of((1 - y) * own, own), own), :], dkv_in, send_sem, recv_sem, partner, dp)
    copy.start()

    d0_ref[...] = mm(dq[...], wq_ref[...], TA)
    step = min(512, ff)

    def mlp(n, carry):
        at = pl.ds(pl.multiple_of(n * step, step), step)
        gate = mm(wg_ref[at, :], u_b[...], TB)
        up = mm(wu_ref[at, :], u_b[...], TB)
        d_hidden = mm(wd_ref[at, :], d_b[...], TB)
        sig = jax.nn.sigmoid(gate)
        hid[at, :] = (gate * sig * up).astype(BF16)
        d_gate[at, :] = (d_hidden * up * sig * (1.0 + gate * (1.0 - sig))).astype(BF16)
        d_up[at, :] = (d_hidden * gate * sig).astype(BF16)
        d0_ref[...] += mm(d_gate[at, :], wg_ref[at, :], TA) + mm(d_up[at, :], wu_ref[at, :], TA)
        return carry

    lax.fori_loop(0, ff // step, mlp, 0)
    copy.wait()
    d_kv = (dkv[pl.ds(pl.multiple_of(y * own, own), own), :] + dkv_in[...]).T
    lo, hi = turn(d_kv[:quarter], d_kv[quarter:hd], cos_t, -sin_t)
    d_kv = jnp.concatenate([lo, hi, d_kv[hd:]], axis=0).astype(BF16)
    small[0:2 * hd, :] = mm(d_kv, u_b[...])
    d_u = d0_ref[...] + mm(d_kv, wkv_ref[...], TA)
    _, u_hat, u_inv = norm_fwd(x0_ref[...], ln_ref[0:1, :])
    d_in, g_in = norm_bwd(d_u, u_hat, u_inv, ln_ref[0:1, :])
    d_zero = d_one[...] + d_in
    d0_ref[...] = d_zero
    high = d_zero.astype(BF16)
    left = d_zero - high.astype(F32)
    middle = left.astype(BF16)
    low = (left - middle.astype(F32)).astype(BF16)
    rows_out[...] = (mm(pick_ref[...], high, TA) + mm(pick_ref[...], middle, TA) + mm(pick_ref[...], low, TA)).reshape(rows_out.shape)

    def row_copy(to):
        return remote(rows_out.at[to], back_ref.at[tp], r_send.at[to], r_recv.at[tp], to, dp)

    peers = [lax.rem(tp + n, shards) for n in range(1, shards)]
    for to in peers:
        row_copy(to).start()
    own_rows = pltpu.make_async_copy(rows_out.at[tp], back_ref.at[tp], out_sem.at[7 * 2 * NZ])
    own_rows.start()

    g_o[...] = mm(ctx_ref[...], d_b[...])
    g_q[...] = mm(dq[...], u_b[...])

    def weight_grads(n, carry):
        at = pl.ds(pl.multiple_of(n * step, step), step)
        g_d[at, :] = mm(hid[at, :], d_b[...])
        g_g[at, :] = mm(d_gate[at, :], u_b[...])
        g_u[at, :] = mm(d_up[at, :], u_b[...])
        return carry

    lax.fori_loop(0, ff // step, weight_grads, 0)
    small[2 * hd:, :] = jnp.zeros_like(small[2 * hd:, :])
    small[2 * hd:2 * hd + 1, :] = g_in.reshape(1, width)
    small[2 * hd + 1:2 * hd + 2, :] = g_fin.reshape(1, width)
    small[2 * hd + 2:2 * hd + 3, :] = loss_ref[...]
    copies = []

    def put(src, first, size, s):
        copies.append(pltpu.make_async_copy(src, rows_ref.at[s, pl.ds(first, size), :], out_sem.at[len(copies)]))

    n_kv = 2 * hd // shards
    for s in range(shards):
        at = 0
        for g, size in ((g_q, nq // shards), (g_o, nq // shards), (g_g, ff // shards), (g_u, ff // shards), (g_d, ff // shards)):
            put(g.at[pl.ds(s * size, size), :], at, size, s)
            at += size
        put(small.at[pl.ds(s * n_kv, n_kv), :], at, n_kv, s)
        put(small.at[pl.ds(2 * hd + (0 if s == 0 else 16), 16), :], at + n_kv, 16, s)
    for c in copies:
        c.start()
    for c in copies:
        c.wait()
    own_rows.wait()
    for source in peers:
        remote(rows_out.at[source], back_ref.at[source], r_send.at[source], r_recv.at[source], source, dp).wait_recv()
        row_copy(source).wait_send()


def layer_bwd(d_fin, x0, x1, loss_row, ln, cos_t, sin_t, weights, saved, pick, collective_id):
    own, width = x0.shape
    nq = weights[0].shape[0]
    two_hd = weights[1].shape[0]
    ff = weights[3].shape[0]
    rows = (2 * nq + 3 * ff + two_hd) // (2 * NZ) + 16
    chunk = (own, width)
    back = (2 * NZ, pick.shape[1] // (2 * NZ), width)
    return pl.pallas_call(
        layer_bwd_kernel,
        out_shape=(jax.ShapeDtypeStruct((2 * NZ, rows, width), F32), jax.ShapeDtypeStruct(chunk, F32), jax.ShapeDtypeStruct(back, F32)),
        in_specs=[VMEM] * 19,
        out_specs=(ANY, VMEM, ANY),
        scratch_shapes=[pltpu.VMEM(chunk, F32), pltpu.VMEM(chunk, BF16), pltpu.VMEM(chunk, BF16), pltpu.VMEM((nq, own), BF16),
                        pltpu.VMEM((nq, own), BF16), pltpu.VMEM((2 * own, two_hd), F32), pltpu.VMEM((own, two_hd), F32)]
        + [pltpu.VMEM((ff, own), BF16)] * 3 + [pltpu.VMEM(back, F32), pltpu.VMEM((nq, width), F32), pltpu.VMEM((nq, width), F32)] + [pltpu.VMEM((ff, width), F32)] * 3
        + [pltpu.VMEM((two_hd + 32, width), F32), pltpu.SemaphoreType.DMA((14 * NZ + 1,)), pltpu.SemaphoreType.DMA, pltpu.SemaphoreType.DMA,
           pltpu.SemaphoreType.DMA((2 * NZ,)), pltpu.SemaphoreType.DMA((2 * NZ,))],
        compiler_params=pltpu.CompilerParams(collective_id=collective_id, has_side_effects=True, vmem_limit_bytes=60000000),
        name="layer_bwd",
    )(d_fin, x0, x1, loss_row, ln, cos_t, sin_t, *weights, *saved, pick)


N_BLOCK = 12
EARLY = 9
W_REDUCE = {
    0: {1: (3,), 3: (2,), 5: (1,), 7: (0,)},
    1: {3: (3,), 5: (2, 0), 7: (1,)},
    2: {3: (0,), 5: (1, 3), 7: (2,)},
    3: {1: (0,), 3: (1,), 5: (2,), 7: (3,)},
}


def tail_kernel(g_ref, p_ref, rows_ref, ids_ref, t_ref, w_out, small_ref,
                s_buf, from_c, from_x, rows_c, ids_c, parts, acc, w_c, w_y, w_l, w_r, w_x,
                g_load, g_send_c, g_recv_c, g_send_x, g_recv_x, g_send_t, g_recv_t, g_store, l_send, l_recv,
                w_load, w_out_sem, send_c, send_y, send_l, send_r, recv_c, recv_y, recv_l, recv_r, last_send, last_recv, small_send, small_recv):
    tp, dp, z, y = place()
    partner = tp + 1 - 2 * y
    core = dp % 2
    twin = dp + 1 - 2 * core
    facing = lax.rem(dp + 2, 4)
    half = g_ref.shape[0] // 2
    size = s_buf.shape[1]
    last = half - (N_BLOCK - 1) * size
    n_look = rows_ref.shape[0]

    def rows(which, b, n):
        return pl.ds(pl.multiple_of(which * half + b * size, 8), n)

    def part(buf, b, n):
        return buf.at[b, pl.ds(0, n), :]

    plane_barrier(tp, dp, [(tp, twin), (tp, facing)])

    look_copies = [remote(rows_ref, rows_c, l_send.at[0], l_recv.at[0], tp, twin), remote(ids_ref, ids_c, l_send.at[1], l_recv.at[1], tp, twin)]
    for c in look_copies:
        c.start()

    def c_copy(b, n):
        return remote(g_ref.at[rows(1 - core, b, n), :], part(from_c, b, n), g_send_c.at[b], g_recv_c.at[b], tp, twin)

    def own_load(b, n):
        return pltpu.make_async_copy(g_ref.at[rows(core, b, n), :], part(s_buf, b, n), g_load.at[b])

    def x_copy(b, n):
        return remote(part(s_buf, b, n), part(from_x, b, n), g_send_x.at[b], g_recv_x.at[b], tp, facing)

    def t_copy(b, n):
        return remote(part(from_x, b, n), t_ref.at[rows(core, b, n), :], g_send_t.at[b], g_recv_t.at[b], tp, twin)

    def t_store(b, n):
        return pltpu.make_async_copy(part(from_x, b, n), t_ref.at[rows(core, b, n), :], g_store.at[b])

    def every(f, first, end):
        def body(b, carry):
            f(b, size)
            return carry
        lax.fori_loop(first, min(end, N_BLOCK - 1), body, 0)
        if end == N_BLOCK:
            f(N_BLOCK - 1, last)

    def chip_sum(b, n):
        own_load(b, n).wait()
        c_copy(b, n).wait_recv()
        ids = jnp.concatenate([ids_ref[...], ids_c[...]], axis=1) - (core * half + b * size)
        hit = (lax.broadcasted_iota(jnp.int32, (n, 2 * n_look), 0) == ids).astype(F32).astype(BF16)
        look = mm(hit, parts[0]) + mm(hit, parts[1]) + mm(hit, parts[2])
        s_buf[b, 0:n, :] = s_buf[b, 0:n, :] + from_c[b, 0:n, :] + look
        x_copy(b, n).start()

    def w_first(k):
        for zz in REDUCE_ORDER[k]:
            for slot in (2 * zz + 1 - y, 2 * zz + y):
                remote(p_ref.at[slot, 1 - core], w_c.at[slot], send_c.at[slot], recv_c.at[slot], tp, twin).start()
                pltpu.make_async_copy(p_ref.at[slot, core], acc.at[slot], w_load.at[slot]).start()

    def w_chip_sum(slot):
        pltpu.make_async_copy(p_ref.at[slot, core], acc.at[slot], w_load.at[slot]).wait()
        remote(acc.at[slot], w_c.at[slot], send_c.at[slot], recv_c.at[slot], tp, twin).wait_recv()
        add_into(acc.at[slot], w_c.at[slot])

    def w_second(k):
        for zz in REDUCE_ORDER[k]:
            slot = 2 * zz + 1 - y
            w_chip_sum(slot)
            remote(acc.at[slot], w_y.at[zz], send_y.at[zz], recv_y.at[zz], partner, dp).start()
        for zz in REDUCE_ORDER[k]:
            w_chip_sum(2 * zz + y)

    def w_reduce(k, shards):
        for zz in shards:
            line = acc.at[2 * zz + y]
            remote(line, w_y.at[zz], send_y.at[zz], recv_y.at[zz], partner, dp).wait_recv()
            add_into(line, w_y.at[zz])
            if zz >= k and k > 0:
                remote(line, w_l.at[zz - 1], send_l.at[zz], recv_l.at[zz], partner, dp).wait_recv()
                add_into(line, w_l.at[zz - 1])
            if zz <= k and k < NZ - 1:
                remote(line, w_r.at[zz], send_r.at[zz], recv_r.at[zz], partner, dp).wait_recv()
                add_into(line, w_r.at[zz])
            if zz > k:
                remote(line, w_l.at[zz - 1], send_r.at[zz], recv_l.at[zz], tp + 2, dp).start()
            if zz < k:
                remote(line, w_r.at[zz], send_l.at[zz], recv_r.at[zz], tp - 2, dp).start()

    def on_position(f):
        for k in range(NZ):
            pl.when(z == k)(functools.partial(f, k))

    def first(b, n):
        c_copy(b, n).start()
        own_load(b, n).start()

    every(first, 0, 4)
    on_position(w_first)
    every(first, 4, N_BLOCK)

    def split(at, value):
        high = value.astype(BF16)
        left = value - high.astype(F32)
        middle = left.astype(BF16)
        parts[0, at, :] = high
        parts[1, at, :] = middle
        parts[2, at, :] = (left - middle.astype(F32)).astype(BF16)

    split(pl.ds(0, n_look), rows_ref[...])
    for c in look_copies:
        c.wait()
    split(pl.ds(n_look, n_look), rows_c[...])
    every(chip_sum, 0, EARLY)
    on_position(w_second)

    total = acc.at[tp]
    w_copy_x = remote(total, w_x, last_send.at[0], last_recv.at[0], tp, facing)
    w_copy_c = remote(total, w_out.at[core], last_send.at[1], last_recv.at[1], tp, twin)
    w_store = pltpu.make_async_copy(total, w_out.at[core], w_out_sem)
    n_small, n_rows = small_ref.shape[1], w_out.shape[1]
    mine = w_out.at[1, pl.ds(n_rows - 32, n_small), :]
    small_here = pltpu.make_async_copy(mine, small_ref.at[tp], w_out_sem)
    peers = [lax.rem(tp + n, 2 * NZ) for n in range(1, 2 * NZ)]
    for b in range(N_BLOCK):
        n = last if b == N_BLOCK - 1 else size
        x_copy(b, n).wait_recv()
        add_into(part(from_x, b, n), part(s_buf, b, n), 24)
        t_copy(b, n).start()
        t_store(b, n).start()
        for k in range(NZ):
            if b in W_REDUCE[k]:
                pl.when(z == k)(functools.partial(w_reduce, k, W_REDUCE[k][b]))
        if b == 7:
            w_copy_x.start()
            every(chip_sum, EARLY, N_BLOCK)
        if b == 8:
            w_copy_x.wait()
            add_into(total, w_x)
            w_copy_c.start()
            w_store.start()
        if b == 9:
            w_copy_c.wait_send()
            remote(total, w_out.at[1 - core], last_send.at[1], last_recv.at[1], tp, twin).wait_recv()
            w_store.wait()
            for to in peers:
                remote(mine, small_ref.at[tp], small_send.at[to], small_recv.at[tp], to, dp).start()
            small_here.start()
    for source in peers:
        remote(small_ref.at[source], small_ref.at[source], small_send.at[source], small_recv.at[source], source, dp).wait_recv()
        remote(mine, small_ref.at[tp], small_send.at[source], small_recv.at[tp], source, dp).wait_send()
    small_here.wait()

    def w_done(k):
        for zz in range(NZ):
            line = acc.at[2 * zz + y]
            for slot in (2 * zz + 1 - y, 2 * zz + y):
                remote(p_ref.at[slot, 1 - core], w_c.at[slot], send_c.at[slot], recv_c.at[slot], tp, twin).wait_send()
            remote(line, w_y.at[zz], send_y.at[zz], recv_y.at[zz], partner, dp).wait_send()
            if zz > k:
                remote(line, w_l.at[zz - 1], send_r.at[zz], recv_l.at[zz], tp + 2, dp).wait_send()
            if zz < k:
                remote(line, w_r.at[zz], send_l.at[zz], recv_r.at[zz], tp - 2, dp).wait_send()

    on_position(w_done)

    def drain(b, n):
        c_copy(b, n).wait_send()
        x_copy(b, n).wait_send()
        t_copy(b, n).wait_send()
        t_store(b, n).wait()
        remote(part(from_x, b, n), t_ref.at[rows(1 - core, b, n), :], g_send_t.at[b], g_recv_t.at[b], tp, twin).wait_recv()

    every(drain, 0, N_BLOCK)


def tail(g_table, g_rows, look_rows, look_ids, collective_id):
    vocab, width = g_table.shape
    rows = g_rows.shape[1]
    half = (rows // 2, width)
    n_look = look_ids.shape[1]
    size = -(-vocab // (2 * N_BLOCK * 24)) * 24
    blocks = pltpu.VMEM((N_BLOCK, size, width), F32)
    dma = lambda *n: pltpu.SemaphoreType.DMA(n)
    t, w_sum, small = pl.pallas_call(
        tail_kernel,
        out_shape=(jax.ShapeDtypeStruct((vocab, width), F32), jax.ShapeDtypeStruct((2,) + half, F32), jax.ShapeDtypeStruct((2 * NZ, 24, width), F32)),
        in_specs=[ANY, ANY, VMEM, VMEM],
        out_specs=(ANY,) * 3,
        scratch_shapes=[blocks] * 3 + [pltpu.VMEM((n_look, width), F32), pltpu.VMEM((1, n_look), jnp.int32), pltpu.VMEM((3, 2 * n_look, width), BF16)]
        + [pltpu.VMEM((2 * NZ,) + half, F32)] * 2 + [pltpu.VMEM((NZ,) + half, F32)] + [pltpu.VMEM((NZ - 1,) + half, F32)] * 2
        + [pltpu.VMEM(half, F32)]
        + [dma(N_BLOCK)] * 8 + [dma(2)] * 2
        + [dma(2 * NZ), pltpu.SemaphoreType.DMA] + [dma(2 * NZ), dma(NZ), dma(NZ), dma(NZ)] * 2 + [dma(2)] * 2 + [dma(2 * NZ)] * 2,
        compiler_params=pltpu.CompilerParams(collective_id=collective_id, has_side_effects=True, vmem_limit_bytes=67000000),
        name="tail",
    )(g_table, g_rows.reshape((2 * NZ, 2) + half), look_rows.reshape(n_look, width), look_ids)
    return t, w_sum.reshape(rows, width), small


UPDATE_ROWS = 512


def update_kernel(t_ref, w_ref, small_ref, *refs):
    state = [refs[7 * i:7 * i + 7] for i in range(3)]
    new = [refs[21 + 7 * i:28 + 7 * i] for i in range(3)]
    loss_ref = refs[42]
    held, made, in_sem, out_sem = refs[43:]
    vocab = t_ref.shape[0]
    n_kv, hd = 2 * state[0][3].shape[1] // small_ref.shape[0], state[0][3].shape[1]
    blocks = [(at, min(UPDATE_ROWS, vocab - at)) for at in range(0, vocab, UPDATE_ROWS)]

    def loads(q):
        at, n = blocks[q]
        return [pltpu.make_async_copy(ref.at[pl.ds(at, n), :], held.at[q % 3, i, pl.ds(0, n), :], in_sem.at[q % 3, i])
                for i, ref in enumerate((t_ref, state[0][0], state[1][0], state[2][0]))]

    def stores(q):
        at, n = blocks[q]
        return [pltpu.make_async_copy(made.at[q % 2, i, pl.ds(0, n), :], new[i][0].at[pl.ds(at, n), :], out_sem.at[q % 2, i]) for i in range(3)]

    for q in range(3):
        for c in loads(q):
            c.start()

    def small_update(index, grad, *where):
        got = adam_update(state[0][index][where], grad, state[1][index][where], state[2][index][where])
        for i in range(3):
            new[i][index][where] = got[i]

    n_q, n_f = state[0][2].shape[0], state[0][6].shape[0]
    small_update(1, small_ref[0, n_kv:n_kv + 2, :], Ellipsis)
    small_update(2, w_ref[0:n_q, :], Ellipsis)
    kv = small_ref[:, 0:n_kv, :].reshape(2 * hd, small_ref.shape[2])
    for i in range(2):
        small_update(3, kv[i * hd:(i + 1) * hd], i)
    small_update(4, w_ref[n_q:2 * n_q, :], Ellipsis)
    for i in range(2):
        small_update(5, w_ref[2 * n_q + i * n_f:2 * n_q + (i + 1) * n_f, :].T, i)
    small_update(6, w_ref[2 * n_q + 2 * n_f:2 * n_q + 3 * n_f, :], Ellipsis)
    loss_ref[...] = jnp.sum(small_ref[0, n_kv + 2:n_kv + 3, :], axis=1, keepdims=True)

    for q, (at, n) in enumerate(blocks):
        for c in loads(q):
            c.wait()
        if q >= 2:
            for c in stores(q - 2):
                c.wait()
        step = 32 if n % 32 == 0 else 16

        def body(j, carry):
            rows = pl.ds(pl.multiple_of(j * step, step), step)
            got = adam_update(held[q % 3, 1, rows, :], held[q % 3, 0, rows, :], held[q % 3, 2, rows, :], held[q % 3, 3, rows, :])
            for i in range(3):
                made[q % 2, i, rows, :] = got[i]
            return carry

        lax.fori_loop(0, n // step, body, 0)
        for c in stores(q):
            c.start()
        if q + 3 < len(blocks):
            for c in loads(q + 3):
                c.start()
    for q in range(len(blocks) - 2, len(blocks)):
        for c in stores(q):
            c.wait()


def update(g_table, g_shard, g_small, state_arrays):
    specs = [ANY] + [VMEM] * 6
    width = g_table.shape[1]

    def flip(arrays):
        return [a.swapaxes(-1, -2) if i % 7 in (2, 3) else a for i, a in enumerate(arrays)]

    given = flip(state_arrays)
    *new, loss = pl.pallas_call(
        update_kernel,
        out_shape=tuple(jax.ShapeDtypeStruct(a.shape, F32) for a in given) + (jax.ShapeDtypeStruct((1, 1), F32),),
        in_specs=[ANY, VMEM, VMEM] + specs * 3,
        out_specs=tuple(specs * 3) + (VMEM,),
        scratch_shapes=[pltpu.VMEM((3, 4, UPDATE_ROWS, width), F32), pltpu.VMEM((2, 3, UPDATE_ROWS, width), F32),
                        pltpu.SemaphoreType.DMA((3, 4)), pltpu.SemaphoreType.DMA((2, 3))],
        compiler_params=pltpu.CompilerParams(vmem_limit_bytes=60000000),
        name="update",
    )(g_table, g_shard, g_small, *given)
    return flip(new) + [loss]


def norm_fwd(x_f32, scale):
    centered = x_f32 - jnp.mean(x_f32, axis=-1, keepdims=True)
    inv_std = lax.rsqrt(jnp.mean(centered * centered, axis=-1, keepdims=True) + LN_EPS)
    x_hat = centered * inv_std
    return (x_hat * scale).astype(BF16), x_hat, inv_std


def norm_bwd(d_out, x_hat, inv_std, scale):
    d_scale = jnp.sum(d_out * x_hat, axis=0)
    d_hat = d_out * scale
    d_in = inv_std * (d_hat - jnp.mean(d_hat, axis=-1, keepdims=True) - x_hat * jnp.mean(d_hat * x_hat, axis=-1, keepdims=True))
    return d_in, d_scale


def adam_update(param_in, grad_in, mom_in, vel_in):
    mom_new = BETA_ONE * mom_in + (1.0 - BETA_ONE) * grad_in
    vel_new = BETA_TWO * vel_in + (1.0 - BETA_TWO) * grad_in * grad_in
    return param_in - LEARN_RATE * mom_new / (jnp.sqrt(vel_new) + ADAM_EPS), mom_new, vel_new


def dot(spec, a, b):
    return jnp.einsum(spec, a, b, preferred_element_type=F32)


def solution(mesh):
    param_specs = (P('tp', None), P(None, None), P(None, 'tp'), P(None, None, None), P('tp', None), P(None, None, 'tp'), P('tp', None))
    n_tp = mesh.shape['tp']
    n_dp = mesh.shape['dp']

    def local_step(tokens, labels, *state_arrays):
        embed, ln_scales, w_q, w_kv, w_o, w_gu, w_down = state_arrays[0:7]
        batch_loc, seq_len = tokens.shape
        vocab_loc, d_model = embed.shape
        head_dim = w_kv.shape[2]
        q_loc = w_q.shape[1]
        f_loc = w_down.shape[0]
        tok_loc = batch_loc * seq_len
        tok_total = tok_loc * n_dp
        own = tok_loc // n_tp
        tp_rank = lax.axis_index('tp')
        half = tp_rank % 2

        strict = (jnp.arange(own)[:, None] > jnp.arange(own)[None, :]).astype(BF16)

        def routing(chunks):
            shard = chunks // vocab_loc
            row = chunks - shard * vocab_loc
            hot = (shard[:, :, None] == jnp.arange(n_tp)[None, None, :])
            before = dot('rs,nsj->nrj', strict, hot.astype(BF16))
            rank = jnp.sum(jnp.where(hot, before, 0.0), axis=-1).astype(jnp.int32)
            most = jnp.max(jnp.sum(hot.astype(jnp.int32), axis=1))
            return shard, row, rank, (most + CAP - 1) // CAP

        chunks = tokens.reshape(n_tp, own)
        shard, row, rank, rounds = routing(chunks)
        slots = jnp.arange(CAP)
        my_shard = lax.dynamic_index_in_dim(shard, tp_rank, 0, keepdims=False)
        my_rank = lax.dynamic_index_in_dim(rank, tp_rank, 0, keepdims=False)

        def fetch(step):
            here = (shard[:, None, :] == tp_rank) & (rank[:, None, :] == slots[None, :, None] + step * CAP)
            ids = jnp.sum(jnp.where(here, row[:, None, :], 0), axis=-1).reshape(-1)
            pick = (my_shard[:, None, None] == jnp.arange(n_tp)[None, :, None]) & (my_rank[:, None, None] == slots[None, None, :] + step * CAP)
            return ids, pick.reshape(own, n_tp * CAP).astype(BF16)

        def fetch_more(state):
            ids, pick = fetch(state[0])
            rows_in = plane_swap(jnp.take(embed, ids, axis=0).reshape(n_tp, CAP, d_model), 1).reshape(n_tp * CAP, d_model).astype(BF16)
            return state[0] + 1, state[1] + dot('rc,cd->rd', pick, rows_in)

        more_rows = lax.while_loop(lambda state: state[0] < rounds, fetch_more, (jnp.int32(1), jnp.zeros((own, d_model), F32)))[1]
        ids_first, pick_first = fetch(0)

        w_rows = jnp.concatenate([w_q.T, w_o, w_gu.transpose(0, 2, 1).reshape(2 * f_loc, d_model), w_down], axis=0)
        cuts = (q_loc, 2 * q_loc, 2 * q_loc + f_loc, 2 * q_loc + 2 * f_loc)
        wkv_t = w_kv.transpose(0, 2, 1).reshape(2 * head_dim, d_model).astype(BF16)
        inv_freq = ROPE_BASE ** (-jnp.arange(0, head_dim, 2).astype(F32) / head_dim)
        angles = inv_freq[:, None] * (half * own + jnp.arange(own)).astype(F32)[None, :]
        cos_t, sin_t = jnp.cos(angles), jnp.sin(angles)
        f_own, x_one, x_zero, *saved = front(ids_first, embed, pick_first, more_rows, w_rows, wkv_t, ln_scales, cos_t, sin_t, n_tp * q_loc, 0)
        saved, (wq_t, wo_b, wg_t, wu_t, wd_b) = saved[:5], saved[5:]
        weights = (wq_t, wkv_t, wo_b, wg_t, wu_t, wd_b)

        logit_scale = d_model ** -0.5
        lab_loc = labels.reshape(n_tp, own) - tp_rank * vocab_loc
        d_fin, g_head_part, log_norm, lab_sum = head(f_own, lab_loc, embed, logit_scale, logit_scale / tok_total, 4)
        log_norm = lax.dynamic_index_in_dim(log_norm, tp_rank, 0, keepdims=False)
        loss_row = (log_norm + LOGIT_ZLOSS * log_norm * log_norm - jnp.sum(lab_sum, axis=0) * logit_scale) / tok_total
        g_rows, d_zero, rows_back = layer_bwd(d_fin, x_zero, x_one, loss_row[None, :], ln_scales, cos_t, sin_t, weights, saved, pick_first, 7)

        def row_ids(step):
            here = (shard[:, None, :] == tp_rank) & (rank[:, None, :] == slots[None, :, None] + step * CAP)
            return jnp.where(jnp.any(here, axis=-1), jnp.sum(jnp.where(here, row[:, None, :], 0), axis=-1), vocab_loc).reshape(-1)

        def give_back(state):
            mine = (my_shard[None, None, :] == jnp.arange(n_tp)[:, None, None]) & (my_rank[None, None, :] == slots[None, :, None] + state[0] * CAP)
            ids = jnp.sum(jnp.where(mine, jnp.arange(own)[None, None, :], 0), axis=-1).reshape(-1)
            rows_in = plane_swap(jnp.take(d_zero, ids, axis=0).reshape(n_tp, CAP, d_model), 9).reshape(-1, d_model)
            return state[0] + 1, state[1].at[row_ids(state[0])].add(rows_in, mode='drop')

        g_table = lax.while_loop(lambda state: state[0] < rounds, give_back, (jnp.int32(1), g_head_part))[1]
        g_table, g_shard, g_small = tail(g_table, g_rows, rows_back, row_ids(0)[None, :], 10)
        *new, loss = update(g_table, g_shard, g_small, state_arrays)
        return tuple(new) + (loss.reshape(()),)

    return jax.shard_map(local_step, mesh=mesh, in_specs=(P('dp', None), P('dp', None)) + param_specs * 3,
                         out_specs=param_specs * 3 + (P(),), check_vma=False)
```

```python
import functools

import jax
import jax.numpy as jnp
from jax import lax
from jax.experimental import pallas as pl
from jax.experimental.pallas import tpu as pltpu
from jax.sharding import PartitionSpec as P

LN_EPS = 1e-5
LOGIT_ZLOSS = 1e-4
LEARN_RATE = 1e-2
BETA_ONE = 0.9
BETA_TWO = 0.95
ADAM_EPS = 1e-8
ROPE_BASE = 10000.0
NZ = 4
CAP = 96
F32 = jnp.float32
BF16 = jnp.bfloat16
ANY = pl.BlockSpec(memory_space=pl.ANY)
VMEM = pl.BlockSpec(memory_space=pltpu.VMEM)

ARRIVALS = {
    0: (("R", 1), ("R", 2), ("R", 3)),
    1: (("L", 0), ("R", 2), ("R", 3)),
    2: (("R", 3), ("L", 1), ("L", 0)),
    3: (("L", 2), ("L", 1), ("L", 0)),
}
REDUCE_ORDER = {0: (3, 2, 1, 0), 1: (3, 0, 2, 1), 2: (0, 3, 1, 2), 3: (0, 1, 2, 3)}


def remote(src, dst, send_sem, recv_sem, tp, dp):
    return pltpu.make_async_remote_copy(src_ref=src, dst_ref=dst, send_sem=send_sem, recv_sem=recv_sem,
                                        device_id=(tp, dp), device_id_type=pl.DeviceIdType.MESH)


def place():
    tp = lax.axis_index("tp")
    dp = lax.axis_index("dp")
    return tp, dp, tp // 2, tp % 2


def signal(tp, dp):
    pl.semaphore_signal(pltpu.get_barrier_semaphore(), inc=1, device_id=(tp, dp), device_id_type=pl.DeviceIdType.MESH)


def add_into(acc, other, step=None):
    rows = acc.shape[0]
    step = step or (64 if rows % 64 == 0 else 8)

    def body(n, carry):
        at = pl.ds(pl.multiple_of(n * step, step), step)
        acc[at, :] = acc[at, :] + other[at, :]
        return carry

    lax.fori_loop(0, rows // step, body, 0)


def plane_barrier(tp, dp, others):
    peers = [(lax.rem(tp + n, 2 * NZ), dp) for n in range(1, 2 * NZ)] + others
    for peer in peers:
        signal(*peer)
    pl.semaphore_wait(pltpu.get_barrier_semaphore(), len(peers))


def swap_kernel(x_ref, out_ref, own_sem, send, recv):
    tp, dp, _, _ = place()
    plane_barrier(tp, dp, [])
    copies = []
    for n in range(1, 2 * NZ):
        to = lax.rem(tp + n, 2 * NZ)
        copy = remote(x_ref.at[to], out_ref.at[tp], send.at[to], recv.at[tp], to, dp)
        copy.start()
        copies.append(copy)
    own = pltpu.make_async_copy(x_ref.at[tp], out_ref.at[tp], own_sem)
    own.start()
    for n in range(1, 2 * NZ):
        source = lax.rem(tp + n, 2 * NZ)
        remote(out_ref.at[source], out_ref.at[source], send.at[source], recv.at[source], source, dp).wait_recv()
    own.wait()
    for copy in copies:
        copy.wait_send()


def plane_swap(x, collective_id):
    return pl.pallas_call(
        swap_kernel,
        out_shape=jax.ShapeDtypeStruct(x.shape, x.dtype),
        in_specs=[ANY],
        out_specs=ANY,
        scratch_shapes=[pltpu.SemaphoreType.DMA] + [pltpu.SemaphoreType.DMA((2 * NZ,))] * 2,
        compiler_params=pltpu.CompilerParams(collective_id=collective_id, has_side_effects=True),
        name="plane_swap",
    )(x)


GATHER_ORDER = {
    0: ((0, 0), (0, 1), (1, 0), (0, 2), (1, 1), (0, 3), (1, 2), (1, 3)),
    1: ((0, 1), (0, 0), (0, 2), (1, 1), (1, 0), (0, 3), (1, 2), (1, 3)),
    2: ((0, 2), (0, 1), (0, 3), (1, 2), (0, 0), (1, 3), (1, 1), (1, 0)),
    3: ((0, 3), (0, 2), (1, 3), (0, 1), (1, 2), (0, 0), (1, 1), (1, 0)),
}
GATHER_EVENTS = {
    0: {
        1: ((0, 1, 0, 'y'), (1, 0, 1, 'r'), (0, 1, 1, 'y'), (1, 0, 0, '')),
        3: ((0, 2, 0, 'y'), (1, 1, 0, ''), (0, 2, 1, 'y'), (1, 1, 1, '')),
        5: ((0, 3, 0, 'y'), (1, 2, 0, ''), (0, 3, 1, ''), (1, 2, 1, '')),
        7: ((1, 3, 0, ''), (1, 3, 1, '')),
    },
    1: {
        1: ((0, 0, 0, 'ry'), (0, 2, 0, 'ly'), (1, 1, 0, ''), (0, 0, 1, 'r'), (0, 2, 1, 'ly'), (1, 1, 1, '')),
        4: ((0, 3, 0, 'ly'), (1, 0, 0, ''), (1, 0, 1, 'r')),
        5: ((0, 3, 1, 'l'), (1, 2, 0, '')),
        6: ((1, 2, 1, ''), (1, 3, 1, 'l')),
        7: ((1, 3, 0, ''),),
    },
    2: {
        1: ((0, 1, 0, 'ry'), (0, 3, 0, 'ly'), (1, 2, 0, ''), (0, 1, 1, 'ry'), (0, 3, 1, 'l'), (1, 2, 1, '')),
        4: ((0, 0, 0, 'ry'), (1, 1, 0, ''), (1, 3, 1, 'l'), (0, 0, 1, 'r'), (1, 3, 0, '')),
        6: ((1, 0, 1, 'r'), (1, 1, 1, '')),
        7: ((1, 0, 0, ''),),
    },
    3: {
        1: ((0, 2, 0, 'y'), (1, 3, 1, 'l'), (0, 2, 1, 'y'), (1, 3, 0, '')),
        3: ((0, 1, 0, 'y'), (1, 2, 0, ''), (0, 1, 1, 'y'), (1, 2, 1, '')),
        5: ((0, 0, 0, 'y'), (1, 1, 0, ''), (0, 0, 1, ''), (1, 1, 1, '')),
        7: ((1, 0, 0, ''), (1, 0, 1, '')),
    },
}
SCATTER_ORDER = {
    0: ((1, 3), (1, 2), (0, 3), (1, 1), (0, 2), (1, 0), (0, 1), (0, 0)),
    1: ((1, 3), (1, 2), (0, 3), (1, 0), (1, 1), (0, 2), (0, 0), (0, 1)),
    2: ((1, 0), (1, 1), (1, 3), (0, 0), (1, 2), (0, 3), (0, 1), (0, 2)),
    3: ((1, 0), (1, 1), (0, 0), (1, 2), (0, 1), (1, 3), (0, 2), (0, 3)),
}
SCATTER_EVENTS = {
    0: {
        0: ((1, 3, 0, '', 'y'), (1, 3, 1, '', 'r')),
        1: ((1, 2, 0, '', 'y'), (1, 2, 1, '', 'y')),
        2: ((0, 3, 1, '', 'r'), (0, 3, 0, 'y', 'r')),
        3: ((1, 1, 0, '', 'y'), (1, 1, 1, '', 'y')),
        4: ((0, 2, 0, 'y', 'r'),),
        5: ((0, 2, 1, 'y', 'r'), (1, 0, 0, '', 'y')),
        6: ((1, 0, 1, 'r', 'y'), (0, 1, 0, 'y', 'r')),
        7: ((0, 1, 1, 'y', 'r'), (0, 0, 0, 'ry', ''), (0, 0, 1, 'ry', '')),
    },
    1: {
        0: ((1, 3, 0, '', 'y'),),
        1: ((1, 2, 0, '', 'y'), (1, 2, 1, '', 'y')),
        2: ((1, 3, 1, 'l', 'r'),),
        3: ((1, 0, 0, '', 'y'),),
        4: ((0, 3, 1, 'l', 'r'), (1, 0, 1, 'r', 'l'), (1, 1, 0, '', 'y'), (1, 1, 1, '', 'y')),
        6: ((0, 3, 0, 'ly', 'r'), (0, 0, 1, 'r', 'l')),
        7: ((0, 2, 0, 'ly', 'r'), (0, 0, 0, 'ry', 'l'), (0, 2, 1, 'ly', 'r'), (0, 1, 0, 'lry', ''), (0, 1, 1, 'lry', '')),
    },
    2: {
        0: ((1, 0, 0, '', 'y'),),
        1: ((1, 1, 0, '', 'y'), (1, 1, 1, '', 'y')),
        2: ((1, 0, 1, 'r', 'l'), (1, 3, 0, '', 'y')),
        4: ((1, 3, 1, 'l', 'r'), (0, 0, 1, 'r', 'l'), (1, 2, 0, '', 'y'), (1, 2, 1, '', 'y')),
        6: ((0, 0, 0, 'ry', 'l'), (0, 3, 1, 'l', 'r')),
        7: ((0, 1, 0, 'ry', 'l'), (0, 3, 0, 'ly', 'r'), (0, 1, 1, 'ry', 'l'), (0, 2, 0, 'lry', ''), (0, 2, 1, 'lry', '')),
    },
    3: {
        0: ((1, 0, 0, '', 'y'), (1, 0, 1, '', 'l')),
        1: ((1, 1, 0, '', 'y'), (1, 1, 1, '', 'y')),
        2: ((0, 0, 1, '', 'l'), (0, 0, 0, 'y', 'l')),
        3: ((1, 2, 0, '', 'y'), (1, 2, 1, '', 'y')),
        4: ((0, 1, 0, 'y', 'l'),),
        5: ((0, 1, 1, 'y', 'l'), (1, 3, 0, '', 'y')),
        6: ((1, 3, 1, 'l', 'y'), (0, 2, 0, 'y', 'l')),
        7: ((0, 2, 1, 'y', 'l'), (0, 3, 0, 'ly', ''), (0, 3, 1, 'ly', '')),
    },
}
SUB = 256
GROUP = 6


def lookup(table, z, step):
    value = jnp.int32(0)
    for k in range(NZ):
        for s in range(2 * NZ):
            value = value + jnp.where((z == k) & (step == s), table[k][s], 0)
    return value


def head_kernel(scale, token_scale, f_ref, lab_ref, e_ref, dfin_ref, ghead_ref, norm_ref, labsum_ref, z_ref,
                e_b, e_t, fbuf, f_b, g_acc, from_y, from_l, from_r, dl, z_buf, z_rest, lse_all, z_sem, load_sem, ag_send, ag_recv,
                send_y, send_l, send_r, recv_y, recv_l, recv_r, st_send, st_recv):
    tp, dp, z, y = place()
    partner = tp + 1 - 2 * y
    vocab, width = e_ref.shape
    own = f_ref.shape[0]
    whole = vocab // (SUB * GROUP)
    rest = vocab - whole * SUB * GROUP
    log2e = 1.4426950408889634
    slope = scale * log2e
    blocks = [(j * SUB, SUB) for j in range(GROUP)]
    tail = [(n, min(SUB, rest - n)) for n in range(0, rest, SUB)]

    plane_barrier(tp, dp, [])

    half = own // 2
    to_tp = {"l": tp - 2, "r": tp + 2, "y": partner}

    def slot_of(o, zz):
        return 2 * zz + (1 - y if o else y)

    def piece(ref, h):
        return ref.at[pl.ds(h * half, half), :]

    def pass_on(o, zz, h, to, own_chunk=False):
        slot = slot_of(o, zz)
        return remote(piece(f_ref if own_chunk else fbuf.at[slot], h), piece(fbuf.at[slot], h), ag_send.at["lry".index(to), slot, h],
                      ag_recv.at[slot, h], to_tp[to], dp)

    def arrived(o, zz, h):
        slot = slot_of(o, zz)
        remote(piece(f_ref, h), piece(fbuf.at[slot], h), ag_send.at[0, slot, h], ag_recv.at[slot, h], partner, dp).wait_recv()

    def own_sends(k):
        first = (1, 0) if k in (0, NZ - 1) else (0, 1)
        return [pass_on(0, k, h, "y", True) for h in first] + [
            pass_on(0, k, h, to, True) for h in range(2) for to in ("l" if k > 0 else "") + ("r" if k < NZ - 1 else "")]

    def on_position(f):
        for k in range(NZ):
            pl.when(z == k)(functools.partial(f, k))

    def first_sends(k):
        for c in own_sends(k):
            c.start()

    on_position(first_sends)
    load = pltpu.make_async_copy(e_ref, g_acc, load_sem.at[0])
    load.start()
    own_copy = pltpu.make_async_copy(f_ref, fbuf.at[tp], load_sem.at[1])
    own_copy.start()
    load.wait()

    def prepare(at, size):
        part = g_acc[at, :]
        e_b[at, :] = part.astype(BF16)
        e_t[:, at] = part.T.astype(BF16)

    def prepare_body(n, carry):
        prepare(pl.ds(pl.multiple_of(n * SUB, SUB), SUB), SUB)
        return carry

    lax.fori_loop(0, vocab // SUB, prepare_body, 0)
    if vocab % SUB:
        prepare(pl.ds(vocab // SUB * SUB, vocab % SUB), vocab % SUB)
    own_copy.wait()

    big = SUB * GROUP

    def z_copies(slot, n, out):
        if n is None:
            pair = (z_rest, z_ref.at[slot, pl.ds(whole * big, rest), :])
            sem = z_sem.at[2]
        else:
            pair = (z_buf.at[lax.rem(n, 2)], z_ref.at[slot, pl.ds(pl.multiple_of(n * big, big), big), :])
            sem = z_sem.at[lax.rem(n, 2)]
        return pltpu.make_async_copy(*(pair if out else pair[::-1]), sem)

    def slot_at(order, step):
        code = lookup({k: [2 * zz + o for o, zz in order[k]] for k in range(NZ)}, z, step)
        other = code % 2
        return code // 2 * 2 + y + other - 2 * y * other

    def gather_step(step, carry):
        for k in range(NZ):
            for at, events in GATHER_EVENTS[k].items():
                def serve(events=events):
                    for o, zz, h, to in events:
                        arrived(o, zz, h)
                        for t in to:
                            pass_on(o, zz, h, t).start()
                pl.when((z == k) & (step == at))(serve)
        slot = slot_at(GATHER_ORDER, step)
        f_b[slot] = fbuf[slot].astype(BF16)
        f_now = f_b[slot]

        def group(base, parts, kept, c):
            top, total = c
            for first, size in parts:
                logit = lax.dot_general(e_b[pl.ds(base + first, size), :], f_now, (((1,), (1,)), ((), ())), preferred_element_type=F32)
                kept[pl.ds(first, size), :] = logit
                logit = logit.reshape(size // 8, 8, own)
                new = jnp.maximum(top, jnp.max(logit, axis=0))
                total = total * jnp.exp2((top - new) * slope) + jnp.sum(jnp.exp2((logit - new[None]) * slope), axis=0)
                top = new
            return top, total

        def body(n, c):
            @pl.when(step * whole + n >= 2)
            def _():
                z_copies(slot, n, True).wait()
            c = group(pl.multiple_of(n * big, big), blocks, z_buf.at[lax.rem(n, 2)], c)
            z_copies(slot, n, True).start()
            return c

        top, total = lax.fori_loop(0, whole, body, (jnp.full((8, own), -3e38, F32), jnp.zeros((8, own), F32)))
        if tail:
            @pl.when(step > 0)
            def _():
                z_copies(slot, None, True).wait()
            top, total = group(whole * big, tail, z_rest, (top, total))
            z_copies(slot, None, True).start()
        most = jnp.max(top, axis=0, keepdims=True)
        total = jnp.sum(total * jnp.exp2((top - most) * slope), axis=0, keepdims=True)
        lse_all[tp, pl.ds(slot, 1), :] = most * scale + jnp.log(total)
        return carry

    lax.fori_loop(0, 2 * NZ, gather_step, 0)
    for n in range(2):
        z_copies(0, jnp.int32(n), True).wait()
    if tail:
        z_copies(0, None, True).wait()

    for n in range(1, 2 * NZ):
        to = lax.rem(tp + n, 2 * NZ)
        remote(lse_all.at[tp], lse_all.at[tp], st_send.at[to], st_recv.at[tp], to, dp).start()

    def gathers_done(k):
        for c in own_sends(k):
            c.wait_send()
        for events in GATHER_EVENTS[k].values():
            for o, zz, h, to in events:
                for t in to:
                    pass_on(o, zz, h, t).wait_send()

    on_position(gathers_done)
    start_slot = slot_at(SCATTER_ORDER, 0)
    for n in range(2):
        z_copies(start_slot, jnp.int32(n), False).start()
    if tail:
        z_copies(start_slot, None, False).start()

    def clear(n, carry):
        g_acc[pl.ds(pl.multiple_of(n * 16, 16), 16), :] = jnp.zeros((16, width), F32)
        return carry

    lax.fori_loop(0, vocab // 16, clear, 0)
    for n in range(1, 2 * NZ):
        source = lax.rem(tp + n, 2 * NZ)
        remote(lse_all.at[source], lse_all.at[source], st_send.at[source], st_recv.at[source], source, dp).wait_recv()
    peak = jnp.max(lse_all[...], axis=0)
    log_norm = peak + jnp.log(jnp.sum(jnp.exp(lse_all[...] - peak[None]), axis=0))
    norm_ref[...] = log_norm

    def leave(o, zz, h, to):
        src = piece(fbuf.at[slot_of(o, zz)], h)
        if to == "y":
            at = 2 * zz + h
            return remote(src, from_y.at[at], send_y.at[at], recv_y.at[at], partner, dp)
        if to == "l":
            at = 6 if o else 2 * zz + h
            return remote(src, from_r.at[at], send_l.at[at], recv_r.at[at], tp - 2, dp)
        at = 6 if o else 2 * zz - 2 + h
        return remote(src, from_l.at[at], send_r.at[at], recv_l.at[at], tp + 2, dp)

    def collect(o, zz, h, sums, to):
        here = piece(fbuf.at[slot_of(o, zz)], h)
        for d in sums:
            at, buf, sem = {"y": (2 * zz + h, from_y, recv_y), "l": (6 if o else 2 * zz - 2 + h, from_l, recv_l),
                            "r": (6 if o else 2 * zz + h, from_r, recv_r)}[d]
            remote(here, buf.at[at], send_y.at[0], sem.at[at], partner, dp).wait_recv()
            add_into(here, buf.at[at])
        if to:
            leave(o, zz, h, to).start()

    def scatter_step(step, lab_sum):
        slot = slot_at(SCATTER_ORDER, step)
        f_now = f_b[slot]
        acc = fbuf.at[slot]
        norm = norm_ref[pl.ds(slot, 1), :]
        shift = norm * log2e
        coef = (1.0 + 2.0 * LOGIT_ZLOSS * norm) * token_scale
        lab = lab_ref[pl.ds(slot, 1), :]
        acc[...] = jnp.zeros((width, own), F32)

        def group(base, parts, kept, hits):
            for first, size in parts:
                at = pl.ds(base + first, size)
                logit = kept[pl.ds(first, size), :]
                hit = lax.broadcasted_iota(jnp.int32, (size, own), 0) == lab - (base + first)
                prob = jnp.exp2(logit * slope - shift) * coef
                grad = jnp.where(hit, prob - token_scale, prob).astype(BF16)
                hits = hits + jnp.sum(jnp.where(hit, logit, 0.0).reshape(size // 8, 8, own), axis=0)
                dl[pl.ds(first, size), :] = grad
                g_acc[at, :] += jnp.dot(grad, f_now, preferred_element_type=F32)
            size = parts[-1][0] + parts[-1][1]
            acc[...] += jnp.dot(e_t[:, pl.ds(base, size)], dl[pl.ds(0, size), :], preferred_element_type=F32)
            return hits

        following = slot_at(SCATTER_ORDER, jnp.minimum(step + 1, 2 * NZ - 1))

        def body(n, hits):
            z_copies(slot, n, False).wait()
            hits = group(pl.multiple_of(n * big, big), blocks, z_buf.at[lax.rem(n, 2)], hits)

            @pl.when(n + 2 < whole)
            def _():
                z_copies(slot, n + 2, False).start()

            @pl.when((n + 2 >= whole) & (step + 1 < 2 * NZ))
            def _():
                z_copies(following, n + 2 - whole, False).start()
            return hits

        lab_sum = lax.fori_loop(0, whole, body, lab_sum)
        if tail:
            z_copies(slot, None, False).wait()
            lab_sum = group(whole * big, tail, z_rest, lab_sum)

            @pl.when(step + 1 < 2 * NZ)
            def _():
                z_copies(following, None, False).start()

        for k in range(NZ):
            for at, events in SCATTER_EVENTS[k].items():
                def reduce(events=events):
                    for event in events:
                        collect(*event)
                pl.when((z == k) & (step == at))(reduce)
        return lab_sum

    lab_sum = lax.fori_loop(0, 2 * NZ, scatter_step, jnp.zeros((8, own), F32))
    labsum_ref[...] = lab_sum
    store = pltpu.make_async_copy(g_acc, ghead_ref, load_sem.at[0])
    store.start()
    dfin_ref[...] = fbuf[tp].T

    def scatters_done(k):
        for events in SCATTER_EVENTS[k].values():
            for o, zz, h, _, to in events:
                if to:
                    leave(o, zz, h, to).wait_send()

    on_position(scatters_done)
    for n in range(1, 2 * NZ):
        to = lax.rem(tp + n, 2 * NZ)
        remote(lse_all.at[tp], lse_all.at[tp], st_send.at[to], st_recv.at[tp], to, dp).wait_send()
    store.wait()


def head(f_own, labels, embed, scale, token_scale, collective_id):
    own, width = f_own.shape
    vocab = embed.shape[0]
    chunk = (own, width)
    strips = lambda n: pltpu.VMEM((n, own // 2, width), F32)
    dma = lambda *n: pltpu.SemaphoreType.DMA(n)
    return pl.pallas_call(
        functools.partial(head_kernel, scale, token_scale),
        out_shape=(jax.ShapeDtypeStruct((own, width), F32), jax.ShapeDtypeStruct((vocab, width), F32),
                   jax.ShapeDtypeStruct((2 * NZ, own), F32), jax.ShapeDtypeStruct((8, own), F32),
                   jax.ShapeDtypeStruct((2 * NZ, vocab, own), F32)),
        in_specs=[VMEM, VMEM, ANY],
        out_specs=(VMEM, ANY, VMEM, VMEM, ANY),
        scratch_shapes=[pltpu.VMEM((vocab, width), BF16), pltpu.VMEM((width, vocab), BF16),
                        pltpu.VMEM((2 * NZ,) + chunk, F32), pltpu.VMEM((2 * NZ,) + chunk, BF16), pltpu.VMEM((vocab, width), F32),
                        strips(8), strips(7), strips(7),
                        pltpu.VMEM((SUB * GROUP, own), BF16), pltpu.VMEM((2, SUB * GROUP, own), F32),
                        pltpu.VMEM((max(vocab % (SUB * GROUP), 8), own), F32), pltpu.VMEM((2 * NZ, 2 * NZ, own), F32),
                        dma(3), dma(2), dma(3, 2 * NZ, 2), dma(2 * NZ, 2), dma(8), dma(7), dma(7), dma(8), dma(7), dma(7), dma(2 * NZ), dma(2 * NZ)],
        compiler_params=pltpu.CompilerParams(collective_id=collective_id, has_side_effects=True, vmem_limit_bytes=67000000),
        cost_estimate=pl.CostEstimate(flops=8 * vocab * width * own * 8, bytes_accessed=3 * 4 * vocab * width, transcendentals=2 * vocab * own * 8),
        name="head",
    )(f_own, labels, embed)


TB = (((1,), (1,)), ((), ()))
TA = (((0,), (0,)), ((), ()))
LOG2E = 1.4426950408889634


def mm(a, b, dims=(((1,), (0,)), ((), ()))):
    return lax.dot_general(a, b, dims, preferred_element_type=F32)


def turn(lo, hi, cos_t, sin_t):
    return lo * cos_t - hi * sin_t, hi * cos_t + lo * sin_t


EVENTS = {
    0: (((("R", 1),), (0,)), ((("R", 2),), (1,)), ((("R", 3),), (2,)), ((), (3,))),
    1: (((("L", 0), ("R", 2)), (1,)), ((("R", 3),), (0,)), ((), (2,)), ((), (3,))),
    2: (((("R", 3), ("L", 1)), (2,)), ((("L", 0),), (3,)), ((), (1,)), ((), (0,))),
    3: (((("L", 2),), (3,)), ((("L", 1),), (2,)), ((("L", 0),), (1,)), ((), (0,))),
}
MLP_ORDER = {k: [2 * k] + [code for line, other in EVENTS[k] for code in [2 * zz for _, zz in line] + [2 * zz + 1 for zz in other]] for k in range(NZ)}


def front_kernel(ids_ref, e_ref, pick_ref, extra_ref, w_ref, wkv_ref, ln_ref, cos_ref, sin_ref,
                 f_ref, x1_ref, x0_ref, q_ref, kv_ref, kvt_ref, lse_ref, ctx_ref, wq_ref, wo_ref, wg_ref, wu_ref, wd_ref,
                 table, rows_ref, wl, rows_in, u_b, kv_out, kv_in, own_sem, r_send, r_recv, a_y, a_l, a_r, a_c, a_recv,
                 b_y, b_l, b_r, b_x, b_c, b_recv, kv_send, kv_recv):
    tp, dp, z, y = place()
    partner = tp + 1 - 2 * y
    core = dp % 2
    twin = dp + 1 - 2 * core
    facing = lax.rem(dp + 2, 4)
    own, width = x0_ref.shape
    shards, w_rows = wl.shape[0], wl.shape[1]
    nq = q_ref.shape[0]
    ff = wg_ref.shape[0]
    n_a = nq // shards
    n_f = ff // shards
    n_b = 3 * n_f // 4
    hd = kv_out.shape[0] // 2
    quarter = hd // 2
    heads = nq // hd

    def a_rows(c):
        return pl.ds(pl.multiple_of(c * n_a, 8), n_a)

    def b_rows(d):
        return pl.ds(pl.multiple_of(2 * n_a + d * n_b, 8), n_b)

    def a_copy(slot, sems, to, to_dp, first=False):
        src = w_ref.at[a_rows(core), :] if first else wl.at[slot, a_rows(core), :]
        return remote(src, wl.at[slot, a_rows(core), :], sems.at[slot], a_recv.at[slot, core], to, to_dp)

    def b_copy(slot, piece, sems, to, to_dp, first=False):
        src = w_ref.at[b_rows(piece), :] if first else wl.at[slot, b_rows(piece), :]
        return remote(src, wl.at[slot, b_rows(piece), :], sems.at[slot], b_recv.at[slot, piece], to, to_dp)

    def a_wait(slot, c):
        remote(w_ref.at[a_rows(c), :], wl.at[slot, a_rows(c), :], a_y.at[slot], a_recv.at[slot, c], partner, dp).wait_recv()

    def b_wait(slot, piece):
        remote(w_ref.at[b_rows(piece), :], wl.at[slot, b_rows(piece), :], b_y.at[slot], b_recv.at[slot, piece], partner, dp).wait_recv()

    def on_position(f):
        for k in range(NZ):
            pl.when(z == k)(functools.partial(f, k))

    def line_sends(k, make, y_sems, l_sems, r_sems, slot, side, first=False):
        sends = [make(slot, y_sems, partner, dp, first)]
        if k > 0 and side != "L":
            sends.append(make(slot, l_sems, tp - 2, dp, first))
        if k < NZ - 1 and side != "R":
            sends.append(make(slot, r_sems, tp + 2, dp, first))
        return sends

    def b_own(slot, sems, to, to_dp, first=False):
        return b_copy(slot, dp, sems, to, to_dp, first)

    def a_sends(k, slot, side, first=False):
        return line_sends(k, a_copy, a_y, a_l, a_r, slot, side, first)

    def b_sends(k, slot, side, first=False):
        return line_sends(k, b_own, b_y, b_l, b_r, slot, side, first)

    def start(copies):
        for c in copies:
            c.start()

    load = pltpu.make_async_copy(e_ref, table, own_sem.at[2])
    load.start()
    plane_barrier(tp, dp, [(tp, twin), (tp, facing)])
    peers = [lax.rem(tp + n, shards) for n in range(1, shards)]

    def row_copy(to):
        return remote(rows_ref.at[to], rows_in.at[tp], r_send.at[to], r_recv.at[tp], to, dp)

    on_position(lambda k: start(b_sends(k, tp, "", True)))
    on_position(lambda k: start(a_sends(k, tp, "", True)))
    own_w = pltpu.make_async_copy(w_ref, wl.at[tp], own_sem.at[1])
    own_w.start()

    def a_event(t, k):
        line, other = EVENTS[k][t]
        for side, zz in line:
            slot = 2 * zz + y
            a_wait(slot, core)
            start(a_sends(k, slot, side))
            a_copy(slot, a_c, tp, twin).start()
        for zz in other:
            slot = 2 * zz + 1 - y
            a_wait(slot, core)
            a_copy(slot, a_c, tp, twin).start()

    def b_event(t, k):
        line, other = EVENTS[k][t]
        for side, zz in line:
            slot = 2 * zz + y
            b_wait(slot, dp)
            start(b_sends(k, slot, side))
            b_copy(slot, dp, b_x, tp, facing).start()
            b_copy(slot, dp, b_c.at[0], tp, twin).start()
        for zz in other:
            slot = 2 * zz + 1 - y
            b_wait(slot, dp)
            b_copy(slot, dp, b_x, tp, facing).start()
            b_copy(slot, dp, b_c.at[0], tp, twin).start()

    load.wait()
    cap = rows_ref.shape[1]

    def pick_rows(n, carry):
        for i in range(8):
            rows_ref[n // (cap // 8), pl.ds(lax.rem(n, cap // 8) * 8 + i, 1), :] = table[pl.ds(ids_ref[n * 8 + i], 1), :]
        return carry

    lax.fori_loop(0, shards * cap // 8, pick_rows, 0)
    on_position(functools.partial(b_event, 0))
    on_position(functools.partial(a_event, 0))
    start([row_copy(to) for to in peers])
    own_rows = pltpu.make_async_copy(rows_ref.at[tp], rows_in.at[tp], own_sem.at[0])
    own_rows.start()
    on_position(functools.partial(b_event, 1))
    on_position(functools.partial(a_event, 1))
    own_rows.wait()
    for source in peers:
        remote(rows_ref.at[source], rows_in.at[source], r_send.at[source], r_recv.at[source], source, dp).wait_recv()
    x0_ref[...] = extra_ref[...] + mm(pick_ref[...], rows_in[...].reshape(pick_ref.shape[1], width).astype(BF16))
    u_b[...] = norm_fwd(x0_ref[...], ln_ref[0:1, :])[0]
    x1_ref[...] = x0_ref[...]
    cos_t = cos_ref[...]
    sin_t = sin_ref[...]
    kv = mm(wkv_ref[...], u_b[...], TB)
    lo, hi = turn(kv[:quarter], kv[quarter:hd], cos_t, sin_t)
    kv_out[0:quarter, :] = lo
    kv_out[quarter:hd, :] = hi
    kv_out[hd:, :] = kv[hd:]
    kv_copy = remote(kv_out, kv_in, kv_send, kv_recv, partner, dp)
    kv_copy.start()

    def slot_of(step):
        code = lookup(MLP_ORDER, z, step)
        other = code % 2
        return code // 2 * 2 + y + other - 2 * y * other

    def mlp(step, carry):
        def pass_on():
            slot = slot_of(step + 1)
            b_wait(slot, facing)
            b_copy(slot, facing, b_c.at[1], tp, twin).start()
        pl.when(step < shards - 1)(pass_on)
        slot = slot_of(step)

        def rest():
            b_wait(slot, twin)
            b_wait(slot, lax.rem(twin + 2, 4))
        pl.when(step > 0)(rest)
        at = pl.ds(pl.multiple_of(slot * n_f, n_f), n_f)
        wg_ref[at, :] = wl[slot, 2 * n_a:2 * n_a + n_f, :].astype(BF16)
        wu_ref[at, :] = wl[slot, 2 * n_a + n_f:2 * n_a + 2 * n_f, :].astype(BF16)
        wd_ref[at, :] = wl[slot, 2 * n_a + 2 * n_f:2 * n_a + 3 * n_f, :].astype(BF16)
        gate = mm(u_b[...], wg_ref[at, :], TB)
        up = mm(u_b[...], wu_ref[at, :], TB)
        x1_ref[...] += mm((gate * jax.nn.sigmoid(gate) * up).astype(BF16), wd_ref[at, :])
        return carry

    own_w.wait()
    lax.fori_loop(0, 3, mlp, 0)
    on_position(functools.partial(b_event, 2))
    on_position(functools.partial(a_event, 2))
    lax.fori_loop(3, 4, mlp, 0)
    on_position(functools.partial(a_event, 3))
    on_position(functools.partial(b_event, 3))
    for source in peers:
        a_wait(source, 1 - core)
    for s in range(shards):
        wq_ref[s * n_a:(s + 1) * n_a, :] = wl[s, 0:n_a, :].astype(BF16)
        wo_ref[s * n_a:(s + 1) * n_a, :] = wl[s, n_a:2 * n_a, :].astype(BF16)

    q_all = mm(wq_ref[...], u_b[...], TB)
    for h in range(heads):
        lo, hi = turn(q_all[h * hd:h * hd + quarter], q_all[h * hd + quarter:(h + 1) * hd], cos_t, sin_t)
        q_ref[h * hd:h * hd + quarter, :] = lo.astype(BF16)
        q_ref[h * hd + quarter:(h + 1) * hd, :] = hi.astype(BF16)
    kv_copy.wait()

    def fill(mine, other):
        kv_ref[mine * own:(mine + 1) * own, :] = kv_out[...].T.astype(BF16)
        kv_ref[other * own:(other + 1) * own, :] = kv_in[...].T.astype(BF16)
        kvt_ref[:, mine * own:(mine + 1) * own] = kv_out[...].astype(BF16)
        kvt_ref[:, other * own:(other + 1) * own] = kv_in[...].astype(BF16)

    pl.when(y == 0)(lambda: fill(0, 1))
    pl.when(y == 1)(lambda: fill(1, 0))
    blank = jnp.zeros((hd, own), BF16)
    slope = hd ** -0.5 * LOG2E

    def attend(h, carry):
        at = pl.ds(pl.multiple_of(h * hd, hd), hd)
        scores = mm(kv_ref[...], jnp.concatenate([q_ref[at, :], blank], axis=0))
        allowed = lax.broadcasted_iota(jnp.int32, scores.shape, 0) <= lax.broadcasted_iota(jnp.int32, scores.shape, 1) + y * own
        scores = jnp.where(allowed, scores * slope, -1e30)
        top = jnp.max(scores, axis=0, keepdims=True)
        prob = jnp.exp2(scores - top)
        total = jnp.sum(prob, axis=0, keepdims=True)
        lse_ref[pl.ds(h, 1), :] = top + jnp.log2(total)
        ctx_ref[at, :] = mm(kvt_ref[hd:, :], (prob * (1.0 / total)).astype(BF16)).astype(BF16)
        return carry

    lax.fori_loop(0, heads, attend, 0)
    x1_ref[...] += mm(ctx_ref[...], wo_ref[...], TA)

    lax.fori_loop(4, shards, mlp, 0)
    f_ref[...] = norm_fwd(x1_ref[...], ln_ref[1:2, :])[0].astype(F32)

    def finish(k):
        done = a_sends(k, tp, "", True) + b_sends(k, tp, "", True)
        for line, other in EVENTS[k]:
            for side, zz in line:
                done += a_sends(k, 2 * zz + y, side) + b_sends(k, 2 * zz + y, side)
        for c in done:
            c.wait_send()

    on_position(finish)
    for to in peers:
        row_copy(to).wait_send()
        a_copy(to, a_c, tp, twin).wait_send()
        b_copy(to, dp, b_x, tp, facing).wait_send()
        b_copy(to, dp, b_c.at[0], tp, twin).wait_send()
        b_copy(to, facing, b_c.at[1], tp, twin).wait_send()


def front(ids, embed, pick, extra, w_rows, wkv_t, ln, cos_t, sin_t, n_q, collective_id):
    own, width = extra.shape
    two_hd = wkv_t.shape[0]
    shards = 2 * NZ
    ff = (w_rows.shape[0] * shards - 2 * n_q) // 3
    dma = lambda *n: pltpu.SemaphoreType.DMA(n)
    s = jax.ShapeDtypeStruct
    rows = (shards, ids.shape[0] // shards, width)
    return pl.pallas_call(
        front_kernel,
        out_shape=(s((own, width), F32),) * 3 + (s((n_q, own), BF16), s((2 * own, two_hd), BF16), s((two_hd, 2 * own), BF16),
                   s((2 * n_q // two_hd, own), F32), s((n_q, own), BF16), s((n_q, width), BF16), s((n_q, width), BF16))
        + (s((ff, width), BF16),) * 3,
        in_specs=[pl.BlockSpec(memory_space=pltpu.SMEM), ANY, VMEM, VMEM, ANY] + [VMEM] * 4,
        out_specs=(VMEM,) * 13,
        scratch_shapes=[pltpu.VMEM(embed.shape, F32), pltpu.VMEM(rows, F32), pltpu.VMEM((shards,) + w_rows.shape, F32), pltpu.VMEM(rows, F32), pltpu.VMEM((own, width), BF16),
                        pltpu.VMEM((two_hd, own), F32), pltpu.VMEM((two_hd, own), F32),
                        dma(3), dma(shards), dma(shards)] + [dma(shards)] * 4 + [dma(shards, 2)]
        + [dma(shards)] * 4 + [dma(2, shards), dma(shards, 4), pltpu.SemaphoreType.DMA, pltpu.SemaphoreType.DMA],
        compiler_params=pltpu.CompilerParams(collective_id=collective_id, has_side_effects=True, vmem_limit_bytes=60000000),
        name="front",
    )(ids, embed, pick, extra, w_rows, wkv_t, ln, cos_t, sin_t)


def layer_bwd_kernel(dfin_ref, x0_ref, x1_ref, loss_ref, ln_ref, cos_ref, sin_ref, wq_ref, wkv_ref, wo_ref, wg_ref, wu_ref, wd_ref,
                     q_ref, kv_ref, kvt_ref, lse_ref, ctx_ref, pick_ref, rows_ref, d0_ref, back_ref, d_one, d_b, u_b, dctx, dq, dkv, dkv_in,
                     hid, d_gate, d_up, rows_out, g_q, g_o, g_g, g_u, g_d, small, out_sem, send_sem, recv_sem, r_send, r_recv):
    tp, dp, _, y = place()
    partner = tp + 1 - 2 * y
    own, width = x0_ref.shape
    hd = kv_ref.shape[1] // 2
    quarter = hd // 2
    nq = q_ref.shape[0]
    heads = nq // hd
    ff = wg_ref.shape[0]
    shards = rows_ref.shape[0]
    plane_barrier(tp, dp, [])
    _, f_hat, f_inv = norm_fwd(x1_ref[...], ln_ref[1:2, :])
    d_in, g_fin = norm_bwd(dfin_ref[...], f_hat, f_inv, ln_ref[1:2, :])
    d_one[...] = d_in
    d_b[...] = d_in.astype(BF16)
    u_b[...] = norm_fwd(x0_ref[...], ln_ref[0:1, :])[0]
    dctx[...] = mm(wo_ref[...], d_b[...], TB).astype(BF16)
    cos_t = cos_ref[...]
    sin_t = sin_ref[...]
    blank = jnp.zeros((hd, own), BF16)
    slope = hd ** -0.5 * LOG2E
    dkv[...] = jnp.zeros_like(dkv)

    def attend(h, carry):
        at = pl.ds(pl.multiple_of(h * hd, hd), hd)
        q_pad = jnp.concatenate([q_ref[at, :], blank], axis=0)
        d_pad = jnp.concatenate([blank, dctx[at, :]], axis=0)
        scores = mm(kv_ref[...], q_pad)
        allowed = lax.broadcasted_iota(jnp.int32, scores.shape, 0) <= lax.broadcasted_iota(jnp.int32, scores.shape, 1) + y * own
        prob = jnp.where(allowed, jnp.exp2(scores * slope - lse_ref[pl.ds(h, 1), :]), 0.0)
        d_prob = mm(kv_ref[...], d_pad)
        mean = jnp.sum(d_prob * prob, axis=0, keepdims=True)
        d_score = (prob * (d_prob - mean) * hd ** -0.5).astype(BF16)
        dkv[...] += mm(d_score, q_pad, TB) + mm(prob.astype(BF16), d_pad, TB)
        d_q = mm(kvt_ref[0:hd, :], d_score)
        lo, hi = turn(d_q[:quarter], d_q[quarter:], cos_t, -sin_t)
        dq[at, :] = jnp.concatenate([lo, hi], axis=0).astype(BF16)
        return carry

    lax.fori_loop(0, heads, attend, 0)
    copy = remote(dkv.at[pl.ds(pl.multiple_of((1 - y) * own, own), own), :], dkv_in, send_sem, recv_sem, partner, dp)
    copy.start()

    d0_ref[...] = mm(dq[...], wq_ref[...], TA)
    step = min(512, ff)

    def mlp(n, carry):
        at = pl.ds(pl.multiple_of(n * step, step), step)
        gate = mm(wg_ref[at, :], u_b[...], TB)
        up = mm(wu_ref[at, :], u_b[...], TB)
        d_hidden = mm(wd_ref[at, :], d_b[...], TB)
        sig = jax.nn.sigmoid(gate)
        hid[at, :] = (gate * sig * up).astype(BF16)
        d_gate[at, :] = (d_hidden * up * sig * (1.0 + gate * (1.0 - sig))).astype(BF16)
        d_up[at, :] = (d_hidden * gate * sig).astype(BF16)
        d0_ref[...] += mm(d_gate[at, :], wg_ref[at, :], TA) + mm(d_up[at, :], wu_ref[at, :], TA)
        return carry

    lax.fori_loop(0, ff // step, mlp, 0)
    copy.wait()
    d_kv = (dkv[pl.ds(pl.multiple_of(y * own, own), own), :] + dkv_in[...]).T
    lo, hi = turn(d_kv[:quarter], d_kv[quarter:hd], cos_t, -sin_t)
    d_kv = jnp.concatenate([lo, hi, d_kv[hd:]], axis=0).astype(BF16)
    small[0:2 * hd, :] = mm(d_kv, u_b[...])
    d_u = d0_ref[...] + mm(d_kv, wkv_ref[...], TA)
    _, u_hat, u_inv = norm_fwd(x0_ref[...], ln_ref[0:1, :])
    d_in, g_in = norm_bwd(d_u, u_hat, u_inv, ln_ref[0:1, :])
    d_zero = d_one[...] + d_in
    d0_ref[...] = d_zero
    high = d_zero.astype(BF16)
    left = d_zero - high.astype(F32)
    middle = left.astype(BF16)
    low = (left - middle.astype(F32)).astype(BF16)
    rows_out[...] = (mm(pick_ref[...], high, TA) + mm(pick_ref[...], middle, TA) + mm(pick_ref[...], low, TA)).reshape(rows_out.shape)

    def row_copy(to):
        return remote(rows_out.at[to], back_ref.at[tp], r_send.at[to], r_recv.at[tp], to, dp)

    peers = [lax.rem(tp + n, shards) for n in range(1, shards)]
    for to in peers:
        row_copy(to).start()
    own_rows = pltpu.make_async_copy(rows_out.at[tp], back_ref.at[tp], out_sem.at[7 * 2 * NZ])
    own_rows.start()

    g_o[...] = mm(ctx_ref[...], d_b[...])
    g_q[...] = mm(dq[...], u_b[...])

    def weight_grads(n, carry):
        at = pl.ds(pl.multiple_of(n * step, step), step)
        g_d[at, :] = mm(hid[at, :], d_b[...])
        g_g[at, :] = mm(d_gate[at, :], u_b[...])
        g_u[at, :] = mm(d_up[at, :], u_b[...])
        return carry

    lax.fori_loop(0, ff // step, weight_grads, 0)
    small[2 * hd:, :] = jnp.zeros_like(small[2 * hd:, :])
    small[2 * hd:2 * hd + 1, :] = g_in.reshape(1, width)
    small[2 * hd + 1:2 * hd + 2, :] = g_fin.reshape(1, width)
    small[2 * hd + 2:2 * hd + 3, :] = loss_ref[...]
    copies = []

    def put(src, first, size, s):
        copies.append(pltpu.make_async_copy(src, rows_ref.at[s, pl.ds(first, size), :], out_sem.at[len(copies)]))

    n_kv = 2 * hd // shards
    for s in range(shards):
        at = 0
        for g, size in ((g_q, nq // shards), (g_o, nq // shards), (g_g, ff // shards), (g_u, ff // shards), (g_d, ff // shards)):
            put(g.at[pl.ds(s * size, size), :], at, size, s)
            at += size
        put(small.at[pl.ds(s * n_kv, n_kv), :], at, n_kv, s)
        put(small.at[pl.ds(2 * hd + (0 if s == 0 else 16), 16), :], at + n_kv, 16, s)
    for c in copies:
        c.start()
    for c in copies:
        c.wait()
    own_rows.wait()
    for source in peers:
        remote(rows_out.at[source], back_ref.at[source], r_send.at[source], r_recv.at[source], source, dp).wait_recv()
        row_copy(source).wait_send()


def layer_bwd(d_fin, x0, x1, loss_row, ln, cos_t, sin_t, weights, saved, pick, collective_id):
    own, width = x0.shape
    nq = weights[0].shape[0]
    two_hd = weights[1].shape[0]
    ff = weights[3].shape[0]
    rows = (2 * nq + 3 * ff + two_hd) // (2 * NZ) + 16
    chunk = (own, width)
    back = (2 * NZ, pick.shape[1] // (2 * NZ), width)
    return pl.pallas_call(
        layer_bwd_kernel,
        out_shape=(jax.ShapeDtypeStruct((2 * NZ, rows, width), F32), jax.ShapeDtypeStruct(chunk, F32), jax.ShapeDtypeStruct(back, F32)),
        in_specs=[VMEM] * 19,
        out_specs=(ANY, VMEM, ANY),
        scratch_shapes=[pltpu.VMEM(chunk, F32), pltpu.VMEM(chunk, BF16), pltpu.VMEM(chunk, BF16), pltpu.VMEM((nq, own), BF16),
                        pltpu.VMEM((nq, own), BF16), pltpu.VMEM((2 * own, two_hd), F32), pltpu.VMEM((own, two_hd), F32)]
        + [pltpu.VMEM((ff, own), BF16)] * 3 + [pltpu.VMEM(back, F32), pltpu.VMEM((nq, width), F32), pltpu.VMEM((nq, width), F32)] + [pltpu.VMEM((ff, width), F32)] * 3
        + [pltpu.VMEM((two_hd + 32, width), F32), pltpu.SemaphoreType.DMA((14 * NZ + 1,)), pltpu.SemaphoreType.DMA, pltpu.SemaphoreType.DMA,
           pltpu.SemaphoreType.DMA((2 * NZ,)), pltpu.SemaphoreType.DMA((2 * NZ,))],
        compiler_params=pltpu.CompilerParams(collective_id=collective_id, has_side_effects=True, vmem_limit_bytes=60000000),
        name="layer_bwd",
    )(d_fin, x0, x1, loss_row, ln, cos_t, sin_t, *weights, *saved, pick)


N_BLOCK = 12
EARLY = 9
W_REDUCE = {
    0: {1: (3,), 3: (2,), 5: (1,), 7: (0,)},
    1: {3: (3,), 5: (2, 0), 7: (1,)},
    2: {3: (0,), 5: (1, 3), 7: (2,)},
    3: {1: (0,), 3: (1,), 5: (2,), 7: (3,)},
}


def tail_kernel(g_ref, p_ref, rows_ref, ids_ref, t_ref, w_out, small_ref,
                s_buf, from_c, from_x, rows_c, ids_c, parts, acc, w_c, w_y, w_l, w_r, w_x,
                g_load, g_send_c, g_recv_c, g_send_x, g_recv_x, g_send_t, g_recv_t, g_store, l_send, l_recv,
                w_load, w_out_sem, send_c, send_y, send_l, send_r, recv_c, recv_y, recv_l, recv_r, last_send, last_recv, small_send, small_recv):
    tp, dp, z, y = place()
    partner = tp + 1 - 2 * y
    core = dp % 2
    twin = dp + 1 - 2 * core
    facing = lax.rem(dp + 2, 4)
    half = g_ref.shape[0] // 2
    size = s_buf.shape[1]
    last = half - (N_BLOCK - 1) * size
    n_look = rows_ref.shape[0]

    def rows(which, b, n):
        return pl.ds(pl.multiple_of(which * half + b * size, 8), n)

    def part(buf, b, n):
        return buf.at[b, pl.ds(0, n), :]

    plane_barrier(tp, dp, [(tp, twin), (tp, facing)])

    look_copies = [remote(rows_ref, rows_c, l_send.at[0], l_recv.at[0], tp, twin), remote(ids_ref, ids_c, l_send.at[1], l_recv.at[1], tp, twin)]
    for c in look_copies:
        c.start()

    def c_copy(b, n):
        return remote(g_ref.at[rows(1 - core, b, n), :], part(from_c, b, n), g_send_c.at[b], g_recv_c.at[b], tp, twin)

    def own_load(b, n):
        return pltpu.make_async_copy(g_ref.at[rows(core, b, n), :], part(s_buf, b, n), g_load.at[b])

    def x_copy(b, n):
        return remote(part(s_buf, b, n), part(from_x, b, n), g_send_x.at[b], g_recv_x.at[b], tp, facing)

    def t_copy(b, n):
        return remote(part(from_x, b, n), t_ref.at[rows(core, b, n), :], g_send_t.at[b], g_recv_t.at[b], tp, twin)

    def t_store(b, n):
        return pltpu.make_async_copy(part(from_x, b, n), t_ref.at[rows(core, b, n), :], g_store.at[b])

    def every(f, first, end):
        def body(b, carry):
            f(b, size)
            return carry
        lax.fori_loop(first, min(end, N_BLOCK - 1), body, 0)
        if end == N_BLOCK:
            f(N_BLOCK - 1, last)

    def chip_sum(b, n):
        own_load(b, n).wait()
        c_copy(b, n).wait_recv()
        ids = jnp.concatenate([ids_ref[...], ids_c[...]], axis=1) - (core * half + b * size)
        hit = (lax.broadcasted_iota(jnp.int32, (n, 2 * n_look), 0) == ids).astype(F32).astype(BF16)
        look = mm(hit, parts[0]) + mm(hit, parts[1]) + mm(hit, parts[2])
        s_buf[b, 0:n, :] = s_buf[b, 0:n, :] + from_c[b, 0:n, :] + look
        x_copy(b, n).start()

    def w_first(k):
        for zz in REDUCE_ORDER[k]:
            for slot in (2 * zz + 1 - y, 2 * zz + y):
                remote(p_ref.at[slot, 1 - core], w_c.at[slot], send_c.at[slot], recv_c.at[slot], tp, twin).start()
                pltpu.make_async_copy(p_ref.at[slot, core], acc.at[slot], w_load.at[slot]).start()

    def w_chip_sum(slot):
        pltpu.make_async_copy(p_ref.at[slot, core], acc.at[slot], w_load.at[slot]).wait()
        remote(acc.at[slot], w_c.at[slot], send_c.at[slot], recv_c.at[slot], tp, twin).wait_recv()
        add_into(acc.at[slot], w_c.at[slot])

    def w_second(k):
        for zz in REDUCE_ORDER[k]:
            slot = 2 * zz + 1 - y
            w_chip_sum(slot)
            remote(acc.at[slot], w_y.at[zz], send_y.at[zz], recv_y.at[zz], partner, dp).start()
        for zz in REDUCE_ORDER[k]:
            w_chip_sum(2 * zz + y)

    def w_reduce(k, shards):
        for zz in shards:
            line = acc.at[2 * zz + y]
            remote(line, w_y.at[zz], send_y.at[zz], recv_y.at[zz], partner, dp).wait_recv()
            add_into(line, w_y.at[zz])
            if zz >= k and k > 0:
                remote(line, w_l.at[zz - 1], send_l.at[zz], recv_l.at[zz], partner, dp).wait_recv()
                add_into(line, w_l.at[zz - 1])
            if zz <= k and k < NZ - 1:
                remote(line, w_r.at[zz], send_r.at[zz], recv_r.at[zz], partner, dp).wait_recv()
                add_into(line, w_r.at[zz])
            if zz > k:
                remote(line, w_l.at[zz - 1], send_r.at[zz], recv_l.at[zz], tp + 2, dp).start()
            if zz < k:
                remote(line, w_r.at[zz], send_l.at[zz], recv_r.at[zz], tp - 2, dp).start()

    def on_position(f):
        for k in range(NZ):
            pl.when(z == k)(functools.partial(f, k))

    def first(b, n):
        c_copy(b, n).start()
        own_load(b, n).start()

    every(first, 0, 4)
    on_position(w_first)
    every(first, 4, N_BLOCK)

    def split(at, value):
        high = value.astype(BF16)
        left = value - high.astype(F32)
        middle = left.astype(BF16)
        parts[0, at, :] = high
        parts[1, at, :] = middle
        parts[2, at, :] = (left - middle.astype(F32)).astype(BF16)

    split(pl.ds(0, n_look), rows_ref[...])
    for c in look_copies:
        c.wait()
    split(pl.ds(n_look, n_look), rows_c[...])
    every(chip_sum, 0, EARLY)
    on_position(w_second)

    total = acc.at[tp]
    w_copy_x = remote(total, w_x, last_send.at[0], last_recv.at[0], tp, facing)
    w_copy_c = remote(total, w_out.at[core], last_send.at[1], last_recv.at[1], tp, twin)
    w_store = pltpu.make_async_copy(total, w_out.at[core], w_out_sem)
    n_small, n_rows = small_ref.shape[1], w_out.shape[1]
    mine = w_out.at[1, pl.ds(n_rows - 32, n_small), :]
    small_here = pltpu.make_async_copy(mine, small_ref.at[tp], w_out_sem)
    peers = [lax.rem(tp + n, 2 * NZ) for n in range(1, 2 * NZ)]
    for b in range(N_BLOCK):
        n = last if b == N_BLOCK - 1 else size
        x_copy(b, n).wait_recv()
        add_into(part(from_x, b, n), part(s_buf, b, n), 24)
        t_copy(b, n).start()
        t_store(b, n).start()
        for k in range(NZ):
            if b in W_REDUCE[k]:
                pl.when(z == k)(functools.partial(w_reduce, k, W_REDUCE[k][b]))
        if b == 7:
            w_copy_x.start()
            every(chip_sum, EARLY, N_BLOCK)
        if b == 8:
            w_copy_x.wait()
            add_into(total, w_x)
            w_copy_c.start()
            w_store.start()
        if b == 9:
            w_copy_c.wait_send()
            remote(total, w_out.at[1 - core], last_send.at[1], last_recv.at[1], tp, twin).wait_recv()
            w_store.wait()
            for to in peers:
                remote(mine, small_ref.at[tp], small_send.at[to], small_recv.at[tp], to, dp).start()
            small_here.start()
    for source in peers:
        remote(small_ref.at[source], small_ref.at[source], small_send.at[source], small_recv.at[source], source, dp).wait_recv()
        remote(mine, small_ref.at[tp], small_send.at[source], small_recv.at[tp], source, dp).wait_send()
    small_here.wait()

    def w_done(k):
        for zz in range(NZ):
            line = acc.at[2 * zz + y]
            for slot in (2 * zz + 1 - y, 2 * zz + y):
                remote(p_ref.at[slot, 1 - core], w_c.at[slot], send_c.at[slot], recv_c.at[slot], tp, twin).wait_send()
            remote(line, w_y.at[zz], send_y.at[zz], recv_y.at[zz], partner, dp).wait_send()
            if zz > k:
                remote(line, w_l.at[zz - 1], send_r.at[zz], recv_l.at[zz], tp + 2, dp).wait_send()
            if zz < k:
                remote(line, w_r.at[zz], send_l.at[zz], recv_r.at[zz], tp - 2, dp).wait_send()

    on_position(w_done)

    def drain(b, n):
        c_copy(b, n).wait_send()
        x_copy(b, n).wait_send()
        t_copy(b, n).wait_send()
        t_store(b, n).wait()
        remote(part(from_x, b, n), t_ref.at[rows(1 - core, b, n), :], g_send_t.at[b], g_recv_t.at[b], tp, twin).wait_recv()

    every(drain, 0, N_BLOCK)


def tail(g_table, g_rows, look_rows, look_ids, collective_id):
    vocab, width = g_table.shape
    rows = g_rows.shape[1]
    half = (rows // 2, width)
    n_look = look_ids.shape[1]
    size = -(-vocab // (2 * N_BLOCK * 24)) * 24
    blocks = pltpu.VMEM((N_BLOCK, size, width), F32)
    dma = lambda *n: pltpu.SemaphoreType.DMA(n)
    t, w_sum, small = pl.pallas_call(
        tail_kernel,
        out_shape=(jax.ShapeDtypeStruct((vocab, width), F32), jax.ShapeDtypeStruct((2,) + half, F32), jax.ShapeDtypeStruct((2 * NZ, 24, width), F32)),
        in_specs=[ANY, ANY, VMEM, VMEM],
        out_specs=(ANY,) * 3,
        scratch_shapes=[blocks] * 3 + [pltpu.VMEM((n_look, width), F32), pltpu.VMEM((1, n_look), jnp.int32), pltpu.VMEM((3, 2 * n_look, width), BF16)]
        + [pltpu.VMEM((2 * NZ,) + half, F32)] * 2 + [pltpu.VMEM((NZ,) + half, F32)] + [pltpu.VMEM((NZ - 1,) + half, F32)] * 2
        + [pltpu.VMEM(half, F32)]
        + [dma(N_BLOCK)] * 8 + [dma(2)] * 2
        + [dma(2 * NZ), pltpu.SemaphoreType.DMA] + [dma(2 * NZ), dma(NZ), dma(NZ), dma(NZ)] * 2 + [dma(2)] * 2 + [dma(2 * NZ)] * 2,
        compiler_params=pltpu.CompilerParams(collective_id=collective_id, has_side_effects=True, vmem_limit_bytes=67000000),
        name="tail",
    )(g_table, g_rows.reshape((2 * NZ, 2) + half), look_rows.reshape(n_look, width), look_ids)
    return t, w_sum.reshape(rows, width), small


UPDATE_ROWS = 512


def update_kernel(t_ref, w_ref, small_ref, *refs):
    state = [refs[7 * i:7 * i + 7] for i in range(3)]
    new = [refs[21 + 7 * i:28 + 7 * i] for i in range(3)]
    loss_ref = refs[42]
    held, made, in_sem, out_sem = refs[43:]
    vocab = t_ref.shape[0]
    n_kv, hd = 2 * state[0][3].shape[1] // small_ref.shape[0], state[0][3].shape[1]
    blocks = [(at, min(UPDATE_ROWS, vocab - at)) for at in range(0, vocab, UPDATE_ROWS)]

    def loads(q):
        at, n = blocks[q]
        return [pltpu.make_async_copy(ref.at[pl.ds(at, n), :], held.at[q % 3, i, pl.ds(0, n), :], in_sem.at[q % 3, i])
                for i, ref in enumerate((t_ref, state[0][0], state[1][0], state[2][0]))]

    def stores(q):
        at, n = blocks[q]
        return [pltpu.make_async_copy(made.at[q % 2, i, pl.ds(0, n), :], new[i][0].at[pl.ds(at, n), :], out_sem.at[q % 2, i]) for i in range(3)]

    for q in range(3):
        for c in loads(q):
            c.start()

    def small_update(index, grad, *where):
        got = adam_update(state[0][index][where], grad, state[1][index][where], state[2][index][where])
        for i in range(3):
            new[i][index][where] = got[i]

    n_q, n_f = state[0][2].shape[0], state[0][6].shape[0]
    small_update(1, small_ref[0, n_kv:n_kv + 2, :], Ellipsis)
    small_update(2, w_ref[0:n_q, :], Ellipsis)
    kv = small_ref[:, 0:n_kv, :].reshape(2 * hd, small_ref.shape[2])
    for i in range(2):
        small_update(3, kv[i * hd:(i + 1) * hd], i)
    small_update(4, w_ref[n_q:2 * n_q, :], Ellipsis)
    for i in range(2):
        small_update(5, w_ref[2 * n_q + i * n_f:2 * n_q + (i + 1) * n_f, :].T, i)
    small_update(6, w_ref[2 * n_q + 2 * n_f:2 * n_q + 3 * n_f, :], Ellipsis)
    loss_ref[...] = jnp.sum(small_ref[0, n_kv + 2:n_kv + 3, :], axis=1, keepdims=True)

    for q, (at, n) in enumerate(blocks):
        for c in loads(q):
            c.wait()
        if q >= 2:
            for c in stores(q - 2):
                c.wait()
        step = 32 if n % 32 == 0 else 16

        def body(j, carry):
            rows = pl.ds(pl.multiple_of(j * step, step), step)
            got = adam_update(held[q % 3, 1, rows, :], held[q % 3, 0, rows, :], held[q % 3, 2, rows, :], held[q % 3, 3, rows, :])
            for i in range(3):
                made[q % 2, i, rows, :] = got[i]
            return carry

        lax.fori_loop(0, n // step, body, 0)
        for c in stores(q):
            c.start()
        if q + 3 < len(blocks):
            for c in loads(q + 3):
                c.start()
    for q in range(len(blocks) - 2, len(blocks)):
        for c in stores(q):
            c.wait()


def update(g_table, g_shard, g_small, state_arrays):
    specs = [ANY] + [VMEM] * 6
    width = g_table.shape[1]

    def flip(arrays):
        return [a.swapaxes(-1, -2) if i % 7 in (2, 3) else a for i, a in enumerate(arrays)]

    given = flip(state_arrays)
    *new, loss = pl.pallas_call(
        update_kernel,
        out_shape=tuple(jax.ShapeDtypeStruct(a.shape, F32) for a in given) + (jax.ShapeDtypeStruct((1, 1), F32),),
        in_specs=[ANY, VMEM, VMEM] + specs * 3,
        out_specs=tuple(specs * 3) + (VMEM,),
        scratch_shapes=[pltpu.VMEM((3, 4, UPDATE_ROWS, width), F32), pltpu.VMEM((2, 3, UPDATE_ROWS, width), F32),
                        pltpu.SemaphoreType.DMA((3, 4)), pltpu.SemaphoreType.DMA((2, 3))],
        compiler_params=pltpu.CompilerParams(vmem_limit_bytes=60000000),
        name="update",
    )(g_table, g_shard, g_small, *given)
    return flip(new) + [loss]


def norm_fwd(x_f32, scale):
    centered = x_f32 - jnp.mean(x_f32, axis=-1, keepdims=True)
    inv_std = lax.rsqrt(jnp.mean(centered * centered, axis=-1, keepdims=True) + LN_EPS)
    x_hat = centered * inv_std
    return (x_hat * scale).astype(BF16), x_hat, inv_std


def norm_bwd(d_out, x_hat, inv_std, scale):
    d_scale = jnp.sum(d_out * x_hat, axis=0)
    d_hat = d_out * scale
    d_in = inv_std * (d_hat - jnp.mean(d_hat, axis=-1, keepdims=True) - x_hat * jnp.mean(d_hat * x_hat, axis=-1, keepdims=True))
    return d_in, d_scale


def adam_update(param_in, grad_in, mom_in, vel_in):
    mom_new = BETA_ONE * mom_in + (1.0 - BETA_ONE) * grad_in
    vel_new = BETA_TWO * vel_in + (1.0 - BETA_TWO) * grad_in * grad_in
    return param_in - LEARN_RATE * mom_new / (jnp.sqrt(vel_new) + ADAM_EPS), mom_new, vel_new


def dot(spec, a, b):
    return jnp.einsum(spec, a, b, preferred_element_type=F32)


def solution(mesh):
    param_specs = (P('tp', None), P(None, None), P(None, 'tp'), P(None, None, None), P('tp', None), P(None, None, 'tp'), P('tp', None))
    n_tp = mesh.shape['tp']
    n_dp = mesh.shape['dp']

    def local_step(tokens, labels, *state_arrays):
        embed, ln_scales, w_q, w_kv, w_o, w_gu, w_down = state_arrays[0:7]
        batch_loc, seq_len = tokens.shape
        vocab_loc, d_model = embed.shape
        head_dim = w_kv.shape[2]
        q_loc = w_q.shape[1]
        f_loc = w_down.shape[0]
        tok_loc = batch_loc * seq_len
        tok_total = tok_loc * n_dp
        own = tok_loc // n_tp
        tp_rank = lax.axis_index('tp')
        half = tp_rank % 2

        strict = (jnp.arange(own)[:, None] > jnp.arange(own)[None, :]).astype(BF16)

        def routing(chunks):
            shard = chunks // vocab_loc
            row = chunks - shard * vocab_loc
            hot = (shard[:, :, None] == jnp.arange(n_tp)[None, None, :])
            before = dot('rs,nsj->nrj', strict, hot.astype(BF16))
            rank = jnp.sum(jnp.where(hot, before, 0.0), axis=-1).astype(jnp.int32)
            most = jnp.max(jnp.sum(hot.astype(jnp.int32), axis=1))
            return shard, row, rank, (most + CAP - 1) // CAP

        chunks = tokens.reshape(n_tp, own)
        shard, row, rank, rounds = routing(chunks)
        slots = jnp.arange(CAP)
        my_shard = lax.dynamic_index_in_dim(shard, tp_rank, 0, keepdims=False)
        my_rank = lax.dynamic_index_in_dim(rank, tp_rank, 0, keepdims=False)

        def fetch(step):
            here = (shard[:, None, :] == tp_rank) & (rank[:, None, :] == slots[None, :, None] + step * CAP)
            ids = jnp.sum(jnp.where(here, row[:, None, :], 0), axis=-1).reshape(-1)
            pick = (my_shard[:, None, None] == jnp.arange(n_tp)[None, :, None]) & (my_rank[:, None, None] == slots[None, None, :] + step * CAP)
            return ids, pick.reshape(own, n_tp * CAP).astype(BF16)

        def fetch_more(state):
            ids, pick = fetch(state[0])
            rows_in = plane_swap(jnp.take(embed, ids, axis=0).reshape(n_tp, CAP, d_model), 1).reshape(n_tp * CAP, d_model).astype(BF16)
            return state[0] + 1, state[1] + dot('rc,cd->rd', pick, rows_in)

        more_rows = lax.while_loop(lambda state: state[0] < rounds, fetch_more, (jnp.int32(1), jnp.zeros((own, d_model), F32)))[1]
        ids_first, pick_first = fetch(0)

        w_rows = jnp.concatenate([w_q.T, w_o, w_gu.transpose(0, 2, 1).reshape(2 * f_loc, d_model), w_down], axis=0)
        cuts = (q_loc, 2 * q_loc, 2 * q_loc + f_loc, 2 * q_loc + 2 * f_loc)
        wkv_t = w_kv.transpose(0, 2, 1).reshape(2 * head_dim, d_model).astype(BF16)
        inv_freq = ROPE_BASE ** (-jnp.arange(0, head_dim, 2).astype(F32) / head_dim)
        angles = inv_freq[:, None] * (half * own + jnp.arange(own)).astype(F32)[None, :]
        cos_t, sin_t = jnp.cos(angles), jnp.sin(angles)
        f_own, x_one, x_zero, *saved = front(ids_first, embed, pick_first, more_rows, w_rows, wkv_t, ln_scales, cos_t, sin_t, n_tp * q_loc, 0)
        saved, (wq_t, wo_b, wg_t, wu_t, wd_b) = saved[:5], saved[5:]
        weights = (wq_t, wkv_t, wo_b, wg_t, wu_t, wd_b)

        logit_scale = d_model ** -0.5
        lab_loc = labels.reshape(n_tp, own) - tp_rank * vocab_loc
        d_fin, g_head_part, log_norm, lab_sum, _ = head(f_own, lab_loc, embed, logit_scale, logit_scale / tok_total, 4)
        log_norm = lax.dynamic_index_in_dim(log_norm, tp_rank, 0, keepdims=False)
        loss_row = (log_norm + LOGIT_ZLOSS * log_norm * log_norm - jnp.sum(lab_sum, axis=0) * logit_scale) / tok_total
        g_rows, d_zero, rows_back = layer_bwd(d_fin, x_zero, x_one, loss_row[None, :], ln_scales, cos_t, sin_t, weights, saved, pick_first, 7)

        def row_ids(step):
            here = (shard[:, None, :] == tp_rank) & (rank[:, None, :] == slots[None, :, None] + step * CAP)
            return jnp.where(jnp.any(here, axis=-1), jnp.sum(jnp.where(here, row[:, None, :], 0), axis=-1), vocab_loc).reshape(-1)

        def give_back(state):
            mine = (my_shard[None, None, :] == jnp.arange(n_tp)[:, None, None]) & (my_rank[None, None, :] == slots[None, :, None] + state[0] * CAP)
            ids = jnp.sum(jnp.where(mine, jnp.arange(own)[None, None, :], 0), axis=-1).reshape(-1)
            rows_in = plane_swap(jnp.take(d_zero, ids, axis=0).reshape(n_tp, CAP, d_model), 9).reshape(-1, d_model)
            return state[0] + 1, state[1].at[row_ids(state[0])].add(rows_in, mode='drop')

        g_table = lax.while_loop(lambda state: state[0] < rounds, give_back, (jnp.int32(1), g_head_part))[1]
        g_table, g_shard, g_small = tail(g_table, g_rows, rows_back, row_ids(0)[None, :], 10)
        *new, loss = update(g_table, g_shard, g_small, state_arrays)
        return tuple(new) + (loss.reshape(()),)

    return jax.shard_map(local_step, mesh=mesh, in_specs=(P('dp', None), P('dp', None)) + param_specs * 3,
                         out_specs=param_specs * 3 + (P(),), check_vma=False)
```

```python
import functools

import jax
import jax.numpy as jnp
from jax import lax
from jax.experimental import pallas as pl
from jax.experimental.pallas import tpu as pltpu
from jax.sharding import PartitionSpec as P

LN_EPS = 1e-5
LOGIT_ZLOSS = 1e-4
LEARN_RATE = 1e-2
BETA_ONE = 0.9
BETA_TWO = 0.95
ADAM_EPS = 1e-8
ROPE_BASE = 10000.0
NZ = 4
CAP = 96
F32 = jnp.float32
BF16 = jnp.bfloat16
ANY = pl.BlockSpec(memory_space=pl.ANY)
VMEM = pl.BlockSpec(memory_space=pltpu.VMEM)

ARRIVALS = {
    0: (("R", 1), ("R", 2), ("R", 3)),
    1: (("L", 0), ("R", 2), ("R", 3)),
    2: (("R", 3), ("L", 1), ("L", 0)),
    3: (("L", 2), ("L", 1), ("L", 0)),
}
REDUCE_ORDER = {0: (3, 2, 1, 0), 1: (3, 0, 2, 1), 2: (0, 3, 1, 2), 3: (0, 1, 2, 3)}


def remote(src, dst, send_sem, recv_sem, tp, dp):
    return pltpu.make_async_remote_copy(src_ref=src, dst_ref=dst, send_sem=send_sem, recv_sem=recv_sem,
                                        device_id=(tp, dp), device_id_type=pl.DeviceIdType.MESH)


def place():
    tp = lax.axis_index("tp")
    dp = lax.axis_index("dp")
    return tp, dp, tp // 2, tp % 2


def signal(tp, dp):
    pl.semaphore_signal(pltpu.get_barrier_semaphore(), inc=1, device_id=(tp, dp), device_id_type=pl.DeviceIdType.MESH)


def add_into(acc, other, step=None):
    rows = acc.shape[0]
    step = step or (64 if rows % 64 == 0 else 8)

    def body(n, carry):
        at = pl.ds(pl.multiple_of(n * step, step), step)
        acc[at, :] = acc[at, :] + other[at, :]
        return carry

    lax.fori_loop(0, rows // step, body, 0)


def plane_barrier(tp, dp, others):
    peers = [(lax.rem(tp + n, 2 * NZ), dp) for n in range(1, 2 * NZ)] + others
    for peer in peers:
        signal(*peer)
    pl.semaphore_wait(pltpu.get_barrier_semaphore(), len(peers))


def swap_kernel(x_ref, out_ref, own_sem, send, recv):
    tp, dp, _, _ = place()
    plane_barrier(tp, dp, [])
    copies = []
    for n in range(1, 2 * NZ):
        to = lax.rem(tp + n, 2 * NZ)
        copy = remote(x_ref.at[to], out_ref.at[tp], send.at[to], recv.at[tp], to, dp)
        copy.start()
        copies.append(copy)
    own = pltpu.make_async_copy(x_ref.at[tp], out_ref.at[tp], own_sem)
    own.start()
    for n in range(1, 2 * NZ):
        source = lax.rem(tp + n, 2 * NZ)
        remote(out_ref.at[source], out_ref.at[source], send.at[source], recv.at[source], source, dp).wait_recv()
    own.wait()
    for copy in copies:
        copy.wait_send()


def plane_swap(x, collective_id):
    return pl.pallas_call(
        swap_kernel,
        out_shape=jax.ShapeDtypeStruct(x.shape, x.dtype),
        in_specs=[ANY],
        out_specs=ANY,
        scratch_shapes=[pltpu.SemaphoreType.DMA] + [pltpu.SemaphoreType.DMA((2 * NZ,))] * 2,
        compiler_params=pltpu.CompilerParams(collective_id=collective_id, has_side_effects=True),
        name="plane_swap",
    )(x)


def group_kernel(x_ref, out_ref, own_sem, send, recv):
    tp, dp, _, _ = place()
    group = [lax.rem(dp + n, 4) for n in range(1, 4)]
    for to in group:
        signal(tp, to)
    pl.semaphore_wait(pltpu.get_barrier_semaphore(), 3)
    own = pltpu.make_async_copy(x_ref, out_ref.at[dp], own_sem)
    own.start()
    for n, to in enumerate(group):
        remote(x_ref, out_ref.at[dp], send.at[n], recv.at[dp], tp, to).start()
    own.wait()
    for n, to in enumerate(group):
        remote(x_ref, out_ref.at[to], send.at[n], recv.at[to], tp, to).wait_recv()
        remote(x_ref, out_ref.at[dp], send.at[n], recv.at[dp], tp, to).wait_send()


def group_gather(x, collective_id):
    return pl.pallas_call(
        group_kernel,
        out_shape=jax.ShapeDtypeStruct((4,) + x.shape, x.dtype),
        in_specs=[ANY],
        out_specs=ANY,
        scratch_shapes=[pltpu.SemaphoreType.DMA, pltpu.SemaphoreType.DMA((3,)), pltpu.SemaphoreType.DMA((4,))],
        compiler_params=pltpu.CompilerParams(collective_id=collective_id, has_side_effects=True),
        name="group_gather",
    )(x)


GATHER_ORDER = {
    0: ((0, 0), (0, 1), (1, 0), (0, 2), (1, 1), (0, 3), (1, 2), (1, 3)),
    1: ((0, 1), (0, 0), (0, 2), (1, 1), (1, 0), (0, 3), (1, 2), (1, 3)),
    2: ((0, 2), (0, 1), (0, 3), (1, 2), (0, 0), (1, 3), (1, 1), (1, 0)),
    3: ((0, 3), (0, 2), (1, 3), (0, 1), (1, 2), (0, 0), (1, 1), (1, 0)),
}
GATHER_EVENTS = {
    0: {
        1: ((0, 1, 0, 'y'), (1, 0, 1, 'r'), (0, 1, 1, 'y'), (1, 0, 0, '')),
        3: ((0, 2, 0, 'y'), (1, 1, 0, ''), (0, 2, 1, 'y'), (1, 1, 1, '')),
        5: ((0, 3, 0, 'y'), (1, 2, 0, ''), (0, 3, 1, ''), (1, 2, 1, '')),
        7: ((1, 3, 0, ''), (1, 3, 1, '')),
    },
    1: {
        1: ((0, 0, 0, 'ry'), (0, 2, 0, 'ly'), (1, 1, 0, ''), (0, 0, 1, 'r'), (0, 2, 1, 'ly'), (1, 1, 1, '')),
        4: ((0, 3, 0, 'ly'), (1, 0, 0, ''), (1, 0, 1, 'r')),
        5: ((0, 3, 1, 'l'), (1, 2, 0, '')),
        6: ((1, 2, 1, ''), (1, 3, 1, 'l')),
        7: ((1, 3, 0, ''),),
    },
    2: {
        1: ((0, 1, 0, 'ry'), (0, 3, 0, 'ly'), (1, 2, 0, ''), (0, 1, 1, 'ry'), (0, 3, 1, 'l'), (1, 2, 1, '')),
        4: ((0, 0, 0, 'ry'), (1, 1, 0, ''), (1, 3, 1, 'l'), (0, 0, 1, 'r'), (1, 3, 0, '')),
        6: ((1, 0, 1, 'r'), (1, 1, 1, '')),
        7: ((1, 0, 0, ''),),
    },
    3: {
        1: ((0, 2, 0, 'y'), (1, 3, 1, 'l'), (0, 2, 1, 'y'), (1, 3, 0, '')),
        3: ((0, 1, 0, 'y'), (1, 2, 0, ''), (0, 1, 1, 'y'), (1, 2, 1, '')),
        5: ((0, 0, 0, 'y'), (1, 1, 0, ''), (0, 0, 1, ''), (1, 1, 1, '')),
        7: ((1, 0, 0, ''), (1, 0, 1, '')),
    },
}
SCATTER_ORDER = {
    0: ((1, 3), (1, 2), (0, 3), (1, 1), (0, 2), (1, 0), (0, 1), (0, 0)),
    1: ((1, 3), (1, 2), (0, 3), (1, 0), (1, 1), (0, 2), (0, 0), (0, 1)),
    2: ((1, 0), (1, 1), (1, 3), (0, 0), (1, 2), (0, 3), (0, 1), (0, 2)),
    3: ((1, 0), (1, 1), (0, 0), (1, 2), (0, 1), (1, 3), (0, 2), (0, 3)),
}
SCATTER_EVENTS = {
    0: {
        0: ((1, 3, 0, '', 'y'), (1, 3, 1, '', 'r')),
        1: ((1, 2, 0, '', 'y'), (1, 2, 1, '', 'y')),
        2: ((0, 3, 1, '', 'r'), (0, 3, 0, 'y', 'r')),
        3: ((1, 1, 0, '', 'y'), (1, 1, 1, '', 'y')),
        4: ((0, 2, 0, 'y', 'r'),),
        5: ((0, 2, 1, 'y', 'r'), (1, 0, 0, '', 'y')),
        6: ((1, 0, 1, 'r', 'y'), (0, 1, 0, 'y', 'r')),
        7: ((0, 1, 1, 'y', 'r'), (0, 0, 0, 'ry', ''), (0, 0, 1, 'ry', '')),
    },
    1: {
        0: ((1, 3, 0, '', 'y'),),
        1: ((1, 2, 0, '', 'y'), (1, 2, 1, '', 'y')),
        2: ((1, 3, 1, 'l', 'r'),),
        3: ((1, 0, 0, '', 'y'),),
        4: ((0, 3, 1, 'l', 'r'), (1, 0, 1, 'r', 'l'), (1, 1, 0, '', 'y'), (1, 1, 1, '', 'y')),
        6: ((0, 3, 0, 'ly', 'r'), (0, 0, 1, 'r', 'l')),
        7: ((0, 2, 0, 'ly', 'r'), (0, 0, 0, 'ry', 'l'), (0, 2, 1, 'ly', 'r'), (0, 1, 0, 'lry', ''), (0, 1, 1, 'lry', '')),
    },
    2: {
        0: ((1, 0, 0, '', 'y'),),
        1: ((1, 1, 0, '', 'y'), (1, 1, 1, '', 'y')),
        2: ((1, 0, 1, 'r', 'l'), (1, 3, 0, '', 'y')),
        4: ((1, 3, 1, 'l', 'r'), (0, 0, 1, 'r', 'l'), (1, 2, 0, '', 'y'), (1, 2, 1, '', 'y')),
        6: ((0, 0, 0, 'ry', 'l'), (0, 3, 1, 'l', 'r')),
        7: ((0, 1, 0, 'ry', 'l'), (0, 3, 0, 'ly', 'r'), (0, 1, 1, 'ry', 'l'), (0, 2, 0, 'lry', ''), (0, 2, 1, 'lry', '')),
    },
    3: {
        0: ((1, 0, 0, '', 'y'), (1, 0, 1, '', 'l')),
        1: ((1, 1, 0, '', 'y'), (1, 1, 1, '', 'y')),
        2: ((0, 0, 1, '', 'l'), (0, 0, 0, 'y', 'l')),
        3: ((1, 2, 0, '', 'y'), (1, 2, 1, '', 'y')),
        4: ((0, 1, 0, 'y', 'l'),),
        5: ((0, 1, 1, 'y', 'l'), (1, 3, 0, '', 'y')),
        6: ((1, 3, 1, 'l', 'y'), (0, 2, 0, 'y', 'l')),
        7: ((0, 2, 1, 'y', 'l'), (0, 3, 0, 'ly', ''), (0, 3, 1, 'ly', '')),
    },
}
SUB = 256
GROUP = 6


def lookup(table, z, step):
    value = jnp.int32(0)
    for k in range(NZ):
        for s in range(2 * NZ):
            value = value + jnp.where((z == k) & (step == s), table[k][s], 0)
    return value


def head_kernel(scale, token_scale, f_ref, lab_ref, e_ref, dfin_ref, ghead_ref, norm_ref, labsum_ref, z_ref,
                e_b, e_t, fbuf, f_b, g_acc, from_y, from_l, from_r, dl, z_buf, z_rest, lse_all, z_sem, load_sem, ag_send, ag_recv,
                send_y, send_l, send_r, recv_y, recv_l, recv_r, st_send, st_recv):
    tp, dp, z, y = place()
    partner = tp + 1 - 2 * y
    vocab, width = e_ref.shape
    own = f_ref.shape[0]
    whole = vocab // (SUB * GROUP)
    rest = vocab - whole * SUB * GROUP
    log2e = 1.4426950408889634
    slope = scale * log2e
    blocks = [(j * SUB, SUB) for j in range(GROUP)]
    tail = [(n, min(SUB, rest - n)) for n in range(0, rest, SUB)]

    plane_barrier(tp, dp, [])

    half = own // 2
    to_tp = {"l": tp - 2, "r": tp + 2, "y": partner}

    def slot_of(o, zz):
        return 2 * zz + (1 - y if o else y)

    def piece(ref, h):
        return ref.at[pl.ds(h * half, half), :]

    def pass_on(o, zz, h, to, own_chunk=False):
        slot = slot_of(o, zz)
        return remote(piece(f_ref if own_chunk else fbuf.at[slot], h), piece(fbuf.at[slot], h), ag_send.at["lry".index(to), slot, h],
                      ag_recv.at[slot, h], to_tp[to], dp)

    def arrived(o, zz, h):
        slot = slot_of(o, zz)
        remote(piece(f_ref, h), piece(fbuf.at[slot], h), ag_send.at[0, slot, h], ag_recv.at[slot, h], partner, dp).wait_recv()

    def own_sends(k):
        first = (1, 0) if k in (0, NZ - 1) else (0, 1)
        return [pass_on(0, k, h, "y", True) for h in first] + [
            pass_on(0, k, h, to, True) for h in range(2) for to in ("l" if k > 0 else "") + ("r" if k < NZ - 1 else "")]

    def on_position(f):
        for k in range(NZ):
            pl.when(z == k)(functools.partial(f, k))

    def first_sends(k):
        for c in own_sends(k):
            c.start()

    on_position(first_sends)
    load = pltpu.make_async_copy(e_ref, g_acc, load_sem.at[0])
    load.start()
    own_copy = pltpu.make_async_copy(f_ref, fbuf.at[tp], load_sem.at[1])
    own_copy.start()
    load.wait()

    def prepare(at, size):
        part = g_acc[at, :]
        e_b[at, :] = part.astype(BF16)
        e_t[:, at] = part.T.astype(BF16)

    def prepare_body(n, carry):
        prepare(pl.ds(pl.multiple_of(n * SUB, SUB), SUB), SUB)
        return carry

    lax.fori_loop(0, vocab // SUB, prepare_body, 0)
    if vocab % SUB:
        prepare(pl.ds(vocab // SUB * SUB, vocab % SUB), vocab % SUB)
    own_copy.wait()

    big = SUB * GROUP

    def z_copies(slot, n, out):
        if n is None:
            pair = (z_rest, z_ref.at[slot, pl.ds(whole * big, rest), :])
            sem = z_sem.at[2]
        else:
            pair = (z_buf.at[lax.rem(n, 2)], z_ref.at[slot, pl.ds(pl.multiple_of(n * big, big), big), :])
            sem = z_sem.at[lax.rem(n, 2)]
        return pltpu.make_async_copy(*(pair if out else pair[::-1]), sem)

    def slot_at(order, step):
        code = lookup({k: [2 * zz + o for o, zz in order[k]] for k in range(NZ)}, z, step)
        other = code % 2
        return code // 2 * 2 + y + other - 2 * y * other

    def gather_step(step, carry):
        for k in range(NZ):
            for at, events in GATHER_EVENTS[k].items():
                def serve(events=events):
                    for o, zz, h, to in events:
                        arrived(o, zz, h)
                        for t in to:
                            pass_on(o, zz, h, t).start()
                pl.when((z == k) & (step == at))(serve)
        slot = slot_at(GATHER_ORDER, step)
        f_b[slot] = fbuf[slot].astype(BF16)
        f_now = f_b[slot]

        def group(base, parts, kept, c):
            top, total = c
            for first, size in parts:
                logit = lax.dot_general(e_b[pl.ds(base + first, size), :], f_now, (((1,), (1,)), ((), ())), preferred_element_type=F32)
                kept[pl.ds(first, size), :] = logit
                logit = logit.reshape(size // 8, 8, own)
                new = jnp.maximum(top, jnp.max(logit, axis=0))
                total = total * jnp.exp2((top - new) * slope) + jnp.sum(jnp.exp2((logit - new[None]) * slope), axis=0)
                top = new
            return top, total

        def body(n, c):
            @pl.when(step * whole + n >= 2)
            def _():
                z_copies(slot, n, True).wait()
            c = group(pl.multiple_of(n * big, big), blocks, z_buf.at[lax.rem(n, 2)], c)
            z_copies(slot, n, True).start()
            return c

        top, total = lax.fori_loop(0, whole, body, (jnp.full((8, own), -3e38, F32), jnp.zeros((8, own), F32)))
        if tail:
            @pl.when(step > 0)
            def _():
                z_copies(slot, None, True).wait()
            top, total = group(whole * big, tail, z_rest, (top, total))
            z_copies(slot, None, True).start()
        most = jnp.max(top, axis=0, keepdims=True)
        total = jnp.sum(total * jnp.exp2((top - most) * slope), axis=0, keepdims=True)
        lse_all[tp, pl.ds(slot, 1), :] = most * scale + jnp.log(total)
        return carry

    lax.fori_loop(0, 2 * NZ, gather_step, 0)
    for n in range(2):
        z_copies(0, jnp.int32(n), True).wait()
    if tail:
        z_copies(0, None, True).wait()

    for n in range(1, 2 * NZ):
        to = lax.rem(tp + n, 2 * NZ)
        remote(lse_all.at[tp], lse_all.at[tp], st_send.at[to], st_recv.at[tp], to, dp).start()

    def gathers_done(k):
        for c in own_sends(k):
            c.wait_send()
        for events in GATHER_EVENTS[k].values():
            for o, zz, h, to in events:
                for t in to:
                    pass_on(o, zz, h, t).wait_send()

    on_position(gathers_done)
    start_slot = slot_at(SCATTER_ORDER, 0)
    for n in range(2):
        z_copies(start_slot, jnp.int32(n), False).start()
    if tail:
        z_copies(start_slot, None, False).start()

    def clear(n, carry):
        g_acc[pl.ds(pl.multiple_of(n * 16, 16), 16), :] = jnp.zeros((16, width), F32)
        return carry

    lax.fori_loop(0, vocab // 16, clear, 0)
    for n in range(1, 2 * NZ):
        source = lax.rem(tp + n, 2 * NZ)
        remote(lse_all.at[source], lse_all.at[source], st_send.at[source], st_recv.at[source], source, dp).wait_recv()
    peak = jnp.max(lse_all[...], axis=0)
    log_norm = peak + jnp.log(jnp.sum(jnp.exp(lse_all[...] - peak[None]), axis=0))
    norm_ref[...] = log_norm

    def leave(o, zz, h, to):
        src = piece(fbuf.at[slot_of(o, zz)], h)
        if to == "y":
            at = 2 * zz + h
            return remote(src, from_y.at[at], send_y.at[at], recv_y.at[at], partner, dp)
        if to == "l":
            at = 6 if o else 2 * zz + h
            return remote(src, from_r.at[at], send_l.at[at], recv_r.at[at], tp - 2, dp)
        at = 6 if o else 2 * zz - 2 + h
        return remote(src, from_l.at[at], send_r.at[at], recv_l.at[at], tp + 2, dp)

    def collect(o, zz, h, sums, to):
        here = piece(fbuf.at[slot_of(o, zz)], h)
        for d in sums:
            at, buf, sem = {"y": (2 * zz + h, from_y, recv_y), "l": (6 if o else 2 * zz - 2 + h, from_l, recv_l),
                            "r": (6 if o else 2 * zz + h, from_r, recv_r)}[d]
            remote(here, buf.at[at], send_y.at[0], sem.at[at], partner, dp).wait_recv()
            add_into(here, buf.at[at])
        if to:
            leave(o, zz, h, to).start()

    def scatter_step(step, lab_sum):
        slot = slot_at(SCATTER_ORDER, step)
        f_now = f_b[slot]
        acc = fbuf.at[slot]
        norm = norm_ref[pl.ds(slot, 1), :]
        shift = norm * log2e
        coef = (1.0 + 2.0 * LOGIT_ZLOSS * norm) * token_scale
        lab = lab_ref[pl.ds(slot, 1), :]
        acc[...] = jnp.zeros((width, own), F32)

        def group(base, parts, kept, hits):
            for first, size in parts:
                at = pl.ds(base + first, size)
                logit = kept[pl.ds(first, size), :]
                hit = lax.broadcasted_iota(jnp.int32, (size, own), 0) == lab - (base + first)
                prob = jnp.exp2(logit * slope - shift) * coef
                grad = jnp.where(hit, prob - token_scale, prob).astype(BF16)
                hits = hits + jnp.sum(jnp.where(hit, logit, 0.0).reshape(size // 8, 8, own), axis=0)
                dl[pl.ds(first, size), :] = grad
                g_acc[at, :] += jnp.dot(grad, f_now, preferred_element_type=F32)
            size = parts[-1][0] + parts[-1][1]
            acc[...] += jnp.dot(e_t[:, pl.ds(base, size)], dl[pl.ds(0, size), :], preferred_element_type=F32)
            return hits

        following = slot_at(SCATTER_ORDER, jnp.minimum(step + 1, 2 * NZ - 1))

        def body(n, hits):
            z_copies(slot, n, False).wait()
            hits = group(pl.multiple_of(n * big, big), blocks, z_buf.at[lax.rem(n, 2)], hits)

            @pl.when(n + 2 < whole)
            def _():
                z_copies(slot, n + 2, False).start()

            @pl.when((n + 2 >= whole) & (step + 1 < 2 * NZ))
            def _():
                z_copies(following, n + 2 - whole, False).start()
            return hits

        lab_sum = lax.fori_loop(0, whole, body, lab_sum)
        if tail:
            z_copies(slot, None, False).wait()
            lab_sum = group(whole * big, tail, z_rest, lab_sum)

            @pl.when(step + 1 < 2 * NZ)
            def _():
                z_copies(following, None, False).start()

        for k in range(NZ):
            for at, events in SCATTER_EVENTS[k].items():
                def reduce(events=events):
                    for event in events:
                        collect(*event)
                pl.when((z == k) & (step == at))(reduce)
        return lab_sum

    lab_sum = lax.fori_loop(0, 2 * NZ, scatter_step, jnp.zeros((8, own), F32))
    labsum_ref[...] = lab_sum
    store = pltpu.make_async_copy(g_acc, ghead_ref, load_sem.at[0])
    store.start()
    dfin_ref[...] = fbuf[tp].T

    def scatters_done(k):
        for events in SCATTER_EVENTS[k].values():
            for o, zz, h, _, to in events:
                if to:
                    leave(o, zz, h, to).wait_send()

    on_position(scatters_done)
    for n in range(1, 2 * NZ):
        to = lax.rem(tp + n, 2 * NZ)
        remote(lse_all.at[tp], lse_all.at[tp], st_send.at[to], st_recv.at[tp], to, dp).wait_send()
    store.wait()


def head(f_own, labels, embed, scale, token_scale, collective_id):
    own, width = f_own.shape
    vocab = embed.shape[0]
    chunk = (own, width)
    strips = lambda n: pltpu.VMEM((n, own // 2, width), F32)
    dma = lambda *n: pltpu.SemaphoreType.DMA(n)
    return pl.pallas_call(
        functools.partial(head_kernel, scale, token_scale),
        out_shape=(jax.ShapeDtypeStruct((own, width), F32), jax.ShapeDtypeStruct((vocab, width), F32),
                   jax.ShapeDtypeStruct((2 * NZ, own), F32), jax.ShapeDtypeStruct((8, own), F32),
                   jax.ShapeDtypeStruct((2 * NZ, vocab, own), F32)),
        in_specs=[VMEM, VMEM, ANY],
        out_specs=(VMEM, ANY, VMEM, VMEM, ANY),
        scratch_shapes=[pltpu.VMEM((vocab, width), BF16), pltpu.VMEM((width, vocab), BF16),
                        pltpu.VMEM((2 * NZ,) + chunk, F32), pltpu.VMEM((2 * NZ,) + chunk, BF16), pltpu.VMEM((vocab, width), F32),
                        strips(8), strips(7), strips(7),
                        pltpu.VMEM((SUB * GROUP, own), BF16), pltpu.VMEM((2, SUB * GROUP, own), F32),
                        pltpu.VMEM((max(vocab % (SUB * GROUP), 8), own), F32), pltpu.VMEM((2 * NZ, 2 * NZ, own), F32),
                        dma(3), dma(2), dma(3, 2 * NZ, 2), dma(2 * NZ, 2), dma(8), dma(7), dma(7), dma(8), dma(7), dma(7), dma(2 * NZ), dma(2 * NZ)],
        compiler_params=pltpu.CompilerParams(collective_id=collective_id, has_side_effects=True, vmem_limit_bytes=67000000),
        cost_estimate=pl.CostEstimate(flops=8 * vocab * width * own * 8, bytes_accessed=3 * 4 * vocab * width, transcendentals=2 * vocab * own * 8),
        name="head",
    )(f_own, labels, embed)


TB = (((1,), (1,)), ((), ()))
TA = (((0,), (0,)), ((), ()))
LOG2E = 1.4426950408889634


def mm(a, b, dims=(((1,), (0,)), ((), ()))):
    return lax.dot_general(a, b, dims, preferred_element_type=F32)


def turn(lo, hi, cos_t, sin_t):
    return lo * cos_t - hi * sin_t, hi * cos_t + lo * sin_t


EVENTS = {
    0: (((("R", 1),), (0,)), ((("R", 2),), (1,)), ((("R", 3),), (2,)), ((), (3,))),
    1: (((("L", 0), ("R", 2)), (1,)), ((("R", 3),), (0,)), ((), (2,)), ((), (3,))),
    2: (((("R", 3), ("L", 1)), (2,)), ((("L", 0),), (3,)), ((), (1,)), ((), (0,))),
    3: (((("L", 2),), (3,)), ((("L", 1),), (2,)), ((("L", 0),), (1,)), ((), (0,))),
}
MLP_ORDER = {k: [2 * k] + [code for line, other in EVENTS[k] for code in [2 * zz for _, zz in line] + [2 * zz + 1 for zz in other]] for k in range(NZ)}


def front_kernel(ids_ref, e_ref, rounds_ref, pick_ref, extra_ref, w_ref, wkv_ref, ln_ref, cos_ref, sin_ref,
                 f_ref, x1_ref, x0_ref, q_ref, kv_ref, kvt_ref, lse_ref, ctx_ref, wq_ref, wo_ref, wg_ref, wu_ref, wd_ref, rounds_all,
                 table, rows_ref, wl, rows_in, u_b, kv_out, kv_in, own_sem, r_send, r_recv, a_y, a_l, a_r, a_c, a_recv,
                 b_y, b_l, b_r, b_x, b_c, b_recv, kv_send, kv_recv, n_send, n_recv):
    tp, dp, z, y = place()
    partner = tp + 1 - 2 * y
    core = dp % 2
    twin = dp + 1 - 2 * core
    facing = lax.rem(dp + 2, 4)
    own, width = x0_ref.shape
    shards, w_rows = wl.shape[0], wl.shape[1]
    nq = q_ref.shape[0]
    ff = wg_ref.shape[0]
    n_a = nq // shards
    n_f = ff // shards
    n_b = 3 * n_f // 4
    hd = kv_out.shape[0] // 2
    quarter = hd // 2
    heads = nq // hd

    def a_rows(c):
        return pl.ds(pl.multiple_of(c * n_a, 8), n_a)

    def b_rows(d):
        return pl.ds(pl.multiple_of(2 * n_a + d * n_b, 8), n_b)

    def a_copy(slot, sems, to, to_dp, first=False):
        src = w_ref.at[a_rows(core), :] if first else wl.at[slot, a_rows(core), :]
        return remote(src, wl.at[slot, a_rows(core), :], sems.at[slot], a_recv.at[slot, core], to, to_dp)

    def b_copy(slot, piece, sems, to, to_dp, first=False):
        src = w_ref.at[b_rows(piece), :] if first else wl.at[slot, b_rows(piece), :]
        return remote(src, wl.at[slot, b_rows(piece), :], sems.at[slot], b_recv.at[slot, piece], to, to_dp)

    def a_wait(slot, c):
        remote(w_ref.at[a_rows(c), :], wl.at[slot, a_rows(c), :], a_y.at[slot], a_recv.at[slot, c], partner, dp).wait_recv()

    def b_wait(slot, piece):
        remote(w_ref.at[b_rows(piece), :], wl.at[slot, b_rows(piece), :], b_y.at[slot], b_recv.at[slot, piece], partner, dp).wait_recv()

    def on_position(f):
        for k in range(NZ):
            pl.when(z == k)(functools.partial(f, k))

    def line_sends(k, make, y_sems, l_sems, r_sems, slot, side, first=False):
        sends = [make(slot, y_sems, partner, dp, first)]
        if k > 0 and side != "L":
            sends.append(make(slot, l_sems, tp - 2, dp, first))
        if k < NZ - 1 and side != "R":
            sends.append(make(slot, r_sems, tp + 2, dp, first))
        return sends

    def b_own(slot, sems, to, to_dp, first=False):
        return b_copy(slot, dp, sems, to, to_dp, first)

    def a_sends(k, slot, side, first=False):
        return line_sends(k, a_copy, a_y, a_l, a_r, slot, side, first)

    def b_sends(k, slot, side, first=False):
        return line_sends(k, b_own, b_y, b_l, b_r, slot, side, first)

    def start(copies):
        for c in copies:
            c.start()

    load = pltpu.make_async_copy(e_ref, table, own_sem.at[2])
    load.start()
    group = [twin, facing, lax.rem(twin + 2, 4)]
    plane_barrier(tp, dp, [(tp, d) for d in group])
    peers = [lax.rem(tp + n, shards) for n in range(1, shards)]

    def rounds_copy(n):
        return remote(rounds_ref, rounds_all.at[dp], n_send.at[n], n_recv.at[dp], tp, group[n])

    for n in range(3):
        rounds_copy(n).start()
    rounds_all[dp] = rounds_ref[...]

    def row_copy(to):
        return remote(rows_ref.at[to], rows_in.at[tp], r_send.at[to], r_recv.at[tp], to, dp)

    on_position(lambda k: start(b_sends(k, tp, "", True)))
    on_position(lambda k: start(a_sends(k, tp, "", True)))
    own_w = pltpu.make_async_copy(w_ref, wl.at[tp], own_sem.at[1])
    own_w.start()

    def a_event(t, k):
        line, other = EVENTS[k][t]
        for side, zz in line:
            slot = 2 * zz + y
            a_wait(slot, core)
            start(a_sends(k, slot, side))
            a_copy(slot, a_c, tp, twin).start()
        for zz in other:
            slot = 2 * zz + 1 - y
            a_wait(slot, core)
            a_copy(slot, a_c, tp, twin).start()

    def b_event(t, k):
        line, other = EVENTS[k][t]
        for side, zz in line:
            slot = 2 * zz + y
            b_wait(slot, dp)
            start(b_sends(k, slot, side))
            b_copy(slot, dp, b_x, tp, facing).start()
            b_copy(slot, dp, b_c.at[0], tp, twin).start()
        for zz in other:
            slot = 2 * zz + 1 - y
            b_wait(slot, dp)
            b_copy(slot, dp, b_x, tp, facing).start()
            b_copy(slot, dp, b_c.at[0], tp, twin).start()

    load.wait()
    cap = rows_ref.shape[1]

    def pick_rows(n, carry):
        for i in range(8):
            rows_ref[n // (cap // 8), pl.ds(lax.rem(n, cap // 8) * 8 + i, 1), :] = table[pl.ds(ids_ref[n * 8 + i], 1), :]
        return carry

    lax.fori_loop(0, shards * cap // 8, pick_rows, 0)
    on_position(functools.partial(b_event, 0))
    on_position(functools.partial(a_event, 0))
    start([row_copy(to) for to in peers])
    own_rows = pltpu.make_async_copy(rows_ref.at[tp], rows_in.at[tp], own_sem.at[0])
    own_rows.start()
    on_position(functools.partial(b_event, 1))
    on_position(functools.partial(a_event, 1))
    own_rows.wait()
    for source in peers:
        remote(rows_ref.at[source], rows_in.at[source], r_send.at[source], r_recv.at[source], source, dp).wait_recv()
    x0_ref[...] = extra_ref[...] + mm(pick_ref[...], rows_in[...].reshape(pick_ref.shape[1], width).astype(BF16))
    u_b[...] = norm_fwd(x0_ref[...], ln_ref[0:1, :])[0]
    x1_ref[...] = x0_ref[...]
    cos_t = cos_ref[...]
    sin_t = sin_ref[...]
    kv = mm(wkv_ref[...], u_b[...], TB)
    lo, hi = turn(kv[:quarter], kv[quarter:hd], cos_t, sin_t)
    kv_out[0:quarter, :] = lo
    kv_out[quarter:hd, :] = hi
    kv_out[hd:, :] = kv[hd:]
    kv_copy = remote(kv_out, kv_in, kv_send, kv_recv, partner, dp)
    kv_copy.start()

    def slot_of(step):
        code = lookup(MLP_ORDER, z, step)
        other = code % 2
        return code // 2 * 2 + y + other - 2 * y * other

    def mlp(step, carry):
        def pass_on():
            slot = slot_of(step + 1)
            b_wait(slot, facing)
            b_copy(slot, facing, b_c.at[1], tp, twin).start()
        pl.when(step < shards - 1)(pass_on)
        slot = slot_of(step)

        def rest():
            b_wait(slot, twin)
            b_wait(slot, lax.rem(twin + 2, 4))
        pl.when(step > 0)(rest)
        at = pl.ds(pl.multiple_of(slot * n_f, n_f), n_f)
        wg_ref[at, :] = wl[slot, 2 * n_a:2 * n_a + n_f, :].astype(BF16)
        wu_ref[at, :] = wl[slot, 2 * n_a + n_f:2 * n_a + 2 * n_f, :].astype(BF16)
        wd_ref[at, :] = wl[slot, 2 * n_a + 2 * n_f:2 * n_a + 3 * n_f, :].astype(BF16)
        gate = mm(u_b[...], wg_ref[at, :], TB)
        up = mm(u_b[...], wu_ref[at, :], TB)
        x1_ref[...] += mm((gate * jax.nn.sigmoid(gate) * up).astype(BF16), wd_ref[at, :])
        return carry

    own_w.wait()
    lax.fori_loop(0, 3, mlp, 0)
    on_position(functools.partial(b_event, 2))
    on_position(functools.partial(a_event, 2))
    lax.fori_loop(3, 4, mlp, 0)
    on_position(functools.partial(a_event, 3))
    on_position(functools.partial(b_event, 3))
    for source in peers:
        a_wait(source, 1 - core)
    for s in range(shards):
        wq_ref[s * n_a:(s + 1) * n_a, :] = wl[s, 0:n_a, :].astype(BF16)
        wo_ref[s * n_a:(s + 1) * n_a, :] = wl[s, n_a:2 * n_a, :].astype(BF16)

    q_all = mm(wq_ref[...], u_b[...], TB)
    for h in range(heads):
        lo, hi = turn(q_all[h * hd:h * hd + quarter], q_all[h * hd + quarter:(h + 1) * hd], cos_t, sin_t)
        q_ref[h * hd:h * hd + quarter, :] = lo.astype(BF16)
        q_ref[h * hd + quarter:(h + 1) * hd, :] = hi.astype(BF16)
    kv_copy.wait()

    def fill(mine, other):
        kv_ref[mine * own:(mine + 1) * own, :] = kv_out[...].T.astype(BF16)
        kv_ref[other * own:(other + 1) * own, :] = kv_in[...].T.astype(BF16)
        kvt_ref[:, mine * own:(mine + 1) * own] = kv_out[...].astype(BF16)
        kvt_ref[:, other * own:(other + 1) * own] = kv_in[...].astype(BF16)

    pl.when(y == 0)(lambda: fill(0, 1))
    pl.when(y == 1)(lambda: fill(1, 0))
    blank = jnp.zeros((hd, own), BF16)
    slope = hd ** -0.5 * LOG2E

    def attend(h, carry):
        at = pl.ds(pl.multiple_of(h * hd, hd), hd)
        scores = mm(kv_ref[...], jnp.concatenate([q_ref[at, :], blank], axis=0))
        allowed = lax.broadcasted_iota(jnp.int32, scores.shape, 0) <= lax.broadcasted_iota(jnp.int32, scores.shape, 1) + y * own
        scores = jnp.where(allowed, scores * slope, -1e30)
        top = jnp.max(scores, axis=0, keepdims=True)
        prob = jnp.exp2(scores - top)
        total = jnp.sum(prob, axis=0, keepdims=True)
        lse_ref[pl.ds(h, 1), :] = top + jnp.log2(total)
        ctx_ref[at, :] = mm(kvt_ref[hd:, :], (prob * (1.0 / total)).astype(BF16)).astype(BF16)
        return carry

    lax.fori_loop(0, heads, attend, 0)
    x1_ref[...] += mm(ctx_ref[...], wo_ref[...], TA)

    lax.fori_loop(4, shards, mlp, 0)
    f_ref[...] = norm_fwd(x1_ref[...], ln_ref[1:2, :])[0].astype(F32)

    def finish(k):
        done = a_sends(k, tp, "", True) + b_sends(k, tp, "", True)
        for line, other in EVENTS[k]:
            for side, zz in line:
                done += a_sends(k, 2 * zz + y, side) + b_sends(k, 2 * zz + y, side)
        for c in done:
            c.wait_send()

    on_position(finish)
    for n in range(3):
        rounds_copy(n).wait_send()
        remote(rounds_ref, rounds_all.at[group[n]], n_send.at[n], n_recv.at[group[n]], tp, twin).wait_recv()
    for to in peers:
        row_copy(to).wait_send()
        a_copy(to, a_c, tp, twin).wait_send()
        b_copy(to, dp, b_x, tp, facing).wait_send()
        b_copy(to, dp, b_c.at[0], tp, twin).wait_send()
        b_copy(to, facing, b_c.at[1], tp, twin).wait_send()


def front(ids, embed, rounds, pick, extra, w_rows, wkv_t, ln, cos_t, sin_t, n_q, collective_id):
    own, width = extra.shape
    two_hd = wkv_t.shape[0]
    shards = 2 * NZ
    ff = (w_rows.shape[0] * shards - 2 * n_q) // 3
    dma = lambda *n: pltpu.SemaphoreType.DMA(n)
    s = jax.ShapeDtypeStruct
    rows = (shards, ids.shape[0] // shards, width)
    return pl.pallas_call(
        front_kernel,
        out_shape=(s((own, width), F32),) * 3 + (s((n_q, own), BF16), s((2 * own, two_hd), BF16), s((two_hd, 2 * own), BF16),
                   s((2 * n_q // two_hd, own), F32), s((n_q, own), BF16), s((n_q, width), BF16), s((n_q, width), BF16))
        + (s((ff, width), BF16),) * 3 + (s((4, 1, 128), jnp.int32),),
        in_specs=[pl.BlockSpec(memory_space=pltpu.SMEM), ANY, VMEM, VMEM, VMEM, ANY] + [VMEM] * 4,
        out_specs=(VMEM,) * 14,
        scratch_shapes=[pltpu.VMEM(embed.shape, F32), pltpu.VMEM(rows, F32), pltpu.VMEM((shards,) + w_rows.shape, F32), pltpu.VMEM(rows, F32), pltpu.VMEM((own, width), BF16),
                        pltpu.VMEM((two_hd, own), F32), pltpu.VMEM((two_hd, own), F32),
                        dma(3), dma(shards), dma(shards)] + [dma(shards)] * 4 + [dma(shards, 2)]
        + [dma(shards)] * 4 + [dma(2, shards), dma(shards, 4), pltpu.SemaphoreType.DMA, pltpu.SemaphoreType.DMA, dma(3), dma(4)],
        compiler_params=pltpu.CompilerParams(collective_id=collective_id, has_side_effects=True, vmem_limit_bytes=60000000),
        name="front",
    )(ids, embed, rounds, pick, extra, w_rows, wkv_t, ln, cos_t, sin_t)


def layer_bwd_kernel(dfin_ref, x0_ref, x1_ref, loss_ref, ln_ref, cos_ref, sin_ref, wq_ref, wkv_ref, wo_ref, wg_ref, wu_ref, wd_ref,
                     q_ref, kv_ref, kvt_ref, lse_ref, ctx_ref, pick_ref, g_ref, ids_ref, rows_ref, d0_ref, back_ref, early_ref, ids_all, d_one, d_b, u_b, dctx, dq, dkv, dkv_in,
                     hid, d_gate, d_up, rows_out, g_q, g_o, g_g, g_u, g_d, small, s_early, c_early, out_sem, send_sem, recv_sem,
                     r_send, x_send, c_send, r_recv, g_load, g_send, g_recv, id_send, id_recv):
    tp, dp, z, y = place()
    partner = tp + 1 - 2 * y
    core = dp % 2
    twin = dp + 1 - 2 * core
    facing = lax.rem(dp + 2, 4)
    across = lax.rem(twin + 2, 4)
    own, width = x0_ref.shape
    hd = kv_ref.shape[1] // 2
    quarter = hd // 2
    nq = q_ref.shape[0]
    heads = nq // hd
    ff = wg_ref.shape[0]
    shards = rows_ref.shape[0]
    plane_barrier(tp, dp, [(tp, twin), (tp, facing), (tp, across)])

    n_early, g_size = s_early.shape[0], s_early.shape[1]

    def g_rows(which, b):
        return g_ref.at[pl.ds(pl.multiple_of(which * (g_ref.shape[0] // 2) + b * g_size, 8), g_size), :]

    def g_load_copy(b):
        return pltpu.make_async_copy(g_rows(core, b), s_early.at[b], g_load.at[b])

    def g_chip_copy(b):
        return remote(g_rows(1 - core, b), c_early.at[b], g_send.at[0, b], g_recv.at[0, b], tp, twin)

    def g_x_copy(b):
        return remote(s_early.at[b], early_ref.at[b], g_send.at[1, b], g_recv.at[1, b], tp, facing)

    for b in range(n_early):
        g_chip_copy(b).start()
        g_load_copy(b).start()

    def ids_copy(n, to):
        return remote(ids_ref, ids_all.at[dp], id_send.at[n], id_recv.at[dp], tp, to)

    for n, to in enumerate((twin, facing, across)):
        ids_copy(n, to).start()
    ids_all[dp] = ids_ref[...]
    _, f_hat, f_inv = norm_fwd(x1_ref[...], ln_ref[1:2, :])
    d_in, g_fin = norm_bwd(dfin_ref[...], f_hat, f_inv, ln_ref[1:2, :])
    d_one[...] = d_in
    d_b[...] = d_in.astype(BF16)
    u_b[...] = norm_fwd(x0_ref[...], ln_ref[0:1, :])[0]
    dctx[...] = mm(wo_ref[...], d_b[...], TB).astype(BF16)
    for b in range(n_early):
        g_load_copy(b).wait()
        g_chip_copy(b).wait_recv()
        add_into(s_early.at[b], c_early.at[b], 24)
        g_x_copy(b).start()
    cos_t = cos_ref[...]
    sin_t = sin_ref[...]
    blank = jnp.zeros((hd, own), BF16)
    slope = hd ** -0.5 * LOG2E
    dkv[...] = jnp.zeros_like(dkv)

    def attend(h, carry):
        at = pl.ds(pl.multiple_of(h * hd, hd), hd)
        q_pad = jnp.concatenate([q_ref[at, :], blank], axis=0)
        d_pad = jnp.concatenate([blank, dctx[at, :]], axis=0)
        scores = mm(kv_ref[...], q_pad)
        allowed = lax.broadcasted_iota(jnp.int32, scores.shape, 0) <= lax.broadcasted_iota(jnp.int32, scores.shape, 1) + y * own
        prob = jnp.where(allowed, jnp.exp2(scores * slope - lse_ref[pl.ds(h, 1), :]), 0.0)
        d_prob = mm(kv_ref[...], d_pad)
        mean = jnp.sum(d_prob * prob, axis=0, keepdims=True)
        d_score = (prob * (d_prob - mean) * hd ** -0.5).astype(BF16)
        dkv[...] += mm(d_score, q_pad, TB) + mm(prob.astype(BF16), d_pad, TB)
        d_q = mm(kvt_ref[0:hd, :], d_score)
        lo, hi = turn(d_q[:quarter], d_q[quarter:], cos_t, -sin_t)
        dq[at, :] = jnp.concatenate([lo, hi], axis=0).astype(BF16)
        return carry

    lax.fori_loop(0, heads, attend, 0)
    copy = remote(dkv.at[pl.ds(pl.multiple_of((1 - y) * own, own), own), :], dkv_in, send_sem, recv_sem, partner, dp)
    copy.start()

    d0_ref[...] = mm(dq[...], wq_ref[...], TA)
    step = min(512, ff)

    def mlp(n, carry):
        at = pl.ds(pl.multiple_of(n * step, step), step)
        gate = mm(wg_ref[at, :], u_b[...], TB)
        up = mm(wu_ref[at, :], u_b[...], TB)
        d_hidden = mm(wd_ref[at, :], d_b[...], TB)
        sig = jax.nn.sigmoid(gate)
        hid[at, :] = (gate * sig * up).astype(BF16)
        d_gate[at, :] = (d_hidden * up * sig * (1.0 + gate * (1.0 - sig))).astype(BF16)
        d_up[at, :] = (d_hidden * gate * sig).astype(BF16)
        d0_ref[...] += mm(d_gate[at, :], wg_ref[at, :], TA) + mm(d_up[at, :], wu_ref[at, :], TA)
        return carry

    lax.fori_loop(0, ff // step, mlp, 0)
    copy.wait()
    d_kv = (dkv[pl.ds(pl.multiple_of(y * own, own), own), :] + dkv_in[...]).T
    lo, hi = turn(d_kv[:quarter], d_kv[quarter:hd], cos_t, -sin_t)
    d_kv = jnp.concatenate([lo, hi, d_kv[hd:]], axis=0).astype(BF16)
    small[0:2 * hd, :] = mm(d_kv, u_b[...])
    d_u = d0_ref[...] + mm(d_kv, wkv_ref[...], TA)
    _, u_hat, u_inv = norm_fwd(x0_ref[...], ln_ref[0:1, :])
    d_in, g_in = norm_bwd(d_u, u_hat, u_inv, ln_ref[0:1, :])
    d_zero = d_one[...] + d_in
    d0_ref[...] = d_zero
    high = d_zero.astype(BF16)
    left = d_zero - high.astype(F32)
    middle = left.astype(BF16)
    low = (left - middle.astype(F32)).astype(BF16)
    rows_out[...] = (mm(pick_ref[...], high, TA) + mm(pick_ref[...], middle, TA) + mm(pick_ref[...], low, TA)).reshape(rows_out.shape)

    def row_copy(to):
        return remote(rows_out.at[to], back_ref.at[dp, tp], r_send.at[to], r_recv.at[dp, tp], to, dp)

    def x_copy(slot):
        return remote(back_ref.at[dp, slot], back_ref.at[dp, slot], x_send.at[slot], r_recv.at[dp, slot], tp, facing)

    def c_copy(group, n, slot):
        return remote(back_ref.at[group, slot], back_ref.at[group, slot], c_send.at[n, slot], r_recv.at[group, slot], tp, twin)

    def back(group, slot):
        remote(rows_out.at[slot], back_ref.at[group, slot], r_send.at[slot], r_recv.at[group, slot], tp, twin).wait_recv()

    def near_first(k):
        return sorted(((o, zz) for o in range(2) for zz in range(NZ)), key=lambda c: (abs(c[1] - k), c[0]))

    def slot_of(o, zz):
        return 2 * zz + (1 - y if o else y)

    def on_position(f):
        for k in range(NZ):
            pl.when(z == k)(functools.partial(f, k))

    def rows_leave(k):
        for c in near_first(k)[:0:-1]:
            row_copy(slot_of(*c)).start()

    on_position(rows_leave)
    own_rows = pltpu.make_async_copy(rows_out.at[tp], back_ref.at[dp, tp], out_sem.at[7 * 2 * NZ])
    own_rows.start()
    own_rows.wait()
    x_copy(tp).start()
    c_copy(dp, 0, tp).start()

    g_o[...] = mm(ctx_ref[...], d_b[...])
    g_q[...] = mm(dq[...], u_b[...])

    def weight_grads(n, carry):
        at = pl.ds(pl.multiple_of(n * step, step), step)
        g_d[at, :] = mm(hid[at, :], d_b[...])
        g_g[at, :] = mm(d_gate[at, :], u_b[...])
        g_u[at, :] = mm(d_up[at, :], u_b[...])
        return carry

    lax.fori_loop(0, ff // step, weight_grads, 0)
    small[2 * hd:, :] = jnp.zeros_like(small[2 * hd:, :])
    small[2 * hd:2 * hd + 1, :] = g_in.reshape(1, width)
    small[2 * hd + 1:2 * hd + 2, :] = g_fin.reshape(1, width)
    small[2 * hd + 2:2 * hd + 3, :] = loss_ref[...]
    copies = []

    def put(src, first, size, s):
        copies.append(pltpu.make_async_copy(src, rows_ref.at[s, pl.ds(first, size), :], out_sem.at[len(copies)]))

    n_kv = 2 * hd // shards
    for s in range(shards):
        at = 0
        for g, size in ((g_q, nq // shards), (g_o, nq // shards), (g_g, ff // shards), (g_u, ff // shards), (g_d, ff // shards)):
            put(g.at[pl.ds(s * size, size), :], at, size, s)
            at += size
        put(small.at[pl.ds(s * n_kv, n_kv), :], at, n_kv, s)
        put(small.at[pl.ds(2 * hd + (0 if s == 0 else 16), 16), :], at + n_kv, 16, s)
    for c in copies:
        c.start()
    for c in copies:
        c.wait()

    def relay(k):
        order = near_first(k)
        for c in order[1:]:
            back(dp, slot_of(*c))
            x_copy(slot_of(*c)).start()
            c_copy(dp, 0, slot_of(*c)).start()
        for c in order:
            back(facing, slot_of(*c))
            c_copy(facing, 1, slot_of(*c)).start()

    on_position(relay)
    for b in range(n_early):
        g_x_copy(b).wait_recv()
        add_into(early_ref.at[b], s_early.at[b], 24)
    for slot in range(shards):
        back(twin, slot)
        back(across, slot)
    for n, to in enumerate((twin, facing, across)):
        remote(ids_ref, ids_all.at[to], id_send.at[n], id_recv.at[to], tp, to).wait_recv()
        ids_copy(n, to).wait_send()
    for n in range(1, shards):
        row_copy(lax.rem(tp + n, shards)).wait_send()
    for slot in range(shards):
        x_copy(slot).wait_send()
        c_copy(dp, 0, slot).wait_send()
        c_copy(facing, 1, slot).wait_send()
    for b in range(n_early):
        g_chip_copy(b).wait_send()
        g_x_copy(b).wait_send()


def layer_bwd(d_fin, x0, x1, loss_row, ln, cos_t, sin_t, weights, saved, pick, g_table, ids, collective_id):
    own, width = x0.shape
    nq = weights[0].shape[0]
    two_hd = weights[1].shape[0]
    ff = weights[3].shape[0]
    rows = (2 * nq + 3 * ff + two_hd) // (2 * NZ) + 16
    chunk = (own, width)
    back = (2 * NZ, pick.shape[1] // (2 * NZ), width)
    blocks = (N_EARLY, table_block(g_table.shape[0]), width)
    dma = lambda *n: pltpu.SemaphoreType.DMA(n)
    return pl.pallas_call(
        layer_bwd_kernel,
        out_shape=(jax.ShapeDtypeStruct((2 * NZ, rows, width), F32), jax.ShapeDtypeStruct(chunk, F32), jax.ShapeDtypeStruct((4,) + back, F32),
                   jax.ShapeDtypeStruct(blocks, F32), jax.ShapeDtypeStruct((4,) + ids.shape, jnp.int32)),
        in_specs=[VMEM] * 19 + [ANY, VMEM],
        out_specs=(ANY, VMEM, ANY, VMEM, VMEM),
        scratch_shapes=[pltpu.VMEM(chunk, F32), pltpu.VMEM(chunk, BF16), pltpu.VMEM(chunk, BF16), pltpu.VMEM((nq, own), BF16),
                        pltpu.VMEM((nq, own), BF16), pltpu.VMEM((2 * own, two_hd), F32), pltpu.VMEM((own, two_hd), F32)]
        + [pltpu.VMEM((ff, own), BF16)] * 3 + [pltpu.VMEM(back, F32), pltpu.VMEM((nq, width), F32), pltpu.VMEM((nq, width), F32)] + [pltpu.VMEM((ff, width), F32)] * 3
        + [pltpu.VMEM((two_hd + 32, width), F32), pltpu.VMEM(blocks, F32), pltpu.VMEM(blocks, F32), dma(14 * NZ + 1),
           pltpu.SemaphoreType.DMA, pltpu.SemaphoreType.DMA, dma(2 * NZ), dma(2 * NZ), dma(2, 2 * NZ), dma(4, 2 * NZ),
           dma(N_EARLY), dma(2, N_EARLY), dma(2, N_EARLY), dma(3), dma(4)],
        compiler_params=pltpu.CompilerParams(collective_id=collective_id, has_side_effects=True, vmem_limit_bytes=66000000),
        name="layer_bwd",
    )(d_fin, x0, x1, loss_row, ln, cos_t, sin_t, *weights, *saved, pick, g_table, ids)


N_BLOCK = 12
N_EARLY = 3
AHEAD = 11


def table_block(vocab):
    return -(-vocab // (2 * N_BLOCK * 24)) * 24


W_REDUCE = {
    0: {4: (3,), 6: (2,), 8: (1,), 9: (0,)},
    1: {6: (3,), 8: (2, 0), 9: (1,)},
    2: {6: (0,), 8: (1, 3), 9: (2,)},
    3: {4: (0,), 6: (1,), 8: (2,), 9: (3,)},
}


def tail_kernel(g_ref, p_ref, rows_ref, ids_ref, early_ref, t_ref, w_out, small_ref,
                s_buf, from_c, from_x, look_in, parts, acc, w_c, w_y, w_l, w_r, w_x,
                g_load, g_send_c, g_recv_c, g_send_x, g_recv_x, g_send_t, g_recv_t, g_store, l_sem,
                w_load, w_out_sem, send_c, send_y, send_l, send_r, recv_c, recv_y, recv_l, recv_r, last_send, last_recv, small_send, small_recv):
    tp, dp, z, y = place()
    partner = tp + 1 - 2 * y
    core = dp % 2
    twin = dp + 1 - 2 * core
    facing = lax.rem(dp + 2, 4)
    half = g_ref.shape[0] // 2
    size = s_buf.shape[1]
    last = half - (N_BLOCK - 1) * size
    n_look = rows_ref.shape[1]

    def rows(which, b, n):
        return pl.ds(pl.multiple_of(which * half + b * size, 8), n)

    def part(buf, b, n):
        return buf.at[b - N_EARLY if buf is not from_x else b, pl.ds(0, n), :]

    plane_barrier(tp, dp, [(tp, twin), (tp, facing)])

    chip = dp // 2
    groups = (2 * chip, 2 * chip + 1, 2 - 2 * chip, 3 - 2 * chip)

    def look_load(n):
        return pltpu.make_async_copy(rows_ref.at[groups[n]], look_in.at[n % 2], l_sem.at[n % 2])

    def early_load(b):
        return pltpu.make_async_copy(early_ref.at[b], from_x.at[b], g_load.at[b])

    for n in range(2):
        look_load(n).start()

    def c_copy(b, n):
        return remote(g_ref.at[rows(1 - core, b, n), :], part(from_c, b, n), g_send_c.at[b], g_recv_c.at[b], tp, twin)

    def own_load(b, n):
        return pltpu.make_async_copy(g_ref.at[rows(core, b, n), :], part(s_buf, b, n), g_load.at[b])

    def x_copy(b, n):
        return remote(part(s_buf, b, n), part(from_x, b, n), g_send_x.at[b], g_recv_x.at[b], tp, facing)

    def t_copy(b, n):
        return remote(part(from_x, b, n), t_ref.at[rows(core, b, n), :], g_send_t.at[b], g_recv_t.at[b], tp, twin)

    def t_store(b, n):
        return pltpu.make_async_copy(part(from_x, b, n), t_ref.at[rows(core, b, n), :], g_store.at[b])

    def every(f, first, end):
        def body(b, carry):
            f(b, size)
            return carry
        lax.fori_loop(first, min(end, N_BLOCK - 1), body, 0)
        if end == N_BLOCK:
            f(N_BLOCK - 1, last)

    def looked_up(b, n, first, count):
        ids = jnp.concatenate([ids_ref[first + g] for g in range(count)], axis=1) - (core * half + b * size)
        hit = (lax.broadcasted_iota(jnp.int32, (n, count * n_look), 0) == ids).astype(F32).astype(BF16)
        span = pl.ds(pl.multiple_of(first * n_look, n_look), count * n_look)
        return mm(hit, parts[0, span, :]) + mm(hit, parts[1, span, :]) + mm(hit, parts[2, span, :])

    def chip_sum(b, n):
        own_load(b, n).wait()
        c_copy(b, n).wait_recv()
        at = b - N_EARLY
        s_buf[at, 0:n, :] = s_buf[at, 0:n, :] + from_c[at, 0:n, :] + looked_up(b, n, 2 * chip, 2)
        x_copy(b, n).start()

    def early_sum(b, n):
        early_load(b).wait()
        from_x[b] = from_x[b] + looked_up(b, n, 0, 4)
        t_copy(b, n).start()
        t_store(b, n).start()

    def w_first(k):
        for zz in REDUCE_ORDER[k]:
            for slot in (2 * zz + 1 - y, 2 * zz + y):
                remote(p_ref.at[slot, 1 - core], w_c.at[slot], send_c.at[slot], recv_c.at[slot], tp, twin).start()
                pltpu.make_async_copy(p_ref.at[slot, core], acc.at[slot], w_load.at[slot]).start()

    def w_chip_sum(slot):
        pltpu.make_async_copy(p_ref.at[slot, core], acc.at[slot], w_load.at[slot]).wait()
        remote(acc.at[slot], w_c.at[slot], send_c.at[slot], recv_c.at[slot], tp, twin).wait_recv()
        add_into(acc.at[slot], w_c.at[slot])

    def w_second(k):
        for zz in REDUCE_ORDER[k]:
            slot = 2 * zz + 1 - y
            w_chip_sum(slot)
            remote(acc.at[slot], w_y.at[zz], send_y.at[zz], recv_y.at[zz], partner, dp).start()
        for zz in REDUCE_ORDER[k]:
            w_chip_sum(2 * zz + y)

    def w_reduce(k, shards):
        for zz in shards:
            line = acc.at[2 * zz + y]
            remote(line, w_y.at[zz], send_y.at[zz], recv_y.at[zz], partner, dp).wait_recv()
            add_into(line, w_y.at[zz])
            if zz >= k and k > 0:
                remote(line, w_l.at[zz - 1], send_l.at[zz], recv_l.at[zz], partner, dp).wait_recv()
                add_into(line, w_l.at[zz - 1])
            if zz <= k and k < NZ - 1:
                remote(line, w_r.at[zz], send_r.at[zz], recv_r.at[zz], partner, dp).wait_recv()
                add_into(line, w_r.at[zz])
            if zz > k:
                remote(line, w_l.at[zz - 1], send_r.at[zz], recv_l.at[zz], tp + 2, dp).start()
            if zz < k:
                remote(line, w_r.at[zz], send_l.at[zz], recv_r.at[zz], tp - 2, dp).start()

    def on_position(f):
        for k in range(NZ):
            pl.when(z == k)(functools.partial(f, k))

    def first(b, n):
        c_copy(b, n).start()
        own_load(b, n).start()

    every(first, N_EARLY, N_EARLY + 2)
    on_position(w_first)
    every(first, N_EARLY + 2, N_BLOCK)
    for b in range(N_EARLY):
        early_load(b).start()

    def split(n):
        look_load(n).wait()
        value = look_in[n % 2]
        high = value.astype(BF16)
        left = value - high.astype(F32)
        middle = left.astype(BF16)
        at = pl.ds(pl.multiple_of(groups[n] * n_look, n_look), n_look)
        parts[0, at, :] = high
        parts[1, at, :] = middle
        parts[2, at, :] = (left - middle.astype(F32)).astype(BF16)
        if n + 2 < 4:
            look_load(n + 2).start()

    split(0)
    split(1)
    every(chip_sum, N_EARLY, N_EARLY + 3)
    on_position(w_second)
    every(chip_sum, N_EARLY + 3, AHEAD)
    split(2)
    split(3)
    every(early_sum, 0, N_EARLY)

    total = acc.at[tp]
    w_copy_x = remote(total, w_x, last_send.at[0], last_recv.at[0], tp, facing)
    w_copy_c = remote(total, w_out.at[core], last_send.at[1], last_recv.at[1], tp, twin)
    w_store = pltpu.make_async_copy(total, w_out.at[core], w_out_sem)
    n_small, n_rows = small_ref.shape[1], w_out.shape[1]
    mine = w_out.at[1, pl.ds(n_rows - 32, n_small), :]
    small_here = pltpu.make_async_copy(mine, small_ref.at[tp], w_out_sem)
    peers = [lax.rem(tp + n, 2 * NZ) for n in range(1, 2 * NZ)]
    for b in range(N_EARLY, N_BLOCK):
        n = last if b == N_BLOCK - 1 else size
        x_copy(b, n).wait_recv()
        add_into(part(from_x, b, n), part(s_buf, b, n), 24)
        t_copy(b, n).start()
        t_store(b, n).start()
        for k in range(NZ):
            if b in W_REDUCE[k]:
                pl.when(z == k)(functools.partial(w_reduce, k, W_REDUCE[k][b]))
        if b == 9:
            w_copy_x.start()
            every(chip_sum, AHEAD, N_BLOCK)
        if b == 10:
            w_copy_x.wait()
            add_into(total, w_x)
            w_copy_c.start()
            w_store.start()
            w_copy_c.wait_send()
            remote(total, w_out.at[1 - core], last_send.at[1], last_recv.at[1], tp, twin).wait_recv()
            w_store.wait()
            for to in peers:
                remote(mine, small_ref.at[tp], small_send.at[to], small_recv.at[tp], to, dp).start()
            small_here.start()
    for source in peers:
        remote(small_ref.at[source], small_ref.at[source], small_send.at[source], small_recv.at[source], source, dp).wait_recv()
        remote(mine, small_ref.at[tp], small_send.at[source], small_recv.at[tp], source, dp).wait_send()
    small_here.wait()

    def w_done(k):
        for zz in range(NZ):
            line = acc.at[2 * zz + y]
            for slot in (2 * zz + 1 - y, 2 * zz + y):
                remote(p_ref.at[slot, 1 - core], w_c.at[slot], send_c.at[slot], recv_c.at[slot], tp, twin).wait_send()
            remote(line, w_y.at[zz], send_y.at[zz], recv_y.at[zz], partner, dp).wait_send()
            if zz > k:
                remote(line, w_l.at[zz - 1], send_r.at[zz], recv_l.at[zz], tp + 2, dp).wait_send()
            if zz < k:
                remote(line, w_r.at[zz], send_l.at[zz], recv_r.at[zz], tp - 2, dp).wait_send()

    on_position(w_done)

    def drain(b, n):
        t_copy(b, n).wait_send()
        t_store(b, n).wait()
        remote(part(from_x, b, n), t_ref.at[rows(1 - core, b, n), :], g_send_t.at[b], g_recv_t.at[b], tp, twin).wait_recv()

    def sent(b, n):
        c_copy(b, n).wait_send()
        x_copy(b, n).wait_send()

    every(drain, 0, N_BLOCK)
    every(sent, N_EARLY, N_BLOCK)


def tail(g_table, g_rows, look_rows, look_ids, early, collective_id):
    vocab, width = g_table.shape
    rows = g_rows.shape[1]
    half = (rows // 2, width)
    n_look = look_ids.shape[2]
    size = table_block(vocab)
    blocks = lambda n: pltpu.VMEM((n, size, width), F32)
    dma = lambda *n: pltpu.SemaphoreType.DMA(n)
    t, w_sum, small = pl.pallas_call(
        tail_kernel,
        out_shape=(jax.ShapeDtypeStruct((vocab, width), F32), jax.ShapeDtypeStruct((2,) + half, F32), jax.ShapeDtypeStruct((2 * NZ, 24, width), F32)),
        in_specs=[ANY, ANY, ANY, VMEM, ANY],
        out_specs=(ANY,) * 3,
        scratch_shapes=[blocks(N_BLOCK - N_EARLY)] * 2 + [blocks(N_BLOCK), pltpu.VMEM((2, n_look, width), F32), pltpu.VMEM((3, 4 * n_look, width), BF16)]
        + [pltpu.VMEM((2 * NZ,) + half, F32)] * 2 + [pltpu.VMEM((NZ,) + half, F32)] + [pltpu.VMEM((NZ - 1,) + half, F32)] * 2
        + [pltpu.VMEM(half, F32)]
        + [dma(N_BLOCK)] * 8 + [dma(2)]
        + [dma(2 * NZ), pltpu.SemaphoreType.DMA] + [dma(2 * NZ), dma(NZ), dma(NZ), dma(NZ)] * 2 + [dma(2)] * 2 + [dma(2 * NZ)] * 2,
        compiler_params=pltpu.CompilerParams(collective_id=collective_id, has_side_effects=True, vmem_limit_bytes=67000000),
        name="tail",
    )(g_table, g_rows.reshape((2 * NZ, 2) + half), look_rows.reshape(4, n_look, width), look_ids, early)
    return t, w_sum.reshape(rows, width), small


UPDATE_ROWS = 512


def update_kernel(t_ref, w_ref, small_ref, *refs):
    state = [refs[7 * i:7 * i + 7] for i in range(3)]
    new = [refs[21 + 7 * i:28 + 7 * i] for i in range(3)]
    loss_ref = refs[42]
    held, made, in_sem, out_sem = refs[43:]
    vocab = t_ref.shape[0]
    n_kv, hd = 2 * state[0][3].shape[1] // small_ref.shape[0], state[0][3].shape[1]
    blocks = [(at, min(UPDATE_ROWS, vocab - at)) for at in range(0, vocab, UPDATE_ROWS)]

    def loads(q):
        at, n = blocks[q]
        return [pltpu.make_async_copy(ref.at[pl.ds(at, n), :], held.at[q % 3, i, pl.ds(0, n), :], in_sem.at[q % 3, i])
                for i, ref in enumerate((t_ref, state[0][0], state[1][0], state[2][0]))]

    def stores(q):
        at, n = blocks[q]
        return [pltpu.make_async_copy(made.at[q % 2, i, pl.ds(0, n), :], new[i][0].at[pl.ds(at, n), :], out_sem.at[q % 2, i]) for i in range(3)]

    for q in range(3):
        for c in loads(q):
            c.start()

    def small_update(index, grad, *where):
        got = adam_update(state[0][index][where], grad, state[1][index][where], state[2][index][where])
        for i in range(3):
            new[i][index][where] = got[i]

    n_q, n_f = state[0][2].shape[0], state[0][6].shape[0]
    small_update(1, small_ref[0, n_kv:n_kv + 2, :], Ellipsis)
    small_update(2, w_ref[0:n_q, :], Ellipsis)
    kv = small_ref[:, 0:n_kv, :].reshape(2 * hd, small_ref.shape[2])
    for i in range(2):
        small_update(3, kv[i * hd:(i + 1) * hd], i)
    small_update(4, w_ref[n_q:2 * n_q, :], Ellipsis)
    for i in range(2):
        small_update(5, w_ref[2 * n_q + i * n_f:2 * n_q + (i + 1) * n_f, :].T, i)
    small_update(6, w_ref[2 * n_q + 2 * n_f:2 * n_q + 3 * n_f, :], Ellipsis)
    loss_ref[...] = jnp.sum(small_ref[0, n_kv + 2:n_kv + 3, :], axis=1, keepdims=True)

    for q, (at, n) in enumerate(blocks):
        for c in loads(q):
            c.wait()
        if q >= 2:
            for c in stores(q - 2):
                c.wait()
        step = 32 if n % 32 == 0 else 16

        def body(j, carry):
            rows = pl.ds(pl.multiple_of(j * step, step), step)
            got = adam_update(held[q % 3, 1, rows, :], held[q % 3, 0, rows, :], held[q % 3, 2, rows, :], held[q % 3, 3, rows, :])
            for i in range(3):
                made[q % 2, i, rows, :] = got[i]
            return carry

        lax.fori_loop(0, n // step, body, 0)
        for c in stores(q):
            c.start()
        if q + 3 < len(blocks):
            for c in loads(q + 3):
                c.start()
    for q in range(len(blocks) - 2, len(blocks)):
        for c in stores(q):
            c.wait()


def update(g_table, g_shard, g_small, state_arrays):
    specs = [ANY] + [VMEM] * 6
    width = g_table.shape[1]

    def flip(arrays):
        return [a.swapaxes(-1, -2) if i % 7 in (2, 3) else a for i, a in enumerate(arrays)]

    given = flip(state_arrays)
    *new, loss = pl.pallas_call(
        update_kernel,
        out_shape=tuple(jax.ShapeDtypeStruct(a.shape, F32) for a in given) + (jax.ShapeDtypeStruct((1, 1), F32),),
        in_specs=[ANY, VMEM, VMEM] + specs * 3,
        out_specs=tuple(specs * 3) + (VMEM,),
        scratch_shapes=[pltpu.VMEM((3, 4, UPDATE_ROWS, width), F32), pltpu.VMEM((2, 3, UPDATE_ROWS, width), F32),
                        pltpu.SemaphoreType.DMA((3, 4)), pltpu.SemaphoreType.DMA((2, 3))],
        compiler_params=pltpu.CompilerParams(vmem_limit_bytes=60000000),
        name="update",
    )(g_table, g_shard, g_small, *given)
    return flip(new) + [loss]


def norm_fwd(x_f32, scale):
    centered = x_f32 - jnp.mean(x_f32, axis=-1, keepdims=True)
    inv_std = lax.rsqrt(jnp.mean(centered * centered, axis=-1, keepdims=True) + LN_EPS)
    x_hat = centered * inv_std
    return (x_hat * scale).astype(BF16), x_hat, inv_std


def norm_bwd(d_out, x_hat, inv_std, scale):
    d_scale = jnp.sum(d_out * x_hat, axis=0)
    d_hat = d_out * scale
    d_in = inv_std * (d_hat - jnp.mean(d_hat, axis=-1, keepdims=True) - x_hat * jnp.mean(d_hat * x_hat, axis=-1, keepdims=True))
    return d_in, d_scale


def adam_update(param_in, grad_in, mom_in, vel_in):
    mom_new = BETA_ONE * mom_in + (1.0 - BETA_ONE) * grad_in
    vel_new = BETA_TWO * vel_in + (1.0 - BETA_TWO) * grad_in * grad_in
    return param_in - LEARN_RATE * mom_new / (jnp.sqrt(vel_new) + ADAM_EPS), mom_new, vel_new


def dot(spec, a, b):
    return jnp.einsum(spec, a, b, preferred_element_type=F32)


def solution(mesh):
    param_specs = (P('tp', None), P(None, None), P(None, 'tp'), P(None, None, None), P('tp', None), P(None, None, 'tp'), P('tp', None))
    n_tp = mesh.shape['tp']
    n_dp = mesh.shape['dp']

    def local_step(tokens, labels, *state_arrays):
        embed, ln_scales, w_q, w_kv, w_o, w_gu, w_down = state_arrays[0:7]
        batch_loc, seq_len = tokens.shape
        vocab_loc, d_model = embed.shape
        head_dim = w_kv.shape[2]
        q_loc = w_q.shape[1]
        f_loc = w_down.shape[0]
        tok_loc = batch_loc * seq_len
        tok_total = tok_loc * n_dp
        own = tok_loc // n_tp
        tp_rank = lax.axis_index('tp')
        half = tp_rank % 2

        strict = (jnp.arange(own)[:, None] > jnp.arange(own)[None, :]).astype(BF16)

        def routing(chunks):
            shard = chunks // vocab_loc
            row = chunks - shard * vocab_loc
            hot = (shard[:, :, None] == jnp.arange(n_tp)[None, None, :])
            before = dot('rs,nsj->nrj', strict, hot.astype(BF16))
            rank = jnp.sum(jnp.where(hot, before, 0.0), axis=-1).astype(jnp.int32)
            most = jnp.max(jnp.sum(hot.astype(jnp.int32), axis=1))
            return shard, row, rank, (most + CAP - 1) // CAP

        chunks = tokens.reshape(n_tp, own)
        shard, row, rank, rounds = routing(chunks)
        slots = jnp.arange(CAP)
        my_shard = lax.dynamic_index_in_dim(shard, tp_rank, 0, keepdims=False)
        my_rank = lax.dynamic_index_in_dim(rank, tp_rank, 0, keepdims=False)

        def fetch(step):
            here = (shard[:, None, :] == tp_rank) & (rank[:, None, :] == slots[None, :, None] + step * CAP)
            ids = jnp.sum(jnp.where(here, row[:, None, :], 0), axis=-1).reshape(-1)
            pick = (my_shard[:, None, None] == jnp.arange(n_tp)[None, :, None]) & (my_rank[:, None, None] == slots[None, None, :] + step * CAP)
            return ids, pick.reshape(own, n_tp * CAP).astype(BF16)

        def fetch_more(state):
            ids, pick = fetch(state[0])
            rows_in = plane_swap(jnp.take(embed, ids, axis=0).reshape(n_tp, CAP, d_model), 1).reshape(n_tp * CAP, d_model).astype(BF16)
            return state[0] + 1, state[1] + dot('rc,cd->rd', pick, rows_in)

        more_rows = lax.while_loop(lambda state: state[0] < rounds, fetch_more, (jnp.int32(1), jnp.zeros((own, d_model), F32)))[1]
        ids_first, pick_first = fetch(0)

        w_rows = jnp.concatenate([w_q.T, w_o, w_gu.transpose(0, 2, 1).reshape(2 * f_loc, d_model), w_down], axis=0)
        cuts = (q_loc, 2 * q_loc, 2 * q_loc + f_loc, 2 * q_loc + 2 * f_loc)
        wkv_t = w_kv.transpose(0, 2, 1).reshape(2 * head_dim, d_model).astype(BF16)
        inv_freq = ROPE_BASE ** (-jnp.arange(0, head_dim, 2).astype(F32) / head_dim)
        angles = inv_freq[:, None] * (half * own + jnp.arange(own)).astype(F32)[None, :]
        cos_t, sin_t = jnp.cos(angles), jnp.sin(angles)
        f_own, x_one, x_zero, *saved = front(ids_first, embed, jnp.broadcast_to(rounds, (1, 128)), pick_first, more_rows, w_rows, wkv_t, ln_scales, cos_t, sin_t, n_tp * q_loc, 0)
        saved, (wq_t, wo_b, wg_t, wu_t, wd_b), rounds_all = saved[:5], saved[5:10], jnp.max(saved[10])
        weights = (wq_t, wkv_t, wo_b, wg_t, wu_t, wd_b)

        logit_scale = d_model ** -0.5
        lab_loc = labels.reshape(n_tp, own) - tp_rank * vocab_loc
        d_fin, g_head_part, log_norm, lab_sum, _ = head(f_own, lab_loc, embed, logit_scale, logit_scale / tok_total, 4)
        log_norm = lax.dynamic_index_in_dim(log_norm, tp_rank, 0, keepdims=False)
        loss_row = (log_norm + LOGIT_ZLOSS * log_norm * log_norm - jnp.sum(lab_sum, axis=0) * logit_scale) / tok_total
        def row_ids(step):
            here = (shard[:, None, :] == tp_rank) & (rank[:, None, :] == slots[None, :, None] + step * CAP)
            return jnp.where(jnp.any(here, axis=-1), jnp.sum(jnp.where(here, row[:, None, :], 0), axis=-1), vocab_loc).reshape(-1)

        g_rows, d_zero, rows_back, early, ids_back = layer_bwd(d_fin, x_zero, x_one, loss_row[None, :], ln_scales, cos_t, sin_t, weights, saved,
                                                               pick_first, g_head_part, row_ids(0)[None, :], 7)
        g_table, g_shard, g_small = tail(g_head_part, g_rows, rows_back, ids_back, early, 10)

        def give_back(state):
            mine = (my_shard[None, None, :] == jnp.arange(n_tp)[:, None, None]) & (my_rank[None, None, :] == slots[None, :, None] + state[0] * CAP)
            ids = jnp.sum(jnp.where(mine, jnp.arange(own)[None, None, :], 0), axis=-1).reshape(-1)
            rows_in = plane_swap(jnp.take(d_zero, ids, axis=0).reshape(n_tp, CAP, d_model), 9).reshape(-1, d_model)
            n_rows = n_tp * CAP
            id_rows = jnp.pad(row_ids(state[0]).astype(F32), (0, -n_rows % (8 * d_model))).reshape(-1, d_model)
            both = group_gather(jnp.concatenate([rows_in, id_rows], axis=0), 11)
            ids = both[:, n_rows:].reshape(n_dp, -1)[:, :n_rows].astype(jnp.int32)
            return state[0] + 1, state[1].at[ids.reshape(-1)].add(both[:, :n_rows].reshape(-1, d_model), mode='drop')

        g_table = lax.while_loop(lambda state: state[0] < rounds_all, give_back, (jnp.int32(1), g_table))[1]
        *new, loss = update(g_table, g_shard, g_small, state_arrays)
        return tuple(new) + (loss.reshape(()),)

    return jax.shard_map(local_step, mesh=mesh, in_specs=(P('dp', None), P('dp', None)) + param_specs * 3,
                         out_specs=param_specs * 3 + (P(),), check_vma=False)
```

```python
import functools

import jax
import jax.numpy as jnp
from jax import lax
from jax.experimental import pallas as pl
from jax.experimental.pallas import tpu as pltpu
from jax.sharding import PartitionSpec as P

LN_EPS = 1e-5
LOGIT_ZLOSS = 1e-4
LEARN_RATE = 1e-2
BETA_ONE = 0.9
BETA_TWO = 0.95
ADAM_EPS = 1e-8
ROPE_BASE = 10000.0
NZ = 4
CAP = 96
F32 = jnp.float32
BF16 = jnp.bfloat16
ANY = pl.BlockSpec(memory_space=pl.ANY)
VMEM = pl.BlockSpec(memory_space=pltpu.VMEM)

ARRIVALS = {
    0: (("R", 1), ("R", 2), ("R", 3)),
    1: (("L", 0), ("R", 2), ("R", 3)),
    2: (("R", 3), ("L", 1), ("L", 0)),
    3: (("L", 2), ("L", 1), ("L", 0)),
}
REDUCE_ORDER = {0: (3, 2, 1, 0), 1: (3, 0, 2, 1), 2: (0, 3, 1, 2), 3: (0, 1, 2, 3)}


def remote(src, dst, send_sem, recv_sem, tp, dp):
    return pltpu.make_async_remote_copy(src_ref=src, dst_ref=dst, send_sem=send_sem, recv_sem=recv_sem,
                                        device_id=(tp, dp), device_id_type=pl.DeviceIdType.MESH)


def place():
    tp = lax.axis_index("tp")
    dp = lax.axis_index("dp")
    return tp, dp, tp // 2, tp % 2


def signal(tp, dp):
    pl.semaphore_signal(pltpu.get_barrier_semaphore(), inc=1, device_id=(tp, dp), device_id_type=pl.DeviceIdType.MESH)


def add_into(acc, other, step=None):
    rows = acc.shape[0]
    step = step or (64 if rows % 64 == 0 else 8)

    def body(n, carry):
        at = pl.ds(pl.multiple_of(n * step, step), step)
        acc[at, :] = acc[at, :] + other[at, :]
        return carry

    lax.fori_loop(0, rows // step, body, 0)


def plane_barrier(tp, dp, others):
    peers = [(lax.rem(tp + n, 2 * NZ), dp) for n in range(1, 2 * NZ)] + others
    for peer in peers:
        signal(*peer)
    pl.semaphore_wait(pltpu.get_barrier_semaphore(), len(peers))


def swap_kernel(x_ref, out_ref, own_sem, send, recv):
    tp, dp, _, _ = place()
    plane_barrier(tp, dp, [])
    copies = []
    for n in range(1, 2 * NZ):
        to = lax.rem(tp + n, 2 * NZ)
        copy = remote(x_ref.at[to], out_ref.at[tp], send.at[to], recv.at[tp], to, dp)
        copy.start()
        copies.append(copy)
    own = pltpu.make_async_copy(x_ref.at[tp], out_ref.at[tp], own_sem)
    own.start()
    for n in range(1, 2 * NZ):
        source = lax.rem(tp + n, 2 * NZ)
        remote(out_ref.at[source], out_ref.at[source], send.at[source], recv.at[source], source, dp).wait_recv()
    own.wait()
    for copy in copies:
        copy.wait_send()


def plane_swap(x, collective_id):
    return pl.pallas_call(
        swap_kernel,
        out_shape=jax.ShapeDtypeStruct(x.shape, x.dtype),
        in_specs=[ANY],
        out_specs=ANY,
        scratch_shapes=[pltpu.SemaphoreType.DMA] + [pltpu.SemaphoreType.DMA((2 * NZ,))] * 2,
        compiler_params=pltpu.CompilerParams(collective_id=collective_id, has_side_effects=True),
        name="plane_swap",
    )(x)


def group_kernel(x_ref, out_ref, own_sem, send, recv):
    tp, dp, _, _ = place()
    group = [lax.rem(dp + n, 4) for n in range(1, 4)]
    for to in group:
        signal(tp, to)
    pl.semaphore_wait(pltpu.get_barrier_semaphore(), 3)
    own = pltpu.make_async_copy(x_ref, out_ref.at[dp], own_sem)
    own.start()
    for n, to in enumerate(group):
        remote(x_ref, out_ref.at[dp], send.at[n], recv.at[dp], tp, to).start()
    own.wait()
    for n, to in enumerate(group):
        remote(x_ref, out_ref.at[to], send.at[n], recv.at[to], tp, to).wait_recv()
        remote(x_ref, out_ref.at[dp], send.at[n], recv.at[dp], tp, to).wait_send()


def group_gather(x, collective_id):
    return pl.pallas_call(
        group_kernel,
        out_shape=jax.ShapeDtypeStruct((4,) + x.shape, x.dtype),
        in_specs=[ANY],
        out_specs=ANY,
        scratch_shapes=[pltpu.SemaphoreType.DMA, pltpu.SemaphoreType.DMA((3,)), pltpu.SemaphoreType.DMA((4,))],
        compiler_params=pltpu.CompilerParams(collective_id=collective_id, has_side_effects=True),
        name="group_gather",
    )(x)


GATHER_ORDER = {
    0: ((0, 0), (0, 1), (1, 0), (0, 2), (1, 1), (0, 3), (1, 2), (1, 3)),
    1: ((0, 1), (0, 0), (0, 2), (1, 1), (1, 0), (0, 3), (1, 2), (1, 3)),
    2: ((0, 2), (0, 1), (0, 3), (1, 2), (0, 0), (1, 3), (1, 1), (1, 0)),
    3: ((0, 3), (0, 2), (1, 3), (0, 1), (1, 2), (0, 0), (1, 1), (1, 0)),
}
GATHER_EVENTS = {
    0: {
        1: ((0, 1, 0, 'y'), (1, 0, 1, 'r'), (0, 1, 1, 'y'), (1, 0, 0, '')),
        3: ((0, 2, 0, 'y'), (1, 1, 0, ''), (0, 2, 1, 'y'), (1, 1, 1, '')),
        5: ((0, 3, 0, 'y'), (1, 2, 0, ''), (0, 3, 1, ''), (1, 2, 1, '')),
        7: ((1, 3, 0, ''), (1, 3, 1, '')),
    },
    1: {
        1: ((0, 0, 0, 'ry'), (0, 2, 0, 'ly'), (1, 1, 0, ''), (0, 0, 1, 'r'), (0, 2, 1, 'ly'), (1, 1, 1, '')),
        4: ((0, 3, 0, 'ly'), (1, 0, 0, ''), (1, 0, 1, 'r')),
        5: ((0, 3, 1, 'l'), (1, 2, 0, '')),
        6: ((1, 2, 1, ''), (1, 3, 1, 'l')),
        7: ((1, 3, 0, ''),),
    },
    2: {
        1: ((0, 1, 0, 'ry'), (0, 3, 0, 'ly'), (1, 2, 0, ''), (0, 1, 1, 'ry'), (0, 3, 1, 'l'), (1, 2, 1, '')),
        4: ((0, 0, 0, 'ry'), (1, 1, 0, ''), (1, 3, 1, 'l'), (0, 0, 1, 'r'), (1, 3, 0, '')),
        6: ((1, 0, 1, 'r'), (1, 1, 1, '')),
        7: ((1, 0, 0, ''),),
    },
    3: {
        1: ((0, 2, 0, 'y'), (1, 3, 1, 'l'), (0, 2, 1, 'y'), (1, 3, 0, '')),
        3: ((0, 1, 0, 'y'), (1, 2, 0, ''), (0, 1, 1, 'y'), (1, 2, 1, '')),
        5: ((0, 0, 0, 'y'), (1, 1, 0, ''), (0, 0, 1, ''), (1, 1, 1, '')),
        7: ((1, 0, 0, ''), (1, 0, 1, '')),
    },
}
SCATTER_ORDER = {
    0: ((1, 3), (1, 2), (0, 3), (1, 1), (0, 2), (1, 0), (0, 1), (0, 0)),
    1: ((1, 3), (1, 2), (0, 3), (1, 0), (1, 1), (0, 2), (0, 0), (0, 1)),
    2: ((1, 0), (1, 1), (1, 3), (0, 0), (1, 2), (0, 3), (0, 1), (0, 2)),
    3: ((1, 0), (1, 1), (0, 0), (1, 2), (0, 1), (1, 3), (0, 2), (0, 3)),
}
SCATTER_EVENTS = {
    0: {
        0: ((1, 3, 0, '', 'y'), (1, 3, 1, '', 'r')),
        1: ((1, 2, 0, '', 'y'), (1, 2, 1, '', 'y')),
        2: ((0, 3, 1, '', 'r'), (0, 3, 0, 'y', 'r')),
        3: ((1, 1, 0, '', 'y'), (1, 1, 1, '', 'y')),
        4: ((0, 2, 0, 'y', 'r'),),
        5: ((0, 2, 1, 'y', 'r'), (1, 0, 0, '', 'y')),
        6: ((1, 0, 1, 'r', 'y'), (0, 1, 0, 'y', 'r')),
        7: ((0, 1, 1, 'y', 'r'), (0, 0, 0, 'ry', ''), (0, 0, 1, 'ry', '')),
    },
    1: {
        0: ((1, 3, 0, '', 'y'),),
        1: ((1, 2, 0, '', 'y'), (1, 2, 1, '', 'y')),
        2: ((1, 3, 1, 'l', 'r'),),
        3: ((1, 0, 0, '', 'y'),),
        4: ((0, 3, 1, 'l', 'r'), (1, 0, 1, 'r', 'l'), (1, 1, 0, '', 'y'), (1, 1, 1, '', 'y')),
        6: ((0, 3, 0, 'ly', 'r'), (0, 0, 1, 'r', 'l')),
        7: ((0, 2, 0, 'ly', 'r'), (0, 0, 0, 'ry', 'l'), (0, 2, 1, 'ly', 'r'), (0, 1, 0, 'lry', ''), (0, 1, 1, 'lry', '')),
    },
    2: {
        0: ((1, 0, 0, '', 'y'),),
        1: ((1, 1, 0, '', 'y'), (1, 1, 1, '', 'y')),
        2: ((1, 0, 1, 'r', 'l'), (1, 3, 0, '', 'y')),
        4: ((1, 3, 1, 'l', 'r'), (0, 0, 1, 'r', 'l'), (1, 2, 0, '', 'y'), (1, 2, 1, '', 'y')),
        6: ((0, 0, 0, 'ry', 'l'), (0, 3, 1, 'l', 'r')),
        7: ((0, 1, 0, 'ry', 'l'), (0, 3, 0, 'ly', 'r'), (0, 1, 1, 'ry', 'l'), (0, 2, 0, 'lry', ''), (0, 2, 1, 'lry', '')),
    },
    3: {
        0: ((1, 0, 0, '', 'y'), (1, 0, 1, '', 'l')),
        1: ((1, 1, 0, '', 'y'), (1, 1, 1, '', 'y')),
        2: ((0, 0, 1, '', 'l'), (0, 0, 0, 'y', 'l')),
        3: ((1, 2, 0, '', 'y'), (1, 2, 1, '', 'y')),
        4: ((0, 1, 0, 'y', 'l'),),
        5: ((0, 1, 1, 'y', 'l'), (1, 3, 0, '', 'y')),
        6: ((1, 3, 1, 'l', 'y'), (0, 2, 0, 'y', 'l')),
        7: ((0, 2, 1, 'y', 'l'), (0, 3, 0, 'ly', ''), (0, 3, 1, 'ly', '')),
    },
}
SUB = 256
GROUP = 6


def lookup(table, z, step):
    value = jnp.int32(0)
    for k in range(NZ):
        for s in range(2 * NZ):
            value = value + jnp.where((z == k) & (step == s), table[k][s], 0)
    return value


def head_kernel(scale, token_scale, f_ref, lab_ref, e_ref, dfin_ref, ghead_ref, norm_ref, labsum_ref, z_ref,
                e_b, e_t, fbuf, f_b, g_acc, from_y, from_l, from_r, dl, z_buf, z_rest, lse_all, z_sem, load_sem, ag_send, ag_recv,
                send_y, send_l, send_r, recv_y, recv_l, recv_r, st_send, st_recv):
    tp, dp, z, y = place()
    partner = tp + 1 - 2 * y
    vocab, width = e_ref.shape
    own = f_ref.shape[0]
    whole = vocab // (SUB * GROUP)
    rest = vocab - whole * SUB * GROUP
    log2e = 1.4426950408889634
    slope = scale * log2e
    blocks = [(j * SUB, SUB) for j in range(GROUP)]
    tail = [(n, min(SUB, rest - n)) for n in range(0, rest, SUB)]

    plane_barrier(tp, dp, [])

    half = own // 2
    to_tp = {"l": tp - 2, "r": tp + 2, "y": partner}

    def slot_of(o, zz):
        return 2 * zz + (1 - y if o else y)

    def piece(ref, h):
        return ref.at[pl.ds(h * half, half), :]

    def pass_on(o, zz, h, to, own_chunk=False):
        slot = slot_of(o, zz)
        return remote(piece(f_ref if own_chunk else fbuf.at[slot], h), piece(fbuf.at[slot], h), ag_send.at["lry".index(to), slot, h],
                      ag_recv.at[slot, h], to_tp[to], dp)

    def arrived(o, zz, h):
        slot = slot_of(o, zz)
        remote(piece(f_ref, h), piece(fbuf.at[slot], h), ag_send.at[0, slot, h], ag_recv.at[slot, h], partner, dp).wait_recv()

    def own_sends(k):
        first = (1, 0) if k in (0, NZ - 1) else (0, 1)
        return [pass_on(0, k, h, "y", True) for h in first] + [
            pass_on(0, k, h, to, True) for h in range(2) for to in ("l" if k > 0 else "") + ("r" if k < NZ - 1 else "")]

    def on_position(f):
        for k in range(NZ):
            pl.when(z == k)(functools.partial(f, k))

    def first_sends(k):
        for c in own_sends(k):
            c.start()

    on_position(first_sends)
    load = pltpu.make_async_copy(e_ref, g_acc, load_sem.at[0])
    load.start()
    own_copy = pltpu.make_async_copy(f_ref, fbuf.at[tp], load_sem.at[1])
    own_copy.start()
    load.wait()

    def prepare(at, size):
        part = g_acc[at, :]
        e_b[at, :] = part.astype(BF16)
        e_t[:, at] = part.T.astype(BF16)

    def prepare_body(n, carry):
        prepare(pl.ds(pl.multiple_of(n * SUB, SUB), SUB), SUB)
        return carry

    lax.fori_loop(0, vocab // SUB, prepare_body, 0)
    if vocab % SUB:
        prepare(pl.ds(vocab // SUB * SUB, vocab % SUB), vocab % SUB)
    own_copy.wait()

    big = SUB * GROUP

    def z_copies(slot, n, out):
        if n is None:
            pair = (z_rest, z_ref.at[slot, pl.ds(whole * big, rest), :])
            sem = z_sem.at[2]
        else:
            pair = (z_buf.at[lax.rem(n, 2)], z_ref.at[slot, pl.ds(pl.multiple_of(n * big, big), big), :])
            sem = z_sem.at[lax.rem(n, 2)]
        return pltpu.make_async_copy(*(pair if out else pair[::-1]), sem)

    def slot_at(order, step):
        code = lookup({k: [2 * zz + o for o, zz in order[k]] for k in range(NZ)}, z, step)
        other = code % 2
        return code // 2 * 2 + y + other - 2 * y * other

    def gather_step(step, carry):
        for k in range(NZ):
            for at, events in GATHER_EVENTS[k].items():
                def serve(events=events):
                    for o, zz, h, to in events:
                        arrived(o, zz, h)
                        for t in to:
                            pass_on(o, zz, h, t).start()
                pl.when((z == k) & (step == at))(serve)
        slot = slot_at(GATHER_ORDER, step)
        f_b[slot] = fbuf[slot].astype(BF16)
        f_now = f_b[slot]

        def group(base, parts, kept, c):
            top, total = c
            for first, size in parts:
                logit = lax.dot_general(e_b[pl.ds(base + first, size), :], f_now, (((1,), (1,)), ((), ())), preferred_element_type=F32)
                kept[pl.ds(first, size), :] = logit
                logit = logit.reshape(size // 8, 8, own)
                new = jnp.maximum(top, jnp.max(logit, axis=0))
                total = total * jnp.exp2((top - new) * slope) + jnp.sum(jnp.exp2((logit - new[None]) * slope), axis=0)
                top = new
            return top, total

        def body(n, c):
            @pl.when(step * whole + n >= 2)
            def _():
                z_copies(slot, n, True).wait()
            c = group(pl.multiple_of(n * big, big), blocks, z_buf.at[lax.rem(n, 2)], c)
            z_copies(slot, n, True).start()
            return c

        top, total = lax.fori_loop(0, whole, body, (jnp.full((8, own), -3e38, F32), jnp.zeros((8, own), F32)))
        if tail:
            @pl.when(step > 0)
            def _():
                z_copies(slot, None, True).wait()
            top, total = group(whole * big, tail, z_rest, (top, total))
            z_copies(slot, None, True).start()
        most = jnp.max(top, axis=0, keepdims=True)
        total = jnp.sum(total * jnp.exp2((top - most) * slope), axis=0, keepdims=True)
        lse_all[tp, pl.ds(slot, 1), :] = most * scale + jnp.log(total)
        return carry

    lax.fori_loop(0, 2 * NZ, gather_step, 0)
    for n in range(2):
        z_copies(0, jnp.int32(n), True).wait()
    if tail:
        z_copies(0, None, True).wait()

    for n in range(1, 2 * NZ):
        to = lax.rem(tp + n, 2 * NZ)
        remote(lse_all.at[tp], lse_all.at[tp], st_send.at[to], st_recv.at[tp], to, dp).start()

    def gathers_done(k):
        for c in own_sends(k):
            c.wait_send()
        for events in GATHER_EVENTS[k].values():
            for o, zz, h, to in events:
                for t in to:
                    pass_on(o, zz, h, t).wait_send()

    on_position(gathers_done)
    start_slot = slot_at(SCATTER_ORDER, 0)
    for n in range(2):
        z_copies(start_slot, jnp.int32(n), False).start()
    if tail:
        z_copies(start_slot, None, False).start()

    def clear(n, carry):
        g_acc[pl.ds(pl.multiple_of(n * 16, 16), 16), :] = jnp.zeros((16, width), F32)
        return carry

    lax.fori_loop(0, vocab // 16, clear, 0)
    for n in range(1, 2 * NZ):
        source = lax.rem(tp + n, 2 * NZ)
        remote(lse_all.at[source], lse_all.at[source], st_send.at[source], st_recv.at[source], source, dp).wait_recv()
    peak = jnp.max(lse_all[...], axis=0)
    log_norm = peak + jnp.log(jnp.sum(jnp.exp(lse_all[...] - peak[None]), axis=0))
    norm_ref[...] = log_norm

    def leave(o, zz, h, to):
        src = piece(fbuf.at[slot_of(o, zz)], h)
        if to == "y":
            at = 2 * zz + h
            return remote(src, from_y.at[at], send_y.at[at], recv_y.at[at], partner, dp)
        if to == "l":
            at = 6 if o else 2 * zz + h
            return remote(src, from_r.at[at], send_l.at[at], recv_r.at[at], tp - 2, dp)
        at = 6 if o else 2 * zz - 2 + h
        return remote(src, from_l.at[at], send_r.at[at], recv_l.at[at], tp + 2, dp)

    def collect(o, zz, h, sums, to):
        here = piece(fbuf.at[slot_of(o, zz)], h)
        for d in sums:
            at, buf, sem = {"y": (2 * zz + h, from_y, recv_y), "l": (6 if o else 2 * zz - 2 + h, from_l, recv_l),
                            "r": (6 if o else 2 * zz + h, from_r, recv_r)}[d]
            remote(here, buf.at[at], send_y.at[0], sem.at[at], partner, dp).wait_recv()
            add_into(here, buf.at[at])
        if to:
            leave(o, zz, h, to).start()

    def scatter_step(step, lab_sum):
        slot = slot_at(SCATTER_ORDER, step)
        f_now = f_b[slot]
        acc = fbuf.at[slot]
        norm = norm_ref[pl.ds(slot, 1), :]
        shift = norm * log2e
        coef = (1.0 + 2.0 * LOGIT_ZLOSS * norm) * token_scale
        lab = lab_ref[pl.ds(slot, 1), :] - tp * vocab
        acc[...] = jnp.zeros((width, own), F32)

        def group(base, parts, kept, hits):
            for first, size in parts:
                at = pl.ds(base + first, size)
                logit = kept[pl.ds(first, size), :]
                hit = lax.broadcasted_iota(jnp.int32, (size, own), 0) == lab - (base + first)
                prob = jnp.exp2(logit * slope - shift) * coef
                grad = jnp.where(hit, prob - token_scale, prob).astype(BF16)
                hits = hits + jnp.sum(jnp.where(hit, logit, 0.0).reshape(size // 8, 8, own), axis=0)
                dl[pl.ds(first, size), :] = grad
                g_acc[at, :] += jnp.dot(grad, f_now, preferred_element_type=F32)
            size = parts[-1][0] + parts[-1][1]
            acc[...] += jnp.dot(e_t[:, pl.ds(base, size)], dl[pl.ds(0, size), :], preferred_element_type=F32)
            return hits

        following = slot_at(SCATTER_ORDER, jnp.minimum(step + 1, 2 * NZ - 1))

        def body(n, hits):
            z_copies(slot, n, False).wait()
            hits = group(pl.multiple_of(n * big, big), blocks, z_buf.at[lax.rem(n, 2)], hits)

            @pl.when(n + 2 < whole)
            def _():
                z_copies(slot, n + 2, False).start()

            @pl.when((n + 2 >= whole) & (step + 1 < 2 * NZ))
            def _():
                z_copies(following, n + 2 - whole, False).start()
            return hits

        lab_sum = lax.fori_loop(0, whole, body, lab_sum)
        if tail:
            z_copies(slot, None, False).wait()
            lab_sum = group(whole * big, tail, z_rest, lab_sum)

            @pl.when(step + 1 < 2 * NZ)
            def _():
                z_copies(following, None, False).start()

        for k in range(NZ):
            for at, events in SCATTER_EVENTS[k].items():
                def reduce(events=events):
                    for event in events:
                        collect(*event)
                pl.when((z == k) & (step == at))(reduce)
        return lab_sum

    lab_sum = lax.fori_loop(0, 2 * NZ, scatter_step, jnp.zeros((8, own), F32))
    labsum_ref[...] = lab_sum
    store = pltpu.make_async_copy(g_acc, ghead_ref, load_sem.at[0])
    store.start()
    dfin_ref[...] = fbuf[tp].T

    def scatters_done(k):
        for events in SCATTER_EVENTS[k].values():
            for o, zz, h, _, to in events:
                if to:
                    leave(o, zz, h, to).wait_send()

    on_position(scatters_done)
    for n in range(1, 2 * NZ):
        to = lax.rem(tp + n, 2 * NZ)
        remote(lse_all.at[tp], lse_all.at[tp], st_send.at[to], st_recv.at[tp], to, dp).wait_send()
    store.wait()


def head(f_own, labels, embed, scale, token_scale, collective_id):
    own, width = f_own.shape
    vocab = embed.shape[0]
    chunk = (own, width)
    strips = lambda n: pltpu.VMEM((n, own // 2, width), F32)
    dma = lambda *n: pltpu.SemaphoreType.DMA(n)
    return pl.pallas_call(
        functools.partial(head_kernel, scale, token_scale),
        out_shape=(jax.ShapeDtypeStruct((own, width), F32), jax.ShapeDtypeStruct((vocab, width), F32),
                   jax.ShapeDtypeStruct((2 * NZ, own), F32), jax.ShapeDtypeStruct((8, own), F32),
                   jax.ShapeDtypeStruct((2 * NZ, vocab, own), F32)),
        in_specs=[VMEM, VMEM, ANY],
        out_specs=(VMEM, ANY, VMEM, VMEM, ANY),
        scratch_shapes=[pltpu.VMEM((vocab, width), BF16), pltpu.VMEM((width, vocab), BF16),
                        pltpu.VMEM((2 * NZ,) + chunk, F32), pltpu.VMEM((2 * NZ,) + chunk, BF16), pltpu.VMEM((vocab, width), F32),
                        strips(8), strips(7), strips(7),
                        pltpu.VMEM((SUB * GROUP, own), BF16), pltpu.VMEM((2, SUB * GROUP, own), F32),
                        pltpu.VMEM((max(vocab % (SUB * GROUP), 8), own), F32), pltpu.VMEM((2 * NZ, 2 * NZ, own), F32),
                        dma(3), dma(2), dma(3, 2 * NZ, 2), dma(2 * NZ, 2), dma(8), dma(7), dma(7), dma(8), dma(7), dma(7), dma(2 * NZ), dma(2 * NZ)],
        compiler_params=pltpu.CompilerParams(collective_id=collective_id, has_side_effects=True, vmem_limit_bytes=67000000),
        cost_estimate=pl.CostEstimate(flops=8 * vocab * width * own * 8, bytes_accessed=3 * 4 * vocab * width, transcendentals=2 * vocab * own * 8),
        name="head",
    )(f_own, labels, embed)


TB = (((1,), (1,)), ((), ()))
TA = (((0,), (0,)), ((), ()))
LOG2E = 1.4426950408889634


def mm(a, b, dims=(((1,), (0,)), ((), ()))):
    return lax.dot_general(a, b, dims, preferred_element_type=F32)


def picks(code, n_slots):
    return (lax.broadcasted_iota(jnp.int32, (n_slots, code.shape[1]), 0) == code).astype(F32).astype(BF16)


def turn(lo, hi, cos_t, sin_t):
    return lo * cos_t - hi * sin_t, hi * cos_t + lo * sin_t


EVENTS = {
    0: (((("R", 1),), (0,)), ((("R", 2),), (1,)), ((("R", 3),), (2,)), ((), (3,))),
    1: (((("L", 0), ("R", 2)), (1,)), ((("R", 3),), (0,)), ((), (2,)), ((), (3,))),
    2: (((("R", 3), ("L", 1)), (2,)), ((("L", 0),), (3,)), ((), (1,)), ((), (0,))),
    3: (((("L", 2),), (3,)), ((("L", 1),), (2,)), ((("L", 0),), (1,)), ((), (0,))),
}
MLP_ORDER = {k: [2 * k] + [code for line, other in EVENTS[k] for code in [2 * zz for _, zz in line] + [2 * zz + 1 for zz in other]] for k in range(NZ)}


def front_kernel(ids_ref, e_ref, rounds_ref, code_ref, extra_ref, w_ref, wkv_ref, ln_ref, cos_ref, sin_ref,
                 f_ref, x1_ref, x0_ref, q_ref, kv_ref, kvt_ref, lse_ref, ctx_ref, wq_ref, wo_ref, wg_ref, wu_ref, wd_ref, rounds_all,
                 table, rows_ref, wl, rows_in, u_b, kv_out, kv_in, own_sem, r_send, r_recv, a_y, a_l, a_r, a_c, a_recv,
                 b_y, b_l, b_r, b_x, b_c, b_recv, kv_send, kv_recv, n_send, n_recv):
    tp, dp, z, y = place()
    partner = tp + 1 - 2 * y
    core = dp % 2
    twin = dp + 1 - 2 * core
    facing = lax.rem(dp + 2, 4)
    own, width = x0_ref.shape
    shards, w_rows = wl.shape[0], wl.shape[1]
    nq = q_ref.shape[0]
    ff = wg_ref.shape[0]
    n_a = nq // shards
    n_f = ff // shards
    n_b = 3 * n_f // 4
    hd = kv_out.shape[0] // 2
    quarter = hd // 2
    heads = nq // hd

    def a_rows(c):
        return pl.ds(pl.multiple_of(c * n_a, 8), n_a)

    def b_rows(d):
        return pl.ds(pl.multiple_of(2 * n_a + d * n_b, 8), n_b)

    def a_copy(slot, sems, to, to_dp, first=False):
        src = w_ref.at[a_rows(core), :] if first else wl.at[slot, a_rows(core), :]
        return remote(src, wl.at[slot, a_rows(core), :], sems.at[slot], a_recv.at[slot, core], to, to_dp)

    def b_copy(slot, piece, sems, to, to_dp, first=False):
        src = w_ref.at[b_rows(piece), :] if first else wl.at[slot, b_rows(piece), :]
        return remote(src, wl.at[slot, b_rows(piece), :], sems.at[slot], b_recv.at[slot, piece], to, to_dp)

    def a_wait(slot, c):
        remote(w_ref.at[a_rows(c), :], wl.at[slot, a_rows(c), :], a_y.at[slot], a_recv.at[slot, c], partner, dp).wait_recv()

    def b_wait(slot, piece):
        remote(w_ref.at[b_rows(piece), :], wl.at[slot, b_rows(piece), :], b_y.at[slot], b_recv.at[slot, piece], partner, dp).wait_recv()

    def on_position(f):
        for k in range(NZ):
            pl.when(z == k)(functools.partial(f, k))

    def line_sends(k, make, y_sems, l_sems, r_sems, slot, side, first=False):
        sends = [make(slot, y_sems, partner, dp, first)]
        if k > 0 and side != "L":
            sends.append(make(slot, l_sems, tp - 2, dp, first))
        if k < NZ - 1 and side != "R":
            sends.append(make(slot, r_sems, tp + 2, dp, first))
        return sends

    def b_own(slot, sems, to, to_dp, first=False):
        return b_copy(slot, dp, sems, to, to_dp, first)

    def a_sends(k, slot, side, first=False):
        return line_sends(k, a_copy, a_y, a_l, a_r, slot, side, first)

    def b_sends(k, slot, side, first=False):
        return line_sends(k, b_own, b_y, b_l, b_r, slot, side, first)

    def start(copies):
        for c in copies:
            c.start()

    load = pltpu.make_async_copy(e_ref, table, own_sem.at[2])
    load.start()
    group = [twin, facing, lax.rem(twin + 2, 4)]
    plane_barrier(tp, dp, [(tp, d) for d in group])
    peers = [lax.rem(tp + n, shards) for n in range(1, shards)]

    def rounds_copy(n):
        return remote(rounds_ref, rounds_all.at[dp], n_send.at[n], n_recv.at[dp], tp, group[n])

    for n in range(3):
        rounds_copy(n).start()
    rounds_all[dp] = rounds_ref[...]

    def row_copy(to):
        return remote(rows_ref.at[to], rows_in.at[tp], r_send.at[to], r_recv.at[tp], to, dp)

    on_position(lambda k: start(b_sends(k, tp, "", True)))
    on_position(lambda k: start(a_sends(k, tp, "", True)))
    own_w = pltpu.make_async_copy(w_ref, wl.at[tp], own_sem.at[1])
    own_w.start()

    def a_event(t, k):
        line, other = EVENTS[k][t]
        for side, zz in line:
            slot = 2 * zz + y
            a_wait(slot, core)
            start(a_sends(k, slot, side))
            a_copy(slot, a_c, tp, twin).start()
        for zz in other:
            slot = 2 * zz + 1 - y
            a_wait(slot, core)
            a_copy(slot, a_c, tp, twin).start()

    def b_event(t, k):
        line, other = EVENTS[k][t]
        for side, zz in line:
            slot = 2 * zz + y
            b_wait(slot, dp)
            start(b_sends(k, slot, side))
            b_copy(slot, dp, b_x, tp, facing).start()
            b_copy(slot, dp, b_c.at[0], tp, twin).start()
        for zz in other:
            slot = 2 * zz + 1 - y
            b_wait(slot, dp)
            b_copy(slot, dp, b_x, tp, facing).start()
            b_copy(slot, dp, b_c.at[0], tp, twin).start()

    load.wait()
    cap = rows_ref.shape[1]

    def pick_rows(n, carry):
        for i in range(8):
            rows_ref[n // (cap // 8), pl.ds(lax.rem(n, cap // 8) * 8 + i, 1), :] = table[pl.ds(ids_ref[n * 8 + i], 1), :]
        return carry

    lax.fori_loop(0, shards * cap // 8, pick_rows, 0)
    start([row_copy(to) for to in peers])
    own_rows = pltpu.make_async_copy(rows_ref.at[tp], rows_in.at[tp], own_sem.at[0])
    own_rows.start()
    on_position(functools.partial(b_event, 0))
    on_position(functools.partial(a_event, 0))
    on_position(functools.partial(b_event, 1))
    on_position(functools.partial(a_event, 1))
    own_rows.wait()
    for source in peers:
        remote(rows_ref.at[source], rows_in.at[source], r_send.at[source], r_recv.at[source], source, dp).wait_recv()
    n_slots = shards * cap
    x0_ref[...] = extra_ref[...] + mm(picks(code_ref[...], n_slots), rows_in[...].reshape(n_slots, width).astype(BF16), TA)
    u_b[...] = norm_fwd(x0_ref[...], ln_ref[0:1, :])[0]
    x1_ref[...] = x0_ref[...]
    cos_t = cos_ref[...]
    sin_t = sin_ref[...]
    kv = mm(wkv_ref[...], u_b[...], TB)
    lo, hi = turn(kv[:quarter], kv[quarter:hd], cos_t, sin_t)
    kv_out[0:quarter, :] = lo
    kv_out[quarter:hd, :] = hi
    kv_out[hd:, :] = kv[hd:]
    kv_copy = remote(kv_out, kv_in, kv_send, kv_recv, partner, dp)
    kv_copy.start()

    def slot_of(step):
        code = lookup(MLP_ORDER, z, step)
        other = code % 2
        return code // 2 * 2 + y + other - 2 * y * other

    def mlp(step, carry):
        def pass_on():
            slot = slot_of(step + 1)
            b_wait(slot, facing)
            b_copy(slot, facing, b_c.at[1], tp, twin).start()
        pl.when(step < shards - 1)(pass_on)
        slot = slot_of(step)

        def rest():
            b_wait(slot, twin)
            b_wait(slot, lax.rem(twin + 2, 4))
        pl.when(step > 0)(rest)
        at = pl.ds(pl.multiple_of(slot * n_f, n_f), n_f)
        wg_ref[at, :] = wl[slot, 2 * n_a:2 * n_a + n_f, :].astype(BF16)
        wu_ref[at, :] = wl[slot, 2 * n_a + n_f:2 * n_a + 2 * n_f, :].astype(BF16)
        wd_ref[at, :] = wl[slot, 2 * n_a + 2 * n_f:2 * n_a + 3 * n_f, :].astype(BF16)
        gate = mm(u_b[...], wg_ref[at, :], TB)
        up = mm(u_b[...], wu_ref[at, :], TB)
        x1_ref[...] += mm((gate * jax.nn.sigmoid(gate) * up).astype(BF16), wd_ref[at, :])
        return carry

    own_w.wait()
    lax.fori_loop(0, 3, mlp, 0)
    on_position(functools.partial(b_event, 2))
    on_position(functools.partial(a_event, 2))
    lax.fori_loop(3, 4, mlp, 0)
    on_position(functools.partial(a_event, 3))
    on_position(functools.partial(b_event, 3))
    for source in peers:
        a_wait(source, 1 - core)
    for s in range(shards):
        wq_ref[s * n_a:(s + 1) * n_a, :] = wl[s, 0:n_a, :].astype(BF16)
        wo_ref[s * n_a:(s + 1) * n_a, :] = wl[s, n_a:2 * n_a, :].astype(BF16)

    q_all = mm(wq_ref[...], u_b[...], TB)
    for h in range(heads):
        lo, hi = turn(q_all[h * hd:h * hd + quarter], q_all[h * hd + quarter:(h + 1) * hd], cos_t, sin_t)
        q_ref[h * hd:h * hd + quarter, :] = lo.astype(BF16)
        q_ref[h * hd + quarter:(h + 1) * hd, :] = hi.astype(BF16)
    kv_copy.wait()

    def fill(mine, other):
        kv_ref[mine * own:(mine + 1) * own, :] = kv_out[...].T.astype(BF16)
        kv_ref[other * own:(other + 1) * own, :] = kv_in[...].T.astype(BF16)
        kvt_ref[:, mine * own:(mine + 1) * own] = kv_out[...].astype(BF16)
        kvt_ref[:, other * own:(other + 1) * own] = kv_in[...].astype(BF16)

    pl.when(y == 0)(lambda: fill(0, 1))
    pl.when(y == 1)(lambda: fill(1, 0))
    blank = jnp.zeros((hd, own), BF16)
    slope = hd ** -0.5 * LOG2E

    def attend(h, carry):
        at = pl.ds(pl.multiple_of(h * hd, hd), hd)
        scores = mm(kv_ref[...], jnp.concatenate([q_ref[at, :], blank], axis=0))
        allowed = lax.broadcasted_iota(jnp.int32, scores.shape, 0) <= lax.broadcasted_iota(jnp.int32, scores.shape, 1) + y * own
        scores = jnp.where(allowed, scores * slope, -1e30)
        top = jnp.max(scores, axis=0, keepdims=True)
        prob = jnp.exp2(scores - top)
        total = jnp.sum(prob, axis=0, keepdims=True)
        lse_ref[pl.ds(h, 1), :] = top + jnp.log2(total)
        ctx_ref[at, :] = mm(kvt_ref[hd:, :], (prob * (1.0 / total)).astype(BF16)).astype(BF16)
        return carry

    lax.fori_loop(0, heads, attend, 0)
    x1_ref[...] += mm(ctx_ref[...], wo_ref[...], TA)

    lax.fori_loop(4, shards, mlp, 0)
    f_ref[...] = norm_fwd(x1_ref[...], ln_ref[1:2, :])[0].astype(F32)

    def finish(k):
        done = a_sends(k, tp, "", True) + b_sends(k, tp, "", True)
        for line, other in EVENTS[k]:
            for side, zz in line:
                done += a_sends(k, 2 * zz + y, side) + b_sends(k, 2 * zz + y, side)
        for c in done:
            c.wait_send()

    on_position(finish)
    for n in range(3):
        rounds_copy(n).wait_send()
        remote(rounds_ref, rounds_all.at[group[n]], n_send.at[n], n_recv.at[group[n]], tp, twin).wait_recv()
    for to in peers:
        row_copy(to).wait_send()
        a_copy(to, a_c, tp, twin).wait_send()
        b_copy(to, dp, b_x, tp, facing).wait_send()
        b_copy(to, dp, b_c.at[0], tp, twin).wait_send()
        b_copy(to, facing, b_c.at[1], tp, twin).wait_send()


def front(ids, embed, rounds, code, extra, w_rows, wkv_t, ln, cos_t, sin_t, n_q, collective_id):
    own, width = extra.shape
    two_hd = wkv_t.shape[0]
    shards = 2 * NZ
    ff = (w_rows.shape[0] * shards - 2 * n_q) // 3
    dma = lambda *n: pltpu.SemaphoreType.DMA(n)
    s = jax.ShapeDtypeStruct
    rows = (shards, ids.shape[0] // shards, width)
    return pl.pallas_call(
        front_kernel,
        out_shape=(s((own, width), F32),) * 3 + (s((n_q, own), BF16), s((2 * own, two_hd), BF16), s((two_hd, 2 * own), BF16),
                   s((2 * n_q // two_hd, own), F32), s((n_q, own), BF16), s((n_q, width), BF16), s((n_q, width), BF16))
        + (s((ff, width), BF16),) * 3 + (s((4, 1, 128), jnp.int32),),
        in_specs=[pl.BlockSpec(memory_space=pltpu.SMEM), ANY, VMEM, VMEM, VMEM, ANY] + [VMEM] * 4,
        out_specs=(VMEM,) * 14,
        scratch_shapes=[pltpu.VMEM(embed.shape, F32), pltpu.VMEM(rows, F32), pltpu.VMEM((shards,) + w_rows.shape, F32), pltpu.VMEM(rows, F32), pltpu.VMEM((own, width), BF16),
                        pltpu.VMEM((two_hd, own), F32), pltpu.VMEM((two_hd, own), F32),
                        dma(3), dma(shards), dma(shards)] + [dma(shards)] * 4 + [dma(shards, 2)]
        + [dma(shards)] * 4 + [dma(2, shards), dma(shards, 4), pltpu.SemaphoreType.DMA, pltpu.SemaphoreType.DMA, dma(3), dma(4)],
        compiler_params=pltpu.CompilerParams(collective_id=collective_id, has_side_effects=True, vmem_limit_bytes=60000000),
        name="front",
    )(ids, embed, rounds, code, extra, w_rows, wkv_t, ln, cos_t, sin_t)


def layer_bwd_kernel(dfin_ref, x0_ref, x1_ref, loss_ref, ln_ref, cos_ref, sin_ref, wq_ref, wkv_ref, wo_ref, wg_ref, wu_ref, wd_ref,
                     q_ref, kv_ref, kvt_ref, lse_ref, ctx_ref, code_ref, g_ref, ids_ref, rows_ref, d0_ref, back_ref, early_ref, ids_all, d_one, d_b, u_b, dctx, dq, dkv, dkv_in,
                     hid, d_gate, d_up, rows_out, g_q, g_o, g_g, g_u, g_d, small, s_early, c_early, out_sem, send_sem, recv_sem,
                     r_send, x_send, c_send, r_recv, g_load, g_send, g_recv, id_send, id_recv):
    tp, dp, z, y = place()
    partner = tp + 1 - 2 * y
    core = dp % 2
    twin = dp + 1 - 2 * core
    facing = lax.rem(dp + 2, 4)
    across = lax.rem(twin + 2, 4)
    own, width = x0_ref.shape
    hd = kv_ref.shape[1] // 2
    quarter = hd // 2
    nq = q_ref.shape[0]
    heads = nq // hd
    ff = wg_ref.shape[0]
    shards = rows_ref.shape[0]
    plane_barrier(tp, dp, [(tp, twin), (tp, facing), (tp, across)])

    n_early, g_size = s_early.shape[0], s_early.shape[1]

    def g_rows(which, b):
        return g_ref.at[pl.ds(pl.multiple_of(which * (g_ref.shape[0] // 2) + b * g_size, 8), g_size), :]

    def g_load_copy(b):
        return pltpu.make_async_copy(g_rows(core, b), s_early.at[b], g_load.at[b])

    def g_chip_copy(b):
        return remote(g_rows(1 - core, b), c_early.at[b], g_send.at[0, b], g_recv.at[0, b], tp, twin)

    def g_x_copy(b):
        return remote(s_early.at[b], early_ref.at[b], g_send.at[1, b], g_recv.at[1, b], tp, facing)

    for b in range(n_early):
        g_chip_copy(b).start()
        g_load_copy(b).start()

    def ids_copy(n, to):
        return remote(ids_ref, ids_all.at[dp], id_send.at[n], id_recv.at[dp], tp, to)

    for n, to in enumerate((twin, facing, across)):
        ids_copy(n, to).start()
    ids_all[dp] = ids_ref[...]
    _, f_hat, f_inv = norm_fwd(x1_ref[...], ln_ref[1:2, :])
    d_in, g_fin = norm_bwd(dfin_ref[...], f_hat, f_inv, ln_ref[1:2, :])
    d_one[...] = d_in
    d_b[...] = d_in.astype(BF16)
    u_b[...] = norm_fwd(x0_ref[...], ln_ref[0:1, :])[0]
    dctx[...] = mm(wo_ref[...], d_b[...], TB).astype(BF16)
    for b in range(n_early):
        g_load_copy(b).wait()
        g_chip_copy(b).wait_recv()
        add_into(s_early.at[b], c_early.at[b], 24)
        g_x_copy(b).start()
    cos_t = cos_ref[...]
    sin_t = sin_ref[...]
    blank = jnp.zeros((hd, own), BF16)
    slope = hd ** -0.5 * LOG2E
    dkv[...] = jnp.zeros_like(dkv)

    def attend(h, carry):
        at = pl.ds(pl.multiple_of(h * hd, hd), hd)
        q_pad = jnp.concatenate([q_ref[at, :], blank], axis=0)
        d_pad = jnp.concatenate([blank, dctx[at, :]], axis=0)
        scores = mm(kv_ref[...], q_pad)
        allowed = lax.broadcasted_iota(jnp.int32, scores.shape, 0) <= lax.broadcasted_iota(jnp.int32, scores.shape, 1) + y * own
        prob = jnp.where(allowed, jnp.exp2(scores * slope - lse_ref[pl.ds(h, 1), :]), 0.0)
        d_prob = mm(kv_ref[...], d_pad)
        mean = jnp.sum(d_prob * prob, axis=0, keepdims=True)
        d_score = (prob * (d_prob - mean) * hd ** -0.5).astype(BF16)
        dkv[...] += mm(d_score, q_pad, TB) + mm(prob.astype(BF16), d_pad, TB)
        d_q = mm(kvt_ref[0:hd, :], d_score)
        lo, hi = turn(d_q[:quarter], d_q[quarter:], cos_t, -sin_t)
        dq[at, :] = jnp.concatenate([lo, hi], axis=0).astype(BF16)
        return carry

    lax.fori_loop(0, heads, attend, 0)
    copy = remote(dkv.at[pl.ds(pl.multiple_of((1 - y) * own, own), own), :], dkv_in, send_sem, recv_sem, partner, dp)
    copy.start()

    d0_ref[...] = mm(dq[...], wq_ref[...], TA)
    step = min(512, ff)

    def mlp(n, carry):
        at = pl.ds(pl.multiple_of(n * step, step), step)
        gate = mm(wg_ref[at, :], u_b[...], TB)
        up = mm(wu_ref[at, :], u_b[...], TB)
        d_hidden = mm(wd_ref[at, :], d_b[...], TB)
        sig = jax.nn.sigmoid(gate)
        hid[at, :] = (gate * sig * up).astype(BF16)
        d_gate[at, :] = (d_hidden * up * sig * (1.0 + gate * (1.0 - sig))).astype(BF16)
        d_up[at, :] = (d_hidden * gate * sig).astype(BF16)
        d0_ref[...] += mm(d_gate[at, :], wg_ref[at, :], TA) + mm(d_up[at, :], wu_ref[at, :], TA)
        return carry

    lax.fori_loop(0, ff // step, mlp, 0)
    copy.wait()
    d_kv = (dkv[pl.ds(pl.multiple_of(y * own, own), own), :] + dkv_in[...]).T
    lo, hi = turn(d_kv[:quarter], d_kv[quarter:hd], cos_t, -sin_t)
    d_kv = jnp.concatenate([lo, hi, d_kv[hd:]], axis=0).astype(BF16)
    small[0:2 * hd, :] = mm(d_kv, u_b[...])
    d_u = d0_ref[...] + mm(d_kv, wkv_ref[...], TA)
    _, u_hat, u_inv = norm_fwd(x0_ref[...], ln_ref[0:1, :])
    d_in, g_in = norm_bwd(d_u, u_hat, u_inv, ln_ref[0:1, :])
    d_zero = d_one[...] + d_in
    d0_ref[...] = d_zero
    high = d_zero.astype(BF16)
    left = d_zero - high.astype(F32)
    middle = left.astype(BF16)
    low = (left - middle.astype(F32)).astype(BF16)
    pick = picks(code_ref[...], rows_out.shape[0] * rows_out.shape[1])
    rows_out[...] = (mm(pick, high) + mm(pick, middle) + mm(pick, low)).reshape(rows_out.shape)

    def row_copy(to):
        return remote(rows_out.at[to], back_ref.at[dp, tp], r_send.at[to], r_recv.at[dp, tp], to, dp)

    def x_copy(slot):
        return remote(back_ref.at[dp, slot], back_ref.at[dp, slot], x_send.at[slot], r_recv.at[dp, slot], tp, facing)

    def c_copy(group, n, slot):
        return remote(back_ref.at[group, slot], back_ref.at[group, slot], c_send.at[n, slot], r_recv.at[group, slot], tp, twin)

    def back(group, slot):
        remote(rows_out.at[slot], back_ref.at[group, slot], r_send.at[slot], r_recv.at[group, slot], tp, twin).wait_recv()

    def near_first(k):
        return sorted(((o, zz) for o in range(2) for zz in range(NZ)), key=lambda c: (abs(c[1] - k), c[0]))

    def slot_of(o, zz):
        return 2 * zz + (1 - y if o else y)

    def on_position(f):
        for k in range(NZ):
            pl.when(z == k)(functools.partial(f, k))

    def rows_leave(k):
        for c in near_first(k)[1:]:
            row_copy(slot_of(*c)).start()

    on_position(rows_leave)
    own_rows = pltpu.make_async_copy(rows_out.at[tp], back_ref.at[dp, tp], out_sem.at[7 * 2 * NZ])
    own_rows.start()
    own_rows.wait()
    x_copy(tp).start()
    c_copy(dp, 0, tp).start()

    g_o[...] = mm(ctx_ref[...], d_b[...])
    g_q[...] = mm(dq[...], u_b[...])

    def weight_grads(n, carry):
        at = pl.ds(pl.multiple_of(n * step, step), step)
        g_d[at, :] = mm(hid[at, :], d_b[...])
        g_g[at, :] = mm(d_gate[at, :], u_b[...])
        g_u[at, :] = mm(d_up[at, :], u_b[...])
        return carry

    lax.fori_loop(0, ff // step, weight_grads, 0)
    small[2 * hd:, :] = jnp.zeros_like(small[2 * hd:, :])
    small[2 * hd:2 * hd + 1, :] = g_in.reshape(1, width)
    small[2 * hd + 1:2 * hd + 2, :] = g_fin.reshape(1, width)
    small[2 * hd + 2:2 * hd + 3, :] = loss_ref[...]
    copies = []

    def put(src, first, size, s):
        copies.append(pltpu.make_async_copy(src, rows_ref.at[s, pl.ds(first, size), :], out_sem.at[len(copies)]))

    n_kv = 2 * hd // shards
    for s in range(shards):
        at = 0
        for g, size in ((g_q, nq // shards), (g_o, nq // shards), (g_g, ff // shards), (g_u, ff // shards), (g_d, ff // shards)):
            put(g.at[pl.ds(s * size, size), :], at, size, s)
            at += size
        put(small.at[pl.ds(s * n_kv, n_kv), :], at, n_kv, s)
        put(small.at[pl.ds(2 * hd + (0 if s == 0 else 16), 16), :], at + n_kv, 16, s)
    for c in copies:
        c.start()
    for c in copies:
        c.wait()

    def relay(k):
        order = near_first(k)
        for c in order[1:]:
            back(dp, slot_of(*c))
            x_copy(slot_of(*c)).start()
            c_copy(dp, 0, slot_of(*c)).start()
        for c in order:
            back(facing, slot_of(*c))
            c_copy(facing, 1, slot_of(*c)).start()

    on_position(relay)
    for b in range(n_early):
        g_x_copy(b).wait_recv()
        add_into(early_ref.at[b], s_early.at[b], 24)
    for slot in range(shards):
        back(twin, slot)
        back(across, slot)
    for n, to in enumerate((twin, facing, across)):
        remote(ids_ref, ids_all.at[to], id_send.at[n], id_recv.at[to], tp, to).wait_recv()
        ids_copy(n, to).wait_send()
    for n in range(1, shards):
        row_copy(lax.rem(tp + n, shards)).wait_send()
    for slot in range(shards):
        x_copy(slot).wait_send()
        c_copy(dp, 0, slot).wait_send()
        c_copy(facing, 1, slot).wait_send()
    for b in range(n_early):
        g_chip_copy(b).wait_send()
        g_x_copy(b).wait_send()


def layer_bwd(d_fin, x0, x1, loss_row, ln, cos_t, sin_t, weights, saved, code, g_table, ids, collective_id):
    own, width = x0.shape
    nq = weights[0].shape[0]
    two_hd = weights[1].shape[0]
    ff = weights[3].shape[0]
    rows = (2 * nq + 3 * ff + two_hd) // (2 * NZ) + 16
    chunk = (own, width)
    back = (2 * NZ, ids.shape[1] // (2 * NZ), width)
    blocks = (N_EARLY, table_block(g_table.shape[0]), width)
    dma = lambda *n: pltpu.SemaphoreType.DMA(n)
    return pl.pallas_call(
        layer_bwd_kernel,
        out_shape=(jax.ShapeDtypeStruct((2 * NZ, rows, width), F32), jax.ShapeDtypeStruct(chunk, F32), jax.ShapeDtypeStruct((4,) + back, F32),
                   jax.ShapeDtypeStruct(blocks, F32), jax.ShapeDtypeStruct((4,) + ids.shape, jnp.int32)),
        in_specs=[VMEM] * 19 + [ANY, VMEM],
        out_specs=(ANY, VMEM, ANY, VMEM, VMEM),
        scratch_shapes=[pltpu.VMEM(chunk, F32), pltpu.VMEM(chunk, BF16), pltpu.VMEM(chunk, BF16), pltpu.VMEM((nq, own), BF16),
                        pltpu.VMEM((nq, own), BF16), pltpu.VMEM((2 * own, two_hd), F32), pltpu.VMEM((own, two_hd), F32)]
        + [pltpu.VMEM((ff, own), BF16)] * 3 + [pltpu.VMEM(back, F32), pltpu.VMEM((nq, width), F32), pltpu.VMEM((nq, width), F32)] + [pltpu.VMEM((ff, width), F32)] * 3
        + [pltpu.VMEM((two_hd + 32, width), F32), pltpu.VMEM(blocks, F32), pltpu.VMEM(blocks, F32), dma(14 * NZ + 1),
           pltpu.SemaphoreType.DMA, pltpu.SemaphoreType.DMA, dma(2 * NZ), dma(2 * NZ), dma(2, 2 * NZ), dma(4, 2 * NZ),
           dma(N_EARLY), dma(2, N_EARLY), dma(2, N_EARLY), dma(3), dma(4)],
        compiler_params=pltpu.CompilerParams(collective_id=collective_id, has_side_effects=True, vmem_limit_bytes=66000000),
        name="layer_bwd",
    )(d_fin, x0, x1, loss_row, ln, cos_t, sin_t, *weights, *saved, code, g_table, ids)


N_BLOCK = 12
N_EARLY = 3
AHEAD = 11


def table_block(vocab):
    return -(-vocab // (2 * N_BLOCK * 24)) * 24


W_REDUCE = {
    0: {4: (3,), 6: (2,), 8: (1,), 9: (0,)},
    1: {6: (3,), 8: (2, 0), 9: (1,)},
    2: {6: (0,), 8: (1, 3), 9: (2,)},
    3: {4: (0,), 6: (1,), 8: (2,), 9: (3,)},
}


def tail_kernel(g_ref, p_ref, rows_ref, ids_ref, early_ref, t_ref, w_out, small_ref,
                s_buf, from_c, from_x, look_in, parts, acc, w_c, w_y, w_l, w_r, w_x,
                g_load, g_send_c, g_recv_c, g_send_x, g_recv_x, g_send_t, g_recv_t, g_store, l_sem,
                w_load, w_out_sem, send_c, send_y, send_l, send_r, recv_c, recv_y, recv_l, recv_r, last_send, last_recv, small_send, small_recv):
    tp, dp, z, y = place()
    partner = tp + 1 - 2 * y
    core = dp % 2
    twin = dp + 1 - 2 * core
    facing = lax.rem(dp + 2, 4)
    half = g_ref.shape[0] // 2
    size = s_buf.shape[1]
    last = half - (N_BLOCK - 1) * size
    n_look = rows_ref.shape[1]

    def rows(which, b, n):
        return pl.ds(pl.multiple_of(which * half + b * size, 8), n)

    def part(buf, b, n):
        return buf.at[b - N_EARLY if buf is not from_x else b, pl.ds(0, n), :]

    plane_barrier(tp, dp, [(tp, twin), (tp, facing)])

    chip = dp // 2
    groups = (2 * chip, 2 * chip + 1, 2 - 2 * chip, 3 - 2 * chip)

    def look_load(n):
        return pltpu.make_async_copy(rows_ref.at[groups[n]], look_in.at[n % 2], l_sem.at[n % 2])

    def early_load(b):
        return pltpu.make_async_copy(early_ref.at[b], from_x.at[b], g_load.at[b])

    for n in range(2):
        look_load(n).start()

    def c_copy(b, n):
        return remote(g_ref.at[rows(1 - core, b, n), :], part(from_c, b, n), g_send_c.at[b], g_recv_c.at[b], tp, twin)

    def own_load(b, n):
        return pltpu.make_async_copy(g_ref.at[rows(core, b, n), :], part(s_buf, b, n), g_load.at[b])

    def x_copy(b, n):
        return remote(part(s_buf, b, n), part(from_x, b, n), g_send_x.at[b], g_recv_x.at[b], tp, facing)

    def t_copy(b, n):
        return remote(part(from_x, b, n), t_ref.at[rows(core, b, n), :], g_send_t.at[b], g_recv_t.at[b], tp, twin)

    def t_store(b, n):
        return pltpu.make_async_copy(part(from_x, b, n), t_ref.at[rows(core, b, n), :], g_store.at[b])

    def every(f, first, end):
        def body(b, carry):
            f(b, size)
            return carry
        lax.fori_loop(first, min(end, N_BLOCK - 1), body, 0)
        if end == N_BLOCK:
            f(N_BLOCK - 1, last)

    def looked_up(b, n, first, count):
        ids = jnp.concatenate([ids_ref[first + g] for g in range(count)], axis=1) - (core * half + b * size)
        hit = (lax.broadcasted_iota(jnp.int32, (n, count * n_look), 0) == ids).astype(F32).astype(BF16)
        span = pl.ds(pl.multiple_of(first * n_look, n_look), count * n_look)
        return mm(hit, parts[0, span, :]) + mm(hit, parts[1, span, :]) + mm(hit, parts[2, span, :])

    def chip_sum(b, n):
        own_load(b, n).wait()
        c_copy(b, n).wait_recv()
        at = b - N_EARLY
        s_buf[at, 0:n, :] = s_buf[at, 0:n, :] + from_c[at, 0:n, :] + looked_up(b, n, 2 * chip, 2)
        x_copy(b, n).start()

    def early_sum(b, n):
        early_load(b).wait()
        from_x[b] = from_x[b] + looked_up(b, n, 0, 4)
        t_copy(b, n).start()
        t_store(b, n).start()

    def w_first(k):
        for zz in REDUCE_ORDER[k]:
            for slot in (2 * zz + 1 - y, 2 * zz + y):
                remote(p_ref.at[slot, 1 - core], w_c.at[slot], send_c.at[slot], recv_c.at[slot], tp, twin).start()
                pltpu.make_async_copy(p_ref.at[slot, core], acc.at[slot], w_load.at[slot]).start()

    def w_chip_sum(slot):
        pltpu.make_async_copy(p_ref.at[slot, core], acc.at[slot], w_load.at[slot]).wait()
        remote(acc.at[slot], w_c.at[slot], send_c.at[slot], recv_c.at[slot], tp, twin).wait_recv()
        add_into(acc.at[slot], w_c.at[slot])

    def w_second(k):
        for zz in REDUCE_ORDER[k]:
            slot = 2 * zz + 1 - y
            w_chip_sum(slot)
            remote(acc.at[slot], w_y.at[zz], send_y.at[zz], recv_y.at[zz], partner, dp).start()
        for zz in REDUCE_ORDER[k]:
            w_chip_sum(2 * zz + y)

    def w_reduce(k, shards):
        for zz in shards:
            line = acc.at[2 * zz + y]
            remote(line, w_y.at[zz], send_y.at[zz], recv_y.at[zz], partner, dp).wait_recv()
            add_into(line, w_y.at[zz])
            if zz >= k and k > 0:
                remote(line, w_l.at[zz - 1], send_l.at[zz], recv_l.at[zz], partner, dp).wait_recv()
                add_into(line, w_l.at[zz - 1])
            if zz <= k and k < NZ - 1:
                remote(line, w_r.at[zz], send_r.at[zz], recv_r.at[zz], partner, dp).wait_recv()
                add_into(line, w_r.at[zz])
            if zz > k:
                remote(line, w_l.at[zz - 1], send_r.at[zz], recv_l.at[zz], tp + 2, dp).start()
            if zz < k:
                remote(line, w_r.at[zz], send_l.at[zz], recv_r.at[zz], tp - 2, dp).start()

    def on_position(f):
        for k in range(NZ):
            pl.when(z == k)(functools.partial(f, k))

    def first(b, n):
        c_copy(b, n).start()
        own_load(b, n).start()

    every(first, N_EARLY, N_EARLY + 2)
    on_position(w_first)
    every(first, N_EARLY + 2, N_BLOCK)
    for b in range(N_EARLY):
        early_load(b).start()

    def split(n):
        look_load(n).wait()
        value = look_in[n % 2]
        high = value.astype(BF16)
        left = value - high.astype(F32)
        middle = left.astype(BF16)
        at = pl.ds(pl.multiple_of(groups[n] * n_look, n_look), n_look)
        parts[0, at, :] = high
        parts[1, at, :] = middle
        parts[2, at, :] = (left - middle.astype(F32)).astype(BF16)
        if n + 2 < 4:
            look_load(n + 2).start()

    split(0)
    split(1)
    every(chip_sum, N_EARLY, N_EARLY + 3)
    on_position(w_second)
    every(chip_sum, N_EARLY + 3, AHEAD)
    split(2)
    split(3)
    every(early_sum, 0, N_EARLY)

    total = acc.at[tp]
    w_copy_x = remote(total, w_x, last_send.at[0], last_recv.at[0], tp, facing)
    w_copy_c = remote(total, w_out.at[core], last_send.at[1], last_recv.at[1], tp, twin)
    w_store = pltpu.make_async_copy(total, w_out.at[core], w_out_sem)
    n_small, n_rows = small_ref.shape[1], w_out.shape[1]
    mine = w_out.at[1, pl.ds(n_rows - 32, n_small), :]
    small_here = pltpu.make_async_copy(mine, small_ref.at[tp], w_out_sem)
    peers = [lax.rem(tp + n, 2 * NZ) for n in range(1, 2 * NZ)]
    for b in range(N_EARLY, N_BLOCK):
        n = last if b == N_BLOCK - 1 else size
        x_copy(b, n).wait_recv()
        add_into(part(from_x, b, n), part(s_buf, b, n), 24)
        t_copy(b, n).start()
        t_store(b, n).start()
        for k in range(NZ):
            if b in W_REDUCE[k]:
                pl.when(z == k)(functools.partial(w_reduce, k, W_REDUCE[k][b]))
        if b == 9:
            w_copy_x.start()
            every(chip_sum, AHEAD, N_BLOCK)
        if b == 10:
            w_copy_x.wait()
            add_into(total, w_x)
            w_copy_c.start()
            w_store.start()
            w_copy_c.wait_send()
            remote(total, w_out.at[1 - core], last_send.at[1], last_recv.at[1], tp, twin).wait_recv()
            w_store.wait()
            for to in peers:
                remote(mine, small_ref.at[tp], small_send.at[to], small_recv.at[tp], to, dp).start()
            small_here.start()
    for source in peers:
        remote(small_ref.at[source], small_ref.at[source], small_send.at[source], small_recv.at[source], source, dp).wait_recv()
        remote(mine, small_ref.at[tp], small_send.at[source], small_recv.at[tp], source, dp).wait_send()
    small_here.wait()

    def w_done(k):
        for zz in range(NZ):
            line = acc.at[2 * zz + y]
            for slot in (2 * zz + 1 - y, 2 * zz + y):
                remote(p_ref.at[slot, 1 - core], w_c.at[slot], send_c.at[slot], recv_c.at[slot], tp, twin).wait_send()
            remote(line, w_y.at[zz], send_y.at[zz], recv_y.at[zz], partner, dp).wait_send()
            if zz > k:
                remote(line, w_l.at[zz - 1], send_r.at[zz], recv_l.at[zz], tp + 2, dp).wait_send()
            if zz < k:
                remote(line, w_r.at[zz], send_l.at[zz], recv_r.at[zz], tp - 2, dp).wait_send()

    on_position(w_done)

    def drain(b, n):
        t_copy(b, n).wait_send()
        t_store(b, n).wait()
        remote(part(from_x, b, n), t_ref.at[rows(1 - core, b, n), :], g_send_t.at[b], g_recv_t.at[b], tp, twin).wait_recv()

    def sent(b, n):
        c_copy(b, n).wait_send()
        x_copy(b, n).wait_send()

    every(drain, 0, N_BLOCK)
    every(sent, N_EARLY, N_BLOCK)


def tail(g_table, g_rows, look_rows, look_ids, early, collective_id):
    vocab, width = g_table.shape
    rows = g_rows.shape[1]
    half = (rows // 2, width)
    n_look = look_ids.shape[2]
    size = table_block(vocab)
    blocks = lambda n: pltpu.VMEM((n, size, width), F32)
    dma = lambda *n: pltpu.SemaphoreType.DMA(n)
    t, w_sum, small = pl.pallas_call(
        tail_kernel,
        out_shape=(jax.ShapeDtypeStruct((vocab, width), F32), jax.ShapeDtypeStruct((2,) + half, F32), jax.ShapeDtypeStruct((2 * NZ, 24, width), F32)),
        in_specs=[ANY, ANY, ANY, VMEM, ANY],
        out_specs=(ANY,) * 3,
        scratch_shapes=[blocks(N_BLOCK - N_EARLY)] * 2 + [blocks(N_BLOCK), pltpu.VMEM((2, n_look, width), F32), pltpu.VMEM((3, 4 * n_look, width), BF16)]
        + [pltpu.VMEM((2 * NZ,) + half, F32)] * 2 + [pltpu.VMEM((NZ,) + half, F32)] + [pltpu.VMEM((NZ - 1,) + half, F32)] * 2
        + [pltpu.VMEM(half, F32)]
        + [dma(N_BLOCK)] * 8 + [dma(2)]
        + [dma(2 * NZ), pltpu.SemaphoreType.DMA] + [dma(2 * NZ), dma(NZ), dma(NZ), dma(NZ)] * 2 + [dma(2)] * 2 + [dma(2 * NZ)] * 2,
        compiler_params=pltpu.CompilerParams(collective_id=collective_id, has_side_effects=True, vmem_limit_bytes=67000000),
        name="tail",
    )(g_table, g_rows.reshape((2 * NZ, 2) + half), look_rows.reshape(4, n_look, width), look_ids, early)
    return t, w_sum.reshape(rows, width), small


UPDATE_ROWS = 512


def update_kernel(t_ref, w_any, small_any, *refs):
    state = [refs[7 * i:7 * i + 7] for i in range(3)]
    new = [refs[21 + 7 * i:28 + 7 * i] for i in range(3)]
    loss_ref, held, made, w_ref, small_ref = refs[42:47]
    old_small = [refs[47 + 6 * i:53 + 6 * i] for i in range(3)]
    new_small = [refs[65 + 6 * i:71 + 6 * i] for i in range(3)]
    in_sem, out_sem, g_sem, small_in, small_out = refs[83:]
    vocab = t_ref.shape[0]
    blocks = [(at, min(UPDATE_ROWS, vocab - at)) for at in range(0, vocab, UPDATE_ROWS)]

    def loads(q):
        at, n = blocks[q]
        return [pltpu.make_async_copy(ref.at[pl.ds(at, n), :], held.at[q % 3, i, pl.ds(0, n), :], in_sem.at[q % 3, i])
                for i, ref in enumerate((t_ref, state[0][0], state[1][0], state[2][0]))]

    def stores(q):
        at, n = blocks[q]
        return [pltpu.make_async_copy(made.at[q % 2, i, pl.ds(0, n), :], new[i][0].at[pl.ds(at, n), :], out_sem.at[q % 2, i]) for i in range(3)]

    for q in range(3):
        for c in loads(q):
            c.start()
    grads = [pltpu.make_async_copy(w_any, w_ref, g_sem.at[0]), pltpu.make_async_copy(small_any, small_ref, g_sem.at[1])]
    pairs = [(i, j) for i in range(3) for j in range(6)]
    small_loads = grads + [pltpu.make_async_copy(state[i][j + 1], old_small[i][j], small_in.at[i, j]) for i, j in pairs]
    small_stores = [pltpu.make_async_copy(new_small[i][j], new[i][j + 1], small_out.at[i, j]) for i, j in pairs]
    for c in small_loads:
        c.start()

    def small_update(index, grad, *where):
        got = adam_update(old_small[0][index - 1][where], grad, old_small[1][index - 1][where], old_small[2][index - 1][where])
        for i in range(3):
            new_small[i][index - 1][where] = got[i]

    def small_updates():
        hd = old_small[0][2].shape[1]
        n_kv = 2 * hd // small_ref.shape[0]
        n_q, n_f = old_small[0][1].shape[0], old_small[0][5].shape[0]
        small_update(1, small_ref[0, n_kv:n_kv + 2, :], Ellipsis)
        small_update(2, w_ref[0:n_q, :], Ellipsis)
        kv = small_ref[:, 0:n_kv, :].reshape(2 * hd, small_ref.shape[2])
        for i in range(2):
            small_update(3, kv[i * hd:(i + 1) * hd], i)
        small_update(4, w_ref[n_q:2 * n_q, :], Ellipsis)
        for i in range(2):
            small_update(5, w_ref[2 * n_q + i * n_f:2 * n_q + (i + 1) * n_f, :].T, i)
        small_update(6, w_ref[2 * n_q + 2 * n_f:2 * n_q + 3 * n_f, :], Ellipsis)
        loss_ref[...] = jnp.sum(small_ref[0, n_kv + 2:n_kv + 3, :], axis=1, keepdims=True)

    for q, (at, n) in enumerate(blocks):
        for c in loads(q):
            c.wait()
        if q >= 2:
            for c in stores(q - 2):
                c.wait()
        step = 32 if n % 32 == 0 else 16

        def body(j, carry):
            rows = pl.ds(pl.multiple_of(j * step, step), step)
            got = adam_update(held[q % 3, 1, rows, :], held[q % 3, 0, rows, :], held[q % 3, 2, rows, :], held[q % 3, 3, rows, :])
            for i in range(3):
                made[q % 2, i, rows, :] = got[i]
            return carry

        lax.fori_loop(0, n // step, body, 0)
        for c in stores(q):
            c.start()
        if q + 3 < len(blocks):
            for c in loads(q + 3):
                c.start()
        if q == min(3, len(blocks) - 1):
            for c in small_loads:
                c.wait()
            small_updates()
            for c in small_stores:
                c.start()
    for q in range(len(blocks) - 2, len(blocks)):
        for c in stores(q):
            c.wait()
    for c in small_stores:
        c.wait()


def update(g_table, g_shard, g_small, state_arrays):
    width = g_table.shape[1]
    dma = lambda *n: pltpu.SemaphoreType.DMA(n)

    def flip(arrays):
        return [a.swapaxes(-1, -2) if i % 7 in (2, 3) else a for i, a in enumerate(arrays)]

    given = flip(state_arrays)
    small = [pltpu.VMEM(a.shape, F32) for i, a in enumerate(given) if i % 7]
    *new, loss = pl.pallas_call(
        update_kernel,
        out_shape=tuple(jax.ShapeDtypeStruct(a.shape, F32) for a in given) + (jax.ShapeDtypeStruct((1, 1), F32),),
        in_specs=[ANY] * 24,
        out_specs=(ANY,) * 21 + (VMEM,),
        scratch_shapes=[pltpu.VMEM((3, 4, UPDATE_ROWS, width), F32), pltpu.VMEM((2, 3, UPDATE_ROWS, width), F32),
                        pltpu.VMEM(g_shard.shape, F32), pltpu.VMEM(g_small.shape, F32)] + small * 2
        + [dma(3, 4), dma(2, 3), dma(2), dma(3, 6), dma(3, 6)],
        compiler_params=pltpu.CompilerParams(vmem_limit_bytes=60000000),
        name="update",
    )(g_table, g_shard, g_small, *given)
    return flip(new) + [loss]


def norm_fwd(x_f32, scale):
    centered = x_f32 - jnp.mean(x_f32, axis=-1, keepdims=True)
    inv_std = lax.rsqrt(jnp.mean(centered * centered, axis=-1, keepdims=True) + LN_EPS)
    x_hat = centered * inv_std
    return (x_hat * scale).astype(BF16), x_hat, inv_std


def norm_bwd(d_out, x_hat, inv_std, scale):
    d_scale = jnp.sum(d_out * x_hat, axis=0)
    d_hat = d_out * scale
    d_in = inv_std * (d_hat - jnp.mean(d_hat, axis=-1, keepdims=True) - x_hat * jnp.mean(d_hat * x_hat, axis=-1, keepdims=True))
    return d_in, d_scale


def adam_update(param_in, grad_in, mom_in, vel_in):
    mom_new = BETA_ONE * mom_in + (1.0 - BETA_ONE) * grad_in
    vel_new = BETA_TWO * vel_in + (1.0 - BETA_TWO) * grad_in * grad_in
    return param_in - LEARN_RATE * mom_new / (jnp.sqrt(vel_new) + ADAM_EPS), mom_new, vel_new


def dot(spec, a, b):
    return jnp.einsum(spec, a, b, preferred_element_type=F32)


def solution(mesh):
    param_specs = (P('tp', None), P(None, None), P(None, 'tp'), P(None, None, None), P('tp', None), P(None, None, 'tp'), P('tp', None))
    n_tp = mesh.shape['tp']
    n_dp = mesh.shape['dp']

    def local_step(tokens, labels, *state_arrays):
        embed, ln_scales, w_q, w_kv, w_o, w_gu, w_down = state_arrays[0:7]
        batch_loc, seq_len = tokens.shape
        vocab_loc, d_model = embed.shape
        head_dim = w_kv.shape[2]
        q_loc = w_q.shape[1]
        f_loc = w_down.shape[0]
        tok_loc = batch_loc * seq_len
        tok_total = tok_loc * n_dp
        own = tok_loc // n_tp
        tp_rank = lax.axis_index('tp')
        half = tp_rank % 2

        strict = (jnp.arange(own)[:, None] > jnp.arange(own)[None, :]).astype(BF16)

        def routing(chunks):
            shard = chunks // vocab_loc
            row = chunks - shard * vocab_loc
            hot = (shard[:, :, None] == jnp.arange(n_tp)[None, None, :])
            before = dot('rs,nsj->nrj', strict, hot.astype(BF16))
            rank = jnp.sum(jnp.where(hot, before, 0.0), axis=-1).astype(jnp.int32)
            most = jnp.max(jnp.sum(hot.astype(jnp.int32), axis=1))
            return shard, row, rank, (most + CAP - 1) // CAP

        chunks = tokens.reshape(n_tp, own)
        shard, row, rank, rounds = routing(chunks)
        slots = jnp.arange(CAP)
        my_shard = lax.dynamic_index_in_dim(shard, tp_rank, 0, keepdims=False)
        my_rank = lax.dynamic_index_in_dim(rank, tp_rank, 0, keepdims=False)

        def fetch(step):
            here = (shard[:, None, :] == tp_rank) & (rank[:, None, :] == slots[None, :, None] + step * CAP)
            ids = jnp.sum(jnp.where(here, row[:, None, :], 0), axis=-1).reshape(-1)
            place = my_rank - step * CAP
            return ids, jnp.where((place >= 0) & (place < CAP), my_shard * CAP + place, -1)

        def fetch_more(state):
            ids, code = fetch(state[0])
            pick = (code[:, None] == jnp.arange(n_tp * CAP)[None, :]).astype(BF16)
            rows_in = plane_swap(jnp.take(embed, ids, axis=0).reshape(n_tp, CAP, d_model), 1).reshape(n_tp * CAP, d_model).astype(BF16)
            return state[0] + 1, state[1] + dot('rc,cd->rd', pick, rows_in)

        more_rows = lax.while_loop(lambda state: state[0] < rounds, fetch_more, (jnp.int32(1), jnp.zeros((own, d_model), F32)))[1]
        ids_first, code_first = fetch(0)
        code_first = code_first[None, :]

        w_rows = jnp.concatenate([w_q.T, w_o, w_gu.transpose(0, 2, 1).reshape(2 * f_loc, d_model), w_down], axis=0)
        cuts = (q_loc, 2 * q_loc, 2 * q_loc + f_loc, 2 * q_loc + 2 * f_loc)
        wkv_t = w_kv.transpose(0, 2, 1).reshape(2 * head_dim, d_model).astype(BF16)
        inv_freq = ROPE_BASE ** (-jnp.arange(0, head_dim, 2).astype(F32) / head_dim)
        angles = inv_freq[:, None] * (half * own + jnp.arange(own)).astype(F32)[None, :]
        cos_t, sin_t = jnp.cos(angles), jnp.sin(angles)
        f_own, x_one, x_zero, *saved = front(ids_first, embed, jnp.broadcast_to(rounds, (1, 128)), code_first, more_rows, w_rows, wkv_t, ln_scales, cos_t, sin_t, n_tp * q_loc, 0)
        saved, (wq_t, wo_b, wg_t, wu_t, wd_b), rounds_all = saved[:5], saved[5:10], jnp.max(saved[10])
        weights = (wq_t, wkv_t, wo_b, wg_t, wu_t, wd_b)

        logit_scale = d_model ** -0.5
        d_fin, g_head_part, log_norm, lab_sum, _ = head(f_own, labels.reshape(n_tp, own), embed, logit_scale, logit_scale / tok_total, 4)
        log_norm = lax.dynamic_index_in_dim(log_norm, tp_rank, 0, keepdims=False)
        loss_row = (log_norm + LOGIT_ZLOSS * log_norm * log_norm - jnp.sum(lab_sum, axis=0) * logit_scale) / tok_total
        def row_ids(step):
            here = (shard[:, None, :] == tp_rank) & (rank[:, None, :] == slots[None, :, None] + step * CAP)
            return jnp.where(jnp.any(here, axis=-1), jnp.sum(jnp.where(here, row[:, None, :], 0), axis=-1), vocab_loc).reshape(-1)

        g_rows, d_zero, rows_back, early, ids_back = layer_bwd(d_fin, x_zero, x_one, loss_row[None, :], ln_scales, cos_t, sin_t, weights, saved,
                                                               code_first, g_head_part, row_ids(0)[None, :], 7)
        g_table, g_shard, g_small = tail(g_head_part, g_rows, rows_back, ids_back, early, 10)

        def give_back(state):
            mine = (my_shard[None, None, :] == jnp.arange(n_tp)[:, None, None]) & (my_rank[None, None, :] == slots[None, :, None] + state[0] * CAP)
            ids = jnp.sum(jnp.where(mine, jnp.arange(own)[None, None, :], 0), axis=-1).reshape(-1)
            rows_in = plane_swap(jnp.take(d_zero, ids, axis=0).reshape(n_tp, CAP, d_model), 9).reshape(-1, d_model)
            n_rows = n_tp * CAP
            id_rows = jnp.pad(row_ids(state[0]).astype(F32), (0, -n_rows % (8 * d_model))).reshape(-1, d_model)
            both = group_gather(jnp.concatenate([rows_in, id_rows], axis=0), 11)
            ids = both[:, n_rows:].reshape(n_dp, -1)[:, :n_rows].astype(jnp.int32)
            return state[0] + 1, state[1].at[ids.reshape(-1)].add(both[:, :n_rows].reshape(-1, d_model), mode='drop')

        g_table = lax.while_loop(lambda state: state[0] < rounds_all, give_back, (jnp.int32(1), g_table))[1]
        *new, loss = update(g_table, g_shard, g_small, state_arrays)
        return tuple(new) + (loss.reshape(()),)

    return jax.shard_map(local_step, mesh=mesh, in_specs=(P('dp', None), P('dp', None)) + param_specs * 3,
                         out_specs=param_specs * 3 + (P(),), check_vma=False)
```

```python
import functools

import jax
import jax.numpy as jnp
from jax import lax
from jax.experimental import pallas as pl
from jax.experimental.pallas import tpu as pltpu
from jax.sharding import PartitionSpec as P

LN_EPS = 1e-5
LOGIT_ZLOSS = 1e-4
LEARN_RATE = 1e-2
BETA_ONE = 0.9
BETA_TWO = 0.95
ADAM_EPS = 1e-8
ROPE_BASE = 10000.0
NZ = 4
CAP = 96
F32 = jnp.float32
BF16 = jnp.bfloat16
ANY = pl.BlockSpec(memory_space=pl.ANY)
VMEM = pl.BlockSpec(memory_space=pltpu.VMEM)

ARRIVALS = {
    0: (("R", 1), ("R", 2), ("R", 3)),
    1: (("L", 0), ("R", 2), ("R", 3)),
    2: (("R", 3), ("L", 1), ("L", 0)),
    3: (("L", 2), ("L", 1), ("L", 0)),
}
REDUCE_ORDER = {0: (3, 2, 1, 0), 1: (3, 0, 2, 1), 2: (0, 3, 1, 2), 3: (0, 1, 2, 3)}


def remote(src, dst, send_sem, recv_sem, tp, dp):
    return pltpu.make_async_remote_copy(src_ref=src, dst_ref=dst, send_sem=send_sem, recv_sem=recv_sem,
                                        device_id=(tp, dp), device_id_type=pl.DeviceIdType.MESH)


def place():
    tp = lax.axis_index("tp")
    dp = lax.axis_index("dp")
    return tp, dp, tp // 2, tp % 2


def signal(tp, dp):
    pl.semaphore_signal(pltpu.get_barrier_semaphore(), inc=1, device_id=(tp, dp), device_id_type=pl.DeviceIdType.MESH)


def add_into(acc, other, step=None):
    rows = acc.shape[0]
    step = step or (64 if rows % 64 == 0 else 8)

    def body(n, carry):
        at = pl.ds(pl.multiple_of(n * step, step), step)
        acc[at, :] = acc[at, :] + other[at, :]
        return carry

    lax.fori_loop(0, rows // step, body, 0)


def plane_barrier(tp, dp, others):
    peers = [(lax.rem(tp + n, 2 * NZ), dp) for n in range(1, 2 * NZ)] + others
    for peer in peers:
        signal(*peer)
    pl.semaphore_wait(pltpu.get_barrier_semaphore(), len(peers))


def swap_kernel(x_ref, out_ref, own_sem, send, recv):
    tp, dp, _, _ = place()
    plane_barrier(tp, dp, [])
    copies = []
    for n in range(1, 2 * NZ):
        to = lax.rem(tp + n, 2 * NZ)
        copy = remote(x_ref.at[to], out_ref.at[tp], send.at[to], recv.at[tp], to, dp)
        copy.start()
        copies.append(copy)
    own = pltpu.make_async_copy(x_ref.at[tp], out_ref.at[tp], own_sem)
    own.start()
    for n in range(1, 2 * NZ):
        source = lax.rem(tp + n, 2 * NZ)
        remote(out_ref.at[source], out_ref.at[source], send.at[source], recv.at[source], source, dp).wait_recv()
    own.wait()
    for copy in copies:
        copy.wait_send()


def plane_swap(x, collective_id):
    return pl.pallas_call(
        swap_kernel,
        out_shape=jax.ShapeDtypeStruct(x.shape, x.dtype),
        in_specs=[ANY],
        out_specs=ANY,
        scratch_shapes=[pltpu.SemaphoreType.DMA] + [pltpu.SemaphoreType.DMA((2 * NZ,))] * 2,
        compiler_params=pltpu.CompilerParams(collective_id=collective_id, has_side_effects=True),
        name="plane_swap",
    )(x)


def group_kernel(x_ref, out_ref, own_sem, send, recv):
    tp, dp, _, _ = place()
    group = [lax.rem(dp + n, 4) for n in range(1, 4)]
    for to in group:
        signal(tp, to)
    pl.semaphore_wait(pltpu.get_barrier_semaphore(), 3)
    own = pltpu.make_async_copy(x_ref, out_ref.at[dp], own_sem)
    own.start()
    for n, to in enumerate(group):
        remote(x_ref, out_ref.at[dp], send.at[n], recv.at[dp], tp, to).start()
    own.wait()
    for n, to in enumerate(group):
        remote(x_ref, out_ref.at[to], send.at[n], recv.at[to], tp, to).wait_recv()
        remote(x_ref, out_ref.at[dp], send.at[n], recv.at[dp], tp, to).wait_send()


def group_gather(x, collective_id):
    return pl.pallas_call(
        group_kernel,
        out_shape=jax.ShapeDtypeStruct((4,) + x.shape, x.dtype),
        in_specs=[ANY],
        out_specs=ANY,
        scratch_shapes=[pltpu.SemaphoreType.DMA, pltpu.SemaphoreType.DMA((3,)), pltpu.SemaphoreType.DMA((4,))],
        compiler_params=pltpu.CompilerParams(collective_id=collective_id, has_side_effects=True),
        name="group_gather",
    )(x)


GATHER_ORDER = {
    0: ((0, 0), (0, 1), (1, 0), (0, 2), (1, 1), (0, 3), (1, 2), (1, 3)),
    1: ((0, 1), (0, 0), (0, 2), (1, 1), (1, 0), (0, 3), (1, 2), (1, 3)),
    2: ((0, 2), (0, 1), (0, 3), (1, 2), (0, 0), (1, 3), (1, 1), (1, 0)),
    3: ((0, 3), (0, 2), (1, 3), (0, 1), (1, 2), (0, 0), (1, 1), (1, 0)),
}
GATHER_EVENTS = {
    0: {
        1: ((0, 1, 0, 'y'), (1, 0, 1, 'r'), (0, 1, 1, 'y'), (1, 0, 0, '')),
        3: ((0, 2, 0, 'y'), (1, 1, 0, ''), (0, 2, 1, 'y'), (1, 1, 1, '')),
        5: ((0, 3, 0, 'y'), (1, 2, 0, ''), (0, 3, 1, ''), (1, 2, 1, '')),
        7: ((1, 3, 0, ''), (1, 3, 1, '')),
    },
    1: {
        1: ((0, 0, 0, 'ry'), (0, 2, 0, 'ly'), (1, 1, 0, ''), (0, 0, 1, 'r'), (0, 2, 1, 'ly'), (1, 1, 1, '')),
        4: ((0, 3, 0, 'ly'), (1, 0, 0, ''), (1, 0, 1, 'r')),
        5: ((0, 3, 1, 'l'), (1, 2, 0, '')),
        6: ((1, 2, 1, ''), (1, 3, 1, 'l')),
        7: ((1, 3, 0, ''),),
    },
    2: {
        1: ((0, 1, 0, 'ry'), (0, 3, 0, 'ly'), (1, 2, 0, ''), (0, 1, 1, 'ry'), (0, 3, 1, 'l'), (1, 2, 1, '')),
        4: ((0, 0, 0, 'ry'), (1, 1, 0, ''), (1, 3, 1, 'l'), (0, 0, 1, 'r'), (1, 3, 0, '')),
        6: ((1, 0, 1, 'r'), (1, 1, 1, '')),
        7: ((1, 0, 0, ''),),
    },
    3: {
        1: ((0, 2, 0, 'y'), (1, 3, 1, 'l'), (0, 2, 1, 'y'), (1, 3, 0, '')),
        3: ((0, 1, 0, 'y'), (1, 2, 0, ''), (0, 1, 1, 'y'), (1, 2, 1, '')),
        5: ((0, 0, 0, 'y'), (1, 1, 0, ''), (0, 0, 1, ''), (1, 1, 1, '')),
        7: ((1, 0, 0, ''), (1, 0, 1, '')),
    },
}
SCATTER_ORDER = {
    0: ((1, 3), (1, 2), (0, 3), (1, 1), (0, 2), (1, 0), (0, 1), (0, 0)),
    1: ((1, 3), (1, 2), (0, 3), (1, 0), (1, 1), (0, 2), (0, 0), (0, 1)),
    2: ((1, 0), (1, 1), (1, 3), (0, 0), (1, 2), (0, 3), (0, 1), (0, 2)),
    3: ((1, 0), (1, 1), (0, 0), (1, 2), (0, 1), (1, 3), (0, 2), (0, 3)),
}
SCATTER_EVENTS = {
    0: {
        0: ((1, 3, 0, '', 'y'), (1, 3, 1, '', 'r')),
        1: ((1, 2, 0, '', 'y'), (1, 2, 1, '', 'y')),
        2: ((0, 3, 1, '', 'r'), (0, 3, 0, 'y', 'r')),
        3: ((1, 1, 0, '', 'y'), (1, 1, 1, '', 'y')),
        4: ((0, 2, 0, 'y', 'r'),),
        5: ((0, 2, 1, 'y', 'r'), (1, 0, 0, '', 'y')),
        6: ((1, 0, 1, 'r', 'y'), (0, 1, 0, 'y', 'r')),
        7: ((0, 1, 1, 'y', 'r'), (0, 0, 0, 'ry', ''), (0, 0, 1, 'ry', '')),
    },
    1: {
        0: ((1, 3, 0, '', 'y'),),
        1: ((1, 2, 0, '', 'y'), (1, 2, 1, '', 'y')),
        2: ((1, 3, 1, 'l', 'r'),),
        3: ((1, 0, 0, '', 'y'),),
        4: ((0, 3, 1, 'l', 'r'), (1, 0, 1, 'r', 'l'), (1, 1, 0, '', 'y'), (1, 1, 1, '', 'y')),
        6: ((0, 3, 0, 'ly', 'r'), (0, 0, 1, 'r', 'l')),
        7: ((0, 2, 0, 'ly', 'r'), (0, 0, 0, 'ry', 'l'), (0, 2, 1, 'ly', 'r'), (0, 1, 0, 'lry', ''), (0, 1, 1, 'lry', '')),
    },
    2: {
        0: ((1, 0, 0, '', 'y'),),
        1: ((1, 1, 0, '', 'y'), (1, 1, 1, '', 'y')),
        2: ((1, 0, 1, 'r', 'l'), (1, 3, 0, '', 'y')),
        4: ((1, 3, 1, 'l', 'r'), (0, 0, 1, 'r', 'l'), (1, 2, 0, '', 'y'), (1, 2, 1, '', 'y')),
        6: ((0, 0, 0, 'ry', 'l'), (0, 3, 1, 'l', 'r')),
        7: ((0, 1, 0, 'ry', 'l'), (0, 3, 0, 'ly', 'r'), (0, 1, 1, 'ry', 'l'), (0, 2, 0, 'lry', ''), (0, 2, 1, 'lry', '')),
    },
    3: {
        0: ((1, 0, 0, '', 'y'), (1, 0, 1, '', 'l')),
        1: ((1, 1, 0, '', 'y'), (1, 1, 1, '', 'y')),
        2: ((0, 0, 1, '', 'l'), (0, 0, 0, 'y', 'l')),
        3: ((1, 2, 0, '', 'y'), (1, 2, 1, '', 'y')),
        4: ((0, 1, 0, 'y', 'l'),),
        5: ((0, 1, 1, 'y', 'l'), (1, 3, 0, '', 'y')),
        6: ((1, 3, 1, 'l', 'y'), (0, 2, 0, 'y', 'l')),
        7: ((0, 2, 1, 'y', 'l'), (0, 3, 0, 'ly', ''), (0, 3, 1, 'ly', '')),
    },
}
SUB = 256
GROUP = 6


def lookup(table, z, step):
    value = jnp.int32(0)
    for k in range(NZ):
        for s in range(2 * NZ):
            value = value + jnp.where((z == k) & (step == s), table[k][s], 0)
    return value


def head_kernel(scale, token_scale, f_ref, lab_ref, e_ref, dfin_ref, ghead_ref, norm_ref, labsum_ref, z_ref,
                e_b, e_t, fbuf, f_b, g_acc, from_y, from_l, from_r, dl, z_buf, z_rest, lse_all, z_sem, load_sem, ag_send, ag_recv,
                send_y, send_l, send_r, recv_y, recv_l, recv_r, st_send, st_recv):
    tp, dp, z, y = place()
    partner = tp + 1 - 2 * y
    vocab, width = e_ref.shape
    own = f_ref.shape[0]
    whole = vocab // (SUB * GROUP)
    rest = vocab - whole * SUB * GROUP
    log2e = 1.4426950408889634
    slope = scale * log2e
    blocks = [(j * SUB, SUB) for j in range(GROUP)]
    tail = [(n, min(SUB, rest - n)) for n in range(0, rest, SUB)]

    plane_barrier(tp, dp, [])

    half = own // 2
    to_tp = {"l": tp - 2, "r": tp + 2, "y": partner}

    def slot_of(o, zz):
        return 2 * zz + (1 - y if o else y)

    def piece(ref, h):
        return ref.at[pl.ds(h * half, half), :]

    def pass_on(o, zz, h, to, own_chunk=False):
        slot = slot_of(o, zz)
        return remote(piece(f_ref if own_chunk else fbuf.at[slot], h), piece(fbuf.at[slot], h), ag_send.at["lry".index(to), slot, h],
                      ag_recv.at[slot, h], to_tp[to], dp)

    def arrived(o, zz, h):
        slot = slot_of(o, zz)
        remote(piece(f_ref, h), piece(fbuf.at[slot], h), ag_send.at[0, slot, h], ag_recv.at[slot, h], partner, dp).wait_recv()

    def own_sends(k):
        first = (1, 0) if k in (0, NZ - 1) else (0, 1)
        return [pass_on(0, k, h, "y", True) for h in first] + [
            pass_on(0, k, h, to, True) for h in range(2) for to in ("l" if k > 0 else "") + ("r" if k < NZ - 1 else "")]

    def on_position(f):
        for k in range(NZ):
            pl.when(z == k)(functools.partial(f, k))

    def first_sends(k):
        for c in own_sends(k):
            c.start()

    on_position(first_sends)
    load = pltpu.make_async_copy(e_ref, g_acc, load_sem.at[0])
    load.start()
    own_copy = pltpu.make_async_copy(f_ref, fbuf.at[tp], load_sem.at[1])
    own_copy.start()
    load.wait()

    def prepare(at, size):
        part = g_acc[at, :]
        e_b[at, :] = part.astype(BF16)
        e_t[:, at] = part.T.astype(BF16)

    def prepare_body(n, carry):
        prepare(pl.ds(pl.multiple_of(n * SUB, SUB), SUB), SUB)
        return carry

    lax.fori_loop(0, vocab // SUB, prepare_body, 0)
    if vocab % SUB:
        prepare(pl.ds(vocab // SUB * SUB, vocab % SUB), vocab % SUB)
    own_copy.wait()

    big = SUB * GROUP

    def z_copies(slot, n, out):
        if n is None:
            pair = (z_rest, z_ref.at[slot, pl.ds(whole * big, rest), :])
            sem = z_sem.at[2]
        else:
            pair = (z_buf.at[lax.rem(n, 2)], z_ref.at[slot, pl.ds(pl.multiple_of(n * big, big), big), :])
            sem = z_sem.at[lax.rem(n, 2)]
        return pltpu.make_async_copy(*(pair if out else pair[::-1]), sem)

    def slot_at(order, step):
        code = lookup({k: [2 * zz + o for o, zz in order[k]] for k in range(NZ)}, z, step)
        other = code % 2
        return code // 2 * 2 + y + other - 2 * y * other

    def gather_step(step, carry):
        for k in range(NZ):
            for at, events in GATHER_EVENTS[k].items():
                def serve(events=events):
                    for o, zz, h, to in events:
                        arrived(o, zz, h)
                        for t in to:
                            pass_on(o, zz, h, t).start()
                pl.when((z == k) & (step == at))(serve)
        slot = slot_at(GATHER_ORDER, step)
        f_b[slot] = fbuf[slot].astype(BF16)
        f_now = f_b[slot]

        def group(base, parts, kept, c):
            top, total = c
            for first, size in parts:
                logit = lax.dot_general(e_b[pl.ds(base + first, size), :], f_now, (((1,), (1,)), ((), ())), preferred_element_type=F32)
                kept[pl.ds(first, size), :] = logit
                logit = logit.reshape(size // 8, 8, own)
                new = jnp.maximum(top, jnp.max(logit, axis=0))
                total = total * jnp.exp2((top - new) * slope) + jnp.sum(jnp.exp2((logit - new[None]) * slope), axis=0)
                top = new
            return top, total

        def body(n, c):
            @pl.when(step * whole + n >= 2)
            def _():
                z_copies(slot, n, True).wait()
            c = group(pl.multiple_of(n * big, big), blocks, z_buf.at[lax.rem(n, 2)], c)
            z_copies(slot, n, True).start()
            return c

        top, total = lax.fori_loop(0, whole, body, (jnp.full((8, own), -3e38, F32), jnp.zeros((8, own), F32)))
        if tail:
            @pl.when(step > 0)
            def _():
                z_copies(slot, None, True).wait()
            top, total = group(whole * big, tail, z_rest, (top, total))
            z_copies(slot, None, True).start()
        most = jnp.max(top, axis=0, keepdims=True)
        total = jnp.sum(total * jnp.exp2((top - most) * slope), axis=0, keepdims=True)
        lse_all[tp, pl.ds(slot, 1), :] = most * scale + jnp.log(total)
        return carry

    lax.fori_loop(0, 2 * NZ, gather_step, 0)
    for n in range(2):
        z_copies(0, jnp.int32(n), True).wait()
    if tail:
        z_copies(0, None, True).wait()

    for n in range(1, 2 * NZ):
        to = lax.rem(tp + n, 2 * NZ)
        remote(lse_all.at[tp], lse_all.at[tp], st_send.at[to], st_recv.at[tp], to, dp).start()

    def gathers_done(k):
        for c in own_sends(k):
            c.wait_send()
        for events in GATHER_EVENTS[k].values():
            for o, zz, h, to in events:
                for t in to:
                    pass_on(o, zz, h, t).wait_send()

    on_position(gathers_done)
    start_slot = slot_at(SCATTER_ORDER, 0)
    for n in range(2):
        z_copies(start_slot, jnp.int32(n), False).start()
    if tail:
        z_copies(start_slot, None, False).start()

    def clear(n, carry):
        g_acc[pl.ds(pl.multiple_of(n * 16, 16), 16), :] = jnp.zeros((16, width), F32)
        return carry

    lax.fori_loop(0, vocab // 16, clear, 0)
    for n in range(1, 2 * NZ):
        source = lax.rem(tp + n, 2 * NZ)
        remote(lse_all.at[source], lse_all.at[source], st_send.at[source], st_recv.at[source], source, dp).wait_recv()
    peak = jnp.max(lse_all[...], axis=0)
    log_norm = peak + jnp.log(jnp.sum(jnp.exp(lse_all[...] - peak[None]), axis=0))
    norm_ref[...] = log_norm

    def leave(o, zz, h, to):
        src = piece(fbuf.at[slot_of(o, zz)], h)
        if to == "y":
            at = 2 * zz + h
            return remote(src, from_y.at[at], send_y.at[at], recv_y.at[at], partner, dp)
        if to == "l":
            at = 6 if o else 2 * zz + h
            return remote(src, from_r.at[at], send_l.at[at], recv_r.at[at], tp - 2, dp)
        at = 6 if o else 2 * zz - 2 + h
        return remote(src, from_l.at[at], send_r.at[at], recv_l.at[at], tp + 2, dp)

    def collect(o, zz, h, sums, to):
        here = piece(fbuf.at[slot_of(o, zz)], h)
        for d in sums:
            at, buf, sem = {"y": (2 * zz + h, from_y, recv_y), "l": (6 if o else 2 * zz - 2 + h, from_l, recv_l),
                            "r": (6 if o else 2 * zz + h, from_r, recv_r)}[d]
            remote(here, buf.at[at], send_y.at[0], sem.at[at], partner, dp).wait_recv()
            add_into(here, buf.at[at])
        if to:
            leave(o, zz, h, to).start()

    def scatter_step(step, lab_sum):
        slot = slot_at(SCATTER_ORDER, step)
        f_now = f_b[slot]
        acc = fbuf.at[slot]
        norm = norm_ref[pl.ds(slot, 1), :]
        shift = norm * log2e
        coef = (1.0 + 2.0 * LOGIT_ZLOSS * norm) * token_scale
        lab = lab_ref[pl.ds(slot // 2, 1), pl.ds(pl.multiple_of(lax.rem(slot, 2) * own, own), own)] - tp * vocab
        acc[...] = jnp.zeros((width, own), F32)

        def group(base, parts, kept, hits):
            for first, size in parts:
                at = pl.ds(base + first, size)
                logit = kept[pl.ds(first, size), :]
                hit = lax.broadcasted_iota(jnp.int32, (size, own), 0) == lab - (base + first)
                prob = jnp.exp2(logit * slope - shift) * coef
                grad = jnp.where(hit, prob - token_scale, prob).astype(BF16)
                hits = hits + jnp.sum(jnp.where(hit, logit, 0.0).reshape(size // 8, 8, own), axis=0)
                dl[pl.ds(first, size), :] = grad
                g_acc[at, :] += jnp.dot(grad, f_now, preferred_element_type=F32)
            size = parts[-1][0] + parts[-1][1]
            acc[...] += jnp.dot(e_t[:, pl.ds(base, size)], dl[pl.ds(0, size), :], preferred_element_type=F32)
            return hits

        following = slot_at(SCATTER_ORDER, jnp.minimum(step + 1, 2 * NZ - 1))

        def body(n, hits):
            z_copies(slot, n, False).wait()
            hits = group(pl.multiple_of(n * big, big), blocks, z_buf.at[lax.rem(n, 2)], hits)

            @pl.when(n + 2 < whole)
            def _():
                z_copies(slot, n + 2, False).start()

            @pl.when((n + 2 >= whole) & (step + 1 < 2 * NZ))
            def _():
                z_copies(following, n + 2 - whole, False).start()
            return hits

        lab_sum = lax.fori_loop(0, whole, body, lab_sum)
        if tail:
            z_copies(slot, None, False).wait()
            lab_sum = group(whole * big, tail, z_rest, lab_sum)

            @pl.when(step + 1 < 2 * NZ)
            def _():
                z_copies(following, None, False).start()

        for k in range(NZ):
            for at, events in SCATTER_EVENTS[k].items():
                def reduce(events=events):
                    for event in events:
                        collect(*event)
                pl.when((z == k) & (step == at))(reduce)
        return lab_sum

    lab_sum = lax.fori_loop(0, 2 * NZ, scatter_step, jnp.zeros((8, own), F32))
    labsum_ref[...] = lab_sum
    store = pltpu.make_async_copy(g_acc, ghead_ref, load_sem.at[0])
    store.start()
    dfin_ref[...] = fbuf[tp].T

    def scatters_done(k):
        for events in SCATTER_EVENTS[k].values():
            for o, zz, h, _, to in events:
                if to:
                    leave(o, zz, h, to).wait_send()

    on_position(scatters_done)
    for n in range(1, 2 * NZ):
        to = lax.rem(tp + n, 2 * NZ)
        remote(lse_all.at[tp], lse_all.at[tp], st_send.at[to], st_recv.at[tp], to, dp).wait_send()
    store.wait()


def head(f_own, labels, embed, scale, token_scale, collective_id):
    own, width = f_own.shape
    vocab = embed.shape[0]
    chunk = (own, width)
    strips = lambda n: pltpu.VMEM((n, own // 2, width), F32)
    dma = lambda *n: pltpu.SemaphoreType.DMA(n)
    return pl.pallas_call(
        functools.partial(head_kernel, scale, token_scale),
        out_shape=(jax.ShapeDtypeStruct((own, width), F32), jax.ShapeDtypeStruct((vocab, width), F32),
                   jax.ShapeDtypeStruct((2 * NZ, own), F32), jax.ShapeDtypeStruct((8, own), F32),
                   jax.ShapeDtypeStruct((2 * NZ, vocab, own), F32)),
        in_specs=[VMEM, VMEM, ANY],
        out_specs=(VMEM, ANY, VMEM, VMEM, ANY),
        scratch_shapes=[pltpu.VMEM((vocab, width), BF16), pltpu.VMEM((width, vocab), BF16),
                        pltpu.VMEM((2 * NZ,) + chunk, F32), pltpu.VMEM((2 * NZ,) + chunk, BF16), pltpu.VMEM((vocab, width), F32),
                        strips(8), strips(7), strips(7),
                        pltpu.VMEM((SUB * GROUP, own), BF16), pltpu.VMEM((2, SUB * GROUP, own), F32),
                        pltpu.VMEM((max(vocab % (SUB * GROUP), 8), own), F32), pltpu.VMEM((2 * NZ, 2 * NZ, own), F32),
                        dma(3), dma(2), dma(3, 2 * NZ, 2), dma(2 * NZ, 2), dma(8), dma(7), dma(7), dma(8), dma(7), dma(7), dma(2 * NZ), dma(2 * NZ)],
        compiler_params=pltpu.CompilerParams(collective_id=collective_id, has_side_effects=True, vmem_limit_bytes=67000000),
        cost_estimate=pl.CostEstimate(flops=8 * vocab * width * own * 8, bytes_accessed=3 * 4 * vocab * width, transcendentals=2 * vocab * own * 8),
        name="head",
    )(f_own, labels, embed)


TB = (((1,), (1,)), ((), ()))
TA = (((0,), (0,)), ((), ()))
LOG2E = 1.4426950408889634


def mm(a, b, dims=(((1,), (0,)), ((), ()))):
    return lax.dot_general(a, b, dims, preferred_element_type=F32)


def picks(code, n_slots):
    return (lax.broadcasted_iota(jnp.int32, (n_slots, code.shape[1]), 0) == code).astype(F32).astype(BF16)


def turn(lo, hi, cos_t, sin_t):
    return lo * cos_t - hi * sin_t, hi * cos_t + lo * sin_t


EVENTS = {
    0: (((("R", 1),), (0,)), ((("R", 2),), (1,)), ((("R", 3),), (2,)), ((), (3,))),
    1: (((("L", 0), ("R", 2)), (1,)), ((("R", 3),), (0,)), ((), (2,)), ((), (3,))),
    2: (((("R", 3), ("L", 1)), (2,)), ((("L", 0),), (3,)), ((), (1,)), ((), (0,))),
    3: (((("L", 2),), (3,)), ((("L", 1),), (2,)), ((("L", 0),), (1,)), ((), (0,))),
}
MLP_ORDER = {k: [2 * k] + [code for line, other in EVENTS[k] for code in [2 * zz for _, zz in line] + [2 * zz + 1 for zz in other]] for k in range(NZ)}


def front_kernel(ids_ref, e_ref, rounds_ref, code_ref, extra_ref, w_ref, wkv_ref, ln_ref, cos_ref, sin_ref,
                 f_ref, x1_ref, x0_ref, q_ref, kv_ref, kvt_ref, lse_ref, ctx_ref, wq_ref, wo_ref, wg_ref, wu_ref, wd_ref, rounds_all,
                 table, rows_ref, wl, rows_in, u_b, kv_out, kv_in, own_sem, r_send, r_recv, a_y, a_l, a_r, a_c, a_recv,
                 b_y, b_l, b_r, b_x, b_c, b_recv, kv_send, kv_recv, n_send, n_recv):
    tp, dp, z, y = place()
    partner = tp + 1 - 2 * y
    core = dp % 2
    twin = dp + 1 - 2 * core
    facing = lax.rem(dp + 2, 4)
    own, width = x0_ref.shape
    shards, w_rows = wl.shape[0], wl.shape[1]
    nq = q_ref.shape[0]
    ff = wg_ref.shape[0]
    n_a = nq // shards
    n_f = ff // shards
    n_b = 3 * n_f // 4
    hd = kv_out.shape[0] // 2
    quarter = hd // 2
    heads = nq // hd

    def a_rows(c):
        return pl.ds(pl.multiple_of(c * n_a, 8), n_a)

    def b_rows(d):
        return pl.ds(pl.multiple_of(2 * n_a + d * n_b, 8), n_b)

    def a_copy(slot, sems, to, to_dp, first=False):
        src = w_ref.at[a_rows(core), :] if first else wl.at[slot, a_rows(core), :]
        return remote(src, wl.at[slot, a_rows(core), :], sems.at[slot], a_recv.at[slot, core], to, to_dp)

    def b_copy(slot, piece, sems, to, to_dp, first=False):
        src = w_ref.at[b_rows(piece), :] if first else wl.at[slot, b_rows(piece), :]
        return remote(src, wl.at[slot, b_rows(piece), :], sems.at[slot], b_recv.at[slot, piece], to, to_dp)

    def a_wait(slot, c):
        remote(w_ref.at[a_rows(c), :], wl.at[slot, a_rows(c), :], a_y.at[slot], a_recv.at[slot, c], partner, dp).wait_recv()

    def b_wait(slot, piece):
        remote(w_ref.at[b_rows(piece), :], wl.at[slot, b_rows(piece), :], b_y.at[slot], b_recv.at[slot, piece], partner, dp).wait_recv()

    def on_position(f):
        for k in range(NZ):
            pl.when(z == k)(functools.partial(f, k))

    def line_sends(k, make, y_sems, l_sems, r_sems, slot, side, first=False):
        sends = [make(slot, y_sems, partner, dp, first)]
        if k > 0 and side != "L":
            sends.append(make(slot, l_sems, tp - 2, dp, first))
        if k < NZ - 1 and side != "R":
            sends.append(make(slot, r_sems, tp + 2, dp, first))
        return sends

    def b_own(slot, sems, to, to_dp, first=False):
        return b_copy(slot, dp, sems, to, to_dp, first)

    def a_sends(k, slot, side, first=False):
        return line_sends(k, a_copy, a_y, a_l, a_r, slot, side, first)

    def b_sends(k, slot, side, first=False):
        return line_sends(k, b_own, b_y, b_l, b_r, slot, side, first)

    def start(copies):
        for c in copies:
            c.start()

    load = pltpu.make_async_copy(e_ref, table, own_sem.at[2])
    load.start()
    group = [twin, facing, lax.rem(twin + 2, 4)]
    plane_barrier(tp, dp, [(tp, d) for d in group])
    peers = [lax.rem(tp + n, shards) for n in range(1, shards)]

    def rounds_copy(n):
        return remote(rounds_ref, rounds_all.at[dp], n_send.at[n], n_recv.at[dp], tp, group[n])

    for n in range(3):
        rounds_copy(n).start()
    rounds_all[dp] = rounds_ref[...]

    def row_copy(to):
        return remote(rows_ref.at[to], rows_in.at[tp], r_send.at[to], r_recv.at[tp], to, dp)

    on_position(lambda k: start(b_sends(k, tp, "", True)))
    on_position(lambda k: start(a_sends(k, tp, "", True)))
    own_w = pltpu.make_async_copy(w_ref, wl.at[tp], own_sem.at[1])
    own_w.start()

    def a_event(t, k):
        line, other = EVENTS[k][t]
        for side, zz in line:
            slot = 2 * zz + y
            a_wait(slot, core)
            start(a_sends(k, slot, side))
            a_copy(slot, a_c, tp, twin).start()
        for zz in other:
            slot = 2 * zz + 1 - y
            a_wait(slot, core)
            a_copy(slot, a_c, tp, twin).start()

    def b_event(t, k):
        line, other = EVENTS[k][t]
        for side, zz in line:
            slot = 2 * zz + y
            b_wait(slot, dp)
            start(b_sends(k, slot, side))
            b_copy(slot, dp, b_x, tp, facing).start()
            b_copy(slot, dp, b_c.at[0], tp, twin).start()
        for zz in other:
            slot = 2 * zz + 1 - y
            b_wait(slot, dp)
            b_copy(slot, dp, b_x, tp, facing).start()
            b_copy(slot, dp, b_c.at[0], tp, twin).start()

    load.wait()
    cap = rows_ref.shape[1]

    def pick_rows(n, carry):
        for i in range(8):
            rows_ref[n // (cap // 8), pl.ds(lax.rem(n, cap // 8) * 8 + i, 1), :] = table[pl.ds(ids_ref[n * 8 + i], 1), :]
        return carry

    lax.fori_loop(0, shards * cap // 8, pick_rows, 0)
    start([row_copy(to) for to in peers])
    own_rows = pltpu.make_async_copy(rows_ref.at[tp], rows_in.at[tp], own_sem.at[0])
    own_rows.start()
    on_position(functools.partial(b_event, 0))
    on_position(functools.partial(a_event, 0))
    on_position(functools.partial(b_event, 1))
    on_position(functools.partial(a_event, 1))
    own_rows.wait()
    for source in peers:
        remote(rows_ref.at[source], rows_in.at[source], r_send.at[source], r_recv.at[source], source, dp).wait_recv()
    n_slots = shards * cap
    x0_ref[...] = extra_ref[...] + mm(picks(code_ref[...], n_slots), rows_in[...].reshape(n_slots, width).astype(BF16), TA)
    u_b[...] = norm_fwd(x0_ref[...], ln_ref[0:1, :])[0]
    x1_ref[...] = x0_ref[...]
    cos_t = cos_ref[...]
    sin_t = sin_ref[...]
    kv = mm(wkv_ref[...].astype(BF16), u_b[...], TB)
    lo, hi = turn(kv[:quarter], kv[quarter:hd], cos_t, sin_t)
    kv_out[0:quarter, :] = lo
    kv_out[quarter:hd, :] = hi
    kv_out[hd:, :] = kv[hd:]
    kv_copy = remote(kv_out, kv_in, kv_send, kv_recv, partner, dp)
    kv_copy.start()

    def slot_of(step):
        code = lookup(MLP_ORDER, z, step)
        other = code % 2
        return code // 2 * 2 + y + other - 2 * y * other

    def mlp(step, carry):
        def pass_on():
            slot = slot_of(step + 1)
            b_wait(slot, facing)
            b_copy(slot, facing, b_c.at[1], tp, twin).start()
        pl.when(step < shards - 1)(pass_on)
        slot = slot_of(step)

        def rest():
            b_wait(slot, twin)
            b_wait(slot, lax.rem(twin + 2, 4))
        pl.when(step > 0)(rest)
        at = pl.ds(pl.multiple_of(slot * n_f, n_f), n_f)
        wg_ref[at, :] = wl[slot, 2 * n_a:2 * n_a + n_f, :].astype(BF16)
        wu_ref[at, :] = wl[slot, 2 * n_a + n_f:2 * n_a + 2 * n_f, :].astype(BF16)
        wd_ref[at, :] = wl[slot, 2 * n_a + 2 * n_f:2 * n_a + 3 * n_f, :].astype(BF16)
        gate = mm(u_b[...], wg_ref[at, :], TB)
        up = mm(u_b[...], wu_ref[at, :], TB)
        x1_ref[...] += mm((gate * jax.nn.sigmoid(gate) * up).astype(BF16), wd_ref[at, :])
        return carry

    own_w.wait()
    lax.fori_loop(0, 3, mlp, 0)
    on_position(functools.partial(b_event, 2))
    on_position(functools.partial(a_event, 2))
    lax.fori_loop(3, 4, mlp, 0)
    on_position(functools.partial(a_event, 3))
    on_position(functools.partial(b_event, 3))
    for source in peers:
        a_wait(source, 1 - core)
    for s in range(shards):
        wq_ref[s * n_a:(s + 1) * n_a, :] = wl[s, 0:n_a, :].astype(BF16)
        wo_ref[s * n_a:(s + 1) * n_a, :] = wl[s, n_a:2 * n_a, :].astype(BF16)

    q_all = mm(wq_ref[...], u_b[...], TB)
    for h in range(heads):
        lo, hi = turn(q_all[h * hd:h * hd + quarter], q_all[h * hd + quarter:(h + 1) * hd], cos_t, sin_t)
        q_ref[h * hd:h * hd + quarter, :] = lo.astype(BF16)
        q_ref[h * hd + quarter:(h + 1) * hd, :] = hi.astype(BF16)
    kv_copy.wait()

    def fill(mine, other):
        kv_ref[mine * own:(mine + 1) * own, :] = kv_out[...].T.astype(BF16)
        kv_ref[other * own:(other + 1) * own, :] = kv_in[...].T.astype(BF16)
        kvt_ref[:, mine * own:(mine + 1) * own] = kv_out[...].astype(BF16)
        kvt_ref[:, other * own:(other + 1) * own] = kv_in[...].astype(BF16)

    pl.when(y == 0)(lambda: fill(0, 1))
    pl.when(y == 1)(lambda: fill(1, 0))
    blank = jnp.zeros((hd, own), BF16)
    slope = hd ** -0.5 * LOG2E

    def attend(h, carry):
        at = pl.ds(pl.multiple_of(h * hd, hd), hd)
        scores = mm(kv_ref[...], jnp.concatenate([q_ref[at, :], blank], axis=0))
        allowed = lax.broadcasted_iota(jnp.int32, scores.shape, 0) <= lax.broadcasted_iota(jnp.int32, scores.shape, 1) + y * own
        scores = jnp.where(allowed, scores * slope, -1e30)
        top = jnp.max(scores, axis=0, keepdims=True)
        prob = jnp.exp2(scores - top)
        total = jnp.sum(prob, axis=0, keepdims=True)
        lse_ref[pl.ds(h, 1), :] = top + jnp.log2(total)
        ctx_ref[at, :] = mm(kvt_ref[hd:, :], (prob * (1.0 / total)).astype(BF16)).astype(BF16)
        return carry

    lax.fori_loop(0, heads, attend, 0)
    x1_ref[...] += mm(ctx_ref[...], wo_ref[...], TA)

    lax.fori_loop(4, shards, mlp, 0)
    f_ref[...] = norm_fwd(x1_ref[...], ln_ref[1:2, :])[0].astype(F32)

    def finish(k):
        done = a_sends(k, tp, "", True) + b_sends(k, tp, "", True)
        for line, other in EVENTS[k]:
            for side, zz in line:
                done += a_sends(k, 2 * zz + y, side) + b_sends(k, 2 * zz + y, side)
        for c in done:
            c.wait_send()

    on_position(finish)
    for n in range(3):
        rounds_copy(n).wait_send()
        remote(rounds_ref, rounds_all.at[group[n]], n_send.at[n], n_recv.at[group[n]], tp, twin).wait_recv()
    for to in peers:
        row_copy(to).wait_send()
        a_copy(to, a_c, tp, twin).wait_send()
        b_copy(to, dp, b_x, tp, facing).wait_send()
        b_copy(to, dp, b_c.at[0], tp, twin).wait_send()
        b_copy(to, facing, b_c.at[1], tp, twin).wait_send()


def front(ids, embed, rounds, code, extra, w_rows, wkv_t, ln, cos_t, sin_t, n_q, collective_id):
    own, width = extra.shape
    two_hd = wkv_t.shape[0]
    shards = 2 * NZ
    ff = (w_rows.shape[0] * shards - 2 * n_q) // 3
    dma = lambda *n: pltpu.SemaphoreType.DMA(n)
    s = jax.ShapeDtypeStruct
    rows = (shards, ids.shape[0] // shards, width)
    return pl.pallas_call(
        front_kernel,
        out_shape=(s((own, width), F32),) * 3 + (s((n_q, own), BF16), s((2 * own, two_hd), BF16), s((two_hd, 2 * own), BF16),
                   s((2 * n_q // two_hd, own), F32), s((n_q, own), BF16), s((n_q, width), BF16), s((n_q, width), BF16))
        + (s((ff, width), BF16),) * 3 + (s((4, 1, 128), jnp.int32),),
        in_specs=[pl.BlockSpec(memory_space=pltpu.SMEM), ANY, VMEM, VMEM, VMEM, ANY] + [VMEM] * 4,
        out_specs=(VMEM,) * 14,
        scratch_shapes=[pltpu.VMEM(embed.shape, F32), pltpu.VMEM(rows, F32), pltpu.VMEM((shards,) + w_rows.shape, F32), pltpu.VMEM(rows, F32), pltpu.VMEM((own, width), BF16),
                        pltpu.VMEM((two_hd, own), F32), pltpu.VMEM((two_hd, own), F32),
                        dma(3), dma(shards), dma(shards)] + [dma(shards)] * 4 + [dma(shards, 2)]
        + [dma(shards)] * 4 + [dma(2, shards), dma(shards, 4), pltpu.SemaphoreType.DMA, pltpu.SemaphoreType.DMA, dma(3), dma(4)],
        compiler_params=pltpu.CompilerParams(collective_id=collective_id, has_side_effects=True, vmem_limit_bytes=60000000),
        name="front",
    )(ids, embed, rounds, code, extra, w_rows, wkv_t, ln, cos_t, sin_t)


def layer_bwd_kernel(scale, tok_total, dfin_ref, x0_ref, x1_ref, norm_ref, hits_ref, ln_ref, cos_ref, sin_ref, wq_ref, wkv_ref, wo_ref, wg_ref, wu_ref, wd_ref,
                     q_ref, kv_ref, kvt_ref, lse_ref, ctx_ref, code_ref, g_ref, ids_ref, rows_ref, d0_ref, back_ref, early_ref, ids_all, d_one, d_b, u_b, dctx, dq, dkv, dkv_in,
                     hid, d_gate, d_up, rows_out, g_q, g_o, g_g, g_u, g_d, small, s_early, c_early, out_sem, send_sem, recv_sem,
                     r_send, x_send, c_send, r_recv, g_load, g_send, g_recv, id_send, id_recv):
    tp, dp, z, y = place()
    partner = tp + 1 - 2 * y
    core = dp % 2
    twin = dp + 1 - 2 * core
    facing = lax.rem(dp + 2, 4)
    across = lax.rem(twin + 2, 4)
    own, width = x0_ref.shape
    hd = kv_ref.shape[1] // 2
    quarter = hd // 2
    nq = q_ref.shape[0]
    heads = nq // hd
    ff = wg_ref.shape[0]
    shards = rows_ref.shape[0]
    plane_barrier(tp, dp, [(tp, twin), (tp, facing), (tp, across)])

    n_early, g_size = s_early.shape[0], s_early.shape[1]

    def g_rows(which, b):
        return g_ref.at[pl.ds(pl.multiple_of(which * (g_ref.shape[0] // 2) + b * g_size, 8), g_size), :]

    def g_load_copy(b):
        return pltpu.make_async_copy(g_rows(core, b), s_early.at[b], g_load.at[b])

    def g_chip_copy(b):
        return remote(g_rows(1 - core, b), c_early.at[b], g_send.at[0, b], g_recv.at[0, b], tp, twin)

    def g_x_copy(b):
        return remote(s_early.at[b], early_ref.at[b], g_send.at[1, b], g_recv.at[1, b], tp, facing)

    for b in range(n_early):
        g_chip_copy(b).start()
        g_load_copy(b).start()

    def ids_copy(n, to):
        return remote(ids_ref, ids_all.at[dp], id_send.at[n], id_recv.at[dp], tp, to)

    for n, to in enumerate((twin, facing, across)):
        ids_copy(n, to).start()
    ids_all[dp] = ids_ref[...]
    _, f_hat, f_inv = norm_fwd(x1_ref[...], ln_ref[1:2, :])
    d_in, g_fin = norm_bwd(dfin_ref[...], f_hat, f_inv, ln_ref[1:2, :])
    d_one[...] = d_in
    d_b[...] = d_in.astype(BF16)
    u_b[...] = norm_fwd(x0_ref[...], ln_ref[0:1, :])[0]
    dctx[...] = mm(wo_ref[...], d_b[...], TB).astype(BF16)
    for b in range(n_early):
        g_load_copy(b).wait()
        g_chip_copy(b).wait_recv()
        add_into(s_early.at[b], c_early.at[b], 24)
        g_x_copy(b).start()
    cos_t = cos_ref[...]
    sin_t = sin_ref[...]
    blank = jnp.zeros((hd, own), BF16)
    slope = hd ** -0.5 * LOG2E
    dkv[...] = jnp.zeros_like(dkv)

    def attend(h, carry):
        at = pl.ds(pl.multiple_of(h * hd, hd), hd)
        q_pad = jnp.concatenate([q_ref[at, :], blank], axis=0)
        d_pad = jnp.concatenate([blank, dctx[at, :]], axis=0)
        scores = mm(kv_ref[...], q_pad)
        allowed = lax.broadcasted_iota(jnp.int32, scores.shape, 0) <= lax.broadcasted_iota(jnp.int32, scores.shape, 1) + y * own
        prob = jnp.where(allowed, jnp.exp2(scores * slope - lse_ref[pl.ds(h, 1), :]), 0.0)
        d_prob = mm(kv_ref[...], d_pad)
        mean = jnp.sum(d_prob * prob, axis=0, keepdims=True)
        d_score = (prob * (d_prob - mean) * hd ** -0.5).astype(BF16)
        dkv[...] += mm(d_score, q_pad, TB) + mm(prob.astype(BF16), d_pad, TB)
        d_q = mm(kvt_ref[0:hd, :], d_score)
        lo, hi = turn(d_q[:quarter], d_q[quarter:], cos_t, -sin_t)
        dq[at, :] = jnp.concatenate([lo, hi], axis=0).astype(BF16)
        return carry

    lax.fori_loop(0, heads, attend, 0)
    copy = remote(dkv.at[pl.ds(pl.multiple_of((1 - y) * own, own), own), :], dkv_in, send_sem, recv_sem, partner, dp)
    copy.start()

    d0_ref[...] = mm(dq[...], wq_ref[...], TA)
    step = min(512, ff)

    def mlp(n, carry):
        at = pl.ds(pl.multiple_of(n * step, step), step)
        gate = mm(wg_ref[at, :], u_b[...], TB)
        up = mm(wu_ref[at, :], u_b[...], TB)
        d_hidden = mm(wd_ref[at, :], d_b[...], TB)
        sig = jax.nn.sigmoid(gate)
        hid[at, :] = (gate * sig * up).astype(BF16)
        d_gate[at, :] = (d_hidden * up * sig * (1.0 + gate * (1.0 - sig))).astype(BF16)
        d_up[at, :] = (d_hidden * gate * sig).astype(BF16)
        d0_ref[...] += mm(d_gate[at, :], wg_ref[at, :], TA) + mm(d_up[at, :], wu_ref[at, :], TA)
        return carry

    lax.fori_loop(0, ff // step, mlp, 0)
    copy.wait()
    d_kv = (dkv[pl.ds(pl.multiple_of(y * own, own), own), :] + dkv_in[...]).T
    lo, hi = turn(d_kv[:quarter], d_kv[quarter:hd], cos_t, -sin_t)
    d_kv = jnp.concatenate([lo, hi, d_kv[hd:]], axis=0).astype(BF16)
    small[0:2 * hd, :] = mm(d_kv, u_b[...])
    d_u = d0_ref[...] + mm(d_kv, wkv_ref[...].astype(BF16), TA)
    _, u_hat, u_inv = norm_fwd(x0_ref[...], ln_ref[0:1, :])
    d_in, g_in = norm_bwd(d_u, u_hat, u_inv, ln_ref[0:1, :])
    d_zero = d_one[...] + d_in
    d0_ref[...] = d_zero
    high = d_zero.astype(BF16)
    left = d_zero - high.astype(F32)
    middle = left.astype(BF16)
    low = (left - middle.astype(F32)).astype(BF16)
    pick = picks(code_ref[...], rows_out.shape[0] * rows_out.shape[1])
    rows_out[...] = (mm(pick, high) + mm(pick, middle) + mm(pick, low)).reshape(rows_out.shape)

    def row_copy(to):
        return remote(rows_out.at[to], back_ref.at[dp, tp], r_send.at[to], r_recv.at[dp, tp], to, dp)

    def x_copy(slot):
        return remote(back_ref.at[dp, slot], back_ref.at[dp, slot], x_send.at[slot], r_recv.at[dp, slot], tp, facing)

    def c_copy(group, n, slot):
        return remote(back_ref.at[group, slot], back_ref.at[group, slot], c_send.at[n, slot], r_recv.at[group, slot], tp, twin)

    def back(group, slot):
        remote(rows_out.at[slot], back_ref.at[group, slot], r_send.at[slot], r_recv.at[group, slot], tp, twin).wait_recv()

    def near_first(k):
        return sorted(((o, zz) for o in range(2) for zz in range(NZ)), key=lambda c: (abs(c[1] - k), c[0]))

    def slot_of(o, zz):
        return 2 * zz + (1 - y if o else y)

    def on_position(f):
        for k in range(NZ):
            pl.when(z == k)(functools.partial(f, k))

    def rows_leave(k):
        for c in near_first(k)[1:]:
            row_copy(slot_of(*c)).start()

    on_position(rows_leave)
    own_rows = pltpu.make_async_copy(rows_out.at[tp], back_ref.at[dp, tp], out_sem.at[7 * 2 * NZ])
    own_rows.start()
    own_rows.wait()
    x_copy(tp).start()
    c_copy(dp, 0, tp).start()

    g_o[...] = mm(ctx_ref[...], d_b[...])
    g_q[...] = mm(dq[...], u_b[...])

    def weight_grads(n, carry):
        at = pl.ds(pl.multiple_of(n * step, step), step)
        g_d[at, :] = mm(hid[at, :], d_b[...])
        g_g[at, :] = mm(d_gate[at, :], u_b[...])
        g_u[at, :] = mm(d_up[at, :], u_b[...])
        return carry

    lax.fori_loop(0, ff // step, weight_grads, 0)
    small[2 * hd:, :] = jnp.zeros_like(small[2 * hd:, :])
    small[2 * hd:2 * hd + 1, :] = g_in.reshape(1, width)
    small[2 * hd + 1:2 * hd + 2, :] = g_fin.reshape(1, width)
    norm = norm_ref[pl.ds(tp, 1), :]
    hits = jnp.sum(hits_ref[...], axis=0, keepdims=True)
    small[2 * hd + 2:2 * hd + 3, :] = (norm + LOGIT_ZLOSS * norm * norm - hits * scale) / tok_total
    copies = []

    def put(src, first, size, s):
        copies.append(pltpu.make_async_copy(src, rows_ref.at[s, pl.ds(first, size), :], out_sem.at[len(copies)]))

    n_kv = 2 * hd // shards
    for s in range(shards):
        at = 0
        for g, size in ((g_q, nq // shards), (g_o, nq // shards), (g_g, ff // shards), (g_u, ff // shards), (g_d, ff // shards)):
            put(g.at[pl.ds(s * size, size), :], at, size, s)
            at += size
        put(small.at[pl.ds(s * n_kv, n_kv), :], at, n_kv, s)
        put(small.at[pl.ds(2 * hd + (0 if s == 0 else 16), 16), :], at + n_kv, 16, s)
    for c in copies:
        c.start()
    for c in copies:
        c.wait()

    def relay(k):
        order = near_first(k)
        for c in order[1:]:
            back(dp, slot_of(*c))
            x_copy(slot_of(*c)).start()
            c_copy(dp, 0, slot_of(*c)).start()
        for c in order:
            back(facing, slot_of(*c))
            c_copy(facing, 1, slot_of(*c)).start()

    on_position(relay)
    for b in range(n_early):
        g_x_copy(b).wait_recv()
        add_into(early_ref.at[b], s_early.at[b], 24)
    for slot in range(shards):
        back(twin, slot)
        back(across, slot)
    for n, to in enumerate((twin, facing, across)):
        remote(ids_ref, ids_all.at[to], id_send.at[n], id_recv.at[to], tp, to).wait_recv()
        ids_copy(n, to).wait_send()
    for n in range(1, shards):
        row_copy(lax.rem(tp + n, shards)).wait_send()
    for slot in range(shards):
        x_copy(slot).wait_send()
        c_copy(dp, 0, slot).wait_send()
        c_copy(facing, 1, slot).wait_send()
    for b in range(n_early):
        g_chip_copy(b).wait_send()
        g_x_copy(b).wait_send()


def layer_bwd(scale, tok_total, d_fin, x0, x1, norms, hits, ln, cos_t, sin_t, weights, saved, code, g_table, ids, collective_id):
    own, width = x0.shape
    nq = weights[0].shape[0]
    two_hd = weights[1].shape[0]
    ff = weights[3].shape[0]
    rows = (2 * nq + 3 * ff + two_hd) // (2 * NZ) + 16
    chunk = (own, width)
    back = (2 * NZ, ids.shape[1] // (2 * NZ), width)
    blocks = (N_EARLY, table_block(g_table.shape[0]), width)
    dma = lambda *n: pltpu.SemaphoreType.DMA(n)
    return pl.pallas_call(
        functools.partial(layer_bwd_kernel, scale, tok_total),
        out_shape=(jax.ShapeDtypeStruct((2 * NZ, rows, width), F32), jax.ShapeDtypeStruct(chunk, F32), jax.ShapeDtypeStruct((4,) + back, F32),
                   jax.ShapeDtypeStruct(blocks, F32), jax.ShapeDtypeStruct((4,) + ids.shape, jnp.int32)),
        in_specs=[VMEM] * 20 + [ANY, VMEM],
        out_specs=(ANY, VMEM, ANY, VMEM, VMEM),
        scratch_shapes=[pltpu.VMEM(chunk, F32), pltpu.VMEM(chunk, BF16), pltpu.VMEM(chunk, BF16), pltpu.VMEM((nq, own), BF16),
                        pltpu.VMEM((nq, own), BF16), pltpu.VMEM((2 * own, two_hd), F32), pltpu.VMEM((own, two_hd), F32)]
        + [pltpu.VMEM((ff, own), BF16)] * 3 + [pltpu.VMEM(back, F32), pltpu.VMEM((nq, width), F32), pltpu.VMEM((nq, width), F32)] + [pltpu.VMEM((ff, width), F32)] * 3
        + [pltpu.VMEM((two_hd + 32, width), F32), pltpu.VMEM(blocks, F32), pltpu.VMEM(blocks, F32), dma(14 * NZ + 1),
           pltpu.SemaphoreType.DMA, pltpu.SemaphoreType.DMA, dma(2 * NZ), dma(2 * NZ), dma(2, 2 * NZ), dma(4, 2 * NZ),
           dma(N_EARLY), dma(2, N_EARLY), dma(2, N_EARLY), dma(3), dma(4)],
        compiler_params=pltpu.CompilerParams(collective_id=collective_id, has_side_effects=True, vmem_limit_bytes=66000000),
        name="layer_bwd",
    )(d_fin, x0, x1, norms, hits, ln, cos_t, sin_t, *weights, *saved, code, g_table, ids)


N_BLOCK = 12
N_EARLY = 4
AHEAD = 11


def table_block(vocab):
    return -(-vocab // (2 * N_BLOCK * 24)) * 24


W_REDUCE = {
    0: {5: (3,), 7: (2,), 9: (1,), 10: (0,)},
    1: {7: (3,), 9: (2, 0), 10: (1,)},
    2: {7: (0,), 9: (1, 3), 10: (2,)},
    3: {5: (0,), 7: (1,), 9: (2,), 10: (3,)},
}


def tail_kernel(g_ref, p_ref, rows_ref, ids_ref, early_ref, t_ref, w_out, small_ref,
                s_buf, from_c, from_x, look_in, parts, acc, w_c, w_y, w_l, w_r, w_x,
                g_load, g_send_c, g_recv_c, g_send_x, g_recv_x, g_send_t, g_recv_t, g_store, l_sem,
                w_load, w_out_sem, send_c, send_y, send_l, send_r, recv_c, recv_y, recv_l, recv_r, last_send, last_recv, small_send, small_recv):
    tp, dp, z, y = place()
    partner = tp + 1 - 2 * y
    core = dp % 2
    twin = dp + 1 - 2 * core
    facing = lax.rem(dp + 2, 4)
    half = g_ref.shape[0] // 2
    size = s_buf.shape[1]
    last = half - (N_BLOCK - 1) * size
    n_look = rows_ref.shape[1]

    def rows(which, b, n):
        return pl.ds(pl.multiple_of(which * half + b * size, 8), n)

    def part(buf, b, n):
        return buf.at[b - N_EARLY if buf is not from_x else b, pl.ds(0, n), :]

    plane_barrier(tp, dp, [(tp, twin), (tp, facing)])

    chip = dp // 2
    groups = (2 * chip, 2 * chip + 1, 2 - 2 * chip, 3 - 2 * chip)

    def look_load(n):
        return pltpu.make_async_copy(rows_ref.at[groups[n]], look_in.at[n % 2], l_sem.at[n % 2])

    def early_load(b):
        return pltpu.make_async_copy(early_ref.at[b], from_x.at[b], g_load.at[b])

    for n in range(2):
        look_load(n).start()

    def c_copy(b, n):
        return remote(g_ref.at[rows(1 - core, b, n), :], part(from_c, b, n), g_send_c.at[b], g_recv_c.at[b], tp, twin)

    def own_load(b, n):
        return pltpu.make_async_copy(g_ref.at[rows(core, b, n), :], part(s_buf, b, n), g_load.at[b])

    def x_copy(b, n):
        return remote(part(s_buf, b, n), part(from_x, b, n), g_send_x.at[b], g_recv_x.at[b], tp, facing)

    def t_copy(b, n):
        return remote(part(from_x, b, n), t_ref.at[rows(core, b, n), :], g_send_t.at[b], g_recv_t.at[b], tp, twin)

    def t_store(b, n):
        return pltpu.make_async_copy(part(from_x, b, n), t_ref.at[rows(core, b, n), :], g_store.at[b])

    def every(f, first, end):
        def body(b, carry):
            f(b, size)
            return carry
        lax.fori_loop(first, min(end, N_BLOCK - 1), body, 0)
        if end == N_BLOCK:
            f(N_BLOCK - 1, last)

    def looked_up(b, n, first, count):
        ids = jnp.concatenate([ids_ref[first + g] for g in range(count)], axis=1) - (core * half + b * size)
        hit = (lax.broadcasted_iota(jnp.int32, (n, count * n_look), 0) == ids).astype(F32).astype(BF16)
        span = pl.ds(pl.multiple_of(first * n_look, n_look), count * n_look)
        return mm(hit, parts[0, span, :]) + mm(hit, parts[1, span, :]) + mm(hit, parts[2, span, :])

    def chip_sum(b, n):
        own_load(b, n).wait()
        c_copy(b, n).wait_recv()
        at = b - N_EARLY
        s_buf[at, 0:n, :] = s_buf[at, 0:n, :] + from_c[at, 0:n, :] + looked_up(b, n, 2 * chip, 2)
        x_copy(b, n).start()

    def early_sum(b, n):
        early_load(b).wait()
        from_x[b] = from_x[b] + looked_up(b, n, 0, 4)
        t_copy(b, n).start()
        t_store(b, n).start()

    def w_first(k):
        for zz in REDUCE_ORDER[k]:
            for slot in (2 * zz + 1 - y, 2 * zz + y):
                remote(p_ref.at[slot, 1 - core], w_c.at[slot], send_c.at[slot], recv_c.at[slot], tp, twin).start()
                pltpu.make_async_copy(p_ref.at[slot, core], acc.at[slot], w_load.at[slot]).start()

    def w_chip_sum(slot):
        pltpu.make_async_copy(p_ref.at[slot, core], acc.at[slot], w_load.at[slot]).wait()
        remote(acc.at[slot], w_c.at[slot], send_c.at[slot], recv_c.at[slot], tp, twin).wait_recv()
        add_into(acc.at[slot], w_c.at[slot])

    def w_second(k):
        for zz in REDUCE_ORDER[k]:
            slot = 2 * zz + 1 - y
            w_chip_sum(slot)
            remote(acc.at[slot], w_y.at[zz], send_y.at[zz], recv_y.at[zz], partner, dp).start()
        for zz in REDUCE_ORDER[k]:
            w_chip_sum(2 * zz + y)

    def w_reduce(k, shards):
        for zz in shards:
            line = acc.at[2 * zz + y]
            remote(line, w_y.at[zz], send_y.at[zz], recv_y.at[zz], partner, dp).wait_recv()
            add_into(line, w_y.at[zz])
            if zz >= k and k > 0:
                remote(line, w_l.at[zz - 1], send_l.at[zz], recv_l.at[zz], partner, dp).wait_recv()
                add_into(line, w_l.at[zz - 1])
            if zz <= k and k < NZ - 1:
                remote(line, w_r.at[zz], send_r.at[zz], recv_r.at[zz], partner, dp).wait_recv()
                add_into(line, w_r.at[zz])
            if zz > k:
                remote(line, w_l.at[zz - 1], send_r.at[zz], recv_l.at[zz], tp + 2, dp).start()
            if zz < k:
                remote(line, w_r.at[zz], send_l.at[zz], recv_r.at[zz], tp - 2, dp).start()

    def on_position(f):
        for k in range(NZ):
            pl.when(z == k)(functools.partial(f, k))

    def first(b, n):
        c_copy(b, n).start()
        own_load(b, n).start()

    every(first, N_EARLY, N_EARLY + 2)
    on_position(w_first)
    every(first, N_EARLY + 2, N_BLOCK)
    for b in range(N_EARLY):
        early_load(b).start()

    def split(n):
        look_load(n).wait()
        value = look_in[n % 2]
        high = value.astype(BF16)
        left = value - high.astype(F32)
        middle = left.astype(BF16)
        at = pl.ds(pl.multiple_of(groups[n] * n_look, n_look), n_look)
        parts[0, at, :] = high
        parts[1, at, :] = middle
        parts[2, at, :] = (left - middle.astype(F32)).astype(BF16)
        if n + 2 < 4:
            look_load(n + 2).start()

    split(0)
    split(1)
    every(chip_sum, N_EARLY, N_EARLY + 3)
    on_position(w_second)
    every(chip_sum, N_EARLY + 3, AHEAD)
    split(2)
    split(3)
    every(early_sum, 0, N_EARLY)

    total = acc.at[tp]
    w_copy_x = remote(total, w_x, last_send.at[0], last_recv.at[0], tp, facing)
    w_copy_c = remote(total, w_out.at[core], last_send.at[1], last_recv.at[1], tp, twin)
    w_store = pltpu.make_async_copy(total, w_out.at[core], w_out_sem)
    n_small, n_rows = small_ref.shape[1], w_out.shape[1]
    mine = w_out.at[1, pl.ds(n_rows - 32, n_small), :]
    small_here = pltpu.make_async_copy(mine, small_ref.at[tp], w_out_sem)
    peers = [lax.rem(tp + n, 2 * NZ) for n in range(1, 2 * NZ)]
    for b in range(N_EARLY, N_BLOCK):
        n = last if b == N_BLOCK - 1 else size
        if b == N_BLOCK - 1:
            w_copy_x.wait()
            add_into(total, w_x)
            w_copy_c.start()
            w_store.start()
            w_copy_c.wait_send()
            remote(total, w_out.at[1 - core], last_send.at[1], last_recv.at[1], tp, twin).wait_recv()
            w_store.wait()
            for to in peers:
                remote(mine, small_ref.at[tp], small_send.at[to], small_recv.at[tp], to, dp).start()
            small_here.start()
        x_copy(b, n).wait_recv()
        add_into(part(from_x, b, n), part(s_buf, b, n), 24)
        t_copy(b, n).start()
        t_store(b, n).start()
        for k in range(NZ):
            if b in W_REDUCE[k]:
                pl.when(z == k)(functools.partial(w_reduce, k, W_REDUCE[k][b]))
        if b == N_BLOCK - 2:
            w_copy_x.start()
            every(chip_sum, AHEAD, N_BLOCK)
    for source in peers:
        remote(small_ref.at[source], small_ref.at[source], small_send.at[source], small_recv.at[source], source, dp).wait_recv()
        remote(mine, small_ref.at[tp], small_send.at[source], small_recv.at[tp], source, dp).wait_send()
    small_here.wait()

    def w_done(k):
        for zz in range(NZ):
            line = acc.at[2 * zz + y]
            for slot in (2 * zz + 1 - y, 2 * zz + y):
                remote(p_ref.at[slot, 1 - core], w_c.at[slot], send_c.at[slot], recv_c.at[slot], tp, twin).wait_send()
            remote(line, w_y.at[zz], send_y.at[zz], recv_y.at[zz], partner, dp).wait_send()
            if zz > k:
                remote(line, w_l.at[zz - 1], send_r.at[zz], recv_l.at[zz], tp + 2, dp).wait_send()
            if zz < k:
                remote(line, w_r.at[zz], send_l.at[zz], recv_r.at[zz], tp - 2, dp).wait_send()

    on_position(w_done)

    def drain(b, n):
        t_copy(b, n).wait_send()
        t_store(b, n).wait()
        remote(part(from_x, b, n), t_ref.at[rows(1 - core, b, n), :], g_send_t.at[b], g_recv_t.at[b], tp, twin).wait_recv()

    def sent(b, n):
        c_copy(b, n).wait_send()
        x_copy(b, n).wait_send()

    every(drain, 0, N_BLOCK)
    every(sent, N_EARLY, N_BLOCK)


def tail(g_table, g_rows, look_rows, look_ids, early, collective_id):
    vocab, width = g_table.shape
    rows = g_rows.shape[1]
    half = (rows // 2, width)
    n_look = look_ids.shape[2]
    size = table_block(vocab)
    blocks = lambda n: pltpu.VMEM((n, size, width), F32)
    dma = lambda *n: pltpu.SemaphoreType.DMA(n)
    t, w_sum, small = pl.pallas_call(
        tail_kernel,
        out_shape=(jax.ShapeDtypeStruct((vocab, width), F32), jax.ShapeDtypeStruct((2,) + half, F32), jax.ShapeDtypeStruct((2 * NZ, 24, width), F32)),
        in_specs=[ANY, ANY, ANY, VMEM, ANY],
        out_specs=(ANY,) * 3,
        scratch_shapes=[blocks(N_BLOCK - N_EARLY)] * 2 + [blocks(N_BLOCK), pltpu.VMEM((2, n_look, width), F32), pltpu.VMEM((3, 4 * n_look, width), BF16)]
        + [pltpu.VMEM((2 * NZ,) + half, F32)] * 2 + [pltpu.VMEM((NZ,) + half, F32)] + [pltpu.VMEM((NZ - 1,) + half, F32)] * 2
        + [pltpu.VMEM(half, F32)]
        + [dma(N_BLOCK)] * 8 + [dma(2)]
        + [dma(2 * NZ), pltpu.SemaphoreType.DMA] + [dma(2 * NZ), dma(NZ), dma(NZ), dma(NZ)] * 2 + [dma(2)] * 2 + [dma(2 * NZ)] * 2,
        compiler_params=pltpu.CompilerParams(collective_id=collective_id, has_side_effects=True, vmem_limit_bytes=67000000),
        name="tail",
    )(g_table, g_rows.reshape((2 * NZ, 2) + half), look_rows.reshape(4, n_look, width), look_ids, early)
    return t, w_sum.reshape(rows, width), small


UPDATE_ROWS = 512


def update_kernel(t_ref, w_any, small_any, *refs):
    state = [refs[7 * i:7 * i + 7] for i in range(3)]
    new = [refs[21 + 7 * i:28 + 7 * i] for i in range(3)]
    loss_ref, held, made, w_ref, small_ref = refs[42:47]
    old_small = [refs[47 + 6 * i:53 + 6 * i] for i in range(3)]
    new_small = [refs[65 + 6 * i:71 + 6 * i] for i in range(3)]
    in_sem, out_sem, g_sem, small_in, small_out = refs[83:]
    vocab = t_ref.shape[0]
    blocks = [(at, min(UPDATE_ROWS, vocab - at)) for at in range(0, vocab, UPDATE_ROWS)]

    def loads(q):
        at, n = blocks[q]
        return [pltpu.make_async_copy(ref.at[pl.ds(at, n), :], held.at[q % 3, i, pl.ds(0, n), :], in_sem.at[q % 3, i])
                for i, ref in enumerate((t_ref, state[0][0], state[1][0], state[2][0]))]

    def stores(q):
        at, n = blocks[q]
        return [pltpu.make_async_copy(made.at[q % 2, i, pl.ds(0, n), :], new[i][0].at[pl.ds(at, n), :], out_sem.at[q % 2, i]) for i in range(3)]

    for q in range(3):
        for c in loads(q):
            c.start()
    grads = [pltpu.make_async_copy(w_any, w_ref, g_sem.at[0]), pltpu.make_async_copy(small_any, small_ref, g_sem.at[1])]
    pairs = [(i, j) for i in range(3) for j in range(6)]
    small_loads = grads + [pltpu.make_async_copy(state[i][j + 1], old_small[i][j], small_in.at[i, j]) for i, j in pairs]
    small_stores = [pltpu.make_async_copy(new_small[i][j], new[i][j + 1], small_out.at[i, j]) for i, j in pairs]
    for c in small_loads:
        c.start()

    def small_update(index, grad, *where):
        got = adam_update(old_small[0][index - 1][where], grad, old_small[1][index - 1][where], old_small[2][index - 1][where])
        for i in range(3):
            new_small[i][index - 1][where] = got[i]

    def small_updates():
        hd = old_small[0][2].shape[1]
        n_kv = 2 * hd // small_ref.shape[0]
        n_q, n_f = old_small[0][1].shape[0], old_small[0][5].shape[0]
        small_update(1, small_ref[0, n_kv:n_kv + 2, :], Ellipsis)
        small_update(2, w_ref[0:n_q, :], Ellipsis)
        kv = small_ref[:, 0:n_kv, :].reshape(2 * hd, small_ref.shape[2])
        for i in range(2):
            small_update(3, kv[i * hd:(i + 1) * hd], i)
        small_update(4, w_ref[n_q:2 * n_q, :], Ellipsis)
        for i in range(2):
            small_update(5, w_ref[2 * n_q + i * n_f:2 * n_q + (i + 1) * n_f, :].T, i)
        small_update(6, w_ref[2 * n_q + 2 * n_f:2 * n_q + 3 * n_f, :], Ellipsis)
        loss_ref[...] = jnp.sum(small_ref[0, n_kv + 2:n_kv + 3, :], axis=1, keepdims=True)

    for q, (at, n) in enumerate(blocks):
        for c in loads(q):
            c.wait()
        if q >= 2:
            for c in stores(q - 2):
                c.wait()
        step = 32 if n % 32 == 0 else 16

        def body(j, carry):
            rows = pl.ds(pl.multiple_of(j * step, step), step)
            got = adam_update(held[q % 3, 1, rows, :], held[q % 3, 0, rows, :], held[q % 3, 2, rows, :], held[q % 3, 3, rows, :])
            for i in range(3):
                made[q % 2, i, rows, :] = got[i]
            return carry

        lax.fori_loop(0, n // step, body, 0)
        for c in stores(q):
            c.start()
        if q + 3 < len(blocks):
            for c in loads(q + 3):
                c.start()
        if q == min(3, len(blocks) - 1):
            for c in small_loads:
                c.wait()
            small_updates()
            for c in small_stores:
                c.start()
    for q in range(len(blocks) - 2, len(blocks)):
        for c in stores(q):
            c.wait()
    for c in small_stores:
        c.wait()


def update(g_table, g_shard, g_small, state_arrays):
    width = g_table.shape[1]
    dma = lambda *n: pltpu.SemaphoreType.DMA(n)

    def flip(arrays):
        return [a.swapaxes(-1, -2) if i % 7 in (2, 3) else a for i, a in enumerate(arrays)]

    given = flip(state_arrays)
    small = [pltpu.VMEM(a.shape, F32) for i, a in enumerate(given) if i % 7]
    *new, loss = pl.pallas_call(
        update_kernel,
        out_shape=tuple(jax.ShapeDtypeStruct(a.shape, F32) for a in given) + (jax.ShapeDtypeStruct((1, 1), F32),),
        in_specs=[ANY] * 24,
        out_specs=(ANY,) * 21 + (VMEM,),
        scratch_shapes=[pltpu.VMEM((3, 4, UPDATE_ROWS, width), F32), pltpu.VMEM((2, 3, UPDATE_ROWS, width), F32),
                        pltpu.VMEM(g_shard.shape, F32), pltpu.VMEM(g_small.shape, F32)] + small * 2
        + [dma(3, 4), dma(2, 3), dma(2), dma(3, 6), dma(3, 6)],
        compiler_params=pltpu.CompilerParams(vmem_limit_bytes=60000000),
        name="update",
    )(g_table, g_shard, g_small, *given)
    return flip(new) + [loss]


def norm_fwd(x_f32, scale):
    centered = x_f32 - jnp.mean(x_f32, axis=-1, keepdims=True)
    inv_std = lax.rsqrt(jnp.mean(centered * centered, axis=-1, keepdims=True) + LN_EPS)
    x_hat = centered * inv_std
    return (x_hat * scale).astype(BF16), x_hat, inv_std


def norm_bwd(d_out, x_hat, inv_std, scale):
    d_scale = jnp.sum(d_out * x_hat, axis=0)
    d_hat = d_out * scale
    d_in = inv_std * (d_hat - jnp.mean(d_hat, axis=-1, keepdims=True) - x_hat * jnp.mean(d_hat * x_hat, axis=-1, keepdims=True))
    return d_in, d_scale


def adam_update(param_in, grad_in, mom_in, vel_in):
    mom_new = BETA_ONE * mom_in + (1.0 - BETA_ONE) * grad_in
    vel_new = BETA_TWO * vel_in + (1.0 - BETA_TWO) * grad_in * grad_in
    return param_in - LEARN_RATE * mom_new / (jnp.sqrt(vel_new) + ADAM_EPS), mom_new, vel_new


def dot(spec, a, b):
    return jnp.einsum(spec, a, b, preferred_element_type=F32)


def solution(mesh):
    param_specs = (P('tp', None), P(None, None), P(None, 'tp'), P(None, None, None), P('tp', None), P(None, None, 'tp'), P('tp', None))
    n_tp = mesh.shape['tp']
    n_dp = mesh.shape['dp']

    def local_step(tokens, labels, *state_arrays):
        embed, ln_scales, w_q, w_kv, w_o, w_gu, w_down = state_arrays[0:7]
        batch_loc, seq_len = tokens.shape
        vocab_loc, d_model = embed.shape
        head_dim = w_kv.shape[2]
        q_loc = w_q.shape[1]
        f_loc = w_down.shape[0]
        tok_loc = batch_loc * seq_len
        tok_total = tok_loc * n_dp
        own = tok_loc // n_tp
        tp_rank = lax.axis_index('tp')
        half = tp_rank % 2

        strict = (jnp.arange(own)[:, None] > jnp.arange(own)[None, :]).astype(BF16)

        def routing(chunks):
            shard = chunks // vocab_loc
            row = chunks - shard * vocab_loc
            hot = (shard[:, :, None] == jnp.arange(n_tp)[None, None, :])
            before = dot('rs,nsj->nrj', strict, hot.astype(BF16))
            rank = jnp.sum(jnp.where(hot, before, 0.0), axis=-1).astype(jnp.int32)
            most = jnp.max(jnp.sum(hot.astype(jnp.int32), axis=1))
            return shard, row, rank, (most + CAP - 1) // CAP

        chunks = tokens.reshape(n_tp, own)
        shard, row, rank, rounds = routing(chunks)
        slots = jnp.arange(CAP)
        my_shard = lax.dynamic_index_in_dim(shard, tp_rank, 0, keepdims=False)
        my_rank = lax.dynamic_index_in_dim(rank, tp_rank, 0, keepdims=False)

        def fetch(step):
            here = (shard[:, None, :] == tp_rank) & (rank[:, None, :] == slots[None, :, None] + step * CAP)
            ids = jnp.sum(jnp.where(here, row[:, None, :], 0), axis=-1).reshape(-1)
            place = my_rank - step * CAP
            return ids, jnp.where((place >= 0) & (place < CAP), my_shard * CAP + place, -1)

        def fetch_more(state):
            ids, code = fetch(state[0])
            pick = (code[:, None] == jnp.arange(n_tp * CAP)[None, :]).astype(BF16)
            rows_in = plane_swap(jnp.take(embed, ids, axis=0).reshape(n_tp, CAP, d_model), 1).reshape(n_tp * CAP, d_model).astype(BF16)
            return state[0] + 1, state[1] + dot('rc,cd->rd', pick, rows_in)

        more_rows = lax.while_loop(lambda state: state[0] < rounds, fetch_more, (jnp.int32(1), jnp.zeros((own, d_model), F32)))[1]
        ids_first, code_first = fetch(0)
        code_first = code_first[None, :]

        w_rows = jnp.concatenate([w_q.T, w_o, w_gu.transpose(0, 2, 1).reshape(2 * f_loc, d_model), w_down], axis=0)
        cuts = (q_loc, 2 * q_loc, 2 * q_loc + f_loc, 2 * q_loc + 2 * f_loc)
        wkv_t = w_kv.transpose(0, 2, 1).reshape(2 * head_dim, d_model)
        inv_freq = ROPE_BASE ** (-jnp.arange(0, head_dim, 2).astype(F32) / head_dim)
        angles = inv_freq[:, None] * (half * own + jnp.arange(own)).astype(F32)[None, :]
        cos_t, sin_t = jnp.cos(angles), jnp.sin(angles)
        f_own, x_one, x_zero, *saved = front(ids_first, embed, jnp.broadcast_to(rounds, (1, 128)), code_first, more_rows, w_rows, wkv_t, ln_scales, cos_t, sin_t, n_tp * q_loc, 0)
        saved, (wq_t, wo_b, wg_t, wu_t, wd_b), rounds_all = saved[:5], saved[5:10], jnp.max(saved[10])
        weights = (wq_t, wkv_t, wo_b, wg_t, wu_t, wd_b)

        logit_scale = d_model ** -0.5
        d_fin, g_head_part, log_norm, lab_sum, _ = head(f_own, labels, embed, logit_scale, logit_scale / tok_total, 4)

        def row_ids(step):
            here = (shard[:, None, :] == tp_rank) & (rank[:, None, :] == slots[None, :, None] + step * CAP)
            return jnp.where(jnp.any(here, axis=-1), jnp.sum(jnp.where(here, row[:, None, :], 0), axis=-1), vocab_loc).reshape(-1)

        g_rows, d_zero, rows_back, early, ids_back = layer_bwd(logit_scale, tok_total, d_fin, x_zero, x_one, log_norm, lab_sum, ln_scales, cos_t, sin_t, weights, saved,
                                                               code_first, g_head_part, row_ids(0)[None, :], 7)
        g_table, g_shard, g_small = tail(g_head_part, g_rows, rows_back, ids_back, early, 10)

        def give_back(state):
            mine = (my_shard[None, None, :] == jnp.arange(n_tp)[:, None, None]) & (my_rank[None, None, :] == slots[None, :, None] + state[0] * CAP)
            ids = jnp.sum(jnp.where(mine, jnp.arange(own)[None, None, :], 0), axis=-1).reshape(-1)
            rows_in = plane_swap(jnp.take(d_zero, ids, axis=0).reshape(n_tp, CAP, d_model), 9).reshape(-1, d_model)
            n_rows = n_tp * CAP
            id_rows = jnp.pad(row_ids(state[0]).astype(F32), (0, -n_rows % (8 * d_model))).reshape(-1, d_model)
            both = group_gather(jnp.concatenate([rows_in, id_rows], axis=0), 11)
            ids = both[:, n_rows:].reshape(n_dp, -1)[:, :n_rows].astype(jnp.int32)
            return state[0] + 1, state[1].at[ids.reshape(-1)].add(both[:, :n_rows].reshape(-1, d_model), mode='drop')

        g_table = lax.while_loop(lambda state: state[0] < rounds_all, give_back, (jnp.int32(1), g_table))[1]
        *new, loss = update(g_table, g_shard, g_small, state_arrays)
        return tuple(new) + (loss.reshape(()),)

    return jax.shard_map(local_step, mesh=mesh, in_specs=(P('dp', None), P('dp', None)) + param_specs * 3,
                         out_specs=param_specs * 3 + (P(),), check_vma=False)
```

```python
import functools

import jax
import jax.numpy as jnp
from jax import lax
from jax.experimental import pallas as pl
from jax.experimental.pallas import tpu as pltpu
from jax.sharding import PartitionSpec as P

LN_EPS = 1e-5
LOGIT_ZLOSS = 1e-4
LEARN_RATE = 1e-2
BETA_ONE = 0.9
BETA_TWO = 0.95
ADAM_EPS = 1e-8
ROPE_BASE = 10000.0
NZ = 4
CAP = 96
F32 = jnp.float32
BF16 = jnp.bfloat16
ANY = pl.BlockSpec(memory_space=pl.ANY)
VMEM = pl.BlockSpec(memory_space=pltpu.VMEM)

ARRIVALS = {
    0: (("R", 1), ("R", 2), ("R", 3)),
    1: (("L", 0), ("R", 2), ("R", 3)),
    2: (("R", 3), ("L", 1), ("L", 0)),
    3: (("L", 2), ("L", 1), ("L", 0)),
}
REDUCE_ORDER = {0: (3, 2, 1, 0), 1: (3, 0, 2, 1), 2: (0, 3, 1, 2), 3: (0, 1, 2, 3)}


def remote(src, dst, send_sem, recv_sem, tp, dp):
    return pltpu.make_async_remote_copy(src_ref=src, dst_ref=dst, send_sem=send_sem, recv_sem=recv_sem,
                                        device_id=(tp, dp), device_id_type=pl.DeviceIdType.MESH)


def place():
    tp = lax.axis_index("tp")
    dp = lax.axis_index("dp")
    return tp, dp, tp // 2, tp % 2


def signal(tp, dp):
    pl.semaphore_signal(pltpu.get_barrier_semaphore(), inc=1, device_id=(tp, dp), device_id_type=pl.DeviceIdType.MESH)


def add_into(acc, other, step=None):
    rows = acc.shape[0]
    step = step or (64 if rows % 64 == 0 else 8)

    def body(n, carry):
        at = pl.ds(pl.multiple_of(n * step, step), step)
        acc[at, :] = acc[at, :] + other[at, :]
        return carry

    lax.fori_loop(0, rows // step, body, 0)


def plane_barrier(tp, dp, others):
    peers = [(lax.rem(tp + n, 2 * NZ), dp) for n in range(1, 2 * NZ)] + others
    for peer in peers:
        signal(*peer)
    pl.semaphore_wait(pltpu.get_barrier_semaphore(), len(peers))


def swap_kernel(x_ref, out_ref, own_sem, send, recv):
    tp, dp, _, _ = place()
    plane_barrier(tp, dp, [])
    copies = []
    for n in range(1, 2 * NZ):
        to = lax.rem(tp + n, 2 * NZ)
        copy = remote(x_ref.at[to], out_ref.at[tp], send.at[to], recv.at[tp], to, dp)
        copy.start()
        copies.append(copy)
    own = pltpu.make_async_copy(x_ref.at[tp], out_ref.at[tp], own_sem)
    own.start()
    for n in range(1, 2 * NZ):
        source = lax.rem(tp + n, 2 * NZ)
        remote(out_ref.at[source], out_ref.at[source], send.at[source], recv.at[source], source, dp).wait_recv()
    own.wait()
    for copy in copies:
        copy.wait_send()


def plane_swap(x, collective_id):
    return pl.pallas_call(
        swap_kernel,
        out_shape=jax.ShapeDtypeStruct(x.shape, x.dtype),
        in_specs=[ANY],
        out_specs=ANY,
        scratch_shapes=[pltpu.SemaphoreType.DMA] + [pltpu.SemaphoreType.DMA((2 * NZ,))] * 2,
        compiler_params=pltpu.CompilerParams(collective_id=collective_id, has_side_effects=True),
        name="plane_swap",
    )(x)


def group_kernel(x_ref, out_ref, own_sem, send, recv):
    tp, dp, _, _ = place()
    group = [lax.rem(dp + n, 4) for n in range(1, 4)]
    for to in group:
        signal(tp, to)
    pl.semaphore_wait(pltpu.get_barrier_semaphore(), 3)
    own = pltpu.make_async_copy(x_ref, out_ref.at[dp], own_sem)
    own.start()
    for n, to in enumerate(group):
        remote(x_ref, out_ref.at[dp], send.at[n], recv.at[dp], tp, to).start()
    own.wait()
    for n, to in enumerate(group):
        remote(x_ref, out_ref.at[to], send.at[n], recv.at[to], tp, to).wait_recv()
        remote(x_ref, out_ref.at[dp], send.at[n], recv.at[dp], tp, to).wait_send()


def group_gather(x, collective_id):
    return pl.pallas_call(
        group_kernel,
        out_shape=jax.ShapeDtypeStruct((4,) + x.shape, x.dtype),
        in_specs=[ANY],
        out_specs=ANY,
        scratch_shapes=[pltpu.SemaphoreType.DMA, pltpu.SemaphoreType.DMA((3,)), pltpu.SemaphoreType.DMA((4,))],
        compiler_params=pltpu.CompilerParams(collective_id=collective_id, has_side_effects=True),
        name="group_gather",
    )(x)


GATHER_ORDER = {
    0: ((0, 0), (0, 1), (1, 0), (0, 2), (1, 1), (0, 3), (1, 2), (1, 3)),
    1: ((0, 1), (0, 0), (0, 2), (1, 1), (1, 0), (0, 3), (1, 2), (1, 3)),
    2: ((0, 2), (0, 1), (0, 3), (1, 2), (0, 0), (1, 3), (1, 1), (1, 0)),
    3: ((0, 3), (0, 2), (1, 3), (0, 1), (1, 2), (0, 0), (1, 1), (1, 0)),
}
GATHER_EVENTS = {
    0: {
        1: ((0, 1, 0, 'y'), (1, 0, 1, 'r'), (0, 1, 1, 'y'), (1, 0, 0, '')),
        3: ((0, 2, 0, 'y'), (1, 1, 0, ''), (0, 2, 1, 'y'), (1, 1, 1, '')),
        5: ((0, 3, 0, 'y'), (1, 2, 0, ''), (0, 3, 1, ''), (1, 2, 1, '')),
        7: ((1, 3, 0, ''), (1, 3, 1, '')),
    },
    1: {
        1: ((0, 0, 0, 'ry'), (0, 2, 0, 'ly'), (1, 1, 0, ''), (0, 0, 1, 'r'), (0, 2, 1, 'ly'), (1, 1, 1, '')),
        4: ((0, 3, 0, 'ly'), (1, 0, 0, ''), (1, 0, 1, 'r')),
        5: ((0, 3, 1, 'l'), (1, 2, 0, '')),
        6: ((1, 2, 1, ''), (1, 3, 1, 'l')),
        7: ((1, 3, 0, ''),),
    },
    2: {
        1: ((0, 1, 0, 'ry'), (0, 3, 0, 'ly'), (1, 2, 0, ''), (0, 1, 1, 'ry'), (0, 3, 1, 'l'), (1, 2, 1, '')),
        4: ((0, 0, 0, 'ry'), (1, 1, 0, ''), (1, 3, 1, 'l'), (0, 0, 1, 'r'), (1, 3, 0, '')),
        6: ((1, 0, 1, 'r'), (1, 1, 1, '')),
        7: ((1, 0, 0, ''),),
    },
    3: {
        1: ((0, 2, 0, 'y'), (1, 3, 1, 'l'), (0, 2, 1, 'y'), (1, 3, 0, '')),
        3: ((0, 1, 0, 'y'), (1, 2, 0, ''), (0, 1, 1, 'y'), (1, 2, 1, '')),
        5: ((0, 0, 0, 'y'), (1, 1, 0, ''), (0, 0, 1, ''), (1, 1, 1, '')),
        7: ((1, 0, 0, ''), (1, 0, 1, '')),
    },
}
SCATTER_ORDER = {
    0: ((1, 3), (1, 2), (0, 3), (1, 1), (0, 2), (1, 0), (0, 1), (0, 0)),
    1: ((1, 3), (1, 2), (0, 3), (1, 0), (1, 1), (0, 2), (0, 0), (0, 1)),
    2: ((1, 0), (1, 1), (1, 3), (0, 0), (1, 2), (0, 3), (0, 1), (0, 2)),
    3: ((1, 0), (1, 1), (0, 0), (1, 2), (0, 1), (1, 3), (0, 2), (0, 3)),
}
SCATTER_EVENTS = {
    0: {
        0: ((1, 3, 0, '', 'y'), (1, 3, 1, '', 'r')),
        1: ((1, 2, 0, '', 'y'), (1, 2, 1, '', 'y')),
        2: ((0, 3, 1, '', 'r'), (0, 3, 0, 'y', 'r')),
        3: ((1, 1, 0, '', 'y'), (1, 1, 1, '', 'y')),
        4: ((0, 2, 0, 'y', 'r'),),
        5: ((0, 2, 1, 'y', 'r'), (1, 0, 0, '', 'y')),
        6: ((1, 0, 1, 'r', 'y'), (0, 1, 0, 'y', 'r')),
        7: ((0, 1, 1, 'y', 'r'), (0, 0, 0, 'ry', ''), (0, 0, 1, 'ry', '')),
    },
    1: {
        0: ((1, 3, 0, '', 'y'),),
        1: ((1, 2, 0, '', 'y'), (1, 2, 1, '', 'y')),
        2: ((1, 3, 1, 'l', 'r'),),
        3: ((1, 0, 0, '', 'y'),),
        4: ((0, 3, 1, 'l', 'r'), (1, 0, 1, 'r', 'l'), (1, 1, 0, '', 'y'), (1, 1, 1, '', 'y')),
        6: ((0, 3, 0, 'ly', 'r'), (0, 0, 1, 'r', 'l')),
        7: ((0, 2, 0, 'ly', 'r'), (0, 0, 0, 'ry', 'l'), (0, 2, 1, 'ly', 'r'), (0, 1, 0, 'lry', ''), (0, 1, 1, 'lry', '')),
    },
    2: {
        0: ((1, 0, 0, '', 'y'),),
        1: ((1, 1, 0, '', 'y'), (1, 1, 1, '', 'y')),
        2: ((1, 0, 1, 'r', 'l'), (1, 3, 0, '', 'y')),
        4: ((1, 3, 1, 'l', 'r'), (0, 0, 1, 'r', 'l'), (1, 2, 0, '', 'y'), (1, 2, 1, '', 'y')),
        6: ((0, 0, 0, 'ry', 'l'), (0, 3, 1, 'l', 'r')),
        7: ((0, 1, 0, 'ry', 'l'), (0, 3, 0, 'ly', 'r'), (0, 1, 1, 'ry', 'l'), (0, 2, 0, 'lry', ''), (0, 2, 1, 'lry', '')),
    },
    3: {
        0: ((1, 0, 0, '', 'y'), (1, 0, 1, '', 'l')),
        1: ((1, 1, 0, '', 'y'), (1, 1, 1, '', 'y')),
        2: ((0, 0, 1, '', 'l'), (0, 0, 0, 'y', 'l')),
        3: ((1, 2, 0, '', 'y'), (1, 2, 1, '', 'y')),
        4: ((0, 1, 0, 'y', 'l'),),
        5: ((0, 1, 1, 'y', 'l'), (1, 3, 0, '', 'y')),
        6: ((1, 3, 1, 'l', 'y'), (0, 2, 0, 'y', 'l')),
        7: ((0, 2, 1, 'y', 'l'), (0, 3, 0, 'ly', ''), (0, 3, 1, 'ly', '')),
    },
}
SUB = 256
GROUP = 6


def lookup(table, z, step):
    value = jnp.int32(0)
    for k in range(NZ):
        for s in range(2 * NZ):
            value = value + jnp.where((z == k) & (step == s), table[k][s], 0)
    return value


def head_kernel(scale, token_scale, f_ref, lab_ref, e_ref, dfin_ref, ghead_ref, norm_ref, labsum_ref, z_ref,
                e_b, e_t, fbuf, f_b, g_acc, from_y, from_l, from_r, dl, z_buf, z_rest, lse_all, z_sem, load_sem, ag_send, ag_recv,
                send_y, send_l, send_r, recv_y, recv_l, recv_r, st_send, st_recv):
    tp, dp, z, y = place()
    partner = tp + 1 - 2 * y
    vocab, width = e_ref.shape
    own = f_ref.shape[0]
    whole = vocab // (SUB * GROUP)
    rest = vocab - whole * SUB * GROUP
    log2e = 1.4426950408889634
    slope = scale * log2e
    blocks = [(j * SUB, SUB) for j in range(GROUP)]
    tail = [(n, min(SUB, rest - n)) for n in range(0, rest, SUB)]

    plane_barrier(tp, dp, [])

    half = own // 2
    to_tp = {"l": tp - 2, "r": tp + 2, "y": partner}

    def slot_of(o, zz):
        return 2 * zz + (1 - y if o else y)

    def piece(ref, h):
        return ref.at[pl.ds(h * half, half), :]

    def pass_on(o, zz, h, to, own_chunk=False):
        slot = slot_of(o, zz)
        return remote(piece(f_ref if own_chunk else fbuf.at[slot], h), piece(fbuf.at[slot], h), ag_send.at["lry".index(to), slot, h],
                      ag_recv.at[slot, h], to_tp[to], dp)

    def arrived(o, zz, h):
        slot = slot_of(o, zz)
        remote(piece(f_ref, h), piece(fbuf.at[slot], h), ag_send.at[0, slot, h], ag_recv.at[slot, h], partner, dp).wait_recv()

    def own_sends(k):
        first = (1, 0) if k in (0, NZ - 1) else (0, 1)
        return [pass_on(0, k, h, "y", True) for h in first] + [
            pass_on(0, k, h, to, True) for h in range(2) for to in ("l" if k > 0 else "") + ("r" if k < NZ - 1 else "")]

    def on_position(f):
        for k in range(NZ):
            pl.when(z == k)(functools.partial(f, k))

    def first_sends(k):
        for c in own_sends(k):
            c.start()

    on_position(first_sends)
    load = pltpu.make_async_copy(e_ref, g_acc, load_sem.at[0])
    load.start()
    own_copy = pltpu.make_async_copy(f_ref, fbuf.at[tp], load_sem.at[1])
    own_copy.start()
    load.wait()

    def prepare(at, size):
        part = g_acc[at, :]
        e_b[at, :] = part.astype(BF16)
        e_t[:, at] = part.T.astype(BF16)

    def prepare_body(n, carry):
        prepare(pl.ds(pl.multiple_of(n * SUB, SUB), SUB), SUB)
        return carry

    lax.fori_loop(0, vocab // SUB, prepare_body, 0)
    if vocab % SUB:
        prepare(pl.ds(vocab // SUB * SUB, vocab % SUB), vocab % SUB)
    own_copy.wait()

    big = SUB * GROUP

    def z_copies(slot, n, out):
        if n is None:
            pair = (z_rest, z_ref.at[slot, pl.ds(whole * big, rest), :])
            sem = z_sem.at[2]
        else:
            pair = (z_buf.at[lax.rem(n, 2)], z_ref.at[slot, pl.ds(pl.multiple_of(n * big, big), big), :])
            sem = z_sem.at[lax.rem(n, 2)]
        return pltpu.make_async_copy(*(pair if out else pair[::-1]), sem)

    def slot_at(order, step):
        code = lookup({k: [2 * zz + o for o, zz in order[k]] for k in range(NZ)}, z, step)
        other = code % 2
        return code // 2 * 2 + y + other - 2 * y * other

    def gather_step(step, carry):
        for k in range(NZ):
            for at, events in GATHER_EVENTS[k].items():
                def serve(events=events):
                    for o, zz, h, to in events:
                        arrived(o, zz, h)
                        for t in to:
                            pass_on(o, zz, h, t).start()
                pl.when((z == k) & (step == at))(serve)
        slot = slot_at(GATHER_ORDER, step)
        f_b[slot] = fbuf[slot].astype(BF16)
        f_now = f_b[slot]

        def group(base, parts, kept, c):
            top, total = c
            for first, size in parts:
                logit = lax.dot_general(e_b[pl.ds(base + first, size), :], f_now, (((1,), (1,)), ((), ())), preferred_element_type=F32)
                kept[pl.ds(first, size), :] = logit
                logit = logit.reshape(size // 8, 8, own)
                new = jnp.maximum(top, jnp.max(logit, axis=0))
                total = total * jnp.exp2((top - new) * slope) + jnp.sum(jnp.exp2((logit - new[None]) * slope), axis=0)
                top = new
            return top, total

        def body(n, c):
            @pl.when(step * whole + n >= 2)
            def _():
                z_copies(slot, n, True).wait()
            c = group(pl.multiple_of(n * big, big), blocks, z_buf.at[lax.rem(n, 2)], c)
            z_copies(slot, n, True).start()
            return c

        top, total = lax.fori_loop(0, whole, body, (jnp.full((8, own), -3e38, F32), jnp.zeros((8, own), F32)))
        if tail:
            @pl.when(step > 0)
            def _():
                z_copies(slot, None, True).wait()
            top, total = group(whole * big, tail, z_rest, (top, total))
            z_copies(slot, None, True).start()
        most = jnp.max(top, axis=0, keepdims=True)
        total = jnp.sum(total * jnp.exp2((top - most) * slope), axis=0, keepdims=True)
        lse_all[tp, pl.ds(slot, 1), :] = most * scale + jnp.log(total)
        return carry

    lax.fori_loop(0, 2 * NZ, gather_step, 0)
    for n in range(2):
        z_copies(0, jnp.int32(n), True).wait()
    if tail:
        z_copies(0, None, True).wait()

    for n in range(1, 2 * NZ):
        to = lax.rem(tp + n, 2 * NZ)
        remote(lse_all.at[tp], lse_all.at[tp], st_send.at[to], st_recv.at[tp], to, dp).start()

    def gathers_done(k):
        for c in own_sends(k):
            c.wait_send()
        for events in GATHER_EVENTS[k].values():
            for o, zz, h, to in events:
                for t in to:
                    pass_on(o, zz, h, t).wait_send()

    on_position(gathers_done)
    start_slot = slot_at(SCATTER_ORDER, 0)
    for n in range(2):
        z_copies(start_slot, jnp.int32(n), False).start()
    if tail:
        z_copies(start_slot, None, False).start()

    def clear(n, carry):
        g_acc[pl.ds(pl.multiple_of(n * 16, 16), 16), :] = jnp.zeros((16, width), F32)
        return carry

    lax.fori_loop(0, vocab // 16, clear, 0)
    for n in range(1, 2 * NZ):
        source = lax.rem(tp + n, 2 * NZ)
        remote(lse_all.at[source], lse_all.at[source], st_send.at[source], st_recv.at[source], source, dp).wait_recv()
    peak = jnp.max(lse_all[...], axis=0)
    log_norm = peak + jnp.log(jnp.sum(jnp.exp(lse_all[...] - peak[None]), axis=0))
    norm_ref[...] = log_norm

    def leave(o, zz, h, to):
        src = piece(fbuf.at[slot_of(o, zz)], h)
        if to == "y":
            at = 2 * zz + h
            return remote(src, from_y.at[at], send_y.at[at], recv_y.at[at], partner, dp)
        if to == "l":
            at = 6 if o else 2 * zz + h
            return remote(src, from_r.at[at], send_l.at[at], recv_r.at[at], tp - 2, dp)
        at = 6 if o else 2 * zz - 2 + h
        return remote(src, from_l.at[at], send_r.at[at], recv_l.at[at], tp + 2, dp)

    def collect(o, zz, h, sums, to):
        here = piece(fbuf.at[slot_of(o, zz)], h)
        for d in sums:
            at, buf, sem = {"y": (2 * zz + h, from_y, recv_y), "l": (6 if o else 2 * zz - 2 + h, from_l, recv_l),
                            "r": (6 if o else 2 * zz + h, from_r, recv_r)}[d]
            remote(here, buf.at[at], send_y.at[0], sem.at[at], partner, dp).wait_recv()
            add_into(here, buf.at[at])
        if to:
            leave(o, zz, h, to).start()

    def scatter_step(step, lab_sum):
        slot = slot_at(SCATTER_ORDER, step)
        f_now = f_b[slot]
        acc = fbuf.at[slot]
        norm = norm_ref[pl.ds(slot, 1), :]
        shift = norm * log2e
        coef = (1.0 + 2.0 * LOGIT_ZLOSS * norm) * token_scale
        lab = lab_ref[pl.ds(slot // 2, 1), pl.ds(pl.multiple_of(lax.rem(slot, 2) * own, own), own)] - tp * vocab
        acc[...] = jnp.zeros((width, own), F32)

        def group(base, parts, kept, hits):
            for first, size in parts:
                at = pl.ds(base + first, size)
                logit = kept[pl.ds(first, size), :]
                hit = lax.broadcasted_iota(jnp.int32, (size, own), 0) == lab - (base + first)
                prob = jnp.exp2(logit * slope - shift) * coef
                grad = jnp.where(hit, prob - token_scale, prob).astype(BF16)
                hits = hits + jnp.sum(jnp.where(hit, logit, 0.0).reshape(size // 8, 8, own), axis=0)
                dl[pl.ds(first, size), :] = grad
                g_acc[at, :] += jnp.dot(grad, f_now, preferred_element_type=F32)
            size = parts[-1][0] + parts[-1][1]
            acc[...] += jnp.dot(e_t[:, pl.ds(base, size)], dl[pl.ds(0, size), :], preferred_element_type=F32)
            return hits

        following = slot_at(SCATTER_ORDER, jnp.minimum(step + 1, 2 * NZ - 1))

        def body(n, hits):
            z_copies(slot, n, False).wait()
            hits = group(pl.multiple_of(n * big, big), blocks, z_buf.at[lax.rem(n, 2)], hits)

            @pl.when(n + 2 < whole)
            def _():
                z_copies(slot, n + 2, False).start()

            @pl.when((n + 2 >= whole) & (step + 1 < 2 * NZ))
            def _():
                z_copies(following, n + 2 - whole, False).start()
            return hits

        lab_sum = lax.fori_loop(0, whole, body, lab_sum)
        if tail:
            z_copies(slot, None, False).wait()
            lab_sum = group(whole * big, tail, z_rest, lab_sum)

            @pl.when(step + 1 < 2 * NZ)
            def _():
                z_copies(following, None, False).start()

        for k in range(NZ):
            for at, events in SCATTER_EVENTS[k].items():
                def reduce(events=events):
                    for event in events:
                        collect(*event)
                pl.when((z == k) & (step == at))(reduce)
        return lab_sum

    lab_sum = lax.fori_loop(0, 2 * NZ, scatter_step, jnp.zeros((8, own), F32))
    labsum_ref[...] = lab_sum
    store = pltpu.make_async_copy(g_acc, ghead_ref, load_sem.at[0])
    store.start()
    dfin_ref[...] = fbuf[tp].T

    def scatters_done(k):
        for events in SCATTER_EVENTS[k].values():
            for o, zz, h, _, to in events:
                if to:
                    leave(o, zz, h, to).wait_send()

    on_position(scatters_done)
    for n in range(1, 2 * NZ):
        to = lax.rem(tp + n, 2 * NZ)
        remote(lse_all.at[tp], lse_all.at[tp], st_send.at[to], st_recv.at[tp], to, dp).wait_send()
    store.wait()


def head(f_own, labels, embed, scale, token_scale, collective_id):
    own, width = f_own.shape
    vocab = embed.shape[0]
    chunk = (own, width)
    strips = lambda n: pltpu.VMEM((n, own // 2, width), F32)
    dma = lambda *n: pltpu.SemaphoreType.DMA(n)
    return pl.pallas_call(
        functools.partial(head_kernel, scale, token_scale),
        out_shape=(jax.ShapeDtypeStruct((own, width), F32), jax.ShapeDtypeStruct((vocab, width), F32),
                   jax.ShapeDtypeStruct((2 * NZ, own), F32), jax.ShapeDtypeStruct((8, own), F32),
                   jax.ShapeDtypeStruct((2 * NZ, vocab, own), F32)),
        in_specs=[VMEM, VMEM, ANY],
        out_specs=(VMEM, ANY, VMEM, VMEM, ANY),
        scratch_shapes=[pltpu.VMEM((vocab, width), BF16), pltpu.VMEM((width, vocab), BF16),
                        pltpu.VMEM((2 * NZ,) + chunk, F32), pltpu.VMEM((2 * NZ,) + chunk, BF16), pltpu.VMEM((vocab, width), F32),
                        strips(8), strips(7), strips(7),
                        pltpu.VMEM((SUB * GROUP, own), BF16), pltpu.VMEM((2, SUB * GROUP, own), F32),
                        pltpu.VMEM((max(vocab % (SUB * GROUP), 8), own), F32), pltpu.VMEM((2 * NZ, 2 * NZ, own), F32),
                        dma(3), dma(2), dma(3, 2 * NZ, 2), dma(2 * NZ, 2), dma(8), dma(7), dma(7), dma(8), dma(7), dma(7), dma(2 * NZ), dma(2 * NZ)],
        compiler_params=pltpu.CompilerParams(collective_id=collective_id, has_side_effects=True, vmem_limit_bytes=67000000),
        cost_estimate=pl.CostEstimate(flops=8 * vocab * width * own * 8, bytes_accessed=3 * 4 * vocab * width, transcendentals=2 * vocab * own * 8),
        name="head",
    )(f_own, labels, embed)


TB = (((1,), (1,)), ((), ()))
TA = (((0,), (0,)), ((), ()))
LOG2E = 1.4426950408889634


def mm(a, b, dims=(((1,), (0,)), ((), ()))):
    return lax.dot_general(a, b, dims, preferred_element_type=F32)


def picks(code, n_slots):
    return (lax.broadcasted_iota(jnp.int32, (n_slots, code.shape[1]), 0) == code).astype(F32).astype(BF16)


def turn(lo, hi, cos_t, sin_t):
    return lo * cos_t - hi * sin_t, hi * cos_t + lo * sin_t


EVENTS = {
    0: (((("R", 1),), (0,)), ((("R", 2),), (1,)), ((("R", 3),), (2,)), ((), (3,))),
    1: (((("L", 0), ("R", 2)), (1,)), ((("R", 3),), (0,)), ((), (2,)), ((), (3,))),
    2: (((("R", 3), ("L", 1)), (2,)), ((("L", 0),), (3,)), ((), (1,)), ((), (0,))),
    3: (((("L", 2),), (3,)), ((("L", 1),), (2,)), ((("L", 0),), (1,)), ((), (0,))),
}
MLP_ORDER = {k: [2 * k] + [code for line, other in EVENTS[k] for code in [2 * zz for _, zz in line] + [2 * zz + 1 for zz in other]] for k in range(NZ)}


def front_kernel(ids_ref, e_ref, rounds_ref, code_ref, extra_ref, w_ref, wkv_ref, ln_ref, cos_ref, sin_ref,
                 f_ref, x1_ref, x0_ref, q_ref, kv_ref, kvt_ref, lse_ref, ctx_ref, wq_ref, wo_ref, wg_out, wu_out, wd_out, rounds_all,
                 wg_ref, wu_ref, wd_ref, w_sem, table, rows_ref, wl, rows_in, u_b, kv_out, kv_in, own_sem, r_send, r_recv, a_y, a_l, a_r, a_c, a_recv,
                 b_y, b_l, b_r, b_x, b_c, b_recv, kv_send, kv_recv, n_send, n_recv):
    tp, dp, z, y = place()
    partner = tp + 1 - 2 * y
    core = dp % 2
    twin = dp + 1 - 2 * core
    facing = lax.rem(dp + 2, 4)
    own, width = x0_ref.shape
    shards, w_rows = wl.shape[0], wl.shape[1]
    nq = q_ref.shape[0]
    ff = wg_out.shape[0]
    n_a = nq // shards
    n_f = ff // shards
    n_b = 3 * n_f // 4
    hd = kv_out.shape[0] // 2
    quarter = hd // 2
    heads = nq // hd

    def a_rows(c):
        return pl.ds(pl.multiple_of(c * n_a, 8), n_a)

    def b_rows(d):
        return pl.ds(pl.multiple_of(2 * n_a + d * n_b, 8), n_b)

    def a_copy(slot, sems, to, to_dp, first=False):
        src = w_ref.at[a_rows(core), :] if first else wl.at[slot, a_rows(core), :]
        return remote(src, wl.at[slot, a_rows(core), :], sems.at[slot], a_recv.at[slot, core], to, to_dp)

    def b_copy(slot, piece, sems, to, to_dp, first=False):
        src = w_ref.at[b_rows(piece), :] if first else wl.at[slot, b_rows(piece), :]
        return remote(src, wl.at[slot, b_rows(piece), :], sems.at[slot], b_recv.at[slot, piece], to, to_dp)

    def a_wait(slot, c):
        remote(w_ref.at[a_rows(c), :], wl.at[slot, a_rows(c), :], a_y.at[slot], a_recv.at[slot, c], partner, dp).wait_recv()

    def b_wait(slot, piece):
        remote(w_ref.at[b_rows(piece), :], wl.at[slot, b_rows(piece), :], b_y.at[slot], b_recv.at[slot, piece], partner, dp).wait_recv()

    def on_position(f):
        for k in range(NZ):
            pl.when(z == k)(functools.partial(f, k))

    def line_sends(k, make, y_sems, l_sems, r_sems, slot, side, first=False):
        sends = [make(slot, y_sems, partner, dp, first)]
        if k > 0 and side != "L":
            sends.append(make(slot, l_sems, tp - 2, dp, first))
        if k < NZ - 1 and side != "R":
            sends.append(make(slot, r_sems, tp + 2, dp, first))
        return sends

    def b_own(slot, sems, to, to_dp, first=False):
        return b_copy(slot, dp, sems, to, to_dp, first)

    def a_sends(k, slot, side, first=False):
        return line_sends(k, a_copy, a_y, a_l, a_r, slot, side, first)

    def b_sends(k, slot, side, first=False):
        return line_sends(k, b_own, b_y, b_l, b_r, slot, side, first)

    def start(copies):
        for c in copies:
            c.start()

    load = pltpu.make_async_copy(e_ref, table, own_sem.at[2])
    load.start()
    group = [twin, facing, lax.rem(twin + 2, 4)]
    plane_barrier(tp, dp, [(tp, d) for d in group])
    peers = [lax.rem(tp + n, shards) for n in range(1, shards)]

    def rounds_copy(n):
        return remote(rounds_ref, rounds_all.at[dp], n_send.at[n], n_recv.at[dp], tp, group[n])

    for n in range(3):
        rounds_copy(n).start()
    rounds_all[dp] = rounds_ref[...]

    def row_copy(to):
        return remote(rows_ref.at[to], rows_in.at[tp], r_send.at[to], r_recv.at[tp], to, dp)

    on_position(lambda k: start(b_sends(k, tp, "", True)))
    on_position(lambda k: start(a_sends(k, tp, "", True)))
    own_w = pltpu.make_async_copy(w_ref, wl.at[tp], own_sem.at[1])
    own_w.start()

    def a_event(t, k):
        line, other = EVENTS[k][t]
        for side, zz in line:
            slot = 2 * zz + y
            a_wait(slot, core)
            start(a_sends(k, slot, side))
            a_copy(slot, a_c, tp, twin).start()
        for zz in other:
            slot = 2 * zz + 1 - y
            a_wait(slot, core)
            a_copy(slot, a_c, tp, twin).start()

    def b_event(t, k):
        line, other = EVENTS[k][t]
        for side, zz in line:
            slot = 2 * zz + y
            b_wait(slot, dp)
            start(b_sends(k, slot, side))
            b_copy(slot, dp, b_x, tp, facing).start()
            b_copy(slot, dp, b_c.at[0], tp, twin).start()
        for zz in other:
            slot = 2 * zz + 1 - y
            b_wait(slot, dp)
            b_copy(slot, dp, b_x, tp, facing).start()
            b_copy(slot, dp, b_c.at[0], tp, twin).start()

    load.wait()
    cap = rows_ref.shape[1]

    def pick_rows(n, carry):
        for i in range(8):
            rows_ref[n // (cap // 8), pl.ds(lax.rem(n, cap // 8) * 8 + i, 1), :] = table[pl.ds(ids_ref[n * 8 + i], 1), :]
        return carry

    lax.fori_loop(0, shards * cap // 8, pick_rows, 0)
    start([row_copy(to) for to in peers])
    own_rows = pltpu.make_async_copy(rows_ref.at[tp], rows_in.at[tp], own_sem.at[0])
    own_rows.start()
    on_position(functools.partial(b_event, 0))
    on_position(functools.partial(a_event, 0))
    on_position(functools.partial(b_event, 1))
    on_position(functools.partial(a_event, 1))
    own_rows.wait()
    for source in peers:
        remote(rows_ref.at[source], rows_in.at[source], r_send.at[source], r_recv.at[source], source, dp).wait_recv()
    n_slots = shards * cap
    x0_ref[...] = extra_ref[...] + mm(picks(code_ref[...], n_slots), rows_in[...].reshape(n_slots, width).astype(BF16), TA)
    u_b[...] = norm_fwd(x0_ref[...], ln_ref[0:1, :])[0]
    x1_ref[...] = x0_ref[...]
    cos_t = cos_ref[...]
    sin_t = sin_ref[...]
    kv = mm(wkv_ref[...].reshape(2 * hd, width).astype(BF16), u_b[...], TB)
    lo, hi = turn(kv[:quarter], kv[quarter:hd], cos_t, sin_t)
    kv_out[0:quarter, :] = lo
    kv_out[quarter:hd, :] = hi
    kv_out[hd:, :] = kv[hd:]
    kv_copy = remote(kv_out, kv_in, kv_send, kv_recv, partner, dp)
    kv_copy.start()

    def slot_of(step):
        code = lookup(MLP_ORDER, z, step)
        other = code % 2
        return code // 2 * 2 + y + other - 2 * y * other

    def w_stores(slot):
        at = pl.ds(pl.multiple_of(slot * n_f, n_f), n_f)
        return [pltpu.make_async_copy(src.at[at, :], dst.at[at, :], w_sem.at[i, slot])
                for i, (src, dst) in enumerate(((wg_ref, wg_out), (wu_ref, wu_out), (wd_ref, wd_out)))]

    def mlp(step, carry):
        def pass_on():
            slot = slot_of(step + 1)
            b_wait(slot, facing)
            b_copy(slot, facing, b_c.at[1], tp, twin).start()
        pl.when(step < shards - 1)(pass_on)
        slot = slot_of(step)

        def rest():
            b_wait(slot, twin)
            b_wait(slot, lax.rem(twin + 2, 4))
        pl.when(step > 0)(rest)
        at = pl.ds(pl.multiple_of(slot * n_f, n_f), n_f)
        wg_ref[at, :] = wl[slot, 2 * n_a:2 * n_a + n_f, :].astype(BF16)
        wu_ref[at, :] = wl[slot, 2 * n_a + n_f:2 * n_a + 2 * n_f, :].astype(BF16)
        wd_ref[at, :] = wl[slot, 2 * n_a + 2 * n_f:2 * n_a + 3 * n_f, :].astype(BF16)
        for c in w_stores(slot):
            c.start()
        gate = mm(u_b[...], wg_ref[at, :], TB)
        up = mm(u_b[...], wu_ref[at, :], TB)
        x1_ref[...] += mm((gate * jax.nn.sigmoid(gate) * up).astype(BF16), wd_ref[at, :])
        return carry

    own_w.wait()
    lax.fori_loop(0, 3, mlp, 0)
    on_position(functools.partial(b_event, 2))
    on_position(functools.partial(a_event, 2))
    lax.fori_loop(3, 4, mlp, 0)
    on_position(functools.partial(a_event, 3))
    on_position(functools.partial(b_event, 3))
    for source in peers:
        a_wait(source, 1 - core)
    for s in range(shards):
        wq_ref[s * n_a:(s + 1) * n_a, :] = wl[s, 0:n_a, :].astype(BF16)
        wo_ref[s * n_a:(s + 1) * n_a, :] = wl[s, n_a:2 * n_a, :].astype(BF16)

    q_all = mm(wq_ref[...], u_b[...], TB)
    for h in range(heads):
        lo, hi = turn(q_all[h * hd:h * hd + quarter], q_all[h * hd + quarter:(h + 1) * hd], cos_t, sin_t)
        q_ref[h * hd:h * hd + quarter, :] = lo.astype(BF16)
        q_ref[h * hd + quarter:(h + 1) * hd, :] = hi.astype(BF16)
    kv_copy.wait()

    def fill(mine, other):
        kv_ref[mine * own:(mine + 1) * own, :] = kv_out[...].T.astype(BF16)
        kv_ref[other * own:(other + 1) * own, :] = kv_in[...].T.astype(BF16)
        kvt_ref[:, mine * own:(mine + 1) * own] = kv_out[...].astype(BF16)
        kvt_ref[:, other * own:(other + 1) * own] = kv_in[...].astype(BF16)

    pl.when(y == 0)(lambda: fill(0, 1))
    pl.when(y == 1)(lambda: fill(1, 0))
    blank = jnp.zeros((hd, own), BF16)
    slope = hd ** -0.5 * LOG2E

    def attend(h, carry):
        at = pl.ds(pl.multiple_of(h * hd, hd), hd)
        scores = mm(kv_ref[...], jnp.concatenate([q_ref[at, :], blank], axis=0))
        allowed = lax.broadcasted_iota(jnp.int32, scores.shape, 0) <= lax.broadcasted_iota(jnp.int32, scores.shape, 1) + y * own
        scores = jnp.where(allowed, scores * slope, -1e30)
        top = jnp.max(scores, axis=0, keepdims=True)
        prob = jnp.exp2(scores - top)
        total = jnp.sum(prob, axis=0, keepdims=True)
        lse_ref[pl.ds(h, 1), :] = top + jnp.log2(total)
        ctx_ref[at, :] = mm(kvt_ref[hd:, :], (prob * (1.0 / total)).astype(BF16)).astype(BF16)
        return carry

    lax.fori_loop(0, heads, attend, 0)
    x1_ref[...] += mm(ctx_ref[...], wo_ref[...], TA)

    lax.fori_loop(4, shards, mlp, 0)
    f_ref[...] = norm_fwd(x1_ref[...], ln_ref[1:2, :])[0].astype(F32)

    def finish(k):
        done = a_sends(k, tp, "", True) + b_sends(k, tp, "", True)
        for line, other in EVENTS[k]:
            for side, zz in line:
                done += a_sends(k, 2 * zz + y, side) + b_sends(k, 2 * zz + y, side)
        for c in done:
            c.wait_send()

    on_position(finish)
    for slot in range(shards):
        for c in w_stores(slot):
            c.wait()
    for n in range(3):
        rounds_copy(n).wait_send()
        remote(rounds_ref, rounds_all.at[group[n]], n_send.at[n], n_recv.at[group[n]], tp, twin).wait_recv()
    for to in peers:
        row_copy(to).wait_send()
        a_copy(to, a_c, tp, twin).wait_send()
        b_copy(to, dp, b_x, tp, facing).wait_send()
        b_copy(to, dp, b_c.at[0], tp, twin).wait_send()
        b_copy(to, facing, b_c.at[1], tp, twin).wait_send()


def front(ids, embed, rounds, code, extra, w_rows, wkv_t, ln, cos_t, sin_t, n_q, collective_id):
    own, width = extra.shape
    two_hd = 2 * wkv_t.shape[1]
    shards = 2 * NZ
    ff = (w_rows.shape[0] * shards - 2 * n_q) // 3
    dma = lambda *n: pltpu.SemaphoreType.DMA(n)
    s = jax.ShapeDtypeStruct
    rows = (shards, ids.shape[0] // shards, width)
    return pl.pallas_call(
        front_kernel,
        out_shape=(s((own, width), F32),) * 3 + (s((n_q, own), BF16), s((2 * own, two_hd), BF16), s((two_hd, 2 * own), BF16),
                   s((2 * n_q // two_hd, own), F32), s((n_q, own), BF16), s((n_q, width), BF16), s((n_q, width), BF16))
        + (s((ff, width), BF16),) * 3 + (s((4, 1, 128), jnp.int32),),
        in_specs=[pl.BlockSpec(memory_space=pltpu.SMEM), ANY, VMEM, VMEM, VMEM, ANY] + [VMEM] * 4,
        out_specs=(VMEM,) * 10 + (ANY,) * 3 + (VMEM,),
        scratch_shapes=[pltpu.VMEM((ff, width), BF16)] * 3 + [dma(3, shards), pltpu.VMEM(embed.shape, F32), pltpu.VMEM(rows, F32), pltpu.VMEM((shards,) + w_rows.shape, F32), pltpu.VMEM(rows, F32), pltpu.VMEM((own, width), BF16),
                        pltpu.VMEM((two_hd, own), F32), pltpu.VMEM((two_hd, own), F32),
                        dma(3), dma(shards), dma(shards)] + [dma(shards)] * 4 + [dma(shards, 2)]
        + [dma(shards)] * 4 + [dma(2, shards), dma(shards, 4), pltpu.SemaphoreType.DMA, pltpu.SemaphoreType.DMA, dma(3), dma(4)],
        compiler_params=pltpu.CompilerParams(collective_id=collective_id, has_side_effects=True, vmem_limit_bytes=60000000),
        name="front",
    )(ids, embed, rounds, code, extra, w_rows, wkv_t, ln, cos_t, sin_t)


def layer_bwd_kernel(scale, tok_total, dfin_ref, x0_ref, x1_ref, norm_ref, hits_ref, ln_ref, cos_ref, sin_ref, wq_ref, wkv_ref, wo_ref, wg_any, wu_any, wd_any,
                     q_ref, kv_ref, kvt_ref, lse_ref, ctx_ref, code_ref, g_ref, ids_ref, rows_ref, d0_ref, back_ref, early_ref, ids_all, d_one, d_b, u_b, dctx, dq, dkv, dkv_in,
                     hid, d_gate, d_up, rows_out, g_q, g_o, g_g, g_u, g_d, small, s_early, c_early, wg_ref, wu_ref, wd_ref, w_sem, out_sem, send_sem, recv_sem,
                     r_send, x_send, c_send, r_recv, g_load, g_send, g_recv, id_send, id_recv):
    tp, dp, z, y = place()
    partner = tp + 1 - 2 * y
    core = dp % 2
    twin = dp + 1 - 2 * core
    facing = lax.rem(dp + 2, 4)
    across = lax.rem(twin + 2, 4)
    own, width = x0_ref.shape
    hd = kv_ref.shape[1] // 2
    quarter = hd // 2
    nq = q_ref.shape[0]
    heads = nq // hd
    ff = wg_ref.shape[0]
    shards = rows_ref.shape[0]
    w_loads = [pltpu.make_async_copy(src, dst, w_sem.at[i]) for i, (src, dst) in enumerate(((wg_any, wg_ref), (wu_any, wu_ref), (wd_any, wd_ref)))]
    for c in w_loads:
        c.start()
    plane_barrier(tp, dp, [(tp, twin), (tp, facing), (tp, across)])

    n_early, g_size = s_early.shape[0], s_early.shape[1]

    def g_rows(which, b):
        return g_ref.at[pl.ds(pl.multiple_of(which * (g_ref.shape[0] // 2) + b * g_size, 8), g_size), :]

    def g_load_copy(b):
        return pltpu.make_async_copy(g_rows(core, b), s_early.at[b], g_load.at[b])

    def g_chip_copy(b):
        return remote(g_rows(1 - core, b), c_early.at[b], g_send.at[0, b], g_recv.at[0, b], tp, twin)

    def g_x_copy(b):
        return remote(s_early.at[b], early_ref.at[b], g_send.at[1, b], g_recv.at[1, b], tp, facing)

    for b in range(n_early):
        g_chip_copy(b).start()
        g_load_copy(b).start()

    def ids_copy(n, to):
        return remote(ids_ref, ids_all.at[dp], id_send.at[n], id_recv.at[dp], tp, to)

    for n, to in enumerate((twin, facing, across)):
        ids_copy(n, to).start()
    ids_all[dp] = ids_ref[...]
    _, f_hat, f_inv = norm_fwd(x1_ref[...], ln_ref[1:2, :])
    d_in, g_fin = norm_bwd(dfin_ref[...], f_hat, f_inv, ln_ref[1:2, :])
    d_one[...] = d_in
    d_b[...] = d_in.astype(BF16)
    u_b[...] = norm_fwd(x0_ref[...], ln_ref[0:1, :])[0]
    dctx[...] = mm(wo_ref[...], d_b[...], TB).astype(BF16)
    for b in range(n_early):
        g_load_copy(b).wait()
        g_chip_copy(b).wait_recv()
        add_into(s_early.at[b], c_early.at[b], 24)
        g_x_copy(b).start()
    cos_t = cos_ref[...]
    sin_t = sin_ref[...]
    blank = jnp.zeros((hd, own), BF16)
    slope = hd ** -0.5 * LOG2E
    dkv[...] = jnp.zeros_like(dkv)

    def attend(h, carry):
        at = pl.ds(pl.multiple_of(h * hd, hd), hd)
        q_pad = jnp.concatenate([q_ref[at, :], blank], axis=0)
        d_pad = jnp.concatenate([blank, dctx[at, :]], axis=0)
        scores = mm(kv_ref[...], q_pad)
        allowed = lax.broadcasted_iota(jnp.int32, scores.shape, 0) <= lax.broadcasted_iota(jnp.int32, scores.shape, 1) + y * own
        prob = jnp.where(allowed, jnp.exp2(scores * slope - lse_ref[pl.ds(h, 1), :]), 0.0)
        d_prob = mm(kv_ref[...], d_pad)
        mean = jnp.sum(d_prob * prob, axis=0, keepdims=True)
        d_score = (prob * (d_prob - mean) * hd ** -0.5).astype(BF16)
        dkv[...] += mm(d_score, q_pad, TB) + mm(prob.astype(BF16), d_pad, TB)
        d_q = mm(kvt_ref[0:hd, :], d_score)
        lo, hi = turn(d_q[:quarter], d_q[quarter:], cos_t, -sin_t)
        dq[at, :] = jnp.concatenate([lo, hi], axis=0).astype(BF16)
        return carry

    lax.fori_loop(0, heads, attend, 0)
    copy = remote(dkv.at[pl.ds(pl.multiple_of((1 - y) * own, own), own), :], dkv_in, send_sem, recv_sem, partner, dp)
    copy.start()

    d0_ref[...] = mm(dq[...], wq_ref[...], TA)
    step = min(512, ff)
    for c in w_loads:
        c.wait()

    def mlp(n, carry):
        at = pl.ds(pl.multiple_of(n * step, step), step)
        gate = mm(wg_ref[at, :], u_b[...], TB)
        up = mm(wu_ref[at, :], u_b[...], TB)
        d_hidden = mm(wd_ref[at, :], d_b[...], TB)
        sig = jax.nn.sigmoid(gate)
        hid[at, :] = (gate * sig * up).astype(BF16)
        d_gate[at, :] = (d_hidden * up * sig * (1.0 + gate * (1.0 - sig))).astype(BF16)
        d_up[at, :] = (d_hidden * gate * sig).astype(BF16)
        d0_ref[...] += mm(d_gate[at, :], wg_ref[at, :], TA) + mm(d_up[at, :], wu_ref[at, :], TA)
        return carry

    lax.fori_loop(0, ff // step, mlp, 0)
    copy.wait()
    d_kv = (dkv[pl.ds(pl.multiple_of(y * own, own), own), :] + dkv_in[...]).T
    lo, hi = turn(d_kv[:quarter], d_kv[quarter:hd], cos_t, -sin_t)
    d_kv = jnp.concatenate([lo, hi, d_kv[hd:]], axis=0).astype(BF16)
    small[0:2 * hd, :] = mm(d_kv, u_b[...])
    d_u = d0_ref[...] + mm(d_kv, wkv_ref[...].reshape(2 * hd, width).astype(BF16), TA)
    _, u_hat, u_inv = norm_fwd(x0_ref[...], ln_ref[0:1, :])
    d_in, g_in = norm_bwd(d_u, u_hat, u_inv, ln_ref[0:1, :])
    d_zero = d_one[...] + d_in
    d0_ref[...] = d_zero
    high = d_zero.astype(BF16)
    left = d_zero - high.astype(F32)
    middle = left.astype(BF16)
    low = (left - middle.astype(F32)).astype(BF16)
    pick = picks(code_ref[...], rows_out.shape[0] * rows_out.shape[1])
    rows_out[...] = (mm(pick, high) + mm(pick, middle) + mm(pick, low)).reshape(rows_out.shape)

    def row_copy(to):
        return remote(rows_out.at[to], back_ref.at[dp, tp], r_send.at[to], r_recv.at[dp, tp], to, dp)

    def x_copy(slot):
        return remote(back_ref.at[dp, slot], back_ref.at[dp, slot], x_send.at[slot], r_recv.at[dp, slot], tp, facing)

    def c_copy(group, n, slot):
        return remote(back_ref.at[group, slot], back_ref.at[group, slot], c_send.at[n, slot], r_recv.at[group, slot], tp, twin)

    def back(group, slot):
        remote(rows_out.at[slot], back_ref.at[group, slot], r_send.at[slot], r_recv.at[group, slot], tp, twin).wait_recv()

    def near_first(k):
        return sorted(((o, zz) for o in range(2) for zz in range(NZ)), key=lambda c: (abs(c[1] - k), c[0]))

    def slot_of(o, zz):
        return 2 * zz + (1 - y if o else y)

    def on_position(f):
        for k in range(NZ):
            pl.when(z == k)(functools.partial(f, k))

    def rows_leave(k):
        for c in near_first(k)[1:]:
            row_copy(slot_of(*c)).start()

    on_position(rows_leave)
    own_rows = pltpu.make_async_copy(rows_out.at[tp], back_ref.at[dp, tp], out_sem.at[7 * 2 * NZ])
    own_rows.start()
    own_rows.wait()
    x_copy(tp).start()
    c_copy(dp, 0, tp).start()

    g_o[...] = mm(ctx_ref[...], d_b[...])
    g_q[...] = mm(dq[...], u_b[...])

    def weight_grads(n, carry):
        at = pl.ds(pl.multiple_of(n * step, step), step)
        g_d[at, :] = mm(hid[at, :], d_b[...])
        g_g[at, :] = mm(d_gate[at, :], u_b[...])
        g_u[at, :] = mm(d_up[at, :], u_b[...])
        return carry

    lax.fori_loop(0, ff // step, weight_grads, 0)
    small[2 * hd:, :] = jnp.zeros_like(small[2 * hd:, :])
    small[2 * hd:2 * hd + 1, :] = g_in.reshape(1, width)
    small[2 * hd + 1:2 * hd + 2, :] = g_fin.reshape(1, width)
    norm = norm_ref[pl.ds(tp, 1), :]
    hits = jnp.sum(hits_ref[...], axis=0, keepdims=True)
    small[2 * hd + 2:2 * hd + 3, :] = (norm + LOGIT_ZLOSS * norm * norm - hits * scale) / tok_total
    copies = []

    def put(src, first, size, s):
        copies.append(pltpu.make_async_copy(src, rows_ref.at[s, pl.ds(first, size), :], out_sem.at[len(copies)]))

    n_kv = 2 * hd // shards
    for s in range(shards):
        at = 0
        for g, size in ((g_q, nq // shards), (g_o, nq // shards), (g_g, ff // shards), (g_u, ff // shards), (g_d, ff // shards)):
            put(g.at[pl.ds(s * size, size), :], at, size, s)
            at += size
        put(small.at[pl.ds(s * n_kv, n_kv), :], at, n_kv, s)
        put(small.at[pl.ds(2 * hd + (0 if s == 0 else 16), 16), :], at + n_kv, 16, s)
    for c in copies:
        c.start()
    for c in copies:
        c.wait()

    def relay(k):
        order = near_first(k)
        for c in order[1:]:
            back(dp, slot_of(*c))
            x_copy(slot_of(*c)).start()
            c_copy(dp, 0, slot_of(*c)).start()
        for c in order:
            back(facing, slot_of(*c))
            c_copy(facing, 1, slot_of(*c)).start()

    on_position(relay)
    for b in range(n_early):
        g_x_copy(b).wait_recv()
        add_into(early_ref.at[b], s_early.at[b], 24)
    for slot in range(shards):
        back(twin, slot)
        back(across, slot)
    for n, to in enumerate((twin, facing, across)):
        remote(ids_ref, ids_all.at[to], id_send.at[n], id_recv.at[to], tp, to).wait_recv()
        ids_copy(n, to).wait_send()
    for n in range(1, shards):
        row_copy(lax.rem(tp + n, shards)).wait_send()
    for slot in range(shards):
        x_copy(slot).wait_send()
        c_copy(dp, 0, slot).wait_send()
        c_copy(facing, 1, slot).wait_send()
    for b in range(n_early):
        g_chip_copy(b).wait_send()
        g_x_copy(b).wait_send()


def layer_bwd(scale, tok_total, d_fin, x0, x1, norms, hits, ln, cos_t, sin_t, weights, saved, code, g_table, ids, collective_id):
    own, width = x0.shape
    nq = weights[0].shape[0]
    two_hd = 2 * weights[1].shape[1]
    ff = weights[3].shape[0]
    rows = (2 * nq + 3 * ff + two_hd) // (2 * NZ) + 16
    chunk = (own, width)
    back = (2 * NZ, ids.shape[1] // (2 * NZ), width)
    blocks = (N_EARLY, table_block(g_table.shape[0]), width)
    dma = lambda *n: pltpu.SemaphoreType.DMA(n)
    return pl.pallas_call(
        functools.partial(layer_bwd_kernel, scale, tok_total),
        out_shape=(jax.ShapeDtypeStruct((2 * NZ, rows, width), F32), jax.ShapeDtypeStruct(chunk, F32), jax.ShapeDtypeStruct((4,) + back, F32),
                   jax.ShapeDtypeStruct(blocks, F32), jax.ShapeDtypeStruct((4,) + ids.shape, jnp.int32)),
        in_specs=[VMEM] * 11 + [ANY] * 3 + [VMEM] * 6 + [ANY, VMEM],
        out_specs=(ANY, VMEM, ANY, VMEM, VMEM),
        scratch_shapes=[pltpu.VMEM(chunk, F32), pltpu.VMEM(chunk, BF16), pltpu.VMEM(chunk, BF16), pltpu.VMEM((nq, own), BF16),
                        pltpu.VMEM((nq, own), BF16), pltpu.VMEM((2 * own, two_hd), F32), pltpu.VMEM((own, two_hd), F32)]
        + [pltpu.VMEM((ff, own), BF16)] * 3 + [pltpu.VMEM(back, F32), pltpu.VMEM((nq, width), F32), pltpu.VMEM((nq, width), F32)] + [pltpu.VMEM((ff, width), F32)] * 3
        + [pltpu.VMEM((two_hd + 32, width), F32), pltpu.VMEM(blocks, F32), pltpu.VMEM(blocks, F32)]
        + [pltpu.VMEM((ff, width), BF16)] * 3 + [dma(3), dma(14 * NZ + 1),
           pltpu.SemaphoreType.DMA, pltpu.SemaphoreType.DMA, dma(2 * NZ), dma(2 * NZ), dma(2, 2 * NZ), dma(4, 2 * NZ),
           dma(N_EARLY), dma(2, N_EARLY), dma(2, N_EARLY), dma(3), dma(4)],
        compiler_params=pltpu.CompilerParams(collective_id=collective_id, has_side_effects=True, vmem_limit_bytes=66000000),
        name="layer_bwd",
    )(d_fin, x0, x1, norms, hits, ln, cos_t, sin_t, *weights, *saved, code, g_table, ids)


N_BLOCK = 12
N_EARLY = 3
AHEAD = 11


def table_block(vocab):
    return -(-vocab // (2 * N_BLOCK * 24)) * 24


W_REDUCE = {
    0: {4: (3,), 6: (2,), 8: (1,), 9: (0,)},
    1: {6: (3,), 8: (2, 0), 9: (1,)},
    2: {6: (0,), 8: (1, 3), 9: (2,)},
    3: {4: (0,), 6: (1,), 8: (2,), 9: (3,)},
}


def tail_kernel(g_ref, p_ref, rows_ref, ids_ref, early_ref, t_ref, w_out, small_ref,
                s_buf, from_c, from_x, look_in, parts, acc, w_c, w_y, w_l, w_r, w_x,
                g_load, g_send_c, g_recv_c, g_send_x, g_recv_x, g_send_t, g_recv_t, g_store, l_sem,
                w_load, w_out_sem, send_c, send_y, send_l, send_r, recv_c, recv_y, recv_l, recv_r, last_send, last_recv, small_send, small_recv):
    tp, dp, z, y = place()
    partner = tp + 1 - 2 * y
    core = dp % 2
    twin = dp + 1 - 2 * core
    facing = lax.rem(dp + 2, 4)
    half = g_ref.shape[0] // 2
    size = s_buf.shape[1]
    last = half - (N_BLOCK - 1) * size
    n_look = rows_ref.shape[1]

    def rows(which, b, n):
        return pl.ds(pl.multiple_of(which * half + b * size, 8), n)

    def part(buf, b, n):
        return buf.at[b - N_EARLY if buf is not from_x else b, pl.ds(0, n), :]

    plane_barrier(tp, dp, [(tp, twin), (tp, facing)])

    chip = dp // 2
    groups = (2 * chip, 2 * chip + 1, 2 - 2 * chip, 3 - 2 * chip)

    def look_load(n):
        return pltpu.make_async_copy(rows_ref.at[groups[n]], look_in.at[n % 2], l_sem.at[n % 2])

    def early_load(b):
        return pltpu.make_async_copy(early_ref.at[b], from_x.at[b], g_load.at[b])

    for n in range(2):
        look_load(n).start()

    def c_copy(b, n):
        return remote(g_ref.at[rows(1 - core, b, n), :], part(from_c, b, n), g_send_c.at[b], g_recv_c.at[b], tp, twin)

    def own_load(b, n):
        return pltpu.make_async_copy(g_ref.at[rows(core, b, n), :], part(s_buf, b, n), g_load.at[b])

    def x_copy(b, n):
        return remote(part(s_buf, b, n), part(from_x, b, n), g_send_x.at[b], g_recv_x.at[b], tp, facing)

    def t_copy(b, n):
        return remote(part(from_x, b, n), t_ref.at[rows(core, b, n), :], g_send_t.at[b], g_recv_t.at[b], tp, twin)

    def t_store(b, n):
        return pltpu.make_async_copy(part(from_x, b, n), t_ref.at[rows(core, b, n), :], g_store.at[b])

    def every(f, first, end):
        def body(b, carry):
            f(b, size)
            return carry
        lax.fori_loop(first, min(end, N_BLOCK - 1), body, 0)
        if end == N_BLOCK:
            f(N_BLOCK - 1, last)

    def looked_up(b, n, first, count):
        ids = jnp.concatenate([ids_ref[first + g] for g in range(count)], axis=1) - (core * half + b * size)
        hit = (lax.broadcasted_iota(jnp.int32, (n, count * n_look), 0) == ids).astype(F32).astype(BF16)
        span = pl.ds(pl.multiple_of(first * n_look, n_look), count * n_look)
        return mm(hit, parts[0, span, :]) + mm(hit, parts[1, span, :]) + mm(hit, parts[2, span, :])

    def chip_sum(b, n):
        own_load(b, n).wait()
        c_copy(b, n).wait_recv()
        at = b - N_EARLY
        s_buf[at, 0:n, :] = s_buf[at, 0:n, :] + from_c[at, 0:n, :] + looked_up(b, n, 2 * chip, 2)
        x_copy(b, n).start()

    def early_sum(b, n):
        early_load(b).wait()
        from_x[b] = from_x[b] + looked_up(b, n, 0, 4)
        t_copy(b, n).start()
        t_store(b, n).start()

    def w_first(k):
        for zz in REDUCE_ORDER[k]:
            for slot in (2 * zz + 1 - y, 2 * zz + y):
                remote(p_ref.at[slot, 1 - core], w_c.at[slot], send_c.at[slot], recv_c.at[slot], tp, twin).start()
                pltpu.make_async_copy(p_ref.at[slot, core], acc.at[slot], w_load.at[slot]).start()

    def w_chip_sum(slot):
        pltpu.make_async_copy(p_ref.at[slot, core], acc.at[slot], w_load.at[slot]).wait()
        remote(acc.at[slot], w_c.at[slot], send_c.at[slot], recv_c.at[slot], tp, twin).wait_recv()
        add_into(acc.at[slot], w_c.at[slot])

    def w_second(k):
        for zz in REDUCE_ORDER[k]:
            slot = 2 * zz + 1 - y
            w_chip_sum(slot)
            remote(acc.at[slot], w_y.at[zz], send_y.at[zz], recv_y.at[zz], partner, dp).start()
        for zz in REDUCE_ORDER[k]:
            w_chip_sum(2 * zz + y)

    def w_reduce(k, shards):
        for zz in shards:
            line = acc.at[2 * zz + y]
            remote(line, w_y.at[zz], send_y.at[zz], recv_y.at[zz], partner, dp).wait_recv()
            add_into(line, w_y.at[zz])
            if zz >= k and k > 0:
                remote(line, w_l.at[zz - 1], send_l.at[zz], recv_l.at[zz], partner, dp).wait_recv()
                add_into(line, w_l.at[zz - 1])
            if zz <= k and k < NZ - 1:
                remote(line, w_r.at[zz], send_r.at[zz], recv_r.at[zz], partner, dp).wait_recv()
                add_into(line, w_r.at[zz])
            if zz > k:
                remote(line, w_l.at[zz - 1], send_r.at[zz], recv_l.at[zz], tp + 2, dp).start()
            if zz < k:
                remote(line, w_r.at[zz], send_l.at[zz], recv_r.at[zz], tp - 2, dp).start()

    def on_position(f):
        for k in range(NZ):
            pl.when(z == k)(functools.partial(f, k))

    def first(b, n):
        c_copy(b, n).start()
        own_load(b, n).start()

    every(first, N_EARLY, N_EARLY + 2)
    on_position(w_first)
    every(first, N_EARLY + 2, N_BLOCK)
    for b in range(N_EARLY):
        early_load(b).start()

    def split(n):
        look_load(n).wait()
        value = look_in[n % 2]
        high = value.astype(BF16)
        left = value - high.astype(F32)
        middle = left.astype(BF16)
        at = pl.ds(pl.multiple_of(groups[n] * n_look, n_look), n_look)
        parts[0, at, :] = high
        parts[1, at, :] = middle
        parts[2, at, :] = (left - middle.astype(F32)).astype(BF16)
        if n + 2 < 4:
            look_load(n + 2).start()

    split(0)
    split(1)
    every(chip_sum, N_EARLY, N_EARLY + 3)
    on_position(w_second)
    every(chip_sum, N_EARLY + 3, AHEAD)
    split(2)
    split(3)
    every(early_sum, 0, N_EARLY)

    total = acc.at[tp]
    w_copy_x = remote(total, w_x, last_send.at[0], last_recv.at[0], tp, facing)
    w_copy_c = remote(total, w_out.at[core], last_send.at[1], last_recv.at[1], tp, twin)
    w_store = pltpu.make_async_copy(total, w_out.at[core], w_out_sem)
    n_small, n_rows = small_ref.shape[1], w_out.shape[1]
    mine = w_out.at[1, pl.ds(n_rows - 32, n_small), :]
    small_here = pltpu.make_async_copy(mine, small_ref.at[tp], w_out_sem)
    peers = [lax.rem(tp + n, 2 * NZ) for n in range(1, 2 * NZ)]
    for b in range(N_EARLY, N_BLOCK):
        n = last if b == N_BLOCK - 1 else size
        if b == N_BLOCK - 1:
            w_copy_x.wait()
            add_into(total, w_x)
            w_copy_c.start()
            w_store.start()
            w_copy_c.wait_send()
            remote(total, w_out.at[1 - core], last_send.at[1], last_recv.at[1], tp, twin).wait_recv()
            w_store.wait()
            for to in peers:
                remote(mine, small_ref.at[tp], small_send.at[to], small_recv.at[tp], to, dp).start()
            small_here.start()
        x_copy(b, n).wait_recv()
        add_into(part(from_x, b, n), part(s_buf, b, n), 24)
        t_copy(b, n).start()
        t_store(b, n).start()
        for k in range(NZ):
            if b in W_REDUCE[k]:
                pl.when(z == k)(functools.partial(w_reduce, k, W_REDUCE[k][b]))
        if b == N_BLOCK - 3:
            w_copy_x.start()
            every(chip_sum, AHEAD, N_BLOCK)
    for source in peers:
        remote(small_ref.at[source], small_ref.at[source], small_send.at[source], small_recv.at[source], source, dp).wait_recv()
        remote(mine, small_ref.at[tp], small_send.at[source], small_recv.at[tp], source, dp).wait_send()
    small_here.wait()

    def w_done(k):
        for zz in range(NZ):
            line = acc.at[2 * zz + y]
            for slot in (2 * zz + 1 - y, 2 * zz + y):
                remote(p_ref.at[slot, 1 - core], w_c.at[slot], send_c.at[slot], recv_c.at[slot], tp, twin).wait_send()
            remote(line, w_y.at[zz], send_y.at[zz], recv_y.at[zz], partner, dp).wait_send()
            if zz > k:
                remote(line, w_l.at[zz - 1], send_r.at[zz], recv_l.at[zz], tp + 2, dp).wait_send()
            if zz < k:
                remote(line, w_r.at[zz], send_l.at[zz], recv_r.at[zz], tp - 2, dp).wait_send()

    on_position(w_done)

    def drain(b, n):
        t_copy(b, n).wait_send()
        t_store(b, n).wait()
        remote(part(from_x, b, n), t_ref.at[rows(1 - core, b, n), :], g_send_t.at[b], g_recv_t.at[b], tp, twin).wait_recv()

    def sent(b, n):
        c_copy(b, n).wait_send()
        x_copy(b, n).wait_send()

    every(drain, 0, N_BLOCK)
    every(sent, N_EARLY, N_BLOCK)


def tail(g_table, g_rows, look_rows, look_ids, early, collective_id):
    vocab, width = g_table.shape
    rows = g_rows.shape[1]
    half = (rows // 2, width)
    n_look = look_ids.shape[2]
    size = table_block(vocab)
    blocks = lambda n: pltpu.VMEM((n, size, width), F32)
    dma = lambda *n: pltpu.SemaphoreType.DMA(n)
    t, w_sum, small = pl.pallas_call(
        tail_kernel,
        out_shape=(jax.ShapeDtypeStruct((vocab, width), F32), jax.ShapeDtypeStruct((2,) + half, F32), jax.ShapeDtypeStruct((2 * NZ, 24, width), F32)),
        in_specs=[ANY, ANY, ANY, VMEM, ANY],
        out_specs=(ANY,) * 3,
        scratch_shapes=[blocks(N_BLOCK - N_EARLY)] * 2 + [blocks(N_BLOCK), pltpu.VMEM((2, n_look, width), F32), pltpu.VMEM((3, 4 * n_look, width), BF16)]
        + [pltpu.VMEM((2 * NZ,) + half, F32)] * 2 + [pltpu.VMEM((NZ,) + half, F32)] + [pltpu.VMEM((NZ - 1,) + half, F32)] * 2
        + [pltpu.VMEM(half, F32)]
        + [dma(N_BLOCK)] * 8 + [dma(2)]
        + [dma(2 * NZ), pltpu.SemaphoreType.DMA] + [dma(2 * NZ), dma(NZ), dma(NZ), dma(NZ)] * 2 + [dma(2)] * 2 + [dma(2 * NZ)] * 2,
        compiler_params=pltpu.CompilerParams(collective_id=collective_id, has_side_effects=True, vmem_limit_bytes=67000000),
        name="tail",
    )(g_table, g_rows.reshape((2 * NZ, 2) + half), look_rows.reshape(4, n_look, width), look_ids, early)
    return t, w_sum.reshape(rows, width), small


UPDATE_ROWS = 512


def update_kernel(t_ref, w_any, small_any, *refs):
    state = [refs[7 * i:7 * i + 7] for i in range(3)]
    new = [refs[21 + 7 * i:28 + 7 * i] for i in range(3)]
    loss_ref, held, made, w_ref, small_ref = refs[42:47]
    old_small = [refs[47 + 6 * i:53 + 6 * i] for i in range(3)]
    new_small = [refs[65 + 6 * i:71 + 6 * i] for i in range(3)]
    in_sem, out_sem, g_sem, small_in, small_out = refs[83:]
    vocab = t_ref.shape[0]
    blocks = [(at, min(UPDATE_ROWS, vocab - at)) for at in range(0, vocab, UPDATE_ROWS)]

    def loads(q):
        at, n = blocks[q]
        return [pltpu.make_async_copy(ref.at[pl.ds(at, n), :], held.at[q % 4, i, pl.ds(0, n), :], in_sem.at[q % 4, i])
                for i, ref in enumerate((t_ref, state[0][0], state[1][0], state[2][0]))]

    def stores(q):
        at, n = blocks[q]
        return [pltpu.make_async_copy(made.at[q % 3, i, pl.ds(0, n), :], new[i][0].at[pl.ds(at, n), :], out_sem.at[q % 3, i]) for i in range(3)]

    for q in range(4):
        for c in loads(q):
            c.start()
    grads = [pltpu.make_async_copy(w_any, w_ref, g_sem.at[0]), pltpu.make_async_copy(small_any, small_ref, g_sem.at[1])]
    pairs = [(i, j) for i in range(3) for j in range(6)]
    small_loads = grads + [pltpu.make_async_copy(state[i][j + 1], old_small[i][j], small_in.at[i, j]) for i, j in pairs]
    small_stores = [pltpu.make_async_copy(new_small[i][j], new[i][j + 1], small_out.at[i, j]) for i, j in pairs]
    for c in small_loads:
        c.start()

    def small_update(index, grad, *where):
        got = adam_update(old_small[0][index - 1][where], grad, old_small[1][index - 1][where], old_small[2][index - 1][where])
        for i in range(3):
            new_small[i][index - 1][where] = got[i]

    def small_updates():
        hd = old_small[0][2].shape[1]
        n_kv = 2 * hd // small_ref.shape[0]
        n_q, n_f = old_small[0][1].shape[0], old_small[0][5].shape[0]
        small_update(1, small_ref[0, n_kv:n_kv + 2, :], Ellipsis)
        small_update(2, w_ref[0:n_q, :], Ellipsis)
        kv = small_ref[:, 0:n_kv, :].reshape(2 * hd, small_ref.shape[2])
        for i in range(2):
            small_update(3, kv[i * hd:(i + 1) * hd], i)
        small_update(4, w_ref[n_q:2 * n_q, :], Ellipsis)
        for i in range(2):
            small_update(5, w_ref[2 * n_q + i * n_f:2 * n_q + (i + 1) * n_f, :].T, i)
        small_update(6, w_ref[2 * n_q + 2 * n_f:2 * n_q + 3 * n_f, :], Ellipsis)
        loss_ref[...] = jnp.sum(small_ref[0, n_kv + 2:n_kv + 3, :], axis=1, keepdims=True)

    for q, (at, n) in enumerate(blocks):
        for c in loads(q):
            c.wait()
        if q >= 3:
            for c in stores(q - 3):
                c.wait()
        step = 32 if n % 32 == 0 else 16

        def body(j, carry):
            rows = pl.ds(pl.multiple_of(j * step, step), step)
            got = adam_update(held[q % 4, 1, rows, :], held[q % 4, 0, rows, :], held[q % 4, 2, rows, :], held[q % 4, 3, rows, :])
            for i in range(3):
                made[q % 3, i, rows, :] = got[i]
            return carry

        lax.fori_loop(0, n // step, body, 0)
        for c in stores(q):
            c.start()
        if q + 4 < len(blocks):
            for c in loads(q + 4):
                c.start()
        if q == min(3, len(blocks) - 1):
            for c in small_loads:
                c.wait()
            small_updates()
            for c in small_stores:
                c.start()
    for q in range(len(blocks) - 3, len(blocks)):
        for c in stores(q):
            c.wait()
    for c in small_stores:
        c.wait()


def update(g_table, g_shard, g_small, state_arrays):
    width = g_table.shape[1]
    dma = lambda *n: pltpu.SemaphoreType.DMA(n)

    def flip(arrays):
        return [a.swapaxes(-1, -2) if i % 7 in (2, 3) else a for i, a in enumerate(arrays)]

    given = flip(state_arrays)
    small = [pltpu.VMEM(a.shape, F32) for i, a in enumerate(given) if i % 7]
    *new, loss = pl.pallas_call(
        update_kernel,
        out_shape=tuple(jax.ShapeDtypeStruct(a.shape, F32) for a in given) + (jax.ShapeDtypeStruct((1, 1), F32),),
        in_specs=[ANY] * 24,
        out_specs=(ANY,) * 21 + (VMEM,),
        scratch_shapes=[pltpu.VMEM((4, 4, UPDATE_ROWS, width), F32), pltpu.VMEM((3, 3, UPDATE_ROWS, width), F32),
                        pltpu.VMEM(g_shard.shape, F32), pltpu.VMEM(g_small.shape, F32)] + small * 2
        + [dma(4, 4), dma(3, 3), dma(2), dma(3, 6), dma(3, 6)],
        compiler_params=pltpu.CompilerParams(vmem_limit_bytes=60000000),
        name="update",
    )(g_table, g_shard, g_small, *given)
    return flip(new) + [loss]


def norm_fwd(x_f32, scale):
    centered = x_f32 - jnp.mean(x_f32, axis=-1, keepdims=True)
    inv_std = lax.rsqrt(jnp.mean(centered * centered, axis=-1, keepdims=True) + LN_EPS)
    x_hat = centered * inv_std
    return (x_hat * scale).astype(BF16), x_hat, inv_std


def norm_bwd(d_out, x_hat, inv_std, scale):
    d_scale = jnp.sum(d_out * x_hat, axis=0)
    d_hat = d_out * scale
    d_in = inv_std * (d_hat - jnp.mean(d_hat, axis=-1, keepdims=True) - x_hat * jnp.mean(d_hat * x_hat, axis=-1, keepdims=True))
    return d_in, d_scale


def adam_update(param_in, grad_in, mom_in, vel_in):
    mom_new = BETA_ONE * mom_in + (1.0 - BETA_ONE) * grad_in
    vel_new = BETA_TWO * vel_in + (1.0 - BETA_TWO) * grad_in * grad_in
    return param_in - LEARN_RATE * mom_new / (jnp.sqrt(vel_new) + ADAM_EPS), mom_new, vel_new


def dot(spec, a, b):
    return jnp.einsum(spec, a, b, preferred_element_type=F32)


def solution(mesh):
    param_specs = (P('tp', None), P(None, None), P(None, 'tp'), P(None, None, None), P('tp', None), P(None, None, 'tp'), P('tp', None))
    n_tp = mesh.shape['tp']
    n_dp = mesh.shape['dp']

    def local_step(tokens, labels, *state_arrays):
        embed, ln_scales, w_q, w_kv, w_o, w_gu, w_down = state_arrays[0:7]
        batch_loc, seq_len = tokens.shape
        vocab_loc, d_model = embed.shape
        head_dim = w_kv.shape[2]
        q_loc = w_q.shape[1]
        f_loc = w_down.shape[0]
        tok_loc = batch_loc * seq_len
        tok_total = tok_loc * n_dp
        own = tok_loc // n_tp
        tp_rank = lax.axis_index('tp')
        half = tp_rank % 2

        strict = (jnp.arange(own)[:, None] > jnp.arange(own)[None, :]).astype(BF16)

        def routing(chunks):
            shard = chunks // vocab_loc
            row = chunks - shard * vocab_loc
            hot = (shard[:, :, None] == jnp.arange(n_tp)[None, None, :])
            before = dot('rs,nsj->nrj', strict, hot.astype(BF16))
            rank = jnp.sum(jnp.where(hot, before, 0.0), axis=-1).astype(jnp.int32)
            most = jnp.max(jnp.sum(hot.astype(jnp.int32), axis=1))
            return shard, row, rank, (most + CAP - 1) // CAP

        chunks = tokens.reshape(n_tp, own)
        shard, row, rank, rounds = routing(chunks)
        slots = jnp.arange(CAP)
        my_shard = lax.dynamic_index_in_dim(shard, tp_rank, 0, keepdims=False)
        my_rank = lax.dynamic_index_in_dim(rank, tp_rank, 0, keepdims=False)

        def fetch(step):
            here = (shard[:, None, :] == tp_rank) & (rank[:, None, :] == slots[None, :, None] + step * CAP)
            ids = jnp.sum(jnp.where(here, row[:, None, :], 0), axis=-1).reshape(-1)
            place = my_rank - step * CAP
            return ids, jnp.where((place >= 0) & (place < CAP), my_shard * CAP + place, -1)

        def fetch_more(state):
            ids, code = fetch(state[0])
            pick = (code[:, None] == jnp.arange(n_tp * CAP)[None, :]).astype(BF16)
            rows_in = plane_swap(jnp.take(embed, ids, axis=0).reshape(n_tp, CAP, d_model), 1).reshape(n_tp * CAP, d_model).astype(BF16)
            return state[0] + 1, state[1] + dot('rc,cd->rd', pick, rows_in)

        more_rows = lax.while_loop(lambda state: state[0] < rounds, fetch_more, (jnp.int32(1), jnp.zeros((own, d_model), F32)))[1]
        ids_first, code_first = fetch(0)
        code_first = code_first[None, :]

        w_rows = jnp.concatenate([w_q.T, w_o, w_gu.transpose(0, 2, 1).reshape(2 * f_loc, d_model), w_down], axis=0)
        cuts = (q_loc, 2 * q_loc, 2 * q_loc + f_loc, 2 * q_loc + 2 * f_loc)
        wkv_t = w_kv.transpose(0, 2, 1)
        inv_freq = ROPE_BASE ** (-jnp.arange(0, head_dim, 2).astype(F32) / head_dim)
        angles = inv_freq[:, None] * (half * own + jnp.arange(own)).astype(F32)[None, :]
        cos_t, sin_t = jnp.cos(angles), jnp.sin(angles)
        f_own, x_one, x_zero, *saved = front(ids_first, embed, jnp.broadcast_to(rounds, (1, 128)), code_first, more_rows, w_rows, wkv_t, ln_scales, cos_t, sin_t, n_tp * q_loc, 0)
        saved, (wq_t, wo_b, wg_t, wu_t, wd_b), rounds_all = saved[:5], saved[5:10], jnp.max(saved[10])
        weights = (wq_t, wkv_t, wo_b, wg_t, wu_t, wd_b)

        logit_scale = d_model ** -0.5
        d_fin, g_head_part, log_norm, lab_sum, _ = head(f_own, labels, embed, logit_scale, logit_scale / tok_total, 4)

        def row_ids(step):
            here = (shard[:, None, :] == tp_rank) & (rank[:, None, :] == slots[None, :, None] + step * CAP)
            return jnp.where(jnp.any(here, axis=-1), jnp.sum(jnp.where(here, row[:, None, :], 0), axis=-1), vocab_loc).reshape(-1)

        g_rows, d_zero, rows_back, early, ids_back = layer_bwd(logit_scale, tok_total, d_fin, x_zero, x_one, log_norm, lab_sum, ln_scales, cos_t, sin_t, weights, saved,
                                                               code_first, g_head_part, row_ids(0)[None, :], 7)
        g_table, g_shard, g_small = tail(g_head_part, g_rows, rows_back, ids_back, early, 10)

        def give_back(state):
            mine = (my_shard[None, None, :] == jnp.arange(n_tp)[:, None, None]) & (my_rank[None, None, :] == slots[None, :, None] + state[0] * CAP)
            ids = jnp.sum(jnp.where(mine, jnp.arange(own)[None, None, :], 0), axis=-1).reshape(-1)
            rows_in = plane_swap(jnp.take(d_zero, ids, axis=0).reshape(n_tp, CAP, d_model), 9).reshape(-1, d_model)
            n_rows = n_tp * CAP
            id_rows = jnp.pad(row_ids(state[0]).astype(F32), (0, -n_rows % (8 * d_model))).reshape(-1, d_model)
            both = group_gather(jnp.concatenate([rows_in, id_rows], axis=0), 11)
            ids = both[:, n_rows:].reshape(n_dp, -1)[:, :n_rows].astype(jnp.int32)
            return state[0] + 1, state[1].at[ids.reshape(-1)].add(both[:, :n_rows].reshape(-1, d_model), mode='drop')

        g_table = lax.while_loop(lambda state: state[0] < rounds_all, give_back, (jnp.int32(1), g_table))[1]
        *new, loss = update(g_table, g_shard, g_small, state_arrays)
        return tuple(new) + (loss.reshape(()),)

    return jax.shard_map(local_step, mesh=mesh, in_specs=(P('dp', None), P('dp', None)) + param_specs * 3,
                         out_specs=param_specs * 3 + (P(),), check_vma=False)
```

```python
import functools

import jax
import jax.numpy as jnp
from jax import lax
from jax.experimental import pallas as pl
from jax.experimental.pallas import tpu as pltpu
from jax.sharding import PartitionSpec as P

LN_EPS = 1e-5
LOGIT_ZLOSS = 1e-4
LEARN_RATE = 1e-2
BETA_ONE = 0.9
BETA_TWO = 0.95
ADAM_EPS = 1e-8
ROPE_BASE = 10000.0
NZ = 4
CAP = 96
F32 = jnp.float32
BF16 = jnp.bfloat16
ANY = pl.BlockSpec(memory_space=pl.ANY)
VMEM = pl.BlockSpec(memory_space=pltpu.VMEM)

ARRIVALS = {
    0: (("R", 1), ("R", 2), ("R", 3)),
    1: (("L", 0), ("R", 2), ("R", 3)),
    2: (("R", 3), ("L", 1), ("L", 0)),
    3: (("L", 2), ("L", 1), ("L", 0)),
}
REDUCE_ORDER = {0: (3, 2, 1, 0), 1: (3, 0, 2, 1), 2: (0, 3, 1, 2), 3: (0, 1, 2, 3)}


def remote(src, dst, send_sem, recv_sem, tp, dp):
    return pltpu.make_async_remote_copy(src_ref=src, dst_ref=dst, send_sem=send_sem, recv_sem=recv_sem,
                                        device_id=(tp, dp), device_id_type=pl.DeviceIdType.MESH)


def place():
    tp = lax.axis_index("tp")
    dp = lax.axis_index("dp")
    return tp, dp, tp // 2, tp % 2


def signal(tp, dp):
    pl.semaphore_signal(pltpu.get_barrier_semaphore(), inc=1, device_id=(tp, dp), device_id_type=pl.DeviceIdType.MESH)


def add_into(acc, other, step=None):
    rows = acc.shape[0]
    step = step or (64 if rows % 64 == 0 else 8)

    def body(n, carry):
        at = pl.ds(pl.multiple_of(n * step, step), step)
        acc[at, :] = acc[at, :] + other[at, :]
        return carry

    lax.fori_loop(0, rows // step, body, 0)


def near_first(k):
    return sorted(((o, zz) for o in range(2) for zz in range(NZ)), key=lambda c: (abs(c[1] - k), c[0]))


def plane_barrier(tp, dp, others):
    peers = [(lax.rem(tp + n, 2 * NZ), dp) for n in range(1, 2 * NZ)] + others
    for peer in peers:
        signal(*peer)
    pl.semaphore_wait(pltpu.get_barrier_semaphore(), len(peers))


def swap_kernel(x_ref, out_ref, own_sem, send, recv):
    tp, dp, _, _ = place()
    plane_barrier(tp, dp, [])
    copies = []
    for n in range(1, 2 * NZ):
        to = lax.rem(tp + n, 2 * NZ)
        copy = remote(x_ref.at[to], out_ref.at[tp], send.at[to], recv.at[tp], to, dp)
        copy.start()
        copies.append(copy)
    own = pltpu.make_async_copy(x_ref.at[tp], out_ref.at[tp], own_sem)
    own.start()
    for n in range(1, 2 * NZ):
        source = lax.rem(tp + n, 2 * NZ)
        remote(out_ref.at[source], out_ref.at[source], send.at[source], recv.at[source], source, dp).wait_recv()
    own.wait()
    for copy in copies:
        copy.wait_send()


def plane_swap(x, collective_id):
    return pl.pallas_call(
        swap_kernel,
        out_shape=jax.ShapeDtypeStruct(x.shape, x.dtype),
        in_specs=[ANY],
        out_specs=ANY,
        scratch_shapes=[pltpu.SemaphoreType.DMA] + [pltpu.SemaphoreType.DMA((2 * NZ,))] * 2,
        compiler_params=pltpu.CompilerParams(collective_id=collective_id, has_side_effects=True),
        name="plane_swap",
    )(x)


def group_kernel(x_ref, out_ref, own_sem, send, recv):
    tp, dp, _, _ = place()
    group = [lax.rem(dp + n, 4) for n in range(1, 4)]
    for to in group:
        signal(tp, to)
    pl.semaphore_wait(pltpu.get_barrier_semaphore(), 3)
    own = pltpu.make_async_copy(x_ref, out_ref.at[dp], own_sem)
    own.start()
    for n, to in enumerate(group):
        remote(x_ref, out_ref.at[dp], send.at[n], recv.at[dp], tp, to).start()
    own.wait()
    for n, to in enumerate(group):
        remote(x_ref, out_ref.at[to], send.at[n], recv.at[to], tp, to).wait_recv()
        remote(x_ref, out_ref.at[dp], send.at[n], recv.at[dp], tp, to).wait_send()


def group_gather(x, collective_id):
    return pl.pallas_call(
        group_kernel,
        out_shape=jax.ShapeDtypeStruct((4,) + x.shape, x.dtype),
        in_specs=[ANY],
        out_specs=ANY,
        scratch_shapes=[pltpu.SemaphoreType.DMA, pltpu.SemaphoreType.DMA((3,)), pltpu.SemaphoreType.DMA((4,))],
        compiler_params=pltpu.CompilerParams(collective_id=collective_id, has_side_effects=True),
        name="group_gather",
    )(x)


GATHER_ORDER = {
    0: ((0, 0), (0, 1), (1, 0), (0, 2), (1, 1), (0, 3), (1, 2), (1, 3)),
    1: ((0, 1), (0, 0), (0, 2), (1, 1), (1, 0), (0, 3), (1, 2), (1, 3)),
    2: ((0, 2), (0, 1), (0, 3), (1, 2), (0, 0), (1, 3), (1, 1), (1, 0)),
    3: ((0, 3), (0, 2), (1, 3), (0, 1), (1, 2), (0, 0), (1, 1), (1, 0)),
}
GATHER_EVENTS = {
    0: {
        1: ((0, 1, 0, 'y'), (1, 0, 1, 'r'), (0, 1, 1, 'y'), (1, 0, 0, '')),
        3: ((0, 2, 0, 'y'), (1, 1, 0, ''), (0, 2, 1, 'y'), (1, 1, 1, '')),
        5: ((0, 3, 0, 'y'), (1, 2, 0, ''), (0, 3, 1, ''), (1, 2, 1, '')),
        7: ((1, 3, 0, ''), (1, 3, 1, '')),
    },
    1: {
        1: ((0, 0, 0, 'ry'), (0, 2, 0, 'ly'), (1, 1, 0, ''), (0, 0, 1, 'r'), (0, 2, 1, 'ly'), (1, 1, 1, '')),
        4: ((0, 3, 0, 'ly'), (1, 0, 0, ''), (1, 0, 1, 'r')),
        5: ((0, 3, 1, 'l'), (1, 2, 0, '')),
        6: ((1, 2, 1, ''), (1, 3, 1, 'l')),
        7: ((1, 3, 0, ''),),
    },
    2: {
        1: ((0, 1, 0, 'ry'), (0, 3, 0, 'ly'), (1, 2, 0, ''), (0, 1, 1, 'ry'), (0, 3, 1, 'l'), (1, 2, 1, '')),
        4: ((0, 0, 0, 'ry'), (1, 1, 0, ''), (1, 3, 1, 'l'), (0, 0, 1, 'r'), (1, 3, 0, '')),
        6: ((1, 0, 1, 'r'), (1, 1, 1, '')),
        7: ((1, 0, 0, ''),),
    },
    3: {
        1: ((0, 2, 0, 'y'), (1, 3, 1, 'l'), (0, 2, 1, 'y'), (1, 3, 0, '')),
        3: ((0, 1, 0, 'y'), (1, 2, 0, ''), (0, 1, 1, 'y'), (1, 2, 1, '')),
        5: ((0, 0, 0, 'y'), (1, 1, 0, ''), (0, 0, 1, ''), (1, 1, 1, '')),
        7: ((1, 0, 0, ''), (1, 0, 1, '')),
    },
}
SCATTER_ORDER = {
    0: ((1, 3), (1, 2), (0, 3), (1, 1), (0, 2), (1, 0), (0, 1), (0, 0)),
    1: ((1, 3), (1, 2), (0, 3), (1, 0), (1, 1), (0, 2), (0, 0), (0, 1)),
    2: ((1, 0), (1, 1), (1, 3), (0, 0), (1, 2), (0, 3), (0, 1), (0, 2)),
    3: ((1, 0), (1, 1), (0, 0), (1, 2), (0, 1), (1, 3), (0, 2), (0, 3)),
}
SCATTER_EVENTS = {
    0: {
        0: ((1, 3, 0, '', 'y'), (1, 3, 1, '', 'r')),
        1: ((1, 2, 0, '', 'y'), (1, 2, 1, '', 'y')),
        2: ((0, 3, 1, '', 'r'), (0, 3, 0, 'y', 'r')),
        3: ((1, 1, 0, '', 'y'), (1, 1, 1, '', 'y')),
        4: ((0, 2, 0, 'y', 'r'),),
        5: ((0, 2, 1, 'y', 'r'), (1, 0, 0, '', 'y')),
        6: ((1, 0, 1, 'r', 'y'), (0, 1, 0, 'y', 'r')),
        7: ((0, 1, 1, 'y', 'r'), (0, 0, 0, 'ry', ''), (0, 0, 1, 'ry', '')),
    },
    1: {
        0: ((1, 3, 0, '', 'y'),),
        1: ((1, 2, 0, '', 'y'), (1, 2, 1, '', 'y')),
        2: ((1, 3, 1, 'l', 'r'),),
        3: ((1, 0, 0, '', 'y'),),
        4: ((0, 3, 1, 'l', 'r'), (1, 0, 1, 'r', 'l'), (1, 1, 0, '', 'y'), (1, 1, 1, '', 'y')),
        6: ((0, 3, 0, 'ly', 'r'), (0, 0, 1, 'r', 'l')),
        7: ((0, 2, 0, 'ly', 'r'), (0, 0, 0, 'ry', 'l'), (0, 2, 1, 'ly', 'r'), (0, 1, 0, 'lry', ''), (0, 1, 1, 'lry', '')),
    },
    2: {
        0: ((1, 0, 0, '', 'y'),),
        1: ((1, 1, 0, '', 'y'), (1, 1, 1, '', 'y')),
        2: ((1, 0, 1, 'r', 'l'), (1, 3, 0, '', 'y')),
        4: ((1, 3, 1, 'l', 'r'), (0, 0, 1, 'r', 'l'), (1, 2, 0, '', 'y'), (1, 2, 1, '', 'y')),
        6: ((0, 0, 0, 'ry', 'l'), (0, 3, 1, 'l', 'r')),
        7: ((0, 1, 0, 'ry', 'l'), (0, 3, 0, 'ly', 'r'), (0, 1, 1, 'ry', 'l'), (0, 2, 0, 'lry', ''), (0, 2, 1, 'lry', '')),
    },
    3: {
        0: ((1, 0, 0, '', 'y'), (1, 0, 1, '', 'l')),
        1: ((1, 1, 0, '', 'y'), (1, 1, 1, '', 'y')),
        2: ((0, 0, 1, '', 'l'), (0, 0, 0, 'y', 'l')),
        3: ((1, 2, 0, '', 'y'), (1, 2, 1, '', 'y')),
        4: ((0, 1, 0, 'y', 'l'),),
        5: ((0, 1, 1, 'y', 'l'), (1, 3, 0, '', 'y')),
        6: ((1, 3, 1, 'l', 'y'), (0, 2, 0, 'y', 'l')),
        7: ((0, 2, 1, 'y', 'l'), (0, 3, 0, 'ly', ''), (0, 3, 1, 'ly', '')),
    },
}
SUB = 256
GROUP = 6


def lookup(table, z, step):
    value = jnp.int32(0)
    for k in range(NZ):
        for s in range(2 * NZ):
            value = value + jnp.where((z == k) & (step == s), table[k][s], 0)
    return value


def head_kernel(scale, token_scale, f_ref, lab_ref, e_ref, dfin_ref, ghead_ref, norm_ref, labsum_ref, z_ref,
                e_b, e_t, fbuf, f_b, g_acc, from_y, from_l, from_r, dl, z_buf, z_rest, lse_all, z_sem, load_sem, ag_send, ag_recv,
                send_y, send_l, send_r, recv_y, recv_l, recv_r, st_send, st_recv):
    tp, dp, z, y = place()
    partner = tp + 1 - 2 * y
    vocab, width = e_ref.shape
    own = f_ref.shape[0]
    whole = vocab // (SUB * GROUP)
    rest = vocab - whole * SUB * GROUP
    log2e = 1.4426950408889634
    slope = scale * log2e
    blocks = [(j * SUB, SUB) for j in range(GROUP)]
    tail = [(n, min(SUB, rest - n)) for n in range(0, rest, SUB)]

    plane_barrier(tp, dp, [])

    half = own // 2
    to_tp = {"l": tp - 2, "r": tp + 2, "y": partner}

    def slot_of(o, zz):
        return 2 * zz + (1 - y if o else y)

    def piece(ref, h):
        return ref.at[pl.ds(h * half, half), :]

    def pass_on(o, zz, h, to, own_chunk=False):
        slot = slot_of(o, zz)
        return remote(piece(f_ref if own_chunk else fbuf.at[slot], h), piece(fbuf.at[slot], h), ag_send.at["lry".index(to), slot, h],
                      ag_recv.at[slot, h], to_tp[to], dp)

    def arrived(o, zz, h):
        slot = slot_of(o, zz)
        remote(piece(f_ref, h), piece(fbuf.at[slot], h), ag_send.at[0, slot, h], ag_recv.at[slot, h], partner, dp).wait_recv()

    def own_sends(k):
        first = (1, 0) if k in (0, NZ - 1) else (0, 1)
        return [pass_on(0, k, h, "y", True) for h in first] + [
            pass_on(0, k, h, to, True) for h in range(2) for to in ("l" if k > 0 else "") + ("r" if k < NZ - 1 else "")]

    def on_position(f):
        for k in range(NZ):
            pl.when(z == k)(functools.partial(f, k))

    def first_sends(k):
        for c in own_sends(k):
            c.start()

    on_position(first_sends)
    load = pltpu.make_async_copy(e_ref, g_acc, load_sem.at[0])
    load.start()
    own_copy = pltpu.make_async_copy(f_ref, fbuf.at[tp], load_sem.at[1])
    own_copy.start()
    load.wait()

    def prepare(at, size):
        part = g_acc[at, :]
        e_b[at, :] = part.astype(BF16)
        e_t[:, at] = part.T.astype(BF16)

    def prepare_body(n, carry):
        prepare(pl.ds(pl.multiple_of(n * SUB, SUB), SUB), SUB)
        return carry

    lax.fori_loop(0, vocab // SUB, prepare_body, 0)
    if vocab % SUB:
        prepare(pl.ds(vocab // SUB * SUB, vocab % SUB), vocab % SUB)
    own_copy.wait()

    big = SUB * GROUP

    def z_copies(slot, n, out):
        if n is None:
            pair = (z_rest, z_ref.at[slot, pl.ds(whole * big, rest), :])
            sem = z_sem.at[2]
        else:
            pair = (z_buf.at[lax.rem(n, 2)], z_ref.at[slot, pl.ds(pl.multiple_of(n * big, big), big), :])
            sem = z_sem.at[lax.rem(n, 2)]
        return pltpu.make_async_copy(*(pair if out else pair[::-1]), sem)

    def slot_at(order, step):
        code = lookup({k: [2 * zz + o for o, zz in order[k]] for k in range(NZ)}, z, step)
        other = code % 2
        return code // 2 * 2 + y + other - 2 * y * other

    def gather_step(step, carry):
        for k in range(NZ):
            for at, events in GATHER_EVENTS[k].items():
                def serve(events=events):
                    for o, zz, h, to in events:
                        arrived(o, zz, h)
                        for t in to:
                            pass_on(o, zz, h, t).start()
                pl.when((z == k) & (step == at))(serve)
        slot = slot_at(GATHER_ORDER, step)
        f_b[slot] = fbuf[slot].astype(BF16)
        f_now = f_b[slot]

        def group(base, parts, kept, c):
            top, total = c
            for first, size in parts:
                logit = lax.dot_general(e_b[pl.ds(base + first, size), :], f_now, (((1,), (1,)), ((), ())), preferred_element_type=F32)
                kept[pl.ds(first, size), :] = logit
                logit = logit.reshape(size // 8, 8, own)
                new = jnp.maximum(top, jnp.max(logit, axis=0))
                total = total * jnp.exp2((top - new) * slope) + jnp.sum(jnp.exp2((logit - new[None]) * slope), axis=0)
                top = new
            return top, total

        def body(n, c):
            @pl.when(step * whole + n >= 2)
            def _():
                z_copies(slot, n, True).wait()
            c = group(pl.multiple_of(n * big, big), blocks, z_buf.at[lax.rem(n, 2)], c)
            z_copies(slot, n, True).start()
            return c

        top, total = lax.fori_loop(0, whole, body, (jnp.full((8, own), -3e38, F32), jnp.zeros((8, own), F32)))
        if tail:
            @pl.when(step > 0)
            def _():
                z_copies(slot, None, True).wait()
            top, total = group(whole * big, tail, z_rest, (top, total))
            z_copies(slot, None, True).start()
        most = jnp.max(top, axis=0, keepdims=True)
        total = jnp.sum(total * jnp.exp2((top - most) * slope), axis=0, keepdims=True)
        lse_all[tp, pl.ds(slot, 1), :] = most * scale + jnp.log(total)
        return carry

    lax.fori_loop(0, 2 * NZ, gather_step, 0)
    for n in range(2):
        z_copies(0, jnp.int32(n), True).wait()
    if tail:
        z_copies(0, None, True).wait()

    for n in range(1, 2 * NZ):
        to = lax.rem(tp + n, 2 * NZ)
        remote(lse_all.at[tp], lse_all.at[tp], st_send.at[to], st_recv.at[tp], to, dp).start()

    def gathers_done(k):
        for c in own_sends(k):
            c.wait_send()
        for events in GATHER_EVENTS[k].values():
            for o, zz, h, to in events:
                for t in to:
                    pass_on(o, zz, h, t).wait_send()

    on_position(gathers_done)
    start_slot = slot_at(SCATTER_ORDER, 0)
    for n in range(2):
        z_copies(start_slot, jnp.int32(n), False).start()
    if tail:
        z_copies(start_slot, None, False).start()

    def clear(n, carry):
        g_acc[pl.ds(pl.multiple_of(n * 16, 16), 16), :] = jnp.zeros((16, width), F32)
        return carry

    lax.fori_loop(0, vocab // 16, clear, 0)
    for n in range(1, 2 * NZ):
        source = lax.rem(tp + n, 2 * NZ)
        remote(lse_all.at[source], lse_all.at[source], st_send.at[source], st_recv.at[source], source, dp).wait_recv()
    peak = jnp.max(lse_all[...], axis=0)
    log_norm = peak + jnp.log(jnp.sum(jnp.exp(lse_all[...] - peak[None]), axis=0))
    norm_ref[...] = log_norm

    def leave(o, zz, h, to):
        src = piece(fbuf.at[slot_of(o, zz)], h)
        if to == "y":
            at = 2 * zz + h
            return remote(src, from_y.at[at], send_y.at[at], recv_y.at[at], partner, dp)
        if to == "l":
            at = 6 if o else 2 * zz + h
            return remote(src, from_r.at[at], send_l.at[at], recv_r.at[at], tp - 2, dp)
        at = 6 if o else 2 * zz - 2 + h
        return remote(src, from_l.at[at], send_r.at[at], recv_l.at[at], tp + 2, dp)

    def collect(o, zz, h, sums, to):
        here = piece(fbuf.at[slot_of(o, zz)], h)
        for d in sums:
            at, buf, sem = {"y": (2 * zz + h, from_y, recv_y), "l": (6 if o else 2 * zz - 2 + h, from_l, recv_l),
                            "r": (6 if o else 2 * zz + h, from_r, recv_r)}[d]
            remote(here, buf.at[at], send_y.at[0], sem.at[at], partner, dp).wait_recv()
            add_into(here, buf.at[at])
        if to:
            leave(o, zz, h, to).start()

    def scatter_step(step, lab_sum):
        slot = slot_at(SCATTER_ORDER, step)
        f_now = f_b[slot]
        acc = fbuf.at[slot]
        norm = norm_ref[pl.ds(slot, 1), :]
        shift = norm * log2e
        coef = (1.0 + 2.0 * LOGIT_ZLOSS * norm) * token_scale
        lab = lab_ref[pl.ds(slot // 2, 1), pl.ds(pl.multiple_of(lax.rem(slot, 2) * own, own), own)] - tp * vocab
        acc[...] = jnp.zeros((width, own), F32)

        def group(base, parts, kept, hits):
            for first, size in parts:
                at = pl.ds(base + first, size)
                logit = kept[pl.ds(first, size), :]
                hit = lax.broadcasted_iota(jnp.int32, (size, own), 0) == lab - (base + first)
                prob = jnp.exp2(logit * slope - shift) * coef
                grad = jnp.where(hit, prob - token_scale, prob).astype(BF16)
                hits = hits + jnp.sum(jnp.where(hit, logit, 0.0).reshape(size // 8, 8, own), axis=0)
                dl[pl.ds(first, size), :] = grad
                g_acc[at, :] += jnp.dot(grad, f_now, preferred_element_type=F32)
            size = parts[-1][0] + parts[-1][1]
            acc[...] += jnp.dot(e_t[:, pl.ds(base, size)], dl[pl.ds(0, size), :], preferred_element_type=F32)
            return hits

        following = slot_at(SCATTER_ORDER, jnp.minimum(step + 1, 2 * NZ - 1))

        def body(n, hits):
            z_copies(slot, n, False).wait()
            hits = group(pl.multiple_of(n * big, big), blocks, z_buf.at[lax.rem(n, 2)], hits)

            @pl.when(n + 2 < whole)
            def _():
                z_copies(slot, n + 2, False).start()

            @pl.when((n + 2 >= whole) & (step + 1 < 2 * NZ))
            def _():
                z_copies(following, n + 2 - whole, False).start()
            return hits

        lab_sum = lax.fori_loop(0, whole, body, lab_sum)
        if tail:
            z_copies(slot, None, False).wait()
            lab_sum = group(whole * big, tail, z_rest, lab_sum)

            @pl.when(step + 1 < 2 * NZ)
            def _():
                z_copies(following, None, False).start()

        for k in range(NZ):
            for at, events in SCATTER_EVENTS[k].items():
                def reduce(events=events):
                    for event in events:
                        collect(*event)
                pl.when((z == k) & (step == at))(reduce)
        return lab_sum

    lab_sum = lax.fori_loop(0, 2 * NZ, scatter_step, jnp.zeros((8, own), F32))
    labsum_ref[...] = lab_sum
    store = pltpu.make_async_copy(g_acc, ghead_ref, load_sem.at[0])
    store.start()
    dfin_ref[...] = fbuf[tp].T

    def scatters_done(k):
        for events in SCATTER_EVENTS[k].values():
            for o, zz, h, _, to in events:
                if to:
                    leave(o, zz, h, to).wait_send()

    on_position(scatters_done)
    for n in range(1, 2 * NZ):
        to = lax.rem(tp + n, 2 * NZ)
        remote(lse_all.at[tp], lse_all.at[tp], st_send.at[to], st_recv.at[tp], to, dp).wait_send()
    store.wait()


def head(f_own, labels, embed, scale, token_scale, collective_id):
    own, width = f_own.shape
    vocab = embed.shape[0]
    chunk = (own, width)
    strips = lambda n: pltpu.VMEM((n, own // 2, width), F32)
    dma = lambda *n: pltpu.SemaphoreType.DMA(n)
    return pl.pallas_call(
        functools.partial(head_kernel, scale, token_scale),
        out_shape=(jax.ShapeDtypeStruct((own, width), F32), jax.ShapeDtypeStruct((vocab, width), F32),
                   jax.ShapeDtypeStruct((2 * NZ, own), F32), jax.ShapeDtypeStruct((8, own), F32),
                   jax.ShapeDtypeStruct((2 * NZ, vocab, own), F32)),
        in_specs=[VMEM, VMEM, ANY],
        out_specs=(VMEM, ANY, VMEM, VMEM, ANY),
        scratch_shapes=[pltpu.VMEM((vocab, width), BF16), pltpu.VMEM((width, vocab), BF16),
                        pltpu.VMEM((2 * NZ,) + chunk, F32), pltpu.VMEM((2 * NZ,) + chunk, BF16), pltpu.VMEM((vocab, width), F32),
                        strips(8), strips(7), strips(7),
                        pltpu.VMEM((SUB * GROUP, own), BF16), pltpu.VMEM((2, SUB * GROUP, own), F32),
                        pltpu.VMEM((max(vocab % (SUB * GROUP), 8), own), F32), pltpu.VMEM((2 * NZ, 2 * NZ, own), F32),
                        dma(3), dma(2), dma(3, 2 * NZ, 2), dma(2 * NZ, 2), dma(8), dma(7), dma(7), dma(8), dma(7), dma(7), dma(2 * NZ), dma(2 * NZ)],
        compiler_params=pltpu.CompilerParams(collective_id=collective_id, has_side_effects=True, vmem_limit_bytes=67000000),
        cost_estimate=pl.CostEstimate(flops=8 * vocab * width * own * 8, bytes_accessed=3 * 4 * vocab * width, transcendentals=2 * vocab * own * 8),
        name="head",
    )(f_own, labels, embed)


TB = (((1,), (1,)), ((), ()))
TA = (((0,), (0,)), ((), ()))
LOG2E = 1.4426950408889634


def mm(a, b, dims=(((1,), (0,)), ((), ()))):
    return lax.dot_general(a, b, dims, preferred_element_type=F32)


def picks(code, n_slots):
    return (lax.broadcasted_iota(jnp.int32, (n_slots, code.shape[1]), 0) == code).astype(F32).astype(BF16)


def turn(lo, hi, cos_t, sin_t):
    return lo * cos_t - hi * sin_t, hi * cos_t + lo * sin_t


EVENTS = {
    0: (((("R", 1),), (0,)), ((("R", 2),), (1,)), ((("R", 3),), (2,)), ((), (3,))),
    1: (((("L", 0), ("R", 2)), (1,)), ((("R", 3),), (0,)), ((), (2,)), ((), (3,))),
    2: (((("R", 3), ("L", 1)), (2,)), ((("L", 0),), (3,)), ((), (1,)), ((), (0,))),
    3: (((("L", 2),), (3,)), ((("L", 1),), (2,)), ((("L", 0),), (1,)), ((), (0,))),
}
MLP_ORDER = {k: [2 * k] + [code for line, other in EVENTS[k] for code in [2 * zz for _, zz in line] + [2 * zz + 1 for zz in other]] for k in range(NZ)}


def front_kernel(ids_ref, e_ref, rounds_ref, code_ref, extra_ref, w_ref, wkv_ref, ln_ref, cos_ref, sin_ref,
                 f_ref, x1_ref, x0_ref, q_ref, kv_ref, kvt_ref, lse_ref, ctx_ref, wq_ref, wo_ref, wg_out, wu_out, wd_out, rounds_all,
                 wg_ref, wu_ref, wd_ref, w_sem, table, rows_ref, wl, rows_in, u_b, kv_out, kv_in, own_sem, r_send, r_recv, a_y, a_l, a_r, a_c, a_recv,
                 b_y, b_l, b_r, b_x, b_c, b_recv, kv_send, kv_recv, n_send, n_recv):
    tp, dp, z, y = place()
    partner = tp + 1 - 2 * y
    core = dp % 2
    twin = dp + 1 - 2 * core
    facing = lax.rem(dp + 2, 4)
    own, width = x0_ref.shape
    shards, w_rows = wl.shape[0], wl.shape[1]
    nq = q_ref.shape[0]
    ff = wg_out.shape[0]
    n_a = nq // shards
    n_f = ff // shards
    n_b = 3 * n_f // 4
    hd = kv_out.shape[0] // 2
    quarter = hd // 2
    heads = nq // hd

    def a_rows(c):
        return pl.ds(pl.multiple_of(c * n_a, 8), n_a)

    def b_rows(d):
        return pl.ds(pl.multiple_of(2 * n_a + d * n_b, 8), n_b)

    def a_copy(slot, sems, to, to_dp, first=False):
        src = w_ref.at[a_rows(core), :] if first else wl.at[slot, a_rows(core), :]
        return remote(src, wl.at[slot, a_rows(core), :], sems.at[slot], a_recv.at[slot, core], to, to_dp)

    def b_copy(slot, piece, sems, to, to_dp, first=False):
        src = w_ref.at[b_rows(piece), :] if first else wl.at[slot, b_rows(piece), :]
        return remote(src, wl.at[slot, b_rows(piece), :], sems.at[slot], b_recv.at[slot, piece], to, to_dp)

    def a_wait(slot, c):
        remote(w_ref.at[a_rows(c), :], wl.at[slot, a_rows(c), :], a_y.at[slot], a_recv.at[slot, c], partner, dp).wait_recv()

    def b_wait(slot, piece):
        remote(w_ref.at[b_rows(piece), :], wl.at[slot, b_rows(piece), :], b_y.at[slot], b_recv.at[slot, piece], partner, dp).wait_recv()

    def on_position(f):
        for k in range(NZ):
            pl.when(z == k)(functools.partial(f, k))

    def line_sends(k, make, y_sems, l_sems, r_sems, slot, side, first=False):
        sends = [make(slot, y_sems, partner, dp, first)]
        if k > 0 and side != "L":
            sends.append(make(slot, l_sems, tp - 2, dp, first))
        if k < NZ - 1 and side != "R":
            sends.append(make(slot, r_sems, tp + 2, dp, first))
        return sends

    def b_own(slot, sems, to, to_dp, first=False):
        return b_copy(slot, dp, sems, to, to_dp, first)

    def a_sends(k, slot, side, first=False):
        return line_sends(k, a_copy, a_y, a_l, a_r, slot, side, first)

    def b_sends(k, slot, side, first=False):
        return line_sends(k, b_own, b_y, b_l, b_r, slot, side, first)

    def start(copies):
        for c in copies:
            c.start()

    load = pltpu.make_async_copy(e_ref, table, own_sem.at[2])
    load.start()
    group = [twin, facing, lax.rem(twin + 2, 4)]
    plane_barrier(tp, dp, [(tp, d) for d in group])
    peers = [lax.rem(tp + n, shards) for n in range(1, shards)]

    def rounds_copy(n):
        return remote(rounds_ref, rounds_all.at[dp], n_send.at[n], n_recv.at[dp], tp, group[n])

    for n in range(3):
        rounds_copy(n).start()
    rounds_all[dp] = rounds_ref[...]

    def row_copy(to):
        return remote(rows_ref.at[to], rows_in.at[tp], r_send.at[to], r_recv.at[tp], to, dp)

    on_position(lambda k: start(b_sends(k, tp, "", True)))
    on_position(lambda k: start(a_sends(k, tp, "", True)))
    own_w = pltpu.make_async_copy(w_ref, wl.at[tp], own_sem.at[1])
    own_w.start()

    def a_event(t, k):
        line, other = EVENTS[k][t]
        for side, zz in line:
            slot = 2 * zz + y
            a_wait(slot, core)
            start(a_sends(k, slot, side))
            a_copy(slot, a_c, tp, twin).start()
        for zz in other:
            slot = 2 * zz + 1 - y
            a_wait(slot, core)
            a_copy(slot, a_c, tp, twin).start()

    def b_event(t, k):
        line, other = EVENTS[k][t]
        for side, zz in line:
            slot = 2 * zz + y
            b_wait(slot, dp)
            start(b_sends(k, slot, side))
            b_copy(slot, dp, b_x, tp, facing).start()
            b_copy(slot, dp, b_c.at[0], tp, twin).start()
        for zz in other:
            slot = 2 * zz + 1 - y
            b_wait(slot, dp)
            b_copy(slot, dp, b_x, tp, facing).start()
            b_copy(slot, dp, b_c.at[0], tp, twin).start()

    load.wait()
    cap = rows_ref.shape[1]

    def pick_rows(n, carry):
        for i in range(8):
            rows_ref[n // (cap // 8), pl.ds(lax.rem(n, cap // 8) * 8 + i, 1), :] = table[pl.ds(ids_ref[n * 8 + i], 1), :]
        return carry

    lax.fori_loop(0, shards * cap // 8, pick_rows, 0)
    on_position(functools.partial(b_event, 0))
    on_position(functools.partial(a_event, 0))
    on_position(lambda k: start([row_copy(2 * zz + (1 - y if o else y)) for o, zz in near_first(k)[1:]]))
    own_rows = pltpu.make_async_copy(rows_ref.at[tp], rows_in.at[tp], own_sem.at[0])
    own_rows.start()
    on_position(functools.partial(b_event, 1))
    on_position(functools.partial(a_event, 1))
    own_rows.wait()
    for source in peers:
        remote(rows_ref.at[source], rows_in.at[source], r_send.at[source], r_recv.at[source], source, dp).wait_recv()
    n_slots = shards * cap
    x0_ref[...] = extra_ref[...] + mm(picks(code_ref[...], n_slots), rows_in[...].reshape(n_slots, width).astype(BF16), TA)
    u_b[...] = norm_fwd(x0_ref[...], ln_ref[0:1, :])[0]
    x1_ref[...] = x0_ref[...]
    cos_t = cos_ref[...]
    sin_t = sin_ref[...]
    kv = mm(wkv_ref[...].reshape(2 * hd, width).astype(BF16), u_b[...], TB)
    lo, hi = turn(kv[:quarter], kv[quarter:hd], cos_t, sin_t)
    kv_out[0:quarter, :] = lo
    kv_out[quarter:hd, :] = hi
    kv_out[hd:, :] = kv[hd:]
    kv_copy = remote(kv_out, kv_in, kv_send, kv_recv, partner, dp)
    kv_copy.start()

    def slot_of(step):
        code = lookup(MLP_ORDER, z, step)
        other = code % 2
        return code // 2 * 2 + y + other - 2 * y * other

    def w_stores(slot):
        at = pl.ds(pl.multiple_of(slot * n_f, n_f), n_f)
        return [pltpu.make_async_copy(src.at[at, :], dst.at[at, :], w_sem.at[i, slot])
                for i, (src, dst) in enumerate(((wg_ref, wg_out), (wu_ref, wu_out), (wd_ref, wd_out)))]

    def mlp(step, carry):
        def pass_on():
            slot = slot_of(step + 1)
            b_wait(slot, facing)
            b_copy(slot, facing, b_c.at[1], tp, twin).start()
        pl.when(step < shards - 1)(pass_on)
        slot = slot_of(step)

        def rest():
            b_wait(slot, twin)
            b_wait(slot, lax.rem(twin + 2, 4))
        pl.when(step > 0)(rest)
        at = pl.ds(pl.multiple_of(slot * n_f, n_f), n_f)
        wg_ref[at, :] = wl[slot, 2 * n_a:2 * n_a + n_f, :].astype(BF16)
        wu_ref[at, :] = wl[slot, 2 * n_a + n_f:2 * n_a + 2 * n_f, :].astype(BF16)
        wd_ref[at, :] = wl[slot, 2 * n_a + 2 * n_f:2 * n_a + 3 * n_f, :].astype(BF16)
        for c in w_stores(slot):
            c.start()
        gate = mm(u_b[...], wg_ref[at, :], TB)
        up = mm(u_b[...], wu_ref[at, :], TB)
        x1_ref[...] += mm((gate * jax.nn.sigmoid(gate) * up).astype(BF16), wd_ref[at, :])
        return carry

    own_w.wait()
    lax.fori_loop(0, 3, mlp, 0)
    on_position(functools.partial(b_event, 2))
    on_position(functools.partial(a_event, 2))
    lax.fori_loop(3, 4, mlp, 0)
    on_position(functools.partial(a_event, 3))
    on_position(functools.partial(b_event, 3))
    for source in peers:
        a_wait(source, 1 - core)
    for s in range(shards):
        wq_ref[s * n_a:(s + 1) * n_a, :] = wl[s, 0:n_a, :].astype(BF16)
        wo_ref[s * n_a:(s + 1) * n_a, :] = wl[s, n_a:2 * n_a, :].astype(BF16)

    q_all = mm(wq_ref[...], u_b[...], TB)
    for h in range(heads):
        lo, hi = turn(q_all[h * hd:h * hd + quarter], q_all[h * hd + quarter:(h + 1) * hd], cos_t, sin_t)
        q_ref[h * hd:h * hd + quarter, :] = lo.astype(BF16)
        q_ref[h * hd + quarter:(h + 1) * hd, :] = hi.astype(BF16)
    kv_copy.wait()

    def fill(mine, other):
        kv_ref[mine * own:(mine + 1) * own, :] = kv_out[...].T.astype(BF16)
        kv_ref[other * own:(other + 1) * own, :] = kv_in[...].T.astype(BF16)
        kvt_ref[:, mine * own:(mine + 1) * own] = kv_out[...].astype(BF16)
        kvt_ref[:, other * own:(other + 1) * own] = kv_in[...].astype(BF16)

    pl.when(y == 0)(lambda: fill(0, 1))
    pl.when(y == 1)(lambda: fill(1, 0))
    blank = jnp.zeros((hd, own), BF16)
    slope = hd ** -0.5 * LOG2E

    def attend(h, carry):
        at = pl.ds(pl.multiple_of(h * hd, hd), hd)
        scores = mm(kv_ref[...], jnp.concatenate([q_ref[at, :], blank], axis=0))
        allowed = lax.broadcasted_iota(jnp.int32, scores.shape, 0) <= lax.broadcasted_iota(jnp.int32, scores.shape, 1) + y * own
        scores = jnp.where(allowed, scores * slope, -1e30)
        top = jnp.max(scores, axis=0, keepdims=True)
        prob = jnp.exp2(scores - top)
        total = jnp.sum(prob, axis=0, keepdims=True)
        lse_ref[pl.ds(h, 1), :] = top + jnp.log2(total)
        ctx_ref[at, :] = mm(kvt_ref[hd:, :], (prob * (1.0 / total)).astype(BF16)).astype(BF16)
        return carry

    lax.fori_loop(0, heads, attend, 0)
    x1_ref[...] += mm(ctx_ref[...], wo_ref[...], TA)

    lax.fori_loop(4, shards, mlp, 0)
    f_ref[...] = norm_fwd(x1_ref[...], ln_ref[1:2, :])[0].astype(F32)

    def finish(k):
        done = a_sends(k, tp, "", True) + b_sends(k, tp, "", True)
        for line, other in EVENTS[k]:
            for side, zz in line:
                done += a_sends(k, 2 * zz + y, side) + b_sends(k, 2 * zz + y, side)
        for c in done:
            c.wait_send()

    on_position(finish)
    for slot in range(shards):
        for c in w_stores(slot):
            c.wait()
    for n in range(3):
        rounds_copy(n).wait_send()
        remote(rounds_ref, rounds_all.at[group[n]], n_send.at[n], n_recv.at[group[n]], tp, twin).wait_recv()
    for to in peers:
        row_copy(to).wait_send()
        a_copy(to, a_c, tp, twin).wait_send()
        b_copy(to, dp, b_x, tp, facing).wait_send()
        b_copy(to, dp, b_c.at[0], tp, twin).wait_send()
        b_copy(to, facing, b_c.at[1], tp, twin).wait_send()


def front(ids, embed, rounds, code, extra, w_rows, wkv_t, ln, cos_t, sin_t, n_q, collective_id):
    own, width = extra.shape
    two_hd = 2 * wkv_t.shape[1]
    shards = 2 * NZ
    ff = (w_rows.shape[0] * shards - 2 * n_q) // 3
    dma = lambda *n: pltpu.SemaphoreType.DMA(n)
    s = jax.ShapeDtypeStruct
    rows = (shards, ids.shape[0] // shards, width)
    return pl.pallas_call(
        front_kernel,
        out_shape=(s((own, width), F32),) * 3 + (s((n_q, own), BF16), s((2 * own, two_hd), BF16), s((two_hd, 2 * own), BF16),
                   s((2 * n_q // two_hd, own), F32), s((n_q, own), BF16), s((n_q, width), BF16), s((n_q, width), BF16))
        + (s((ff, width), BF16),) * 3 + (s((4, 1, 128), jnp.int32),),
        in_specs=[pl.BlockSpec(memory_space=pltpu.SMEM), ANY, VMEM, VMEM, VMEM, ANY] + [VMEM] * 4,
        out_specs=(VMEM,) * 10 + (ANY,) * 3 + (VMEM,),
        scratch_shapes=[pltpu.VMEM((ff, width), BF16)] * 3 + [dma(3, shards), pltpu.VMEM(embed.shape, F32), pltpu.VMEM(rows, F32), pltpu.VMEM((shards,) + w_rows.shape, F32), pltpu.VMEM(rows, F32), pltpu.VMEM((own, width), BF16),
                        pltpu.VMEM((two_hd, own), F32), pltpu.VMEM((two_hd, own), F32),
                        dma(3), dma(shards), dma(shards)] + [dma(shards)] * 4 + [dma(shards, 2)]
        + [dma(shards)] * 4 + [dma(2, shards), dma(shards, 4), pltpu.SemaphoreType.DMA, pltpu.SemaphoreType.DMA, dma(3), dma(4)],
        compiler_params=pltpu.CompilerParams(collective_id=collective_id, has_side_effects=True, vmem_limit_bytes=60000000),
        name="front",
    )(ids, embed, rounds, code, extra, w_rows, wkv_t, ln, cos_t, sin_t)


def layer_bwd_kernel(scale, tok_total, dfin_ref, x0_ref, x1_ref, norm_ref, hits_ref, ln_ref, cos_ref, sin_ref, wq_ref, wkv_ref, wo_ref, wg_any, wu_any, wd_any,
                     q_ref, kv_ref, kvt_ref, lse_ref, ctx_ref, code_ref, g_ref, ids_ref, rows_ref, d0_ref, back_ref, early_ref, ids_all, d_one, d_b, u_b, dctx, dq, dkv, dkv_in,
                     hid, d_gate, d_up, rows_out, g_q, g_o, g_g, g_u, g_d, small, s_early, c_early, wg_ref, wu_ref, wd_ref, w_sem, out_sem, send_sem, recv_sem,
                     r_send, x_send, c_send, r_recv, g_load, g_send, g_recv, id_send, id_recv):
    tp, dp, z, y = place()
    partner = tp + 1 - 2 * y
    core = dp % 2
    twin = dp + 1 - 2 * core
    facing = lax.rem(dp + 2, 4)
    across = lax.rem(twin + 2, 4)
    own, width = x0_ref.shape
    hd = kv_ref.shape[1] // 2
    quarter = hd // 2
    nq = q_ref.shape[0]
    heads = nq // hd
    ff = wg_ref.shape[0]
    shards = rows_ref.shape[0]
    w_loads = [pltpu.make_async_copy(src, dst, w_sem.at[i]) for i, (src, dst) in enumerate(((wg_any, wg_ref), (wu_any, wu_ref), (wd_any, wd_ref)))]
    for c in w_loads:
        c.start()
    plane_barrier(tp, dp, [(tp, twin), (tp, facing), (tp, across)])

    n_early, g_size = s_early.shape[0], s_early.shape[1]

    def g_rows(which, b):
        return g_ref.at[pl.ds(pl.multiple_of(which * (g_ref.shape[0] // 2) + b * g_size, 8), g_size), :]

    def g_load_copy(b):
        return pltpu.make_async_copy(g_rows(core, b), s_early.at[b], g_load.at[b])

    def g_chip_copy(b):
        return remote(g_rows(1 - core, b), c_early.at[b], g_send.at[0, b], g_recv.at[0, b], tp, twin)

    def g_x_copy(b):
        return remote(s_early.at[b], early_ref.at[b], g_send.at[1, b], g_recv.at[1, b], tp, facing)

    for b in range(n_early):
        g_chip_copy(b).start()
        g_load_copy(b).start()

    def ids_copy(n, to):
        return remote(ids_ref, ids_all.at[dp], id_send.at[n], id_recv.at[dp], tp, to)

    for n, to in enumerate((twin, facing, across)):
        ids_copy(n, to).start()
    ids_all[dp] = ids_ref[...]
    _, f_hat, f_inv = norm_fwd(x1_ref[...], ln_ref[1:2, :])
    d_in, g_fin = norm_bwd(dfin_ref[...], f_hat, f_inv, ln_ref[1:2, :])
    d_one[...] = d_in
    d_b[...] = d_in.astype(BF16)
    u_b[...] = norm_fwd(x0_ref[...], ln_ref[0:1, :])[0]
    dctx[...] = mm(wo_ref[...], d_b[...], TB).astype(BF16)
    for b in range(n_early):
        g_load_copy(b).wait()
        g_chip_copy(b).wait_recv()
        add_into(s_early.at[b], c_early.at[b], 24)
        g_x_copy(b).start()
    cos_t = cos_ref[...]
    sin_t = sin_ref[...]
    blank = jnp.zeros((hd, own), BF16)
    slope = hd ** -0.5 * LOG2E
    dkv[...] = jnp.zeros_like(dkv)

    def attend(h, carry):
        at = pl.ds(pl.multiple_of(h * hd, hd), hd)
        q_pad = jnp.concatenate([q_ref[at, :], blank], axis=0)
        d_pad = jnp.concatenate([blank, dctx[at, :]], axis=0)
        scores = mm(kv_ref[...], q_pad)
        allowed = lax.broadcasted_iota(jnp.int32, scores.shape, 0) <= lax.broadcasted_iota(jnp.int32, scores.shape, 1) + y * own
        prob = jnp.where(allowed, jnp.exp2(scores * slope - lse_ref[pl.ds(h, 1), :]), 0.0)
        d_prob = mm(kv_ref[...], d_pad)
        mean = jnp.sum(d_prob * prob, axis=0, keepdims=True)
        d_score = (prob * (d_prob - mean) * hd ** -0.5).astype(BF16)
        dkv[...] += mm(d_score, q_pad, TB) + mm(prob.astype(BF16), d_pad, TB)
        d_q = mm(kvt_ref[0:hd, :], d_score)
        lo, hi = turn(d_q[:quarter], d_q[quarter:], cos_t, -sin_t)
        dq[at, :] = jnp.concatenate([lo, hi], axis=0).astype(BF16)
        return carry

    lax.fori_loop(0, heads, attend, 0)
    copy = remote(dkv.at[pl.ds(pl.multiple_of((1 - y) * own, own), own), :], dkv_in, send_sem, recv_sem, partner, dp)
    copy.start()

    d0_ref[...] = mm(dq[...], wq_ref[...], TA)
    step = min(512, ff)
    for c in w_loads:
        c.wait()

    def mlp(n, carry):
        at = pl.ds(pl.multiple_of(n * step, step), step)
        gate = mm(wg_ref[at, :], u_b[...], TB)
        up = mm(wu_ref[at, :], u_b[...], TB)
        d_hidden = mm(wd_ref[at, :], d_b[...], TB)
        sig = jax.nn.sigmoid(gate)
        hid[at, :] = (gate * sig * up).astype(BF16)
        d_gate[at, :] = (d_hidden * up * sig * (1.0 + gate * (1.0 - sig))).astype(BF16)
        d_up[at, :] = (d_hidden * gate * sig).astype(BF16)
        d0_ref[...] += mm(d_gate[at, :], wg_ref[at, :], TA) + mm(d_up[at, :], wu_ref[at, :], TA)
        return carry

    lax.fori_loop(0, ff // step, mlp, 0)
    copy.wait()
    d_kv = (dkv[pl.ds(pl.multiple_of(y * own, own), own), :] + dkv_in[...]).T
    lo, hi = turn(d_kv[:quarter], d_kv[quarter:hd], cos_t, -sin_t)
    d_kv = jnp.concatenate([lo, hi, d_kv[hd:]], axis=0).astype(BF16)
    small[0:2 * hd, :] = mm(d_kv, u_b[...])
    d_u = d0_ref[...] + mm(d_kv, wkv_ref[...].reshape(2 * hd, width).astype(BF16), TA)
    _, u_hat, u_inv = norm_fwd(x0_ref[...], ln_ref[0:1, :])
    d_in, g_in = norm_bwd(d_u, u_hat, u_inv, ln_ref[0:1, :])
    d_zero = d_one[...] + d_in
    d0_ref[...] = d_zero
    high = d_zero.astype(BF16)
    left = d_zero - high.astype(F32)
    middle = left.astype(BF16)
    low = (left - middle.astype(F32)).astype(BF16)
    pick = picks(code_ref[...], rows_out.shape[0] * rows_out.shape[1])
    rows_out[...] = (mm(pick, high) + mm(pick, middle) + mm(pick, low)).reshape(rows_out.shape)

    def row_copy(to):
        return remote(rows_out.at[to], back_ref.at[dp, tp], r_send.at[to], r_recv.at[dp, tp], to, dp)

    def x_copy(slot):
        return remote(back_ref.at[dp, slot], back_ref.at[dp, slot], x_send.at[slot], r_recv.at[dp, slot], tp, facing)

    def c_copy(group, n, slot):
        return remote(back_ref.at[group, slot], back_ref.at[group, slot], c_send.at[n, slot], r_recv.at[group, slot], tp, twin)

    def back(group, slot):
        remote(rows_out.at[slot], back_ref.at[group, slot], r_send.at[slot], r_recv.at[group, slot], tp, twin).wait_recv()

    def slot_of(o, zz):
        return 2 * zz + (1 - y if o else y)

    def on_position(f):
        for k in range(NZ):
            pl.when(z == k)(functools.partial(f, k))

    def rows_leave(k):
        for c in near_first(k)[1:]:
            row_copy(slot_of(*c)).start()

    on_position(rows_leave)
    own_rows = pltpu.make_async_copy(rows_out.at[tp], back_ref.at[dp, tp], out_sem.at[7 * 2 * NZ])
    own_rows.start()
    own_rows.wait()
    x_copy(tp).start()
    c_copy(dp, 0, tp).start()

    g_o[...] = mm(ctx_ref[...], d_b[...])
    g_q[...] = mm(dq[...], u_b[...])

    def weight_grads(n, carry):
        at = pl.ds(pl.multiple_of(n * step, step), step)
        g_d[at, :] = mm(hid[at, :], d_b[...])
        g_g[at, :] = mm(d_gate[at, :], u_b[...])
        g_u[at, :] = mm(d_up[at, :], u_b[...])
        return carry

    lax.fori_loop(0, ff // step, weight_grads, 0)
    small[2 * hd:, :] = jnp.zeros_like(small[2 * hd:, :])
    small[2 * hd:2 * hd + 1, :] = g_in.reshape(1, width)
    small[2 * hd + 1:2 * hd + 2, :] = g_fin.reshape(1, width)
    norm = norm_ref[pl.ds(tp, 1), :]
    hits = jnp.sum(hits_ref[...], axis=0, keepdims=True)
    small[2 * hd + 2:2 * hd + 3, :] = (norm + LOGIT_ZLOSS * norm * norm - hits * scale) / tok_total
    copies = []

    def put(src, first, size, s):
        copies.append(pltpu.make_async_copy(src, rows_ref.at[s, pl.ds(first, size), :], out_sem.at[len(copies)]))

    n_kv = 2 * hd // shards
    for s in range(shards):
        at = 0
        for g, size in ((g_q, nq // shards), (g_o, nq // shards), (g_g, ff // shards), (g_u, ff // shards), (g_d, ff // shards)):
            put(g.at[pl.ds(s * size, size), :], at, size, s)
            at += size
        put(small.at[pl.ds(s * n_kv, n_kv), :], at, n_kv, s)
        put(small.at[pl.ds(2 * hd + (0 if s == 0 else 16), 16), :], at + n_kv, 16, s)
    for c in copies:
        c.start()
    for c in copies:
        c.wait()

    def relay(k):
        order = near_first(k)
        for c in order[1:]:
            back(dp, slot_of(*c))
            x_copy(slot_of(*c)).start()
            c_copy(dp, 0, slot_of(*c)).start()
        for c in order:
            back(facing, slot_of(*c))
            c_copy(facing, 1, slot_of(*c)).start()

    on_position(relay)
    for b in range(n_early):
        g_x_copy(b).wait_recv()
        add_into(early_ref.at[b], s_early.at[b], 24)
    for slot in range(shards):
        back(twin, slot)
        back(across, slot)
    for n, to in enumerate((twin, facing, across)):
        remote(ids_ref, ids_all.at[to], id_send.at[n], id_recv.at[to], tp, to).wait_recv()
        ids_copy(n, to).wait_send()
    for n in range(1, shards):
        row_copy(lax.rem(tp + n, shards)).wait_send()
    for slot in range(shards):
        x_copy(slot).wait_send()
        c_copy(dp, 0, slot).wait_send()
        c_copy(facing, 1, slot).wait_send()
    for b in range(n_early):
        g_chip_copy(b).wait_send()
        g_x_copy(b).wait_send()


def layer_bwd(scale, tok_total, d_fin, x0, x1, norms, hits, ln, cos_t, sin_t, weights, saved, code, g_table, ids, collective_id):
    own, width = x0.shape
    nq = weights[0].shape[0]
    two_hd = 2 * weights[1].shape[1]
    ff = weights[3].shape[0]
    rows = (2 * nq + 3 * ff + two_hd) // (2 * NZ) + 16
    chunk = (own, width)
    back = (2 * NZ, ids.shape[1] // (2 * NZ), width)
    blocks = (N_EARLY, table_block(g_table.shape[0]), width)
    dma = lambda *n: pltpu.SemaphoreType.DMA(n)
    return pl.pallas_call(
        functools.partial(layer_bwd_kernel, scale, tok_total),
        out_shape=(jax.ShapeDtypeStruct((2 * NZ, rows, width), F32), jax.ShapeDtypeStruct(chunk, F32), jax.ShapeDtypeStruct((4,) + back, F32),
                   jax.ShapeDtypeStruct(blocks, F32), jax.ShapeDtypeStruct((4,) + ids.shape, jnp.int32)),
        in_specs=[VMEM] * 11 + [ANY] * 3 + [VMEM] * 6 + [ANY, VMEM],
        out_specs=(ANY, VMEM, ANY, VMEM, VMEM),
        scratch_shapes=[pltpu.VMEM(chunk, F32), pltpu.VMEM(chunk, BF16), pltpu.VMEM(chunk, BF16), pltpu.VMEM((nq, own), BF16),
                        pltpu.VMEM((nq, own), BF16), pltpu.VMEM((2 * own, two_hd), F32), pltpu.VMEM((own, two_hd), F32)]
        + [pltpu.VMEM((ff, own), BF16)] * 3 + [pltpu.VMEM(back, F32), pltpu.VMEM((nq, width), F32), pltpu.VMEM((nq, width), F32)] + [pltpu.VMEM((ff, width), F32)] * 3
        + [pltpu.VMEM((two_hd + 32, width), F32), pltpu.VMEM(blocks, F32), pltpu.VMEM(blocks, F32)]
        + [pltpu.VMEM((ff, width), BF16)] * 3 + [dma(3), dma(14 * NZ + 1),
           pltpu.SemaphoreType.DMA, pltpu.SemaphoreType.DMA, dma(2 * NZ), dma(2 * NZ), dma(2, 2 * NZ), dma(4, 2 * NZ),
           dma(N_EARLY), dma(2, N_EARLY), dma(2, N_EARLY), dma(3), dma(4)],
        compiler_params=pltpu.CompilerParams(collective_id=collective_id, has_side_effects=True, vmem_limit_bytes=66000000),
        name="layer_bwd",
    )(d_fin, x0, x1, norms, hits, ln, cos_t, sin_t, *weights, *saved, code, g_table, ids)


N_BLOCK = 12
N_EARLY = 3
AHEAD = 11


def table_block(vocab):
    return -(-vocab // (2 * N_BLOCK * 24)) * 24


W_REDUCE = {
    0: {4: (3,), 6: (2,), 8: (1,), 9: (0,)},
    1: {6: (3,), 8: (2, 0), 9: (1,)},
    2: {6: (0,), 8: (1, 3), 9: (2,)},
    3: {4: (0,), 6: (1,), 8: (2,), 9: (3,)},
}


def tail_kernel(g_ref, p_ref, rows_ref, ids_ref, early_ref, t_ref, w_out, small_ref,
                s_buf, from_c, from_x, look_in, parts, acc, w_c, w_y, w_l, w_r, w_x,
                g_load, g_send_c, g_recv_c, g_send_x, g_recv_x, g_send_t, g_recv_t, g_store, l_sem,
                w_load, w_out_sem, send_c, send_y, send_l, send_r, recv_c, recv_y, recv_l, recv_r, last_send, last_recv, small_send, small_recv):
    tp, dp, z, y = place()
    partner = tp + 1 - 2 * y
    core = dp % 2
    twin = dp + 1 - 2 * core
    facing = lax.rem(dp + 2, 4)
    half = g_ref.shape[0] // 2
    size = s_buf.shape[1]
    last = half - (N_BLOCK - 1) * size
    n_look = rows_ref.shape[1]

    def rows(which, b, n):
        return pl.ds(pl.multiple_of(which * half + b * size, 8), n)

    def part(buf, b, n):
        return buf.at[b - N_EARLY if buf is not from_x else b, pl.ds(0, n), :]

    plane_barrier(tp, dp, [(tp, twin), (tp, facing)])

    chip = dp // 2
    groups = (2 * chip, 2 * chip + 1, 2 - 2 * chip, 3 - 2 * chip)

    def look_load(n):
        return pltpu.make_async_copy(rows_ref.at[groups[n]], look_in.at[n % 2], l_sem.at[n % 2])

    def early_load(b):
        return pltpu.make_async_copy(early_ref.at[b], from_x.at[b], g_load.at[b])

    for n in range(2):
        look_load(n).start()

    def c_copy(b, n):
        return remote(g_ref.at[rows(1 - core, b, n), :], part(from_c, b, n), g_send_c.at[b], g_recv_c.at[b], tp, twin)

    def own_load(b, n):
        return pltpu.make_async_copy(g_ref.at[rows(core, b, n), :], part(s_buf, b, n), g_load.at[b])

    def x_copy(b, n):
        return remote(part(s_buf, b, n), part(from_x, b, n), g_send_x.at[b], g_recv_x.at[b], tp, facing)

    def t_copy(b, n):
        return remote(part(from_x, b, n), t_ref.at[rows(core, b, n), :], g_send_t.at[b], g_recv_t.at[b], tp, twin)

    def t_store(b, n):
        return pltpu.make_async_copy(part(from_x, b, n), t_ref.at[rows(core, b, n), :], g_store.at[b])

    def every(f, first, end):
        def body(b, carry):
            f(b, size)
            return carry
        lax.fori_loop(first, min(end, N_BLOCK - 1), body, 0)
        if end == N_BLOCK:
            f(N_BLOCK - 1, last)

    def looked_up(b, n, first, count):
        ids = jnp.concatenate([ids_ref[first + g] for g in range(count)], axis=1) - (core * half + b * size)
        hit = (lax.broadcasted_iota(jnp.int32, (n, count * n_look), 0) == ids).astype(F32).astype(BF16)
        span = pl.ds(pl.multiple_of(first * n_look, n_look), count * n_look)
        return mm(hit, parts[0, span, :]) + mm(hit, parts[1, span, :]) + mm(hit, parts[2, span, :])

    def chip_sum(b, n):
        own_load(b, n).wait()
        c_copy(b, n).wait_recv()
        at = b - N_EARLY
        s_buf[at, 0:n, :] = s_buf[at, 0:n, :] + from_c[at, 0:n, :] + looked_up(b, n, 2 * chip, 2)
        x_copy(b, n).start()

    def early_sum(b, n):
        early_load(b).wait()
        from_x[b] = from_x[b] + looked_up(b, n, 0, 4)
        t_copy(b, n).start()
        t_store(b, n).start()

    def w_first(k):
        for zz in REDUCE_ORDER[k]:
            for slot in (2 * zz + 1 - y, 2 * zz + y):
                remote(p_ref.at[slot, 1 - core], w_c.at[slot], send_c.at[slot], recv_c.at[slot], tp, twin).start()
                pltpu.make_async_copy(p_ref.at[slot, core], acc.at[slot], w_load.at[slot]).start()

    def w_chip_sum(slot):
        pltpu.make_async_copy(p_ref.at[slot, core], acc.at[slot], w_load.at[slot]).wait()
        remote(acc.at[slot], w_c.at[slot], send_c.at[slot], recv_c.at[slot], tp, twin).wait_recv()
        add_into(acc.at[slot], w_c.at[slot])

    def w_second(k):
        for zz in REDUCE_ORDER[k]:
            slot = 2 * zz + 1 - y
            w_chip_sum(slot)
            remote(acc.at[slot], w_y.at[zz], send_y.at[zz], recv_y.at[zz], partner, dp).start()
        for zz in REDUCE_ORDER[k]:
            w_chip_sum(2 * zz + y)

    def w_reduce(k, shards):
        for zz in shards:
            line = acc.at[2 * zz + y]
            remote(line, w_y.at[zz], send_y.at[zz], recv_y.at[zz], partner, dp).wait_recv()
            add_into(line, w_y.at[zz])
            if zz >= k and k > 0:
                remote(line, w_l.at[zz - 1], send_l.at[zz], recv_l.at[zz], partner, dp).wait_recv()
                add_into(line, w_l.at[zz - 1])
            if zz <= k and k < NZ - 1:
                remote(line, w_r.at[zz], send_r.at[zz], recv_r.at[zz], partner, dp).wait_recv()
                add_into(line, w_r.at[zz])
            if zz > k:
                remote(line, w_l.at[zz - 1], send_r.at[zz], recv_l.at[zz], tp + 2, dp).start()
            if zz < k:
                remote(line, w_r.at[zz], send_l.at[zz], recv_r.at[zz], tp - 2, dp).start()

    def on_position(f):
        for k in range(NZ):
            pl.when(z == k)(functools.partial(f, k))

    def first(b, n):
        c_copy(b, n).start()
        own_load(b, n).start()

    every(first, N_EARLY, N_EARLY + 2)
    on_position(w_first)
    every(first, N_EARLY + 2, N_BLOCK)
    for b in range(N_EARLY):
        early_load(b).start()

    def split(n):
        look_load(n).wait()
        value = look_in[n % 2]
        high = value.astype(BF16)
        left = value - high.astype(F32)
        middle = left.astype(BF16)
        at = pl.ds(pl.multiple_of(groups[n] * n_look, n_look), n_look)
        parts[0, at, :] = high
        parts[1, at, :] = middle
        parts[2, at, :] = (left - middle.astype(F32)).astype(BF16)
        if n + 2 < 4:
            look_load(n + 2).start()

    split(0)
    split(1)
    every(chip_sum, N_EARLY, N_EARLY + 3)
    on_position(w_second)
    every(chip_sum, N_EARLY + 3, AHEAD)
    split(2)
    split(3)
    every(early_sum, 0, N_EARLY)

    total = acc.at[tp]
    w_copy_x = remote(total, w_x, last_send.at[0], last_recv.at[0], tp, facing)
    w_copy_c = remote(total, w_out.at[core], last_send.at[1], last_recv.at[1], tp, twin)
    w_store = pltpu.make_async_copy(total, w_out.at[core], w_out_sem)
    n_small, n_rows = small_ref.shape[1], w_out.shape[1]
    mine = w_out.at[1, pl.ds(n_rows - 32, n_small), :]
    small_here = pltpu.make_async_copy(mine, small_ref.at[tp], w_out_sem)
    peers = [lax.rem(tp + n, 2 * NZ) for n in range(1, 2 * NZ)]
    for b in range(N_EARLY, N_BLOCK):
        n = last if b == N_BLOCK - 1 else size
        if b == N_BLOCK - 1:
            w_copy_x.wait()
            add_into(total, w_x)
            w_copy_c.start()
            w_store.start()
            w_copy_c.wait_send()
            remote(total, w_out.at[1 - core], last_send.at[1], last_recv.at[1], tp, twin).wait_recv()
            w_store.wait()
            for to in peers:
                remote(mine, small_ref.at[tp], small_send.at[to], small_recv.at[tp], to, dp).start()
            small_here.start()
        x_copy(b, n).wait_recv()
        add_into(part(from_x, b, n), part(s_buf, b, n), 24)
        t_copy(b, n).start()
        t_store(b, n).start()
        for k in range(NZ):
            if b in W_REDUCE[k]:
                pl.when(z == k)(functools.partial(w_reduce, k, W_REDUCE[k][b]))
        if b == N_BLOCK - 3:
            w_copy_x.start()
            every(chip_sum, AHEAD, N_BLOCK)
    for source in peers:
        remote(small_ref.at[source], small_ref.at[source], small_send.at[source], small_recv.at[source], source, dp).wait_recv()
        remote(mine, small_ref.at[tp], small_send.at[source], small_recv.at[tp], source, dp).wait_send()
    small_here.wait()

    def w_done(k):
        for zz in range(NZ):
            line = acc.at[2 * zz + y]
            for slot in (2 * zz + 1 - y, 2 * zz + y):
                remote(p_ref.at[slot, 1 - core], w_c.at[slot], send_c.at[slot], recv_c.at[slot], tp, twin).wait_send()
            remote(line, w_y.at[zz], send_y.at[zz], recv_y.at[zz], partner, dp).wait_send()
            if zz > k:
                remote(line, w_l.at[zz - 1], send_r.at[zz], recv_l.at[zz], tp + 2, dp).wait_send()
            if zz < k:
                remote(line, w_r.at[zz], send_l.at[zz], recv_r.at[zz], tp - 2, dp).wait_send()

    on_position(w_done)

    def drain(b, n):
        t_copy(b, n).wait_send()
        t_store(b, n).wait()
        remote(part(from_x, b, n), t_ref.at[rows(1 - core, b, n), :], g_send_t.at[b], g_recv_t.at[b], tp, twin).wait_recv()

    def sent(b, n):
        c_copy(b, n).wait_send()
        x_copy(b, n).wait_send()

    every(drain, 0, N_BLOCK)
    every(sent, N_EARLY, N_BLOCK)


def tail(g_table, g_rows, look_rows, look_ids, early, collective_id):
    vocab, width = g_table.shape
    rows = g_rows.shape[1]
    half = (rows // 2, width)
    n_look = look_ids.shape[2]
    size = table_block(vocab)
    blocks = lambda n: pltpu.VMEM((n, size, width), F32)
    dma = lambda *n: pltpu.SemaphoreType.DMA(n)
    t, w_sum, small = pl.pallas_call(
        tail_kernel,
        out_shape=(jax.ShapeDtypeStruct((vocab, width), F32), jax.ShapeDtypeStruct((2,) + half, F32), jax.ShapeDtypeStruct((2 * NZ, 24, width), F32)),
        in_specs=[ANY, ANY, ANY, VMEM, ANY],
        out_specs=(ANY,) * 3,
        scratch_shapes=[blocks(N_BLOCK - N_EARLY)] * 2 + [blocks(N_BLOCK), pltpu.VMEM((2, n_look, width), F32), pltpu.VMEM((3, 4 * n_look, width), BF16)]
        + [pltpu.VMEM((2 * NZ,) + half, F32)] * 2 + [pltpu.VMEM((NZ,) + half, F32)] + [pltpu.VMEM((NZ - 1,) + half, F32)] * 2
        + [pltpu.VMEM(half, F32)]
        + [dma(N_BLOCK)] * 8 + [dma(2)]
        + [dma(2 * NZ), pltpu.SemaphoreType.DMA] + [dma(2 * NZ), dma(NZ), dma(NZ), dma(NZ)] * 2 + [dma(2)] * 2 + [dma(2 * NZ)] * 2,
        compiler_params=pltpu.CompilerParams(collective_id=collective_id, has_side_effects=True, vmem_limit_bytes=67000000),
        name="tail",
    )(g_table, g_rows.reshape((2 * NZ, 2) + half), look_rows.reshape(4, n_look, width), look_ids, early)
    return t, w_sum.reshape(rows, width), small


UPDATE_ROWS = 512


def update_kernel(t_ref, w_any, small_any, *refs):
    state = [refs[7 * i:7 * i + 7] for i in range(3)]
    new = [refs[21 + 7 * i:28 + 7 * i] for i in range(3)]
    loss_ref, held, made, w_ref, small_ref = refs[42:47]
    old_small = [refs[47 + 6 * i:53 + 6 * i] for i in range(3)]
    new_small = [refs[65 + 6 * i:71 + 6 * i] for i in range(3)]
    in_sem, out_sem, g_sem, small_in, small_out = refs[83:]
    vocab = t_ref.shape[0]
    blocks = [(at, min(UPDATE_ROWS, vocab - at)) for at in range(0, vocab, UPDATE_ROWS)]

    def loads(q):
        at, n = blocks[q]
        return [pltpu.make_async_copy(ref.at[pl.ds(at, n), :], held.at[q % 4, i, pl.ds(0, n), :], in_sem.at[q % 4, i])
                for i, ref in enumerate((t_ref, state[0][0], state[1][0], state[2][0]))]

    def stores(q):
        at, n = blocks[q]
        return [pltpu.make_async_copy(made.at[q % 3, i, pl.ds(0, n), :], new[i][0].at[pl.ds(at, n), :], out_sem.at[q % 3, i]) for i in range(3)]

    for q in range(4):
        for c in loads(q):
            c.start()
    grads = [pltpu.make_async_copy(w_any, w_ref, g_sem.at[0]), pltpu.make_async_copy(small_any, small_ref, g_sem.at[1])]
    pairs = [(i, j) for i in range(3) for j in range(6)]
    small_loads = grads + [pltpu.make_async_copy(state[i][j + 1], old_small[i][j], small_in.at[i, j]) for i, j in pairs]
    small_stores = [pltpu.make_async_copy(new_small[i][j], new[i][j + 1], small_out.at[i, j]) for i, j in pairs]
    for c in small_loads:
        c.start()

    def small_update(index, grad, *where):
        got = adam_update(old_small[0][index - 1][where], grad, old_small[1][index - 1][where], old_small[2][index - 1][where])
        for i in range(3):
            new_small[i][index - 1][where] = got[i]

    def small_updates():
        hd = old_small[0][2].shape[1]
        n_kv = 2 * hd // small_ref.shape[0]
        n_q, n_f = old_small[0][1].shape[0], old_small[0][5].shape[0]
        small_update(1, small_ref[0, n_kv:n_kv + 2, :], Ellipsis)
        small_update(2, w_ref[0:n_q, :], Ellipsis)
        kv = small_ref[:, 0:n_kv, :].reshape(2 * hd, small_ref.shape[2])
        for i in range(2):
            small_update(3, kv[i * hd:(i + 1) * hd], i)
        small_update(4, w_ref[n_q:2 * n_q, :], Ellipsis)
        for i in range(2):
            small_update(5, w_ref[2 * n_q + i * n_f:2 * n_q + (i + 1) * n_f, :].T, i)
        small_update(6, w_ref[2 * n_q + 2 * n_f:2 * n_q + 3 * n_f, :], Ellipsis)
        loss_ref[...] = jnp.sum(small_ref[0, n_kv + 2:n_kv + 3, :], axis=1, keepdims=True)

    for q, (at, n) in enumerate(blocks):
        for c in loads(q):
            c.wait()
        if q >= 3:
            for c in stores(q - 3):
                c.wait()
        step = 32 if n % 32 == 0 else 16

        def body(j, carry):
            rows = pl.ds(pl.multiple_of(j * step, step), step)
            got = adam_update(held[q % 4, 1, rows, :], held[q % 4, 0, rows, :], held[q % 4, 2, rows, :], held[q % 4, 3, rows, :])
            for i in range(3):
                made[q % 3, i, rows, :] = got[i]
            return carry

        lax.fori_loop(0, n // step, body, 0)
        for c in stores(q):
            c.start()
        if q + 4 < len(blocks):
            for c in loads(q + 4):
                c.start()
        if q == min(3, len(blocks) - 1):
            for c in small_loads:
                c.wait()
            small_updates()
            for c in small_stores:
                c.start()
    for q in range(len(blocks) - 3, len(blocks)):
        for c in stores(q):
            c.wait()
    for c in small_stores:
        c.wait()


def update(g_table, g_shard, g_small, state_arrays):
    width = g_table.shape[1]
    dma = lambda *n: pltpu.SemaphoreType.DMA(n)

    def flip(arrays):
        return [a.swapaxes(-1, -2) if i % 7 in (2, 3) else a for i, a in enumerate(arrays)]

    given = flip(state_arrays)
    small = [pltpu.VMEM(a.shape, F32) for i, a in enumerate(given) if i % 7]
    *new, loss = pl.pallas_call(
        update_kernel,
        out_shape=tuple(jax.ShapeDtypeStruct(a.shape, F32) for a in given) + (jax.ShapeDtypeStruct((1, 1), F32),),
        in_specs=[ANY] * 24,
        out_specs=(ANY,) * 21 + (VMEM,),
        scratch_shapes=[pltpu.VMEM((4, 4, UPDATE_ROWS, width), F32), pltpu.VMEM((3, 3, UPDATE_ROWS, width), F32),
                        pltpu.VMEM(g_shard.shape, F32), pltpu.VMEM(g_small.shape, F32)] + small * 2
        + [dma(4, 4), dma(3, 3), dma(2), dma(3, 6), dma(3, 6)],
        compiler_params=pltpu.CompilerParams(vmem_limit_bytes=60000000),
        name="update",
    )(g_table, g_shard, g_small, *given)
    return flip(new) + [loss]


def norm_fwd(x_f32, scale):
    centered = x_f32 - jnp.mean(x_f32, axis=-1, keepdims=True)
    inv_std = lax.rsqrt(jnp.mean(centered * centered, axis=-1, keepdims=True) + LN_EPS)
    x_hat = centered * inv_std
    return (x_hat * scale).astype(BF16), x_hat, inv_std


def norm_bwd(d_out, x_hat, inv_std, scale):
    d_scale = jnp.sum(d_out * x_hat, axis=0)
    d_hat = d_out * scale
    d_in = inv_std * (d_hat - jnp.mean(d_hat, axis=-1, keepdims=True) - x_hat * jnp.mean(d_hat * x_hat, axis=-1, keepdims=True))
    return d_in, d_scale


def adam_update(param_in, grad_in, mom_in, vel_in):
    mom_new = BETA_ONE * mom_in + (1.0 - BETA_ONE) * grad_in
    vel_new = BETA_TWO * vel_in + (1.0 - BETA_TWO) * grad_in * grad_in
    return param_in - LEARN_RATE * mom_new / (jnp.sqrt(vel_new) + ADAM_EPS), mom_new, vel_new


def dot(spec, a, b):
    return jnp.einsum(spec, a, b, preferred_element_type=F32)


def solution(mesh):
    param_specs = (P('tp', None), P(None, None), P(None, 'tp'), P(None, None, None), P('tp', None), P(None, None, 'tp'), P('tp', None))
    n_tp = mesh.shape['tp']
    n_dp = mesh.shape['dp']

    def local_step(tokens, labels, *state_arrays):
        embed, ln_scales, w_q, w_kv, w_o, w_gu, w_down = state_arrays[0:7]
        batch_loc, seq_len = tokens.shape
        vocab_loc, d_model = embed.shape
        head_dim = w_kv.shape[2]
        q_loc = w_q.shape[1]
        f_loc = w_down.shape[0]
        tok_loc = batch_loc * seq_len
        tok_total = tok_loc * n_dp
        own = tok_loc // n_tp
        tp_rank = lax.axis_index('tp')
        half = tp_rank % 2

        strict = (jnp.arange(own)[:, None] > jnp.arange(own)[None, :]).astype(BF16)

        def routing(chunks):
            shard = chunks // vocab_loc
            row = chunks - shard * vocab_loc
            hot = (shard[:, :, None] == jnp.arange(n_tp)[None, None, :])
            before = dot('rs,nsj->nrj', strict, hot.astype(BF16))
            rank = jnp.sum(jnp.where(hot, before, 0.0), axis=-1).astype(jnp.int32)
            most = jnp.max(jnp.sum(hot.astype(jnp.int32), axis=1))
            return shard, row, rank, (most + CAP - 1) // CAP

        chunks = tokens.reshape(n_tp, own)
        shard, row, rank, rounds = routing(chunks)
        slots = jnp.arange(CAP)
        my_shard = lax.dynamic_index_in_dim(shard, tp_rank, 0, keepdims=False)
        my_rank = lax.dynamic_index_in_dim(rank, tp_rank, 0, keepdims=False)

        def fetch(step):
            here = (shard[:, None, :] == tp_rank) & (rank[:, None, :] == slots[None, :, None] + step * CAP)
            ids = jnp.sum(jnp.where(here, row[:, None, :], 0), axis=-1).reshape(-1)
            place = my_rank - step * CAP
            return ids, jnp.where((place >= 0) & (place < CAP), my_shard * CAP + place, -1)

        def fetch_more(state):
            ids, code = fetch(state[0])
            pick = (code[:, None] == jnp.arange(n_tp * CAP)[None, :]).astype(BF16)
            rows_in = plane_swap(jnp.take(embed, ids, axis=0).reshape(n_tp, CAP, d_model), 1).reshape(n_tp * CAP, d_model).astype(BF16)
            return state[0] + 1, state[1] + dot('rc,cd->rd', pick, rows_in)

        more_rows = lax.while_loop(lambda state: state[0] < rounds, fetch_more, (jnp.int32(1), jnp.zeros((own, d_model), F32)))[1]
        ids_first, code_first = fetch(0)
        code_first = code_first[None, :]

        w_rows = jnp.concatenate([w_q.T, w_o, w_gu.transpose(0, 2, 1).reshape(2 * f_loc, d_model), w_down], axis=0)
        cuts = (q_loc, 2 * q_loc, 2 * q_loc + f_loc, 2 * q_loc + 2 * f_loc)
        wkv_t = w_kv.transpose(0, 2, 1)
        inv_freq = ROPE_BASE ** (-jnp.arange(0, head_dim, 2).astype(F32) / head_dim)
        angles = inv_freq[:, None] * (half * own + jnp.arange(own)).astype(F32)[None, :]
        cos_t, sin_t = jnp.cos(angles), jnp.sin(angles)
        f_own, x_one, x_zero, *saved = front(ids_first, embed, jnp.broadcast_to(rounds, (1, 128)), code_first, more_rows, w_rows, wkv_t, ln_scales, cos_t, sin_t, n_tp * q_loc, 0)
        saved, (wq_t, wo_b, wg_t, wu_t, wd_b), rounds_all = saved[:5], saved[5:10], jnp.max(saved[10])
        weights = (wq_t, wkv_t, wo_b, wg_t, wu_t, wd_b)

        logit_scale = d_model ** -0.5
        d_fin, g_head_part, log_norm, lab_sum, _ = head(f_own, labels, embed, logit_scale, logit_scale / tok_total, 4)

        def row_ids(step):
            here = (shard[:, None, :] == tp_rank) & (rank[:, None, :] == slots[None, :, None] + step * CAP)
            return jnp.where(jnp.any(here, axis=-1), jnp.sum(jnp.where(here, row[:, None, :], 0), axis=-1), vocab_loc).reshape(-1)

        g_rows, d_zero, rows_back, early, ids_back = layer_bwd(logit_scale, tok_total, d_fin, x_zero, x_one, log_norm, lab_sum, ln_scales, cos_t, sin_t, weights, saved,
                                                               code_first, g_head_part, row_ids(0)[None, :], 7)
        g_table, g_shard, g_small = tail(g_head_part, g_rows, rows_back, ids_back, early, 10)

        def give_back(state):
            mine = (my_shard[None, None, :] == jnp.arange(n_tp)[:, None, None]) & (my_rank[None, None, :] == slots[None, :, None] + state[0] * CAP)
            ids = jnp.sum(jnp.where(mine, jnp.arange(own)[None, None, :], 0), axis=-1).reshape(-1)
            rows_in = plane_swap(jnp.take(d_zero, ids, axis=0).reshape(n_tp, CAP, d_model), 9).reshape(-1, d_model)
            n_rows = n_tp * CAP
            id_rows = jnp.pad(row_ids(state[0]).astype(F32), (0, -n_rows % (8 * d_model))).reshape(-1, d_model)
            both = group_gather(jnp.concatenate([rows_in, id_rows], axis=0), 11)
            ids = both[:, n_rows:].reshape(n_dp, -1)[:, :n_rows].astype(jnp.int32)
            return state[0] + 1, state[1].at[ids.reshape(-1)].add(both[:, :n_rows].reshape(-1, d_model), mode='drop')

        g_table = lax.while_loop(lambda state: state[0] < rounds_all, give_back, (jnp.int32(1), g_table))[1]
        *new, loss = update(g_table, g_shard, g_small, state_arrays)
        return tuple(new) + (loss.reshape(()),)

    return jax.shard_map(local_step, mesh=mesh, in_specs=(P('dp', None), P('dp', None)) + param_specs * 3,
                         out_specs=param_specs * 3 + (P(),), check_vma=False)
```

```python
import functools

import jax
import jax.numpy as jnp
from jax import lax
from jax.experimental import pallas as pl
from jax.experimental.pallas import tpu as pltpu
from jax.sharding import PartitionSpec as P

LN_EPS = 1e-5
LOGIT_ZLOSS = 1e-4
LEARN_RATE = 1e-2
BETA_ONE = 0.9
BETA_TWO = 0.95
ADAM_EPS = 1e-8
ROPE_BASE = 10000.0
NZ = 4
CAP = 96
F32 = jnp.float32
BF16 = jnp.bfloat16
ANY = pl.BlockSpec(memory_space=pl.ANY)
VMEM = pl.BlockSpec(memory_space=pltpu.VMEM)

ARRIVALS = {
    0: (("R", 1), ("R", 2), ("R", 3)),
    1: (("L", 0), ("R", 2), ("R", 3)),
    2: (("R", 3), ("L", 1), ("L", 0)),
    3: (("L", 2), ("L", 1), ("L", 0)),
}
REDUCE_ORDER = {0: (3, 2, 1, 0), 1: (3, 0, 2, 1), 2: (0, 3, 1, 2), 3: (0, 1, 2, 3)}


def remote(src, dst, send_sem, recv_sem, tp, dp):
    return pltpu.make_async_remote_copy(src_ref=src, dst_ref=dst, send_sem=send_sem, recv_sem=recv_sem,
                                        device_id=(tp, dp), device_id_type=pl.DeviceIdType.MESH)


def place():
    tp = lax.axis_index("tp")
    dp = lax.axis_index("dp")
    return tp, dp, tp // 2, tp % 2


def signal(tp, dp):
    pl.semaphore_signal(pltpu.get_barrier_semaphore(), inc=1, device_id=(tp, dp), device_id_type=pl.DeviceIdType.MESH)


def add_into(acc, other, step=None):
    rows = acc.shape[0]
    step = step or (64 if rows % 64 == 0 else 8)

    def body(n, carry):
        at = pl.ds(pl.multiple_of(n * step, step), step)
        acc[at, :] = acc[at, :] + other[at, :]
        return carry

    lax.fori_loop(0, rows // step, body, 0)


def near_first(k):
    return sorted(((o, zz) for o in range(2) for zz in range(NZ)), key=lambda c: (abs(c[1] - k), c[0]))


def plane_barrier(tp, dp, others):
    peers = [(lax.rem(tp + n, 2 * NZ), dp) for n in range(1, 2 * NZ)] + others
    for peer in peers:
        signal(*peer)
    pl.semaphore_wait(pltpu.get_barrier_semaphore(), len(peers))


def swap_kernel(x_ref, out_ref, own_sem, send, recv):
    tp, dp, _, _ = place()
    plane_barrier(tp, dp, [])
    copies = []
    for n in range(1, 2 * NZ):
        to = lax.rem(tp + n, 2 * NZ)
        copy = remote(x_ref.at[to], out_ref.at[tp], send.at[to], recv.at[tp], to, dp)
        copy.start()
        copies.append(copy)
    own = pltpu.make_async_copy(x_ref.at[tp], out_ref.at[tp], own_sem)
    own.start()
    for n in range(1, 2 * NZ):
        source = lax.rem(tp + n, 2 * NZ)
        remote(out_ref.at[source], out_ref.at[source], send.at[source], recv.at[source], source, dp).wait_recv()
    own.wait()
    for copy in copies:
        copy.wait_send()


def plane_swap(x, collective_id):
    return pl.pallas_call(
        swap_kernel,
        out_shape=jax.ShapeDtypeStruct(x.shape, x.dtype),
        in_specs=[ANY],
        out_specs=ANY,
        scratch_shapes=[pltpu.SemaphoreType.DMA] + [pltpu.SemaphoreType.DMA((2 * NZ,))] * 2,
        compiler_params=pltpu.CompilerParams(collective_id=collective_id, has_side_effects=True),
        name="plane_swap",
    )(x)


def group_kernel(x_ref, out_ref, own_sem, send, recv):
    tp, dp, _, _ = place()
    group = [lax.rem(dp + n, 4) for n in range(1, 4)]
    for to in group:
        signal(tp, to)
    pl.semaphore_wait(pltpu.get_barrier_semaphore(), 3)
    own = pltpu.make_async_copy(x_ref, out_ref.at[dp], own_sem)
    own.start()
    for n, to in enumerate(group):
        remote(x_ref, out_ref.at[dp], send.at[n], recv.at[dp], tp, to).start()
    own.wait()
    for n, to in enumerate(group):
        remote(x_ref, out_ref.at[to], send.at[n], recv.at[to], tp, to).wait_recv()
        remote(x_ref, out_ref.at[dp], send.at[n], recv.at[dp], tp, to).wait_send()


def group_gather(x, collective_id):
    return pl.pallas_call(
        group_kernel,
        out_shape=jax.ShapeDtypeStruct((4,) + x.shape, x.dtype),
        in_specs=[ANY],
        out_specs=ANY,
        scratch_shapes=[pltpu.SemaphoreType.DMA, pltpu.SemaphoreType.DMA((3,)), pltpu.SemaphoreType.DMA((4,))],
        compiler_params=pltpu.CompilerParams(collective_id=collective_id, has_side_effects=True),
        name="group_gather",
    )(x)


GATHER_ORDER = {
    0: ((0, 0), (0, 1), (1, 0), (0, 2), (1, 1), (0, 3), (1, 2), (1, 3)),
    1: ((0, 1), (0, 0), (0, 2), (1, 1), (1, 0), (0, 3), (1, 2), (1, 3)),
    2: ((0, 2), (0, 1), (0, 3), (1, 2), (0, 0), (1, 3), (1, 1), (1, 0)),
    3: ((0, 3), (0, 2), (1, 3), (0, 1), (1, 2), (0, 0), (1, 1), (1, 0)),
}
GATHER_EVENTS = {
    0: {
        1: ((0, 1, 0, 'y'), (1, 0, 1, 'r'), (0, 1, 1, 'y'), (1, 0, 0, '')),
        3: ((0, 2, 0, 'y'), (1, 1, 0, ''), (0, 2, 1, 'y'), (1, 1, 1, '')),
        5: ((0, 3, 0, 'y'), (1, 2, 0, ''), (0, 3, 1, ''), (1, 2, 1, '')),
        7: ((1, 3, 0, ''), (1, 3, 1, '')),
    },
    1: {
        1: ((0, 0, 0, 'ry'), (0, 2, 0, 'ly'), (1, 1, 0, ''), (0, 0, 1, 'r'), (0, 2, 1, 'ly'), (1, 1, 1, '')),
        4: ((0, 3, 0, 'ly'), (1, 0, 0, ''), (1, 0, 1, 'r')),
        5: ((0, 3, 1, 'l'), (1, 2, 0, '')),
        6: ((1, 2, 1, ''), (1, 3, 1, 'l')),
        7: ((1, 3, 0, ''),),
    },
    2: {
        1: ((0, 1, 0, 'ry'), (0, 3, 0, 'ly'), (1, 2, 0, ''), (0, 1, 1, 'ry'), (0, 3, 1, 'l'), (1, 2, 1, '')),
        4: ((0, 0, 0, 'ry'), (1, 1, 0, ''), (1, 3, 1, 'l'), (0, 0, 1, 'r'), (1, 3, 0, '')),
        6: ((1, 0, 1, 'r'), (1, 1, 1, '')),
        7: ((1, 0, 0, ''),),
    },
    3: {
        1: ((0, 2, 0, 'y'), (1, 3, 1, 'l'), (0, 2, 1, 'y'), (1, 3, 0, '')),
        3: ((0, 1, 0, 'y'), (1, 2, 0, ''), (0, 1, 1, 'y'), (1, 2, 1, '')),
        5: ((0, 0, 0, 'y'), (1, 1, 0, ''), (0, 0, 1, ''), (1, 1, 1, '')),
        7: ((1, 0, 0, ''), (1, 0, 1, '')),
    },
}
SCATTER_ORDER = {
    0: ((1, 3), (1, 2), (0, 3), (1, 1), (0, 2), (1, 0), (0, 1), (0, 0)),
    1: ((1, 3), (1, 2), (0, 3), (1, 0), (1, 1), (0, 2), (0, 0), (0, 1)),
    2: ((1, 0), (1, 1), (1, 3), (0, 0), (1, 2), (0, 3), (0, 1), (0, 2)),
    3: ((1, 0), (1, 1), (0, 0), (1, 2), (0, 1), (1, 3), (0, 2), (0, 3)),
}
SCATTER_EVENTS = {
    0: {
        0: ((1, 3, 0, '', 'y'), (1, 3, 1, '', 'r')),
        1: ((1, 2, 0, '', 'y'), (1, 2, 1, '', 'y')),
        2: ((0, 3, 1, '', 'r'), (0, 3, 0, 'y', 'r')),
        3: ((1, 1, 0, '', 'y'), (1, 1, 1, '', 'y')),
        4: ((0, 2, 0, 'y', 'r'),),
        5: ((0, 2, 1, 'y', 'r'), (1, 0, 0, '', 'y')),
        6: ((1, 0, 1, 'r', 'y'), (0, 1, 0, 'y', 'r')),
        7: ((0, 1, 1, 'y', 'r'), (0, 0, 0, 'ry', ''), (0, 0, 1, 'ry', '')),
    },
    1: {
        0: ((1, 3, 0, '', 'y'),),
        1: ((1, 2, 0, '', 'y'), (1, 2, 1, '', 'y')),
        2: ((1, 3, 1, 'l', 'r'),),
        3: ((1, 0, 0, '', 'y'),),
        4: ((0, 3, 1, 'l', 'r'), (1, 0, 1, 'r', 'l'), (1, 1, 0, '', 'y'), (1, 1, 1, '', 'y')),
        6: ((0, 3, 0, 'ly', 'r'), (0, 0, 1, 'r', 'l')),
        7: ((0, 2, 0, 'ly', 'r'), (0, 0, 0, 'ry', 'l'), (0, 2, 1, 'ly', 'r'), (0, 1, 0, 'lry', ''), (0, 1, 1, 'lry', '')),
    },
    2: {
        0: ((1, 0, 0, '', 'y'),),
        1: ((1, 1, 0, '', 'y'), (1, 1, 1, '', 'y')),
        2: ((1, 0, 1, 'r', 'l'), (1, 3, 0, '', 'y')),
        4: ((1, 3, 1, 'l', 'r'), (0, 0, 1, 'r', 'l'), (1, 2, 0, '', 'y'), (1, 2, 1, '', 'y')),
        6: ((0, 0, 0, 'ry', 'l'), (0, 3, 1, 'l', 'r')),
        7: ((0, 1, 0, 'ry', 'l'), (0, 3, 0, 'ly', 'r'), (0, 1, 1, 'ry', 'l'), (0, 2, 0, 'lry', ''), (0, 2, 1, 'lry', '')),
    },
    3: {
        0: ((1, 0, 0, '', 'y'), (1, 0, 1, '', 'l')),
        1: ((1, 1, 0, '', 'y'), (1, 1, 1, '', 'y')),
        2: ((0, 0, 1, '', 'l'), (0, 0, 0, 'y', 'l')),
        3: ((1, 2, 0, '', 'y'), (1, 2, 1, '', 'y')),
        4: ((0, 1, 0, 'y', 'l'),),
        5: ((0, 1, 1, 'y', 'l'), (1, 3, 0, '', 'y')),
        6: ((1, 3, 1, 'l', 'y'), (0, 2, 0, 'y', 'l')),
        7: ((0, 2, 1, 'y', 'l'), (0, 3, 0, 'ly', ''), (0, 3, 1, 'ly', '')),
    },
}
SUB = 256
GROUP = 6


def lookup(table, z, step):
    value = jnp.int32(0)
    for k in range(NZ):
        for s in range(2 * NZ):
            value = value + jnp.where((z == k) & (step == s), table[k][s], 0)
    return value


def head_kernel(scale, token_scale, f_ref, lab_ref, e_ref, dfin_ref, ghead_ref, norm_ref, labsum_ref, z_ref,
                e_b, e_t, fbuf, f_b, g_acc, from_y, from_l, from_r, dl, z_buf, z_rest, lse_all, z_sem, load_sem, ag_send, ag_recv,
                send_y, send_l, send_r, recv_y, recv_l, recv_r, st_send, st_recv):
    tp, dp, z, y = place()
    partner = tp + 1 - 2 * y
    vocab, width = e_ref.shape
    own = f_ref.shape[0]
    whole = vocab // (SUB * GROUP)
    rest = vocab - whole * SUB * GROUP
    log2e = 1.4426950408889634
    slope = scale * log2e
    blocks = [(j * SUB, SUB) for j in range(GROUP)]
    tail = [(n, min(SUB, rest - n)) for n in range(0, rest, SUB)]

    plane_barrier(tp, dp, [])

    half = own // 2
    to_tp = {"l": tp - 2, "r": tp + 2, "y": partner}

    def slot_of(o, zz):
        return 2 * zz + (1 - y if o else y)

    def piece(ref, h):
        return ref.at[pl.ds(h * half, half), :]

    def pass_on(o, zz, h, to, own_chunk=False):
        slot = slot_of(o, zz)
        return remote(piece(f_ref if own_chunk else fbuf.at[slot], h), piece(fbuf.at[slot], h), ag_send.at["lry".index(to), slot, h],
                      ag_recv.at[slot, h], to_tp[to], dp)

    def arrived(o, zz, h):
        slot = slot_of(o, zz)
        remote(piece(f_ref, h), piece(fbuf.at[slot], h), ag_send.at[0, slot, h], ag_recv.at[slot, h], partner, dp).wait_recv()

    def own_sends(k):
        first = (1, 0) if k in (0, NZ - 1) else (0, 1)
        return [pass_on(0, k, h, "y", True) for h in first] + [
            pass_on(0, k, h, to, True) for h in range(2) for to in ("l" if k > 0 else "") + ("r" if k < NZ - 1 else "")]

    def on_position(f):
        for k in range(NZ):
            pl.when(z == k)(functools.partial(f, k))

    def first_sends(k):
        for c in own_sends(k):
            c.start()

    on_position(first_sends)
    load = pltpu.make_async_copy(e_ref, g_acc, load_sem.at[0])
    load.start()
    own_copy = pltpu.make_async_copy(f_ref, fbuf.at[tp], load_sem.at[1])
    own_copy.start()
    load.wait()

    def prepare(at, size):
        part = g_acc[at, :]
        e_b[at, :] = part.astype(BF16)
        e_t[:, at] = part.T.astype(BF16)

    def prepare_body(n, carry):
        prepare(pl.ds(pl.multiple_of(n * SUB, SUB), SUB), SUB)
        return carry

    lax.fori_loop(0, vocab // SUB, prepare_body, 0)
    if vocab % SUB:
        prepare(pl.ds(vocab // SUB * SUB, vocab % SUB), vocab % SUB)
    own_copy.wait()

    big = SUB * GROUP

    def z_copies(slot, n, out):
        if n is None:
            pair = (z_rest, z_ref.at[slot, pl.ds(whole * big, rest), :])
            sem = z_sem.at[2]
        else:
            pair = (z_buf.at[lax.rem(n, 2)], z_ref.at[slot, pl.ds(pl.multiple_of(n * big, big), big), :])
            sem = z_sem.at[lax.rem(n, 2)]
        return pltpu.make_async_copy(*(pair if out else pair[::-1]), sem)

    def slot_at(order, step):
        code = lookup({k: [2 * zz + o for o, zz in order[k]] for k in range(NZ)}, z, step)
        other = code % 2
        return code // 2 * 2 + y + other - 2 * y * other

    def gather_step(step, carry):
        for k in range(NZ):
            for at, events in GATHER_EVENTS[k].items():
                def serve(events=events):
                    for o, zz, h, to in events:
                        arrived(o, zz, h)
                        for t in to:
                            pass_on(o, zz, h, t).start()
                pl.when((z == k) & (step == at))(serve)
        slot = slot_at(GATHER_ORDER, step)
        f_b[slot] = fbuf[slot].astype(BF16)
        f_now = f_b[slot]

        def group(base, parts, kept, c):
            top, total = c
            for first, size in parts:
                logit = lax.dot_general(e_b[pl.ds(base + first, size), :], f_now, (((1,), (1,)), ((), ())), preferred_element_type=F32)
                kept[pl.ds(first, size), :] = logit
                logit = logit.reshape(size // 8, 8, own)
                new = jnp.maximum(top, jnp.max(logit, axis=0))
                total = total * jnp.exp2((top - new) * slope) + jnp.sum(jnp.exp2((logit - new[None]) * slope), axis=0)
                top = new
            return top, total

        def body(n, c):
            @pl.when(step * whole + n >= 2)
            def _():
                z_copies(slot, n, True).wait()
            c = group(pl.multiple_of(n * big, big), blocks, z_buf.at[lax.rem(n, 2)], c)
            z_copies(slot, n, True).start()
            return c

        top, total = lax.fori_loop(0, whole, body, (jnp.full((8, own), -3e38, F32), jnp.zeros((8, own), F32)))
        if tail:
            @pl.when(step > 0)
            def _():
                z_copies(slot, None, True).wait()
            top, total = group(whole * big, tail, z_rest, (top, total))
            z_copies(slot, None, True).start()
        most = jnp.max(top, axis=0, keepdims=True)
        total = jnp.sum(total * jnp.exp2((top - most) * slope), axis=0, keepdims=True)
        lse_all[tp, pl.ds(slot, 1), :] = most * scale + jnp.log(total)
        return carry

    lax.fori_loop(0, 2 * NZ, gather_step, 0)
    for n in range(2):
        z_copies(0, jnp.int32(n), True).wait()
    if tail:
        z_copies(0, None, True).wait()

    for n in range(1, 2 * NZ):
        to = lax.rem(tp + n, 2 * NZ)
        remote(lse_all.at[tp], lse_all.at[tp], st_send.at[to], st_recv.at[tp], to, dp).start()

    def gathers_done(k):
        for c in own_sends(k):
            c.wait_send()
        for events in GATHER_EVENTS[k].values():
            for o, zz, h, to in events:
                for t in to:
                    pass_on(o, zz, h, t).wait_send()

    on_position(gathers_done)
    start_slot = slot_at(SCATTER_ORDER, 0)
    for n in range(2):
        z_copies(start_slot, jnp.int32(n), False).start()
    if tail:
        z_copies(start_slot, None, False).start()

    def clear(n, carry):
        g_acc[pl.ds(pl.multiple_of(n * 16, 16), 16), :] = jnp.zeros((16, width), F32)
        return carry

    lax.fori_loop(0, vocab // 16, clear, 0)
    for n in range(1, 2 * NZ):
        source = lax.rem(tp + n, 2 * NZ)
        remote(lse_all.at[source], lse_all.at[source], st_send.at[source], st_recv.at[source], source, dp).wait_recv()
    peak = jnp.max(lse_all[...], axis=0)
    log_norm = peak + jnp.log(jnp.sum(jnp.exp(lse_all[...] - peak[None]), axis=0))
    norm_ref[...] = log_norm

    def leave(o, zz, h, to):
        src = piece(fbuf.at[slot_of(o, zz)], h)
        if to == "y":
            at = 2 * zz + h
            return remote(src, from_y.at[at], send_y.at[at], recv_y.at[at], partner, dp)
        if to == "l":
            at = 6 if o else 2 * zz + h
            return remote(src, from_r.at[at], send_l.at[at], recv_r.at[at], tp - 2, dp)
        at = 6 if o else 2 * zz - 2 + h
        return remote(src, from_l.at[at], send_r.at[at], recv_l.at[at], tp + 2, dp)

    def collect(o, zz, h, sums, to):
        here = piece(fbuf.at[slot_of(o, zz)], h)
        for d in sums:
            at, buf, sem = {"y": (2 * zz + h, from_y, recv_y), "l": (6 if o else 2 * zz - 2 + h, from_l, recv_l),
                            "r": (6 if o else 2 * zz + h, from_r, recv_r)}[d]
            remote(here, buf.at[at], send_y.at[0], sem.at[at], partner, dp).wait_recv()
            add_into(here, buf.at[at])
        if to:
            leave(o, zz, h, to).start()

    def scatter_step(step, lab_sum):
        slot = slot_at(SCATTER_ORDER, step)
        f_now = f_b[slot]
        acc = fbuf.at[slot]
        norm = norm_ref[pl.ds(slot, 1), :]
        shift = norm * log2e
        coef = (1.0 + 2.0 * LOGIT_ZLOSS * norm) * token_scale
        lab = lab_ref[pl.ds(slot // 2, 1), pl.ds(pl.multiple_of(lax.rem(slot, 2) * own, own), own)] - tp * vocab
        acc[...] = jnp.zeros((width, own), F32)

        def group(base, parts, kept, hits):
            for first, size in parts:
                at = pl.ds(base + first, size)
                logit = kept[pl.ds(first, size), :]
                hit = lax.broadcasted_iota(jnp.int32, (size, own), 0) == lab - (base + first)
                prob = jnp.exp2(logit * slope - shift) * coef
                grad = jnp.where(hit, prob - token_scale, prob).astype(BF16)
                hits = hits + jnp.sum(jnp.where(hit, logit, 0.0).reshape(size // 8, 8, own), axis=0)
                dl[pl.ds(first, size), :] = grad
                g_acc[at, :] += jnp.dot(grad, f_now, preferred_element_type=F32)
            size = parts[-1][0] + parts[-1][1]
            acc[...] += jnp.dot(e_t[:, pl.ds(base, size)], dl[pl.ds(0, size), :], preferred_element_type=F32)
            return hits

        following = slot_at(SCATTER_ORDER, jnp.minimum(step + 1, 2 * NZ - 1))

        def body(n, hits):
            z_copies(slot, n, False).wait()
            hits = group(pl.multiple_of(n * big, big), blocks, z_buf.at[lax.rem(n, 2)], hits)

            @pl.when(n + 2 < whole)
            def _():
                z_copies(slot, n + 2, False).start()

            @pl.when((n + 2 >= whole) & (step + 1 < 2 * NZ))
            def _():
                z_copies(following, n + 2 - whole, False).start()
            return hits

        lab_sum = lax.fori_loop(0, whole, body, lab_sum)
        if tail:
            z_copies(slot, None, False).wait()
            lab_sum = group(whole * big, tail, z_rest, lab_sum)

            @pl.when(step + 1 < 2 * NZ)
            def _():
                z_copies(following, None, False).start()

        for k in range(NZ):
            for at, events in SCATTER_EVENTS[k].items():
                def reduce(events=events):
                    for event in events:
                        collect(*event)
                pl.when((z == k) & (step == at))(reduce)
        return lab_sum

    lab_sum = lax.fori_loop(0, 2 * NZ, scatter_step, jnp.zeros((8, own), F32))
    labsum_ref[...] = lab_sum
    store = pltpu.make_async_copy(g_acc, ghead_ref, load_sem.at[0])
    store.start()
    dfin_ref[...] = fbuf[tp].T

    def scatters_done(k):
        for events in SCATTER_EVENTS[k].values():
            for o, zz, h, _, to in events:
                if to:
                    leave(o, zz, h, to).wait_send()

    on_position(scatters_done)
    for n in range(1, 2 * NZ):
        to = lax.rem(tp + n, 2 * NZ)
        remote(lse_all.at[tp], lse_all.at[tp], st_send.at[to], st_recv.at[tp], to, dp).wait_send()
    store.wait()


def head(f_own, labels, embed, scale, token_scale, collective_id):
    own, width = f_own.shape
    vocab = embed.shape[0]
    chunk = (own, width)
    strips = lambda n: pltpu.VMEM((n, own // 2, width), F32)
    dma = lambda *n: pltpu.SemaphoreType.DMA(n)
    return pl.pallas_call(
        functools.partial(head_kernel, scale, token_scale),
        out_shape=(jax.ShapeDtypeStruct((own, width), F32), jax.ShapeDtypeStruct((vocab, width), F32),
                   jax.ShapeDtypeStruct((2 * NZ, own), F32), jax.ShapeDtypeStruct((8, own), F32),
                   jax.ShapeDtypeStruct((2 * NZ, vocab, own), F32)),
        in_specs=[VMEM, VMEM, ANY],
        out_specs=(VMEM, ANY, VMEM, VMEM, ANY),
        scratch_shapes=[pltpu.VMEM((vocab, width), BF16), pltpu.VMEM((width, vocab), BF16),
                        pltpu.VMEM((2 * NZ,) + chunk, F32), pltpu.VMEM((2 * NZ,) + chunk, BF16), pltpu.VMEM((vocab, width), F32),
                        strips(8), strips(7), strips(7),
                        pltpu.VMEM((SUB * GROUP, own), BF16), pltpu.VMEM((2, SUB * GROUP, own), F32),
                        pltpu.VMEM((max(vocab % (SUB * GROUP), 8), own), F32), pltpu.VMEM((2 * NZ, 2 * NZ, own), F32),
                        dma(3), dma(2), dma(3, 2 * NZ, 2), dma(2 * NZ, 2), dma(8), dma(7), dma(7), dma(8), dma(7), dma(7), dma(2 * NZ), dma(2 * NZ)],
        compiler_params=pltpu.CompilerParams(collective_id=collective_id, has_side_effects=True, vmem_limit_bytes=67000000),
        cost_estimate=pl.CostEstimate(flops=8 * vocab * width * own * 8, bytes_accessed=3 * 4 * vocab * width, transcendentals=2 * vocab * own * 8),
        name="head",
    )(f_own, labels, embed)


TB = (((1,), (1,)), ((), ()))
TA = (((0,), (0,)), ((), ()))
LOG2E = 1.4426950408889634


def mm(a, b, dims=(((1,), (0,)), ((), ()))):
    return lax.dot_general(a, b, dims, preferred_element_type=F32)


def picks(code, n_slots):
    return (lax.broadcasted_iota(jnp.int32, (n_slots, code.shape[1]), 0) == code).astype(F32).astype(BF16)


def turn(lo, hi, cos_t, sin_t):
    return lo * cos_t - hi * sin_t, hi * cos_t + lo * sin_t


EVENTS = {
    0: (((("R", 1),), (0,)), ((("R", 2),), (1,)), ((("R", 3),), (2,)), ((), (3,))),
    1: (((("L", 0), ("R", 2)), (1,)), ((("R", 3),), (0,)), ((), (2,)), ((), (3,))),
    2: (((("R", 3), ("L", 1)), (2,)), ((("L", 0),), (3,)), ((), (1,)), ((), (0,))),
    3: (((("L", 2),), (3,)), ((("L", 1),), (2,)), ((("L", 0),), (1,)), ((), (0,))),
}
MLP_ORDER = {k: [2 * k] + [code for line, other in EVENTS[k] for code in [2 * zz for _, zz in line] + [2 * zz + 1 for zz in other]] for k in range(NZ)}


def front_kernel(ids_ref, e_ref, rounds_ref, code_ref, extra_ref, w_ref, wkv_ref, ln_ref, cos_ref, sin_ref,
                 f_ref, x1_ref, x0_ref, q_ref, kv_ref, kvt_ref, lse_ref, ctx_ref, wq_ref, wo_ref, wg_out, wu_out, wd_out, rounds_all,
                 wg_ref, wu_ref, wd_ref, w_sem, table, rows_ref, wl, rows_in, u_b, kv_out, kv_in, own_sem, r_send, r_recv, a_y, a_l, a_r, a_c, a_recv,
                 b_y, b_l, b_r, b_x, b_c, b_recv, kv_send, kv_recv, n_send, n_recv):
    tp, dp, z, y = place()
    partner = tp + 1 - 2 * y
    core = dp % 2
    twin = dp + 1 - 2 * core
    facing = lax.rem(dp + 2, 4)
    own, width = x0_ref.shape
    shards, w_rows = wl.shape[0], wl.shape[1]
    nq = q_ref.shape[0]
    ff = wg_out.shape[0]
    n_a = nq // shards
    n_f = ff // shards
    n_b = 3 * n_f // 4
    hd = kv_out.shape[0] // 2
    quarter = hd // 2
    heads = nq // hd

    def a_rows(c):
        return pl.ds(pl.multiple_of(c * n_a, 8), n_a)

    def b_rows(d):
        return pl.ds(pl.multiple_of(2 * n_a + d * n_b, 8), n_b)

    def a_copy(slot, sems, to, to_dp, first=False):
        src = w_ref.at[a_rows(core), :] if first else wl.at[slot, a_rows(core), :]
        return remote(src, wl.at[slot, a_rows(core), :], sems.at[slot], a_recv.at[slot, core], to, to_dp)

    def b_copy(slot, piece, sems, to, to_dp, first=False):
        src = w_ref.at[b_rows(piece), :] if first else wl.at[slot, b_rows(piece), :]
        return remote(src, wl.at[slot, b_rows(piece), :], sems.at[slot], b_recv.at[slot, piece], to, to_dp)

    def a_wait(slot, c):
        remote(w_ref.at[a_rows(c), :], wl.at[slot, a_rows(c), :], a_y.at[slot], a_recv.at[slot, c], partner, dp).wait_recv()

    def b_wait(slot, piece):
        remote(w_ref.at[b_rows(piece), :], wl.at[slot, b_rows(piece), :], b_y.at[slot], b_recv.at[slot, piece], partner, dp).wait_recv()

    def on_position(f):
        for k in range(NZ):
            pl.when(z == k)(functools.partial(f, k))

    def line_sends(k, make, y_sems, l_sems, r_sems, slot, side, first=False):
        sends = [make(slot, y_sems, partner, dp, first)]
        if k > 0 and side != "L":
            sends.append(make(slot, l_sems, tp - 2, dp, first))
        if k < NZ - 1 and side != "R":
            sends.append(make(slot, r_sems, tp + 2, dp, first))
        return sends

    def b_own(slot, sems, to, to_dp, first=False):
        return b_copy(slot, dp, sems, to, to_dp, first)

    def a_sends(k, slot, side, first=False):
        return line_sends(k, a_copy, a_y, a_l, a_r, slot, side, first)

    def b_sends(k, slot, side, first=False):
        return line_sends(k, b_own, b_y, b_l, b_r, slot, side, first)

    def start(copies):
        for c in copies:
            c.start()

    load = pltpu.make_async_copy(e_ref, table, own_sem.at[2])
    load.start()
    group = [twin, facing, lax.rem(twin + 2, 4)]
    plane_barrier(tp, dp, [(tp, d) for d in group])
    peers = [lax.rem(tp + n, shards) for n in range(1, shards)]

    def rounds_copy(n):
        return remote(rounds_ref, rounds_all.at[dp], n_send.at[n], n_recv.at[dp], tp, group[n])

    for n in range(3):
        rounds_copy(n).start()
    rounds_all[dp] = rounds_ref[...]

    def row_copy(to):
        return remote(rows_ref.at[to], rows_in.at[tp], r_send.at[to], r_recv.at[tp], to, dp)

    on_position(lambda k: start(b_sends(k, tp, "", True)))
    on_position(lambda k: start(a_sends(k, tp, "", True)))
    own_w = pltpu.make_async_copy(w_ref, wl.at[tp], own_sem.at[1])
    own_w.start()

    def a_event(t, k):
        line, other = EVENTS[k][t]
        for side, zz in line:
            slot = 2 * zz + y
            a_wait(slot, core)
            start(a_sends(k, slot, side))
            a_copy(slot, a_c, tp, twin).start()
        for zz in other:
            slot = 2 * zz + 1 - y
            a_wait(slot, core)
            a_copy(slot, a_c, tp, twin).start()

    def b_event(t, k):
        line, other = EVENTS[k][t]
        for side, zz in line:
            slot = 2 * zz + y
            b_wait(slot, dp)
            start(b_sends(k, slot, side))
            b_copy(slot, dp, b_x, tp, facing).start()
            b_copy(slot, dp, b_c.at[0], tp, twin).start()
        for zz in other:
            slot = 2 * zz + 1 - y
            b_wait(slot, dp)
            b_copy(slot, dp, b_x, tp, facing).start()
            b_copy(slot, dp, b_c.at[0], tp, twin).start()

    load.wait()
    cap = rows_ref.shape[1]

    def pick_rows(n, carry):
        for i in range(8):
            rows_ref[n // (cap // 8), pl.ds(lax.rem(n, cap // 8) * 8 + i, 1), :] = table[pl.ds(ids_ref[n * 8 + i], 1), :]
        return carry

    lax.fori_loop(0, shards * cap // 8, pick_rows, 0)
    on_position(functools.partial(b_event, 0))
    on_position(functools.partial(a_event, 0))
    on_position(functools.partial(b_event, 1))
    on_position(functools.partial(a_event, 1))
    on_position(lambda k: start([row_copy(2 * zz + (1 - y if o else y)) for o, zz in near_first(k)[1:]]))
    own_rows = pltpu.make_async_copy(rows_ref.at[tp], rows_in.at[tp], own_sem.at[0])
    own_rows.start()
    own_rows.wait()
    for source in peers:
        remote(rows_ref.at[source], rows_in.at[source], r_send.at[source], r_recv.at[source], source, dp).wait_recv()
    n_slots = shards * cap
    x0_ref[...] = extra_ref[...] + mm(picks(code_ref[...], n_slots), rows_in[...].reshape(n_slots, width).astype(BF16), TA)
    u_b[...] = norm_fwd(x0_ref[...], ln_ref[0:1, :])[0]
    x1_ref[...] = x0_ref[...]
    cos_t = cos_ref[...]
    sin_t = sin_ref[...]
    kv = mm(wkv_ref[...].reshape(2 * hd, width).astype(BF16), u_b[...], TB)
    lo, hi = turn(kv[:quarter], kv[quarter:hd], cos_t, sin_t)
    kv_out[0:quarter, :] = lo
    kv_out[quarter:hd, :] = hi
    kv_out[hd:, :] = kv[hd:]
    kv_copy = remote(kv_out, kv_in, kv_send, kv_recv, partner, dp)
    kv_copy.start()

    def slot_of(step):
        code = lookup(MLP_ORDER, z, step)
        other = code % 2
        return code // 2 * 2 + y + other - 2 * y * other

    def w_stores(slot):
        at = pl.ds(pl.multiple_of(slot * n_f, n_f), n_f)
        return [pltpu.make_async_copy(src.at[at, :], dst.at[at, :], w_sem.at[i, slot])
                for i, (src, dst) in enumerate(((wg_ref, wg_out), (wu_ref, wu_out), (wd_ref, wd_out)))]

    def mlp(step, carry):
        def pass_on():
            slot = slot_of(step + 1)
            b_wait(slot, facing)
            b_copy(slot, facing, b_c.at[1], tp, twin).start()
        pl.when(step < shards - 1)(pass_on)
        slot = slot_of(step)

        def rest():
            b_wait(slot, twin)
            b_wait(slot, lax.rem(twin + 2, 4))
        pl.when(step > 0)(rest)
        at = pl.ds(pl.multiple_of(slot * n_f, n_f), n_f)
        wg_ref[at, :] = wl[slot, 2 * n_a:2 * n_a + n_f, :].astype(BF16)
        wu_ref[at, :] = wl[slot, 2 * n_a + n_f:2 * n_a + 2 * n_f, :].astype(BF16)
        wd_ref[at, :] = wl[slot, 2 * n_a + 2 * n_f:2 * n_a + 3 * n_f, :].astype(BF16)
        for c in w_stores(slot):
            c.start()
        gate = mm(u_b[...], wg_ref[at, :], TB)
        up = mm(u_b[...], wu_ref[at, :], TB)
        x1_ref[...] += mm((gate * jax.nn.sigmoid(gate) * up).astype(BF16), wd_ref[at, :])
        return carry

    own_w.wait()
    lax.fori_loop(0, 3, mlp, 0)
    on_position(functools.partial(b_event, 2))
    on_position(functools.partial(a_event, 2))
    lax.fori_loop(3, 4, mlp, 0)
    on_position(functools.partial(a_event, 3))
    on_position(functools.partial(b_event, 3))
    for source in peers:
        a_wait(source, 1 - core)
    for s in range(shards):
        wq_ref[s * n_a:(s + 1) * n_a, :] = wl[s, 0:n_a, :].astype(BF16)
        wo_ref[s * n_a:(s + 1) * n_a, :] = wl[s, n_a:2 * n_a, :].astype(BF16)

    q_all = mm(wq_ref[...], u_b[...], TB)
    for h in range(heads):
        lo, hi = turn(q_all[h * hd:h * hd + quarter], q_all[h * hd + quarter:(h + 1) * hd], cos_t, sin_t)
        q_ref[h * hd:h * hd + quarter, :] = lo.astype(BF16)
        q_ref[h * hd + quarter:(h + 1) * hd, :] = hi.astype(BF16)
    kv_copy.wait()

    def fill(mine, other):
        kv_ref[mine * own:(mine + 1) * own, :] = kv_out[...].T.astype(BF16)
        kv_ref[other * own:(other + 1) * own, :] = kv_in[...].T.astype(BF16)
        kvt_ref[:, mine * own:(mine + 1) * own] = kv_out[...].astype(BF16)
        kvt_ref[:, other * own:(other + 1) * own] = kv_in[...].astype(BF16)

    pl.when(y == 0)(lambda: fill(0, 1))
    pl.when(y == 1)(lambda: fill(1, 0))
    blank = jnp.zeros((hd, own), BF16)
    slope = hd ** -0.5 * LOG2E

    def attend(h, carry):
        at = pl.ds(pl.multiple_of(h * hd, hd), hd)
        scores = mm(kv_ref[...], jnp.concatenate([q_ref[at, :], blank], axis=0))
        allowed = lax.broadcasted_iota(jnp.int32, scores.shape, 0) <= lax.broadcasted_iota(jnp.int32, scores.shape, 1) + y * own
        scores = jnp.where(allowed, scores * slope, -1e30)
        top = jnp.max(scores, axis=0, keepdims=True)
        prob = jnp.exp2(scores - top)
        total = jnp.sum(prob, axis=0, keepdims=True)
        lse_ref[pl.ds(h, 1), :] = top + jnp.log2(total)
        ctx_ref[at, :] = mm(kvt_ref[hd:, :], (prob * (1.0 / total)).astype(BF16)).astype(BF16)
        return carry

    lax.fori_loop(0, heads, attend, 0)
    x1_ref[...] += mm(ctx_ref[...], wo_ref[...], TA)

    lax.fori_loop(4, shards, mlp, 0)
    f_ref[...] = norm_fwd(x1_ref[...], ln_ref[1:2, :])[0].astype(F32)

    def finish(k):
        done = a_sends(k, tp, "", True) + b_sends(k, tp, "", True)
        for line, other in EVENTS[k]:
            for side, zz in line:
                done += a_sends(k, 2 * zz + y, side) + b_sends(k, 2 * zz + y, side)
        for c in done:
            c.wait_send()

    on_position(finish)
    for slot in range(shards):
        for c in w_stores(slot):
            c.wait()
    for n in range(3):
        rounds_copy(n).wait_send()
        remote(rounds_ref, rounds_all.at[group[n]], n_send.at[n], n_recv.at[group[n]], tp, twin).wait_recv()
    for to in peers:
        row_copy(to).wait_send()
        a_copy(to, a_c, tp, twin).wait_send()
        b_copy(to, dp, b_x, tp, facing).wait_send()
        b_copy(to, dp, b_c.at[0], tp, twin).wait_send()
        b_copy(to, facing, b_c.at[1], tp, twin).wait_send()


def front(ids, embed, rounds, code, extra, w_rows, wkv_t, ln, cos_t, sin_t, n_q, collective_id):
    own, width = extra.shape
    two_hd = 2 * wkv_t.shape[1]
    shards = 2 * NZ
    ff = (w_rows.shape[0] * shards - 2 * n_q) // 3
    dma = lambda *n: pltpu.SemaphoreType.DMA(n)
    s = jax.ShapeDtypeStruct
    rows = (shards, ids.shape[0] // shards, width)
    return pl.pallas_call(
        front_kernel,
        out_shape=(s((own, width), F32),) * 3 + (s((n_q, own), BF16), s((2 * own, two_hd), BF16), s((two_hd, 2 * own), BF16),
                   s((2 * n_q // two_hd, own), F32), s((n_q, own), BF16), s((n_q, width), BF16), s((n_q, width), BF16))
        + (s((ff, width), BF16),) * 3 + (s((4, 1, 128), jnp.int32),),
        in_specs=[pl.BlockSpec(memory_space=pltpu.SMEM), ANY, VMEM, VMEM, VMEM, ANY] + [VMEM] * 4,
        out_specs=(VMEM,) * 10 + (ANY,) * 3 + (VMEM,),
        scratch_shapes=[pltpu.VMEM((ff, width), BF16)] * 3 + [dma(3, shards), pltpu.VMEM(embed.shape, F32), pltpu.VMEM(rows, F32), pltpu.VMEM((shards,) + w_rows.shape, F32), pltpu.VMEM(rows, F32), pltpu.VMEM((own, width), BF16),
                        pltpu.VMEM((two_hd, own), F32), pltpu.VMEM((two_hd, own), F32),
                        dma(3), dma(shards), dma(shards)] + [dma(shards)] * 4 + [dma(shards, 2)]
        + [dma(shards)] * 4 + [dma(2, shards), dma(shards, 4), pltpu.SemaphoreType.DMA, pltpu.SemaphoreType.DMA, dma(3), dma(4)],
        compiler_params=pltpu.CompilerParams(collective_id=collective_id, has_side_effects=True, vmem_limit_bytes=60000000),
        name="front",
    )(ids, embed, rounds, code, extra, w_rows, wkv_t, ln, cos_t, sin_t)


def layer_bwd_kernel(scale, tok_total, dfin_ref, x0_ref, x1_ref, norm_ref, hits_ref, ln_ref, cos_ref, sin_ref, wq_ref, wkv_ref, wo_ref, wg_any, wu_any, wd_any,
                     q_ref, kv_ref, kvt_ref, lse_ref, ctx_ref, code_ref, g_ref, ids_ref, rows_ref, d0_ref, back_ref, early_ref, ids_all, d_one, d_b, u_b, dctx, dq, dkv, dkv_in,
                     hid, d_gate, d_up, rows_out, g_q, g_o, g_g, g_u, g_d, small, s_early, c_early, wg_ref, wu_ref, wd_ref, w_sem, out_sem, send_sem, recv_sem,
                     r_send, x_send, c_send, r_recv, g_load, g_send, g_recv, id_send, id_recv):
    tp, dp, z, y = place()
    partner = tp + 1 - 2 * y
    core = dp % 2
    twin = dp + 1 - 2 * core
    facing = lax.rem(dp + 2, 4)
    across = lax.rem(twin + 2, 4)
    own, width = x0_ref.shape
    hd = kv_ref.shape[1] // 2
    quarter = hd // 2
    nq = q_ref.shape[0]
    heads = nq // hd
    ff = wg_ref.shape[0]
    shards = rows_ref.shape[0]
    w_loads = [pltpu.make_async_copy(src, dst, w_sem.at[i]) for i, (src, dst) in enumerate(((wg_any, wg_ref), (wu_any, wu_ref), (wd_any, wd_ref)))]
    for c in w_loads:
        c.start()
    plane_barrier(tp, dp, [(tp, twin), (tp, facing), (tp, across)])

    n_early, g_size = s_early.shape[0], s_early.shape[1]

    def g_rows(which, b):
        return g_ref.at[pl.ds(pl.multiple_of(which * (g_ref.shape[0] // 2) + b * g_size, 8), g_size), :]

    def g_load_copy(b):
        return pltpu.make_async_copy(g_rows(core, b), s_early.at[b], g_load.at[b])

    def g_chip_copy(b):
        return remote(g_rows(1 - core, b), c_early.at[b], g_send.at[0, b], g_recv.at[0, b], tp, twin)

    def g_x_copy(b):
        return remote(s_early.at[b], early_ref.at[b], g_send.at[1, b], g_recv.at[1, b], tp, facing)

    for b in range(n_early):
        g_chip_copy(b).start()
        g_load_copy(b).start()

    def ids_copy(n, to):
        return remote(ids_ref, ids_all.at[dp], id_send.at[n], id_recv.at[dp], tp, to)

    for n, to in enumerate((twin, facing, across)):
        ids_copy(n, to).start()
    ids_all[dp] = ids_ref[...]
    _, f_hat, f_inv = norm_fwd(x1_ref[...], ln_ref[1:2, :])
    d_in, g_fin = norm_bwd(dfin_ref[...], f_hat, f_inv, ln_ref[1:2, :])
    d_one[...] = d_in
    d_b[...] = d_in.astype(BF16)
    u_b[...] = norm_fwd(x0_ref[...], ln_ref[0:1, :])[0]
    dctx[...] = mm(wo_ref[...], d_b[...], TB).astype(BF16)
    for b in range(n_early):
        g_load_copy(b).wait()
        g_chip_copy(b).wait_recv()
        add_into(s_early.at[b], c_early.at[b], 24)
        g_x_copy(b).start()
    cos_t = cos_ref[...]
    sin_t = sin_ref[...]
    blank = jnp.zeros((hd, own), BF16)
    slope = hd ** -0.5 * LOG2E
    dkv[...] = jnp.zeros_like(dkv)

    def attend(h, carry):
        at = pl.ds(pl.multiple_of(h * hd, hd), hd)
        q_pad = jnp.concatenate([q_ref[at, :], blank], axis=0)
        d_pad = jnp.concatenate([blank, dctx[at, :]], axis=0)
        scores = mm(kv_ref[...], q_pad)
        allowed = lax.broadcasted_iota(jnp.int32, scores.shape, 0) <= lax.broadcasted_iota(jnp.int32, scores.shape, 1) + y * own
        prob = jnp.where(allowed, jnp.exp2(scores * slope - lse_ref[pl.ds(h, 1), :]), 0.0)
        d_prob = mm(kv_ref[...], d_pad)
        mean = jnp.sum(d_prob * prob, axis=0, keepdims=True)
        d_score = (prob * (d_prob - mean) * hd ** -0.5).astype(BF16)
        dkv[...] += mm(d_score, q_pad, TB) + mm(prob.astype(BF16), d_pad, TB)
        d_q = mm(kvt_ref[0:hd, :], d_score)
        lo, hi = turn(d_q[:quarter], d_q[quarter:], cos_t, -sin_t)
        dq[at, :] = jnp.concatenate([lo, hi], axis=0).astype(BF16)
        return carry

    lax.fori_loop(0, heads, attend, 0)
    copy = remote(dkv.at[pl.ds(pl.multiple_of((1 - y) * own, own), own), :], dkv_in, send_sem, recv_sem, partner, dp)
    copy.start()

    d0_ref[...] = mm(dq[...], wq_ref[...], TA)
    step = min(512, ff)
    for c in w_loads:
        c.wait()

    def mlp(n, carry):
        at = pl.ds(pl.multiple_of(n * step, step), step)
        gate = mm(wg_ref[at, :], u_b[...], TB)
        up = mm(wu_ref[at, :], u_b[...], TB)
        d_hidden = mm(wd_ref[at, :], d_b[...], TB)
        sig = jax.nn.sigmoid(gate)
        hid[at, :] = (gate * sig * up).astype(BF16)
        d_gate[at, :] = (d_hidden * up * sig * (1.0 + gate * (1.0 - sig))).astype(BF16)
        d_up[at, :] = (d_hidden * gate * sig).astype(BF16)
        d0_ref[...] += mm(d_gate[at, :], wg_ref[at, :], TA) + mm(d_up[at, :], wu_ref[at, :], TA)
        return carry

    lax.fori_loop(0, ff // step, mlp, 0)
    copy.wait()
    d_kv = (dkv[pl.ds(pl.multiple_of(y * own, own), own), :] + dkv_in[...]).T
    lo, hi = turn(d_kv[:quarter], d_kv[quarter:hd], cos_t, -sin_t)
    d_kv = jnp.concatenate([lo, hi, d_kv[hd:]], axis=0).astype(BF16)
    small[0:2 * hd, :] = mm(d_kv, u_b[...])
    d_u = d0_ref[...] + mm(d_kv, wkv_ref[...].reshape(2 * hd, width).astype(BF16), TA)
    _, u_hat, u_inv = norm_fwd(x0_ref[...], ln_ref[0:1, :])
    d_in, g_in = norm_bwd(d_u, u_hat, u_inv, ln_ref[0:1, :])
    d_zero = d_one[...] + d_in
    d0_ref[...] = d_zero
    high = d_zero.astype(BF16)
    left = d_zero - high.astype(F32)
    middle = left.astype(BF16)
    low = (left - middle.astype(F32)).astype(BF16)
    pick = picks(code_ref[...], rows_out.shape[0] * rows_out.shape[1])
    rows_out[...] = (mm(pick, high) + mm(pick, middle) + mm(pick, low)).reshape(rows_out.shape)

    def row_copy(to):
        return remote(rows_out.at[to], back_ref.at[dp, tp], r_send.at[to], r_recv.at[dp, tp], to, dp)

    def x_copy(slot):
        return remote(back_ref.at[dp, slot], back_ref.at[dp, slot], x_send.at[slot], r_recv.at[dp, slot], tp, facing)

    def c_copy(group, n, slot):
        return remote(back_ref.at[group, slot], back_ref.at[group, slot], c_send.at[n, slot], r_recv.at[group, slot], tp, twin)

    def back(group, slot):
        remote(rows_out.at[slot], back_ref.at[group, slot], r_send.at[slot], r_recv.at[group, slot], tp, twin).wait_recv()

    def slot_of(o, zz):
        return 2 * zz + (1 - y if o else y)

    def on_position(f):
        for k in range(NZ):
            pl.when(z == k)(functools.partial(f, k))

    def rows_leave(k):
        for c in near_first(k)[1:]:
            row_copy(slot_of(*c)).start()

    on_position(rows_leave)
    own_rows = pltpu.make_async_copy(rows_out.at[tp], back_ref.at[dp, tp], out_sem.at[7 * 2 * NZ])
    own_rows.start()
    own_rows.wait()
    x_copy(tp).start()
    c_copy(dp, 0, tp).start()

    g_o[...] = mm(ctx_ref[...], d_b[...])
    g_q[...] = mm(dq[...], u_b[...])

    def weight_grads(n, carry):
        at = pl.ds(pl.multiple_of(n * step, step), step)
        g_d[at, :] = mm(hid[at, :], d_b[...])
        g_g[at, :] = mm(d_gate[at, :], u_b[...])
        g_u[at, :] = mm(d_up[at, :], u_b[...])
        return carry

    lax.fori_loop(0, ff // step, weight_grads, 0)
    small[2 * hd:, :] = jnp.zeros_like(small[2 * hd:, :])
    small[2 * hd:2 * hd + 1, :] = g_in.reshape(1, width)
    small[2 * hd + 1:2 * hd + 2, :] = g_fin.reshape(1, width)
    norm = norm_ref[pl.ds(tp, 1), :]
    hits = jnp.sum(hits_ref[...], axis=0, keepdims=True)
    small[2 * hd + 2:2 * hd + 3, :] = (norm + LOGIT_ZLOSS * norm * norm - hits * scale) / tok_total
    copies = []

    def put(src, first, size, s):
        copies.append(pltpu.make_async_copy(src, rows_ref.at[s, pl.ds(first, size), :], out_sem.at[len(copies)]))

    n_kv = 2 * hd // shards
    for s in range(shards):
        at = 0
        for g, size in ((g_q, nq // shards), (g_o, nq // shards), (g_g, ff // shards), (g_u, ff // shards), (g_d, ff // shards)):
            put(g.at[pl.ds(s * size, size), :], at, size, s)
            at += size
        put(small.at[pl.ds(s * n_kv, n_kv), :], at, n_kv, s)
        put(small.at[pl.ds(2 * hd + (0 if s == 0 else 16), 16), :], at + n_kv, 16, s)
    for c in copies:
        c.start()
    for c in copies:
        c.wait()

    def relay(k):
        order = near_first(k)
        for c in order[1:]:
            back(dp, slot_of(*c))
            x_copy(slot_of(*c)).start()
            c_copy(dp, 0, slot_of(*c)).start()
        for c in order:
            back(facing, slot_of(*c))
            c_copy(facing, 1, slot_of(*c)).start()

    on_position(relay)
    for b in range(n_early):
        g_x_copy(b).wait_recv()
        add_into(early_ref.at[b], s_early.at[b], 24)
    for slot in range(shards):
        back(twin, slot)
        back(across, slot)
    for n, to in enumerate((twin, facing, across)):
        remote(ids_ref, ids_all.at[to], id_send.at[n], id_recv.at[to], tp, to).wait_recv()
        ids_copy(n, to).wait_send()
    for n in range(1, shards):
        row_copy(lax.rem(tp + n, shards)).wait_send()
    for slot in range(shards):
        x_copy(slot).wait_send()
        c_copy(dp, 0, slot).wait_send()
        c_copy(facing, 1, slot).wait_send()
    for b in range(n_early):
        g_chip_copy(b).wait_send()
        g_x_copy(b).wait_send()


def layer_bwd(scale, tok_total, d_fin, x0, x1, norms, hits, ln, cos_t, sin_t, weights, saved, code, g_table, ids, collective_id):
    own, width = x0.shape
    nq = weights[0].shape[0]
    two_hd = 2 * weights[1].shape[1]
    ff = weights[3].shape[0]
    rows = (2 * nq + 3 * ff + two_hd) // (2 * NZ) + 16
    chunk = (own, width)
    back = (2 * NZ, ids.shape[1] // (2 * NZ), width)
    blocks = (N_EARLY, table_block(g_table.shape[0]), width)
    dma = lambda *n: pltpu.SemaphoreType.DMA(n)
    return pl.pallas_call(
        functools.partial(layer_bwd_kernel, scale, tok_total),
        out_shape=(jax.ShapeDtypeStruct((2 * NZ, rows, width), F32), jax.ShapeDtypeStruct(chunk, F32), jax.ShapeDtypeStruct((4,) + back, F32),
                   jax.ShapeDtypeStruct(blocks, F32), jax.ShapeDtypeStruct((4,) + ids.shape, jnp.int32)),
        in_specs=[VMEM] * 11 + [ANY] * 3 + [VMEM] * 6 + [ANY, VMEM],
        out_specs=(ANY, VMEM, ANY, VMEM, VMEM),
        scratch_shapes=[pltpu.VMEM(chunk, F32), pltpu.VMEM(chunk, BF16), pltpu.VMEM(chunk, BF16), pltpu.VMEM((nq, own), BF16),
                        pltpu.VMEM((nq, own), BF16), pltpu.VMEM((2 * own, two_hd), F32), pltpu.VMEM((own, two_hd), F32)]
        + [pltpu.VMEM((ff, own), BF16)] * 3 + [pltpu.VMEM(back, F32), pltpu.VMEM((nq, width), F32), pltpu.VMEM((nq, width), F32)] + [pltpu.VMEM((ff, width), F32)] * 3
        + [pltpu.VMEM((two_hd + 32, width), F32), pltpu.VMEM(blocks, F32), pltpu.VMEM(blocks, F32)]
        + [pltpu.VMEM((ff, width), BF16)] * 3 + [dma(3), dma(14 * NZ + 1),
           pltpu.SemaphoreType.DMA, pltpu.SemaphoreType.DMA, dma(2 * NZ), dma(2 * NZ), dma(2, 2 * NZ), dma(4, 2 * NZ),
           dma(N_EARLY), dma(2, N_EARLY), dma(2, N_EARLY), dma(3), dma(4)],
        compiler_params=pltpu.CompilerParams(collective_id=collective_id, has_side_effects=True, vmem_limit_bytes=66000000),
        name="layer_bwd",
    )(d_fin, x0, x1, norms, hits, ln, cos_t, sin_t, *weights, *saved, code, g_table, ids)


N_BLOCK = 12
N_EARLY = 3
AHEAD = 11


def table_block(vocab):
    return -(-vocab // (2 * N_BLOCK * 24)) * 24


W_REDUCE = {
    0: {4: (3,), 6: (2,), 8: (1,), 9: (0,)},
    1: {6: (3,), 8: (2, 0), 9: (1,)},
    2: {6: (0,), 8: (1, 3), 9: (2,)},
    3: {4: (0,), 6: (1,), 8: (2,), 9: (3,)},
}


def tail_kernel(g_ref, p_ref, rows_ref, ids_ref, early_ref, t_ref, w_out, small_ref,
                s_buf, from_c, from_x, look_in, parts, acc, w_c, w_y, w_l, w_r, w_x,
                g_load, g_send_c, g_recv_c, g_send_x, g_recv_x, g_send_t, g_recv_t, g_store, l_sem,
                w_load, w_out_sem, send_c, send_y, send_l, send_r, recv_c, recv_y, recv_l, recv_r, last_send, last_recv, small_send, small_recv):
    tp, dp, z, y = place()
    partner = tp + 1 - 2 * y
    core = dp % 2
    twin = dp + 1 - 2 * core
    facing = lax.rem(dp + 2, 4)
    half = g_ref.shape[0] // 2
    size = s_buf.shape[1]
    last = half - (N_BLOCK - 1) * size
    n_look = rows_ref.shape[1]

    def rows(which, b, n):
        return pl.ds(pl.multiple_of(which * half + b * size, 8), n)

    def part(buf, b, n):
        return buf.at[b - N_EARLY if buf is not from_x else b, pl.ds(0, n), :]

    plane_barrier(tp, dp, [(tp, twin), (tp, facing)])

    chip = dp // 2
    groups = (2 * chip, 2 * chip + 1, 2 - 2 * chip, 3 - 2 * chip)

    def look_load(n):
        return pltpu.make_async_copy(rows_ref.at[groups[n]], look_in.at[n % 2], l_sem.at[n % 2])

    def early_load(b):
        return pltpu.make_async_copy(early_ref.at[b], from_x.at[b], g_load.at[b])

    for n in range(2):
        look_load(n).start()

    def c_copy(b, n):
        return remote(g_ref.at[rows(1 - core, b, n), :], part(from_c, b, n), g_send_c.at[b], g_recv_c.at[b], tp, twin)

    def own_load(b, n):
        return pltpu.make_async_copy(g_ref.at[rows(core, b, n), :], part(s_buf, b, n), g_load.at[b])

    def x_copy(b, n):
        return remote(part(s_buf, b, n), part(from_x, b, n), g_send_x.at[b], g_recv_x.at[b], tp, facing)

    def t_copy(b, n):
        return remote(part(from_x, b, n), t_ref.at[rows(core, b, n), :], g_send_t.at[b], g_recv_t.at[b], tp, twin)

    def t_store(b, n):
        return pltpu.make_async_copy(part(from_x, b, n), t_ref.at[rows(core, b, n), :], g_store.at[b])

    def every(f, first, end):
        def body(b, carry):
            f(b, size)
            return carry
        lax.fori_loop(first, min(end, N_BLOCK - 1), body, 0)
        if end == N_BLOCK:
            f(N_BLOCK - 1, last)

    def looked_up(b, n, first, count):
        ids = jnp.concatenate([ids_ref[first + g] for g in range(count)], axis=1) - (core * half + b * size)
        hit = (lax.broadcasted_iota(jnp.int32, (n, count * n_look), 0) == ids).astype(F32).astype(BF16)
        span = pl.ds(pl.multiple_of(first * n_look, n_look), count * n_look)
        return mm(hit, parts[0, span, :]) + mm(hit, parts[1, span, :]) + mm(hit, parts[2, span, :])

    def chip_sum(b, n):
        own_load(b, n).wait()
        c_copy(b, n).wait_recv()
        at = b - N_EARLY
        s_buf[at, 0:n, :] = s_buf[at, 0:n, :] + from_c[at, 0:n, :] + looked_up(b, n, 2 * chip, 2)
        x_copy(b, n).start()

    def early_sum(b, n):
        early_load(b).wait()
        from_x[b] = from_x[b] + looked_up(b, n, 0, 4)
        t_copy(b, n).start()
        t_store(b, n).start()

    def w_first(k):
        for zz in REDUCE_ORDER[k]:
            for slot in (2 * zz + 1 - y, 2 * zz + y):
                remote(p_ref.at[slot, 1 - core], w_c.at[slot], send_c.at[slot], recv_c.at[slot], tp, twin).start()
                pltpu.make_async_copy(p_ref.at[slot, core], acc.at[slot], w_load.at[slot]).start()

    def w_chip_sum(slot):
        pltpu.make_async_copy(p_ref.at[slot, core], acc.at[slot], w_load.at[slot]).wait()
        remote(acc.at[slot], w_c.at[slot], send_c.at[slot], recv_c.at[slot], tp, twin).wait_recv()
        add_into(acc.at[slot], w_c.at[slot])

    def w_second(k):
        for zz in REDUCE_ORDER[k]:
            slot = 2 * zz + 1 - y
            w_chip_sum(slot)
            remote(acc.at[slot], w_y.at[zz], send_y.at[zz], recv_y.at[zz], partner, dp).start()
        for zz in REDUCE_ORDER[k]:
            w_chip_sum(2 * zz + y)

    def w_reduce(k, shards):
        for zz in shards:
            line = acc.at[2 * zz + y]
            remote(line, w_y.at[zz], send_y.at[zz], recv_y.at[zz], partner, dp).wait_recv()
            add_into(line, w_y.at[zz])
            if zz >= k and k > 0:
                remote(line, w_l.at[zz - 1], send_l.at[zz], recv_l.at[zz], partner, dp).wait_recv()
                add_into(line, w_l.at[zz - 1])
            if zz <= k and k < NZ - 1:
                remote(line, w_r.at[zz], send_r.at[zz], recv_r.at[zz], partner, dp).wait_recv()
                add_into(line, w_r.at[zz])
            if zz > k:
                remote(line, w_l.at[zz - 1], send_r.at[zz], recv_l.at[zz], tp + 2, dp).start()
            if zz < k:
                remote(line, w_r.at[zz], send_l.at[zz], recv_r.at[zz], tp - 2, dp).start()

    def on_position(f):
        for k in range(NZ):
            pl.when(z == k)(functools.partial(f, k))

    def first(b, n):
        c_copy(b, n).start()
        own_load(b, n).start()

    every(first, N_EARLY, N_EARLY + 2)
    on_position(w_first)
    every(first, N_EARLY + 2, N_BLOCK)
    for b in range(N_EARLY):
        early_load(b).start()

    def split(n):
        look_load(n).wait()
        value = look_in[n % 2]
        high = value.astype(BF16)
        left = value - high.astype(F32)
        middle = left.astype(BF16)
        at = pl.ds(pl.multiple_of(groups[n] * n_look, n_look), n_look)
        parts[0, at, :] = high
        parts[1, at, :] = middle
        parts[2, at, :] = (left - middle.astype(F32)).astype(BF16)
        if n + 2 < 4:
            look_load(n + 2).start()

    split(0)
    split(1)
    every(chip_sum, N_EARLY, N_EARLY + 3)
    on_position(w_second)
    every(chip_sum, N_EARLY + 3, AHEAD)
    split(2)
    split(3)
    every(early_sum, 0, N_EARLY)

    total = acc.at[tp]
    w_copy_x = remote(total, w_x, last_send.at[0], last_recv.at[0], tp, facing)
    w_copy_c = remote(total, w_out.at[core], last_send.at[1], last_recv.at[1], tp, twin)
    w_store = pltpu.make_async_copy(total, w_out.at[core], w_out_sem)
    n_small, n_rows = small_ref.shape[1], w_out.shape[1]
    mine = w_out.at[1, pl.ds(n_rows - 32, n_small), :]
    small_here = pltpu.make_async_copy(mine, small_ref.at[tp], w_out_sem)
    peers = [lax.rem(tp + n, 2 * NZ) for n in range(1, 2 * NZ)]
    for b in range(N_EARLY, N_BLOCK):
        n = last if b == N_BLOCK - 1 else size
        if b == N_BLOCK - 1:
            w_copy_x.wait()
            add_into(total, w_x)
            w_copy_c.start()
            w_store.start()
            w_copy_c.wait_send()
            remote(total, w_out.at[1 - core], last_send.at[1], last_recv.at[1], tp, twin).wait_recv()
            w_store.wait()
            for to in peers:
                remote(mine, small_ref.at[tp], small_send.at[to], small_recv.at[tp], to, dp).start()
            small_here.start()
        x_copy(b, n).wait_recv()
        add_into(part(from_x, b, n), part(s_buf, b, n), 24)
        t_copy(b, n).start()
        t_store(b, n).start()
        for k in range(NZ):
            if b in W_REDUCE[k]:
                pl.when(z == k)(functools.partial(w_reduce, k, W_REDUCE[k][b]))
        if b == N_BLOCK - 3:
            w_copy_x.start()
            every(chip_sum, AHEAD, N_BLOCK)
    for source in peers:
        remote(small_ref.at[source], small_ref.at[source], small_send.at[source], small_recv.at[source], source, dp).wait_recv()
        remote(mine, small_ref.at[tp], small_send.at[source], small_recv.at[tp], source, dp).wait_send()
    small_here.wait()

    def w_done(k):
        for zz in range(NZ):
            line = acc.at[2 * zz + y]
            for slot in (2 * zz + 1 - y, 2 * zz + y):
                remote(p_ref.at[slot, 1 - core], w_c.at[slot], send_c.at[slot], recv_c.at[slot], tp, twin).wait_send()
            remote(line, w_y.at[zz], send_y.at[zz], recv_y.at[zz], partner, dp).wait_send()
            if zz > k:
                remote(line, w_l.at[zz - 1], send_r.at[zz], recv_l.at[zz], tp + 2, dp).wait_send()
            if zz < k:
                remote(line, w_r.at[zz], send_l.at[zz], recv_r.at[zz], tp - 2, dp).wait_send()

    on_position(w_done)

    def drain(b, n):
        t_copy(b, n).wait_send()
        t_store(b, n).wait()
        remote(part(from_x, b, n), t_ref.at[rows(1 - core, b, n), :], g_send_t.at[b], g_recv_t.at[b], tp, twin).wait_recv()

    def sent(b, n):
        c_copy(b, n).wait_send()
        x_copy(b, n).wait_send()

    every(drain, 0, N_BLOCK)
    every(sent, N_EARLY, N_BLOCK)


def tail(g_table, g_rows, look_rows, look_ids, early, collective_id):
    vocab, width = g_table.shape
    rows = g_rows.shape[1]
    half = (rows // 2, width)
    n_look = look_ids.shape[2]
    size = table_block(vocab)
    blocks = lambda n: pltpu.VMEM((n, size, width), F32)
    dma = lambda *n: pltpu.SemaphoreType.DMA(n)
    t, w_sum, small = pl.pallas_call(
        tail_kernel,
        out_shape=(jax.ShapeDtypeStruct((vocab, width), F32), jax.ShapeDtypeStruct((2,) + half, F32), jax.ShapeDtypeStruct((2 * NZ, 24, width), F32)),
        in_specs=[ANY, ANY, ANY, VMEM, ANY],
        out_specs=(ANY,) * 3,
        scratch_shapes=[blocks(N_BLOCK - N_EARLY)] * 2 + [blocks(N_BLOCK), pltpu.VMEM((2, n_look, width), F32), pltpu.VMEM((3, 4 * n_look, width), BF16)]
        + [pltpu.VMEM((2 * NZ,) + half, F32)] * 2 + [pltpu.VMEM((NZ,) + half, F32)] + [pltpu.VMEM((NZ - 1,) + half, F32)] * 2
        + [pltpu.VMEM(half, F32)]
        + [dma(N_BLOCK)] * 8 + [dma(2)]
        + [dma(2 * NZ), pltpu.SemaphoreType.DMA] + [dma(2 * NZ), dma(NZ), dma(NZ), dma(NZ)] * 2 + [dma(2)] * 2 + [dma(2 * NZ)] * 2,
        compiler_params=pltpu.CompilerParams(collective_id=collective_id, has_side_effects=True, vmem_limit_bytes=67000000),
        name="tail",
    )(g_table, g_rows.reshape((2 * NZ, 2) + half), look_rows.reshape(4, n_look, width), look_ids, early)
    return t, w_sum.reshape(rows, width), small


UPDATE_ROWS = 512


def update_kernel(t_ref, w_any, small_any, *refs):
    state = [refs[7 * i:7 * i + 7] for i in range(3)]
    new = [refs[21 + 7 * i:28 + 7 * i] for i in range(3)]
    loss_ref, held, made, w_ref, small_ref = refs[42:47]
    old_small = [refs[47 + 6 * i:53 + 6 * i] for i in range(3)]
    new_small = [refs[65 + 6 * i:71 + 6 * i] for i in range(3)]
    in_sem, out_sem, g_sem, small_in, small_out = refs[83:]
    vocab = t_ref.shape[0]
    blocks = [(at, min(UPDATE_ROWS, vocab - at)) for at in range(0, vocab, UPDATE_ROWS)]

    def loads(q):
        at, n = blocks[q]
        return [pltpu.make_async_copy(ref.at[pl.ds(at, n), :], held.at[q % 4, i, pl.ds(0, n), :], in_sem.at[q % 4, i])
                for i, ref in enumerate((t_ref, state[0][0], state[1][0], state[2][0]))]

    def stores(q):
        at, n = blocks[q]
        return [pltpu.make_async_copy(made.at[q % 3, i, pl.ds(0, n), :], new[i][0].at[pl.ds(at, n), :], out_sem.at[q % 3, i]) for i in range(3)]

    for q in range(4):
        for c in loads(q):
            c.start()
    grads = [pltpu.make_async_copy(w_any, w_ref, g_sem.at[0]), pltpu.make_async_copy(small_any, small_ref, g_sem.at[1])]
    pairs = [(i, j) for i in range(3) for j in range(6)]
    small_loads = grads + [pltpu.make_async_copy(state[i][j + 1], old_small[i][j], small_in.at[i, j]) for i, j in pairs]
    small_stores = [pltpu.make_async_copy(new_small[i][j], new[i][j + 1], small_out.at[i, j]) for i, j in pairs]
    for c in small_loads:
        c.start()

    def small_update(index, grad, *where):
        got = adam_update(old_small[0][index - 1][where], grad, old_small[1][index - 1][where], old_small[2][index - 1][where])
        for i in range(3):
            new_small[i][index - 1][where] = got[i]

    def small_updates():
        hd = old_small[0][2].shape[1]
        n_kv = 2 * hd // small_ref.shape[0]
        n_q, n_f = old_small[0][1].shape[0], old_small[0][5].shape[0]
        small_update(1, small_ref[0, n_kv:n_kv + 2, :], Ellipsis)
        small_update(2, w_ref[0:n_q, :], Ellipsis)
        kv = small_ref[:, 0:n_kv, :].reshape(2 * hd, small_ref.shape[2])
        for i in range(2):
            small_update(3, kv[i * hd:(i + 1) * hd], i)
        small_update(4, w_ref[n_q:2 * n_q, :], Ellipsis)
        for i in range(2):
            small_update(5, w_ref[2 * n_q + i * n_f:2 * n_q + (i + 1) * n_f, :].T, i)
        small_update(6, w_ref[2 * n_q + 2 * n_f:2 * n_q + 3 * n_f, :], Ellipsis)
        loss_ref[...] = jnp.sum(small_ref[0, n_kv + 2:n_kv + 3, :], axis=1, keepdims=True)

    for q, (at, n) in enumerate(blocks):
        for c in loads(q):
            c.wait()
        if q >= 3:
            for c in stores(q - 3):
                c.wait()
        step = 32 if n % 32 == 0 else 16

        def body(j, carry):
            rows = pl.ds(pl.multiple_of(j * step, step), step)
            got = adam_update(held[q % 4, 1, rows, :], held[q % 4, 0, rows, :], held[q % 4, 2, rows, :], held[q % 4, 3, rows, :])
            for i in range(3):
                made[q % 3, i, rows, :] = got[i]
            return carry

        lax.fori_loop(0, n // step, body, 0)
        for c in stores(q):
            c.start()
        if q + 4 < len(blocks):
            for c in loads(q + 4):
                c.start()
        if q == min(3, len(blocks) - 1):
            for c in small_loads:
                c.wait()
            small_updates()
            for c in small_stores:
                c.start()
    for q in range(len(blocks) - 3, len(blocks)):
        for c in stores(q):
            c.wait()
    for c in small_stores:
        c.wait()


def update(g_table, g_shard, g_small, state_arrays):
    width = g_table.shape[1]
    dma = lambda *n: pltpu.SemaphoreType.DMA(n)

    def flip(arrays):
        return [a.swapaxes(-1, -2) if i % 7 in (2, 3) else a for i, a in enumerate(arrays)]

    given = flip(state_arrays)
    small = [pltpu.VMEM(a.shape, F32) for i, a in enumerate(given) if i % 7]
    *new, loss = pl.pallas_call(
        update_kernel,
        out_shape=tuple(jax.ShapeDtypeStruct(a.shape, F32) for a in given) + (jax.ShapeDtypeStruct((1, 1), F32),),
        in_specs=[ANY] * 24,
        out_specs=(ANY,) * 21 + (VMEM,),
        scratch_shapes=[pltpu.VMEM((4, 4, UPDATE_ROWS, width), F32), pltpu.VMEM((3, 3, UPDATE_ROWS, width), F32),
                        pltpu.VMEM(g_shard.shape, F32), pltpu.VMEM(g_small.shape, F32)] + small * 2
        + [dma(4, 4), dma(3, 3), dma(2), dma(3, 6), dma(3, 6)],
        compiler_params=pltpu.CompilerParams(vmem_limit_bytes=60000000),
        name="update",
    )(g_table, g_shard, g_small, *given)
    return flip(new) + [loss]


def norm_fwd(x_f32, scale):
    centered = x_f32 - jnp.mean(x_f32, axis=-1, keepdims=True)
    inv_std = lax.rsqrt(jnp.mean(centered * centered, axis=-1, keepdims=True) + LN_EPS)
    x_hat = centered * inv_std
    return (x_hat * scale).astype(BF16), x_hat, inv_std


def norm_bwd(d_out, x_hat, inv_std, scale):
    d_scale = jnp.sum(d_out * x_hat, axis=0)
    d_hat = d_out * scale
    d_in = inv_std * (d_hat - jnp.mean(d_hat, axis=-1, keepdims=True) - x_hat * jnp.mean(d_hat * x_hat, axis=-1, keepdims=True))
    return d_in, d_scale


def adam_update(param_in, grad_in, mom_in, vel_in):
    mom_new = BETA_ONE * mom_in + (1.0 - BETA_ONE) * grad_in
    vel_new = BETA_TWO * vel_in + (1.0 - BETA_TWO) * grad_in * grad_in
    return param_in - LEARN_RATE * mom_new / (jnp.sqrt(vel_new) + ADAM_EPS), mom_new, vel_new


def dot(spec, a, b):
    return jnp.einsum(spec, a, b, preferred_element_type=F32)


def solution(mesh):
    param_specs = (P('tp', None), P(None, None), P(None, 'tp'), P(None, None, None), P('tp', None), P(None, None, 'tp'), P('tp', None))
    n_tp = mesh.shape['tp']
    n_dp = mesh.shape['dp']

    def local_step(tokens, labels, *state_arrays):
        embed, ln_scales, w_q, w_kv, w_o, w_gu, w_down = state_arrays[0:7]
        batch_loc, seq_len = tokens.shape
        vocab_loc, d_model = embed.shape
        head_dim = w_kv.shape[2]
        q_loc = w_q.shape[1]
        f_loc = w_down.shape[0]
        tok_loc = batch_loc * seq_len
        tok_total = tok_loc * n_dp
        own = tok_loc // n_tp
        tp_rank = lax.axis_index('tp')
        half = tp_rank % 2

        strict = (jnp.arange(own)[:, None] > jnp.arange(own)[None, :]).astype(BF16)

        def routing(chunks):
            shard = chunks // vocab_loc
            row = chunks - shard * vocab_loc
            hot = (shard[:, :, None] == jnp.arange(n_tp)[None, None, :])
            before = dot('rs,nsj->nrj', strict, hot.astype(BF16))
            rank = jnp.sum(jnp.where(hot, before, 0.0), axis=-1).astype(jnp.int32)
            most = jnp.max(jnp.sum(hot.astype(jnp.int32), axis=1))
            return shard, row, rank, (most + CAP - 1) // CAP

        chunks = tokens.reshape(n_tp, own)
        shard, row, rank, rounds = routing(chunks)
        slots = jnp.arange(CAP)
        my_shard = lax.dynamic_index_in_dim(shard, tp_rank, 0, keepdims=False)
        my_rank = lax.dynamic_index_in_dim(rank, tp_rank, 0, keepdims=False)

        def fetch(step):
            here = (shard[:, None, :] == tp_rank) & (rank[:, None, :] == slots[None, :, None] + step * CAP)
            ids = jnp.sum(jnp.where(here, row[:, None, :], 0), axis=-1).reshape(-1)
            place = my_rank - step * CAP
            return ids, jnp.where((place >= 0) & (place < CAP), my_shard * CAP + place, -1)

        def fetch_more(state):
            ids, code = fetch(state[0])
            pick = (code[:, None] == jnp.arange(n_tp * CAP)[None, :]).astype(BF16)
            rows_in = plane_swap(jnp.take(embed, ids, axis=0).reshape(n_tp, CAP, d_model), 1).reshape(n_tp * CAP, d_model).astype(BF16)
            return state[0] + 1, state[1] + dot('rc,cd->rd', pick, rows_in)

        more_rows = lax.while_loop(lambda state: state[0] < rounds, fetch_more, (jnp.int32(1), jnp.zeros((own, d_model), F32)))[1]
        ids_first, code_first = fetch(0)
        code_first = code_first[None, :]

        w_rows = jnp.concatenate([w_q.T, w_o, w_gu.transpose(0, 2, 1).reshape(2 * f_loc, d_model), w_down], axis=0)
        cuts = (q_loc, 2 * q_loc, 2 * q_loc + f_loc, 2 * q_loc + 2 * f_loc)
        wkv_t = w_kv.transpose(0, 2, 1)
        inv_freq = ROPE_BASE ** (-jnp.arange(0, head_dim, 2).astype(F32) / head_dim)
        angles = inv_freq[:, None] * (half * own + jnp.arange(own)).astype(F32)[None, :]
        cos_t, sin_t = jnp.cos(angles), jnp.sin(angles)
        f_own, x_one, x_zero, *saved = front(ids_first, embed, jnp.broadcast_to(rounds, (1, 128)), code_first, more_rows, w_rows, wkv_t, ln_scales, cos_t, sin_t, n_tp * q_loc, 0)
        saved, (wq_t, wo_b, wg_t, wu_t, wd_b), rounds_all = saved[:5], saved[5:10], jnp.max(saved[10])
        weights = (wq_t, wkv_t, wo_b, wg_t, wu_t, wd_b)

        logit_scale = d_model ** -0.5
        d_fin, g_head_part, log_norm, lab_sum, _ = head(f_own, labels, embed, logit_scale, logit_scale / tok_total, 4)

        def row_ids(step):
            here = (shard[:, None, :] == tp_rank) & (rank[:, None, :] == slots[None, :, None] + step * CAP)
            return jnp.where(jnp.any(here, axis=-1), jnp.sum(jnp.where(here, row[:, None, :], 0), axis=-1), vocab_loc).reshape(-1)

        g_rows, d_zero, rows_back, early, ids_back = layer_bwd(logit_scale, tok_total, d_fin, x_zero, x_one, log_norm, lab_sum, ln_scales, cos_t, sin_t, weights, saved,
                                                               code_first, g_head_part, row_ids(0)[None, :], 7)
        g_table, g_shard, g_small = tail(g_head_part, g_rows, rows_back, ids_back, early, 10)

        def give_back(state):
            mine = (my_shard[None, None, :] == jnp.arange(n_tp)[:, None, None]) & (my_rank[None, None, :] == slots[None, :, None] + state[0] * CAP)
            ids = jnp.sum(jnp.where(mine, jnp.arange(own)[None, None, :], 0), axis=-1).reshape(-1)
            rows_in = plane_swap(jnp.take(d_zero, ids, axis=0).reshape(n_tp, CAP, d_model), 9).reshape(-1, d_model)
            n_rows = n_tp * CAP
            id_rows = jnp.pad(row_ids(state[0]).astype(F32), (0, -n_rows % (8 * d_model))).reshape(-1, d_model)
            both = group_gather(jnp.concatenate([rows_in, id_rows], axis=0), 11)
            ids = both[:, n_rows:].reshape(n_dp, -1)[:, :n_rows].astype(jnp.int32)
            return state[0] + 1, state[1].at[ids.reshape(-1)].add(both[:, :n_rows].reshape(-1, d_model), mode='drop')

        g_table = lax.while_loop(lambda state: state[0] < rounds_all, give_back, (jnp.int32(1), g_table))[1]
        *new, loss = update(g_table, g_shard, g_small, state_arrays)
        return tuple(new) + (loss.reshape(()),)

    return jax.shard_map(local_step, mesh=mesh, in_specs=(P('dp', None), P('dp', None)) + param_specs * 3,
                         out_specs=param_specs * 3 + (P(),), check_vma=False)
```
